32 devices in a mesh: cp: 32 (over z, y, x, core).
Axes of the slice: x: 2, y: 2, z: 4, core: 2. Of those that a mesh axis runs over, the one named last changes fastest.
Arguments:
- hidden: bfloat16 [4, 4096, 2048], P(None, 'cp')
- grad_out: bfloat16 [4, 4096, 2048], P(None, 'cp')
- positions: int32 [4, 4096], P(None, 'cp')
- seg_ids: int32 [4, 4096], P(None, 'cp')
- w_q: bfloat16 [2048, 2048], replicated
- w_k: bfloat16 [2048, 256], replicated
- w_v: bfloat16 [2048, 256], replicated
- w_o: bfloat16 [2048, 2048], replicated
- norm_gain: bfloat16 [2048], replicated
Outputs:
- output 1: bfloat16 [4, 4096, 2048], P(None, 'cp')
- output 2: bfloat16 [4, 4096, 2048], P(None, 'cp')
- output 3: float32 [2048, 2048], replicated
- output 4: float32 [2048, 256], replicated
- output 5: float32 [2048, 256], replicated
- output 6: float32 [2048, 2048], replicated
- output 7: float32 [2048], replicated
All inputs are finite; a program needn't handle non-finite values.
Results may differ from the reference program's by a relative error of at most 0.0143505.
Values are sent between devices in bfloat16 or wider.
A program may use at most 1 GiB of HBM per device.

```python
import jax
import jax.numpy as jnp
from jax import lax

BATCH = 4
CHUNK = 64
CP_SIZE = 32
D_MODEL = 2048
HEADS = 16
KV_HEADS = 2
HEAD_DIM = 128
NUM_CUTS = 12

SEQ_LEN = 2 * CP_SIZE * CHUNK
GROUP_SIZE = HEADS // KV_HEADS
NORM_EPS = 1e-5
ROPE_BASE = 500000.0
ATTN_SCALE = HEAD_DIM ** -0.5
NEG_BIG = -1e30


def storage_order(glob_rows):
    blocks = glob_rows.reshape(BATCH, 2 * CP_SIZE, CHUNK)
    front_half = blocks[:, :CP_SIZE]
    back_half = blocks[:, CP_SIZE:][:, ::-1]
    return jnp.stack([front_half, back_half], axis=2).reshape(BATCH, SEQ_LEN)


def draw_layout(layout_key):
    key_start, key_len, key_cut = jax.random.split(layout_key, 3)
    long_start = jax.random.randint(key_start, (BATCH, 1), 0, SEQ_LEN // 4 + 1)
    long_end = long_start + SEQ_LEN // 2 + jax.random.randint(key_len, (BATCH, 1), 0, SEQ_LEN // 4 + 1)
    cut_points = jax.random.randint(key_cut, (BATCH, NUM_CUTS), 1, SEQ_LEN)
    keep_cut = (cut_points <= long_start) | (cut_points >= long_end)
    bounds = jnp.concatenate([jnp.where(keep_cut, cut_points, 0), long_start, long_end], axis=1)
    token_idx = jnp.arange(SEQ_LEN)
    passed = (bounds[:, :, None] <= token_idx[None, None, :]) & (bounds[:, :, None] > 0)
    seg_glob = jnp.sum(passed.astype(jnp.int32), axis=1)
    doc_start = jnp.max(jnp.where(passed, bounds[:, :, None], 0), axis=1)
    pos_glob = token_idx[None, :] - doc_start
    return storage_order(pos_glob.astype(jnp.int32)), storage_order(seg_glob.astype(jnp.int32))


def setup_inputs(seed: int = 0) -> dict:
    root_key = jax.random.key(seed)
    key_list = jax.random.split(root_key, 9)
    positions, seg_ids = draw_layout(key_list[0])
    hidden = jax.random.normal(key_list[1], (BATCH, SEQ_LEN, D_MODEL), jnp.float32)
    grad_out = jax.random.normal(key_list[2], (BATCH, SEQ_LEN, D_MODEL), jnp.float32)
    w_q = jax.random.normal(key_list[3], (D_MODEL, HEADS * HEAD_DIM), jnp.float32) * D_MODEL ** -0.5
    w_k = jax.random.normal(key_list[4], (D_MODEL, KV_HEADS * HEAD_DIM), jnp.float32) * D_MODEL ** -0.5
    w_v = jax.random.normal(key_list[5], (D_MODEL, KV_HEADS * HEAD_DIM), jnp.float32) * D_MODEL ** -0.5
    w_o = jax.random.normal(key_list[6], (HEADS * HEAD_DIM, D_MODEL), jnp.float32) * (HEADS * HEAD_DIM) ** -0.5
    norm_gain = jax.random.uniform(key_list[7], (D_MODEL,), jnp.float32, 0.5, 1.5)
    return {
        'hidden': hidden.astype(jnp.bfloat16),
        'grad_out': grad_out.astype(jnp.bfloat16),
        'positions': positions,
        'seg_ids': seg_ids,
        'w_q': w_q.astype(jnp.bfloat16),
        'w_k': w_k.astype(jnp.bfloat16),
        'w_v': w_v.astype(jnp.bfloat16),
        'w_o': w_o.astype(jnp.bfloat16),
        'norm_gain': norm_gain.astype(jnp.bfloat16),
    }


def global_index():
    chunk_slots = jnp.arange(2 * CP_SIZE)
    owner_rank = chunk_slots // 2
    glob_chunk = jnp.where(chunk_slots % 2 == 0, owner_rank, 2 * CP_SIZE - 1 - owner_rank)
    return (glob_chunk[:, None] * CHUNK + jnp.arange(CHUNK)[None, :]).reshape(SEQ_LEN)


def rms_norm(hidden_f32, gain_f32):
    inv_rms = lax.rsqrt(jnp.mean(hidden_f32 * hidden_f32, axis=-1, keepdims=True) + NORM_EPS)
    return (hidden_f32 * inv_rms * gain_f32).astype(jnp.bfloat16)


def rope_tables(positions):
    inv_freq = ROPE_BASE ** (-jnp.arange(0, HEAD_DIM, 2).astype(jnp.float32) / HEAD_DIM)
    angles = positions.astype(jnp.float32)[..., None] * inv_freq
    angles = jnp.concatenate([angles, angles], axis=-1)
    return jnp.cos(angles), jnp.sin(angles)


def rotate(proj_in, cos_t, sin_t):
    half_dim = proj_in.shape[-1] // 2
    turned = jnp.concatenate([-proj_in[..., half_dim:], proj_in[..., :half_dim]], axis=-1)
    return proj_in * cos_t + turned * sin_t


def attention(queries, keys_all, values_all, seg_ids):
    glob_all = global_index()
    n_blocks = 2 * CP_SIZE * KV_HEADS
    q_blocks = queries.reshape(BATCH, 2 * CP_SIZE, CHUNK, KV_HEADS, GROUP_SIZE, HEAD_DIM).transpose(1, 3, 0, 2, 4, 5).reshape(n_blocks, BATCH, CHUNK, GROUP_SIZE, HEAD_DIM)
    glob_blocks = jnp.repeat(glob_all.reshape(2 * CP_SIZE, CHUNK), KV_HEADS, axis=0)
    seg_blocks = jnp.repeat(seg_ids.reshape(BATCH, 2 * CP_SIZE, CHUNK).transpose(1, 0, 2), KV_HEADS, axis=0)
    head_ids = jnp.tile(jnp.arange(KV_HEADS), 2 * CP_SIZE)
    keys_t = jnp.moveaxis(keys_all, 2, 0)
    values_t = jnp.moveaxis(values_all, 2, 0)

    def block_attend(operands):
        q_blk, glob_q, seg_q, head_id = operands
        scores = jnp.einsum('bqgd,bsd->bgqs', q_blk, keys_t[head_id]) * ATTN_SCALE
        allowed = (seg_q[:, :, None] == seg_ids[:, None, :]) & (glob_q[:, None] >= glob_all[None, :])[None]
        attn_probs = jax.nn.softmax(jnp.where(allowed[:, None], scores, NEG_BIG), axis=-1)
        attn_probs = attn_probs.astype(jnp.bfloat16).astype(jnp.float32)
        return jnp.einsum('bgqs,bsd->bqgd', attn_probs, values_t[head_id])

    out_blocks = lax.map(jax.checkpoint(block_attend), (q_blocks, glob_blocks, seg_blocks, head_ids))
    attn_out = out_blocks.reshape(2 * CP_SIZE, KV_HEADS, BATCH, CHUNK, GROUP_SIZE, HEAD_DIM).transpose(2, 0, 3, 1, 4, 5)
    return attn_out.reshape(BATCH * SEQ_LEN, HEADS * HEAD_DIM).astype(jnp.bfloat16).astype(jnp.float32)


def forward(hidden, positions, seg_ids, wq_f32, wk_f32, wv_f32, wo_f32, gain_f32):
    hidden_f32 = hidden.astype(jnp.float32)
    normed = rms_norm(hidden_f32, gain_f32).astype(jnp.float32).reshape(BATCH * SEQ_LEN, D_MODEL)
    cos_t, sin_t = rope_tables(positions)
    q_lin = jnp.dot(normed, wq_f32, preferred_element_type=jnp.float32).reshape(BATCH, SEQ_LEN, KV_HEADS, GROUP_SIZE, HEAD_DIM)
    queries = rotate(q_lin, cos_t[:, :, None, None], sin_t[:, :, None, None]).astype(jnp.bfloat16).astype(jnp.float32)
    k_lin = jnp.dot(normed, wk_f32, preferred_element_type=jnp.float32).reshape(BATCH, SEQ_LEN, KV_HEADS, HEAD_DIM)
    keys_all = rotate(k_lin, cos_t[:, :, None], sin_t[:, :, None]).astype(jnp.bfloat16).astype(jnp.float32)
    values_all = jnp.dot(normed, wv_f32, preferred_element_type=jnp.float32).astype(jnp.bfloat16).astype(jnp.float32).reshape(BATCH, SEQ_LEN, KV_HEADS, HEAD_DIM)
    attn_flat = attention(queries, keys_all, values_all, seg_ids)
    proj_out = jnp.dot(attn_flat, wo_f32, preferred_element_type=jnp.float32).reshape(BATCH, SEQ_LEN, D_MODEL)
    return (hidden_f32 + proj_out).astype(jnp.bfloat16)


def reference(hidden, grad_out, positions, seg_ids, w_q, w_k, w_v, w_o, norm_gain):
    def run_block(hidden_in, wq_f32, wk_f32, wv_f32, wo_f32, gain_f32):
        return forward(hidden_in, positions, seg_ids, wq_f32, wk_f32, wv_f32, wo_f32, gain_f32)

    block_out, pullback = jax.vjp(run_block, hidden, w_q.astype(jnp.float32), w_k.astype(jnp.float32), w_v.astype(jnp.float32), w_o.astype(jnp.float32), norm_gain.astype(jnp.float32))
    grad_hidden, grad_wq, grad_wk, grad_wv, grad_wo, grad_gain = pullback(grad_out)
    return block_out, grad_hidden, grad_wq, grad_wk, grad_wv, grad_wo, grad_gain
```

```python
import functools

import jax
import jax.numpy as jnp
from jax import lax
from jax.experimental import pallas as pl
from jax.experimental.pallas import tpu as pltpu
from jax.sharding import PartitionSpec as P

HEAD_DIM = 128
NORM_EPS = 1e-5
ROPE_BASE = 500000.0
NEG_BIG = -1e30
LOG2E = 1.4426950408889634
ATTN_SCALE = HEAD_DIM**-0.5
EXP2_SCALE = ATTN_SCALE * LOG2E
BLK = 256
N_HEADS = 8
N_PAIRS = 8
N_SUPER = 2 * N_PAIRS
SLOTS = 14
MESH = pl.DeviceIdType.MESH
F32 = jnp.float32
BF16 = jnp.bfloat16

T_SQ, T_LO, T_MX = 16, 18, 22


def rope_tables(positions):
    inv_freq = ROPE_BASE ** (-jnp.arange(0, HEAD_DIM, 2).astype(F32) / HEAD_DIM)
    angles = positions.astype(F32)[..., None] * inv_freq
    return jnp.cos(angles), jnp.sin(angles)


def rotate(x, cos_t, sin_t):
    a, b = x[..., : HEAD_DIM // 2], x[..., HEAD_DIM // 2 :]
    return jnp.concatenate([a * cos_t - b * sin_t, b * cos_t + a * sin_t], axis=-1)


def dot(a, b, ca, cb):
    return lax.dot_general(a, b, ((ca, cb), ((), ())), preferred_element_type=F32)


def row_mean(x):
    return jnp.mean(x, axis=-1, keepdims=True)


def head(h):
    return pl.ds(h * HEAD_DIM, HEAD_DIM)


def dot_t(a, b):
    return dot(a, b, (1,), (1,))


def dyn(x, index, size, axis):
    return lax.dynamic_slice_in_dim(x, index, size, axis)


def pick(x, index, axis):
    return lax.dynamic_index_in_dim(x, index, axis, keepdims=False)


def fwd_kernel(tab, q_ref, kv_ref, st_ref, qi_ref, ko_ref, o_ref, lse_ref, acc, m_s, l_s):
    b, hf = pl.program_id(0), pl.program_id(1)
    sq, lo, mx = tab[T_SQ + hf], tab[T_LO + 2 * b + hf], tab[T_MX + 2 * b + hf]
    m_s[...] = jnp.full_like(m_s, NEG_BIG)
    l_s[...] = jnp.zeros_like(l_s)
    acc[...] = jnp.zeros_like(acc)

    def step(s, carry):
        slot, hk = tab[s], (s >= N_PAIRS).astype(jnp.int32)
        full = jnp.logical_and(s < sq, s * BLK >= mx)

        def run(masked):
            k = kv_ref[slot, 0, 0, hk]
            v_t = kv_ref[slot, 1, 0, hk].T
            if masked:
                ko = ko_ref[hk]
                mask = jnp.logical_and(ko >= st_ref[0, 0] - s * BLK, ko <= qi_ref[0, 0] - s * BLK)
            for h in range(N_HEADS):
                q = q_ref[0, 0, :, head(h)]
                sc = dot_t(k, q) * EXP2_SCALE
                if masked:
                    sc = jnp.where(mask, sc, NEG_BIG)
                m_old = m_s[h : h + 1, :]
                m_new = jnp.maximum(m_old, jnp.max(sc, axis=0, keepdims=True))
                alpha = jnp.exp2(m_old - m_new)
                p = jnp.exp2(sc - m_new)
                m_s[h : h + 1, :] = m_new
                l_s[h : h + 1, :] = l_s[h : h + 1, :] * alpha + jnp.sum(p, axis=0, keepdims=True)
                acc[h] = acc[h] * alpha + jnp.dot(v_t, p.astype(BF16), preferred_element_type=F32)

        pl.when(full)(lambda: run(False))
        pl.when(jnp.logical_not(full))(lambda: run(True))
        return carry

    lax.fori_loop(lo, sq + 1, step, 0)
    for h in range(N_HEADS):
        o_ref[0, 0, :, head(h)] = (acc[h] / l_s[h : h + 1, :]).T.astype(BF16)
    lse_ref[0, 0] = m_s[...] + jnp.log2(l_s[...])


def bwd_kernel(tab, q_ref, do_ref, kv_ref, lse_ref, dl_ref, st_ref, qi_ref, ko_ref, cos_ref, sin_ref, dq_ref, dkv_ref, dq_acc):
    b, hf = pl.program_id(0), pl.program_id(1)
    sq, lo, mx = tab[T_SQ + hf], tab[T_LO + 2 * b + hf], tab[T_MX + 2 * b + hf]
    dq_acc[...] = jnp.zeros_like(dq_acc)

    @pl.when(hf == 0)
    def _():
        dkv_ref[...] = jnp.zeros_like(dkv_ref)

    def step(s, carry):
        slot, hk = tab[s], (s >= N_PAIRS).astype(jnp.int32)
        pair = jnp.where(s >= N_PAIRS, N_SUPER - 1 - s, s)
        full = jnp.logical_and(s < sq, s * BLK >= mx)

        def run(masked):
            k = kv_ref[slot, 0, 0, hk]
            v = kv_ref[slot, 1, 0, hk]
            k_t = k.T
            if masked:
                ko = ko_ref[hk]
                mask = jnp.logical_and(ko >= st_ref[0, 0] - s * BLK, ko <= qi_ref[0, 0] - s * BLK)
            dk = dv = jnp.zeros((BLK, HEAD_DIM), F32)
            for h in range(N_HEADS):
                q = q_ref[0, 0, :, head(h)]
                do = do_ref[0, 0, :, head(h)]
                sc = dot_t(k, q)
                p = jnp.exp2(sc * EXP2_SCALE - lse_ref[0, 0, h : h + 1, :])
                if masked:
                    p = jnp.where(mask, p, 0.0)
                dp = dot_t(v, do)
                ds = (p * (dp - dl_ref[0, 0, h : h + 1, :])).astype(BF16)
                dv += jnp.dot(p.astype(BF16), do, preferred_element_type=F32)
                dk += jnp.dot(ds, q, preferred_element_type=F32)
                dq_acc[h] += jnp.dot(k_t, ds, preferred_element_type=F32)
            dkv_ref[pair, 0, 0, hk] += dk
            dkv_ref[pair, 1, 0, hk] += dv

        pl.when(full)(lambda: run(False))
        pl.when(jnp.logical_not(full))(lambda: run(True))
        return carry

    lax.fori_loop(lo, sq + 1, step, 0)
    cos_t, sin_t = cos_ref[0, 0], sin_ref[0, 0]
    half = HEAD_DIM // 2
    for h in range(N_HEADS):
        a, c = dq_acc[h, :half] * ATTN_SCALE, dq_acc[h, half:] * ATTN_SCALE
        lin = jnp.concatenate([a * cos_t + c * sin_t, c * cos_t - a * sin_t], axis=0)
        dq_ref[0, 0, :, head(h)] = lin.T.astype(BF16)


def attn_specs():
    def at_tile(b, h, t):
        return (b, h) + (0,) * 2

    def at_row(b, h, t):
        return (0, 0, b) + (0,) * 3

    tile = pl.BlockSpec((1, 1, BLK, N_HEADS * HEAD_DIM), at_tile)
    row = pl.BlockSpec((1, 1, 1, BLK), at_tile)
    stat = pl.BlockSpec((1, 1, N_HEADS, BLK), at_tile)
    rope = pl.BlockSpec((1, 1, HEAD_DIM // 2, BLK), at_tile)
    kv, dkv = (pl.BlockSpec((n, 2, 1, 2, BLK, HEAD_DIM), at_row) for n in (SLOTS, N_PAIRS))
    ko = pl.BlockSpec((2, BLK, BLK), lambda b, h, t: (0,) * 3)
    return tile, row, stat, kv, ko, rope, dkv


def flash_fwd(tab, q, kv, start, qidx, koff):
    tile, row, stat, kvs, ko, *_ = attn_specs()
    return pl.pallas_call(
        fwd_kernel,
        name="attn_fwd",
        out_shape=(jax.ShapeDtypeStruct(q.shape, BF16), jax.ShapeDtypeStruct((2, 2, N_HEADS, BLK), F32)),
        grid_spec=pltpu.PrefetchScalarGridSpec(
            num_scalar_prefetch=1,
            grid=(2, 2),
            in_specs=[tile, kvs, row, row, ko],
            out_specs=[tile, stat],
            scratch_shapes=[pltpu.VMEM((N_HEADS, HEAD_DIM, BLK), F32)] + [pltpu.VMEM((N_HEADS, BLK), F32)] * 2,
        ),
        compiler_params=pltpu.CompilerParams(vmem_limit_bytes=40 << 20),
        cost_estimate=pl.CostEstimate(flops=20 * 10**9, bytes_accessed=16 << 20, transcendentals=18 * 10**6),
    )(tab, q, kv, start, qidx, koff)


def flash_bwd(tab, q, do, kv, lse, delta, start, qidx, koff, cos_t, sin_t):
    tile, row, stat, kvs, ko, rope, dkv = attn_specs()
    return pl.pallas_call(
        bwd_kernel,
        name="attn_bwd",
        out_shape=(
            jax.ShapeDtypeStruct(q.shape, BF16),
            jax.ShapeDtypeStruct((N_PAIRS,) + kv.shape[1:], F32),
        ),
        grid_spec=pltpu.PrefetchScalarGridSpec(
            num_scalar_prefetch=1,
            grid=(2, 2),
            in_specs=[tile, tile, kvs, stat, stat, row, row, ko, rope, rope],
            out_specs=[tile, dkv],
            scratch_shapes=[pltpu.VMEM((N_HEADS, HEAD_DIM, BLK), F32)],
        ),
        compiler_params=pltpu.CompilerParams(vmem_limit_bytes=48 << 20),
        cost_estimate=pl.CostEstimate(flops=50 * 10**9, bytes_accessed=32 << 20, transcendentals=18 * 10**6),
    )(tab, q, do, kv, lse, delta, start, qidx, koff, cos_t, sin_t)


def place(me):
    return me // 8, lax.rem(me // 4, 2), lax.rem(me // 2, 2), lax.rem(me, 2)


def gather_kernel(w_ref, w_all, own_sem, zs, fs, ls, cs, zr, fr, lr, cr):
    me = lax.axis_index("cp")
    z, y, x, core = place(me)

    def dev(zz, yy, xx, cc):
        return ((zz * 2 + yy) * 2 + xx) * 2 + cc

    up_down = {1: dev(z + 1, y, x, core), -1: dev(z - 1, y, x, core)}
    inside = {1: z < 3, -1: z > 0}
    across_x, across_y, partner = dev(z, y, 1 - x, core), dev(z, 1 - y, x, core), dev(z, y, x, 1 - core)

    barrier = pltpu.get_barrier_semaphore()
    for d in (partner, across_x, across_y):
        pl.semaphore_signal(barrier, device_id=(d,), device_id_type=MESH)
    for step, to in up_down.items():
        pl.when(inside[step])(lambda to=to: pl.semaphore_signal(barrier, device_id=(to,), device_id_type=MESH))
    pl.semaphore_wait(barrier, 3 + sum(c.astype(jnp.int32) for c in inside.values()))

    def held(dz):
        return jnp.logical_and(z + dz >= 0, z + dz <= 3)

    def block(half, dz, first, last, cc):
        over_x, over_y = (first, last) if half == 0 else (last, first)
        return dev(z + dz, 1 - y if over_y else y, 1 - x if over_x else x, cc)

    def copy(half, idx, own, send, arrive, to):
        src = w_ref.at[half] if own else w_all.at[idx, half]
        return pltpu.make_async_remote_copy(
            src_ref=src, dst_ref=w_all.at[idx, half], send_sem=send, recv_sem=arrive, device_id=(to,), device_id_type=MESH
        )

    def z_copy(half, dz, d):
        at, there = (half, (d + 1) // 2, dz + 3), (half, dz - d + 3)
        return copy(half, block(half, dz, 0, 0, core), dz == 0, zs.at[at], zr.at[there], up_down[d])

    def first_copy(half, dz):
        at, to = (half, dz + 3), (across_x, across_y)[half]
        return copy(half, block(half, dz, 0, 0, core), dz == 0, fs.at[at], fr.at[at], to)

    def last_copy(half, dz, first):
        at, to = (half, first, dz + 3), (across_y, across_x)[half]
        return copy(half, block(half, dz, first, 0, core), dz == first == 0, ls.at[at], lr.at[at], to)

    def core_copy(half, dz, first, last):
        at = (half, first, last, dz + 3)
        return copy(half, block(half, dz, first, last, core), dz == first == last == 0, cs.at[at], cr.at[at], partner)

    def arrived(half, idx, sem):
        copy(half, idx, False, own_sem, sem, me).wait_recv()

    def ways(dz):
        for d in (1, -1):
            if d * dz <= 0:
                yield d, inside[d] if dz == 0 else jnp.logical_and(inside[d], held(dz))

    def send(half, dz):
        for d, on in ways(dz):
            pl.when(on)(lambda d=d: z_copy(half, dz, d).start())

        @pl.when(held(dz))
        def _():
            first_copy(half, dz).start()
            last_copy(half, dz, 0).start()
            core_copy(half, dz, 0, 0).start()

    halves = range(2)
    order = (0, 1, -1, 2, -2, 3, -3)
    own = pltpu.make_async_copy(w_ref, w_all.at[me], own_sem)
    own.start()
    for dz in order:
        for half in halves:
            if dz != 0:
                pl.when(held(dz))(lambda half=half: arrived(half, block(half, dz, 0, 0, core), zr.at[half, dz + 3]))
            send(half, dz)

        @pl.when(held(dz))
        def _(dz=dz):
            for half in halves:
                arrived(half, block(half, dz, 1, 0, core), fr.at[half, dz + 3])
                last_copy(half, dz, 1).start()
                core_copy(half, dz, 1, 0).start()

    own.wait()
    for first in (0, 1):
        for dz in order:

            @pl.when(held(dz))
            def _(dz=dz):
                for half in halves:
                    arrived(half, block(half, dz, first, 1, core), lr.at[half, first, dz + 3])
                    core_copy(half, dz, first, 1).start()

    for dz in order:
        for half in halves:

            @pl.when(held(dz))
            def _(dz=dz, half=half):
                first_copy(half, dz).wait_send()
                for first in (0, 1):
                    last_copy(half, dz, first).wait_send()
                    for last in (0, 1):
                        arrived(half, block(half, dz, first, last, 1 - core), cr.at[half, first, last, dz + 3])
                        core_copy(half, dz, first, last).wait_send()

            for d, on in ways(dz):
                pl.when(on)(lambda d=d: z_copy(half, dz, d).wait_send())


def gather_all(shard):
    dma = pltpu.SemaphoreType.DMA
    hops = [dma((2, 7)), dma((2, 2, 7)), dma((2, 2, 2, 7))]
    return pl.pallas_call(
        gather_kernel,
        name="gather_all",
        out_shape=jax.ShapeDtypeStruct((32,) + shard.shape, shard.dtype),
        in_specs=[pl.BlockSpec(memory_space=pl.ANY)],
        out_specs=pl.BlockSpec(memory_space=pl.ANY),
        scratch_shapes=[dma(()), dma((2, 2, 7))] + hops + [dma((2, 7))] + hops,
        compiler_params=pltpu.CompilerParams(collective_id=0),
        cost_estimate=pl.CostEstimate(flops=10**9, bytes_accessed=76 << 20, transcendentals=0),
    )(shard)


def quad_pairs(d):
    return [(r, r ^ d) for r in range(32)]


def z_pairs(step, sources):
    return [(r, r + 8 * step) for r in range(32) if r // 8 in sources]


def y_pairs(zs):
    return [(r, r ^ 4) for r in range(32) if r // 8 in zs]


def perm(x, pairs):
    return lax.ppermute(x, "cp", pairs)


def gather_pairs(own, y, z):
    got = {0: own}
    up = down = own
    for k in (1, 2, 3):
        up = perm(up, z_pairs(1, range(k - 1, 3)))
        down = perm(down, z_pairs(-1, range(1, 5 - k)))
        got[-k], got[k] = up, down
    near = [got[d] for d in range(-3, 4)]
    far = {}
    for d in (0, -1, 1, -2, 2, -3, 3):
        far[d] = perm(got[d], y_pairs([zz for zz in range(4) if 0 <= zz + d <= 3]))
    return jnp.stack(near + [far[d] for d in range(-3, 4)])


def reduce_z(blocks, z):
    right = left = None
    for t in (1, 2, 3):
        a = pick(blocks, jnp.clip(4 + z - t, 0, 3), 0)
        b = pick(blocks, jnp.clip(z + t - 4, 0, 3), 0)
        if right is not None:
            a, b = a + right, b + left
        right = perm(a, z_pairs(1, range(0, t)))
        left = perm(b, z_pairs(-1, range(4 - t, 4)))
    return pick(blocks, z, 0) + right + left


def reduce_pairs(parts, y, z, axis, cut):
    size = parts.shape[axis]
    out = []
    if cut > 0:
        a = lax.slice_in_dim(parts, 0, cut, axis=axis)
        got = perm(pick(a, 1 - y, 1), quad_pairs(4))
        out.append(reduce_z(pick(a, y, 1) + got, z))
    if cut < size:
        b = reduce_z(lax.slice_in_dim(parts, cut, size, axis=axis), z)
        got = perm(pick(b, 1 - y, 0), quad_pairs(4))
        out.append(pick(b, y, 0) + got)
    return out[0] if len(out) == 1 else jnp.concatenate(out, axis=axis - 2)


def solution(mesh):
    def local_step(hidden, grad_out, positions, seg_ids, w_q, w_k, w_v, w_o, norm_gain):
        n_batch, n_tok, d_model = hidden.shape
        n_rows = n_batch * n_tok
        wide = N_HEADS * HEAD_DIM
        me = lax.axis_index("cp")
        z, y, x, core = place(me)
        quad, pair = me % 4, me // 4
        relations = range(4)
        halves = (2, n_tok // 2)

        def side(d):
            return x ^ (d >> 1), core ^ (d & 1)

        def rows_of(arr, d):
            part = pick(arr.reshape((2, 2) + halves + arr.shape[2:]), side(d)[1], 0)
            return part

        def for_quad(arr):
            return [rows_of(arr, d) for d in relations]

        def swap(pieces):
            return [perm(p, quad_pairs(d)) if d else p for d, p in enumerate(pieces)]

        def unite(pieces, axis=2):
            joined = jnp.stack(swap(pieces), axis=axis)
            return joined.reshape(joined.shape[:axis] + (BLK,) + joined.shape[axis + 2 :])

        hidden_f32 = hidden.astype(F32)
        gain = norm_gain.astype(F32)
        inv_rms = lax.rsqrt(row_mean(hidden_f32 * hidden_f32) + NORM_EPS)
        normed = (hidden_f32 * inv_rms * gain).astype(BF16)
        normed_flat = normed.reshape(n_rows, d_model)
        cos_h, sin_h = (t[:, :, None] for t in rope_tables(positions))
        k_lin = jnp.dot(normed_flat, w_k, preferred_element_type=F32).reshape(n_batch, n_tok, 2, HEAD_DIM)
        keys = rotate(k_lin, cos_h, sin_h).astype(BF16)
        values = jnp.dot(normed_flat, w_v, preferred_element_type=F32).astype(BF16).reshape(n_batch, n_tok, 2, HEAD_DIM)
        kv_home = jnp.stack([keys, values]).transpose(3, 0, 1, 2, 4)

        def kv_piece(d):
            xx, cc = side(d)
            part = dyn(pick(kv_home, xx, 0), 2 * cc, 2, 1)
            return part.reshape((2, 2) + halves + (HEAD_DIM,))

        pos_u = unite(for_quad(positions))
        kv_own = unite([kv_piece(d) for d in relations], 3)
        kv_all = gather_pairs(kv_own, y, z)

        q_lin = jnp.dot(normed_flat, w_q, preferred_element_type=F32).reshape(n_batch, n_tok, 2 * N_HEADS, HEAD_DIM)
        queries = rotate(q_lin, cos_h, sin_h).astype(BF16).reshape(n_batch, n_tok, 2, wide)

        def q_piece(d):
            return rows_of(pick(queries, side(d)[0], 2), d)

        q_u = unite([q_piece(d) for d in relations])
        dy_pieces, q_u = lax.optimization_barrier((for_quad(grad_out), q_u))
        dy_u = unite(dy_pieces)
        normed_pieces, dy_u = lax.optimization_barrier((for_quad(normed), dy_u))
        normed_u = unite(normed_pieces)

        member = quad ^ jnp.arange(4)
        front = (member[:, None] * (n_tok // 2) + jnp.arange(n_tok // 2)[None, :]).reshape(BLK)
        back = ((3 - member)[:, None] * (n_tok // 2) + jnp.arange(n_tok // 2)[None, :]).reshape(BLK)
        offsets = jnp.stack([front, back]).astype(jnp.int32)
        own_super = jnp.stack([pair, N_SUPER - 1 - pair]).astype(jnp.int32)
        q_index = own_super[:, None] * BLK + offsets
        start = q_index[None] - pos_u
        koff = jnp.broadcast_to(offsets[:, :, None], (2, BLK, BLK))
        supers = jnp.arange(N_SUPER)
        of_pair = jnp.where(supers < N_PAIRS, supers, N_SUPER - 1 - supers)
        slot = ((of_pair % 2) ^ y) * 7 + 3 + of_pair // 2 - z
        tab = jnp.concatenate([
            slot.astype(jnp.int32), own_super, (jnp.min(start, axis=-1) // BLK).reshape(-1), jnp.max(start, axis=-1).reshape(-1),
        ])
        start_r = start[:, :, None, :]
        q_index_r = jnp.broadcast_to(q_index[None, :, None, :], start_r.shape)
        cos_u, sin_u = rope_tables(pos_u)
        cos_ut, sin_ut = jnp.swapaxes(cos_u, 2, 3), jnp.swapaxes(sin_u, 2, 3)

        attn_u, lse = flash_fwd(tab, q_u, kv_all, start_r, q_index_r, koff)

        def home(arr):
            return swap([piece[:, :, 0] for piece in jnp.split(arr.reshape(2, 2, 4, n_tok // 2, -1), 4, axis=2)])

        def in_order(place, own, other, axis):
            first = place == 0
            return jnp.concatenate([jnp.where(first, own, other), jnp.where(first, other, own)], axis=axis)

        def join(pieces):
            w = pieces[0].shape[-1]
            flat = [p.reshape(2, n_tok, w) for p in pieces]
            near, far = (in_order(core, *flat[i : i + 2], 0) for i in (0, 2))
            return in_order(x, near, far, -1)

        attn_home = join(home(attn_u)).reshape(n_rows, 2 * wide)
        block_out = (hidden_f32 + jnp.dot(attn_home, w_o, preferred_element_type=F32).reshape(hidden.shape)).astype(BF16)

        half_model = d_model // 2
        tok = tuple(range(3))

        def model_half(arr, i):
            return dyn(arr, i * half_model, half_model, 3)

        wo_send = dot(attn_u, model_half(dy_u, 1 - core), tok, tok)
        wo_sum = dot(attn_u, model_half(dy_u, core), tok, tok) + perm(wo_send, quad_pairs(1))
        wo_own = reduce_pairs(wo_sum.reshape(4, 2, wide // 8, half_model), y, z, 3, 640)

        d_attn = dot(dy_u, dyn(w_o, x * wide, wide, 0), (3,), (1,)).astype(BF16)
        delta = jnp.sum((d_attn.astype(F32) * attn_u.astype(F32)).reshape(2, 2, BLK, N_HEADS, HEAD_DIM), axis=-1)
        delta = jnp.swapaxes(delta, 2, 3)
        dq_u, dkv = flash_bwd(tab, q_u, d_attn, kv_all, lse, delta, start_r, q_index_r, koff, cos_ut, sin_ut)

        dkv_own = reduce_pairs(dkv.reshape(4, 2, 2, 2, 2, BLK, HEAD_DIM), y, z, 5, 160)
        dk_u = rotate(dkv_own[0] * ATTN_SCALE, cos_u, -sin_u).astype(BF16)
        dv_u = dkv_own[1].astype(BF16)

        def split_sum(d_out):
            send = dot(model_half(normed_u, 1 - core), d_out, tok, tok)
            return dot(model_half(normed_u, core), d_out, tok, tok) + perm(send, quad_pairs(1))

        wq_own = reduce_pairs(split_sum(dq_u).reshape(4, 2, half_model // 8, wide), y, z, 3, 640)
        dkv_u = jnp.concatenate([dk_u, dv_u], axis=-1)
        wkv_own = reduce_pairs(split_sum(dkv_u).reshape(4, 2, half_model // 8, 2 * HEAD_DIM), y, z, 3, 2 * HEAD_DIM)

        dq_home = join(home(dq_u)).reshape(n_rows, 2 * wide)
        dkv_home = join(home(dkv_u)).reshape(n_rows, 2, 2, HEAD_DIM)
        dk_home, dv_home = (dkv_home[:, :, i].reshape(n_rows, -1) for i in range(2))
        d_normed = dot(dq_home, w_q, (1,), (1,)) + dot(dk_home, w_k, (1,), (1,)) + dot(dv_home, w_v, (1,), (1,))
        d_normed = d_normed.astype(BF16).astype(F32).reshape(hidden.shape)
        scaled = d_normed * gain
        unit = hidden_f32 * inv_rms
        d_hidden = inv_rms * (scaled - unit * row_mean(scaled * unit))
        grad_hidden = (grad_out.astype(F32) + d_hidden).astype(BF16)
        d_gain = jnp.sum(d_normed * unit, axis=(0, 1)).reshape(d_model // 128, 128)
        for d in (1, 2, 4, 8, 16):
            d_gain = d_gain + perm(d_gain, quad_pairs(d))

        shard = jnp.concatenate([wo_own, wq_own, wkv_own], axis=-1)
        shard = shard.reshape(2, shard.shape[0] // 2, shard.shape[1])
        w_all = gather_all(shard).reshape(8, 2, 2, 128, shard.shape[-1])
        grad_wo = w_all[..., :half_model].transpose(1, 0, 3, 2, 4).reshape(2 * wide, d_model)
        grad_wq = w_all[..., half_model : half_model + wide].transpose(2, 0, 3, 1, 4).reshape(d_model, 2 * wide)
        rest = w_all[..., half_model + wide :].reshape(8, 2, 2, 128, 2, HEAD_DIM).transpose(4, 2, 0, 3, 1, 5)
        rest = rest.reshape(2, d_model, 2 * HEAD_DIM)
        return block_out, grad_hidden, grad_wq, rest[0], rest[1], grad_wo, d_gain.reshape(d_model)

    seq_spec = P(None, "cp", None)
    tok_spec = P(None, "cp")
    full_spec = P()
    return jax.shard_map(
        local_step,
        mesh=mesh,
        in_specs=(seq_spec, seq_spec, tok_spec, tok_spec, full_spec, full_spec, full_spec, full_spec, full_spec),
        out_specs=(seq_spec, seq_spec, full_spec, full_spec, full_spec, full_spec, full_spec),
        check_vma=False,
    )
```

```python
import functools

import jax
import jax.numpy as jnp
from jax import lax
from jax.experimental import pallas as pl
from jax.experimental.pallas import tpu as pltpu
from jax.sharding import PartitionSpec as P

HEAD_DIM = 128
NORM_EPS = 1e-5
ROPE_BASE = 500000.0
NEG_BIG = -1e30
LOG2E = 1.4426950408889634
ATTN_SCALE = HEAD_DIM**-0.5
EXP2_SCALE = ATTN_SCALE * LOG2E
CHUNK = 64
BLK = 4 * CHUNK
N_HEADS = 8
N_PAIRS = 8
N_SUPER = 2 * N_PAIRS
MESH = pl.DeviceIdType.MESH
LATER = 2, 3
F32 = jnp.float32
BF16 = jnp.bfloat16

T_SQ, T_LO, T_MX = 0, 2, 6


def rope_tables(positions):
    inv_freq = ROPE_BASE ** (-jnp.arange(0, HEAD_DIM, 2).astype(F32) / HEAD_DIM)
    angles = positions.astype(F32)[..., None] * inv_freq
    return jnp.cos(angles), jnp.sin(angles)


def rotate(x, cos_t, sin_t):
    a, b = x[..., : HEAD_DIM // 2], x[..., HEAD_DIM // 2 :]
    return jnp.concatenate([a * cos_t - b * sin_t, b * cos_t + a * sin_t], axis=-1)


def dot(a, b, ca, cb):
    return lax.dot_general(a, b, ((ca, cb), ((), ())), preferred_element_type=F32)


def row_mean(x):
    return jnp.mean(x, axis=-1, keepdims=True)


def head(h):
    return pl.ds(h * HEAD_DIM, HEAD_DIM)


def dot_t(a, b):
    return dot(a, b, (1,), (1,))


def dyn(x, index, size, axis):
    return lax.dynamic_slice_in_dim(x, index, size, axis)


def pick(x, index, axis):
    return lax.dynamic_index_in_dim(x, index, axis, keepdims=False)


def steps(tab, body):
    b, hf = pl.program_id(0), pl.program_id(1)
    own, first, last_start = tab[T_SQ + hf], tab[T_LO + 2 * b + hf], tab[T_MX + 2 * b + hf]

    def step(s, carry):
        late = s >= N_PAIRS
        at = jnp.where(late, N_SUPER - 1 - s, s), late.astype(jnp.int32)
        full = jnp.logical_and(s < own, s * BLK >= last_start)
        pl.when(full)(lambda: body(s, at, False))
        pl.when(jnp.logical_not(full))(lambda: body(s, at, True))
        return carry

    lax.fori_loop(first, own + 1, step, 0)


def may_use(s, off, st_ref, qi_ref):
    return jnp.logical_and(off >= st_ref[0, 0] - s * BLK, off <= qi_ref[0, 0] - s * BLK)


def fwd_kernel(tab, q_ref, kv_ref, st_ref, qi_ref, ko_ref, o_ref, lse_ref, acc, m_s, l_s):
    m_s[...] = jnp.full_like(m_s, NEG_BIG)
    l_s[...] = jnp.zeros_like(l_s)
    acc[...] = jnp.zeros_like(acc)

    def body(s, at, masked):
        pair, hk = at
        k = kv_ref[pair, 0, 0, hk]
        v_t = kv_ref[pair, 1, 0, hk].T
        mask = may_use(s, ko_ref[hk], st_ref, qi_ref) if masked else None
        for h in range(N_HEADS):
            sc = dot_t(k, q_ref[0, 0, :, head(h)]) * EXP2_SCALE
            if masked:
                sc = jnp.where(mask, sc, NEG_BIG)
            m_old = m_s[h]
            m_new = jnp.maximum(m_old, jnp.max(sc, axis=0, keepdims=True))
            alpha = jnp.exp2(m_old - m_new)
            p = jnp.exp2(sc - m_new)
            m_s[h] = m_new
            l_s[h] = l_s[h] * alpha + jnp.sum(p, axis=0, keepdims=True)
            acc[h] = acc[h] * alpha + jnp.dot(v_t, p.astype(BF16), preferred_element_type=F32)

    steps(tab, body)
    for h in range(N_HEADS):
        o_ref[0, 0, :, head(h)] = (acc[h] / l_s[h]).T.astype(BF16)
        lse_ref[0, 0, h] = m_s[h] + jnp.log2(l_s[h])


def bwd_kernel(tab, q_ref, do_ref, o_ref, kv_ref, lse_ref, st_ref, qi_ref, ko_ref, cos_ref, sin_ref, dq_ref, dkv_ref, dq_acc, delta):
    dq_acc[...] = jnp.zeros_like(dq_acc)
    for h in range(N_HEADS):
        terms = do_ref[0, 0, :, head(h)].astype(F32) * o_ref[0, 0, :, head(h)].astype(F32)
        delta[h] = jnp.sum(terms.T, axis=0, keepdims=True)

    @pl.when(pl.program_id(1) == 0)
    def _():
        dkv_ref[...] = jnp.zeros_like(dkv_ref)

    def body(s, at, masked):
        pair, hk = at
        k = kv_ref[pair, 0, 0, hk]
        v = kv_ref[pair, 1, 0, hk]
        k_t = k.T
        mask = may_use(s, ko_ref[hk], st_ref, qi_ref) if masked else None
        dk = dv = jnp.zeros((BLK, HEAD_DIM), F32)
        for h in range(N_HEADS):
            q = q_ref[0, 0, :, head(h)]
            do = do_ref[0, 0, :, head(h)]
            p = jnp.exp2(dot_t(k, q) * EXP2_SCALE - lse_ref[0, 0, h])
            if masked:
                p = jnp.where(mask, p, 0.0)
            ds = (p * (dot_t(v, do) - delta[h])).astype(BF16)
            dv += jnp.dot(p.astype(BF16), do, preferred_element_type=F32)
            dk += jnp.dot(ds, q, preferred_element_type=F32)
            dq_acc[h] += jnp.dot(k_t, ds, preferred_element_type=F32)
        dkv_ref[pair, 0, 0, hk] += dk
        dkv_ref[pair, 1, 0, hk] += dv

    steps(tab, body)
    cos_t, sin_t = cos_ref[0, 0], sin_ref[0, 0]
    half = HEAD_DIM // 2
    for h in range(N_HEADS):
        a, c = dq_acc[h, :half] * ATTN_SCALE, dq_acc[h, half:] * ATTN_SCALE
        lin = jnp.concatenate([a * cos_t + c * sin_t, c * cos_t - a * sin_t], axis=0)
        dq_ref[0, 0, :, head(h)] = lin.T.astype(BF16)


def attn_specs():
    def at_tile(b, h, t):
        return (b, h) + (0,) * 2

    def at_row(b, h, t):
        return (0, 0, b) + (0,) * 3

    tile = pl.BlockSpec((1, 1, BLK, N_HEADS * HEAD_DIM), at_tile)
    row = pl.BlockSpec((1, 1, 1, BLK), at_tile)
    stat = pl.BlockSpec((1, 1, N_HEADS, 1, BLK), lambda b, h, t: (b, h) + (0,) * 3)
    rope = pl.BlockSpec((1, 1, HEAD_DIM // 2, BLK), at_tile)
    kv = pl.BlockSpec((N_PAIRS, 2, 1, 2, BLK, HEAD_DIM), at_row)
    ko = pl.BlockSpec((2, BLK, BLK), lambda b, h, t: (0,) * 3)
    return tile, row, stat, kv, ko, rope


def flash_fwd(tab, q, kv, start, qidx, koff):
    tile, row, stat, kvs, ko, *_ = attn_specs()
    return pl.pallas_call(
        fwd_kernel,
        name="attn_fwd",
        out_shape=(jax.ShapeDtypeStruct(q.shape, BF16), jax.ShapeDtypeStruct((2, 2, N_HEADS, 1, BLK), F32)),
        grid_spec=pltpu.PrefetchScalarGridSpec(
            num_scalar_prefetch=1,
            grid=(2, 2),
            in_specs=[tile, kvs, row, row, ko],
            out_specs=[tile, stat],
            scratch_shapes=[pltpu.VMEM((N_HEADS, HEAD_DIM, BLK), F32)] + [pltpu.VMEM((N_HEADS, 1, BLK), F32)] * 2,
        ),
        compiler_params=pltpu.CompilerParams(vmem_limit_bytes=40 << 20),
        cost_estimate=pl.CostEstimate(flops=20 * 10**9, bytes_accessed=16 << 20, transcendentals=18 * 10**6),
    )(tab, q, kv, start, qidx, koff)


def flash_bwd(tab, q, do, o, kv, lse, start, qidx, koff, cos_t, sin_t):
    tile, row, stat, kvs, ko, rope = attn_specs()
    return pl.pallas_call(
        bwd_kernel,
        name="attn_bwd",
        out_shape=(
            jax.ShapeDtypeStruct(q.shape, BF16),
            jax.ShapeDtypeStruct(kv.shape, F32),
        ),
        grid_spec=pltpu.PrefetchScalarGridSpec(
            num_scalar_prefetch=1,
            grid=(2, 2),
            in_specs=[tile, tile, tile, kvs, stat, row, row, ko, rope, rope],
            out_specs=[tile, kvs],
            scratch_shapes=[pltpu.VMEM((N_HEADS, HEAD_DIM, BLK), F32), pltpu.VMEM((N_HEADS, 1, BLK), F32)],
        ),
        compiler_params=pltpu.CompilerParams(vmem_limit_bytes=48 << 20),
        cost_estimate=pl.CostEstimate(flops=50 * 10**9, bytes_accessed=32 << 20, transcendentals=18 * 10**6),
    )(tab, q, do, o, kv, lse, start, qidx, koff, cos_t, sin_t)


def turn(x, cos_ref, sin_ref):
    return x * cos_ref[...] + pltpu.roll(x, HEAD_DIM // 2, 1) * sin_ref[...]


def first_kernel(x_ref, g_ref, wk_ref, wv_ref, cos_ref, sin_ref, h_ref, kv_ref):
    x = x_ref[...].astype(F32)
    h = (x * lax.rsqrt(row_mean(x * x) + NORM_EPS) * g_ref[...]).astype(BF16)
    h_ref[...] = h
    k = jnp.dot(h, wk_ref[...], preferred_element_type=F32)
    v = jnp.dot(h, wv_ref[...], preferred_element_type=F32)
    n = kv_ref.shape[3]
    for i in range(2):
        for j, val in enumerate((turn(k[:, i * HEAD_DIM :][:, :HEAD_DIM], cos_ref, sin_ref), v[:, i * HEAD_DIM :][:, :HEAD_DIM])):
            for c in range(2):
                kv_ref[i, c, j] = val[c * n : (c + 1) * n].astype(BF16)


def query_kernel(h_ref, w_ref, cos_ref, sin_ref, q_ref):
    q = jnp.dot(h_ref[...], w_ref[...], preferred_element_type=F32)
    n = q_ref.shape[2]
    for j in range(q.shape[1] // HEAD_DIM):
        val = turn(q[:, j * HEAD_DIM :][:, :HEAD_DIM], cos_ref, sin_ref).astype(BF16)
        for c in range(2):
            q_ref[0, c, :, head(j)] = val[c * n : (c + 1) * n]


def project(x, gain, w_q, w_k, w_v, cos_f, sin_f):
    n, d = x.shape
    params = pltpu.CompilerParams(vmem_limit_bytes=40 << 20)
    h, kv = pl.pallas_call(
        first_kernel,
        name="norm_kv",
        out_shape=(jax.ShapeDtypeStruct(x.shape, BF16), jax.ShapeDtypeStruct((2,) * 3 + (n // 2, HEAD_DIM), BF16)),
        compiler_params=params,
        cost_estimate=pl.CostEstimate(flops=2 * 10**9, bytes_accessed=7 << 20, transcendentals=0),
    )(x, gain, w_k, w_v, cos_f, sin_f)
    tile = 4 * HEAD_DIM
    rope = pl.BlockSpec(cos_f.shape, lambda j: (0, 0))
    q = pl.pallas_call(
        query_kernel,
        name="query",
        grid=(d // tile,),
        out_shape=jax.ShapeDtypeStruct((2, 2, n // 2, d // 2), BF16),
        in_specs=[pl.BlockSpec(h.shape, lambda j: (0, 0)), pl.BlockSpec((d, tile), lambda j: (0, j)), rope, rope],
        out_specs=pl.BlockSpec((1, 2, n // 2, tile), lambda j: (j // 2, 0, 0, j % 2)),
        compiler_params=params,
        cost_estimate=pl.CostEstimate(flops=5 * 10**9, bytes_accessed=12 << 20, transcendentals=0),
    )(h, w_q, cos_f, sin_f)
    return h, kv, q


def place(me):
    return me // 8, lax.rem(me // 4, 2), lax.rem(me // 2, 2), lax.rem(me, 2)


def dev(z, y, x, core):
    return ((z * 2 + y) * 2 + x) * 2 + core


def z_peers(z):
    return [(k, lax.rem(z + k, 4)) for k in (1, 2, 3)]


def meet(peers):
    barrier = pltpu.get_barrier_semaphore()
    for d in peers:
        pl.semaphore_signal(barrier, device_id=(d,), device_id_type=MESH)
    pl.semaphore_wait(barrier, len(peers))


def remote(src, dst, send, arrive, to):
    return pltpu.make_async_remote_copy(
        src_ref=src, dst_ref=dst, send_sem=send, recv_sem=arrive, device_id=(to,), device_id_type=MESH
    )


def exchange_kernel(kv_ref, q_ref, dy_ref, kv_all, q_u, dy_u, own_sem, quad_s, quad_r, z_s, z_r, y_s, y_r):
    me = lax.axis_index("cp")
    z, y, x, core = place(me)
    pair = me // 4
    quad = [dev(z, y, 1 - x if d // 2 else x, 1 - core if d % 2 else core) for d in range(4)]
    across = dev(z, 1 - y, x, core)
    meet(quad[1:] + [across] + [dev(zz, y, x, core) for _, zz in z_peers(z)])

    def source(a, d):
        xx, cc = 1 - x if d // 2 else x, 1 - core if d % 2 else core
        return dy_ref.at[cc] if a == 2 else (kv_ref, q_ref)[a].at[xx, cc]

    def target(a, d):
        tok = pl.ds(d * CHUNK, CHUNK)
        return kv_all.at[pair, :, :, :, tok] if a == 0 else (q_u, dy_u)[a - 1].at[:, :, tok]

    def quad_copy(a, d):
        return remote(source(a, d), target(a, d), quad_s.at[a, d], quad_r.at[a, d], quad[d])

    def own_copy(a):
        return pltpu.make_async_copy(source(a, 0), target(a, 0), own_sem.at[a])

    sent = [(a, d) for a in range(3) for d in (1, 2, 3) if (a, d) != LATER]
    for a, d in sent:
        quad_copy(a, d).start()
    for a in range(3):
        own_copy(a).start()
    own_copy(0).wait()
    for d in (1, 2, 3):
        quad_copy(0, d).wait_recv()

    def pass_on(zz, k):
        block = kv_all.at[2 * zz + y]
        return remote(block, block, y_s.at[k], y_r.at[k], across)

    mine = kv_all.at[pair]
    to_z = [remote(mine, mine, z_s.at[k], z_r.at[k], dev(zz, y, x, core)) for k, zz in z_peers(z)]
    for c in to_z:
        c.start()
    pass_on(z, 0).start()
    came = [(k, lax.rem(z + 4 - k, 4)) for k in (1, 3, 2)]
    for k, zz in came:
        block = kv_all.at[2 * zz + y]
        remote(block, block, z_s.at[k], z_r.at[k], me).wait_recv()
        pass_on(zz, k).start()
    for k, zz in [(0, z)] + came:
        block = kv_all.at[2 * zz + 1 - y]
        remote(block, block, y_s.at[k], y_r.at[k], me).wait_recv()
        pass_on(zz, k).wait_send()
    for c in to_z:
        c.wait_send()
    for a, d in sent:
        quad_copy(a, d).wait_send()
        if a > 0:
            quad_copy(a, d).wait_recv()
    own_copy(1).wait()
    own_copy(2).wait()


def exchange(kv, q, dy):
    dma = pltpu.SemaphoreType.DMA
    vmem, hbm = pl.BlockSpec(memory_space=pltpu.VMEM), pl.BlockSpec(memory_space=pl.ANY)
    wide = q.shape[-1]
    return pl.pallas_call(
        exchange_kernel,
        name="exchange",
        out_shape=(
            jax.ShapeDtypeStruct((N_PAIRS,) + (2,) * 3 + (BLK, HEAD_DIM), BF16),
            jax.ShapeDtypeStruct((2, 2, BLK, wide), BF16),
            jax.ShapeDtypeStruct((2, 2, LATER[1] * CHUNK, 2 * wide), BF16),
        ),
        in_specs=[vmem] * 3,
        out_specs=[hbm] * 3,
        scratch_shapes=[dma((3,))] + [dma((3, 4))] * 2 + [dma((4,))] * 4,
        compiler_params=pltpu.CompilerParams(collective_id=1),
        cost_estimate=pl.CostEstimate(flops=10**9, bytes_accessed=20 << 20, transcendentals=0),
    )(kv, q, dy)


def reduce_kernel(cuts, shared, *refs):
    n = len(cuts)
    ins, outs, refs = refs[:n], refs[n : 2 * n], refs[2 * n :]
    own, from_core, from_y, from_z = refs[:n], refs[n : 2 * n], refs[2 * n : 3 * n], refs[3 * n : 4 * n]
    load_sem, core_s, core_r, y_s, y_r, z_s, z_r = refs[4 * n :]
    me = lax.axis_index("cp")
    z, y, x, core = place(me)
    partner, across = dev(z, y, x, 1 - core), dev(z, 1 - y, x, core)
    peers = [across] + [dev(zz, y, x, core) for _, zz in z_peers(z)]
    meet(peers + [partner] * any(shared))

    def rows(i, j):
        size = own[i].shape[2] // cuts[i]
        return pl.ds(j * size, size)

    def load(i, j):
        src = ins[i].at[core] if shared[i] else ins[i]
        return pltpu.make_async_copy(src.at[:, :, rows(i, j)], own[i].at[:, :, rows(i, j)], load_sem.at[i, j])

    def core_copy(i, j):
        at = rows(i, j)
        return remote(ins[i].at[1 - core, :, :, at], from_core[i].at[:, :, at], core_s.at[i, j], core_r.at[i, j], partner)

    def y_copy(i, j):
        src = own[i] if shared[i] else ins[i]
        at = rows(i, j)
        return remote(src.at[:, 1 - y, at], from_y[i].at[:, at], y_s.at[i, j], y_r.at[i, j], across)

    def z_copy(i, j, k, zz):
        at = rows(i, j)
        return remote(
            own[i].at[zz, y, at], from_z[i].at[k - 1, at], z_s.at[i, j, k - 1], z_r.at[i, j, k - 1], dev(zz, y, x, core)
        )

    pieces = [(i, j) for i in range(n) for j in range(cuts[i])]
    for i, j in pieces:
        if shared[i]:
            core_copy(i, j).start()
        else:
            y_copy(i, j).start()
        load(i, j).start()
    for i, j in pieces:
        load(i, j).wait()
        if shared[i]:
            core_copy(i, j).wait_recv()
            at = rows(i, j)
            for zz in range(4):
                own[i][zz, :, at] += from_core[i][zz, :, at]
            y_copy(i, j).start()
    for i, j in pieces:
        y_copy(i, j).wait_recv()
        at = rows(i, j)
        for zz in range(4):
            own[i][zz, y, at] += from_y[i][zz, at]
        for k, zz in z_peers(z):
            z_copy(i, j, k, zz).start()
    for i, j in pieces:
        at = rows(i, j)
        for k, zz in z_peers(z):
            z_copy(i, j, k, zz).wait_recv()
        outs[i][at] = own[i][z, y, at] + sum(from_z[i][k, at] for k in range(3))
    for i, j in pieces:
        if shared[i]:
            core_copy(i, j).wait_send()
        y_copy(i, j).wait_send()
        for k, zz in z_peers(z):
            z_copy(i, j, k, zz).wait_send()


def reduce_pairs(arrays, cuts, shared, collective_id):
    dma = pltpu.SemaphoreType.DMA
    vmem, hbm = pl.BlockSpec(memory_space=pltpu.VMEM), pl.BlockSpec(memory_space=pl.ANY)
    n, most = len(arrays), max(cuts)
    blocks = [a.shape[-2:] for a in arrays]
    ins = [a.reshape(a.shape[:-3] + (4, 2) + b) for a, b in zip(arrays, blocks)]
    own = [pltpu.VMEM((4, 2) + b, F32) for b in blocks]
    scratch = own + [o if s else pltpu.VMEM((8, HEAD_DIM), F32) for o, s in zip(own, shared)]
    scratch += [pltpu.VMEM((4,) + b, F32) for b in blocks] + [pltpu.VMEM((3,) + b, F32) for b in blocks]
    return pl.pallas_call(
        functools.partial(reduce_kernel, cuts, shared),
        name="reduce_pairs",
        out_shape=[jax.ShapeDtypeStruct(b, F32) for b in blocks],
        in_specs=[hbm] * n,
        out_specs=[vmem] * n,
        scratch_shapes=scratch + [dma((n, most))] * 5 + [dma((n, most, 3))] * 2,
        compiler_params=pltpu.CompilerParams(collective_id=collective_id, vmem_limit_bytes=56 << 20),
        cost_estimate=pl.CostEstimate(flops=10**9, bytes_accessed=20 << 20, transcendentals=0),
    )(*ins)


def gather_kernel(*refs):
    shards, outs = refs[:4], refs[4:8]
    own_sem, zs, fs, ls, cs, zr, fr, lr, cr = refs[8:]
    me = lax.axis_index("cp")
    z, y, x, core = place(me)
    across = (dev(z, y, 1 - x, core), dev(z, 1 - y, x, core))
    partner = dev(z, y, x, 1 - core)
    meet([partner, *across] + [dev(zz, y, x, core) for _, zz in z_peers(z)])

    def windows(half, zz, yy, xx, cc):
        pair = 2 * zz + yy
        rows = shards[0].shape[0] // 2
        out_rows = pl.ds(((xx * 2 + cc) * N_PAIRS + pair) * 2 * rows + half * rows, rows)
        yield shards[0], pl.ds(half * rows, rows), outs[0].at[out_rows]
        rows = shards[1].shape[0] // 2
        out_rows = pl.ds((cc * N_PAIRS + pair) * 2 * rows + half * rows, rows)
        for s, o in zip(shards[1:], outs[1:]):
            yield s, pl.ds(half * rows, rows), o.at[out_rows, pl.ds(xx * s.shape[1], s.shape[1])]

    total = sum(s.size for s in shards) // 2 // outs[0].shape[1]
    whole = outs[0].at[pl.ds(0, total)]

    def flip(v, on):
        return 1 - v if on else v

    class Copy:
        def __init__(self, half, zz, first, last, send, arrive, to, is_own, cc=core):
            over_x, over_y = (first, last) if half == 0 else (last, first)
            self.at = half, zz, flip(y, over_y), flip(x, over_x), cc
            self.send, self.arrive, self.to, self.is_own = send, arrive, to, is_own

        def start(self):
            for shard, rows, window in windows(*self.at):
                remote(shard.at[rows] if self.is_own else window, window, self.send, self.arrive, self.to).start()

        def wait_recv(self):
            remote(whole, whole, self.send, self.arrive, me).wait_recv()

        def wait_send(self):
            remote(whole, whole, self.send, self.arrive, me).wait_send()

    places = [(0, z)] + [(k, lax.rem(z + 4 - k, 4)) for k in (1, 3, 2)]
    halves = range(2)

    def z_copy(half, k, zz):
        return Copy(half, z, 0, 0, zs.at[half, k], zr.at[half, k], dev(zz, y, x, core), True)

    def first_copy(half, k, zz):
        at = half, k
        return Copy(half, zz, 0, 0, fs.at[at], fr.at[at], across[half], k == 0)

    def last_copy(half, k, zz, first):
        at = half, first, k
        return Copy(half, zz, first, 0, ls.at[at], lr.at[at], across[1 - half], k == first == 0)

    def core_copy(half, k, zz, first, last):
        at = half, first, last, k
        return Copy(half, zz, first, last, cs.at[at], cr.at[at], partner, k == first == last == 0)

    owns = []
    for half in halves:
        for shard, rows, window in windows(half, z, y, x, core):
            owns.append(pltpu.make_async_copy(shard.at[rows], window, own_sem.at[len(owns)]))
    for k, zz in z_peers(z):
        for half in halves:
            z_copy(half, k, zz).start()
    for k, zz in places:
        for half in halves:
            if k > 0:
                z_copy(half, k, zz).wait_recv()
            first_copy(half, k, zz).start()
            last_copy(half, k, zz, 0).start()
            core_copy(half, k, zz, 0, 0).start()
        if k == 0:
            for o in owns:
                o.start()
        for half in halves:
            first_copy(half, k, zz).wait_recv()
            last_copy(half, k, zz, 1).start()
            core_copy(half, k, zz, 1, 0).start()
    for first in halves:
        for k, zz in places:
            for half in halves:
                last_copy(half, k, zz, first).wait_recv()
                core_copy(half, k, zz, first, 1).start()
    for o in owns:
        o.wait()
    for k, zz in z_peers(z):
        for half in halves:
            z_copy(half, k, zz).wait_send()
    for k, zz in places:
        for half in halves:
            first_copy(half, k, zz).wait_send()
            for first in halves:
                last_copy(half, k, zz, first).wait_send()
                for last in halves:
                    core_copy(half, k, zz, first, last).wait_recv()
                    core_copy(half, k, zz, first, last).wait_send()


def gather_all(shards, shapes):
    dma = pltpu.SemaphoreType.DMA
    vmem, hbm = pl.BlockSpec(memory_space=pltpu.VMEM), pl.BlockSpec(memory_space=pl.ANY)
    hops = [dma((2,) * i + (4,)) for i in (1, 1, 2, 3)]
    n = len(shards)
    return pl.pallas_call(
        gather_kernel,
        name="gather_all",
        out_shape=[jax.ShapeDtypeStruct(s, F32) for s in shapes],
        in_specs=[vmem] * n,
        out_specs=[hbm] * n,
        scratch_shapes=[dma((2 * n,))] + hops + hops,
        compiler_params=pltpu.CompilerParams(collective_id=0),
        cost_estimate=pl.CostEstimate(flops=10**9, bytes_accessed=76 << 20, transcendentals=0),
    )(*shards)


def perm(x, pairs):
    return lax.ppermute(x, "cp", pairs)


def flip_pairs(d):
    return [(r, r ^ d) for r in range(32)]


def turn_z(k):
    return [(r, (r + 8 * k) % 32) for r in range(32)]


def solution(mesh):
    def local_step(hidden, grad_out, positions, seg_ids, w_q, w_k, w_v, w_o, norm_gain):
        n_batch, n_tok, d_model = hidden.shape
        n_rows = n_batch * n_tok
        wide = N_HEADS * HEAD_DIM
        me = lax.axis_index("cp")
        z, y, x, core = place(me)
        quad, pair = me % 4, me // 4
        relations = range(4)

        def rows_of(arr, d):
            return pick(arr.reshape((2, 2, 2, CHUNK) + arr.shape[2:]), core ^ (d % 2), 0)

        def swap(pieces):
            return [perm(p, flip_pairs(d)) if d else p for d, p in enumerate(pieces)]

        def unite(arr):
            joined = jnp.stack(swap([rows_of(arr, d) for d in relations]), axis=2)
            return joined.reshape((2, 2, BLK) + joined.shape[4:])

        gain = norm_gain.astype(F32)
        cos_t, sin_t = rope_tables(positions.reshape(n_rows))
        cos_f, sin_f = jnp.concatenate([cos_t, cos_t], axis=1), jnp.concatenate([-sin_t, sin_t], axis=1)
        normed, kv_home, q_home = project(hidden.reshape(n_rows, d_model), gain[None], w_q, w_k, w_v, cos_f, sin_f)
        pos_u = unite(positions)
        kv_all, q_u, dy_part = exchange(
            kv_home.reshape((2,) * 5 + (CHUNK, HEAD_DIM)),
            q_home.reshape((2,) * 4 + (CHUNK, wide)),
            grad_out.reshape((2,) * 3 + (CHUNK, d_model)),
        )
        dy_last, dy_part = lax.optimization_barrier((rows_of(grad_out, LATER[1]), dy_part))
        dy_last = perm(dy_last, flip_pairs(LATER[1]))
        normed_home, dy_part = lax.optimization_barrier((normed.reshape(hidden.shape), dy_part))
        normed_u = unite(normed_home)

        member = quad ^ jnp.arange(4)
        front, back = ((m[:, None] * CHUNK + jnp.arange(CHUNK)[None]).reshape(BLK) for m in (member, 3 - member))
        offsets = jnp.stack([front, back]).astype(jnp.int32)
        own_super = jnp.stack([pair, N_SUPER - 1 - pair]).astype(jnp.int32)
        q_index = own_super[:, None] * BLK + offsets
        start = q_index[None] - pos_u
        koff = jnp.broadcast_to(offsets[:, :, None], (2, BLK, BLK))
        tab = jnp.concatenate(
            [own_super, (jnp.min(start, axis=-1) // BLK).reshape(-1), jnp.max(start, axis=-1).reshape(-1)]
        )
        start_r = start[:, :, None, :]
        q_index_r = jnp.broadcast_to(q_index[None, :, None, :], start_r.shape)
        cos_u, sin_u = rope_tables(pos_u)
        cos_ut, sin_ut = jnp.swapaxes(cos_u, 2, 3), jnp.swapaxes(sin_u, 2, 3)

        attn_u, lse = flash_fwd(tab, q_u, kv_all, start_r, q_index_r, koff)

        def home(arr):
            return swap([piece[:, :, 0] for piece in jnp.split(arr.reshape(2, 2, 4, CHUNK, -1), 4, axis=2)])

        def in_order(place, own, other, axis):
            first = place == 0
            return jnp.concatenate([jnp.where(first, own, other), jnp.where(first, other, own)], axis=axis)

        def join(pieces):
            flat = [p.reshape(n_rows // 2, -1) for p in pieces]
            near, far = (in_order(core, *flat[i : i + 2], 0) for i in (0, 2))
            return in_order(x, near, far, -1)

        tok = tuple(range(3))
        half_wide = wide // 2
        dy_u = jnp.concatenate([dy_part, dy_last], axis=2)
        wo_send = dot(dyn(attn_u, (1 - core) * half_wide, half_wide, 3), dy_u, tok, tok)
        wo_sum = dot(dyn(attn_u, core * half_wide, half_wide, 3), dy_u, tok, tok) + perm(wo_send, flip_pairs(1))
        wo_sum = wo_sum.reshape(4, 2, half_wide // N_PAIRS, d_model)
        wo_y = perm(pick(wo_sum, 1 - y, 1), flip_pairs(4))

        d_attn = dot(dy_u, dyn(w_o, x * wide, wide, 0), (3,), (1,)).astype(BF16)
        d_attn, wo_sum = lax.optimization_barrier((d_attn, wo_sum))
        dq_u, dkv = flash_bwd(tab, q_u, d_attn, attn_u, kv_all, lse, start_r, q_index_r, koff, cos_ut, sin_ut)

        attn_home = join(home(attn_u))
        block_out = (hidden.astype(F32) + jnp.dot(attn_home, w_o, preferred_element_type=F32).reshape(hidden.shape)).astype(BF16)

        wo_sum = pick(wo_sum, y, 1) + wo_y
        wo_own = pick(wo_sum, z, 0)
        for k, zz in z_peers(z):
            wo_own = wo_own + perm(pick(wo_sum, zz, 0), turn_z(k))

        dq_home = join(home(dq_u))
        half_model = d_model // 2

        def by_core(d_out):
            part = lax.optimization_barrier(dot(normed_u, d_out, tok, tok))
            return part.reshape(2, N_PAIRS, half_model // N_PAIRS, -1)

        dkv_own, wq_own = reduce_pairs([dkv.reshape(N_PAIRS, -1, HEAD_DIM), by_core(dq_u)], (4, 2), (False, True), 2)
        dkv_own = dkv_own.reshape((2,) * 3 + (BLK, HEAD_DIM))
        dk_u = rotate(dkv_own[0] * ATTN_SCALE, cos_u, -sin_u).astype(BF16)
        dkv_u = jnp.concatenate([dk_u, dkv_own[1].astype(BF16)], axis=-1)
        (wkv_own,) = reduce_pairs([by_core(dkv_u)], (1,), (True,), 3)

        dkv_home = join(home(dkv_u)).reshape(n_rows, 2, 2, HEAD_DIM)
        dk_home, dv_home = (dkv_home[:, :, i].reshape(n_rows, -1) for i in range(2))
        d_normed = dot_t(dq_home, w_q) + dot_t(dk_home, w_k) + dot_t(dv_home, w_v)
        d_normed = d_normed.astype(BF16).astype(F32).reshape(hidden.shape)
        hidden_f32 = hidden.astype(F32)
        inv_rms = lax.rsqrt(row_mean(hidden_f32 * hidden_f32) + NORM_EPS)
        scaled = d_normed * gain
        unit = hidden_f32 * inv_rms
        d_hidden = inv_rms * (scaled - unit * row_mean(scaled * unit))
        grad_hidden = (grad_out.astype(F32) + d_hidden).astype(BF16)
        d_gain = jnp.sum(d_normed * unit, axis=(0, 1)).reshape(-1, 128)
        for i in range(5):
            d_gain = d_gain + perm(d_gain, flip_pairs(1 << i))

        wk_own, wv_own = jnp.split(wkv_own, 2, axis=1)
        grad_wo, grad_wq, grad_wk, grad_wv = gather_all(
            [wo_own, wq_own, wk_own, wv_own], [w_o.shape, w_q.shape, w_k.shape, w_v.shape]
        )
        return block_out, grad_hidden, grad_wq, grad_wk, grad_wv, grad_wo, d_gain.reshape(d_model)

    seq_spec = P(None, "cp", None)
    tok_spec = P(None, "cp")
    full_spec = P()
    return jax.shard_map(
        local_step,
        mesh=mesh,
        in_specs=(seq_spec, seq_spec, tok_spec, tok_spec, full_spec, full_spec, full_spec, full_spec, full_spec),
        out_specs=(seq_spec, seq_spec, full_spec, full_spec, full_spec, full_spec, full_spec),
        check_vma=False,
    )
```

```python
import functools

import jax
import jax.numpy as jnp
from jax import lax
from jax.experimental import pallas as pl
from jax.experimental.pallas import tpu as pltpu
from jax.sharding import PartitionSpec as P

HEAD_DIM = 128
NORM_EPS = 1e-5
ROPE_BASE = 500000.0
NEG_BIG = -1e30
LOG2E = 1.4426950408889634
ATTN_SCALE = HEAD_DIM**-0.5
EXP2_SCALE = ATTN_SCALE * LOG2E
CHUNK = 64
BLK = 4 * CHUNK
N_HEADS = 8
N_PAIRS = 8
N_SUPER = 2 * N_PAIRS
MESH = pl.DeviceIdType.MESH
ONE = pl.Squeezed()
LATER = 2, 3
F32 = jnp.float32
BF16 = jnp.bfloat16

T_SQ, T_LO, T_MX = 0, 2, 6


def rope_tables(positions):
    inv_freq = ROPE_BASE ** (-jnp.arange(0, HEAD_DIM, 2).astype(F32) / HEAD_DIM)
    angles = positions.astype(F32)[..., None] * inv_freq
    return jnp.cos(angles), jnp.sin(angles)


def rotate(x, cos_t, sin_t):
    a, b = x[..., : HEAD_DIM // 2], x[..., HEAD_DIM // 2 :]
    return jnp.concatenate([a * cos_t - b * sin_t, b * cos_t + a * sin_t], axis=-1)


def dot(a, b, ca, cb):
    return lax.dot_general(a, b, ((ca, cb), ((), ())), preferred_element_type=F32)


def cost(gflop, mib):
    return pl.CostEstimate(flops=gflop * 10**9, bytes_accessed=mib << 20, transcendentals=0)


def params(mib, **more):
    return pltpu.CompilerParams(vmem_limit_bytes=mib << 20, **more)


def row_mean(x):
    return jnp.mean(x, axis=-1, keepdims=True)


def head(h):
    return pl.ds(h * HEAD_DIM, HEAD_DIM)


def head_slice(h):
    return slice(h * HEAD_DIM, (h + 1) * HEAD_DIM)


def dot_t(a, b):
    return dot(a, b, (1,), (1,))


def dyn(x, index, size, axis):
    return lax.dynamic_slice_in_dim(x, index, size, axis)


def pick(x, index, axis):
    return lax.dynamic_index_in_dim(x, index, axis, keepdims=False)


def steps(tab, body):
    b, hf = pl.program_id(0), pl.program_id(1)
    own, first, last_start = tab[T_SQ + hf], tab[T_LO + 2 * b + hf], tab[T_MX + 2 * b + hf]

    def step(s, carry):
        late = s >= N_PAIRS
        at = jnp.where(late, N_SUPER - 1 - s, s), late.astype(jnp.int32)
        full = jnp.logical_and(s < own, s * BLK >= last_start)
        pl.when(full)(lambda: body(s, at, False))
        pl.when(jnp.logical_not(full))(lambda: body(s, at, True))
        return carry

    lax.fori_loop(first, own + 1, step, 0)


def may_use(s, off, st_ref, qi_ref):
    return jnp.logical_and(off >= st_ref[...] - s * BLK, off <= qi_ref[...] - s * BLK)


def fwd_kernel(tab, q_ref, kv_ref, st_ref, qi_ref, ko_ref, o_ref, lse_ref, q_s, acc, m_s, l_s):
    m_s[...] = jnp.full_like(m_s, NEG_BIG)
    l_s[...] = jnp.zeros_like(l_s)
    acc[...] = jnp.zeros_like(acc)
    for h in range(N_HEADS):
        q_s[pl.ds(h * BLK, BLK)] = q_ref[:, head(h)]

    def body(s, at, masked):
        pair, hk = at
        k, v = kv_ref[pair, 0, hk], kv_ref[pair, 1, hk]
        if masked:
            off = ko_ref[hk] + s * BLK
            mask = [
                jnp.logical_and(off[:, lanes] >= st_ref[...], off[:, lanes] <= qi_ref[...])
                for lanes in (slice(HEAD_DIM), slice(HEAD_DIM, BLK))
            ]
        for h in range(N_HEADS):
            rows = pl.ds(h * BLK, BLK)
            sc = dot_t(q_s[rows], k)
            sc = [sc[:, :HEAD_DIM] * EXP2_SCALE, sc[:, HEAD_DIM:] * EXP2_SCALE]
            if masked:
                sc = [jnp.where(m, x, NEG_BIG) for m, x in zip(mask, sc)]
            m_old = m_s[rows]
            m_new = jnp.maximum(m_old, jnp.max(jnp.maximum(*sc), axis=1, keepdims=True))
            alpha = jnp.exp2(m_old - m_new)
            p = [jnp.exp2(x - m_new) for x in sc]
            m_s[rows] = m_new
            l_s[rows] = l_s[rows] * alpha + (p[0] + p[1])
            p = jnp.hstack([x.astype(BF16) for x in p])
            acc[rows] = acc[rows] * alpha + jnp.dot(p, v, preferred_element_type=F32)

    steps(tab, body)
    for h in range(N_HEADS):
        rows = pl.ds(h * BLK, BLK)
        total = jnp.sum(l_s[rows], axis=1, keepdims=True)
        o_ref[:, head(h)] = (acc[rows] / total).astype(BF16)
        lse_ref[h] = (m_s[rows] + jnp.log2(total)).T[:1]


def bwd_kernel(tab, q_ref, do_ref, o_ref, kv_ref, lse_ref, st_ref, qi_ref, ko_ref, cos_ref, sin_ref, dq_ref, dkv_ref, dq_acc, delta):
    dq_acc[...] = jnp.zeros_like(dq_acc)
    for h in range(N_HEADS):
        terms = do_ref[:, head(h)].astype(F32) * o_ref[:, head(h)].astype(F32)
        delta[h] = jnp.sum(terms.T, axis=0, keepdims=True)

    @pl.when(pl.program_id(1) == 0)
    def _():
        dkv_ref[...] = jnp.zeros_like(dkv_ref)

    def body(s, at, masked):
        pair, hk = at
        k = kv_ref[pair, 0, hk]
        v = kv_ref[pair, 1, hk]
        k_t = k.T
        mask = may_use(s, ko_ref[hk], st_ref, qi_ref) if masked else None
        dk = dv = jnp.zeros((BLK, HEAD_DIM), F32)
        for h in range(N_HEADS):
            q = q_ref[:, head(h)]
            do = do_ref[:, head(h)]
            p = jnp.exp2(dot_t(k, q) * EXP2_SCALE - lse_ref[h])
            if masked:
                p = jnp.where(mask, p, 0.0)
            ds = (p * (dot_t(v, do) - delta[h])).astype(BF16)
            dv += jnp.dot(p.astype(BF16), do, preferred_element_type=F32)
            dk += jnp.dot(ds, q, preferred_element_type=F32)
            dq_acc[h] += jnp.dot(k_t, ds, preferred_element_type=F32)
        dkv_ref[pair, 0, hk] += dk
        dkv_ref[pair, 1, hk] += dv

    steps(tab, body)
    cos_t, sin_t = cos_ref[...], sin_ref[...]
    half = HEAD_DIM // 2
    for h in range(N_HEADS):
        a, c = dq_acc[h, :half] * ATTN_SCALE, dq_acc[h, half:] * ATTN_SCALE
        lin = jnp.concatenate([a * cos_t + c * sin_t, c * cos_t - a * sin_t], axis=0)
        dq_ref[:, head(h)] = lin.T.astype(BF16)


def attn_specs():
    def at_tile(b, h, t):
        return (b, h) + (0,) * 2

    def at_row(b, h, t):
        return (0, 0, b) + (0,) * 3

    tile = pl.BlockSpec((ONE, ONE, BLK, N_HEADS * HEAD_DIM), at_tile)
    row = pl.BlockSpec((ONE, ONE, 1, BLK), at_tile)
    stat = pl.BlockSpec((ONE, ONE, N_HEADS, 1, BLK), lambda b, h, t: (b, h) + (0,) * 3)
    rope = pl.BlockSpec((ONE, ONE, HEAD_DIM // 2, BLK), at_tile)
    kv = pl.BlockSpec((N_PAIRS, 2, ONE, 2, BLK, HEAD_DIM), at_row)
    ko = pl.BlockSpec((2, BLK, BLK), lambda b, h, t: (0,) * 3)
    return tile, row, stat, kv, ko, rope


def flash_fwd(tab, q, kv, start, qidx, koff):
    tile, _, stat, kvs, *_ = attn_specs()
    col = pl.BlockSpec((ONE, ONE, BLK, HEAD_DIM), lambda b, h, t: (b, h) + (0,) * 2)
    ko = pl.BlockSpec((2, 1, BLK), lambda b, h, t: (0,) * 3)
    return pl.pallas_call(
        fwd_kernel,
        name="attn_fwd",
        out_shape=(jax.ShapeDtypeStruct(q.shape, BF16), jax.ShapeDtypeStruct((2, 2, N_HEADS, 1, BLK), F32)),
        grid_spec=pltpu.PrefetchScalarGridSpec(
            num_scalar_prefetch=1,
            grid=(2, 2),
            in_specs=[tile, kvs, col, col, ko],
            out_specs=[tile, stat],
            scratch_shapes=[pltpu.VMEM((N_HEADS * BLK, HEAD_DIM), t) for t in (BF16, F32, F32, F32)],
        ),
        compiler_params=params(40),
        cost_estimate=cost(20, 16),
    )(tab, q, kv, start, qidx, koff)


def flash_bwd(tab, q, do, o, kv, lse, start, qidx, koff, cos_t, sin_t):
    tile, row, stat, kvs, ko, rope = attn_specs()
    return pl.pallas_call(
        bwd_kernel,
        name="attn_bwd",
        out_shape=(
            jax.ShapeDtypeStruct(q.shape, BF16),
            jax.ShapeDtypeStruct(kv.shape, F32),
        ),
        grid_spec=pltpu.PrefetchScalarGridSpec(
            num_scalar_prefetch=1,
            grid=(2, 2),
            in_specs=[tile, tile, tile, kvs, stat, row, row, ko, rope, rope],
            out_specs=[tile, kvs],
            scratch_shapes=[pltpu.VMEM((N_HEADS, HEAD_DIM, BLK), F32), pltpu.VMEM((N_HEADS, 1, BLK), F32)],
        ),
        compiler_params=params(48),
        cost_estimate=cost(50, 32),
    )(tab, q, do, o, kv, lse, start, qidx, koff, cos_t, sin_t)


def turn(x, cos_ref, sin_ref):
    return x * cos_ref[...] + pltpu.roll(x, HEAD_DIM // 2, 1) * sin_ref[...]


def first_kernel(x_ref, g_ref, wk_ref, wv_ref, cos_ref, sin_ref, h_ref, kv_ref):
    x = x_ref[...].astype(F32)
    h = (x * lax.rsqrt(row_mean(x * x) + NORM_EPS) * g_ref[...]).astype(BF16)
    h_ref[...] = h
    k = jnp.dot(h, wk_ref[...], preferred_element_type=F32)
    v = jnp.dot(h, wv_ref[...], preferred_element_type=F32)
    n = kv_ref.shape[3]
    for i in range(2):
        for j, val in enumerate((turn(k[:, head_slice(i)], cos_ref, sin_ref), v[:, head_slice(i)])):
            for c in range(2):
                kv_ref[i, c, j] = val[c * n : (c + 1) * n].astype(BF16)


def query_kernel(h_ref, w_ref, cos_ref, sin_ref, q_ref):
    q = jnp.dot(h_ref[...], w_ref[...], preferred_element_type=F32)
    n = q_ref.shape[2]
    for j in range(q.shape[1] // HEAD_DIM):
        val = turn(q[:, head_slice(j)], cos_ref, sin_ref).astype(BF16)
        for c in range(2):
            q_ref[0, c, :, head(j)] = val[c * n : (c + 1) * n]


def project(x, gain, w_q, w_k, w_v, cos_f, sin_f):
    n, d = x.shape
    h, kv = pl.pallas_call(
        first_kernel,
        name="norm_kv",
        out_shape=(jax.ShapeDtypeStruct(x.shape, BF16), jax.ShapeDtypeStruct((2,) * 3 + (n // 2, HEAD_DIM), BF16)),
        compiler_params=params(40),
        cost_estimate=cost(2, 7),
    )(x, gain, w_k, w_v, cos_f, sin_f)
    tile = 4 * HEAD_DIM
    rope = pl.BlockSpec(cos_f.shape, lambda j: (0, 0))
    q = pl.pallas_call(
        query_kernel,
        name="query",
        grid=(d // tile,),
        out_shape=jax.ShapeDtypeStruct((2, 2, n // 2, d // 2), BF16),
        in_specs=[pl.BlockSpec(h.shape, lambda j: (0, 0)), pl.BlockSpec((d, tile), lambda j: (0, j)), rope, rope],
        out_specs=pl.BlockSpec((1, 2, n // 2, tile), lambda j: (j // 2, 0, 0, j % 2)),
        compiler_params=params(40),
        cost_estimate=cost(5, 12),
    )(h, w_q, cos_f, sin_f)
    return h, kv, q


def place(me):
    return me // 8, lax.rem(me // 4, 2), lax.rem(me // 2, 2), lax.rem(me, 2)


def dev(z, y, x, core):
    return ((z * 2 + y) * 2 + x) * 2 + core


def z_peers(z):
    return [(k, lax.rem(z + k, 4)) for k in (1, 2, 3)]


def meet(peers):
    barrier = pltpu.get_barrier_semaphore()
    for d in peers:
        pl.semaphore_signal(barrier, device_id=(d,), device_id_type=MESH)
    pl.semaphore_wait(barrier, len(peers))


def remote(src, dst, send, arrive, to):
    return pltpu.make_async_remote_copy(
        src_ref=src, dst_ref=dst, send_sem=send, recv_sem=arrive, device_id=(to,), device_id_type=MESH
    )


def exchange_kernel(kv_ref, q_ref, dy_ref, kv_all, q_u, dy_u, own_sem, quad_s, quad_r, z_s, z_r, y_s, y_r):
    me = lax.axis_index("cp")
    z, y, x, core = place(me)
    pair = me // 4
    quad = quad_of(me)
    across = dev(z, 1 - y, x, core)
    meet(quad[1:] + [across] + [dev(zz, y, x, core) for _, zz in z_peers(z)])

    def source(a, d):
        xx, cc = 1 - x if d // 2 else x, 1 - core if d % 2 else core
        return dy_ref.at[cc] if a == 2 else (kv_ref, q_ref)[a].at[xx, cc]

    def target(a, d):
        tok = pl.ds(d * CHUNK, CHUNK)
        return kv_all.at[pair, :, :, :, tok] if a == 0 else (q_u, dy_u)[a - 1].at[:, :, tok]

    def quad_copy(a, d):
        return remote(source(a, d), target(a, d), quad_s.at[a, d], quad_r.at[a, d], quad[d])

    def own_copy(a):
        return pltpu.make_async_copy(source(a, 0), target(a, 0), own_sem.at[a])

    sent = [(a, d) for a in range(3) for d in (1, 2, 3) if (a, d) != LATER]
    for a, d in sent:
        quad_copy(a, d).start()
    for a in range(3):
        own_copy(a).start()
    own_copy(0).wait()
    for d in (1, 2, 3):
        quad_copy(0, d).wait_recv()

    def pass_on(zz, k):
        block = kv_all.at[2 * zz + y]
        return remote(block, block, y_s.at[k], y_r.at[k], across)

    mine = kv_all.at[pair]
    to_z = [remote(mine, mine, z_s.at[k], z_r.at[k], dev(zz, y, x, core)) for k, zz in z_peers(z)]
    for c in to_z:
        c.start()
    pass_on(z, 0).start()
    came = [(k, lax.rem(z + 4 - k, 4)) for k in (1, 3, 2)]
    for k, zz in came:
        block = kv_all.at[2 * zz + y]
        remote(block, block, z_s.at[k], z_r.at[k], me).wait_recv()
        pass_on(zz, k).start()
    for k, zz in [(0, z)] + came:
        block = kv_all.at[2 * zz + 1 - y]
        remote(block, block, y_s.at[k], y_r.at[k], me).wait_recv()
        pass_on(zz, k).wait_send()
    for c in to_z:
        c.wait_send()
    for a, d in sent:
        quad_copy(a, d).wait_send()
        if a > 0:
            quad_copy(a, d).wait_recv()
    own_copy(1).wait()
    own_copy(2).wait()


def exchange(kv, q, dy):
    dma = pltpu.SemaphoreType.DMA
    vmem, hbm = pl.BlockSpec(memory_space=pltpu.VMEM), pl.BlockSpec(memory_space=pl.ANY)
    wide = q.shape[-1]
    return pl.pallas_call(
        exchange_kernel,
        name="exchange",
        out_shape=(
            jax.ShapeDtypeStruct((N_PAIRS,) + (2,) * 3 + (BLK, HEAD_DIM), BF16),
            jax.ShapeDtypeStruct((2, 2, BLK, wide), BF16),
            jax.ShapeDtypeStruct((2, 2, LATER[1] * CHUNK, 2 * wide), BF16),
        ),
        in_specs=[vmem] * 3,
        out_specs=[hbm] * 3,
        scratch_shapes=[dma((3,))] + [dma((3, 4))] * 2 + [dma((4,))] * 4,
        compiler_params=pltpu.CompilerParams(collective_id=1),
        cost_estimate=cost(1, 20),
    )(kv, q, dy)


def reduce_kernel(cuts, kinds, work, *refs):
    n = len(cuts)
    ins, refs = refs[:n], refs[n:]
    extra = work and work.ins
    more_in, refs = refs[: extra or 0], refs[extra or 0 :]
    outs, refs = refs[:n], refs[n:]
    more_out, refs = refs[: work.outs if work else 0], refs[work.outs if work else 0 :]
    own, from_core, from_y, from_z = refs[:n], refs[n : 2 * n], refs[2 * n : 3 * n], refs[3 * n : 4 * n]
    load_sem, core_s, core_r, y_s, y_r, z_s, z_r = refs[4 * n : 4 * n + 7]
    me = lax.axis_index("cp")
    z, y, x, core = place(me)
    partner, across = dev(z, y, x, 1 - core), dev(z, 1 - y, x, core)
    peers = [across, partner] + [dev(zz, y, x, core) for _, zz in z_peers(z)]
    meet(peers + (quad_of(me)[2:] if work else []))
    if work:
        job = Work(me, more_in, more_out, refs[4 * n + 7 :])
        job.send()

    def rows(i, j):
        size = from_z[i].shape[1] // cuts[i]
        return pl.ds(j * size, size)

    def mine(i, zz, at):
        return own[i].at[zz, y, at] if kinds[i] == "core" else own[i].at[zz, at]

    def load(i, j):
        src, at = ins[i], rows(i, j)
        src = {"core": lambda: src.at[core, :, :, at], "z": lambda: src.at[:, at], "": lambda: src.at[:, y, at]}[kinds[i]]()
        dst = own[i].at[:, :, at] if kinds[i] == "core" else own[i].at[:, at]
        return pltpu.make_async_copy(src, dst, load_sem.at[i, j])

    def core_copy(i, j):
        at = rows(i, j)
        return remote(ins[i].at[1 - core, :, :, at], from_core[i].at[:, :, at], core_s.at[i, j], core_r.at[i, j], partner)

    def y_copy(i, j):
        src = own[i] if kinds[i] == "core" else ins[i]
        at = rows(i, j)
        return remote(src.at[:, 1 - y, at], from_y[i].at[:, at], y_s.at[i, j], y_r.at[i, j], across)

    def z_copies(i, j):
        at = rows(i, j)
        for k, zz in z_peers(z):
            yield remote(
                mine(i, zz, at), from_z[i].at[k - 1, at], z_s.at[i, j, k - 1], z_r.at[i, j, k - 1], dev(zz, y, x, core)
            )

    pieces = [(i, j) for i in range(n) for j in range(cuts[i])]
    for i, j in pieces:
        load(i, j).start()
        if kinds[i] == "core":
            core_copy(i, j).start()
        elif not kinds[i]:
            y_copy(i, j).start()
    for i, j in pieces:
        load(i, j).wait()
        if kinds[i] == "z":
            for c in z_copies(i, j):
                c.start()
        if kinds[i] == "core":
            core_copy(i, j).wait_recv()
            at = rows(i, j)
            for zz in range(4):
                own[i][zz, :, at] += from_core[i][zz, :, at]
            y_copy(i, j).start()
    if work:
        job.run()
    for i, j in pieces:
        if kinds[i] != "z":
            y_copy(i, j).wait_recv()
            at = rows(i, j)
            for zz in range(4):
                mine(i, zz, at)[...] += from_y[i][zz, at]
            for c in z_copies(i, j):
                c.start()
    for i, j in pieces:
        at = rows(i, j)
        for c in z_copies(i, j):
            c.wait_recv()
        outs[i][at] = mine(i, z, at)[...] + sum(from_z[i][k, at] for k in range(3))
    for i, j in pieces:
        if kinds[i] == "core":
            core_copy(i, j).wait_send()
        if kinds[i] != "z":
            y_copy(i, j).wait_send()
        for c in z_copies(i, j):
            c.wait_send()
    if work:
        job.finish()


def quad_of(me):
    z, y, x, core = place(me)
    return [dev(z, y, 1 - x if d // 2 else x, 1 - core if d % 2 else core) for d in range(4)]


class Home:
    def __init__(self, me, src, out, own_sem, send, arrive):
        _, _, x, core = place(me)
        w = src.shape[-1]
        to = out.at[core, :, :, :, pl.ds(x * w, w)]

        def piece(d):
            return src.at[:, :, pl.ds(d * CHUNK, CHUNK)]

        self.own = pltpu.make_async_copy(piece(0), to, own_sem)
        self.copies = [remote(piece(d), to, send.at[d], arrive.at[d], quad_of(me)[d]) for d in (1, 2, 3)]

    def start(self):
        self.own.start()
        for c in self.copies:
            c.start()

    def wait_recv(self):
        self.own.wait()
        for c in self.copies:
            c.wait_recv()

    def wait_send(self):
        for c in self.copies:
            c.wait_send()


class Work:
    ins, outs = 5, 2

    def __init__(self, me, ins, outs, scratch):
        attn, dq, self.hidden, self.w_o, self.w_q = ins
        self.block_out, self.d_part = outs
        self.attn_home, self.dq_home, self.buf_o, self.buf_q, own_sem, quad_s, quad_r, self.w_sem = scratch
        self.homes = [
            Home(me, src, out, own_sem.at[i], quad_s.at[i], quad_r.at[i])
            for i, (src, out) in enumerate([(attn, self.attn_home), (dq, self.dq_home)])
        ]

    def send(self):
        for h in self.homes:
            h.start()

    def tiles(self, fetch, use):
        n = self.w_o.shape[0] // BLK
        fetch(0, 0).start()

        @pl.loop(0, n)
        def _(t):
            slot = lax.rem(t, 2)
            fetch(t, slot).wait()

            @pl.when(t + 1 < n)
            def _():
                fetch(t + 1, 1 - slot).start()

            use(pl.ds(pl.multiple_of(t * BLK, BLK), BLK), slot)

    def run(self):
        def cols(t):
            return pl.ds(pl.multiple_of(t * BLK, BLK), BLK)

        def fetch_o(t, slot):
            return pltpu.make_async_copy(self.w_o.at[:, cols(t)], self.buf_o.at[slot], self.w_sem.at[0, slot])

        def fetch_q(t, slot):
            return pltpu.make_async_copy(self.w_q.at[cols(t)], self.buf_q.at[slot], self.w_sem.at[1, slot])

        def project(at, slot):
            attn = self.attn_home[...].reshape(-1, self.w_o.shape[0])
            out = jnp.dot(attn, self.buf_o[slot], preferred_element_type=F32)
            self.block_out[:, at] = (self.hidden[:, at].astype(F32) + out).astype(BF16)

        def pull(at, slot):
            dq = self.dq_home[...].reshape(-1, self.w_o.shape[0])
            self.d_part[:, at] = dot_t(dq, self.buf_q[slot])

        self.homes[0].wait_recv()
        self.tiles(fetch_o, project)
        self.homes[1].wait_recv()
        self.tiles(fetch_q, pull)

    def finish(self):
        for h in self.homes:
            h.wait_send()


def reduce_pairs(arrays, cuts, kinds, collective_id, more=()):
    dma = pltpu.SemaphoreType.DMA
    vmem, hbm = pl.BlockSpec(memory_space=pltpu.VMEM), pl.BlockSpec(memory_space=pl.ANY)
    n, most = len(arrays), max(cuts)
    blocks = [a.shape[-2:] for a in arrays]
    own = [pltpu.VMEM(((4, 2) if k == "core" else (4,)) + b, F32) for b, k in zip(blocks, kinds)]
    unused = pltpu.VMEM((8, HEAD_DIM), F32)
    scratch = own + [o if k == "core" else unused for o, k in zip(own, kinds)]
    scratch += [unused if k == "z" else pltpu.VMEM((4,) + b, F32) for b, k in zip(blocks, kinds)]
    scratch += [pltpu.VMEM((3,) + b, F32) for b in blocks]
    scratch += [dma((n, most))] * 5 + [dma((n, most, 3))] * 2
    outs = [jax.ShapeDtypeStruct(b, F32) for b in blocks]
    if more:
        hidden, w_o = more[2:4]
        outs += [jax.ShapeDtypeStruct(hidden.shape, t) for t in (BF16, F32)]
        scratch += [pltpu.VMEM((2,) * 3 + (CHUNK, w_o.shape[0]), BF16)] * 2
        scratch += [pltpu.VMEM((2,) + b, BF16) for b in ((w_o.shape[0], BLK), (BLK, w_o.shape[0]))]
        scratch += [dma((2,)), dma((2, 4)), dma((2, 4)), dma((2, 2))]
    return pl.pallas_call(
        functools.partial(reduce_kernel, cuts, kinds, Work if more else None),
        name="reduce_pairs",
        out_shape=outs,
        in_specs=[hbm] * n + [vmem] * 3 * bool(more) + [hbm] * 2 * bool(more),
        out_specs=[vmem] * len(outs),
        scratch_shapes=scratch,
        compiler_params=params(60, collective_id=collective_id),
        cost_estimate=cost(1, 20),
    )(*arrays, *more)


def gather_kernel(*refs):
    shards, refs = refs[:4], refs[4:]
    dkv_ref, part_ref, wkv_ref, x_ref, dy_ref, gain_ref, *refs = refs
    outs, refs = refs[:4], refs[4:]
    dx_ref, dgain_ref, *refs = refs
    own_sem, zs, fs, ls, cs, zr, fr, lr, cr, dkv_home, terms, all_terms, home_own, home_s, home_r, g_s, g_r = refs
    me = lax.axis_index("cp")
    z, y, x, core = place(me)
    across = (dev(z, y, 1 - x, core), dev(z, 1 - y, x, core))
    partner = dev(z, y, x, 1 - core)
    others = [(i, me ^ i) for i in range(1, all_terms.shape[0])]
    meet([d for _, d in others])
    back = Home(me, dkv_ref, dkv_home, home_own, home_s, home_r)
    back.start()

    def windows(half, zz, yy, xx, cc):
        pair = 2 * zz + yy
        rows = shards[0].shape[0] // 2
        out_rows = pl.ds(((xx * 2 + cc) * N_PAIRS + pair) * 2 * rows + half * rows, rows)
        yield shards[0], pl.ds(half * rows, rows), outs[0].at[out_rows]
        rows = shards[1].shape[0] // 2
        out_rows = pl.ds((cc * N_PAIRS + pair) * 2 * rows + half * rows, rows)
        for s, o in zip(shards[1:], outs[1:]):
            yield s, pl.ds(half * rows, rows), o.at[out_rows, pl.ds(xx * s.shape[1], s.shape[1])]

    total = sum(s.size for s in shards) // 2 // outs[0].shape[1]
    whole = outs[0].at[pl.ds(0, total)]

    def flip(v, on):
        return 1 - v if on else v

    class Copy:
        def __init__(self, half, zz, first, last, send, arrive, to, is_own, cc=core):
            over_x, over_y = (first, last) if half == 0 else (last, first)
            self.at = half, zz, flip(y, over_y), flip(x, over_x), cc
            self.send, self.arrive, self.to, self.is_own = send, arrive, to, is_own

        def start(self):
            for shard, rows, window in windows(*self.at):
                remote(shard.at[rows] if self.is_own else window, window, self.send, self.arrive, self.to).start()

        def wait_recv(self):
            remote(whole, whole, self.send, self.arrive, me).wait_recv()

        def wait_send(self):
            remote(whole, whole, self.send, self.arrive, me).wait_send()

    places = [(0, z)] + [(k, lax.rem(z + 4 - k, 4)) for k in (1, 3, 2)]
    halves = range(2)

    def z_copy(half, k, zz):
        return Copy(half, z, 0, 0, zs.at[half, k], zr.at[half, k], dev(zz, y, x, core), True)

    def first_copy(half, k, zz):
        at = half, k
        return Copy(half, zz, 0, 0, fs.at[at], fr.at[at], across[half], k == 0)

    def last_copy(half, k, zz, first):
        at = half, first, k
        return Copy(half, zz, first, 0, ls.at[at], lr.at[at], across[1 - half], k == first == 0)

    def core_copy(half, k, zz, first, last):
        at = half, first, last, k
        return Copy(half, zz, first, last, cs.at[at], cr.at[at], partner, k == first == last == 0)

    def term_copy(i, d):
        return remote(terms, all_terms.at[i], g_s.at[i], g_r.at[i], d)

    owns = []
    for half in halves:
        for shard, rows, window in windows(half, z, y, x, core):
            owns.append(pltpu.make_async_copy(shard.at[rows], window, own_sem.at[len(owns)]))
    for k, zz in z_peers(z):
        for half in halves:
            z_copy(half, k, zz).start()
    for k, zz in places:
        for half in halves:
            if k > 0:
                z_copy(half, k, zz).wait_recv()
            first_copy(half, k, zz).start()
            last_copy(half, k, zz, 0).start()
            core_copy(half, k, zz, 0, 0).start()
        if k == 0:
            for o in owns:
                o.start()
            back.wait_recv()
            hidden_gradient(dkv_home, part_ref, wkv_ref, x_ref, dy_ref, gain_ref, dx_ref, terms)
            for i, d in others:
                term_copy(i, d).start()
        for half in halves:
            first_copy(half, k, zz).wait_recv()
            last_copy(half, k, zz, 1).start()
            core_copy(half, k, zz, 1, 0).start()
    for first in halves:
        for k, zz in places:
            for half in halves:
                last_copy(half, k, zz, first).wait_recv()
                core_copy(half, k, zz, first, 1).start()
    for o in owns:
        o.wait()
    for k, zz in z_peers(z):
        for half in halves:
            z_copy(half, k, zz).wait_send()
    total_gain = terms[...]
    for i, d in others:
        term_copy(i, d).wait_recv()
        total_gain += all_terms[i]
    dgain_ref[...] = total_gain
    for i, d in others:
        term_copy(i, d).wait_send()
    back.wait_send()
    for k, zz in places:
        for half in halves:
            first_copy(half, k, zz).wait_send()
            for first in halves:
                last_copy(half, k, zz, first).wait_send()
                for last in halves:
                    core_copy(half, k, zz, first, last).wait_recv()
                    core_copy(half, k, zz, first, last).wait_send()


def hidden_gradient(dkv_home, part_ref, wkv_ref, x_ref, dy_ref, gain_ref, dx_ref, terms):
    size = CHUNK
    gain = gain_ref[...]
    terms[...] = jnp.zeros_like(terms)

    @pl.loop(0, x_ref.shape[0] // size)
    def _(t):
        at = pl.ds(pl.multiple_of(t * size, size), size)
        dkv = dkv_home[t // 4, lax.rem(t // 2, 2), lax.rem(t, 2)]
        d = part_ref[at] + dot_t(dkv, wkv_ref[...])
        d = d.astype(BF16).astype(F32)
        x = x_ref[at].astype(F32)
        inv_rms = lax.rsqrt(row_mean(x * x) + NORM_EPS)
        unit, scaled = x * inv_rms, d * gain
        dx = inv_rms * (scaled - unit * row_mean(scaled * unit))
        dx_ref[at] = (dy_ref[at].astype(F32) + dx).astype(BF16)
        terms[...] += jnp.sum((d * unit).reshape((-1,) + terms.shape), axis=0)


def gather_all(shards, shapes, dkv, part, wkv, x, dy, gain):
    dma = pltpu.SemaphoreType.DMA
    vmem, hbm = pl.BlockSpec(memory_space=pltpu.VMEM), pl.BlockSpec(memory_space=pl.ANY)
    hops = [dma((2,) * i + (4,)) for i in (1, 1, 2, 3)]
    n = len(shards)
    terms = 8, x.shape[1]
    return pl.pallas_call(
        gather_kernel,
        name="gather_all",
        out_shape=[jax.ShapeDtypeStruct(s, F32) for s in shapes]
        + [jax.ShapeDtypeStruct(x.shape, BF16), jax.ShapeDtypeStruct(terms, F32)],
        in_specs=[vmem] * (n + 6),
        out_specs=[hbm] * n + [vmem] * 2,
        scratch_shapes=[dma((2 * n,))]
        + hops
        + hops
        + [pltpu.VMEM((2,) * 3 + (CHUNK, 2 * dkv.shape[-1]), BF16), pltpu.VMEM(terms, F32)]
        + [pltpu.VMEM((32,) + terms, F32), dma(()), dma((4,)), dma((4,)), dma((32,)), dma((32,))],
        compiler_params=params(40, collective_id=0),
        cost_estimate=cost(1, 76),
    )(*shards, dkv, part, wkv, x, dy, gain)


def perm(x, pairs):
    return lax.ppermute(x, "cp", pairs)


def flip_pairs(d):
    return [(r, r ^ d) for r in range(32)]


def solution(mesh):
    def local_step(hidden, grad_out, positions, seg_ids, w_q, w_k, w_v, w_o, norm_gain):
        n_batch, n_tok, d_model = hidden.shape
        n_rows = n_batch * n_tok
        wide = N_HEADS * HEAD_DIM
        me = lax.axis_index("cp")
        _, y, x, core = place(me)
        quad, pair = me % 4, me // 4
        relations = range(4)

        def rows_of(arr, d):
            return pick(arr.reshape((2, 2, 2, CHUNK) + arr.shape[2:]), core ^ (d % 2), 0)

        def swap(pieces):
            return [perm(p, flip_pairs(d)) if d else p for d, p in enumerate(pieces)]

        def unite(arr):
            joined = jnp.stack(swap([rows_of(arr, d) for d in relations]), axis=2)
            return joined.reshape((2, 2, BLK) + joined.shape[4:])

        gain = norm_gain.astype(F32)
        cos_t, sin_t = rope_tables(positions.reshape(n_rows))
        cos_f, sin_f = jnp.hstack([cos_t, cos_t]), jnp.hstack([-sin_t, sin_t])
        normed, kv_home, q_home = project(hidden.reshape(n_rows, d_model), gain[None], w_q, w_k, w_v, cos_f, sin_f)
        pos_u = unite(positions)
        kv_all, q_u, dy_part = exchange(
            kv_home.reshape((2,) * 5 + (CHUNK, HEAD_DIM)),
            q_home.reshape((2,) * 4 + (CHUNK, wide)),
            grad_out.reshape((2,) * 3 + (CHUNK, d_model)),
        )
        dy_last, dy_part = lax.optimization_barrier((rows_of(grad_out, LATER[1]), dy_part))
        dy_last = perm(dy_last, flip_pairs(LATER[1]))
        normed_home, dy_part = lax.optimization_barrier((normed.reshape(hidden.shape), dy_part))
        normed_u = unite(normed_home)

        member = quad ^ jnp.arange(4)
        front, back = ((m[:, None] * CHUNK + jnp.arange(CHUNK)[None]).reshape(BLK) for m in (member, 3 - member))
        offsets = jnp.stack([front, back]).astype(jnp.int32)
        own_super = jnp.stack([pair, N_SUPER - 1 - pair]).astype(jnp.int32)
        q_index = own_super[:, None] * BLK + offsets
        start = q_index[None] - pos_u
        koff = jnp.broadcast_to(offsets[:, :, None], (2, BLK, BLK))
        tab = jnp.concatenate(
            [own_super, (jnp.min(start, axis=-1) // BLK).reshape(-1), jnp.max(start, axis=-1).reshape(-1)]
        )
        start_r = start[:, :, None, :]
        q_index_r = jnp.broadcast_to(q_index[None, :, None, :], start_r.shape)
        cos_u, sin_u = rope_tables(pos_u)
        cos_ut, sin_ut = jnp.swapaxes(cos_u, 2, 3), jnp.swapaxes(sin_u, 2, 3)

        lanes = start.shape + (HEAD_DIM,)
        start_l, q_index_l = (jnp.broadcast_to(a[..., None], lanes) for a in (start, q_index[None]))
        attn_u, lse = flash_fwd(tab, q_u, kv_all, start_l, q_index_l, offsets[:, None])

        tok = tuple(range(3))
        half_wide = wide // 2
        dy_u = jnp.concatenate([dy_part, dy_last], axis=2)
        wo_send = dot(dyn(attn_u, (1 - core) * half_wide, half_wide, 3), dy_u, tok, tok)
        wo_sum = dot(dyn(attn_u, core * half_wide, half_wide, 3), dy_u, tok, tok) + perm(wo_send, flip_pairs(1))
        wo_sum = wo_sum.reshape(4, 2, half_wide // N_PAIRS, d_model)
        wo_y = perm(pick(wo_sum, 1 - y, 1), flip_pairs(4))

        d_attn = dot(dy_u, dyn(w_o, x * wide, wide, 0), (3,), (1,)).astype(BF16)
        d_attn, wo_sum = lax.optimization_barrier((d_attn, wo_sum))
        dq_u, dkv = flash_bwd(tab, q_u, d_attn, attn_u, kv_all, lse, start_r, q_index_r, koff, cos_ut, sin_ut)

        wo_sum = pick(wo_sum, y, 1) + wo_y
        half_model = d_model // 2

        def by_core(d_out):
            part = lax.optimization_barrier(dot(normed_u, d_out, tok, tok))
            return part.reshape(2, 4, 2, half_model // N_PAIRS, -1)

        x_flat = hidden.reshape(n_rows, d_model)
        dkv_own, wq_own, wo_own, block_out, d_part = reduce_pairs(
            [dkv.reshape(4, 2, -1, HEAD_DIM), by_core(dq_u), wo_sum], (4, 2, 1), ("", "core", "z"), 2, (attn_u, dq_u, x_flat, w_o, w_q)
        )
        dkv_own = dkv_own.reshape((2,) * 3 + (BLK, HEAD_DIM))
        dk_u = rotate(dkv_own[0] * ATTN_SCALE, cos_u, -sin_u).astype(BF16)
        dkv_u = jnp.concatenate([dk_u, dkv_own[1].astype(BF16)], axis=-1)
        (wkv_own,) = reduce_pairs([by_core(dkv_u)], (1,), ("core",), 3)

        wk_own, wv_own = jnp.split(wkv_own, 2, axis=1)
        w_kv = jnp.hstack([w[:, head_slice(i)] for i in range(2) for w in (w_k, w_v)])
        grad_wo, grad_wq, grad_wk, grad_wv, grad_x, d_gain = gather_all(
            [wo_own, wq_own, wk_own, wv_own],
            [w_o.shape, w_q.shape, w_k.shape, w_v.shape],
            dkv_u,
            d_part,
            w_kv,
            x_flat,
            grad_out.reshape(n_rows, d_model),
            gain[None],
        )
        block_out, grad_x = (a.reshape(hidden.shape) for a in (block_out, grad_x))
        return block_out, grad_x, grad_wq, grad_wk, grad_wv, grad_wo, jnp.sum(d_gain, axis=0)

    seq_spec = P(None, "cp", None)
    tok_spec = P(None, "cp")
    full_spec = P()
    return jax.shard_map(
        local_step,
        mesh=mesh,
        in_specs=(seq_spec, seq_spec, tok_spec, tok_spec, full_spec, full_spec, full_spec, full_spec, full_spec),
        out_specs=(seq_spec, seq_spec, full_spec, full_spec, full_spec, full_spec, full_spec),
        check_vma=False,
    )
```

```python
import functools

import jax
import jax.numpy as jnp
from jax import lax
from jax.experimental import pallas as pl
from jax.experimental.pallas import tpu as pltpu
from jax.sharding import PartitionSpec as P

HEAD_DIM = 128
NORM_EPS = 1e-5
ROPE_BASE = 500000.0
NEG_BIG = -1e30
LOG2E = 1.4426950408889634
ATTN_SCALE = HEAD_DIM**-0.5
EXP2_SCALE = ATTN_SCALE * LOG2E
CHUNK = 64
TWO = 2
NEW = jnp.newaxis
BLK = 4 * CHUNK
N_HEADS = 8
N_PAIRS = 8
N_SUPER = 2 * N_PAIRS
MESH = pl.DeviceIdType.MESH
ONE = pl.Squeezed()
LATER = 2, 3
PRODUCTS_AT = 3, 7
F32 = jnp.float32
BF16 = jnp.bfloat16

T_SQ, T_LO, T_MX = 0, 2, 6


def rope_tables(positions):
    inv_freq = ROPE_BASE ** (-jnp.arange(0, HEAD_DIM, TWO).astype(F32) / HEAD_DIM)
    angles = positions.astype(F32)[..., None] * inv_freq
    return jnp.cos(angles), jnp.sin(angles)


def rotate(x, cos_t, sin_t):
    a, b = x[..., : HEAD_DIM // TWO], x[..., HEAD_DIM // TWO :]
    return jnp.concatenate([a * cos_t - b * sin_t, b * cos_t + a * sin_t], axis=-1)


def dot(a, b, ca, cb):
    return lax.dot_general(a, b, ((ca, cb), ((), ())), preferred_element_type=F32)


def cost(gflop, mib):
    return pl.CostEstimate(flops=gflop * 10**9, bytes_accessed=mib << 20, transcendentals=0)


def params(mib, **more):
    return pltpu.CompilerParams(vmem_limit_bytes=mib << 20, **more)


def row_mean(x):
    return jnp.mean(x, axis=-1, keepdims=True)


def head(h):
    return pl.ds(h * HEAD_DIM, HEAD_DIM)


def head_slice(h):
    return slice(h * HEAD_DIM, (h + 1) * HEAD_DIM)


def dot_t(a, b):
    return dot(a, b, (1,), (1,))


def dyn(x, index, size, axis):
    return lax.dynamic_slice_in_dim(x, index, size, axis)


def pick(x, index, axis):
    return lax.dynamic_index_in_dim(x, index, axis, keepdims=False)


def steps(tab, body):
    b, hf = pl.program_id(0), pl.program_id(1)
    own, first, last_start = tab[T_SQ + hf], tab[T_LO + TWO * b + hf], tab[T_MX + TWO * b + hf]

    def step(s, carry):
        late = s >= N_PAIRS
        at = jnp.where(late, N_SUPER - 1 - s, s), late.astype(jnp.int32)
        full = jnp.logical_and(s < own, s * BLK >= last_start)
        pl.when(full)(lambda: body(s, at, False))
        pl.when(jnp.logical_not(full))(lambda: body(s, at, True))
        return carry

    lax.fori_loop(first, own + 1, step, 0)


def may_use(s, off, st_ref, qi_ref):
    return jnp.logical_and(off >= st_ref[...] - s * BLK, off <= qi_ref[...] - s * BLK)


def fwd_kernel(tab, q_ref, kv_ref, st_ref, qi_ref, ko_ref, o_ref, lse_ref, q_s, acc, m_s, l_s):
    m_s[...] = jnp.full_like(m_s, NEG_BIG)
    l_s[...] = jnp.zeros_like(l_s)
    acc[...] = jnp.zeros_like(acc)
    for h in range(N_HEADS):
        q_s[pl.ds(h * BLK, BLK)] = q_ref[:, head(h)]

    def body(s, at, masked):
        pair, hk = at
        k, v = kv_ref[pair, 0, hk], kv_ref[pair, 1, hk]
        if masked:
            off = ko_ref[hk] + s * BLK
            mask = [
                jnp.logical_and(off[:, lanes] >= st_ref[...], off[:, lanes] <= qi_ref[...])
                for lanes in (slice(HEAD_DIM), slice(HEAD_DIM, BLK))
            ]
        for h in range(N_HEADS):
            rows = pl.ds(h * BLK, BLK)
            sc = dot_t(q_s[rows], k)
            sc = [sc[:, :HEAD_DIM] * EXP2_SCALE, sc[:, HEAD_DIM:] * EXP2_SCALE]
            if masked:
                sc = [jnp.where(m, x, NEG_BIG) for m, x in zip(mask, sc)]
            m_old = m_s[rows]
            m_new = jnp.maximum(m_old, jnp.max(jnp.maximum(*sc), axis=1, keepdims=True))
            alpha = jnp.exp2(m_old - m_new)
            p = [jnp.exp2(x - m_new) for x in sc]
            m_s[rows] = m_new
            l_s[rows] = l_s[rows] * alpha + (p[0] + p[1])
            p = jnp.hstack([x.astype(BF16) for x in p])
            acc[rows] = acc[rows] * alpha + jnp.dot(p, v, preferred_element_type=F32)

    steps(tab, body)
    for h in range(N_HEADS):
        rows = pl.ds(h * BLK, BLK)
        total = jnp.sum(l_s[rows], axis=1, keepdims=True)
        o_ref[:, head(h)] = (acc[rows] / total).astype(BF16)
        lse_ref[h] = (m_s[rows] + jnp.log2(total)).T[:1]


def bwd_kernel(tab, q_ref, do_ref, o_ref, kv_ref, lse_ref, st_ref, qi_ref, ko_ref, cos_ref, sin_ref, dq_ref, dkv_ref, dq_acc, delta):
    dq_acc[...] = jnp.zeros_like(dq_acc)
    for h in range(N_HEADS):
        terms = do_ref[:, head(h)].astype(F32) * o_ref[:, head(h)].astype(F32)
        delta[h] = jnp.sum(terms.T, axis=0, keepdims=True)

    @pl.when(pl.program_id(1) == 0)
    def _():
        dkv_ref[...] = jnp.zeros_like(dkv_ref)

    def body(s, at, masked):
        pair, hk = at
        k = kv_ref[pair, 0, hk]
        v = kv_ref[pair, 1, hk]
        k_t = k.T
        mask = may_use(s, ko_ref[hk], st_ref, qi_ref) if masked else None
        dk = dv = jnp.zeros((BLK, HEAD_DIM), F32)
        for h in range(N_HEADS):
            q = q_ref[:, head(h)]
            do = do_ref[:, head(h)]
            p = jnp.exp2(dot_t(k, q) * EXP2_SCALE - lse_ref[h])
            if masked:
                p = jnp.where(mask, p, 0.0)
            ds = (p * (dot_t(v, do) - delta[h])).astype(BF16)
            dv += jnp.dot(p.astype(BF16), do, preferred_element_type=F32)
            dk += jnp.dot(ds, q, preferred_element_type=F32)
            dq_acc[h] += jnp.dot(k_t, ds, preferred_element_type=F32)
        dkv_ref[pair, 0, hk] += dk
        dkv_ref[pair, 1, hk] += dv

    steps(tab, body)
    cos_t, sin_t = cos_ref[...], sin_ref[...]
    half = HEAD_DIM // TWO
    for h in range(N_HEADS):
        a, c = dq_acc[h, :half] * ATTN_SCALE, dq_acc[h, half:] * ATTN_SCALE
        lin = jnp.concatenate([a * cos_t + c * sin_t, c * cos_t - a * sin_t], axis=0)
        dq_ref[:, head(h)] = lin.T.astype(BF16)


def attn_specs():
    def at_tile(b, h, t):
        return (b, h) + (0,) * TWO

    def at_row(b, h, t):
        return (0, 0, b) + (0,) * 3

    tile = pl.BlockSpec((ONE, ONE, BLK, N_HEADS * HEAD_DIM), at_tile)
    row = pl.BlockSpec((ONE, ONE, 1, BLK), at_tile)
    stat = pl.BlockSpec((ONE, ONE, N_HEADS, 1, BLK), lambda b, h, t: (b, h) + (0,) * 3)
    rope = pl.BlockSpec((ONE, ONE, HEAD_DIM // TWO, BLK), at_tile)
    kv = pl.BlockSpec((N_PAIRS, TWO, ONE, TWO, BLK, HEAD_DIM), at_row)
    ko = pl.BlockSpec((TWO, BLK, BLK), lambda b, h, t: (0,) * 3)
    return tile, row, stat, kv, ko, rope


def flash_fwd(tab, q, kv, start, qidx, koff):
    tile, _, stat, kvs, *_ = attn_specs()
    col = pl.BlockSpec((ONE, ONE, BLK, HEAD_DIM), lambda b, h, t: (b, h) + (0,) * TWO)
    ko = pl.BlockSpec((TWO, 1, BLK), lambda b, h, t: (0,) * 3)
    return pl.pallas_call(
        fwd_kernel,
        name="attn_fwd",
        out_shape=(jax.ShapeDtypeStruct(q.shape, BF16), jax.ShapeDtypeStruct((TWO, TWO, N_HEADS, 1, BLK), F32)),
        grid_spec=pltpu.PrefetchScalarGridSpec(
            num_scalar_prefetch=1,
            grid=(TWO, TWO),
            in_specs=[tile, kvs, col, col, ko],
            out_specs=[tile, stat],
            scratch_shapes=[pltpu.VMEM((N_HEADS * BLK, HEAD_DIM), t) for t in (BF16, F32, F32, F32)],
        ),
        compiler_params=params(40),
        cost_estimate=cost(20, 16),
    )(tab, q, kv, start, qidx, koff)


def flash_bwd(tab, q, do, o, kv, lse, start, qidx, koff, cos_t, sin_t):
    tile, row, stat, kvs, ko, rope = attn_specs()
    return pl.pallas_call(
        bwd_kernel,
        name="attn_bwd",
        out_shape=(
            jax.ShapeDtypeStruct(q.shape, BF16),
            jax.ShapeDtypeStruct(kv.shape, F32),
        ),
        grid_spec=pltpu.PrefetchScalarGridSpec(
            num_scalar_prefetch=1,
            grid=(TWO, TWO),
            in_specs=[tile, tile, tile, kvs, stat, row, row, ko, rope, rope],
            out_specs=[tile, kvs],
            scratch_shapes=[pltpu.VMEM((N_HEADS, HEAD_DIM, BLK), F32), pltpu.VMEM((N_HEADS, 1, BLK), F32)],
        ),
        compiler_params=params(48),
        cost_estimate=cost(50, 32),
    )(tab, q, do, o, kv, lse, start, qidx, koff, cos_t, sin_t)


def turn(x, cos_ref, sin_ref):
    return x * cos_ref[...] + pltpu.roll(x, HEAD_DIM // TWO, 1) * sin_ref[...]


def first_kernel(x_ref, g_ref, wk_ref, wv_ref, cos_ref, sin_ref, h_ref, kv_ref):
    x = x_ref[...].astype(F32)
    h = (x * lax.rsqrt(row_mean(x * x) + NORM_EPS) * g_ref[...]).astype(BF16)
    h_ref[...] = h
    k = jnp.dot(h, wk_ref[...], preferred_element_type=F32)
    v = jnp.dot(h, wv_ref[...], preferred_element_type=F32)
    n = kv_ref.shape[3]
    for i in range(TWO):
        for j, val in enumerate((turn(k[:, head_slice(i)], cos_ref, sin_ref), v[:, head_slice(i)])):
            for c in range(TWO):
                kv_ref[i, c, j] = val[c * n : (c + 1) * n].astype(BF16)


def query_kernel(h_ref, w_ref, cos_ref, sin_ref, q_ref):
    q = jnp.dot(h_ref[...], w_ref[...], preferred_element_type=F32)
    n = q_ref.shape[TWO]
    for j in range(q.shape[1] // HEAD_DIM):
        val = turn(q[:, head_slice(j)], cos_ref, sin_ref).astype(BF16)
        for c in range(TWO):
            q_ref[0, c, :, head(j)] = val[c * n : (c + 1) * n]


def project(x, gain, w_q, w_k, w_v, cos_f, sin_f):
    n, d = x.shape
    h, kv = pl.pallas_call(
        first_kernel,
        name="norm_kv",
        out_shape=(jax.ShapeDtypeStruct(x.shape, BF16), jax.ShapeDtypeStruct((TWO,) * 3 + (n // TWO, HEAD_DIM), BF16)),
        compiler_params=params(40),
        cost_estimate=cost(TWO, 7),
    )(x, gain, w_k, w_v, cos_f, sin_f)
    tile = 4 * HEAD_DIM
    rope = pl.BlockSpec(cos_f.shape, lambda j: (0, 0))
    q = pl.pallas_call(
        query_kernel,
        name="query",
        grid=(d // tile,),
        out_shape=jax.ShapeDtypeStruct((TWO, TWO, n // TWO, d // TWO), BF16),
        in_specs=[pl.BlockSpec(h.shape, lambda j: (0, 0)), pl.BlockSpec((d, tile), lambda j: (0, j)), rope, rope],
        out_specs=pl.BlockSpec((1, TWO, n // TWO, tile), lambda j: (j // TWO, 0, 0, j % TWO)),
        compiler_params=params(40),
        cost_estimate=cost(5, 12),
    )(h, w_q, cos_f, sin_f)
    return h, kv, q


def place(me):
    return me // 8, lax.rem(me // 4, TWO), lax.rem(me // TWO, TWO), lax.rem(me, TWO)


def dev(z, y, x, core):
    return ((z * TWO + y) * TWO + x) * TWO + core


def z_peers(z):
    return [(k, lax.rem(z + k, 4)) for k in (1, TWO, 3)]


def meet(peers):
    barrier = pltpu.get_barrier_semaphore()
    for d in peers:
        pl.semaphore_signal(barrier, device_id=(d,), device_id_type=MESH)
    pl.semaphore_wait(barrier, len(peers))


def remote(src, dst, send, arrive, to):
    return pltpu.make_async_remote_copy(
        src_ref=src, dst_ref=dst, send_sem=send, recv_sem=arrive, device_id=(to,), device_id_type=MESH
    )


class Line:
    order = (0, 1, -1, TWO, -TWO, 3, -3)

    def __init__(self, me):
        self.z, y, x, core = place(me)
        self.next = {1: dev(self.z + 1, y, x, core), -1: dev(self.z - 1, y, x, core)}
        self.inside = {1: self.z < 3, -1: self.z > 0}

    def held(self, dz):
        return jnp.logical_and(self.z + dz >= 0, self.z + dz <= 3)

    def ways(self, dz):
        for d in self.next:
            if d * dz <= 0:
                yield d, self.inside[d] if dz == 0 else jnp.logical_and(self.inside[d], self.held(dz))


def exchange_kernel(kv_ref, q_ref, dy_ref, kv_all, q_u, dy_u, own_sem, quad_s, quad_r, z_s, z_r, y_s, y_r):
    me = lax.axis_index("cp")
    z, y, x, core = place(me)
    quad, line = quad_of(me), Line(me)
    across = dev(z, 1 - y, x, core)
    meet(quad[1:] + [across] + [dev(zz, y, x, core) for _, zz in z_peers(z)])

    def source(a, d):
        xx, cc = 1 - x if d // TWO else x, 1 - core if d % TWO else core
        return dy_ref.at[cc] if a == TWO else (kv_ref, q_ref)[a].at[xx, cc]

    def target(a, d):
        tok = pl.ds(d * CHUNK, CHUNK)
        return kv_all.at[me // 4, :, :, :, tok] if a == 0 else (q_u, dy_u)[a - 1].at[:, :, tok]

    def quad_copy(a, d):
        return remote(source(a, d), target(a, d), quad_s.at[a, d], quad_r.at[a, d], quad[d])

    def own_copy(a):
        return pltpu.make_async_copy(source(a, 0), target(a, 0), own_sem.at[a])

    sent = [(a, d) for a in range(3) for d in (1, TWO, 3) if (a, d) != LATER]
    for a, d in sent:
        quad_copy(a, d).start()
    for a in range(3):
        own_copy(a).start()
    own_copy(0).wait()
    for d in (1, TWO, 3):
        quad_copy(0, d).wait_recv()

    def z_copy(part, dz, d):
        block = kv_all.at[TWO * (z + dz) + y, part]
        return remote(block, block, z_s.at[part, (d + 1) // TWO, dz + 3], z_r.at[part, dz - d + 3], line.next[d])

    def y_copy(part, dz, yy=y):
        block = kv_all.at[TWO * (z + dz) + yy, part]
        return remote(block, block, y_s.at[part, dz + 3], y_r.at[part, dz + 3], across)

    parts = range(TWO)
    moves = [(part, dz) for dz in line.order for part in parts]
    for part, dz in moves:
        if dz:
            block = kv_all.at[TWO * (z + dz) + y, part]
            arrival = remote(block, block, own_sem.at[0], z_r.at[part, dz + 3], me)
            pl.when(line.held(dz))(arrival.wait_recv)
        for d, on in line.ways(dz):
            pl.when(on)(z_copy(part, dz, d).start)
        pl.when(line.held(dz))(y_copy(part, dz).start)
    for part, dz in moves:
        for d, on in line.ways(dz):
            pl.when(on)(z_copy(part, dz, d).wait_send)
        pl.when(line.held(dz))(y_copy(part, dz, 1 - y).wait_recv)
        pl.when(line.held(dz))(y_copy(part, dz).wait_send)
    for a, d in sent:
        quad_copy(a, d).wait_send()
        if a > 0:
            quad_copy(a, d).wait_recv()
    own_copy(1).wait()
    own_copy(TWO).wait()


def exchange(kv, q, dy):
    dma = pltpu.SemaphoreType.DMA
    vmem, hbm = pl.BlockSpec(memory_space=pltpu.VMEM), pl.BlockSpec(memory_space=pl.ANY)
    wide = q.shape[-1]
    return pl.pallas_call(
        exchange_kernel,
        name="exchange",
        out_shape=(
            jax.ShapeDtypeStruct((N_PAIRS,) + (TWO,) * 3 + (BLK, HEAD_DIM), BF16),
            jax.ShapeDtypeStruct((TWO, TWO, BLK, wide), BF16),
            jax.ShapeDtypeStruct((TWO, TWO, LATER[1] * CHUNK, TWO * wide), BF16),
        ),
        in_specs=[vmem] * 3,
        out_specs=[hbm] * 3,
        scratch_shapes=[dma((3,))] + [dma((3, 4))] * TWO + [dma((TWO, TWO, 7))] + [dma((TWO, 7))] * 3,
        compiler_params=pltpu.CompilerParams(collective_id=1),
        cost_estimate=cost(1, 20),
    )(kv, q, dy)


def reduce_kernel(cuts, kinds, work, *refs):
    n = len(cuts)

    def take(count):
        nonlocal refs
        first, refs = refs[:count], refs[count:]
        return first

    ins, more_in, outs, more_out = take(n), take(work.ins), take(n), take(work.outs)
    own, from_core, from_y, from_z = take(n), take(n), take(n), take(n)
    load_sem, core_s, core_r, y_s, y_r, z_s, z_r = take(7)
    me = lax.axis_index("cp")
    z, y, x, core = place(me)
    partner, across = dev(z, y, x, 1 - core), dev(z, 1 - y, x, core)
    next_z = dev(z + 1, y, x, core), dev(z - 1, y, x, core)
    meet(quad_of(me)[1:] + [across] + [dev(zz, y, x, core) for _, zz in z_peers(z)])
    job = work(me, more_in, more_out, refs)

    def rows(i, j):
        size = outs[i].shape[0] // cuts[i]
        return pl.ds(j * size, size)

    def mine(i, j, zz):
        at = rows(i, j)
        return own[i].at[zz, y, at] if kinds[i] == "core" else own[i].at[zz, at]

    def load(i, j):
        src, at = ins[i], rows(i, j)
        src = {"core": lambda: src.at[core, :, :, at], "z": lambda: src.at[:, at], "": lambda: src.at[:, y, at]}[kinds[i]]()
        dst = own[i].at[:, :, at] if kinds[i] == "core" else own[i].at[:, at]
        return pltpu.make_async_copy(src, dst, load_sem.at[i, j])

    def core_copy(i, j):
        at = rows(i, j)
        return remote(ins[i].at[1 - core, :, :, at], from_core[i].at[:, :, at], core_s.at[i, j], core_r.at[i, j], partner)

    def y_copy(i, j):
        src = own[i] if kinds[i] == "core" else ins[i]
        at = rows(i, j)
        return remote(src.at[:, 1 - y, at], from_y[i].at[:, at], y_s.at[i, j], y_r.at[i, j], across)

    def z_copy(i, j, way, zz, to):
        at = way, zz + way - 1
        return remote(mine(i, j, zz), from_z[i].at[*at, rows(i, j)], z_s.at[i, j, *at], z_r.at[i, j, *at], to)

    def relay(i, j, way, zz, add):
        if add:
            z_copy(i, j, way, zz, me).wait_recv()
            mine(i, j, zz)[...] += from_z[i][way, zz + way - 1, rows(i, j)]
        z_copy(i, j, way, zz, next_z[way]).start()

    def hop(i, j, h):
        @pl.when(z == h)
        def _():
            for zz in range(3, h, -1):
                relay(i, j, 0, zz, h > 0)

        @pl.when(z == 3 - h)
        def _():
            for zz in range(3 - h):
                relay(i, j, 1, zz, h > 0)

    def across_y(i, j):
        if kinds[i] != "z":
            y_copy(i, j).wait_recv()
            for zz in range(4):
                mine(i, j, zz)[...] += from_y[i][zz, rows(i, j)]

    def last(i, j):
        at = rows(i, j)
        outs[i][at] = mine(i, j, z)[...]
        for way, on in enumerate((z > 0, z < 3)):

            @pl.when(on)
            def _(way=way):
                z_copy(i, j, way, z, me).wait_recv()
                outs[i][at] += from_z[i][way, z + way - 1, at]

    pieces = [(i, j) for i in range(n) for j in range(cuts[i])]
    for i, j in pieces:
        load(i, j).start()
        if kinds[i] == "core":
            core_copy(i, j).start()
        elif not kinds[i]:
            y_copy(i, j).start()
    for i, j in pieces:
        load(i, j).wait()
        if kinds[i] == "core":
            core_copy(i, j).wait_recv()
            at = rows(i, j)
            for zz in range(4):
                own[i][zz, :, at] += from_core[i][zz, :, at]
            y_copy(i, j).start()
        if kinds[i] == "z":
            hop(i, j, 0)
    for t in range(len(pieces) + 3):
        for h, (i, j) in enumerate(reversed(pieces[max(t - 3, 0) : t + 1]), max(t + 1 - len(pieces), 0)):
            if h == 0:
                across_y(i, j)
            if h == 3:
                last(i, j)
            elif h > 0 or kinds[i] != "z":
                hop(i, j, h)
        job.step(t)
    for i, j in pieces:
        if kinds[i] == "core":
            core_copy(i, j).wait_send()
        if kinds[i] != "z":
            y_copy(i, j).wait_send()
        for zz in range(4):
            if zz > 0:
                pl.when(z < zz)(z_copy(i, j, 0, zz, next_z[0]).wait_send)
            if zz < 3:
                pl.when(z > zz)(z_copy(i, j, 1, zz, next_z[1]).wait_send)
    job.finish()


def quad_of(me):
    z, y, x, core = place(me)
    return [dev(z, y, 1 - x if d // TWO else x, 1 - core if d % TWO else core) for d in range(4)]


class Home:
    def __init__(self, me, src, out, own_sem, send, arrive):
        _, _, x, core = place(me)
        w = src.shape[-1]
        to = out.at[core, :, :, :, pl.ds(x * w, w)]

        def piece(d):
            return src.at[:, :, pl.ds(d * CHUNK, CHUNK)]

        self.own = pltpu.make_async_copy(piece(0), to, own_sem)
        self.copies = [remote(piece(d), to, send.at[d], arrive.at[d], quad_of(me)[d]) for d in (1, TWO, 3)]

    def start(self):
        self.own.start()
        for c in self.copies:
            c.start()

    def wait_recv(self):
        self.own.wait()
        for c in self.copies:
            c.wait_recv()

    def wait_send(self):
        for c in self.copies:
            c.wait_send()


class Products:
    ins, outs = 5, TWO

    def __init__(self, me, ins, outs, scratch):
        attn, dq, self.hidden, self.w_o, self.w_q = ins
        self.block_out, self.d_part = outs
        self.attn_home, self.dq_home, self.buf_o, self.buf_q, own_sem, quad_s, quad_r, self.w_sem = scratch
        self.homes = [
            Home(me, src, out, own_sem.at[i], quad_s.at[i], quad_r.at[i])
            for i, (src, out) in enumerate([(attn, self.attn_home), (dq, self.dq_home)])
        ]
        for h in self.homes:
            h.start()

    @staticmethod
    def scratch(arrays):
        dma, d = pltpu.SemaphoreType.DMA, arrays[3].shape[0]
        home = pltpu.VMEM((TWO,) * 3 + (CHUNK, d), BF16)
        buf = [pltpu.VMEM((TWO,) + b, BF16) for b in ((d, BLK), (BLK, d))]
        return [home] * TWO + buf + [dma((TWO,)), dma((TWO, 4)), dma((TWO, 4)), dma((TWO, TWO))]

    @staticmethod
    def results(arrays):
        return [jax.ShapeDtypeStruct(arrays[TWO].shape, t) for t in (BF16, F32)]

    spaces = [pltpu.VMEM] * 3 + [pl.ANY] * TWO

    def tiles(self, fetch, use):
        n = self.w_o.shape[0] // BLK
        fetch(0, 0).start()

        @pl.loop(0, n)
        def _(t):
            slot = lax.rem(t, TWO)
            fetch(t, slot).wait()

            @pl.when(t + 1 < n)
            def _():
                fetch(t + 1, 1 - slot).start()

            use(pl.ds(pl.multiple_of(t * BLK, BLK), BLK), slot)

    def step(self, t):
        def cols(t):
            return pl.ds(pl.multiple_of(t * BLK, BLK), BLK)

        def fetch_o(t, slot):
            return pltpu.make_async_copy(self.w_o.at[:, cols(t)], self.buf_o.at[slot], self.w_sem.at[0, slot])

        def fetch_q(t, slot):
            return pltpu.make_async_copy(self.w_q.at[cols(t)], self.buf_q.at[slot], self.w_sem.at[1, slot])

        def project(at, slot):
            attn = self.attn_home[...].reshape(-1, self.w_o.shape[0])
            out = jnp.dot(attn, self.buf_o[slot], preferred_element_type=F32)
            self.block_out[:, at] = (self.hidden[:, at].astype(F32) + out).astype(BF16)

        def pull(at, slot):
            dq = self.dq_home[...].reshape(-1, self.w_o.shape[0])
            self.d_part[:, at] = dot_t(dq, self.buf_q[slot])

        if t in PRODUCTS_AT:
            i = PRODUCTS_AT.index(t)
            self.homes[i].wait_recv()
            self.tiles(*((fetch_o, project), (fetch_q, pull))[i])

    def finish(self):
        for h in self.homes:
            h.wait_send()


class HiddenGradient:
    ins, outs = 6, TWO

    def __init__(self, me, ins, outs, scratch):
        dkv, self.part, self.w_kv, self.x, self.dy, self.gain = ins
        self.dx, self.terms = outs
        self.dkv_home, self.rows, *sems = scratch
        self.home = Home(me, dkv, self.dkv_home, *sems)
        self.home.start()

    @staticmethod
    def scratch(arrays):
        dma = pltpu.SemaphoreType.DMA
        dkv, x = arrays[0], arrays[3]
        home = pltpu.VMEM((TWO,) * 3 + (CHUNK, TWO * dkv.shape[-1]), BF16)
        return [home, pltpu.VMEM((8, x.shape[1]), F32), dma(()), dma((4,)), dma((4,))]

    @staticmethod
    def results(arrays):
        x = arrays[3]
        return [jax.ShapeDtypeStruct(x.shape, BF16), jax.ShapeDtypeStruct((1, x.shape[1]), F32)]

    spaces = [pltpu.VMEM] * 6

    def step(self, t):
        if t == 0:
            self.home.wait_recv()
            self.rows[...] = jnp.zeros_like(self.rows)
            pl.loop(0, 4)(self.tile)
            self.terms[...] = jnp.sum(self.rows[...], axis=0, keepdims=True)

    def tile(self, t):
        size = TWO * CHUNK
        at = pl.ds(pl.multiple_of(t * size, size), size)
        dkv = self.dkv_home[t // TWO, lax.rem(t, TWO)].reshape(size, -1)
        d = self.part[at] + dot_t(dkv, self.w_kv[...])
        d = d.astype(BF16).astype(F32)
        x = self.x[at].astype(F32)
        inv_rms = lax.rsqrt(row_mean(x * x) + NORM_EPS)
        unit, scaled = x * inv_rms, d * self.gain[...]
        dx = inv_rms * (scaled - unit * row_mean(scaled * unit))
        self.dx[at] = (self.dy[at].astype(F32) + dx).astype(BF16)
        self.rows[...] += jnp.sum((d * unit).reshape((-1,) + self.rows.shape), axis=0)

    def finish(self):
        self.home.wait_send()


def reduce_pairs(arrays, cuts, kinds, collective_id, work, more):
    dma = pltpu.SemaphoreType.DMA
    n, most = len(arrays), max(cuts)
    blocks = [a.shape[-TWO:] for a in arrays]
    own = [pltpu.VMEM(((4, TWO) if k == "core" else (4,)) + b, F32) for b, k in zip(blocks, kinds)]
    unused = pltpu.VMEM((8, HEAD_DIM), F32)
    scratch = own + [o if k == "core" else unused for o, k in zip(own, kinds)]
    scratch += [unused if k == "z" else pltpu.VMEM((4,) + b, F32) for b, k in zip(blocks, kinds)]
    scratch += [pltpu.VMEM((TWO, 3) + b, F32) for b in blocks]
    scratch += [dma((n, most))] * 5 + [dma((n, most, TWO, 3))] * TWO
    outs = [jax.ShapeDtypeStruct(b, F32) for b in blocks] + work.results(more)
    return pl.pallas_call(
        functools.partial(reduce_kernel, cuts, kinds, work),
        name="reduce_pairs",
        out_shape=outs,
        in_specs=[pl.BlockSpec(memory_space=m) for m in [pl.ANY] * n + work.spaces],
        out_specs=[pl.BlockSpec(memory_space=pltpu.VMEM)] * len(outs),
        scratch_shapes=scratch + work.scratch(more),
        compiler_params=params(60, collective_id=collective_id),
        cost_estimate=cost(1, 20),
    )(*arrays, *more)


def gather_kernel(*refs):
    shards, refs = refs[:4], refs[4:]
    terms, *outs, dgain_ref = refs[:6]
    own_sem, zs, fs, ls, cs, zr, fr, lr, cr, all_terms, g_s, g_r = refs[6:]
    me = lax.axis_index("cp")
    z, y, x, core = place(me)
    across = (dev(z, y, 1 - x, core), dev(z, 1 - y, x, core))
    partner = dev(z, y, x, 1 - core)
    others = [(i, me ^ i) for i in range(1, all_terms.shape[0])]
    meet([d for _, d in others])

    def windows(half, zz, yy, xx, cc):
        pair = TWO * zz + yy
        rows = shards[0].shape[0] // TWO
        out_rows = pl.ds(((xx * TWO + cc) * N_PAIRS + pair) * TWO * rows + half * rows, rows)
        yield shards[0], pl.ds(half * rows, rows), outs[0].at[out_rows]
        rows = shards[1].shape[0] // TWO
        out_rows = pl.ds((cc * N_PAIRS + pair) * TWO * rows + half * rows, rows)
        for s, o in zip(shards[1:], outs[1:]):
            yield s, pl.ds(half * rows, rows), o.at[out_rows, pl.ds(xx * s.shape[1], s.shape[1])]

    total = sum(s.size for s in shards) // TWO // outs[0].shape[1]
    whole = outs[0].at[pl.ds(0, total)]

    def flip(v, on):
        return 1 - v if on else v

    class Copy:
        def __init__(self, half, zz, first, last, send, arrive, to, is_own, cc=core):
            over_x, over_y = (first, last) if half == 0 else (last, first)
            self.at = half, zz, flip(y, over_y), flip(x, over_x), cc
            self.send, self.arrive, self.to, self.is_own = send, arrive, to, is_own

        def start(self):
            for shard, rows, window in windows(*self.at):
                remote(shard.at[rows] if self.is_own else window, window, self.send, self.arrive, self.to).start()

        def wait_recv(self):
            remote(whole, whole, self.send, self.arrive, me).wait_recv()

        def wait_send(self):
            remote(whole, whole, self.send, self.arrive, me).wait_send()

    places = [(0, z)] + [(k, lax.rem(z + 4 - k, 4)) for k in (1, 3, TWO)]
    halves = range(TWO)

    def z_copy(half, k, zz):
        return Copy(half, z, 0, 0, zs.at[half, k], zr.at[half, k], dev(zz, y, x, core), True)

    def first_copy(half, k, zz):
        at = half, k
        return Copy(half, zz, 0, 0, fs.at[at], fr.at[at], across[half], k == 0)

    def last_copy(half, k, zz, first):
        at = half, first, k
        return Copy(half, zz, first, 0, ls.at[at], lr.at[at], across[1 - half], k == first == 0)

    def core_copy(half, k, zz, first, last):
        at = half, first, last, k
        return Copy(half, zz, first, last, cs.at[at], cr.at[at], partner, k == first == last == 0)

    def term_copy(i, d):
        return remote(terms, all_terms.at[i], g_s.at[i], g_r.at[i], d)

    owns = []
    for half in halves:
        for shard, rows, window in windows(half, z, y, x, core):
            owns.append(pltpu.make_async_copy(shard.at[rows], window, own_sem.at[len(owns)]))
    for k, zz in z_peers(z):
        for half in halves:
            z_copy(half, k, zz).start()
    for k, zz in places:
        for half in halves:
            if k > 0:
                z_copy(half, k, zz).wait_recv()
            first_copy(half, k, zz).start()
            last_copy(half, k, zz, 0).start()
            core_copy(half, k, zz, 0, 0).start()
        if k == 0:
            for o in owns:
                o.start()
            for i, d in others:
                term_copy(i, d).start()
        for half in halves:
            first_copy(half, k, zz).wait_recv()
            last_copy(half, k, zz, 1).start()
            core_copy(half, k, zz, 1, 0).start()
    for first in halves:
        for k, zz in places:
            for half in halves:
                last_copy(half, k, zz, first).wait_recv()
                core_copy(half, k, zz, first, 1).start()
    for o in owns:
        o.wait()
    for k, zz in z_peers(z):
        for half in halves:
            z_copy(half, k, zz).wait_send()
    total_gain = terms[...]
    for i, d in others:
        term_copy(i, d).wait_recv()
        total_gain += all_terms[i]
    dgain_ref[...] = total_gain
    for i, d in others:
        term_copy(i, d).wait_send()
    for k, zz in places:
        for half in halves:
            first_copy(half, k, zz).wait_send()
            for first in halves:
                last_copy(half, k, zz, first).wait_send()
                for last in halves:
                    core_copy(half, k, zz, first, last).wait_recv()
                    core_copy(half, k, zz, first, last).wait_send()


def gather_all(shards, shapes, terms):
    dma = pltpu.SemaphoreType.DMA
    vmem, hbm = pl.BlockSpec(memory_space=pltpu.VMEM), pl.BlockSpec(memory_space=pl.ANY)
    hops = [dma((TWO,) * i + (4,)) for i in (1, 1, TWO, 3)]
    n = len(shards)
    return pl.pallas_call(
        gather_kernel,
        name="gather_all",
        out_shape=[jax.ShapeDtypeStruct(s, F32) for s in shapes + [terms.shape]],
        in_specs=[vmem] * (n + 1),
        out_specs=[hbm] * n + [vmem],
        scratch_shapes=[dma((TWO * n,))] + hops + hops + [pltpu.VMEM((32,) + terms.shape, F32), dma((32,)), dma((32,))],
        compiler_params=pltpu.CompilerParams(collective_id=0),
        cost_estimate=cost(1, 76),
    )(*shards, terms)


def perm(x, pairs):
    return lax.ppermute(x, "cp", pairs)


def flip_pairs(d):
    return [(r, r ^ d) for r in range(32)]


def solution(mesh):
    def local_step(hidden, grad_out, positions, seg_ids, w_q, w_k, w_v, w_o, norm_gain):
        n_batch, n_tok, d_model = hidden.shape
        n_rows = n_batch * n_tok
        wide = N_HEADS * HEAD_DIM
        me = lax.axis_index("cp")
        _, y, x, core = place(me)
        quad, pair = me % 4, me // 4
        relations = range(4)

        def rows_of(arr, d):
            return pick(arr.reshape((TWO, TWO, TWO, CHUNK) + arr.shape[TWO:]), core ^ (d % TWO), 0)

        def swap(pieces):
            return [perm(p, flip_pairs(d)) if d else p for d, p in enumerate(pieces)]

        def unite(arr):
            joined = jnp.stack(swap([rows_of(arr, d) for d in relations]), axis=TWO)
            return joined.reshape((TWO, TWO, BLK) + joined.shape[4:])

        gain = norm_gain.astype(F32)
        cos_t, sin_t = rope_tables(positions.reshape(n_rows))
        cos_f, sin_f = jnp.hstack([cos_t, cos_t]), jnp.hstack([-sin_t, sin_t])
        normed, kv_home, q_home = project(hidden.reshape(n_rows, d_model), gain[NEW], w_q, w_k, w_v, cos_f, sin_f)
        pos_u = unite(positions)
        kv_all, q_u, dy_part = exchange(
            kv_home.reshape((TWO,) * 5 + (CHUNK, HEAD_DIM)),
            q_home.reshape((TWO,) * 4 + (CHUNK, wide)),
            grad_out.reshape((TWO,) * 3 + (CHUNK, d_model)),
        )
        dy_last, dy_part = lax.optimization_barrier((rows_of(grad_out, LATER[1]), dy_part))
        dy_last = perm(dy_last, flip_pairs(LATER[1]))
        normed_home, dy_part = lax.optimization_barrier((normed.reshape(hidden.shape), dy_part))
        normed_u = unite(normed_home)

        member = quad ^ jnp.arange(4)
        front, back = ((m[:, NEW] * CHUNK + jnp.arange(CHUNK)[NEW]).reshape(BLK) for m in (member, 3 - member))
        offsets = jnp.stack([front, back]).astype(jnp.int32)
        own_super = jnp.stack([pair, N_SUPER - 1 - pair]).astype(jnp.int32)
        q_index = own_super[:, NEW] * BLK + offsets
        start = q_index[NEW] - pos_u
        koff = jnp.broadcast_to(offsets[:, :, NEW], (TWO, BLK, BLK))
        tab = jnp.concatenate(
            [own_super, (jnp.min(start, axis=-1) // BLK).reshape(-1), jnp.max(start, axis=-1).reshape(-1)]
        )
        start_r = start[:, :, NEW, :]
        q_index_r = jnp.broadcast_to(q_index[NEW, :, NEW, :], start_r.shape)
        cos_u, sin_u = rope_tables(pos_u)
        cos_ut, sin_ut = jnp.swapaxes(cos_u, TWO, 3), jnp.swapaxes(sin_u, TWO, 3)

        lanes = start.shape + (HEAD_DIM,)
        start_l, q_index_l = (jnp.broadcast_to(a[..., NEW], lanes) for a in (start, q_index[NEW]))
        attn_u, lse = flash_fwd(tab, q_u, kv_all, start_l, q_index_l, offsets[:, NEW])

        tok = tuple(range(3))
        half_wide = wide // TWO
        dy_u = jnp.concatenate([dy_part, dy_last], axis=TWO)
        wo_send = dot(dyn(attn_u, (1 - core) * half_wide, half_wide, 3), dy_u, tok, tok)
        wo_sum = dot(dyn(attn_u, core * half_wide, half_wide, 3), dy_u, tok, tok) + perm(wo_send, flip_pairs(1))
        wo_sum = wo_sum.reshape(4, TWO, half_wide // N_PAIRS, d_model)
        wo_y = perm(pick(wo_sum, 1 - y, 1), flip_pairs(4))

        d_attn = dot(dy_u, dyn(w_o, x * wide, wide, 0), (3,), (1,)).astype(BF16)
        d_attn, wo_sum = lax.optimization_barrier((d_attn, wo_sum))
        dq_u, dkv = flash_bwd(tab, q_u, d_attn, attn_u, kv_all, lse, start_r, q_index_r, koff, cos_ut, sin_ut)

        wo_sum = pick(wo_sum, y, 1) + wo_y
        half_model = d_model // TWO

        def by_core(d_out):
            part = lax.optimization_barrier(dot(normed_u, d_out, tok, tok))
            return part.reshape(TWO, 4, TWO, half_model // N_PAIRS, -1)

        x_flat = hidden.reshape(n_rows, d_model)
        wo_own, dkv_own, wq_own, block_out, d_part = reduce_pairs(
            [wo_sum, dkv.reshape(4, TWO, -1, HEAD_DIM), by_core(dq_u)],
            (TWO, 8, 4),
            ("z", "", "core"),
            TWO,
            Products,
            (attn_u, dq_u, x_flat, w_o, w_q),
        )
        dkv_own = dkv_own.reshape((TWO,) * 3 + (BLK, HEAD_DIM))
        dk_u = rotate(dkv_own[0] * ATTN_SCALE, cos_u, -sin_u).astype(BF16)
        dkv_u = jnp.concatenate([dk_u, dkv_own[1].astype(BF16)], axis=-1)
        w_kv = jnp.hstack([w[:, head_slice(i)] for i in range(TWO) for w in (w_k, w_v)])
        more = dkv_u, d_part, w_kv, x_flat, grad_out.reshape(n_rows, d_model), gain[NEW]
        wkv_own, grad_x, terms = reduce_pairs([by_core(dkv_u)], (TWO,), ("core",), 3, HiddenGradient, more)

        wk_own, wv_own = jnp.split(wkv_own, TWO, axis=1)
        grad_wo, grad_wq, grad_wk, grad_wv, d_gain = gather_all(
            [wo_own, wq_own, wk_own, wv_own], [w_o.shape, w_q.shape, w_k.shape, w_v.shape], terms
        )
        block_out, grad_x = (a.reshape(hidden.shape) for a in (block_out, grad_x))
        return block_out, grad_x, grad_wq, grad_wk, grad_wv, grad_wo, d_gain.reshape(d_model)

    seq_spec = P(None, "cp", None)
    tok_spec = P(None, "cp")
    full_spec = P()
    return jax.shard_map(
        local_step,
        mesh=mesh,
        in_specs=(seq_spec, seq_spec, tok_spec, tok_spec, full_spec, full_spec, full_spec, full_spec, full_spec),
        out_specs=(seq_spec, seq_spec, full_spec, full_spec, full_spec, full_spec, full_spec),
        check_vma=False,
    )
```

```python
import functools
import heapq

import jax
import jax.numpy as jnp
from jax import lax
from jax.experimental import pallas as pl
from jax.experimental.pallas import tpu as pltpu
from jax.sharding import PartitionSpec as P

HEAD_DIM = 128
NORM_EPS = 1e-5
ROPE_BASE = 500000.0
NEG_BIG = -1e30
LOG2E = 1.4426950408889634
ATTN_SCALE = HEAD_DIM**-0.5
EXP2_SCALE = ATTN_SCALE * LOG2E
CHUNK = 64
TWO = 2
NEW = jnp.newaxis
BLK = 4 * CHUNK
N_HEADS = 8
N_PAIRS = 8
N_SUPER = 2 * N_PAIRS
MESH = pl.DeviceIdType.MESH
ONE = pl.Squeezed()
LATER = 2, 3
PRODUCTS_AT = 3, 7
F32 = jnp.float32
BF16 = jnp.bfloat16

T_SQ, T_LO, T_MX = 0, 2, 6


def rope_tables(positions):
    inv_freq = ROPE_BASE ** (-jnp.arange(0, HEAD_DIM, TWO).astype(F32) / HEAD_DIM)
    angles = positions.astype(F32)[..., None] * inv_freq
    return jnp.cos(angles), jnp.sin(angles)


def rotate(x, cos_t, sin_t):
    a, b = x[..., : HEAD_DIM // TWO], x[..., HEAD_DIM // TWO :]
    return jnp.concatenate([a * cos_t - b * sin_t, b * cos_t + a * sin_t], axis=-1)


def dot(a, b, ca, cb):
    return lax.dot_general(a, b, ((ca, cb), ((), ())), preferred_element_type=F32)


def cost(gflop, mib):
    return pl.CostEstimate(flops=gflop * 10**9, bytes_accessed=mib << 20, transcendentals=0)


def params(mib, **more):
    return pltpu.CompilerParams(vmem_limit_bytes=mib << 20, **more)


def row_mean(x):
    return jnp.mean(x, axis=-1, keepdims=True)


def head(h):
    return pl.ds(h * HEAD_DIM, HEAD_DIM)


def head_slice(h):
    return slice(h * HEAD_DIM, (h + 1) * HEAD_DIM)


def dot_t(a, b):
    return dot(a, b, (1,), (1,))


def dyn(x, index, size, axis):
    return lax.dynamic_slice_in_dim(x, index, size, axis)


def pick(x, index, axis):
    return lax.dynamic_index_in_dim(x, index, axis, keepdims=False)


def steps(tab, body):
    b, hf = pl.program_id(0), pl.program_id(1)
    own, first, last_start = tab[T_SQ + hf], tab[T_LO + TWO * b + hf], tab[T_MX + TWO * b + hf]

    def step(s, carry):
        late = s >= N_PAIRS
        at = jnp.where(late, N_SUPER - 1 - s, s), late.astype(jnp.int32)
        full = jnp.logical_and(s < own, s * BLK >= last_start)
        pl.when(full)(lambda: body(s, at, False))
        pl.when(jnp.logical_not(full))(lambda: body(s, at, True))
        return carry

    lax.fori_loop(first, own + 1, step, 0)


def may_use(s, off, st_ref, qi_ref):
    return jnp.logical_and(off >= st_ref[...] - s * BLK, off <= qi_ref[...] - s * BLK)


def fwd_kernel(tab, q_ref, kv_ref, st_ref, qi_ref, ko_ref, o_ref, lse_ref, q_s, acc, m_s, l_s):
    m_s[...] = jnp.full_like(m_s, NEG_BIG)
    l_s[...] = jnp.zeros_like(l_s)
    acc[...] = jnp.zeros_like(acc)
    for h in range(N_HEADS):
        q_s[pl.ds(h * BLK, BLK)] = q_ref[:, head(h)]

    def body(s, at, masked):
        pair, hk = at
        k, v = kv_ref[pair, 0, hk], kv_ref[pair, 1, hk]
        if masked:
            off = ko_ref[hk] + s * BLK
            mask = [
                jnp.logical_and(off[:, lanes] >= st_ref[...], off[:, lanes] <= qi_ref[...])
                for lanes in (slice(HEAD_DIM), slice(HEAD_DIM, BLK))
            ]
        for h in range(N_HEADS):
            rows = pl.ds(h * BLK, BLK)
            sc = dot_t(q_s[rows], k)
            sc = [sc[:, :HEAD_DIM] * EXP2_SCALE, sc[:, HEAD_DIM:] * EXP2_SCALE]
            if masked:
                sc = [jnp.where(m, x, NEG_BIG) for m, x in zip(mask, sc)]
            m_old = m_s[rows]
            m_new = jnp.maximum(m_old, jnp.max(jnp.maximum(*sc), axis=1, keepdims=True))
            alpha = jnp.exp2(m_old - m_new)
            p = [jnp.exp2(x - m_new) for x in sc]
            m_s[rows] = m_new
            l_s[rows] = l_s[rows] * alpha + (p[0] + p[1])
            p = jnp.hstack([x.astype(BF16) for x in p])
            acc[rows] = acc[rows] * alpha + jnp.dot(p, v, preferred_element_type=F32)

    steps(tab, body)
    for h in range(N_HEADS):
        rows = pl.ds(h * BLK, BLK)
        total = jnp.sum(l_s[rows], axis=1, keepdims=True)
        o_ref[:, head(h)] = (acc[rows] / total).astype(BF16)
        lse_ref[h] = (m_s[rows] + jnp.log2(total)).T[:1]


def bwd_kernel(tab, q_ref, do_ref, o_ref, kv_ref, lse_ref, st_ref, qi_ref, ko_ref, cos_ref, sin_ref, dq_ref, dkv_ref, dq_acc, delta):
    dq_acc[...] = jnp.zeros_like(dq_acc)
    for h in range(N_HEADS):
        terms = do_ref[:, head(h)].astype(F32) * o_ref[:, head(h)].astype(F32)
        delta[h] = jnp.sum(terms.T, axis=0, keepdims=True)

    @pl.when(pl.program_id(1) == 0)
    def _():
        dkv_ref[...] = jnp.zeros_like(dkv_ref)

    def body(s, at, masked):
        pair, hk = at
        k = kv_ref[pair, 0, hk]
        v = kv_ref[pair, 1, hk]
        k_t = k.T
        mask = may_use(s, ko_ref[hk], st_ref, qi_ref) if masked else None
        dk = dv = jnp.zeros((BLK, HEAD_DIM), F32)
        for h in range(N_HEADS):
            q = q_ref[:, head(h)]
            do = do_ref[:, head(h)]
            p = jnp.exp2(dot_t(k, q) * EXP2_SCALE - lse_ref[h])
            if masked:
                p = jnp.where(mask, p, 0.0)
            ds = (p * (dot_t(v, do) - delta[h])).astype(BF16)
            dv += jnp.dot(p.astype(BF16), do, preferred_element_type=F32)
            dk += jnp.dot(ds, q, preferred_element_type=F32)
            dq_acc[h] += jnp.dot(k_t, ds, preferred_element_type=F32)
        dkv_ref[pair, 0, hk] += dk
        dkv_ref[pair, 1, hk] += dv

    steps(tab, body)
    cos_t, sin_t = cos_ref[...], sin_ref[...]
    half = HEAD_DIM // TWO
    for h in range(N_HEADS):
        a, c = dq_acc[h, :half] * ATTN_SCALE, dq_acc[h, half:] * ATTN_SCALE
        lin = jnp.concatenate([a * cos_t + c * sin_t, c * cos_t - a * sin_t], axis=0)
        dq_ref[:, head(h)] = lin.T.astype(BF16)


def attn_specs():
    def at_tile(b, h, t):
        return (b, h) + (0,) * TWO

    def at_row(b, h, t):
        return (0, 0, b) + (0,) * 3

    tile = pl.BlockSpec((ONE, ONE, BLK, N_HEADS * HEAD_DIM), at_tile)
    row = pl.BlockSpec((ONE, ONE, 1, BLK), at_tile)
    stat = pl.BlockSpec((ONE, ONE, N_HEADS, 1, BLK), lambda b, h, t: (b, h) + (0,) * 3)
    rope = pl.BlockSpec((ONE, ONE, HEAD_DIM // TWO, BLK), at_tile)
    kv = pl.BlockSpec((N_PAIRS, TWO, ONE, TWO, BLK, HEAD_DIM), at_row)
    ko = pl.BlockSpec((TWO, BLK, BLK), lambda b, h, t: (0,) * 3)
    return tile, row, stat, kv, ko, rope


def flash_fwd(tab, q, kv, start, qidx, koff):
    tile, _, stat, kvs, *_ = attn_specs()
    col = pl.BlockSpec((ONE, ONE, BLK, HEAD_DIM), lambda b, h, t: (b, h) + (0,) * TWO)
    ko = pl.BlockSpec((TWO, 1, BLK), lambda b, h, t: (0,) * 3)
    return pl.pallas_call(
        fwd_kernel,
        name="attn_fwd",
        out_shape=(jax.ShapeDtypeStruct(q.shape, BF16), jax.ShapeDtypeStruct((TWO, TWO, N_HEADS, 1, BLK), F32)),
        grid_spec=pltpu.PrefetchScalarGridSpec(
            num_scalar_prefetch=1,
            grid=(TWO, TWO),
            in_specs=[tile, kvs, col, col, ko],
            out_specs=[tile, stat],
            scratch_shapes=[pltpu.VMEM((N_HEADS * BLK, HEAD_DIM), t) for t in (BF16, F32, F32, F32)],
        ),
        compiler_params=params(40),
        cost_estimate=cost(20, 16),
    )(tab, q, kv, start, qidx, koff)


def flash_bwd(tab, q, do, o, kv, lse, start, qidx, koff, cos_t, sin_t):
    tile, row, stat, kvs, ko, rope = attn_specs()
    return pl.pallas_call(
        bwd_kernel,
        name="attn_bwd",
        out_shape=(
            jax.ShapeDtypeStruct(q.shape, BF16),
            jax.ShapeDtypeStruct(kv.shape, F32),
        ),
        grid_spec=pltpu.PrefetchScalarGridSpec(
            num_scalar_prefetch=1,
            grid=(TWO, TWO),
            in_specs=[tile, tile, tile, kvs, stat, row, row, ko, rope, rope],
            out_specs=[tile, kvs],
            scratch_shapes=[pltpu.VMEM((N_HEADS, HEAD_DIM, BLK), F32), pltpu.VMEM((N_HEADS, 1, BLK), F32)],
        ),
        compiler_params=params(48),
        cost_estimate=cost(50, 32),
    )(tab, q, do, o, kv, lse, start, qidx, koff, cos_t, sin_t)


def turn(x, cos_ref, sin_ref):
    return x * cos_ref[...] + pltpu.roll(x, HEAD_DIM // TWO, 1) * sin_ref[...]


def first_kernel(x_ref, g_ref, wk_ref, wv_ref, cos_ref, sin_ref, h_ref, kv_ref):
    x = x_ref[...].astype(F32)
    h = (x * lax.rsqrt(row_mean(x * x) + NORM_EPS) * g_ref[...]).astype(BF16)
    h_ref[...] = h
    k = jnp.dot(h, wk_ref[...], preferred_element_type=F32)
    v = jnp.dot(h, wv_ref[...], preferred_element_type=F32)
    n = kv_ref.shape[3]
    for i in range(TWO):
        for j, val in enumerate((turn(k[:, head_slice(i)], cos_ref, sin_ref), v[:, head_slice(i)])):
            for c in range(TWO):
                kv_ref[i, c, j] = val[c * n : (c + 1) * n].astype(BF16)


def query_kernel(h_ref, w_ref, cos_ref, sin_ref, q_ref):
    q = jnp.dot(h_ref[...], w_ref[...], preferred_element_type=F32)
    n = q_ref.shape[TWO]
    for j in range(q.shape[1] // HEAD_DIM):
        val = turn(q[:, head_slice(j)], cos_ref, sin_ref).astype(BF16)
        for c in range(TWO):
            q_ref[0, c, :, head(j)] = val[c * n : (c + 1) * n]


def project(x, gain, w_q, w_k, w_v, cos_f, sin_f):
    n, d = x.shape
    h, kv = pl.pallas_call(
        first_kernel,
        name="norm_kv",
        out_shape=(jax.ShapeDtypeStruct(x.shape, BF16), jax.ShapeDtypeStruct((TWO,) * 3 + (n // TWO, HEAD_DIM), BF16)),
        compiler_params=params(40),
        cost_estimate=cost(TWO, 7),
    )(x, gain, w_k, w_v, cos_f, sin_f)
    tile = 4 * HEAD_DIM
    rope = pl.BlockSpec(cos_f.shape, lambda j: (0, 0))
    q = pl.pallas_call(
        query_kernel,
        name="query",
        grid=(d // tile,),
        out_shape=jax.ShapeDtypeStruct((TWO, TWO, n // TWO, d // TWO), BF16),
        in_specs=[pl.BlockSpec(h.shape, lambda j: (0, 0)), pl.BlockSpec((d, tile), lambda j: (0, j)), rope, rope],
        out_specs=pl.BlockSpec((1, TWO, n // TWO, tile), lambda j: (j // TWO, 0, 0, j % TWO)),
        compiler_params=params(40),
        cost_estimate=cost(5, 12),
    )(h, w_q, cos_f, sin_f)
    return h, kv, q


def place(me):
    return me // 8, lax.rem(me // 4, TWO), lax.rem(me // TWO, TWO), lax.rem(me, TWO)


def dev(z, y, x, core):
    return ((z * TWO + y) * TWO + x) * TWO + core


def z_peers(z):
    return [(k, lax.rem(z + k, 4)) for k in (1, TWO, 3)]


def meet(peers):
    barrier = pltpu.get_barrier_semaphore()
    for d in peers:
        pl.semaphore_signal(barrier, device_id=(d,), device_id_type=MESH)
    pl.semaphore_wait(barrier, len(peers))


def remote(src, dst, send, arrive, to):
    return pltpu.make_async_remote_copy(
        src_ref=src, dst_ref=dst, send_sem=send, recv_sem=arrive, device_id=(to,), device_id_type=MESH
    )


class Line:
    order = (0, 1, -1, TWO, -TWO, 3, -3)

    def __init__(self, me):
        self.z, y, x, core = place(me)
        self.next = {1: dev(self.z + 1, y, x, core), -1: dev(self.z - 1, y, x, core)}
        self.inside = {1: self.z < 3, -1: self.z > 0}

    def held(self, dz):
        return jnp.logical_and(self.z + dz >= 0, self.z + dz <= 3)

    def ways(self, dz):
        for d in self.next:
            if d * dz <= 0:
                yield d, self.inside[d] if dz == 0 else jnp.logical_and(self.inside[d], self.held(dz))


def exchange_kernel(kv_ref, q_ref, dy_ref, kv_all, q_u, dy_u, own_sem, quad_s, quad_r, z_s, z_r, y_s, y_r):
    me = lax.axis_index("cp")
    z, y, x, core = place(me)
    quad, line = quad_of(me), Line(me)
    across = dev(z, 1 - y, x, core)
    meet(quad[1:] + [across] + [dev(zz, y, x, core) for _, zz in z_peers(z)])

    def source(a, d):
        xx, cc = 1 - x if d // TWO else x, 1 - core if d % TWO else core
        return dy_ref.at[cc] if a == TWO else (kv_ref, q_ref)[a].at[xx, cc]

    def target(a, d):
        tok = pl.ds(d * CHUNK, CHUNK)
        return kv_all.at[me // 4, :, :, :, tok] if a == 0 else (q_u, dy_u)[a - 1].at[:, :, tok]

    def quad_copy(a, d):
        return remote(source(a, d), target(a, d), quad_s.at[a, d], quad_r.at[a, d], quad[d])

    def own_copy(a):
        return pltpu.make_async_copy(source(a, 0), target(a, 0), own_sem.at[a])

    sent = [(a, d) for a in range(3) for d in (1, TWO, 3) if (a, d) != LATER]
    for a, d in sent:
        quad_copy(a, d).start()
    for a in range(3):
        own_copy(a).start()
    own_copy(0).wait()
    for d in (1, TWO, 3):
        quad_copy(0, d).wait_recv()

    def z_copy(part, dz, d):
        block = kv_all.at[TWO * (z + dz) + y, part]
        return remote(block, block, z_s.at[part, (d + 1) // TWO, dz + 3], z_r.at[part, dz - d + 3], line.next[d])

    def y_copy(part, dz, yy=y):
        block = kv_all.at[TWO * (z + dz) + yy, part]
        return remote(block, block, y_s.at[part, dz + 3], y_r.at[part, dz + 3], across)

    parts = range(TWO)
    moves = [(part, dz) for dz in line.order for part in parts]
    for part, dz in moves:
        if dz:
            block = kv_all.at[TWO * (z + dz) + y, part]
            arrival = remote(block, block, own_sem.at[0], z_r.at[part, dz + 3], me)
            pl.when(line.held(dz))(arrival.wait_recv)
        for d, on in line.ways(dz):
            pl.when(on)(z_copy(part, dz, d).start)
        pl.when(line.held(dz))(y_copy(part, dz).start)
    for part, dz in moves:
        for d, on in line.ways(dz):
            pl.when(on)(z_copy(part, dz, d).wait_send)
        pl.when(line.held(dz))(y_copy(part, dz, 1 - y).wait_recv)
        pl.when(line.held(dz))(y_copy(part, dz).wait_send)
    for a, d in sent:
        quad_copy(a, d).wait_send()
        if a > 0:
            quad_copy(a, d).wait_recv()
    own_copy(1).wait()
    own_copy(TWO).wait()


def exchange(kv, q, dy):
    dma = pltpu.SemaphoreType.DMA
    vmem, hbm = pl.BlockSpec(memory_space=pltpu.VMEM), pl.BlockSpec(memory_space=pl.ANY)
    wide = q.shape[-1]
    return pl.pallas_call(
        exchange_kernel,
        name="exchange",
        out_shape=(
            jax.ShapeDtypeStruct((N_PAIRS,) + (TWO,) * 3 + (BLK, HEAD_DIM), BF16),
            jax.ShapeDtypeStruct((TWO, TWO, BLK, wide), BF16),
            jax.ShapeDtypeStruct((TWO, TWO, LATER[1] * CHUNK, TWO * wide), BF16),
        ),
        in_specs=[vmem] * 3,
        out_specs=[hbm] * 3,
        scratch_shapes=[dma((3,))] + [dma((3, 4))] * TWO + [dma((TWO, TWO, 7))] + [dma((TWO, 7))] * 3,
        compiler_params=pltpu.CompilerParams(collective_id=1),
        cost_estimate=cost(1, 20),
    )(kv, q, dy)


class PairSum:
    def __init__(self, me, kind, cut, src, out, buffers, sems):
        self.me, self.kind, self.src, self.out = me, kind, src, out
        self.size = out.shape[0] // cut
        self.own, self.from_core, self.from_y, self.from_z = buffers
        self.load_sem, self.core_s, self.core_r, self.y_s, self.y_r, self.z_s, self.z_r = sems
        self.z, self.y, x, core = place(me)
        self.core, self.partner = core, dev(self.z, self.y, x, 1 - core)
        self.across = dev(self.z, 1 - self.y, x, core)
        self.next_z = dev(self.z + 1, self.y, x, core), dev(self.z - 1, self.y, x, core)

    def rows(self, j):
        return pl.ds(j * self.size, self.size)

    def mine(self, j, zz):
        at = self.rows(j)
        return self.own.at[zz, self.y, at] if self.kind == "core" else self.own.at[zz, at]

    def load(self, j):
        src, at = self.src, self.rows(j)
        if self.kind == "core":
            src, dst = src.at[self.core, :, :, at], self.own.at[:, :, at]
        else:
            src, dst = (src.at[:, at] if self.kind else src.at[:, self.y, at]), self.own.at[:, at]
        return pltpu.make_async_copy(src, dst, self.load_sem.at[j])

    def core_copy(self, j):
        src, dst = (r.at[:, :, self.rows(j)] for r in (self.src.at[1 - self.core], self.from_core))
        return remote(src, dst, self.core_s.at[j], self.core_r.at[j], self.partner)

    def y_copy(self, j):
        src = self.own if self.kind == "core" else self.src
        at = self.rows(j)
        return remote(src.at[:, 1 - self.y, at], self.from_y.at[:, at], self.y_s.at[j], self.y_r.at[j], self.across)

    def z_copy(self, j, way, zz, to):
        at = way, zz + way - 1
        return remote(self.mine(j, zz), self.from_z.at[*at, self.rows(j)], self.z_s.at[j, *at], self.z_r.at[j, *at], to)

    def begin(self, j):
        self.load(j).start()
        if self.kind == "core":
            self.core_copy(j).start()
        elif not self.kind:
            self.y_copy(j).start()

    def loaded(self, j):
        self.load(j).wait()
        if self.kind == "core":
            self.core_copy(j).wait_recv()
            at = self.rows(j)
            for zz in range(4):
                self.own[zz, :, at] += self.from_core[zz, :, at]
            self.y_copy(j).start()
        if self.kind == "z":
            self.hop(j, 0)

    def relay(self, j, way, zz, add):
        if add:
            self.z_copy(j, way, zz, self.me).wait_recv()
            self.mine(j, zz)[...] += self.from_z[way, zz + way - 1, self.rows(j)]
        self.z_copy(j, way, zz, self.next_z[way]).start()

    def hop(self, j, h):
        @pl.when(self.z == h)
        def _():
            for zz in range(3, h, -1):
                self.relay(j, 0, zz, h > 0)

        @pl.when(self.z == 3 - h)
        def _():
            for zz in range(3 - h):
                self.relay(j, 1, zz, h > 0)

    def step(self, j, h):
        if h == 0 and self.kind != "z":
            self.y_copy(j).wait_recv()
            for zz in range(4):
                self.mine(j, zz)[...] += self.from_y[zz, self.rows(j)]
            self.hop(j, 0)
        elif 0 < h < 3:
            self.hop(j, h)
        elif h == 3:
            at = self.rows(j)
            self.out[at] = self.mine(j, self.z)[...]
            for way, on in enumerate((self.z > 0, self.z < 3)):

                @pl.when(on)
                def _(way=way):
                    self.z_copy(j, way, self.z, self.me).wait_recv()
                    self.out[at] += self.from_z[way, self.z + way - 1, at]

    def wait_send(self, j):
        if self.kind == "core":
            self.core_copy(j).wait_send()
        if self.kind != "z":
            self.y_copy(j).wait_send()
        for zz in range(4):
            if zz > 0:
                pl.when(self.z < zz)(self.z_copy(j, 0, zz, self.next_z[0]).wait_send)
            if zz < 3:
                pl.when(self.z > zz)(self.z_copy(j, 1, zz, self.next_z[1]).wait_send)

    @staticmethod
    def scratch(kind, block):
        unused = pltpu.VMEM((8, HEAD_DIM), F32)
        own = pltpu.VMEM(((4, TWO) if kind == "core" else (4,)) + block, F32)
        from_y = unused if kind == "z" else pltpu.VMEM((4,) + block, F32)
        return [own, own if kind == "core" else unused, from_y, pltpu.VMEM((TWO, 3) + block, F32)]

    @staticmethod
    def sems(*dims):
        dma = pltpu.SemaphoreType.DMA
        return [dma(dims)] * 5 + [dma(dims + (TWO, 3))] * TWO


def reduce_kernel(cuts, kinds, work, *refs):
    n = len(cuts)

    def take(count):
        nonlocal refs
        first, refs = refs[:count], refs[count:]
        return first

    ins, more_in, outs, more_out = take(n), take(work.ins), take(n), take(work.outs)
    buffers, sems = [take(4) for _ in kinds], take(7)
    me = lax.axis_index("cp")
    z, y, x, core = place(me)
    meet(quad_of(me)[1:] + [dev(z, 1 - y, x, core)] + [dev(zz, y, x, core) for _, zz in z_peers(z)])
    job = work(me, more_in, more_out, refs)
    sums = [PairSum(me, *a, [r.at[i] for r in sems]) for i, a in enumerate(zip(kinds, cuts, ins, outs, buffers))]
    pieces = [(s, j) for s, cut in zip(sums, cuts) for j in range(cut)]
    for s, j in pieces:
        s.begin(j)
    for s, j in pieces:
        s.loaded(j)
    for t in range(len(pieces) + 3):
        for h in range(4):
            if 0 <= t - h < len(pieces):
                s, j = pieces[t - h]
                s.step(j, h)
        job.step(t)
    for s, j in pieces:
        s.wait_send(j)
    job.finish()


def quad_of(me):
    z, y, x, core = place(me)
    return [dev(z, y, 1 - x if d // TWO else x, 1 - core if d % TWO else core) for d in range(4)]


class Home:
    def __init__(self, me, src, out, own_sem, send, arrive):
        _, _, x, core = place(me)
        w = src.shape[-1]
        to = out.at[core, :, :, :, pl.ds(x * w, w)]

        def piece(d):
            return src.at[:, :, pl.ds(d * CHUNK, CHUNK)]

        self.own = pltpu.make_async_copy(piece(0), to, own_sem)
        self.copies = [remote(piece(d), to, send.at[d], arrive.at[d], quad_of(me)[d]) for d in (1, TWO, 3)]

    def start(self):
        self.own.start()
        for c in self.copies:
            c.start()

    def wait_recv(self):
        self.own.wait()
        for c in self.copies:
            c.wait_recv()

    def wait_send(self):
        for c in self.copies:
            c.wait_send()


class Products:
    ins, outs = 5, TWO

    def __init__(self, me, ins, outs, scratch):
        attn, dq, self.hidden, self.w_o, self.w_q = ins
        self.block_out, self.d_part = outs
        self.attn_home, self.dq_home, self.buf_o, self.buf_q, own_sem, quad_s, quad_r, self.w_sem = scratch
        self.homes = [
            Home(me, src, out, own_sem.at[i], quad_s.at[i], quad_r.at[i])
            for i, (src, out) in enumerate([(attn, self.attn_home), (dq, self.dq_home)])
        ]
        for h in self.homes:
            h.start()

    @staticmethod
    def scratch(arrays):
        dma, d = pltpu.SemaphoreType.DMA, arrays[3].shape[0]
        home = pltpu.VMEM((TWO,) * 3 + (CHUNK, d), BF16)
        buf = [pltpu.VMEM((TWO,) + b, BF16) for b in ((d, BLK), (BLK, d))]
        return [home] * TWO + buf + [dma((TWO,)), dma((TWO, 4)), dma((TWO, 4)), dma((TWO, TWO))]

    @staticmethod
    def results(arrays):
        return [jax.ShapeDtypeStruct(arrays[TWO].shape, t) for t in (BF16, F32)]

    spaces = [pltpu.VMEM] * 3 + [pl.ANY] * TWO

    def tiles(self, fetch, use):
        n = self.w_o.shape[0] // BLK
        fetch(0, 0).start()

        @pl.loop(0, n)
        def _(t):
            slot = lax.rem(t, TWO)
            fetch(t, slot).wait()

            @pl.when(t + 1 < n)
            def _():
                fetch(t + 1, 1 - slot).start()

            use(pl.ds(pl.multiple_of(t * BLK, BLK), BLK), slot)

    def step(self, t):
        def cols(t):
            return pl.ds(pl.multiple_of(t * BLK, BLK), BLK)

        def fetch_o(t, slot):
            return pltpu.make_async_copy(self.w_o.at[:, cols(t)], self.buf_o.at[slot], self.w_sem.at[0, slot])

        def fetch_q(t, slot):
            return pltpu.make_async_copy(self.w_q.at[cols(t)], self.buf_q.at[slot], self.w_sem.at[1, slot])

        def project(at, slot):
            attn = self.attn_home[...].reshape(-1, self.w_o.shape[0])
            out = jnp.dot(attn, self.buf_o[slot], preferred_element_type=F32)
            self.block_out[:, at] = (self.hidden[:, at].astype(F32) + out).astype(BF16)

        def pull(at, slot):
            dq = self.dq_home[...].reshape(-1, self.w_o.shape[0])
            self.d_part[:, at] = dot_t(dq, self.buf_q[slot])

        if t in PRODUCTS_AT:
            i = PRODUCTS_AT.index(t)
            self.homes[i].wait_recv()
            self.tiles(*((fetch_o, project), (fetch_q, pull))[i])

    def finish(self):
        for h in self.homes:
            h.wait_send()


class HiddenGradient:
    tiles = 4

    def __init__(self, me, ins, outs, scratch):
        dkv, self.part, self.w_kv, self.x, self.dy, self.gain = ins
        self.dx, self.terms = outs
        self.dkv_home, self.rows, *sems = scratch
        self.home = Home(me, dkv, self.dkv_home, *sems)
        self.home.start()

    @staticmethod
    def scratch(dkv, x):
        dma = pltpu.SemaphoreType.DMA
        home = pltpu.VMEM((TWO,) * 3 + (CHUNK, TWO * dkv.shape[-1]), BF16)
        return [home, pltpu.VMEM((8, x.shape[1]), F32), dma(()), dma((4,)), dma((4,))]

    def tile(self, t):
        if t == 0:
            self.home.wait_recv()
            self.rows[...] = jnp.zeros_like(self.rows)
        size = TWO * CHUNK
        at = pl.ds(t * size, size)
        dkv = self.dkv_home[t // TWO, t % TWO].reshape(size, -1)
        d = self.part[at] + dot_t(dkv, self.w_kv[...])
        d = d.astype(BF16).astype(F32)
        x = self.x[at].astype(F32)
        inv_rms = lax.rsqrt(row_mean(x * x) + NORM_EPS)
        unit, scaled = x * inv_rms, d * self.gain[...]
        dx = inv_rms * (scaled - unit * row_mean(scaled * unit))
        self.dx[at] = (self.dy[at].astype(F32) + dx).astype(BF16)
        self.rows[...] += jnp.sum((d * unit).reshape((-1,) + self.rows.shape), axis=0)
        if t == self.tiles - 1:
            self.terms[...] = jnp.sum(self.rows[...], axis=0, keepdims=True)

    def finish(self):
        self.home.wait_send()


def reduce_pairs(arrays, cuts, kinds, collective_id, work, more):
    n = len(arrays)
    blocks = [a.shape[-TWO:] for a in arrays]
    scratch = sum((PairSum.scratch(k, b) for k, b in zip(kinds, blocks)), []) + PairSum.sems(n, max(cuts))
    outs = [jax.ShapeDtypeStruct(b, F32) for b in blocks] + work.results(more)
    return pl.pallas_call(
        functools.partial(reduce_kernel, cuts, kinds, work),
        name="reduce_pairs",
        out_shape=outs,
        in_specs=[pl.BlockSpec(memory_space=m) for m in [pl.ANY] * n + work.spaces],
        out_specs=[pl.BlockSpec(memory_space=pltpu.VMEM)] * len(outs),
        scratch_shapes=scratch + work.scratch(more),
        compiler_params=params(60, collective_id=collective_id),
        cost_estimate=cost(1, 20),
    )(*arrays, *more)


LINKS = "xyud"
ORDERS = "zxy", "zyx", "xyz", "zxy"
SIZES = 9.5, 9.5, 6.3, 2.8
LATENCY, TILES_FROM, TILE_EVERY = 3.0, 14.0, 8.0
SUM_AT = 42.0, 56.0, 70.0, 84.0


def onward(order, key):
    dz, ry, rx = key
    stage = max((order.index(a) for a, r in zip("zyx", key) if r), default=-1)
    for axis in order[stage + 1 :]:
        if axis == "x":
            yield "x", (dz, ry, 1)
        elif axis == "y":
            yield "y", (dz, 1, rx)
        else:
            yield "u", (-1, ry, rx)
            yield "d", (1, ry, rx)
    if stage >= 0 and order[stage] == "z" and abs(dz) < 3:
        yield ("u", (dz - 1, ry, rx)) if dz < 0 else ("d", (dz + 1, ry, rx))


def arrivals():
    busy = dict.fromkeys(LINKS, 0.0)
    starts = [0.0] * 3 + [SUM_AT[-1] + LATENCY]
    here, seen = [(t, part, (0, 0, 0)) for part, t in enumerate(starts)], []
    while here:
        now, part, key = heapq.heappop(here)
        seen.append((now, part, key))
        for link, there in onward(ORDERS[part], key):
            busy[link] = max(busy[link], now) + SIZES[part]
            heapq.heappush(here, (busy[link] + LATENCY, part, there))
    return seen


def gather_kernel(*refs):
    wo_ref, wq_ref, wkv_ref, *refs = refs
    grad_ins, outs, (dx_ref, dgain_ref), refs = refs[:6], refs[6:10], refs[10:12], refs[12:]
    own_sem, send_sem, come_sem, core_sem, all_terms, g_s, g_r, terms, wkv_own = refs[:9]
    buffers, sems, refs = refs[9:13], refs[13:20], refs[20:]
    me = lax.axis_index("cp")
    z, y, x, core = place(me)
    line = Line(me)
    to = {"x": dev(z, y, 1 - x, core), "y": dev(z, 1 - y, x, core), "u": line.next[1], "d": line.next[-1]}
    partner = dev(z, y, x, 1 - core)
    others = [(i, me ^ i) for i in range(1, all_terms.shape[0])]
    meet([d for _, d in others])
    job = HiddenGradient(me, grad_ins, (dx_ref, terms), refs)
    wkv = PairSum(me, "core", 1, wkv_ref, wkv_own, buffers, [r.at[0] for r in sems])
    wkv.begin(0)

    def windows(part, zz, yy, xx, cc):
        pair = TWO * zz + yy
        wide, narrow = wq_ref.shape[1], wkv_own.shape[1] // TWO
        wo_at, wq_at = ((xx * TWO + cc) * N_PAIRS + pair) * wo_ref.shape[0], (cc * N_PAIRS + pair) * wq_ref.shape[0]
        if part == 3:
            for i, out in enumerate(outs[TWO:]):
                cols = pl.ds(xx * narrow, narrow)
                yield wkv_own.at[:, head_slice(i)], out.at[pl.ds(wq_at, wkv_own.shape[0]), cols]
            return
        eighth = wo_ref.shape[0] // 8
        at, rows = (part * 3 * eighth, (TWO if part == TWO else 3) * eighth)
        yield wo_ref.at[pl.ds(at, rows)], outs[0].at[pl.ds(wo_at + at, rows)]
        at, rows = TWO * at, TWO * rows
        yield wq_ref.at[pl.ds(at, rows)], outs[1].at[pl.ds(wq_at + at, rows), pl.ds(xx * wide, wide)]

    def block(part, key, cc=core):
        dz, ry, rx = key
        return windows(part, z + dz, 1 - y if ry else y, 1 - x if rx else x, cc)

    def index(part, key):
        return (part, key[0] + 3) + key[1:]

    def send(part, key, link, there):
        arrive = (core_sem if link is None else come_sem).at[index(part, there)]
        for shard, window in block(part, key):
            src = window if any(key) else shard
            remote(src, window, send_sem.at[index(part, key) + (LINKS.find(link or "-") + 1,)], arrive, to.get(link, partner)).start()

    def whole(part, send, arrive):
        size = sum(shard.size for shard, _ in block(part, (0, 0, 0))) // outs[0].shape[1]
        dst = outs[0].at[pl.ds(0, size)]
        return remote(dst, dst, send, arrive, me)

    def when(on, do):
        pl.when(on)(do)

    def each_way(part, key):
        held = line.held(key[0])
        yield None, key, held
        for link, there in onward(ORDERS[part], key):
            inside = {"u": line.inside[1], "d": line.inside[-1]}.get(link)
            yield link, there, held if inside is None else jnp.logical_and(held, inside)

    def pass_on(part, key):
        for link, there, on in each_way(part, key):
            when(on, functools.partial(send, part, key, link, there))

    def term_copy(i, d):
        return remote(terms, all_terms.at[i], g_s.at[i], g_r.at[i], d)

    owns = []

    def put_own(part):
        for shard, window in block(part, (0, 0, 0)):
            owns.append(pltpu.make_async_copy(shard, window, own_sem.at[len(owns)]))
            owns[-1].start()

    def tile(t):
        job.tile(t)
        if t == job.tiles - 1:
            for i, d in others:
                term_copy(i, d).start()

    def sum_step(h):
        wkv.step(0, h)
        if h == 3:
            put_own(3)

    steps = [(TILES_FROM + t * TILE_EVERY, functools.partial(tile, t)) for t in range(job.tiles)]
    steps += [(at, functools.partial(sum_step, h)) for h, at in enumerate(SUM_AT)]
    steps.sort(key=lambda s: s[0])
    events = arrivals()
    for part in range(3):
        pass_on(part, (0, 0, 0))
        put_own(part)
    wkv.loaded(0)
    for now, part, key in events:
        while steps and steps[0][0] <= now:
            steps.pop(0)[1]()
        if any(key):
            arrive = come_sem.at[index(part, key)]
            when(line.held(key[0]), whole(part, own_sem.at[0], arrive).wait_recv)
            pass_on(part, key)
        elif part == 3:
            pass_on(part, key)
    for o in owns:
        o.wait()
    total_gain = terms[...]
    for i, d in others:
        term_copy(i, d).wait_recv()
        total_gain += all_terms[i]
    dgain_ref[...] = total_gain
    for i, d in others:
        term_copy(i, d).wait_send()
    for _, part, key in events:
        when(line.held(key[0]), whole(part, own_sem.at[0], core_sem.at[index(part, key)]).wait_recv)
        for link, there, on in each_way(part, key):
            sent = send_sem.at[index(part, key) + (LINKS.find(link or "-") + 1,)]
            when(on, whole(part, sent, own_sem.at[0]).wait_send)
    wkv.wait_send(0)
    job.finish()


def gather_all(wo, wq, wkv, dkv, part, w_kv, x, dy, gain, shapes):
    dma = pltpu.SemaphoreType.DMA
    vmem, hbm = pl.BlockSpec(memory_space=pltpu.VMEM), pl.BlockSpec(memory_space=pl.ANY)
    block = wkv.shape[-TWO:]
    parts = len(ORDERS)
    keys = (parts, 7, TWO, TWO)
    terms = 1, x.shape[1]
    scratch = [dma((TWO * parts,)), dma(keys + (len(LINKS) + 1,)), dma(keys), dma(keys)]
    scratch += [pltpu.VMEM((32,) + terms, F32), dma((32,)), dma((32,)), pltpu.VMEM(terms, F32), pltpu.VMEM(block, F32)]
    return pl.pallas_call(
        gather_kernel,
        name="gather_all",
        out_shape=[jax.ShapeDtypeStruct(s, F32) for s in shapes]
        + [jax.ShapeDtypeStruct(x.shape, BF16), jax.ShapeDtypeStruct(terms, F32)],
        in_specs=[vmem] * TWO + [hbm] + [vmem] * 6,
        out_specs=[hbm] * len(shapes) + [vmem] * TWO,
        scratch_shapes=scratch + PairSum.scratch("core", block) + PairSum.sems(1, 1) + HiddenGradient.scratch(dkv, x),
        compiler_params=params(40, collective_id=0),
        cost_estimate=cost(1, 76),
    )(wo, wq, wkv, dkv, part, w_kv, x, dy, gain)


def perm(x, pairs):
    return lax.ppermute(x, "cp", pairs)


def flip_pairs(d):
    return [(r, r ^ d) for r in range(32)]


def solution(mesh):
    def local_step(hidden, grad_out, positions, seg_ids, w_q, w_k, w_v, w_o, norm_gain):
        n_batch, n_tok, d_model = hidden.shape
        n_rows = n_batch * n_tok
        wide = N_HEADS * HEAD_DIM
        me = lax.axis_index("cp")
        _, y, x, core = place(me)
        quad, pair = me % 4, me // 4
        relations = range(4)

        def rows_of(arr, d):
            return pick(arr.reshape((TWO, TWO, TWO, CHUNK) + arr.shape[TWO:]), core ^ (d % TWO), 0)

        def swap(pieces):
            return [perm(p, flip_pairs(d)) if d else p for d, p in enumerate(pieces)]

        def unite(arr):
            joined = jnp.stack(swap([rows_of(arr, d) for d in relations]), axis=TWO)
            return joined.reshape((TWO, TWO, BLK) + joined.shape[4:])

        gain = norm_gain.astype(F32)
        cos_t, sin_t = rope_tables(positions.reshape(n_rows))
        cos_f, sin_f = jnp.hstack([cos_t, cos_t]), jnp.hstack([-sin_t, sin_t])
        normed, kv_home, q_home = project(hidden.reshape(n_rows, d_model), gain[NEW], w_q, w_k, w_v, cos_f, sin_f)
        pos_u = unite(positions)
        kv_all, q_u, dy_part = exchange(
            kv_home.reshape((TWO,) * 5 + (CHUNK, HEAD_DIM)),
            q_home.reshape((TWO,) * 4 + (CHUNK, wide)),
            grad_out.reshape((TWO,) * 3 + (CHUNK, d_model)),
        )
        dy_last, dy_part = lax.optimization_barrier((rows_of(grad_out, LATER[1]), dy_part))
        dy_last = perm(dy_last, flip_pairs(LATER[1]))
        normed_home, dy_part = lax.optimization_barrier((normed.reshape(hidden.shape), dy_part))
        normed_u = unite(normed_home)

        member = quad ^ jnp.arange(4)
        front, back = ((m[:, NEW] * CHUNK + jnp.arange(CHUNK)[NEW]).reshape(BLK) for m in (member, 3 - member))
        offsets = jnp.stack([front, back]).astype(jnp.int32)
        own_super = jnp.stack([pair, N_SUPER - 1 - pair]).astype(jnp.int32)
        q_index = own_super[:, NEW] * BLK + offsets
        start = q_index[NEW] - pos_u
        koff = jnp.broadcast_to(offsets[:, :, NEW], (TWO, BLK, BLK))
        tab = jnp.concatenate(
            [own_super, (jnp.min(start, axis=-1) // BLK).reshape(-1), jnp.max(start, axis=-1).reshape(-1)]
        )
        start_r = start[:, :, NEW, :]
        q_index_r = jnp.broadcast_to(q_index[NEW, :, NEW, :], start_r.shape)
        cos_u, sin_u = rope_tables(pos_u)
        cos_ut, sin_ut = jnp.swapaxes(cos_u, TWO, 3), jnp.swapaxes(sin_u, TWO, 3)

        lanes = start.shape + (HEAD_DIM,)
        start_l, q_index_l = (jnp.broadcast_to(a[..., NEW], lanes) for a in (start, q_index[NEW]))
        attn_u, lse = flash_fwd(tab, q_u, kv_all, start_l, q_index_l, offsets[:, NEW])

        tok = tuple(range(3))
        half_wide = wide // TWO
        dy_u = jnp.concatenate([dy_part, dy_last], axis=TWO)
        wo_send = dot(dyn(attn_u, (1 - core) * half_wide, half_wide, 3), dy_u, tok, tok)
        wo_sum = dot(dyn(attn_u, core * half_wide, half_wide, 3), dy_u, tok, tok) + perm(wo_send, flip_pairs(1))
        wo_sum = wo_sum.reshape(4, TWO, half_wide // N_PAIRS, d_model)
        wo_y = perm(pick(wo_sum, 1 - y, 1), flip_pairs(4))

        d_attn = dot(dy_u, dyn(w_o, x * wide, wide, 0), (3,), (1,)).astype(BF16)
        d_attn, wo_sum = lax.optimization_barrier((d_attn, wo_sum))
        dq_u, dkv = flash_bwd(tab, q_u, d_attn, attn_u, kv_all, lse, start_r, q_index_r, koff, cos_ut, sin_ut)

        wo_sum = pick(wo_sum, y, 1) + wo_y
        half_model = d_model // TWO

        def by_core(d_out):
            part = lax.optimization_barrier(dot(normed_u, d_out, tok, tok))
            return part.reshape(TWO, 4, TWO, half_model // N_PAIRS, -1)

        x_flat = hidden.reshape(n_rows, d_model)
        wo_own, dkv_own, wq_own, block_out, d_part = reduce_pairs(
            [wo_sum, dkv.reshape(4, TWO, -1, HEAD_DIM), by_core(dq_u)],
            (TWO, 8, 4),
            ("z", "", "core"),
            TWO,
            Products,
            (attn_u, dq_u, x_flat, w_o, w_q),
        )
        dkv_own = dkv_own.reshape((TWO,) * 3 + (BLK, HEAD_DIM))
        dk_u = rotate(dkv_own[0] * ATTN_SCALE, cos_u, -sin_u).astype(BF16)
        dkv_u = jnp.concatenate([dk_u, dkv_own[1].astype(BF16)], axis=-1)
        w_kv = jnp.hstack([w[:, head_slice(i)] for i in range(TWO) for w in (w_k, w_v)])
        grad_wo, grad_wq, grad_wk, grad_wv, grad_x, d_gain = gather_all(
            wo_own,
            wq_own,
            by_core(dkv_u),
            dkv_u,
            d_part,
            w_kv,
            x_flat,
            grad_out.reshape(n_rows, d_model),
            gain[NEW],
            [w_o.shape, w_q.shape, w_k.shape, w_v.shape],
        )
        block_out, grad_x = (a.reshape(hidden.shape) for a in (block_out, grad_x))
        return block_out, grad_x, grad_wq, grad_wk, grad_wv, grad_wo, d_gain.reshape(d_model)

    seq_spec = P(None, "cp", None)
    tok_spec = P(None, "cp")
    full_spec = P()
    return jax.shard_map(
        local_step,
        mesh=mesh,
        in_specs=(seq_spec, seq_spec, tok_spec, tok_spec, full_spec, full_spec, full_spec, full_spec, full_spec),
        out_specs=(seq_spec, seq_spec, full_spec, full_spec, full_spec, full_spec, full_spec),
        check_vma=False,
    )
```

```python
import functools
import heapq
import itertools

import jax
import jax.numpy as jnp
from jax import lax
from jax.experimental import pallas as pl
from jax.experimental.pallas import tpu as pltpu
from jax.sharding import PartitionSpec as P

HEAD_DIM = 128
NORM_EPS = 1e-5
ROPE_BASE = 500000.0
NEG_BIG = -1e30
LOG2E = 1.4426950408889634
ATTN_SCALE = HEAD_DIM**-0.5
EXP2_SCALE = ATTN_SCALE * LOG2E
CHUNK = 64
TWO = 2
FOUR = 4
NEW = jnp.newaxis
BLK = 4 * CHUNK
N_HEADS = 8
N_PAIRS = 8
N_SUPER = 2 * N_PAIRS
MESH = pl.DeviceIdType.MESH
ONE = pl.Squeezed()
LATER = 2, 3
MADE_AT = 5
PRODUCTS_AT = 7, 9
F32 = jnp.float32
BF16 = jnp.bfloat16

T_SQ, T_LO, T_MX = 0, 2, 6


def rope_tables(positions):
    inv_freq = ROPE_BASE ** (-jnp.arange(0, HEAD_DIM, TWO).astype(F32) / HEAD_DIM)
    angles = positions.astype(F32)[..., None] * inv_freq
    return jnp.cos(angles), jnp.sin(angles)


def dot(a, b, ca, cb):
    return lax.dot_general(a, b, ((ca, cb), ((), ())), preferred_element_type=F32)


def cost(gflop, mib):
    return pl.CostEstimate(flops=gflop * 10**9, bytes_accessed=mib << 20, transcendentals=0)


def params(mib, **more):
    return pltpu.CompilerParams(vmem_limit_bytes=mib << 20, **more)


def row_mean(x):
    return jnp.mean(x, axis=-1, keepdims=True)


def head(h):
    return pl.ds(h * HEAD_DIM, HEAD_DIM)


def head_slice(h):
    return slice(h * HEAD_DIM, (h + 1) * HEAD_DIM)


def dot_t(a, b):
    return dot(a, b, (1,), (1,))


def dyn(x, index, size, axis):
    return lax.dynamic_slice_in_dim(x, index, size, axis)


def pick(x, index, axis):
    return lax.dynamic_index_in_dim(x, index, axis, keepdims=False)


def steps(tab, body):
    b, hf = pl.program_id(0), pl.program_id(1)
    own, first, last_start = tab[T_SQ + hf], tab[T_LO + TWO * b + hf], tab[T_MX + TWO * b + hf]

    def step(s, carry):
        late = s >= N_PAIRS
        at = jnp.where(late, N_SUPER - 1 - s, s), late.astype(jnp.int32)
        full = jnp.logical_and(s < own, s * BLK >= last_start)
        pl.when(full)(lambda: body(s, at, False))
        pl.when(jnp.logical_not(full))(lambda: body(s, at, True))
        return carry

    lax.fori_loop(first, own + 1, step, 0)


def may_use(s, off, st_ref, qi_ref):
    return jnp.logical_and(off >= st_ref[...] - s * BLK, off <= qi_ref[...] - s * BLK)


def fwd_kernel(tab, q_ref, kv_ref, st_ref, qi_ref, ko_ref, o_ref, lse_ref, q_s, acc, m_s, l_s, k_t):
    m_s[...] = jnp.full_like(m_s, NEG_BIG)
    l_s[...] = jnp.zeros_like(l_s)
    acc[...] = jnp.zeros_like(acc)
    for h in range(N_HEADS):
        q_s[pl.ds(h * BLK, BLK)] = q_ref[:, head(h)]

    @pl.when(pl.program_id(1) == 0)
    def _():
        @pl.loop(0, N_PAIRS)
        def _(pair):
            for hk in range(TWO):
                k_t[pair, hk] = kv_ref[pair, 0, hk].T

    def body(s, at, masked):
        pair, hk = at
        v = kv_ref[pair, 1, hk]
        if masked:
            off = ko_ref[hk] + s * BLK
            mask = [
                jnp.logical_and(off[:, lanes] >= st_ref[...], off[:, lanes] <= qi_ref[...])
                for lanes in (slice(HEAD_DIM), slice(HEAD_DIM, BLK))
            ]
            mask = [jnp.concatenate([m, m], axis=0) for m in mask]
        for g in range(N_HEADS // TWO):
            rows = pl.ds(g * TWO * BLK, TWO * BLK)
            sc = jnp.dot(q_s[rows], k_t[pair, hk], preferred_element_type=F32)
            sc = [sc[:, :HEAD_DIM], sc[:, HEAD_DIM:]]
            if masked:
                sc = [jnp.where(m, x, NEG_BIG) for m, x in zip(mask, sc)]
            m_old = m_s[rows]
            m_new = jnp.maximum(m_old, jnp.max(jnp.maximum(*sc), axis=1, keepdims=True))
            alpha = jnp.exp2((m_old - m_new) * EXP2_SCALE)
            p = [jnp.exp2((x - m_new) * EXP2_SCALE) for x in sc]
            m_s[rows] = m_new
            l_s[rows] = l_s[rows] * alpha + (p[0] + p[1])
            p = jnp.hstack([x.astype(BF16) for x in p])
            acc[rows] = acc[rows] * alpha + jnp.dot(p, v, preferred_element_type=F32)

    steps(tab, body)
    for h in range(N_HEADS):
        rows = pl.ds(h * BLK, BLK)
        total = jnp.sum(l_s[rows], axis=1, keepdims=True)
        o_ref[:, head(h)] = (acc[rows] / total).astype(BF16)
        lse_ref[h] = (m_s[rows] * EXP2_SCALE + jnp.log2(total)).T[:1]


def bwd_kernel(tab, q_ref, do_ref, o_ref, kv_ref, lse_ref, st_ref, qi_ref, ko_ref, cos_ref, sin_ref, dq_ref, dkv_ref, dq_acc, delta):
    dq_acc[...] = jnp.zeros_like(dq_acc)
    for h in range(N_HEADS):
        terms = do_ref[:, head(h)].astype(F32) * o_ref[:, head(h)].astype(F32)
        delta[h] = jnp.sum(terms.T, axis=0, keepdims=True)

    @pl.when(pl.program_id(1) == 0)
    def _():
        dkv_ref[...] = jnp.zeros_like(dkv_ref)

    def body(s, at, masked):
        pair, hk = at
        k = kv_ref[pair, 0, hk]
        v = kv_ref[pair, 1, hk]
        k_t = k.T
        mask = may_use(s, ko_ref[hk], st_ref, qi_ref) if masked else None
        dk = dv = jnp.zeros((BLK, HEAD_DIM), F32)
        for h in range(N_HEADS):
            q = q_ref[:, head(h)]
            do = do_ref[:, head(h)]
            p = jnp.exp2(dot_t(k, q) * EXP2_SCALE - lse_ref[h])
            if masked:
                p = jnp.where(mask, p, 0.0)
            ds = (p * (dot_t(v, do) - delta[h])).astype(BF16)
            dv += jnp.dot(p.astype(BF16), do, preferred_element_type=F32)
            dk += jnp.dot(ds, q, preferred_element_type=F32)
            dq_acc[h] += jnp.dot(k_t, ds, preferred_element_type=F32)
        dkv_ref[pair, 0, hk] += dk
        dkv_ref[pair, 1, hk] += dv

    steps(tab, body)
    cos_t, sin_t = cos_ref[...], sin_ref[...]
    half = HEAD_DIM // TWO
    for h in range(N_HEADS):
        a, c = dq_acc[h, :half] * ATTN_SCALE, dq_acc[h, half:] * ATTN_SCALE
        lin = jnp.concatenate([a * cos_t + c * sin_t, c * cos_t - a * sin_t], axis=0)
        dq_ref[:, head(h)] = lin.T.astype(BF16)


def attn_specs():
    def at_tile(b, h, t):
        return (b, h) + (0,) * TWO

    def at_row(b, h, t):
        return (0, 0, b) + (0,) * 3

    tile = pl.BlockSpec((ONE, ONE, BLK, N_HEADS * HEAD_DIM), at_tile)
    row = pl.BlockSpec((ONE, ONE, 1, BLK), at_tile)
    stat = pl.BlockSpec((ONE, ONE, N_HEADS, 1, BLK), lambda b, h, t: (b, h) + (0,) * 3)
    rope = pl.BlockSpec((ONE, ONE, HEAD_DIM // TWO, BLK), at_tile)
    kv = pl.BlockSpec((N_PAIRS, TWO, ONE, TWO, BLK, HEAD_DIM), at_row)
    ko = pl.BlockSpec((TWO, BLK, BLK), lambda b, h, t: (0,) * 3)
    return tile, row, stat, kv, ko, rope


def flash_fwd(tab, q, kv, start, qidx, koff):
    tile, _, stat, kvs, *_ = attn_specs()
    col = pl.BlockSpec((ONE, ONE, BLK, HEAD_DIM), lambda b, h, t: (b, h) + (0,) * TWO)
    ko = pl.BlockSpec((TWO, 1, BLK), lambda b, h, t: (0,) * 3)
    return pl.pallas_call(
        fwd_kernel,
        name="attn_fwd",
        out_shape=(jax.ShapeDtypeStruct(q.shape, BF16), jax.ShapeDtypeStruct((TWO, TWO, N_HEADS, 1, BLK), F32)),
        grid_spec=pltpu.PrefetchScalarGridSpec(
            num_scalar_prefetch=1,
            grid=(TWO, TWO),
            in_specs=[tile, kvs, col, col, ko],
            out_specs=[tile, stat],
            scratch_shapes=[pltpu.VMEM((N_HEADS * BLK, HEAD_DIM), t) for t in (BF16, F32, F32, F32)]
            + [pltpu.VMEM((N_PAIRS, TWO, HEAD_DIM, BLK), BF16)],
        ),
        compiler_params=params(40),
        cost_estimate=cost(20, 16),
    )(tab, q, kv, start, qidx, koff)


def flash_bwd(tab, q, do, o, kv, lse, start, qidx, koff, cos_t, sin_t):
    tile, row, stat, kvs, ko, rope = attn_specs()
    return pl.pallas_call(
        bwd_kernel,
        name="attn_bwd",
        out_shape=(
            jax.ShapeDtypeStruct(q.shape, BF16),
            jax.ShapeDtypeStruct(kv.shape, F32),
        ),
        grid_spec=pltpu.PrefetchScalarGridSpec(
            num_scalar_prefetch=1,
            grid=(TWO, TWO),
            in_specs=[tile, tile, tile, kvs, stat, row, row, ko, rope, rope],
            out_specs=[tile, kvs],
            scratch_shapes=[pltpu.VMEM((N_HEADS, HEAD_DIM, BLK), F32), pltpu.VMEM((N_HEADS, 1, BLK), F32)],
        ),
        compiler_params=params(48),
        cost_estimate=cost(50, 32),
    )(tab, q, do, o, kv, lse, start, qidx, koff, cos_t, sin_t)


def turn(x, cos_ref, sin_ref):
    return x * cos_ref[...] + pltpu.roll(x, HEAD_DIM // TWO, 1) * sin_ref[...]


def first_kernel(x_ref, g_ref, wk_ref, wv_ref, cos_ref, sin_ref, h_ref, kv_ref):
    x = x_ref[...].astype(F32)
    h = (x * lax.rsqrt(row_mean(x * x) + NORM_EPS) * g_ref[...]).astype(BF16)
    h_ref[...] = h
    k = jnp.dot(h, wk_ref[...], preferred_element_type=F32)
    v = jnp.dot(h, wv_ref[...], preferred_element_type=F32)
    n = kv_ref.shape[3]
    for i in range(TWO):
        for j, val in enumerate((turn(k[:, head_slice(i)], cos_ref, sin_ref), v[:, head_slice(i)])):
            for c in range(TWO):
                kv_ref[i, c, j] = val[c * n : (c + 1) * n].astype(BF16)


def query_kernel(h_ref, w_ref, cos_ref, sin_ref, q_ref):
    q = jnp.dot(h_ref[...], w_ref[...], preferred_element_type=F32)
    n = q_ref.shape[TWO]
    for j in range(q.shape[1] // HEAD_DIM):
        val = turn(q[:, head_slice(j)], cos_ref, sin_ref).astype(BF16)
        for c in range(TWO):
            q_ref[0, c, :, head(j)] = val[c * n : (c + 1) * n]


def project(x, gain, w_q, w_k, w_v, cos_f, sin_f):
    n, d = x.shape
    h, kv = pl.pallas_call(
        first_kernel,
        name="norm_kv",
        out_shape=(jax.ShapeDtypeStruct(x.shape, BF16), jax.ShapeDtypeStruct((TWO,) * 3 + (n // TWO, HEAD_DIM), BF16)),
        compiler_params=params(40),
        cost_estimate=cost(TWO, 7),
    )(x, gain, w_k, w_v, cos_f, sin_f)
    tile = FOUR * HEAD_DIM
    rope = pl.BlockSpec(cos_f.shape, lambda j: (0, 0))
    q = pl.pallas_call(
        query_kernel,
        name="query",
        grid=(d // tile,),
        out_shape=jax.ShapeDtypeStruct((TWO, TWO, n // TWO, d // TWO), BF16),
        in_specs=[pl.BlockSpec(h.shape, lambda j: (0, 0)), pl.BlockSpec((d, tile), lambda j: (0, j)), rope, rope],
        out_specs=pl.BlockSpec((1, TWO, n // TWO, tile), lambda j: (j // TWO, 0, 0, j % TWO)),
        compiler_params=params(40),
        cost_estimate=cost(5, 12),
    )(h, w_q, cos_f, sin_f)
    return h, kv, q


def place(me):
    return me // 8, lax.rem(me // FOUR, TWO), lax.rem(me // TWO, TWO), lax.rem(me, TWO)


def dev(z, y, x, core):
    return ((z * TWO + y) * TWO + x) * TWO + core


def z_peers(z):
    return [(k, lax.rem(z + k, FOUR)) for k in (1, TWO, 3)]


def meet(peers):
    barrier = pltpu.get_barrier_semaphore()
    for d in peers:
        pl.semaphore_signal(barrier, device_id=(d,), device_id_type=MESH)
    pl.semaphore_wait(barrier, len(peers))


def remote(src, dst, send, arrive, to):
    return pltpu.make_async_remote_copy(
        src_ref=src, dst_ref=dst, send_sem=send, recv_sem=arrive, device_id=(to,), device_id_type=MESH
    )


class Line:
    order = (0, 1, -1, TWO, -TWO, 3, -3)

    def __init__(self, me):
        self.z, y, x, core = place(me)
        self.next = {1: dev(self.z + 1, y, x, core), -1: dev(self.z - 1, y, x, core)}
        self.inside = {1: self.z < 3, -1: self.z > 0}

    def held(self, dz):
        return jnp.logical_and(self.z + dz >= 0, self.z + dz <= 3)

    def ways(self, dz):
        for d in self.next:
            if d * dz <= 0:
                yield d, self.inside[d] if dz == 0 else jnp.logical_and(self.inside[d], self.held(dz))


def exchange_kernel(kv_ref, q_ref, dy_ref, kv_all, q_u, dy_u, own_sem, quad_s, quad_r, z_s, z_r, y_s, y_r):
    me = lax.axis_index("cp")
    z, y, x, core = place(me)
    quad, line = quad_of(me), Line(me)
    across = dev(z, 1 - y, x, core)
    meet(quad[1:] + [across] + [dev(zz, y, x, core) for _, zz in z_peers(z)])

    def source(a, d):
        xx, cc = 1 - x if d // TWO else x, 1 - core if d % TWO else core
        return dy_ref.at[cc] if a == TWO else (kv_ref, q_ref)[a].at[xx, cc]

    def target(a, d):
        tok = pl.ds(d * CHUNK, CHUNK)
        return kv_all.at[me // FOUR, :, :, :, tok] if a == 0 else (q_u, dy_u)[a - 1].at[:, :, tok]

    def quad_copy(a, d):
        return remote(source(a, d), target(a, d), quad_s.at[a, d], quad_r.at[a, d], quad[d])

    def own_copy(a):
        return pltpu.make_async_copy(source(a, 0), target(a, 0), own_sem.at[a])

    sent = [(a, d) for a in range(3) for d in (1, TWO, 3) if (a, d) != LATER]
    for a, d in sent:
        quad_copy(a, d).start()
    for a in range(3):
        own_copy(a).start()
    own_copy(0).wait()
    for d in (1, TWO, 3):
        quad_copy(0, d).wait_recv()

    def z_copy(part, dz, d):
        block = kv_all.at[TWO * (z + dz) + y, part]
        return remote(block, block, z_s.at[part, (d + 1) // TWO, dz + 3], z_r.at[part, dz - d + 3], line.next[d])

    def y_copy(part, dz, yy=y):
        block = kv_all.at[TWO * (z + dz) + yy, part]
        return remote(block, block, y_s.at[part, dz + 3], y_r.at[part, dz + 3], across)

    parts = range(TWO)
    moves = [(part, dz) for dz in line.order for part in parts]
    for part, dz in moves:
        if dz:
            block = kv_all.at[TWO * (z + dz) + y, part]
            arrival = remote(block, block, own_sem.at[0], z_r.at[part, dz + 3], me)
            pl.when(line.held(dz))(arrival.wait_recv)
        for d, on in line.ways(dz):
            pl.when(on)(z_copy(part, dz, d).start)
        pl.when(line.held(dz))(y_copy(part, dz).start)
    for part, dz in moves:
        for d, on in line.ways(dz):
            pl.when(on)(z_copy(part, dz, d).wait_send)
        pl.when(line.held(dz))(y_copy(part, dz, 1 - y).wait_recv)
        pl.when(line.held(dz))(y_copy(part, dz).wait_send)
    for a, d in sent:
        quad_copy(a, d).wait_send()
        if a > 0:
            quad_copy(a, d).wait_recv()
    own_copy(1).wait()
    own_copy(TWO).wait()


def exchange(kv, q, dy):
    dma = pltpu.SemaphoreType.DMA
    vmem, hbm = pl.BlockSpec(memory_space=pltpu.VMEM), pl.BlockSpec(memory_space=pl.ANY)
    wide = q.shape[-1]
    return pl.pallas_call(
        exchange_kernel,
        name="exchange",
        out_shape=(
            jax.ShapeDtypeStruct((N_PAIRS,) + (TWO,) * 3 + (BLK, HEAD_DIM), BF16),
            jax.ShapeDtypeStruct((TWO, TWO, BLK, wide), BF16),
            jax.ShapeDtypeStruct((TWO, TWO, LATER[1] * CHUNK, TWO * wide), BF16),
        ),
        in_specs=[vmem] * 3,
        out_specs=[hbm] * 3,
        scratch_shapes=[dma((3,))] + [dma((3, FOUR))] * TWO + [dma((TWO, TWO, 7))] + [dma((TWO, 7))] * 3,
        compiler_params=pltpu.CompilerParams(collective_id=1),
        cost_estimate=cost(1, 20),
    )(kv, q, dy)


class PairSum:
    def __init__(self, me, kind, cut, src, out, buffers, sems):
        self.me, self.kind, self.src, self.out = me, kind, src, out
        self.size = out.shape[0] // cut
        self.own, self.from_core, self.from_y, self.from_z = buffers
        self.load_sem, self.core_s, self.core_r, self.y_s, self.y_r, self.z_s, self.z_r = sems
        self.z, self.y, x, core = place(me)
        self.partner = dev(self.z, self.y, x, 1 - core)
        self.across = dev(self.z, 1 - self.y, x, core)
        self.next_z = dev(self.z + 1, self.y, x, core), dev(self.z - 1, self.y, x, core)

    def rows(self, j):
        return pl.ds(j * self.size, self.size)

    def mine(self, j, zz):
        at = self.rows(j)
        return self.own.at[zz, self.y, at] if self.kind == "core" else self.own.at[zz, at]

    def load(self, j):
        at = self.rows(j)
        src = self.src.at[:, at] if self.kind else self.src.at[:, self.y, at]
        return pltpu.make_async_copy(src, self.own.at[:, at], self.load_sem.at[j])

    def core_copy(self, j):
        src, dst = (r.at[:, :, self.rows(j)] for r in (self.src, self.from_core))
        return remote(src, dst, self.core_s.at[j], self.core_r.at[j], self.partner)

    def y_copy(self, j):
        src = self.own if self.kind == "core" else self.src
        at = self.rows(j)
        return remote(src.at[:, 1 - self.y, at], self.from_y.at[:, at], self.y_s.at[j], self.y_r.at[j], self.across)

    def z_copy(self, j, way, zz, to):
        at = way, zz + way - 1
        return remote(self.mine(j, zz), self.from_z.at[*at, self.rows(j)], self.z_s.at[j, *at], self.z_r.at[j, *at], to)

    def begin(self, j):
        if self.kind == "core":
            self.core_copy(j).start()
            return
        self.load(j).start()
        if not self.kind:
            self.y_copy(j).start()

    def loaded(self, j):
        if self.kind != "core":
            self.load(j).wait()
        else:
            self.core_copy(j).wait_recv()
            at = self.rows(j)
            for zz in range(FOUR):
                self.own[zz, :, at] += self.from_core[zz, :, at]
            self.y_copy(j).start()
        if self.kind == "z":
            self.hop(j, 0)

    def relay(self, j, way, zz, add):
        if add:
            self.z_copy(j, way, zz, self.me).wait_recv()
            self.mine(j, zz)[...] += self.from_z[way, zz + way - 1, self.rows(j)]
        self.z_copy(j, way, zz, self.next_z[way]).start()

    def hop(self, j, h):
        @pl.when(self.z == h)
        def _():
            for zz in range(3, h, -1):
                self.relay(j, 0, zz, h > 0)

        @pl.when(self.z == 3 - h)
        def _():
            for zz in range(3 - h):
                self.relay(j, 1, zz, h > 0)

    def step(self, j, h):
        if h == 0 and self.kind != "z":
            self.y_copy(j).wait_recv()
            for zz in range(FOUR):
                self.mine(j, zz)[...] += self.from_y[zz, self.rows(j)]
            self.hop(j, 0)
        elif 0 < h < 3:
            self.hop(j, h)
        elif h == 3:
            at = self.rows(j)
            self.out[at] = self.mine(j, self.z)[...]
            for way, on in enumerate((self.z > 0, self.z < 3)):

                @pl.when(on)
                def _(way=way):
                    self.z_copy(j, way, self.z, self.me).wait_recv()
                    self.out[at] += self.from_z[way, self.z + way - 1, at]

    def wait_send(self, j):
        if self.kind == "core":
            self.core_copy(j).wait_send()
        if self.kind != "z":
            self.y_copy(j).wait_send()
        for zz in range(FOUR):
            if zz > 0:
                pl.when(self.z < zz)(self.z_copy(j, 0, zz, self.next_z[0]).wait_send)
            if zz < 3:
                pl.when(self.z > zz)(self.z_copy(j, 1, zz, self.next_z[1]).wait_send)

    @staticmethod
    def scratch(kind, block):
        unused = pltpu.VMEM((8, HEAD_DIM), F32)
        own = pltpu.VMEM(((FOUR, TWO) if kind == "core" else (FOUR,)) + block, F32)
        from_y = unused if kind == "z" else pltpu.VMEM((FOUR,) + block, F32)
        return [own, own if kind == "core" else unused, from_y, pltpu.VMEM((TWO, 3) + block, F32)]

    @staticmethod
    def sems(*dims):
        dma = pltpu.SemaphoreType.DMA
        return [dma(dims)] * 5 + [dma(dims + (TWO, 3))] * TWO


def taker(refs):
    rest = iter(refs)
    return lambda count: list(itertools.islice(rest, count))


def reduce_kernel(cuts, kinds, work, *refs):
    n = len(cuts)

    take = taker(refs)
    ins, more_in, outs, more_out, made = take(n - 1), take(work.ins), take(n), take(work.outs), take(1)
    buffers, sems = [take(FOUR) for _ in kinds], take(7)
    me = lax.axis_index("cp")
    z, y, x, core = place(me)
    meet(quad_of(me)[1:] + [dev(z, 1 - y, x, core)] + [dev(zz, y, x, core) for _, zz in z_peers(z)])
    job = work(me, more_in, more_out, take(len(refs)))
    sums = [PairSum(me, *a, [r.at[i] for r in sems]) for i, a in enumerate(zip(kinds, cuts, ins + made, outs, buffers))]
    pieces = [(s, j) for s, cut in zip(sums, cuts) for j in range(cut)]
    early, late = pieces[: -cuts[-1]], pieces[-cuts[-1] :]
    for s, j in early:
        s.begin(j)
    for s, j in early:
        s.loaded(j)
    for t in range(len(pieces) + 3):
        if t == MADE_AT:
            job.wq_terms(sums[-1].own, made[0])
            for s, j in late:
                s.begin(j)
        if t == MADE_AT + 1:
            for s, j in late:
                s.loaded(j)
        for h in range(FOUR):
            if 0 <= t - h < len(pieces):
                s, j = pieces[t - h]
                s.step(j, h)
        job.step(t)
    for s, j in pieces:
        s.wait_send(j)
    job.finish()


def quad_of(me):
    z, y, x, core = place(me)
    return [dev(z, y, 1 - x if d // TWO else x, 1 - core if d % TWO else core) for d in range(FOUR)]


class Home:
    def __init__(self, me, src, out, own_sem, send, arrive):
        _, _, x, core = place(me)
        w = src.shape[-1]
        to = out.at[core, :, :, :, pl.ds(x * w, w)]

        def piece(d):
            return src.at[:, :, pl.ds(d * CHUNK, CHUNK)]

        self.own = pltpu.make_async_copy(piece(0), to, own_sem)
        self.copies = [remote(piece(d), to, send.at[d], arrive.at[d], quad_of(me)[d]) for d in (1, TWO, 3)]

    def start(self):
        self.own.start()
        for c in self.copies:
            c.start()

    def wait_recv(self):
        self.own.wait()
        for c in self.copies:
            c.wait_recv()

    def wait_send(self):
        for c in self.copies:
            c.wait_send()


class Products:
    ins, outs = 6, 3

    def __init__(self, me, ins, outs, scratch):
        attn, self.dq, hidden, normed, self.w_o, self.w_q = ins
        self.block_out, self.d_part, self.h_u = outs
        self.attn_home, self.dq_home, self.buf_o, self.buf_q, self.h_own, *sems = scratch
        self.w_sem, self.load_sem, own_sem, quad_s, quad_r = sems
        _, _, _, core = place(me)

        def piece(d):
            return normed.at[1 - core if d % TWO else core]

        def tokens(d):
            return self.h_u.at[:, :, pl.ds(d * CHUNK, CHUNK)]

        self.h_copies = [remote(piece(d), tokens(d), quad_s.at[TWO, d], quad_r.at[TWO, d], quad_of(me)[d]) for d in (1, TWO, 3)]
        self.h_mine = pltpu.make_async_copy(piece(0), self.h_own.at[:, :, pl.ds(0, CHUNK)], own_sem.at[TWO])
        self.h_rest = pltpu.make_async_copy(
            self.h_u.at[:, :, pl.ds(CHUNK, BLK - CHUNK)], self.h_own.at[:, :, pl.ds(CHUNK, BLK - CHUNK)], self.load_sem
        )
        self.h_back = pltpu.make_async_copy(self.h_own.at[:, :, pl.ds(0, CHUNK)], tokens(0), self.load_sem)
        self.residual = pltpu.make_async_copy(hidden, self.block_out, own_sem.at[3])
        self.residual.start()
        for c in self.h_copies:
            c.start()
        self.h_mine.start()
        self.homes = [
            Home(me, src, out, own_sem.at[i], quad_s.at[i], quad_r.at[i])
            for i, (src, out) in enumerate([(attn, self.attn_home), (self.dq, self.dq_home)])
        ]
        for h in self.homes:
            h.start()

    @staticmethod
    def scratch(arrays):
        dma, d = pltpu.SemaphoreType.DMA, arrays[-1].shape[0]
        home = pltpu.VMEM((TWO,) * 3 + (CHUNK, d), BF16)
        buf = [pltpu.VMEM((TWO,) + b, BF16) for b in ((d, BLK), (BLK, d))]
        unit = pltpu.VMEM((TWO, TWO, BLK, d), BF16)
        return [home] * TWO + buf + [unit, dma((TWO, TWO)), dma(()), dma((FOUR,)), dma((3, FOUR)), dma((3, FOUR))]

    @staticmethod
    def results(arrays):
        unit = TWO, TWO, BLK, arrays[-1].shape[0]
        return [jax.ShapeDtypeStruct(arrays[TWO].shape, t) for t in (BF16, F32)] + [jax.ShapeDtypeStruct(unit, BF16)]

    spaces, out_spaces = [pl.ANY, pltpu.VMEM] + [pl.ANY] * FOUR, [pltpu.VMEM] * TWO + [pl.ANY]

    def tiles(self, fetch, use):
        n = self.w_o.shape[0] // BLK
        fetch(0, 0).start()

        @pl.loop(0, n)
        def _(t):
            slot = lax.rem(t, TWO)
            fetch(t, slot).wait()

            @pl.when(t + 1 < n)
            def _():
                fetch(t + 1, 1 - slot).start()

            use(pl.ds(pl.multiple_of(t * BLK, BLK), BLK), slot)

    def step(self, t):
        def cols(t):
            return pl.ds(pl.multiple_of(t * BLK, BLK), BLK)

        def fetch_o(t, slot):
            return pltpu.make_async_copy(self.w_o.at[:, cols(t)], self.buf_o.at[slot], self.w_sem.at[0, slot])

        def fetch_q(t, slot):
            return pltpu.make_async_copy(self.w_q.at[cols(t)], self.buf_q.at[slot], self.w_sem.at[1, slot])

        def project(at, slot):
            attn = self.attn_home[...].reshape(-1, self.w_o.shape[0])
            out = jnp.dot(attn, self.buf_o[slot], preferred_element_type=F32)
            self.block_out[:, at] = (self.block_out[:, at].astype(F32) + out).astype(BF16)

        def pull(at, slot):
            dq = self.dq_home[...].reshape(-1, self.w_o.shape[0])
            self.d_part[:, at] = dot_t(dq, self.buf_q[slot])

        if t in PRODUCTS_AT:
            i = PRODUCTS_AT.index(t)
            self.homes[i].wait_recv()
            if i == 0:
                self.residual.wait()
            self.tiles(*((fetch_o, project), (fetch_q, pull))[i])

    def wq_terms(self, own, other):
        self.h_mine.wait()
        self.h_back.start()
        for c in self.h_copies:
            c.wait_recv()
        self.h_back.wait()
        self.h_rest.start()
        self.h_rest.wait()
        core = lax.rem(lax.axis_index("cp"), TWO)
        d_out = self.dq[...].reshape(-1, self.dq.shape[-1])
        for out, half in ((other, 1 - core), (own, core)):

            @pl.loop(0, FOUR)
            def _(zz, out=out, half=half):
                at = pl.multiple_of((half * FOUR + zz) * BLK, BLK)
                h = self.h_own[:, :, :, pl.ds(at, BLK)].reshape(-1, BLK)
                out[zz] = dot(h, d_out, (0,), (0,)).reshape(out.shape[1:])

    def finish(self):
        for c in self.h_copies + self.homes:
            c.wait_send()


class HiddenGradient:
    tiles = FOUR

    def __init__(self, me, dk, dv, ins, outs, scratch):
        self.part, self.w_k, self.w_v, self.x, self.dy, self.gain = ins
        self.dx, self.terms = outs
        self.dk_home, self.dv_home, self.rows, *sems = scratch
        pairs = (dk, self.dk_home), (dv, self.dv_home)
        self.homes = [Home(me, src, out, *[r.at[i] for r in sems]) for i, (src, out) in enumerate(pairs)]
        for h in self.homes:
            h.start()

    @staticmethod
    def scratch(x):
        dma = pltpu.SemaphoreType.DMA
        home = pltpu.VMEM((TWO,) * 3 + (CHUNK, TWO * HEAD_DIM), BF16)
        return [home, home, pltpu.VMEM((8, x.shape[1]), F32), dma((TWO,)), dma((TWO, FOUR)), dma((TWO, FOUR))]

    def tile(self, t):
        if t == 0:
            for h in self.homes:
                h.wait_recv()
            self.rows[...] = jnp.zeros_like(self.rows)
        size = TWO * CHUNK
        at = pl.ds(t * size, size)
        d = self.part[at]
        for home, w in ((self.dk_home, self.w_k), (self.dv_home, self.w_v)):
            d += dot_t(home[t // TWO, t % TWO].reshape(size, -1), w[...])
        d = d.astype(BF16).astype(F32)
        x = self.x[at].astype(F32)
        inv_rms = lax.rsqrt(row_mean(x * x) + NORM_EPS)
        unit, scaled = x * inv_rms, d * self.gain[...]
        dx = inv_rms * (scaled - unit * row_mean(scaled * unit))
        self.dx[at] = (self.dy[at].astype(F32) + dx).astype(BF16)
        self.rows[...] += jnp.sum((d * unit).reshape((-1,) + self.rows.shape), axis=0)
        if t == self.tiles - 1:
            self.terms[...] = jnp.sum(self.rows[...], axis=0, keepdims=True)

    def finish(self):
        for h in self.homes:
            h.wait_send()


def reduce_pairs(arrays, blocks, cuts, kinds, collective_id, work, more):
    vmem, hbm = pl.BlockSpec(memory_space=pltpu.VMEM), pl.BlockSpec(memory_space=pl.ANY)
    n = len(blocks)
    scratch = [pltpu.VMEM((FOUR, TWO) + blocks[-1], F32)]
    scratch += sum((PairSum.scratch(k, b) for k, b in zip(kinds, blocks)), []) + PairSum.sems(n, max(cuts))
    outs = [jax.ShapeDtypeStruct(b, F32) for b in blocks] + work.results(more)
    return pl.pallas_call(
        functools.partial(reduce_kernel, cuts, kinds, work),
        name="reduce_pairs",
        out_shape=outs,
        in_specs=[hbm] * len(arrays) + [pl.BlockSpec(memory_space=m) for m in work.spaces],
        out_specs=[vmem] * n + [pl.BlockSpec(memory_space=m) for m in work.out_spaces],
        scratch_shapes=scratch + work.scratch(more),
        compiler_params=params(63, collective_id=collective_id),
        cost_estimate=cost(1, 20),
    )(*arrays, *more)


HERE = 0, 0, 0
LINKS = "xyud"
ORDERS = "zxy", "zyx", "xyz", "zyx"
SIZES = 8.4, 8.4, 5.6, 2.8
LATENCY, TILES_FROM, TILE_EVERY = 3.0, 14.0, 8.0
SUM_AT = 30.0, 42.0, 54.0, 66.0


def onward(order, key):
    dz, ry, rx = key
    stage = max((order.index(a) for a, r in zip("zyx", key) if r), default=-1)
    for axis in order[stage + 1 :]:
        if axis == "x":
            yield "x", (dz, ry, 1)
        elif axis == "y":
            yield "y", (dz, 1, rx)
        else:
            yield "u", (-1, ry, rx)
            yield "d", (1, ry, rx)
    if stage >= 0 and order[stage] == "z" and abs(dz) < 3:
        yield ("u", (dz - 1, ry, rx)) if dz < 0 else ("d", (dz + 1, ry, rx))


def arrivals():
    busy, times = {}, {}
    starts = [0.0] * 3 + [SUM_AT[-1] + LATENCY]
    here = [(t, z, part, HERE) for part, t in enumerate(starts) for z in range(FOUR)]
    while here:
        now, z, part, key = heapq.heappop(here)
        times.setdefault((part, key), []).append(now)
        for link, there in onward(ORDERS[part], key):
            to = z + {"u": 1, "d": -1}.get(link, 0)
            if 0 <= to <= 3:
                busy[z, link] = max(busy.get((z, link), 0), now) + SIZES[part]
                heapq.heappush(here, (busy[z, link] + LATENCY, to, part, there))
    return sorted((sum(t) / len(t), *at) for at, t in times.items())


def turn_back(dkv_ref, cos_ref, sin_ref, dk_u, dv_u):
    n = dk_u.shape[0] * dk_u.shape[1] * dk_u.shape[TWO]
    dk = turn(dkv_ref[pl.ds(0, n)] * ATTN_SCALE, cos_ref, sin_ref)
    dk_u[...] = dk.astype(BF16).reshape(dk_u.shape)
    dv_u[...] = dkv_ref[pl.ds(n, n)].astype(BF16).reshape(dv_u.shape)


def wkv_terms(h_own, dk_u, dv_u, outs):
    d_out = jnp.hstack([r[...].reshape(-1, HEAD_DIM) for r in (dk_u, dv_u)])
    for out, half in outs:

        @pl.loop(0, FOUR)
        def _(zz, out=out, half=half):
            at = pl.multiple_of((half * FOUR + zz) * BLK, BLK)
            h = h_own[:, :, :, pl.ds(at, BLK)].reshape(-1, BLK)
            out[zz] = dot(h, d_out, (0,), (0,)).reshape(out.shape[1:])


def gather_kernel(*refs):
    take = taker(refs)
    wo_ref, wq_ref, dkv_ref, cos_ref, sin_ref, h_ref = take(6)
    grad_ins, outs, (dx_ref, dgain_ref) = take(6), take(FOUR), take(TWO)
    own_sem, send_sem, come_sem, core_sem, all_terms, g_s, g_r = take(7)
    terms, wkv_own, wkv_ref, h_own, dk_u, dv_u = take(6)
    buffers, sems, refs = take(FOUR), take(7), take(len(refs))
    me = lax.axis_index("cp")
    z, y, x, core = place(me)
    line = Line(me)
    to = {"x": dev(z, y, 1 - x, core), "y": dev(z, 1 - y, x, core), "u": line.next[1], "d": line.next[-1]}
    partner = dev(z, y, x, 1 - core)
    others = [(i, me ^ i) for i in range(1, all_terms.shape[0])]
    meet([d for _, d in others])
    load_h = pltpu.make_async_copy(h_ref, h_own, own_sem.at[0])
    load_h.start()
    wkv = PairSum(me, "core", 1, wkv_ref, wkv_own, buffers, [r.at[0] for r in sems])

    def windows(part, zz, yy, xx, cc):
        pair = TWO * zz + yy
        wide, narrow = wq_ref.shape[1], wkv_own.shape[1] // TWO
        wo_at, wq_at = ((xx * TWO + cc) * N_PAIRS + pair) * wo_ref.shape[0], (cc * N_PAIRS + pair) * wq_ref.shape[0]
        if part == 3:
            for i, out in enumerate(outs[TWO:]):
                cols = pl.ds(xx * narrow, narrow)
                yield wkv_own.at[:, head_slice(i)], out.at[pl.ds(wq_at, wkv_own.shape[0]), cols]
            return
        eighth = wo_ref.shape[0] // 8
        at, rows = (part * 3 * eighth, (TWO if part == TWO else 3) * eighth)
        yield wo_ref.at[pl.ds(at, rows)], outs[0].at[pl.ds(wo_at + at, rows)]
        at, rows = TWO * at, TWO * rows
        yield wq_ref.at[pl.ds(at, rows)], outs[1].at[pl.ds(wq_at + at, rows), pl.ds(xx * wide, wide)]

    def block(part, key, cc=core):
        dz, ry, rx = key
        return windows(part, z + dz, 1 - y if ry else y, 1 - x if rx else x, cc)

    def index(part, key):
        return (part, key[0] + 3) + key[1:]

    def send(part, key, link, there):
        arrive = (core_sem if link is None else come_sem).at[index(part, there)]
        for shard, window in block(part, key):
            src = window if any(key) else shard
            remote(src, window, send_sem.at[index(part, key) + (LINKS.find(link or "-") + 1,)], arrive, to.get(link, partner)).start()

    def whole(part, send, arrive):
        size = sum(shard.size for shard, _ in block(part, HERE)) // outs[0].shape[1]
        dst = outs[0].at[pl.ds(0, size)]
        return remote(dst, dst, send, arrive, me)

    def when(on, do):
        pl.when(on)(do)

    def each_way(part, key):
        held = line.held(key[0])
        yield None, key, held
        for link, there in onward(ORDERS[part], key):
            inside = {"u": line.inside[1], "d": line.inside[-1]}.get(link)
            yield link, there, held if inside is None else jnp.logical_and(held, inside)

    def pass_on(part, key):
        for link, there, on in each_way(part, key):
            when(on, functools.partial(send, part, key, link, there))

    def term_copy(i, d):
        return remote(terms, all_terms.at[i], g_s.at[i], g_r.at[i], d)

    owns = []

    def put_own(part):
        for shard, window in block(part, HERE):
            owns.append(pltpu.make_async_copy(shard, window, own_sem.at[len(owns)]))
            owns[-1].start()

    def tile(t):
        job.tile(t)
        if t == job.tiles - 1:
            for i, d in others:
                term_copy(i, d).start()

    def sum_step(h):
        wkv.step(0, h)
        if h == 3:
            put_own(3)

    steps = [(TILES_FROM + t * TILE_EVERY, functools.partial(tile, t)) for t in range(HiddenGradient.tiles)]
    steps += [(at, functools.partial(sum_step, h)) for h, at in enumerate(SUM_AT)]
    steps.sort(key=lambda s: s[0])
    events = arrivals()
    for part in range(3):
        pass_on(part, HERE)
    turn_back(dkv_ref, cos_ref, sin_ref, dk_u, dv_u)
    job = HiddenGradient(me, dk_u, dv_u, grad_ins, (dx_ref, terms), refs)
    load_h.wait()
    wkv_terms(h_own, dk_u, dv_u, ((wkv_ref, 1 - core), (buffers[0], core)))
    wkv.begin(0)
    for part in range(3):
        put_own(part)
    wkv.loaded(0)
    for now, part, key in events:
        while steps and steps[0][0] <= now:
            steps.pop(0)[1]()
        if any(key):
            arrive = come_sem.at[index(part, key)]
            when(line.held(key[0]), whole(part, own_sem.at[0], arrive).wait_recv)
            pass_on(part, key)
        elif part == 3:
            pass_on(part, key)
    for o in owns:
        o.wait()
    total_gain = terms[...]
    for i, d in others:
        term_copy(i, d).wait_recv()
        total_gain += all_terms[i]
    dgain_ref[...] = total_gain
    for i, d in others:
        term_copy(i, d).wait_send()
    for _, part, key in events:
        when(line.held(key[0]), whole(part, own_sem.at[0], core_sem.at[index(part, key)]).wait_recv)
        for link, there, on in each_way(part, key):
            sent = send_sem.at[index(part, key) + (LINKS.find(link or "-") + 1,)]
            when(on, whole(part, sent, own_sem.at[0]).wait_send)
    wkv.wait_send(0)
    job.finish()


def gather_all(wo, wq, dkv, cos_f, sin_f, h_u, part, w_k, w_v, x, dy, gain, shapes):
    dma = pltpu.SemaphoreType.DMA
    vmem, hbm = pl.BlockSpec(memory_space=pltpu.VMEM), pl.BlockSpec(memory_space=pl.ANY)
    block = w_k.shape[0] // TWO // N_PAIRS, w_k.shape[1]
    parts = len(ORDERS)
    keys = (parts, 7, TWO, TWO)
    terms = 1, x.shape[1]
    scratch = [dma((TWO * parts,)), dma(keys + (len(LINKS) + 1,)), dma(keys), dma(keys)]
    scratch += [pltpu.VMEM((32,) + terms, F32), dma((32,)), dma((32,)), pltpu.VMEM(terms, F32), pltpu.VMEM(block, F32)]
    scratch += [pltpu.VMEM((FOUR, TWO) + block, F32), pltpu.VMEM(h_u.shape, BF16)]
    scratch += [pltpu.VMEM((TWO, TWO, BLK, HEAD_DIM), BF16)] * TWO
    return pl.pallas_call(
        gather_kernel,
        name="gather_all",
        out_shape=[jax.ShapeDtypeStruct(s, F32) for s in shapes]
        + [jax.ShapeDtypeStruct(x.shape, BF16), jax.ShapeDtypeStruct(terms, F32)],
        in_specs=[vmem] * 5 + [hbm] + [vmem] * 6,
        out_specs=[hbm] * len(shapes) + [vmem] * TWO,
        scratch_shapes=scratch + PairSum.scratch("core", block) + PairSum.sems(1, 1) + HiddenGradient.scratch(x),
        compiler_params=params(56, collective_id=0),
        cost_estimate=cost(1, 76),
    )(wo, wq, dkv, cos_f, sin_f, h_u, part, w_k, w_v, x, dy, gain)


def perm(x, pairs):
    return lax.ppermute(x, "cp", pairs)


def flip_pairs(d):
    return [(r, r ^ d) for r in range(32)]


def solution(mesh):
    def local_step(hidden, grad_out, positions, seg_ids, w_q, w_k, w_v, w_o, norm_gain):
        n_batch, n_tok, d_model = hidden.shape
        n_rows = n_batch * n_tok
        wide = N_HEADS * HEAD_DIM
        me = lax.axis_index("cp")
        _, y, x, core = place(me)
        quad, pair = me % FOUR, me // FOUR
        relations = range(FOUR)

        def rows_of(arr, d):
            return pick(arr.reshape((TWO, TWO, TWO, CHUNK) + arr.shape[TWO:]), core ^ (d % TWO), 0)

        def swap(pieces):
            return [perm(p, flip_pairs(d)) if d else p for d, p in enumerate(pieces)]

        def unite(arr):
            joined = jnp.stack(swap([rows_of(arr, d) for d in relations]), axis=TWO)
            return joined.reshape((TWO, TWO, BLK) + joined.shape[FOUR:])

        gain = norm_gain.astype(F32)
        cos_t, sin_t = rope_tables(positions.reshape(n_rows))
        cos_f, sin_f = jnp.hstack([cos_t, cos_t]), jnp.hstack([-sin_t, sin_t])
        normed, kv_home, q_home = project(hidden.reshape(n_rows, d_model), gain[NEW], w_q, w_k, w_v, cos_f, sin_f)
        pos_u = unite(positions)
        kv_all, q_u, dy_part = exchange(
            kv_home.reshape((TWO,) * 5 + (CHUNK, HEAD_DIM)),
            q_home.reshape((TWO,) * FOUR + (CHUNK, wide)),
            grad_out.reshape((TWO,) * 3 + (CHUNK, d_model)),
        )
        dy_last, dy_part = lax.optimization_barrier((rows_of(grad_out, LATER[1]), dy_part))
        dy_last = perm(dy_last, flip_pairs(LATER[1]))

        member = quad ^ jnp.arange(FOUR)
        front, back = ((m[:, NEW] * CHUNK + jnp.arange(CHUNK)[NEW]).reshape(BLK) for m in (member, 3 - member))
        offsets = jnp.stack([front, back]).astype(jnp.int32)
        own_super = jnp.stack([pair, N_SUPER - 1 - pair]).astype(jnp.int32)
        q_index = own_super[:, NEW] * BLK + offsets
        start = q_index[NEW] - pos_u
        koff = jnp.broadcast_to(offsets[:, :, NEW], (TWO, BLK, BLK))
        tab = jnp.concatenate(
            [own_super, (jnp.min(start, axis=-1) // BLK).reshape(-1), jnp.max(start, axis=-1).reshape(-1)]
        )
        start_r = start[:, :, NEW, :]
        q_index_r = jnp.broadcast_to(q_index[NEW, :, NEW, :], start_r.shape)
        cos_u, sin_u = rope_tables(pos_u)
        cos_ut, sin_ut = jnp.swapaxes(cos_u, TWO, 3), jnp.swapaxes(sin_u, TWO, 3)

        lanes = start.shape + (HEAD_DIM,)
        start_l, q_index_l = (jnp.broadcast_to(a[..., NEW], lanes) for a in (start, q_index[NEW]))
        attn_u, lse = flash_fwd(tab, q_u, kv_all, start_l, q_index_l, offsets[:, NEW])

        tok = tuple(range(3))
        half_wide = wide // TWO
        dy_u = jnp.concatenate([dy_part, dy_last], axis=TWO)
        wo_send = dot(dyn(attn_u, (1 - core) * half_wide, half_wide, 3), dy_u, tok, tok)
        wo_sum = dot(dyn(attn_u, core * half_wide, half_wide, 3), dy_u, tok, tok) + perm(wo_send, flip_pairs(1))
        wo_sum = wo_sum.reshape(FOUR, TWO, half_wide // N_PAIRS, d_model)
        wo_y = perm(pick(wo_sum, 1 - y, 1), flip_pairs(FOUR))

        d_attn = dot(dy_u, dyn(w_o, x * wide, wide, 0), (3,), (1,)).astype(BF16)
        d_attn, wo_sum = lax.optimization_barrier((d_attn, wo_sum))
        dq_u, dkv = flash_bwd(tab, q_u, d_attn, attn_u, kv_all, lse, start_r, q_index_r, koff, cos_ut, sin_ut)

        wo_sum = pick(wo_sum, y, 1) + wo_y

        x_flat = hidden.reshape(n_rows, d_model)
        wo_own, dkv_own, wq_own, block_out, d_part, h_u = reduce_pairs(
            [wo_sum, dkv.reshape(FOUR, TWO, -1, HEAD_DIM)],
            [wo_sum.shape[1:], (dkv.size // N_PAIRS // HEAD_DIM, HEAD_DIM), (d_model // TWO // N_PAIRS, wide)],
            (TWO, 8, FOUR),
            ("z", "", "core"),
            TWO,
            Products,
            (attn_u, dq_u, x_flat, normed.reshape((TWO,) * 3 + (CHUNK, d_model)), w_o, w_q),
        )
        cos_uf, sin_uf = jnp.concatenate([cos_u, cos_u], axis=-1), jnp.concatenate([sin_u, -sin_u], axis=-1)
        grad_wo, grad_wq, grad_wk, grad_wv, grad_x, d_gain = gather_all(
            wo_own,
            wq_own,
            dkv_own,
            cos_uf.reshape(-1, HEAD_DIM),
            sin_uf.reshape(-1, HEAD_DIM),
            h_u,
            d_part,
            w_k,
            w_v,
            x_flat,
            grad_out.reshape(n_rows, d_model),
            gain[NEW],
            [w_o.shape, w_q.shape, w_k.shape, w_v.shape],
        )
        block_out, grad_x = (a.reshape(hidden.shape) for a in (block_out, grad_x))
        return block_out, grad_x, grad_wq, grad_wk, grad_wv, grad_wo, d_gain.reshape(d_model)

    seq_spec = P(None, "cp", None)
    tok_spec = P(None, "cp")
    full_spec = P()
    return jax.shard_map(
        local_step,
        mesh=mesh,
        in_specs=(seq_spec, seq_spec, tok_spec, tok_spec, full_spec, full_spec, full_spec, full_spec, full_spec),
        out_specs=(seq_spec, seq_spec, full_spec, full_spec, full_spec, full_spec, full_spec),
        check_vma=False,
    )
```

```python
import functools
import heapq
import itertools

import jax
import jax.numpy as jnp
from jax import lax
from jax.experimental import pallas as pl
from jax.experimental.pallas import tpu as pltpu
from jax.sharding import PartitionSpec as P

HEAD_DIM = 128
NORM_EPS = 1e-5
ROPE_BASE = 500000.0
NEG_BIG = -1e30
LOG2E = 1.4426950408889634
ATTN_SCALE = HEAD_DIM**-0.5
EXP2_SCALE = ATTN_SCALE * LOG2E
CHUNK = 64
TWO = 2
FOUR = 4
NEW = jnp.newaxis
BLK = 4 * CHUNK
N_HEADS = 8
N_PAIRS = 8
N_SUPER = 2 * N_PAIRS
MESH = pl.DeviceIdType.MESH
ONE = pl.Squeezed()
MADE_AT = 5
PRODUCTS_AT = 7, 9
F32 = jnp.float32
BF16 = jnp.bfloat16

T_SQ, T_LO, T_MX = 0, 2, 6


def rope_tables(positions):
    inv_freq = ROPE_BASE ** (-jnp.arange(0, HEAD_DIM, TWO).astype(F32) / HEAD_DIM)
    angles = positions.astype(F32)[..., None] * inv_freq
    return jnp.cos(angles), jnp.sin(angles)


def dot(a, b, ca, cb):
    return lax.dot_general(a, b, ((ca, cb), ((), ())), preferred_element_type=F32)


def cost(gflop, mib):
    return pl.CostEstimate(flops=gflop * 10**9, bytes_accessed=mib << 20, transcendentals=0)


def params(mib, **more):
    return pltpu.CompilerParams(vmem_limit_bytes=mib << 20, **more)


def row_mean(x):
    return jnp.mean(x, axis=-1, keepdims=True)


def head(h):
    return pl.ds(h * HEAD_DIM, HEAD_DIM)


def head_slice(h):
    return slice(h * HEAD_DIM, (h + 1) * HEAD_DIM)


def dot_t(a, b):
    return dot(a, b, (1,), (1,))


def pick(x, index, axis):
    return lax.dynamic_index_in_dim(x, index, axis, keepdims=False)


def steps(tab, body):
    b, hf = pl.program_id(0), pl.program_id(1)
    own, first, last_start = tab[T_SQ + hf], tab[T_LO + TWO * b + hf], tab[T_MX + TWO * b + hf]

    def step(s, carry):
        late = s >= N_PAIRS
        at = jnp.where(late, N_SUPER - 1 - s, s), late.astype(jnp.int32)
        full = jnp.logical_and(s < own, s * BLK >= last_start)
        pl.when(full)(lambda: body(s, at, False))
        pl.when(jnp.logical_not(full))(lambda: body(s, at, True))
        return carry

    lax.fori_loop(first, own + 1, step, 0)


def down(row, n):
    return jnp.broadcast_to(row, (n, row.shape[-1])).T


def may_use(s, off, st_ref, qi_ref):
    return jnp.logical_and(off >= st_ref[...] - s * BLK, off <= qi_ref[...] - s * BLK)


def fwd_kernel(tab, q_ref, kv_ref, st_ref, qi_ref, ko_ref, o_ref, lse_ref, q_s, acc, m_s, l_s, k_t, bounds):
    m_s[...] = jnp.full_like(m_s, NEG_BIG)
    l_s[...] = jnp.zeros_like(l_s)
    acc[...] = jnp.zeros_like(acc)
    for i, ref in enumerate((st_ref, qi_ref)):
        bounds[i] = down(ref[...], HEAD_DIM)
    for h in range(N_HEADS):
        q_s[pl.ds(h * BLK, BLK)] = q_ref[:, head(h)]

    @pl.when(pl.program_id(1) == 0)
    def _():
        @pl.loop(0, N_PAIRS)
        def _(pair):
            for hk in range(TWO):
                k_t[pair, hk] = kv_ref[pair, 0, hk].T

    def body(s, at, masked):
        pair, hk = at
        v = kv_ref[pair, 1, hk]
        if masked:
            off = ko_ref[hk] + s * BLK
            mask = [
                jnp.logical_and(off[:, lanes] >= bounds[0], off[:, lanes] <= bounds[1])
                for lanes in (slice(HEAD_DIM), slice(HEAD_DIM, BLK))
            ]
            mask = [jnp.concatenate([m, m], axis=0) for m in mask]
        for g in range(N_HEADS // TWO):
            rows = pl.ds(g * TWO * BLK, TWO * BLK)
            sc = jnp.dot(q_s[rows], k_t[pair, hk], preferred_element_type=F32)
            sc = [sc[:, :HEAD_DIM], sc[:, HEAD_DIM:]]
            if masked:
                sc = [jnp.where(m, x, NEG_BIG) for m, x in zip(mask, sc)]
            m_old = m_s[rows]
            m_new = jnp.maximum(m_old, jnp.max(jnp.maximum(*sc), axis=1, keepdims=True))
            alpha = jnp.exp2((m_old - m_new) * EXP2_SCALE)
            p = [jnp.exp2((x - m_new) * EXP2_SCALE) for x in sc]
            m_s[rows] = m_new
            l_s[rows] = l_s[rows] * alpha + (p[0] + p[1])
            p = jnp.hstack([x.astype(BF16) for x in p])
            acc[rows] = acc[rows] * alpha + jnp.dot(p, v, preferred_element_type=F32)

    steps(tab, body)
    for h in range(N_HEADS):
        rows = pl.ds(h * BLK, BLK)
        total = jnp.sum(l_s[rows], axis=1, keepdims=True)
        o_ref[:, head(h)] = (acc[rows] / total).astype(BF16)
        lse_ref[h] = (m_s[rows] * EXP2_SCALE + jnp.log2(total)).T[:1]


def bwd_kernel(tab, q_ref, do_ref, o_ref, kv_ref, lse_ref, st_ref, qi_ref, ko_ref, cos_ref, sin_ref, dq_ref, dkv_ref, dq_acc, delta, off_s):
    dq_acc[...] = jnp.zeros_like(dq_acc)
    for h in range(N_HEADS):
        terms = do_ref[:, head(h)].astype(F32) * o_ref[:, head(h)].astype(F32)
        delta[h] = jnp.sum(terms.T, axis=0, keepdims=True)

    @pl.when(pl.program_id(1) == 0)
    def _():
        dkv_ref[...] = jnp.zeros_like(dkv_ref)
        for hk in range(TWO):
            off_s[hk] = down(ko_ref[hk], BLK)

    def body(s, at, masked):
        pair, hk = at
        k = kv_ref[pair, 0, hk]
        v = kv_ref[pair, 1, hk]
        k_t = k.T
        mask = may_use(s, off_s[hk], st_ref, qi_ref) if masked else None
        dk = dv = jnp.zeros((BLK, HEAD_DIM), F32)
        for h in range(N_HEADS):
            q = q_ref[:, head(h)]
            do = do_ref[:, head(h)]
            p = jnp.exp2(dot_t(k, q) * EXP2_SCALE - lse_ref[h])
            if masked:
                p = jnp.where(mask, p, 0.0)
            ds = (p * (dot_t(v, do) - delta[h])).astype(BF16)
            dv += jnp.dot(p.astype(BF16), do, preferred_element_type=F32)
            dk += jnp.dot(ds, q, preferred_element_type=F32)
            dq_acc[h] += jnp.dot(k_t, ds, preferred_element_type=F32)
        dkv_ref[pair, 0, hk] += dk
        dkv_ref[pair, 1, hk] += dv

    steps(tab, body)
    cos_t, sin_t = cos_ref[...], sin_ref[...]
    half = HEAD_DIM // TWO
    for h in range(N_HEADS):
        a, c = dq_acc[h, :half] * ATTN_SCALE, dq_acc[h, half:] * ATTN_SCALE
        lin = jnp.concatenate([a * cos_t + c * sin_t, c * cos_t - a * sin_t], axis=0)
        dq_ref[:, head(h)] = lin.T.astype(BF16)


def attn_specs():
    def at_tile(b, h, t):
        return (b, h) + (0,) * TWO

    def at_row(b, h, t):
        return (0, 0, b) + (0,) * 3

    tile = pl.BlockSpec((ONE, ONE, BLK, N_HEADS * HEAD_DIM), at_tile)
    row = pl.BlockSpec((ONE, ONE, 1, BLK), at_tile)
    stat = pl.BlockSpec((ONE, ONE, N_HEADS, 1, BLK), lambda b, h, t: (b, h) + (0,) * 3)
    rope = pl.BlockSpec((ONE, ONE, HEAD_DIM // TWO, BLK), at_tile)
    kv = pl.BlockSpec((N_PAIRS, TWO, ONE, TWO, BLK, HEAD_DIM), at_row)
    ko = pl.BlockSpec((TWO, 1, BLK), lambda b, h, t: (0,) * 3)
    return tile, row, stat, kv, ko, rope


def flash_fwd(tab, q, kv, start, qidx, koff):
    tile, row, stat, kvs, ko, _ = attn_specs()
    return pl.pallas_call(
        fwd_kernel,
        name="attn_fwd",
        out_shape=(jax.ShapeDtypeStruct(q.shape, BF16), jax.ShapeDtypeStruct((TWO, TWO, N_HEADS, 1, BLK), F32)),
        grid_spec=pltpu.PrefetchScalarGridSpec(
            num_scalar_prefetch=1,
            grid=(TWO, TWO),
            in_specs=[tile, kvs, row, row, ko],
            out_specs=[tile, stat],
            scratch_shapes=[pltpu.VMEM((N_HEADS * BLK, HEAD_DIM), t) for t in (BF16, F32, F32, F32)]
            + [pltpu.VMEM((N_PAIRS, TWO, HEAD_DIM, BLK), BF16), pltpu.VMEM((TWO, BLK, HEAD_DIM), jnp.int32)],
        ),
        compiler_params=params(40),
        cost_estimate=cost(20, 16),
    )(tab, q, kv, start, qidx, koff)


def flash_bwd(tab, q, do, o, kv, lse, start, qidx, koff, cos_t, sin_t):
    tile, row, stat, kvs, ko, rope = attn_specs()
    return pl.pallas_call(
        bwd_kernel,
        name="attn_bwd",
        out_shape=(
            jax.ShapeDtypeStruct(q.shape, BF16),
            jax.ShapeDtypeStruct(kv.shape, F32),
        ),
        grid_spec=pltpu.PrefetchScalarGridSpec(
            num_scalar_prefetch=1,
            grid=(TWO, TWO),
            in_specs=[tile, tile, tile, kvs, stat, row, row, ko, rope, rope],
            out_specs=[tile, kvs],
            scratch_shapes=[pltpu.VMEM((N_HEADS, HEAD_DIM, BLK), F32), pltpu.VMEM((N_HEADS, 1, BLK), F32)]
            + [pltpu.VMEM((TWO, BLK, BLK), jnp.int32)],
        ),
        compiler_params=params(48),
        cost_estimate=cost(50, 32),
    )(tab, q, do, o, kv, lse, start, qidx, koff, cos_t, sin_t)


def turn(x, cos_ref, sin_ref):
    return x * cos_ref[...] + pltpu.roll(x, HEAD_DIM // TWO, 1) * sin_ref[...]


def first_kernel(x_ref, g_ref, wk_ref, wv_ref, cos_ref, sin_ref, h_ref, kv_ref):
    x = x_ref[...].astype(F32)
    h = (x * lax.rsqrt(row_mean(x * x) + NORM_EPS) * g_ref[...]).astype(BF16)
    h_ref[...] = h
    k = jnp.dot(h, wk_ref[...], preferred_element_type=F32)
    v = jnp.dot(h, wv_ref[...], preferred_element_type=F32)
    n = kv_ref.shape[3]
    for i in range(TWO):
        for j, val in enumerate((turn(k[:, head_slice(i)], cos_ref, sin_ref), v[:, head_slice(i)])):
            for c in range(TWO):
                kv_ref[i, c, j] = val[c * n : (c + 1) * n].astype(BF16)


def project(x, gain, w_k, w_v, cos_f, sin_f):
    n = x.shape[0] // TWO
    return pl.pallas_call(
        first_kernel,
        name="norm_kv",
        out_shape=(jax.ShapeDtypeStruct(x.shape, BF16), jax.ShapeDtypeStruct((TWO,) * 3 + (n, HEAD_DIM), BF16)),
        compiler_params=params(40),
        cost_estimate=cost(TWO, 7),
    )(x, gain, w_k, w_v, cos_f, sin_f)


def place(me):
    return me // 8, lax.rem(me // FOUR, TWO), lax.rem(me // TWO, TWO), lax.rem(me, TWO)


def dev(z, y, x, core):
    return ((z * TWO + y) * TWO + x) * TWO + core


def z_peers(z):
    return [(k, lax.rem(z + k, FOUR)) for k in (1, TWO, 3)]


def meet(peers):
    barrier = pltpu.get_barrier_semaphore()
    for d in peers:
        pl.semaphore_signal(barrier, device_id=(d,), device_id_type=MESH)
    pl.semaphore_wait(barrier, len(peers))


def remote(src, dst, send, arrive, to):
    return pltpu.make_async_remote_copy(
        src_ref=src, dst_ref=dst, send_sem=send, recv_sem=arrive, device_id=(to,), device_id_type=MESH
    )


class Line:
    order = (0, 1, -1, TWO, -TWO, 3, -3)

    def __init__(self, me):
        self.z, y, x, core = place(me)
        self.next = {1: dev(self.z + 1, y, x, core), -1: dev(self.z - 1, y, x, core)}
        self.inside = {1: self.z < 3, -1: self.z > 0}

    def held(self, dz):
        return jnp.logical_and(self.z + dz >= 0, self.z + dz <= 3)

    def ways(self, dz):
        for d in self.next:
            if d * dz <= 0:
                yield d, self.inside[d] if dz == 0 else jnp.logical_and(self.inside[d], self.held(dz))


def tiled(n, fetch, use, first=0):
    fetch(first, 0).start()

    @pl.loop(0, n)
    def _(t):
        slot = lax.rem(t, TWO)
        fetch(first + t, slot).wait()

        @pl.when(t + 1 < n)
        def _():
            fetch(first + t + 1, 1 - slot).start()

        use(first + t, slot)


def aligned(t, size=BLK):
    return pl.ds(pl.multiple_of(t * size, size), size)


def exchange_kernel(*refs):
    take = taker(refs)
    kv_ref, h_ref, dy_ref, cos_ref, sin_ref, wq_ref, wo_ref, kv_all, q_u, do_u = take(10)
    own_sem, quad_s, quad_r, z_s, z_r, y_s, y_r, q_home, do_home, wq_buf, wo_buf, w_sem = take(len(refs))
    me = lax.axis_index("cp")
    z, y, x, core = place(me)
    quad, line = quad_of(me), Line(me)
    across = dev(z, 1 - y, x, core)
    meet(quad[1:] + [across] + [dev(zz, y, x, core) for _, zz in z_peers(z)])

    def source(a, d):
        xx, cc = 1 - x if d // TWO else x, 1 - core if d % TWO else core
        return (kv_ref, q_home, do_home)[a].at[xx, cc]

    def target(a, d):
        tok = pl.ds(d * CHUNK, CHUNK)
        return kv_all.at[me // FOUR, :, :, :, tok] if a == 0 else (q_u, do_u)[a - 1].at[:, :, tok]

    def quad_copy(a, d):
        return remote(source(a, d), target(a, d), quad_s.at[a, d], quad_r.at[a, d], quad[d])

    def own_copy(a):
        return pltpu.make_async_copy(source(a, 0), target(a, 0), own_sem.at[a])

    def z_copy(part, dz, d):
        block = kv_all.at[TWO * (z + dz) + y, part]
        return remote(block, block, z_s.at[part, (d + 1) // TWO, dz + 3], z_r.at[part, dz - d + 3], line.next[d])

    def y_copy(part, dz, yy=y):
        block = kv_all.at[TWO * (z + dz) + yy, part]
        return remote(block, block, y_s.at[part, dz + 3], y_r.at[part, dz + 3], across)

    parts = range(TWO)
    moves = [(part, dz) for dz in line.order for part in parts]

    def pass_on(count):
        for part, dz in [moves.pop(0) for _ in range(count)]:
            if dz:
                block = kv_all.at[TWO * (z + dz) + y, part]
                arrival = remote(block, block, own_sem.at[0], z_r.at[part, dz + 3], me)
                pl.when(line.held(dz))(arrival.wait_recv)
            for d, on in line.ways(dz):
                pl.when(on)(z_copy(part, dz, d).start)
            pl.when(line.held(dz))(y_copy(part, dz).start)

    n = h_ref.shape[1] // BLK // TWO

    def fetch_q(t, slot):
        return pltpu.make_async_copy(wq_ref.at[:, aligned(t)], wq_buf.at[slot], w_sem.at[0, slot])

    def fetch_o(t, slot):
        return pltpu.make_async_copy(wo_ref.at[aligned(t)], wo_buf.at[slot], w_sem.at[1, slot])

    def put(home, t, val):
        home[t // n, :, :, :, :, aligned(lax.rem(t, n))] = val.astype(BF16).reshape(home.shape[1:-1] + (BLK,))

    def query(t, slot):
        q = jnp.dot(h_ref[...], wq_buf[slot], preferred_element_type=F32)
        put(q_home, t, jnp.hstack([turn(q[:, head_slice(j)], cos_ref, sin_ref) for j in range(BLK // HEAD_DIM)]))

    def pull(t, slot):
        put(do_home, t, dot_t(dy_ref[...], wo_buf[slot]))

    all_moves = list(moves)
    for d in (1, TWO, 3):
        quad_copy(0, d).start()
    own_copy(0).start()
    for a, (fetch, use) in enumerate(((fetch_q, query), (fetch_o, pull)), 1):
        for near in range(TWO):
            tiled(n, fetch, use, n * (x if near else 1 - x))
            for d in range(TWO):
                if d or not near:
                    quad_copy(a, d if near else d + TWO).start()
            if near:
                own_copy(a).start()
            if len(moves) == len(all_moves):
                own_copy(0).wait()
                for d in (1, TWO, 3):
                    quad_copy(0, d).wait_recv()
            pass_on(TWO)
    pass_on(len(moves))
    for part, dz in all_moves:
        for d, on in line.ways(dz):
            pl.when(on)(z_copy(part, dz, d).wait_send)
        pl.when(line.held(dz))(y_copy(part, dz, 1 - y).wait_recv)
        pl.when(line.held(dz))(y_copy(part, dz).wait_send)
    for a in range(3):
        for d in (1, TWO, 3):
            quad_copy(a, d).wait_send()
            if a > 0:
                quad_copy(a, d).wait_recv()
    own_copy(1).wait()
    own_copy(TWO).wait()


def exchange(kv, h, dy, cos_f, sin_f, w_q, w_o):
    dma = pltpu.SemaphoreType.DMA
    vmem, hbm = pl.BlockSpec(memory_space=pltpu.VMEM), pl.BlockSpec(memory_space=pl.ANY)
    wide = w_q.shape[1] // TWO
    unit = jax.ShapeDtypeStruct((TWO, TWO, BLK, wide), BF16)
    home = pltpu.VMEM((TWO,) * FOUR + (CHUNK, wide), BF16)
    sems = [dma((3,))] + [dma((3, FOUR))] * TWO + [dma((TWO, TWO, 7))] + [dma((TWO, 7))] * 3
    bufs = [pltpu.VMEM((TWO,) + b, BF16) for b in ((w_q.shape[0], BLK), (BLK, w_o.shape[1]))]
    return pl.pallas_call(
        exchange_kernel,
        name="exchange",
        out_shape=(jax.ShapeDtypeStruct((N_PAIRS,) + (TWO,) * 3 + (BLK, HEAD_DIM), BF16), unit, unit),
        in_specs=[vmem] * 5 + [hbm] * TWO,
        out_specs=[hbm] * 3,
        scratch_shapes=sems + [home, home] + bufs + [dma((TWO, TWO))],
        compiler_params=params(40, collective_id=1),
        cost_estimate=cost(1, 20),
    )(kv, h, dy, cos_f, sin_f, w_q, w_o)


def taker(refs):
    rest = iter(refs)
    return lambda count: list(itertools.islice(rest, count))


def wo_kernel(*refs):
    take = taker(refs)
    o_ref, dy_ref, pieces = take(1) + take(1) + [take(3)]
    keep, away, dy_u, o_t, terms, came, load_sem, core_s, core_r = take(len(refs))
    me = lax.axis_index("cp")
    _, y, _, core = place(me)
    meet(quad_of(me)[1:TWO])
    loads = [
        pltpu.make_async_copy(src, dy_u.at[:, :, pl.ds(d * CHUNK, CHUNK)], load_sem.at[d])
        for d, src in enumerate([dy_ref.at[core]] + pieces)
    ]
    for c in loads:
        c.start()
    for h in range(N_HEADS):
        o_t[head(h)] = o_ref[:, :, :, head(h)].reshape(-1, HEAD_DIM).T
    for c in loads:
        c.wait()
    half = terms.shape[1]

    def half_terms(i, to):
        @pl.loop(0, terms.shape[TWO] // BLK)
        def _(t):
            dy = dy_u[:, :, :, aligned(t)].reshape(-1, BLK)
            terms[to, :, aligned(t)] = jnp.dot(o_t[aligned(i, half)], dy, preferred_element_type=F32)

    half_terms(1 - core, 0)
    swap = remote(terms.at[0], came, core_s, core_r, quad_of(me)[1])
    swap.start()
    half_terms(core, 1)
    swap.wait_recv()
    rows = keep.shape[1]
    for zz in range(FOUR):
        for out, yy in ((keep, y), (away, 1 - y)):
            at = aligned(TWO * zz + yy, rows)
            out[zz] = terms[1, at] + came[at]
    swap.wait_send()


def wo_terms(o, dy, pieces):
    dma = pltpu.SemaphoreType.DMA
    vmem, hbm = pl.BlockSpec(memory_space=pltpu.VMEM), pl.BlockSpec(memory_space=pl.ANY)
    n, d, wide = o.shape[0] * o.shape[1] * o.shape[TWO], dy.shape[-1], o.shape[-1]
    half = wide // TWO
    return pl.pallas_call(
        wo_kernel,
        name="wo_terms",
        out_shape=[jax.ShapeDtypeStruct((FOUR, half // N_PAIRS, d), F32)] * TWO,
        in_specs=[vmem] + [hbm] * FOUR,
        out_specs=[vmem] * TWO,
        scratch_shapes=[pltpu.VMEM((TWO, TWO, BLK, d), BF16), pltpu.VMEM((wide, n), BF16)]
        + [pltpu.VMEM((TWO, half, d), F32), pltpu.VMEM((half, d), F32), dma((FOUR,)), dma(()), dma(())],
        compiler_params=params(40, collective_id=3),
        cost_estimate=cost(FOUR, 20),
    )(o, dy, *pieces)


class PairSum:
    def __init__(self, me, kind, cut, src, out, buffers, sems):
        self.me, self.kind, self.src, self.out = me, kind, src, out
        self.size = out.shape[0] // cut
        self.own, self.from_core, self.from_y, self.from_z = buffers
        self.load_sem, self.core_s, self.core_r, self.y_s, self.y_r, self.z_s, self.z_r = sems
        self.z, self.y, x, core = place(me)
        self.partner = dev(self.z, self.y, x, 1 - core)
        self.across = dev(self.z, 1 - self.y, x, core)
        self.next_z = dev(self.z + 1, self.y, x, core), dev(self.z - 1, self.y, x, core)

    def rows(self, j):
        return pl.ds(j * self.size, self.size)

    def mine(self, j, zz):
        at = self.rows(j)
        return self.own.at[zz, self.y, at] if self.kind == "core" else self.own.at[zz, at]

    def load(self, j):
        at = self.rows(j)
        src = self.src.at[:, at] if self.kind else self.src.at[:, self.y, at]
        return pltpu.make_async_copy(src, self.own.at[:, at], self.load_sem.at[j])

    def core_copy(self, j):
        src, dst = (r.at[:, :, self.rows(j)] for r in (self.src, self.from_core))
        return remote(src, dst, self.core_s.at[j], self.core_r.at[j], self.partner)

    def y_copy(self, j):
        src = self.own if self.kind == "core" else self.src
        at = self.rows(j)
        return remote(src.at[:, 1 - self.y, at], self.from_y.at[:, at], self.y_s.at[j], self.y_r.at[j], self.across)

    def z_copy(self, j, way, zz, to):
        at = way, zz + way - 1
        return remote(self.mine(j, zz), self.from_z.at[*at, self.rows(j)], self.z_s.at[j, *at], self.z_r.at[j, *at], to)

    def begin(self, j):
        if self.kind == "core":
            self.core_copy(j).start()
            return
        self.load(j).start()
        if not self.kind:
            self.y_copy(j).start()

    def loaded(self, j):
        if self.kind != "core":
            self.load(j).wait()
        else:
            self.core_copy(j).wait_recv()
            at = self.rows(j)
            for zz in range(FOUR):
                self.own[zz, :, at] += self.from_core[zz, :, at]
            self.y_copy(j).start()
        if self.kind == "z":
            self.hop(j, 0)

    def relay(self, j, way, zz, add):
        if add:
            self.z_copy(j, way, zz, self.me).wait_recv()
            self.mine(j, zz)[...] += self.from_z[way, zz + way - 1, self.rows(j)]
        self.z_copy(j, way, zz, self.next_z[way]).start()

    def hop(self, j, h):
        @pl.when(self.z == h)
        def _():
            for zz in range(3, h, -1):
                self.relay(j, 0, zz, h > 0)

        @pl.when(self.z == 3 - h)
        def _():
            for zz in range(3 - h):
                self.relay(j, 1, zz, h > 0)

    def step(self, j, h):
        if h == 0 and self.kind != "z":
            self.y_copy(j).wait_recv()
            for zz in range(FOUR):
                self.mine(j, zz)[...] += self.from_y[zz, self.rows(j)]
            self.hop(j, 0)
        elif 0 < h < 3:
            self.hop(j, h)
        elif h == 3:
            at = self.rows(j)
            self.out[at] = self.mine(j, self.z)[...]
            for way, on in enumerate((self.z > 0, self.z < 3)):

                @pl.when(on)
                def _(way=way):
                    self.z_copy(j, way, self.z, self.me).wait_recv()
                    self.out[at] += self.from_z[way, self.z + way - 1, at]

    def wait_send(self, j):
        if self.kind == "core":
            self.core_copy(j).wait_send()
        if self.kind != "z":
            self.y_copy(j).wait_send()
        for zz in range(FOUR):
            if zz > 0:
                pl.when(self.z < zz)(self.z_copy(j, 0, zz, self.next_z[0]).wait_send)
            if zz < 3:
                pl.when(self.z > zz)(self.z_copy(j, 1, zz, self.next_z[1]).wait_send)

    @staticmethod
    def scratch(kind, block):
        unused = pltpu.VMEM((8, HEAD_DIM), F32)
        own = pltpu.VMEM(((FOUR, TWO) if kind == "core" else (FOUR,)) + block, F32)
        from_y = unused if kind == "z" else pltpu.VMEM((FOUR,) + block, F32)
        return [own, own if kind == "core" else unused, from_y, pltpu.VMEM((TWO, 3) + block, F32)]

    @staticmethod
    def sems(*dims):
        dma = pltpu.SemaphoreType.DMA
        return [dma(dims)] * 5 + [dma(dims + (TWO, 3))] * TWO


def reduce_kernel(cuts, kinds, work, *refs):
    n = len(cuts)

    take = taker(refs)
    ins, more_in, outs, more_out, made = take(n - 1), take(work.ins), take(n), take(work.outs), take(1)
    buffers, sems = [take(FOUR) for _ in kinds], take(7)
    me = lax.axis_index("cp")
    z, y, x, core = place(me)
    meet(quad_of(me)[1:] + [dev(z, 1 - y, x, core)] + [dev(zz, y, x, core) for _, zz in z_peers(z)])
    job = work(me, more_in, more_out, take(len(refs)))
    sums = [PairSum(me, *a, [r.at[i] for r in sems]) for i, a in enumerate(zip(kinds, cuts, ins + made, outs, buffers))]
    pieces = [(s, j) for s, cut in zip(sums, cuts) for j in range(cut)]
    early, late = pieces[: -cuts[-1]], pieces[-cuts[-1] :]
    for s, j in early:
        s.begin(j)
    for s, j in early:
        s.loaded(j)
    for t in range(len(pieces) + 3):
        if t == MADE_AT:
            job.wq_terms(sums[-1].own, made[0])
            for s, j in late:
                s.begin(j)
        if t == MADE_AT + 1:
            for s, j in late:
                s.loaded(j)
        for h in range(FOUR):
            if 0 <= t - h < len(pieces):
                s, j = pieces[t - h]
                s.step(j, h)
        job.step(t)
    for s, j in pieces:
        s.wait_send(j)
    job.finish()


def quad_of(me):
    z, y, x, core = place(me)
    return [dev(z, y, 1 - x if d // TWO else x, 1 - core if d % TWO else core) for d in range(FOUR)]


class Home:
    def __init__(self, me, src, out, own_sem, send, arrive):
        _, _, x, core = place(me)
        w = src.shape[-1]
        to = out.at[core, :, :, :, pl.ds(x * w, w)]

        def piece(d):
            return src.at[:, :, pl.ds(d * CHUNK, CHUNK)]

        self.own = pltpu.make_async_copy(piece(0), to, own_sem)
        self.copies = [remote(piece(d), to, send.at[d], arrive.at[d], quad_of(me)[d]) for d in (1, TWO, 3)]

    def start(self):
        self.own.start()
        for c in self.copies:
            c.start()

    def wait_recv(self):
        self.own.wait()
        for c in self.copies:
            c.wait_recv()

    def wait_send(self):
        for c in self.copies:
            c.wait_send()


class Products:
    ins, outs = 6, 3

    def __init__(self, me, ins, outs, scratch):
        attn, self.dq, hidden, normed, self.w_o, self.w_q = ins
        self.block_out, self.d_part, self.h_u = outs
        self.attn_home, self.dq_home, self.buf_o, self.buf_q, self.h_own, *sems = scratch
        self.w_sem, self.load_sem, own_sem, quad_s, quad_r = sems
        _, _, _, core = place(me)

        def piece(d):
            return normed.at[1 - core if d % TWO else core]

        def tokens(d):
            return self.h_u.at[:, :, pl.ds(d * CHUNK, CHUNK)]

        self.h_copies = [remote(piece(d), tokens(d), quad_s.at[TWO, d], quad_r.at[TWO, d], quad_of(me)[d]) for d in (1, TWO, 3)]
        self.h_mine = pltpu.make_async_copy(piece(0), self.h_own.at[:, :, pl.ds(0, CHUNK)], own_sem.at[TWO])
        self.h_rest = pltpu.make_async_copy(
            self.h_u.at[:, :, pl.ds(CHUNK, BLK - CHUNK)], self.h_own.at[:, :, pl.ds(CHUNK, BLK - CHUNK)], self.load_sem
        )
        self.h_back = pltpu.make_async_copy(self.h_own.at[:, :, pl.ds(0, CHUNK)], tokens(0), self.load_sem)
        self.residual = pltpu.make_async_copy(hidden, self.block_out, own_sem.at[3])
        self.residual.start()
        for c in self.h_copies:
            c.start()
        self.h_mine.start()
        self.homes = [
            Home(me, src, out, own_sem.at[i], quad_s.at[i], quad_r.at[i])
            for i, (src, out) in enumerate([(attn, self.attn_home), (self.dq, self.dq_home)])
        ]
        for h in self.homes:
            h.start()

    @staticmethod
    def scratch(arrays):
        dma, d = pltpu.SemaphoreType.DMA, arrays[-1].shape[0]
        home = pltpu.VMEM((TWO,) * 3 + (CHUNK, d), BF16)
        buf = [pltpu.VMEM((TWO,) + b, BF16) for b in ((d, BLK), (BLK, d))]
        unit = pltpu.VMEM((TWO, TWO, BLK, d), BF16)
        return [home] * TWO + buf + [unit, dma((TWO, TWO)), dma(()), dma((FOUR,)), dma((3, FOUR)), dma((3, FOUR))]

    @staticmethod
    def results(arrays):
        unit = TWO, TWO, BLK, arrays[-1].shape[0]
        return [jax.ShapeDtypeStruct(arrays[TWO].shape, t) for t in (BF16, F32)] + [jax.ShapeDtypeStruct(unit, BF16)]

    spaces, out_spaces = [pl.ANY, pltpu.VMEM] + [pl.ANY] * FOUR, [pltpu.VMEM] * TWO + [pl.ANY]

    def step(self, t):
        def fetch_o(t, slot):
            return pltpu.make_async_copy(self.w_o.at[:, aligned(t)], self.buf_o.at[slot], self.w_sem.at[0, slot])

        def fetch_q(t, slot):
            return pltpu.make_async_copy(self.w_q.at[aligned(t)], self.buf_q.at[slot], self.w_sem.at[1, slot])

        def project(t, slot):
            at = aligned(t)
            attn = self.attn_home[...].reshape(-1, self.w_o.shape[0])
            out = jnp.dot(attn, self.buf_o[slot], preferred_element_type=F32)
            self.block_out[:, at] = (self.block_out[:, at].astype(F32) + out).astype(BF16)

        def pull(t, slot):
            dq = self.dq_home[...].reshape(-1, self.w_o.shape[0])
            self.d_part[:, aligned(t)] = dot_t(dq, self.buf_q[slot])

        if t in PRODUCTS_AT:
            i = PRODUCTS_AT.index(t)
            self.homes[i].wait_recv()
            if i == 0:
                self.residual.wait()
            tiled(self.w_o.shape[0] // BLK, *((fetch_o, project), (fetch_q, pull))[i])

    def wq_terms(self, own, other):
        self.h_mine.wait()
        self.h_back.start()
        for c in self.h_copies:
            c.wait_recv()
        self.h_back.wait()
        self.h_rest.start()
        self.h_rest.wait()
        core = lax.rem(lax.axis_index("cp"), TWO)
        d_out = self.dq[...].reshape(-1, self.dq.shape[-1])
        for out, half in ((other, 1 - core), (own, core)):

            @pl.loop(0, FOUR)
            def _(zz, out=out, half=half):
                h = self.h_own[:, :, :, aligned(half * FOUR + zz)].reshape(-1, BLK)
                out[zz] = dot(h, d_out, (0,), (0,)).reshape(out.shape[1:])

    def finish(self):
        for c in self.h_copies + self.homes:
            c.wait_send()


class HiddenGradient:
    tiles = FOUR

    def __init__(self, me, dk, dv, ins, outs, scratch):
        self.part, self.w_k, self.w_v, self.x, self.dy, self.gain = ins
        self.dx, self.terms = outs
        self.dk_home, self.dv_home, self.rows, *sems = scratch
        pairs = (dk, self.dk_home), (dv, self.dv_home)
        self.homes = [Home(me, src, out, *[r.at[i] for r in sems]) for i, (src, out) in enumerate(pairs)]
        for h in self.homes:
            h.start()

    @staticmethod
    def scratch(x):
        dma = pltpu.SemaphoreType.DMA
        home = pltpu.VMEM((TWO,) * 3 + (CHUNK, TWO * HEAD_DIM), BF16)
        return [home, home, pltpu.VMEM((8, x.shape[1]), F32), dma((TWO,)), dma((TWO, FOUR)), dma((TWO, FOUR))]

    def tile(self, t):
        if t == 0:
            for h in self.homes:
                h.wait_recv()
            self.rows[...] = jnp.zeros_like(self.rows)
        size = TWO * CHUNK
        at = pl.ds(t * size, size)
        d = self.part[at]
        for home, w in ((self.dk_home, self.w_k), (self.dv_home, self.w_v)):
            d += dot_t(home[t // TWO, t % TWO].reshape(size, -1), w[...])
        d = d.astype(BF16).astype(F32)
        x = self.x[at].astype(F32)
        inv_rms = lax.rsqrt(row_mean(x * x) + NORM_EPS)
        unit, scaled = x * inv_rms, d * self.gain[...]
        dx = inv_rms * (scaled - unit * row_mean(scaled * unit))
        self.dx[at] = (self.dy[at].astype(F32) + dx).astype(BF16)
        self.rows[...] += jnp.sum((d * unit).reshape((-1,) + self.rows.shape), axis=0)
        if t == self.tiles - 1:
            self.terms[...] = jnp.sum(self.rows[...], axis=0, keepdims=True)

    def finish(self):
        for h in self.homes:
            h.wait_send()


def reduce_pairs(arrays, blocks, cuts, kinds, collective_id, work, more):
    vmem, hbm = pl.BlockSpec(memory_space=pltpu.VMEM), pl.BlockSpec(memory_space=pl.ANY)
    n = len(blocks)
    scratch = [pltpu.VMEM((FOUR, TWO) + blocks[-1], F32)]
    scratch += sum((PairSum.scratch(k, b) for k, b in zip(kinds, blocks)), []) + PairSum.sems(n, max(cuts))
    outs = [jax.ShapeDtypeStruct(b, F32) for b in blocks] + work.results(more)
    return pl.pallas_call(
        functools.partial(reduce_kernel, cuts, kinds, work),
        name="reduce_pairs",
        out_shape=outs,
        in_specs=[hbm] * len(arrays) + [pl.BlockSpec(memory_space=m) for m in work.spaces],
        out_specs=[vmem] * n + [pl.BlockSpec(memory_space=m) for m in work.out_spaces],
        scratch_shapes=scratch + work.scratch(more),
        compiler_params=params(63, collective_id=collective_id),
        cost_estimate=cost(1, 20),
    )(*arrays, *more)


HERE = 0, 0, 0
LINKS = "xyud"
ORDERS = "zxy", "zyx", "yxz", "zxy"
WO_CUTS, WQ_CUTS = (0, 3, 7, 8), (0, 3, 6, 8)
SIZES = 8.4, 9.8, 4.2, 2.8
LATENCY, TILES_FROM, TILE_EVERY = 3.0, 14.0, 8.0
SUM_AT = 30.0, 41.0, 52.0, 63.0


def onward(order, key):
    dz, ry, rx = key
    stage = max((order.index(a) for a, r in zip("zyx", key) if r), default=-1)
    for axis in order[stage + 1 :]:
        if axis == "x":
            yield "x", (dz, ry, 1)
        elif axis == "y":
            yield "y", (dz, 1, rx)
        else:
            yield "u", (-1, ry, rx)
            yield "d", (1, ry, rx)
    if stage >= 0 and order[stage] == "z" and abs(dz) < 3:
        yield ("u", (dz - 1, ry, rx)) if dz < 0 else ("d", (dz + 1, ry, rx))


def arrivals():
    busy, times = {}, {}
    starts = [0.0] * 3 + [SUM_AT[-1] + LATENCY]
    here = [(t, z, part, HERE) for part, t in enumerate(starts) for z in range(FOUR)]
    while here:
        now, z, part, key = heapq.heappop(here)
        times.setdefault((part, key), []).append(now)
        for link, there in onward(ORDERS[part], key):
            to = z + {"u": 1, "d": -1}.get(link, 0)
            if 0 <= to <= 3:
                busy[z, link] = max(busy.get((z, link), 0), now) + SIZES[part]
                heapq.heappush(here, (busy[z, link] + LATENCY, to, part, there))
    return sorted((sum(t) / len(t), *at) for at, t in times.items())


def turn_back(dkv_ref, cos_ref, sin_ref, dk_u, dv_u):
    n = TWO * TWO * BLK
    for i in range(TWO):
        for j in range(TWO):
            cos_t, sin_t = (jnp.hstack([t, t * sign]) for t, sign in ((cos_ref[i, j].T, 1), (sin_ref[i, j].T, -1)))
            dk = dkv_ref[pl.ds((i * TWO + j) * BLK, BLK)] * ATTN_SCALE
            dk_u[i, j] = (dk * cos_t + pltpu.roll(dk, HEAD_DIM // TWO, 1) * sin_t).astype(BF16)
    dv_u[...] = dkv_ref[pl.ds(n, n)].astype(BF16).reshape(dv_u.shape)


def wkv_terms(h_own, dk_u, dv_u, outs):
    d_out = jnp.hstack([r[...].reshape(-1, HEAD_DIM) for r in (dk_u, dv_u)])
    for out, half in outs:

        @pl.loop(0, FOUR)
        def _(zz, out=out, half=half):
            h = h_own[:, :, :, aligned(half * FOUR + zz)].reshape(-1, BLK)
            out[zz] = dot(h, d_out, (0,), (0,)).reshape(out.shape[1:])


def gather_kernel(*refs):
    take = taker(refs)
    wo_ref, wq_ref, dkv_ref, cos_ref, sin_ref, h_ref = take(6)
    grad_ins, outs, (dx_ref, dgain_ref) = take(6), take(FOUR), take(TWO)
    own_sem, send_sem, come_sem, core_sem, all_terms, g_s, g_r = take(7)
    terms, wkv_own, wkv_ref, h_own, dk_u, dv_u = take(6)
    buffers, sems, refs = take(FOUR), take(7), take(len(refs))
    me = lax.axis_index("cp")
    z, y, x, core = place(me)
    line = Line(me)
    to = {"x": dev(z, y, 1 - x, core), "y": dev(z, 1 - y, x, core), "u": line.next[1], "d": line.next[-1]}
    partner = dev(z, y, x, 1 - core)
    others = [(i, me ^ i) for i in range(1, all_terms.shape[0])]
    meet([d for _, d in others])
    load_h = pltpu.make_async_copy(h_ref, h_own, own_sem.at[0])
    load_h.start()
    wkv = PairSum(me, "core", 1, wkv_ref, wkv_own, buffers, [r.at[0] for r in sems])

    def windows(part, zz, yy, xx, cc):
        pair = TWO * zz + yy
        wide, narrow = wq_ref.shape[1], wkv_own.shape[1] // TWO
        wo_at, wq_at = ((xx * TWO + cc) * N_PAIRS + pair) * wo_ref.shape[0], (cc * N_PAIRS + pair) * wq_ref.shape[0]
        if part == 3:
            for i, out in enumerate(outs[TWO:]):
                cols = pl.ds(xx * narrow, narrow)
                yield wkv_own.at[:, head_slice(i)], out.at[pl.ds(wq_at, wkv_own.shape[0]), cols]
            return

        def cut(ref, cuts):
            first, last = (c * ref.shape[0] // 8 for c in cuts[part : part + TWO])
            return first, last - first

        at, rows = cut(wo_ref, WO_CUTS)
        yield wo_ref.at[pl.ds(at, rows)], outs[0].at[pl.ds(wo_at + at, rows)]
        at, rows = cut(wq_ref, WQ_CUTS)
        yield wq_ref.at[pl.ds(at, rows)], outs[1].at[pl.ds(wq_at + at, rows), pl.ds(xx * wide, wide)]

    def block(part, key, cc=core):
        dz, ry, rx = key
        return windows(part, z + dz, 1 - y if ry else y, 1 - x if rx else x, cc)

    def index(part, key):
        return (part, key[0] + 3) + key[1:]

    def send(part, key, link, there):
        arrive = (core_sem if link is None else come_sem).at[index(part, there)]
        for shard, window in block(part, key):
            src = window if any(key) else shard
            remote(src, window, send_sem.at[index(part, key) + (LINKS.find(link or "-") + 1,)], arrive, to.get(link, partner)).start()

    def whole(part, send, arrive):
        size = sum(shard.size for shard, _ in block(part, HERE)) // outs[0].shape[1]
        dst = outs[0].at[pl.ds(0, size)]
        return remote(dst, dst, send, arrive, me)

    def when(on, do):
        pl.when(on)(do)

    def each_way(part, key):
        held = line.held(key[0])
        yield None, key, held
        for link, there in onward(ORDERS[part], key):
            inside = {"u": line.inside[1], "d": line.inside[-1]}.get(link)
            yield link, there, held if inside is None else jnp.logical_and(held, inside)

    def pass_on(part, key):
        for link, there, on in each_way(part, key):
            when(on, functools.partial(send, part, key, link, there))

    def term_copy(i, d):
        return remote(terms, all_terms.at[i], g_s.at[i], g_r.at[i], d)

    owns = []

    def put_own(part):
        for shard, window in block(part, HERE):
            owns.append(pltpu.make_async_copy(shard, window, own_sem.at[len(owns)]))
            owns[-1].start()

    def tile(t):
        job.tile(t)
        if t == job.tiles - 1:
            for i, d in others:
                term_copy(i, d).start()

    def sum_step(h):
        wkv.step(0, h)
        if h == 3:
            put_own(3)

    steps = [(TILES_FROM + t * TILE_EVERY, functools.partial(tile, t)) for t in range(HiddenGradient.tiles)]
    steps += [(at, functools.partial(sum_step, h)) for h, at in enumerate(SUM_AT)]
    steps.sort(key=lambda s: s[0])
    events = arrivals()
    for part in range(3):
        pass_on(part, HERE)
    turn_back(dkv_ref, cos_ref, sin_ref, dk_u, dv_u)
    job = HiddenGradient(me, dk_u, dv_u, grad_ins, (dx_ref, terms), refs)
    load_h.wait()
    wkv_terms(h_own, dk_u, dv_u, ((wkv_ref, 1 - core), (buffers[0], core)))
    wkv.begin(0)
    for part in range(3):
        put_own(part)
    wkv.loaded(0)
    for now, part, key in events:
        while steps and steps[0][0] <= now:
            steps.pop(0)[1]()
        if any(key):
            arrive = come_sem.at[index(part, key)]
            when(line.held(key[0]), whole(part, own_sem.at[0], arrive).wait_recv)
            pass_on(part, key)
        elif part == 3:
            pass_on(part, key)
    for o in owns:
        o.wait()
    total_gain = terms[...]
    for i, d in others:
        term_copy(i, d).wait_recv()
        total_gain += all_terms[i]
    dgain_ref[...] = total_gain
    for i, d in others:
        term_copy(i, d).wait_send()
    for _, part, key in events:
        when(line.held(key[0]), whole(part, own_sem.at[0], core_sem.at[index(part, key)]).wait_recv)
        for link, there, on in each_way(part, key):
            sent = send_sem.at[index(part, key) + (LINKS.find(link or "-") + 1,)]
            when(on, whole(part, sent, own_sem.at[0]).wait_send)
    wkv.wait_send(0)
    job.finish()


def gather_all(wo, wq, dkv, cos_f, sin_f, h_u, part, w_k, w_v, x, dy, gain, shapes):
    dma = pltpu.SemaphoreType.DMA
    vmem, hbm = pl.BlockSpec(memory_space=pltpu.VMEM), pl.BlockSpec(memory_space=pl.ANY)
    block = w_k.shape[0] // TWO // N_PAIRS, w_k.shape[1]
    parts = len(ORDERS)
    keys = (parts, 7, TWO, TWO)
    terms = 1, x.shape[1]
    scratch = [dma((TWO * parts,)), dma(keys + (len(LINKS) + 1,)), dma(keys), dma(keys)]
    scratch += [pltpu.VMEM((32,) + terms, F32), dma((32,)), dma((32,)), pltpu.VMEM(terms, F32), pltpu.VMEM(block, F32)]
    scratch += [pltpu.VMEM((FOUR, TWO) + block, F32), pltpu.VMEM(h_u.shape, BF16)]
    scratch += [pltpu.VMEM((TWO, TWO, BLK, HEAD_DIM), BF16)] * TWO
    return pl.pallas_call(
        gather_kernel,
        name="gather_all",
        out_shape=[jax.ShapeDtypeStruct(s, F32) for s in shapes]
        + [jax.ShapeDtypeStruct(x.shape, BF16), jax.ShapeDtypeStruct(terms, F32)],
        in_specs=[vmem] * 5 + [hbm] + [vmem] * 6,
        out_specs=[hbm] * len(shapes) + [vmem] * TWO,
        scratch_shapes=scratch + PairSum.scratch("core", block) + PairSum.sems(1, 1) + HiddenGradient.scratch(x),
        compiler_params=params(56, collective_id=0),
        cost_estimate=cost(1, 76),
    )(wo, wq, dkv, cos_f, sin_f, h_u, part, w_k, w_v, x, dy, gain)


def perm(x, pairs):
    return lax.ppermute(x, "cp", pairs)


def flip_pairs(d):
    return [(r, r ^ d) for r in range(32)]


def solution(mesh):
    def local_step(hidden, grad_out, positions, seg_ids, w_q, w_k, w_v, w_o, norm_gain):
        n_batch, n_tok, d_model = hidden.shape
        n_rows = n_batch * n_tok
        wide = N_HEADS * HEAD_DIM
        me = lax.axis_index("cp")
        _, _, _, core = place(me)
        quad, pair = me % FOUR, me // FOUR
        relations = range(FOUR)

        def rows_of(arr, d):
            return pick(arr.reshape((TWO, TWO, TWO, CHUNK) + arr.shape[TWO:]), core ^ (d % TWO), 0)

        def swap(pieces):
            return [perm(p, flip_pairs(d)) if d else p for d, p in enumerate(pieces)]

        def unite(arr):
            joined = jnp.stack(swap([rows_of(arr, d) for d in relations]), axis=TWO)
            return joined.reshape((TWO, TWO, BLK) + joined.shape[FOUR:])

        gain = norm_gain.astype(F32)
        cos_t, sin_t = rope_tables(positions.reshape(n_rows))
        cos_f, sin_f = jnp.hstack([cos_t, cos_t]), jnp.hstack([-sin_t, sin_t])
        dy_flat = grad_out.reshape(n_rows, d_model)
        normed, kv_home = project(hidden.reshape(n_rows, d_model), gain[NEW], w_k, w_v, cos_f, sin_f)
        pos_u = unite(positions)
        kv_home = kv_home.reshape((TWO,) * 5 + (CHUNK, HEAD_DIM))
        kv_all, q_u, do_u = exchange(kv_home, normed, dy_flat, cos_f, sin_f, w_q, w_o)
        dy_quad = grad_out.reshape((TWO,) * 3 + (CHUNK, d_model))
        dy_pieces, q_u = lax.optimization_barrier(([rows_of(grad_out, d) for d in relations], q_u))
        dy_pieces = swap(dy_pieces)[1:]

        member = quad ^ jnp.arange(FOUR)
        front, back = ((m[:, NEW] * CHUNK + jnp.arange(CHUNK)[NEW]).reshape(BLK) for m in (member, 3 - member))
        offsets = jnp.stack([front, back]).astype(jnp.int32)
        own_super = jnp.stack([pair, N_SUPER - 1 - pair]).astype(jnp.int32)
        q_index = own_super[:, NEW] * BLK + offsets
        start = q_index[NEW] - pos_u
        tab = jnp.concatenate(
            [own_super, (jnp.min(start, axis=-1) // BLK).reshape(-1), jnp.max(start, axis=-1).reshape(-1)]
        )
        start_r = start[:, :, NEW, :]
        q_index_r = jnp.broadcast_to(q_index[NEW, :, NEW, :], start_r.shape)
        cos_u, sin_u = rope_tables(pos_u)
        cos_ut, sin_ut = jnp.swapaxes(cos_u, TWO, 3), jnp.swapaxes(sin_u, TWO, 3)

        koff = offsets[:, NEW]
        attn_u, lse = flash_fwd(tab, q_u, kv_all, start_r, q_index_r, koff)

        wo_keep, wo_away = wo_terms(attn_u, dy_quad, dy_pieces)
        wo_come = perm(wo_away, flip_pairs(FOUR))
        do_u, wo_keep = lax.optimization_barrier((do_u, wo_keep))
        dq_u, dkv = flash_bwd(tab, q_u, do_u, attn_u, kv_all, lse, start_r, q_index_r, koff, cos_ut, sin_ut)
        wo_sum = wo_keep + wo_come

        x_flat = hidden.reshape(n_rows, d_model)
        wo_own, dkv_own, wq_own, block_out, d_part, h_u = reduce_pairs(
            [wo_sum, dkv.reshape(FOUR, TWO, -1, HEAD_DIM)],
            [wo_sum.shape[1:], (dkv.size // N_PAIRS // HEAD_DIM, HEAD_DIM), (d_model // TWO // N_PAIRS, wide)],
            (TWO, 8, FOUR),
            ("z", "", "core"),
            TWO,
            Products,
            (attn_u, dq_u, x_flat, normed.reshape((TWO,) * 3 + (CHUNK, d_model)), w_o, w_q),
        )
        grad_wo, grad_wq, grad_wk, grad_wv, grad_x, d_gain = gather_all(
            wo_own,
            wq_own,
            dkv_own,
            cos_ut,
            sin_ut,
            h_u,
            d_part,
            w_k,
            w_v,
            x_flat,
            dy_flat,
            gain[NEW],
            [w_o.shape, w_q.shape, w_k.shape, w_v.shape],
        )
        block_out, grad_x = (a.reshape(hidden.shape) for a in (block_out, grad_x))
        return block_out, grad_x, grad_wq, grad_wk, grad_wv, grad_wo, d_gain.reshape(d_model)

    seq_spec = P(None, "cp", None)
    tok_spec = P(None, "cp")
    full_spec = P()
    return jax.shard_map(
        local_step,
        mesh=mesh,
        in_specs=(seq_spec, seq_spec, tok_spec, tok_spec, full_spec, full_spec, full_spec, full_spec, full_spec),
        out_specs=(seq_spec, seq_spec, full_spec, full_spec, full_spec, full_spec, full_spec),
        check_vma=False,
    )
```

```python
import functools
import heapq
import itertools

import jax
import jax.numpy as jnp
from jax import lax
from jax.experimental import pallas as pl
from jax.experimental.pallas import tpu as pltpu
from jax.sharding import PartitionSpec as P

HEAD_DIM = 128
NORM_EPS = 1e-5
ROPE_BASE = 500000.0
NEG_BIG = -1e30
LOG2E = 1.4426950408889634
ATTN_SCALE = HEAD_DIM**-0.5
EXP2_SCALE = ATTN_SCALE * LOG2E
CHUNK = 64
TWO = 2
FOUR = 4
NEW = jnp.newaxis
BLK = 4 * CHUNK
N_HEADS = 8
N_PAIRS = 8
N_SUPER = 2 * N_PAIRS
MESH = pl.DeviceIdType.MESH
ONE = pl.Squeezed()
GROUP = 4
MADE_AT = 5
PRODUCTS_AT = 7, 9
F32 = jnp.float32
BF16 = jnp.bfloat16

T_SQ, T_LO, T_MX = 0, 2, 6


def rope_tables(positions):
    inv_freq = ROPE_BASE ** (-jnp.arange(0, HEAD_DIM, TWO).astype(F32) / HEAD_DIM)
    angles = positions.astype(F32)[..., None] * inv_freq
    return jnp.cos(angles), jnp.sin(angles)


def dot(a, b, ca, cb):
    return lax.dot_general(a, b, ((ca, cb), ((), ())), preferred_element_type=F32)


def cost(gflop, mib):
    return pl.CostEstimate(flops=gflop * 10**9, bytes_accessed=mib << 20, transcendentals=0)


def params(mib, **more):
    return pltpu.CompilerParams(vmem_limit_bytes=mib << 20, **more)


def row_mean(x):
    return jnp.mean(x, axis=-1, keepdims=True)


def head(h):
    return pl.ds(h * HEAD_DIM, HEAD_DIM)


def head_slice(h):
    return slice(h * HEAD_DIM, (h + 1) * HEAD_DIM)


def dot_t(a, b):
    return dot(a, b, (1,), (1,))


def pick(x, index, axis):
    return lax.dynamic_index_in_dim(x, index, axis, keepdims=False)


def steps(tab, body):
    b, hf = pl.program_id(0), pl.program_id(1)
    own, first, last_start = tab[T_SQ + hf], tab[T_LO + TWO * b + hf], tab[T_MX + TWO * b + hf]

    def step(s, carry):
        late = s >= N_PAIRS
        at = jnp.where(late, N_SUPER - 1 - s, s), late.astype(jnp.int32)
        full = jnp.logical_and(s < own, s * BLK >= last_start)
        pl.when(full)(lambda: body(s, at, False))
        pl.when(jnp.logical_not(full))(lambda: body(s, at, True))
        return carry

    lax.fori_loop(first, own + 1, step, 0)


def down(row, n):
    return jnp.broadcast_to(row, (n, row.shape[-1])).T


def may_use(s, off, st_ref, qi_ref):
    return jnp.logical_and(off >= st_ref[...] - s * BLK, off <= qi_ref[...] - s * BLK)


def fwd_kernel(tab, q_ref, kv_ref, st_ref, qi_ref, ko_ref, o_ref, lse_ref, q_s, acc, m_s, l_s, k_t, bounds):
    m_s[...] = jnp.full_like(m_s, NEG_BIG)
    l_s[...] = jnp.zeros_like(l_s)
    acc[...] = jnp.zeros_like(acc)
    for i, ref in enumerate((st_ref, qi_ref)):
        bounds[i] = down(ref[...], HEAD_DIM)
    for h in range(N_HEADS):
        q_s[pl.ds(h * BLK, BLK)] = q_ref[:, head(h)]

    @pl.when(pl.program_id(1) == 0)
    def _():
        @pl.loop(0, N_PAIRS)
        def _(pair):
            for hk in range(TWO):
                k_t[pair, hk] = kv_ref[pair, 0, hk].T

    def body(s, at, masked):
        pair, hk = at
        v = kv_ref[pair, 1, hk]
        if masked:
            off = ko_ref[hk] + s * BLK
            mask = [
                jnp.logical_and(off[:, lanes] >= bounds[0], off[:, lanes] <= bounds[1])
                for lanes in (slice(HEAD_DIM), slice(HEAD_DIM, BLK))
            ]
            mask = [jnp.concatenate([m, m], axis=0) for m in mask]
        for g in range(N_HEADS // TWO):
            rows = pl.ds(g * TWO * BLK, TWO * BLK)
            sc = jnp.dot(q_s[rows], k_t[pair, hk], preferred_element_type=F32)
            sc = [sc[:, :HEAD_DIM], sc[:, HEAD_DIM:]]
            if masked:
                sc = [jnp.where(m, x, NEG_BIG) for m, x in zip(mask, sc)]
            m_old = m_s[rows]
            m_new = jnp.maximum(m_old, jnp.max(jnp.maximum(*sc), axis=1, keepdims=True))
            alpha = jnp.exp2((m_old - m_new) * EXP2_SCALE)
            p = [jnp.exp2((x - m_new) * EXP2_SCALE) for x in sc]
            m_s[rows] = m_new
            l_s[rows] = l_s[rows] * alpha + (p[0] + p[1])
            p = jnp.hstack([x.astype(BF16) for x in p])
            acc[rows] = acc[rows] * alpha + jnp.dot(p, v, preferred_element_type=F32)

    steps(tab, body)
    for h in range(N_HEADS):
        rows = pl.ds(h * BLK, BLK)
        total = jnp.sum(l_s[rows], axis=1, keepdims=True)
        o_ref[:, head(h)] = (acc[rows] / total).astype(BF16)
        lse_ref[h] = (m_s[rows] * EXP2_SCALE + jnp.log2(total)).T[:1]


def bwd_kernel(tab, q_ref, do_ref, o_ref, kv_ref, lse_ref, st_ref, qi_ref, ko_ref, cos_ref, sin_ref, dq_ref, dkv_ref, *scratch):
    dq_acc, delta, off_s, q_s, do_s, q_t, do_t, p_s, ds_s = scratch
    dq_acc[...] = jnp.zeros_like(dq_acc)
    for h in range(N_HEADS):
        q, do = q_ref[:, head(h)], do_ref[:, head(h)]
        delta[h] = jnp.sum((do.astype(F32) * o_ref[:, head(h)].astype(F32)).T, axis=0, keepdims=True)
        q_s[pl.ds(h * BLK, BLK)], do_s[pl.ds(h * BLK, BLK)] = q, do
        q_t[h], do_t[h] = q.T, do.T

    @pl.when(pl.program_id(1) == 0)
    def _():
        dkv_ref[...] = jnp.zeros_like(dkv_ref)
        for hk in range(TWO):
            off_s[hk] = down(ko_ref[hk], BLK)

    def body(s, at, masked):
        pair, hk = at
        k = kv_ref[pair, 0, hk]
        v = kv_ref[pair, 1, hk]
        k_t = k.T
        mask = may_use(s, off_s[hk], st_ref, qi_ref) if masked else None
        for first in range(0, N_HEADS, GROUP):
            rows = pl.ds(first * BLK, GROUP * BLK)
            for h in range(first, first + GROUP):
                cols = pl.ds(h * BLK, BLK)
                p = jnp.exp2(jnp.dot(k, q_t[h], preferred_element_type=F32) * EXP2_SCALE - lse_ref[h])
                if masked:
                    p = jnp.where(mask, p, 0.0)
                ds = p * (jnp.dot(v, do_t[h], preferred_element_type=F32) - delta[h])
                p_s[:, cols] = p.astype(BF16)
                ds_s[:, cols] = ds.astype(BF16)
            dkv_ref[pair, 0, hk] += jnp.dot(ds_s[:, rows], q_s[rows], preferred_element_type=F32)
            dkv_ref[pair, 1, hk] += jnp.dot(p_s[:, rows], do_s[rows], preferred_element_type=F32)
            dq_acc[:, rows] += jnp.dot(k_t, ds_s[:, rows], preferred_element_type=F32)

    steps(tab, body)
    cos_t, sin_t = cos_ref[...], sin_ref[...]
    half = HEAD_DIM // TWO
    for h in range(N_HEADS):
        cols = pl.ds(h * BLK, BLK)
        a, c = dq_acc[:half, cols] * ATTN_SCALE, dq_acc[half:, cols] * ATTN_SCALE
        lin = jnp.concatenate([a * cos_t + c * sin_t, c * cos_t - a * sin_t], axis=0)
        dq_ref[:, head(h)] = lin.T.astype(BF16)


def attn_specs():
    def at_tile(b, h, t):
        return (b, h) + (0,) * TWO

    def at_row(b, h, t):
        return (0, 0, b) + (0,) * 3

    tile = pl.BlockSpec((ONE, ONE, BLK, N_HEADS * HEAD_DIM), at_tile)
    row = pl.BlockSpec((ONE, ONE, 1, BLK), at_tile)
    stat = pl.BlockSpec((ONE, ONE, N_HEADS, 1, BLK), lambda b, h, t: (b, h) + (0,) * 3)
    rope = pl.BlockSpec((ONE, ONE, HEAD_DIM // TWO, BLK), at_tile)
    kv = pl.BlockSpec((N_PAIRS, TWO, ONE, TWO, BLK, HEAD_DIM), at_row)
    ko = pl.BlockSpec((TWO, 1, BLK), lambda b, h, t: (0,) * 3)
    return tile, row, stat, kv, ko, rope


def flash_fwd(tab, q, kv, start, qidx, koff):
    tile, row, stat, kvs, ko, _ = attn_specs()
    return pl.pallas_call(
        fwd_kernel,
        name="attn_fwd",
        out_shape=(jax.ShapeDtypeStruct(q.shape, BF16), jax.ShapeDtypeStruct((TWO, TWO, N_HEADS, 1, BLK), F32)),
        grid_spec=pltpu.PrefetchScalarGridSpec(
            num_scalar_prefetch=1,
            grid=(TWO, TWO),
            in_specs=[tile, kvs, row, row, ko],
            out_specs=[tile, stat],
            scratch_shapes=[pltpu.VMEM((N_HEADS * BLK, HEAD_DIM), t) for t in (BF16, F32, F32, F32)]
            + [pltpu.VMEM((N_PAIRS, TWO, HEAD_DIM, BLK), BF16), pltpu.VMEM((TWO, BLK, HEAD_DIM), jnp.int32)],
        ),
        compiler_params=params(63),
        cost_estimate=cost(20, 16),
    )(tab, q, kv, start, qidx, koff)


def flash_bwd(tab, q, do, o, kv, lse, start, qidx, koff, cos_t, sin_t):
    tile, row, stat, kvs, ko, rope = attn_specs()
    return pl.pallas_call(
        bwd_kernel,
        name="attn_bwd",
        out_shape=(
            jax.ShapeDtypeStruct(q.shape, BF16),
            jax.ShapeDtypeStruct(kv.shape, F32),
        ),
        grid_spec=pltpu.PrefetchScalarGridSpec(
            num_scalar_prefetch=1,
            grid=(TWO, TWO),
            in_specs=[tile, tile, tile, kvs, stat, row, row, ko, rope, rope],
            out_specs=[tile, kvs],
            scratch_shapes=[pltpu.VMEM((HEAD_DIM, N_HEADS * BLK), F32), pltpu.VMEM((N_HEADS, 1, BLK), F32)]
            + [pltpu.VMEM((TWO, BLK, BLK), jnp.int32)]
            + [pltpu.VMEM((N_HEADS * BLK, HEAD_DIM), BF16)] * TWO
            + [pltpu.VMEM((N_HEADS, HEAD_DIM, BLK), BF16)] * TWO
            + [pltpu.VMEM((BLK, N_HEADS * BLK), BF16)] * TWO,
        ),
        compiler_params=params(63),
        cost_estimate=cost(50, 32),
    )(tab, q, do, o, kv, lse, start, qidx, koff, cos_t, sin_t)


def turn(x, cos_ref, sin_ref):
    return x * cos_ref[...] + pltpu.roll(x, HEAD_DIM // TWO, 1) * sin_ref[...]


def first_kernel(x_ref, g_ref, wk_ref, wv_ref, cos_ref, sin_ref, h_ref, kv_ref):
    x = x_ref[...].astype(F32)
    h = (x * lax.rsqrt(row_mean(x * x) + NORM_EPS) * g_ref[...]).astype(BF16)
    h_ref[...] = h
    k = jnp.dot(h, wk_ref[...], preferred_element_type=F32)
    v = jnp.dot(h, wv_ref[...], preferred_element_type=F32)
    n = kv_ref.shape[3]
    for i in range(TWO):
        for j, val in enumerate((turn(k[:, head_slice(i)], cos_ref, sin_ref), v[:, head_slice(i)])):
            for c in range(TWO):
                kv_ref[i, c, j] = val[c * n : (c + 1) * n].astype(BF16)


def project(x, gain, w_k, w_v, cos_f, sin_f):
    n = x.shape[0] // TWO
    return pl.pallas_call(
        first_kernel,
        name="norm_kv",
        out_shape=(jax.ShapeDtypeStruct(x.shape, BF16), jax.ShapeDtypeStruct((TWO,) * 3 + (n, HEAD_DIM), BF16)),
        compiler_params=params(63),
        cost_estimate=cost(TWO, 7),
    )(x, gain, w_k, w_v, cos_f, sin_f)


def place(me):
    return me // 8, lax.rem(me // FOUR, TWO), lax.rem(me // TWO, TWO), lax.rem(me, TWO)


def dev(z, y, x, core):
    return ((z * TWO + y) * TWO + x) * TWO + core


def z_peers(z):
    return [(k, lax.rem(z + k, FOUR)) for k in (1, TWO, 3)]


def meet(peers):
    barrier = pltpu.get_barrier_semaphore()
    for d in peers:
        pl.semaphore_signal(barrier, device_id=(d,), device_id_type=MESH)
    pl.semaphore_wait(barrier, len(peers))


def remote(src, dst, send, arrive, to):
    return pltpu.make_async_remote_copy(
        src_ref=src, dst_ref=dst, send_sem=send, recv_sem=arrive, device_id=(to,), device_id_type=MESH
    )


class Line:
    order = (0, 1, -1, TWO, -TWO, 3, -3)

    def __init__(self, me):
        self.z, y, x, core = place(me)
        self.next = {1: dev(self.z + 1, y, x, core), -1: dev(self.z - 1, y, x, core)}
        self.inside = {1: self.z < 3, -1: self.z > 0}

    def held(self, dz):
        return jnp.logical_and(self.z + dz >= 0, self.z + dz <= 3)

    def ways(self, dz):
        for d in self.next:
            if d * dz <= 0:
                yield d, self.inside[d] if dz == 0 else jnp.logical_and(self.inside[d], self.held(dz))


def tiled(n, fetch, use, first=0):
    fetch(first, 0).start()

    @pl.loop(0, n)
    def _(t):
        slot = lax.rem(t, TWO)
        fetch(first + t, slot).wait()

        @pl.when(t + 1 < n)
        def _():
            fetch(first + t + 1, 1 - slot).start()

        use(first + t, slot)


def aligned(t, size=BLK):
    return pl.ds(pl.multiple_of(t * size, size), size)


def exchange_kernel(*refs):
    take = taker(refs)
    kv_ref, h_ref, dy_ref, cos_ref, sin_ref, wq_ref, wo_ref, kv_all, q_u, do_u, *dy_rows = take(12)
    own_sem, quad_s, quad_r, z_s, z_r, y_s, y_r, q_home, do_home, wq_buf, wo_buf, w_sem, dy_sem = take(len(refs))
    me = lax.axis_index("cp")
    z, y, x, core = place(me)
    quad, line = quad_of(me), Line(me)
    across = dev(z, 1 - y, x, core)
    meet(quad[1:] + [across] + [dev(zz, y, x, core) for _, zz in z_peers(z)])

    def source(a, d):
        xx, cc = 1 - x if d // TWO else x, 1 - core if d % TWO else core
        return (kv_ref, q_home, do_home)[a].at[xx, cc]

    def target(a, d):
        tok = pl.ds(d * CHUNK, CHUNK)
        return kv_all.at[me // FOUR, :, :, :, tok] if a == 0 else (q_u, do_u)[a - 1].at[:, :, tok]

    def quad_copy(a, d):
        return remote(source(a, d), target(a, d), quad_s.at[a, d], quad_r.at[a, d], quad[d])

    def own_copy(a):
        return pltpu.make_async_copy(source(a, 0), target(a, 0), own_sem.at[a])

    def z_copy(part, dz, d):
        block = kv_all.at[TWO * (z + dz) + y, part]
        return remote(block, block, z_s.at[part, (d + 1) // TWO, dz + 3], z_r.at[part, dz - d + 3], line.next[d])

    def y_copy(part, dz, yy=y):
        block = kv_all.at[TWO * (z + dz) + yy, part]
        return remote(block, block, y_s.at[part, dz + 3], y_r.at[part, dz + 3], across)

    parts = range(TWO)
    moves = [(part, dz) for dz in line.order for part in parts]

    def pass_on(count):
        for part, dz in [moves.pop(0) for _ in range(count)]:
            if dz:
                block = kv_all.at[TWO * (z + dz) + y, part]
                arrival = remote(block, block, own_sem.at[0], z_r.at[part, dz + 3], me)
                pl.when(line.held(dz))(arrival.wait_recv)
            for d, on in line.ways(dz):
                pl.when(on)(z_copy(part, dz, d).start)
            pl.when(line.held(dz))(y_copy(part, dz).start)

    n = h_ref.shape[1] // BLK // TWO

    def fetch_q(t, slot):
        return pltpu.make_async_copy(wq_ref.at[:, aligned(t)], wq_buf.at[slot], w_sem.at[0, slot])

    def fetch_o(t, slot):
        return pltpu.make_async_copy(wo_ref.at[aligned(t)], wo_buf.at[slot], w_sem.at[1, slot])

    def put(home, t, val):
        home[t // n, :, :, :, :, aligned(lax.rem(t, n))] = val.astype(BF16).reshape(home.shape[1:-1] + (BLK,))

    def query(t, slot):
        q = jnp.dot(h_ref[...], wq_buf[slot], preferred_element_type=F32)
        put(q_home, t, jnp.hstack([turn(q[:, head_slice(j)], cos_ref, sin_ref) for j in range(BLK // HEAD_DIM)]))

    def pull(t, slot):
        put(do_home, t, dot_t(dy_ref[...], wo_buf[slot]))

    all_moves = list(moves)
    half = dy_ref.shape[0] // TWO
    for i, out in enumerate(dy_rows):
        pltpu.make_async_copy(dy_ref.at[aligned(core if i == 0 else 1 - core, half)], out, dy_sem.at[i]).start()
    for d in (1, TWO, 3):
        quad_copy(0, d).start()
    own_copy(0).start()
    for a, (fetch, use) in enumerate(((fetch_q, query), (fetch_o, pull)), 1):
        for near in range(TWO):
            tiled(n, fetch, use, n * (x if near else 1 - x))
            for d in range(TWO):
                if d or not near:
                    quad_copy(a, d if near else d + TWO).start()
            if near:
                own_copy(a).start()
            if len(moves) == len(all_moves):
                own_copy(0).wait()
                for d in (1, TWO, 3):
                    quad_copy(0, d).wait_recv()
            pass_on(TWO)
    pass_on(len(moves))
    for part, dz in all_moves:
        for d, on in line.ways(dz):
            pl.when(on)(z_copy(part, dz, d).wait_send)
        pl.when(line.held(dz))(y_copy(part, dz, 1 - y).wait_recv)
        pl.when(line.held(dz))(y_copy(part, dz).wait_send)
    for a in range(3):
        for d in (1, TWO, 3):
            quad_copy(a, d).wait_send()
            if a > 0:
                quad_copy(a, d).wait_recv()
    own_copy(1).wait()
    own_copy(TWO).wait()
    for i, out in enumerate(dy_rows):
        pltpu.make_async_copy(dy_ref.at[aligned(core if i == 0 else 1 - core, half)], out, dy_sem.at[i]).wait()


def exchange(kv, h, dy, cos_f, sin_f, w_q, w_o):
    dma = pltpu.SemaphoreType.DMA
    vmem, hbm = pl.BlockSpec(memory_space=pltpu.VMEM), pl.BlockSpec(memory_space=pl.ANY)
    wide = w_q.shape[1] // TWO
    unit = jax.ShapeDtypeStruct((TWO, TWO, BLK, wide), BF16)
    dy_half = jax.ShapeDtypeStruct((dy.shape[0] // TWO, dy.shape[1]), BF16)
    home = pltpu.VMEM((TWO,) * FOUR + (CHUNK, wide), BF16)
    sems = [dma((3,))] + [dma((3, FOUR))] * TWO + [dma((TWO, TWO, 7))] + [dma((TWO, 7))] * 3
    bufs = [pltpu.VMEM((TWO,) + b, BF16) for b in ((w_q.shape[0], BLK), (BLK, w_o.shape[1]))]
    return pl.pallas_call(
        exchange_kernel,
        name="exchange",
        out_shape=(jax.ShapeDtypeStruct((N_PAIRS,) + (TWO,) * 3 + (BLK, HEAD_DIM), BF16), unit, unit, dy_half, dy_half),
        in_specs=[vmem] * 5 + [hbm] * TWO,
        out_specs=[hbm] * 5,
        scratch_shapes=sems + [home, home] + bufs + [dma((TWO, TWO)), dma((TWO,))],
        compiler_params=params(63, collective_id=1),
        cost_estimate=cost(1, 20),
    )(kv, h, dy, cos_f, sin_f, w_q, w_o)


def taker(refs):
    rest = iter(refs)
    return lambda count: list(itertools.islice(rest, count))


def wo_kernel(*refs):
    take = taker(refs)
    o_ref, *pieces = take(5)
    keep, away, dy_u, o_t, terms, came, load_sem, core_s, core_r = take(len(refs))
    me = lax.axis_index("cp")
    _, y, _, core = place(me)
    meet(quad_of(me)[1:TWO])
    loads = [
        pltpu.make_async_copy(src, dy_u.at[:, :, pl.ds(d * CHUNK, CHUNK)], load_sem.at[d])
        for d, src in enumerate(pieces)
    ]
    for c in loads:
        c.start()
    for h in range(N_HEADS):
        o_t[head(h)] = o_ref[:, :, :, head(h)].reshape(-1, HEAD_DIM).T
    for c in loads:
        c.wait()
    half, tiles = terms.shape[1], terms.shape[TWO] // BLK

    def swap(t):
        return remote(terms.at[0, :, aligned(t)], came.at[:, aligned(t)], core_s.at[t], core_r.at[t], quad_of(me)[1])

    def half_terms(i, to, then):
        @pl.loop(0, tiles)
        def _(t):
            dy = dy_u[:, :, :, aligned(t)].reshape(-1, BLK)
            terms[to, :, aligned(t)] = jnp.dot(o_t[aligned(i, half)], dy, preferred_element_type=F32)
            then(t)

    half_terms(1 - core, 0, lambda t: swap(t).start())
    half_terms(core, 1, lambda t: swap(t).wait_recv())
    rows = keep.shape[1]
    for zz in range(FOUR):
        for out, yy in ((keep, y), (away, 1 - y)):
            at = aligned(TWO * zz + yy, rows)
            out[zz] = terms[1, at] + came[at]
    for t in range(tiles):
        swap(t).wait_send()


def wo_terms(o, pieces):
    dma = pltpu.SemaphoreType.DMA
    vmem, hbm = pl.BlockSpec(memory_space=pltpu.VMEM), pl.BlockSpec(memory_space=pl.ANY)
    n, d, wide = o.shape[0] * o.shape[1] * o.shape[TWO], pieces[0].shape[-1], o.shape[-1]
    half = wide // TWO
    return pl.pallas_call(
        wo_kernel,
        name="wo_terms",
        out_shape=[jax.ShapeDtypeStruct((FOUR, half // N_PAIRS, d), F32)] * TWO,
        in_specs=[vmem] + [hbm] * FOUR,
        out_specs=[vmem] * TWO,
        scratch_shapes=[pltpu.VMEM((TWO, TWO, BLK, d), BF16), pltpu.VMEM((wide, n), BF16)]
        + [pltpu.VMEM((TWO, half, d), F32), pltpu.VMEM((half, d), F32), dma((FOUR,)), dma((d // BLK,)), dma((d // BLK,))],
        compiler_params=params(63, collective_id=3),
        cost_estimate=cost(FOUR, 20),
    )(o, *pieces)


class PairSum:
    def __init__(self, me, kind, cut, src, out, buffers, sems):
        self.me, self.kind, self.src, self.out = me, kind, src, out
        self.size = out.shape[0] // cut
        self.own, self.from_core, self.from_y, self.from_z = buffers
        self.load_sem, self.core_s, self.core_r, self.y_s, self.y_r, self.z_s, self.z_r = sems
        self.z, self.y, x, core = place(me)
        self.partner = dev(self.z, self.y, x, 1 - core)
        self.across = dev(self.z, 1 - self.y, x, core)
        self.next_z = dev(self.z + 1, self.y, x, core), dev(self.z - 1, self.y, x, core)

    def rows(self, j):
        return pl.ds(j * self.size, self.size)

    def mine(self, j, zz):
        at = self.rows(j)
        return self.own.at[zz, self.y, at] if self.kind == "core" else self.own.at[zz, at]

    def load(self, j):
        at = self.rows(j)
        src = self.src.at[:, at] if self.kind else self.src.at[:, self.y, at]
        return pltpu.make_async_copy(src, self.own.at[:, at], self.load_sem.at[j])

    def core_copy(self, j):
        src, dst = (r.at[:, :, self.rows(j)] for r in (self.src, self.from_core))
        return remote(src, dst, self.core_s.at[j], self.core_r.at[j], self.partner)

    def y_copy(self, j):
        src = self.own if self.kind == "core" else self.src
        at = self.rows(j)
        return remote(src.at[:, 1 - self.y, at], self.from_y.at[:, at], self.y_s.at[j], self.y_r.at[j], self.across)

    def z_copy(self, j, way, zz, to):
        at = way, zz + way - 1
        return remote(self.mine(j, zz), self.from_z.at[*at, self.rows(j)], self.z_s.at[j, *at], self.z_r.at[j, *at], to)

    def begin(self, j):
        if self.kind == "core":
            self.core_copy(j).start()
            return
        self.load(j).start()
        if not self.kind:
            self.y_copy(j).start()

    def loaded(self, j):
        if self.kind != "core":
            self.load(j).wait()
        else:
            self.core_copy(j).wait_recv()
            at = self.rows(j)
            for zz in range(FOUR):
                self.own[zz, :, at] += self.from_core[zz, :, at]
            self.y_copy(j).start()
        if self.kind == "z":
            self.hop(j, 0)

    def relay(self, j, way, zz, add):
        if add:
            self.z_copy(j, way, zz, self.me).wait_recv()
            self.mine(j, zz)[...] += self.from_z[way, zz + way - 1, self.rows(j)]
        self.z_copy(j, way, zz, self.next_z[way]).start()

    def hop(self, j, h):
        @pl.when(self.z == h)
        def _():
            for zz in range(3, h, -1):
                self.relay(j, 0, zz, h > 0)

        @pl.when(self.z == 3 - h)
        def _():
            for zz in range(3 - h):
                self.relay(j, 1, zz, h > 0)

    def step(self, j, h):
        if h == 0 and self.kind != "z":
            self.y_copy(j).wait_recv()
            for zz in range(FOUR):
                self.mine(j, zz)[...] += self.from_y[zz, self.rows(j)]
            self.hop(j, 0)
        elif 0 < h < 3:
            self.hop(j, h)
        elif h == 3:
            at = self.rows(j)
            self.out[at] = self.mine(j, self.z)[...]
            for way, on in enumerate((self.z > 0, self.z < 3)):

                @pl.when(on)
                def _(way=way):
                    self.z_copy(j, way, self.z, self.me).wait_recv()
                    self.out[at] += self.from_z[way, self.z + way - 1, at]

    def wait_send(self, j):
        if self.kind == "core":
            self.core_copy(j).wait_send()
        if self.kind != "z":
            self.y_copy(j).wait_send()
        for zz in range(FOUR):
            if zz > 0:
                pl.when(self.z < zz)(self.z_copy(j, 0, zz, self.next_z[0]).wait_send)
            if zz < 3:
                pl.when(self.z > zz)(self.z_copy(j, 1, zz, self.next_z[1]).wait_send)

    @staticmethod
    def scratch(kind, block):
        unused = pltpu.VMEM((8, HEAD_DIM), F32)
        own = pltpu.VMEM(((FOUR, TWO) if kind == "core" else (FOUR,)) + block, F32)
        from_y = unused if kind == "z" else pltpu.VMEM((FOUR,) + block, F32)
        return [own, own if kind == "core" else unused, from_y, pltpu.VMEM((TWO, 3) + block, F32)]

    @staticmethod
    def sems(*dims):
        dma = pltpu.SemaphoreType.DMA
        return [dma(dims)] * 5 + [dma(dims + (TWO, 3))] * TWO


def reduce_kernel(cuts, kinds, work, *refs):
    n = len(cuts)

    take = taker(refs)
    ins, more_in, outs, more_out, made = take(n - 1), take(work.ins), take(n), take(work.outs), take(1)
    buffers, sems = [take(FOUR) for _ in kinds], take(7)
    me = lax.axis_index("cp")
    z, y, x, core = place(me)
    meet(quad_of(me)[1:] + [dev(z, 1 - y, x, core)] + [dev(zz, y, x, core) for _, zz in z_peers(z)])
    job = work(me, more_in, more_out, take(len(refs)))
    sums = [PairSum(me, *a, [r.at[i] for r in sems]) for i, a in enumerate(zip(kinds, cuts, ins + made, outs, buffers))]
    pieces = [(s, j) for s, cut in zip(sums, cuts) for j in range(cut)]
    early, late = pieces[: -cuts[-1]], pieces[-cuts[-1] :]
    for s, j in early:
        s.begin(j)
    for s, j in early:
        s.loaded(j)
    for t in range(len(pieces) + 3):
        if t == MADE_AT:
            job.wq_terms(sums[-1].own, made[0])
            for s, j in late:
                s.begin(j)
        if t == MADE_AT + 1:
            for s, j in late:
                s.loaded(j)
        for h in range(FOUR):
            if 0 <= t - h < len(pieces):
                s, j = pieces[t - h]
                s.step(j, h)
        job.step(t)
    for s, j in pieces:
        s.wait_send(j)
    job.finish()


def quad_of(me):
    z, y, x, core = place(me)
    return [dev(z, y, 1 - x if d // TWO else x, 1 - core if d % TWO else core) for d in range(FOUR)]


class Home:
    def __init__(self, me, src, out, own_sem, send, arrive):
        _, _, x, core = place(me)
        w = src.shape[-1]
        to = out.at[core, :, :, :, pl.ds(x * w, w)]

        def piece(d):
            return src.at[:, :, pl.ds(d * CHUNK, CHUNK)]

        self.own = pltpu.make_async_copy(piece(0), to, own_sem)
        self.copies = [remote(piece(d), to, send.at[d], arrive.at[d], quad_of(me)[d]) for d in (1, TWO, 3)]

    def start(self):
        self.own.start()
        for c in self.copies:
            c.start()

    def wait_recv(self):
        self.own.wait()
        for c in self.copies:
            c.wait_recv()

    def wait_send(self):
        for c in self.copies:
            c.wait_send()


class Products:
    ins, outs = 6, 3

    def __init__(self, me, ins, outs, scratch):
        attn, self.dq, hidden, normed, self.w_o, self.w_q = ins
        self.block_out, self.d_part, self.h_u = outs
        self.attn_home, self.dq_home, self.buf_o, self.buf_q, self.h_own, *sems = scratch
        self.w_sem, self.load_sem, own_sem, quad_s, quad_r = sems
        _, _, _, core = place(me)

        def piece(d):
            return normed.at[1 - core if d % TWO else core]

        def tokens(d):
            return self.h_u.at[:, :, pl.ds(d * CHUNK, CHUNK)]

        self.h_copies = [remote(piece(d), tokens(d), quad_s.at[TWO, d], quad_r.at[TWO, d], quad_of(me)[d]) for d in (1, TWO, 3)]
        self.h_mine = pltpu.make_async_copy(piece(0), self.h_own.at[:, :, pl.ds(0, CHUNK)], own_sem.at[TWO])
        self.h_rest = pltpu.make_async_copy(
            self.h_u.at[:, :, pl.ds(CHUNK, BLK - CHUNK)], self.h_own.at[:, :, pl.ds(CHUNK, BLK - CHUNK)], self.load_sem
        )
        self.h_back = pltpu.make_async_copy(self.h_own.at[:, :, pl.ds(0, CHUNK)], tokens(0), self.load_sem)
        self.residual = pltpu.make_async_copy(hidden, self.block_out, own_sem.at[3])
        self.residual.start()
        for c in self.h_copies:
            c.start()
        self.h_mine.start()
        self.homes = [
            Home(me, src, out, own_sem.at[i], quad_s.at[i], quad_r.at[i])
            for i, (src, out) in enumerate([(attn, self.attn_home), (self.dq, self.dq_home)])
        ]
        for h in self.homes:
            h.start()

    @staticmethod
    def scratch(arrays):
        dma, d = pltpu.SemaphoreType.DMA, arrays[-1].shape[0]
        home = pltpu.VMEM((TWO,) * 3 + (CHUNK, d), BF16)
        buf = [pltpu.VMEM((TWO,) + b, BF16) for b in ((d, BLK), (BLK, d))]
        unit = pltpu.VMEM((TWO, TWO, BLK, d), BF16)
        return [home] * TWO + buf + [unit, dma((TWO, TWO)), dma(()), dma((FOUR,)), dma((3, FOUR)), dma((3, FOUR))]

    @staticmethod
    def results(arrays):
        unit = TWO, TWO, BLK, arrays[-1].shape[0]
        return [jax.ShapeDtypeStruct(arrays[TWO].shape, t) for t in (BF16, F32)] + [jax.ShapeDtypeStruct(unit, BF16)]

    spaces, out_spaces = [pl.ANY, pltpu.VMEM] + [pl.ANY] * FOUR, [pltpu.VMEM] * TWO + [pl.ANY]

    def step(self, t):
        def fetch_o(t, slot):
            return pltpu.make_async_copy(self.w_o.at[:, aligned(t)], self.buf_o.at[slot], self.w_sem.at[0, slot])

        def fetch_q(t, slot):
            return pltpu.make_async_copy(self.w_q.at[aligned(t)], self.buf_q.at[slot], self.w_sem.at[1, slot])

        def project(t, slot):
            at = aligned(t)
            attn = self.attn_home[...].reshape(-1, self.w_o.shape[0])
            out = jnp.dot(attn, self.buf_o[slot], preferred_element_type=F32)
            self.block_out[:, at] = (self.block_out[:, at].astype(F32) + out).astype(BF16)

        def pull(t, slot):
            dq = self.dq_home[...].reshape(-1, self.w_o.shape[0])
            self.d_part[:, aligned(t)] = dot_t(dq, self.buf_q[slot])

        if t in PRODUCTS_AT:
            i = PRODUCTS_AT.index(t)
            self.homes[i].wait_recv()
            if i == 0:
                self.residual.wait()
            tiled(self.w_o.shape[0] // BLK, *((fetch_o, project), (fetch_q, pull))[i])

    def wq_terms(self, own, other):
        self.h_mine.wait()
        self.h_back.start()
        for c in self.h_copies:
            c.wait_recv()
        self.h_back.wait()
        self.h_rest.start()
        self.h_rest.wait()
        core = lax.rem(lax.axis_index("cp"), TWO)
        d_out = self.dq[...].reshape(-1, self.dq.shape[-1])
        for out, half in ((other, 1 - core), (own, core)):

            @pl.loop(0, FOUR)
            def _(zz, out=out, half=half):
                h = self.h_own[:, :, :, aligned(half * FOUR + zz)].reshape(-1, BLK)
                out[zz] = dot(h, d_out, (0,), (0,)).reshape(out.shape[1:])

    def finish(self):
        for c in self.h_copies + self.homes:
            c.wait_send()


class HiddenGradient:
    tiles = FOUR

    def __init__(self, me, dk, dv, ins, outs, scratch):
        self.part, self.w_k, self.w_v, self.x, self.dy, self.gain = ins
        self.dx, self.terms = outs
        self.dk_home, self.dv_home, self.rows, *sems = scratch
        pairs = (dk, self.dk_home), (dv, self.dv_home)
        self.homes = [Home(me, src, out, *[r.at[i] for r in sems]) for i, (src, out) in enumerate(pairs)]
        for h in self.homes:
            h.start()

    @staticmethod
    def scratch(x):
        dma = pltpu.SemaphoreType.DMA
        home = pltpu.VMEM((TWO,) * 3 + (CHUNK, TWO * HEAD_DIM), BF16)
        return [home, home, pltpu.VMEM((8, x.shape[1]), F32), dma((TWO,)), dma((TWO, FOUR)), dma((TWO, FOUR))]

    def tile(self, t):
        if t == 0:
            for h in self.homes:
                h.wait_recv()
            self.rows[...] = jnp.zeros_like(self.rows)
        size = TWO * CHUNK
        at = pl.ds(t * size, size)
        d = self.part[at]
        for home, w in ((self.dk_home, self.w_k), (self.dv_home, self.w_v)):
            d += dot_t(home[t // TWO, t % TWO].reshape(size, -1), w[...])
        d = d.astype(BF16).astype(F32)
        x = self.x[at].astype(F32)
        inv_rms = lax.rsqrt(row_mean(x * x) + NORM_EPS)
        unit, scaled = x * inv_rms, d * self.gain[...]
        dx = inv_rms * (scaled - unit * row_mean(scaled * unit))
        self.dx[at] = (self.dy[at].astype(F32) + dx).astype(BF16)
        self.rows[...] += jnp.sum((d * unit).reshape((-1,) + self.rows.shape), axis=0)
        if t == self.tiles - 1:
            self.terms[...] = jnp.sum(self.rows[...], axis=0, keepdims=True)

    def finish(self):
        for h in self.homes:
            h.wait_send()


def reduce_pairs(arrays, blocks, cuts, kinds, collective_id, work, more):
    vmem, hbm = pl.BlockSpec(memory_space=pltpu.VMEM), pl.BlockSpec(memory_space=pl.ANY)
    n = len(blocks)
    scratch = [pltpu.VMEM((FOUR, TWO) + blocks[-1], F32)]
    scratch += sum((PairSum.scratch(k, b) for k, b in zip(kinds, blocks)), []) + PairSum.sems(n, max(cuts))
    outs = [jax.ShapeDtypeStruct(b, F32) for b in blocks] + work.results(more)
    return pl.pallas_call(
        functools.partial(reduce_kernel, cuts, kinds, work),
        name="reduce_pairs",
        out_shape=outs,
        in_specs=[hbm] * len(arrays) + [pl.BlockSpec(memory_space=m) for m in work.spaces],
        out_specs=[vmem] * n + [pl.BlockSpec(memory_space=m) for m in work.out_spaces],
        scratch_shapes=scratch + work.scratch(more),
        compiler_params=params(63, collective_id=collective_id),
        cost_estimate=cost(1, 20),
    )(*arrays, *more)


HERE = 0, 0, 0
LINKS = "xyud"
ORDERS = "zxy", "zyx", "yxz", "zyx"
WO_CUTS, WQ_CUTS = (0, 2, 6, 8), (0, 3, 6, 8)
SIZES = 7.0, 9.8, 5.6, 2.8
LATENCY, TILES_FROM, TILE_EVERY = 3.0, 14.0, 8.0
SUM_AT = 25.0, 31.0, 37.0, 43.0


def onward(order, key):
    dz, ry, rx = key
    stage = max((order.index(a) for a, r in zip("zyx", key) if r), default=-1)
    for axis in order[stage + 1 :]:
        if axis == "x":
            yield "x", (dz, ry, 1)
        elif axis == "y":
            yield "y", (dz, 1, rx)
        else:
            yield "u", (-1, ry, rx)
            yield "d", (1, ry, rx)
    if stage >= 0 and order[stage] == "z" and abs(dz) < 3:
        yield ("u", (dz - 1, ry, rx)) if dz < 0 else ("d", (dz + 1, ry, rx))


def arrivals():
    busy, times = {}, {}
    starts = [0.0] * 3 + [SUM_AT[-1] + LATENCY]
    here = [(t, z, part, HERE) for part, t in enumerate(starts) for z in range(FOUR)]
    while here:
        now, z, part, key = heapq.heappop(here)
        times.setdefault((part, key), []).append(now)
        for link, there in onward(ORDERS[part], key):
            to = z + {"u": 1, "d": -1}.get(link, 0)
            if 0 <= to <= 3:
                busy[z, link] = max(busy.get((z, link), 0), now) + SIZES[part]
                heapq.heappush(here, (busy[z, link] + LATENCY, to, part, there))
    return sorted((sum(t) / len(t), *at) for at, t in times.items())


def turn_back(dkv_ref, cos_ref, sin_ref, dk_u, dv_u):
    n = TWO * TWO * BLK
    for i in range(TWO):
        for j in range(TWO):
            cos_t, sin_t = (jnp.hstack([t, t * sign]) for t, sign in ((cos_ref[i, j].T, 1), (sin_ref[i, j].T, -1)))
            dk = dkv_ref[pl.ds((i * TWO + j) * BLK, BLK)] * ATTN_SCALE
            dk_u[i, j] = (dk * cos_t + pltpu.roll(dk, HEAD_DIM // TWO, 1) * sin_t).astype(BF16)
    dv_u[...] = dkv_ref[pl.ds(n, n)].astype(BF16).reshape(dv_u.shape)


def wkv_terms(h_own, dk_u, dv_u, outs):
    d_out = jnp.hstack([r[...].reshape(-1, HEAD_DIM) for r in (dk_u, dv_u)])
    for out, half in outs:

        @pl.loop(0, FOUR)
        def _(zz, out=out, half=half):
            h = h_own[:, :, :, aligned(half * FOUR + zz)].reshape(-1, BLK)
            out[zz] = dot(h, d_out, (0,), (0,)).reshape(out.shape[1:])


def gather_kernel(*refs):
    take = taker(refs)
    wo_ref, wq_ref, dkv_ref, cos_ref, sin_ref, h_ref = take(6)
    grad_ins, outs, (dx_ref, dgain_ref) = take(6), take(FOUR), take(TWO)
    own_sem, send_sem, come_sem, core_sem, all_terms, g_s, g_r = take(7)
    terms, wkv_own, wkv_ref, h_own, dk_u, dv_u = take(6)
    buffers, sems, refs = take(FOUR), take(7), take(len(refs))
    me = lax.axis_index("cp")
    z, y, x, core = place(me)
    line = Line(me)
    to = {"x": dev(z, y, 1 - x, core), "y": dev(z, 1 - y, x, core), "u": line.next[1], "d": line.next[-1]}
    partner = dev(z, y, x, 1 - core)
    others = [(i, me ^ i) for i in range(1, all_terms.shape[0])]
    meet([d for _, d in others])
    load_h = pltpu.make_async_copy(h_ref, h_own, own_sem.at[0])
    load_h.start()
    wkv = PairSum(me, "core", 1, wkv_ref, wkv_own, buffers, [r.at[0] for r in sems])

    def windows(part, zz, yy, xx, cc):
        pair = TWO * zz + yy
        wide, narrow = wq_ref.shape[1], wkv_own.shape[1] // TWO
        wo_at, wq_at = ((xx * TWO + cc) * N_PAIRS + pair) * wo_ref.shape[0], (cc * N_PAIRS + pair) * wq_ref.shape[0]
        if part == 3:
            for i, out in enumerate(outs[TWO:]):
                cols = pl.ds(xx * narrow, narrow)
                yield wkv_own.at[:, head_slice(i)], out.at[pl.ds(wq_at, wkv_own.shape[0]), cols]
            return

        def cut(ref, cuts):
            first, last = (c * ref.shape[0] // 8 for c in cuts[part : part + TWO])
            return first, last - first

        at, rows = cut(wo_ref, WO_CUTS)
        yield wo_ref.at[pl.ds(at, rows)], outs[0].at[pl.ds(wo_at + at, rows)]
        at, rows = cut(wq_ref, WQ_CUTS)
        yield wq_ref.at[pl.ds(at, rows)], outs[1].at[pl.ds(wq_at + at, rows), pl.ds(xx * wide, wide)]

    def block(part, key, cc=core):
        dz, ry, rx = key
        return windows(part, z + dz, 1 - y if ry else y, 1 - x if rx else x, cc)

    def index(part, key):
        return (part, key[0] + 3) + key[1:]

    def send(part, key, link, there):
        arrive = (core_sem if link is None else come_sem).at[index(part, there)]
        for shard, window in block(part, key):
            src = window if any(key) else shard
            remote(src, window, send_sem.at[index(part, key) + (LINKS.find(link or "-") + 1,)], arrive, to.get(link, partner)).start()

    def whole(part, send, arrive):
        size = sum(shard.size for shard, _ in block(part, HERE)) // outs[0].shape[1]
        dst = outs[0].at[pl.ds(0, size)]
        return remote(dst, dst, send, arrive, me)

    def when(on, do):
        pl.when(on)(do)

    def each_way(part, key):
        held = line.held(key[0])
        yield None, key, held
        for link, there in onward(ORDERS[part], key):
            inside = {"u": line.inside[1], "d": line.inside[-1]}.get(link)
            yield link, there, held if inside is None else jnp.logical_and(held, inside)

    def pass_on(part, key):
        for link, there, on in each_way(part, key):
            when(on, functools.partial(send, part, key, link, there))

    def term_copy(i, d):
        return remote(terms, all_terms.at[i], g_s.at[i], g_r.at[i], d)

    owns = []

    def put_own(part):
        for shard, window in block(part, HERE):
            owns.append(pltpu.make_async_copy(shard, window, own_sem.at[len(owns)]))
            owns[-1].start()

    def tile(t):
        job.tile(t)
        if t == job.tiles - 1:
            for i, d in others:
                term_copy(i, d).start()

    def sum_step(h):
        wkv.step(0, h)
        if h == 3:
            put_own(3)

    steps = [(TILES_FROM + t * TILE_EVERY, functools.partial(tile, t)) for t in range(HiddenGradient.tiles)]
    steps += [(at, functools.partial(sum_step, h)) for h, at in enumerate(SUM_AT)]
    steps.sort(key=lambda s: s[0])
    events = arrivals()
    for part in range(3):
        pass_on(part, HERE)
    turn_back(dkv_ref, cos_ref, sin_ref, dk_u, dv_u)
    job = HiddenGradient(me, dk_u, dv_u, grad_ins, (dx_ref, terms), refs)
    load_h.wait()
    wkv_terms(h_own, dk_u, dv_u, ((wkv_ref, 1 - core), (buffers[0], core)))
    wkv.begin(0)
    for part in range(3):
        put_own(part)
    wkv.loaded(0)
    for now, part, key in events:
        while steps and steps[0][0] <= now:
            steps.pop(0)[1]()
        if any(key):
            arrive = come_sem.at[index(part, key)]
            when(line.held(key[0]), whole(part, own_sem.at[0], arrive).wait_recv)
            pass_on(part, key)
        elif part == 3:
            pass_on(part, key)
    for o in owns:
        o.wait()
    total_gain = terms[...]
    for i, d in others:
        term_copy(i, d).wait_recv()
        total_gain += all_terms[i]
    dgain_ref[...] = total_gain
    for i, d in others:
        term_copy(i, d).wait_send()
    for _, part, key in events:
        when(line.held(key[0]), whole(part, own_sem.at[0], core_sem.at[index(part, key)]).wait_recv)
        for link, there, on in each_way(part, key):
            sent = send_sem.at[index(part, key) + (LINKS.find(link or "-") + 1,)]
            when(on, whole(part, sent, own_sem.at[0]).wait_send)
    wkv.wait_send(0)
    job.finish()


def gather_all(wo, wq, dkv, cos_f, sin_f, h_u, part, w_k, w_v, x, dy, gain, shapes):
    dma = pltpu.SemaphoreType.DMA
    vmem, hbm = pl.BlockSpec(memory_space=pltpu.VMEM), pl.BlockSpec(memory_space=pl.ANY)
    block = w_k.shape[0] // TWO // N_PAIRS, w_k.shape[1]
    parts = len(ORDERS)
    keys = (parts, 7, TWO, TWO)
    terms = 1, x.shape[1]
    scratch = [dma((TWO * parts,)), dma(keys + (len(LINKS) + 1,)), dma(keys), dma(keys)]
    scratch += [pltpu.VMEM((32,) + terms, F32), dma((32,)), dma((32,)), pltpu.VMEM(terms, F32), pltpu.VMEM(block, F32)]
    scratch += [pltpu.VMEM((FOUR, TWO) + block, F32), pltpu.VMEM(h_u.shape, BF16)]
    scratch += [pltpu.VMEM((TWO, TWO, BLK, HEAD_DIM), BF16)] * TWO
    return pl.pallas_call(
        gather_kernel,
        name="gather_all",
        out_shape=[jax.ShapeDtypeStruct(s, F32) for s in shapes]
        + [jax.ShapeDtypeStruct(x.shape, BF16), jax.ShapeDtypeStruct(terms, F32)],
        in_specs=[vmem] * 5 + [hbm] + [vmem] * 6,
        out_specs=[hbm] * len(shapes) + [vmem] * TWO,
        scratch_shapes=scratch + PairSum.scratch("core", block) + PairSum.sems(1, 1) + HiddenGradient.scratch(x),
        compiler_params=params(56, collective_id=0),
        cost_estimate=cost(1, 76),
    )(wo, wq, dkv, cos_f, sin_f, h_u, part, w_k, w_v, x, dy, gain)


def perm(x, pairs):
    return lax.ppermute(x, "cp", pairs)


def flip_pairs(d):
    return [(r, r ^ d) for r in range(32)]


def solution(mesh):
    def local_step(hidden, grad_out, positions, seg_ids, w_q, w_k, w_v, w_o, norm_gain):
        n_batch, n_tok, d_model = hidden.shape
        n_rows = n_batch * n_tok
        wide = N_HEADS * HEAD_DIM
        me = lax.axis_index("cp")
        _, _, _, core = place(me)
        quad, pair = me % FOUR, me // FOUR
        relations = range(FOUR)

        def rows_of(arr, d):
            return pick(arr.reshape((TWO, TWO, TWO, CHUNK) + arr.shape[TWO:]), core ^ (d % TWO), 0)

        def swap(pieces):
            return [perm(p, flip_pairs(d)) if d else p for d, p in enumerate(pieces)]

        def unite(arr):
            joined = jnp.stack(swap([rows_of(arr, d) for d in relations]), axis=TWO)
            return joined.reshape((TWO, TWO, BLK) + joined.shape[FOUR:])

        gain = norm_gain.astype(F32)
        cos_t, sin_t = rope_tables(positions.reshape(n_rows))
        cos_f, sin_f = jnp.hstack([cos_t, cos_t]), jnp.hstack([-sin_t, sin_t])
        dy_flat = grad_out.reshape(n_rows, d_model)
        normed, kv_home = project(hidden.reshape(n_rows, d_model), gain[NEW], w_k, w_v, cos_f, sin_f)
        pos_u = unite(positions)
        kv_home = kv_home.reshape((TWO,) * 5 + (CHUNK, HEAD_DIM))
        kv_all, q_u, do_u, *dy_rows = exchange(kv_home, normed, dy_flat, cos_f, sin_f, w_q, w_o)
        dy_rows = [a.reshape(TWO, TWO, CHUNK, d_model) for a in dy_rows]
        dy_pieces = swap([dy_rows[d % TWO] for d in relations])

        member = quad ^ jnp.arange(FOUR)
        front, back = ((m[:, NEW] * CHUNK + jnp.arange(CHUNK)[NEW]).reshape(BLK) for m in (member, 3 - member))
        offsets = jnp.stack([front, back]).astype(jnp.int32)
        own_super = jnp.stack([pair, N_SUPER - 1 - pair]).astype(jnp.int32)
        q_index = own_super[:, NEW] * BLK + offsets
        start = q_index[NEW] - pos_u
        tab = jnp.concatenate(
            [own_super, (jnp.min(start, axis=-1) // BLK).reshape(-1), jnp.max(start, axis=-1).reshape(-1)]
        )
        start_r = start[:, :, NEW, :]
        q_index_r = jnp.broadcast_to(q_index[NEW, :, NEW, :], start_r.shape)
        cos_u, sin_u = rope_tables(pos_u)
        cos_ut, sin_ut = jnp.swapaxes(cos_u, TWO, 3), jnp.swapaxes(sin_u, TWO, 3)

        koff = offsets[:, NEW]
        attn_u, lse = flash_fwd(tab, q_u, kv_all, start_r, q_index_r, koff)

        wo_keep, wo_away = wo_terms(attn_u, dy_pieces)
        wo_come = perm(wo_away, flip_pairs(FOUR))
        do_u, wo_keep = lax.optimization_barrier((do_u, wo_keep))
        dq_u, dkv = flash_bwd(tab, q_u, do_u, attn_u, kv_all, lse, start_r, q_index_r, koff, cos_ut, sin_ut)
        wo_sum = wo_keep + wo_come

        x_flat = hidden.reshape(n_rows, d_model)
        wo_own, dkv_own, wq_own, block_out, d_part, h_u = reduce_pairs(
            [wo_sum, dkv.reshape(FOUR, TWO, -1, HEAD_DIM)],
            [wo_sum.shape[1:], (dkv.size // N_PAIRS // HEAD_DIM, HEAD_DIM), (d_model // TWO // N_PAIRS, wide)],
            (TWO, 8, 8),
            ("z", "", "core"),
            TWO,
            Products,
            (attn_u, dq_u, x_flat, normed.reshape((TWO,) * 3 + (CHUNK, d_model)), w_o, w_q),
        )
        grad_wo, grad_wq, grad_wk, grad_wv, grad_x, d_gain = gather_all(
            wo_own,
            wq_own,
            dkv_own,
            cos_ut,
            sin_ut,
            h_u,
            d_part,
            w_k,
            w_v,
            x_flat,
            dy_flat,
            gain[NEW],
            [w_o.shape, w_q.shape, w_k.shape, w_v.shape],
        )
        block_out, grad_x = (a.reshape(hidden.shape) for a in (block_out, grad_x))
        return block_out, grad_x, grad_wq, grad_wk, grad_wv, grad_wo, d_gain.reshape(d_model)

    seq_spec = P(None, "cp", None)
    tok_spec = P(None, "cp")
    full_spec = P()
    return jax.shard_map(
        local_step,
        mesh=mesh,
        in_specs=(seq_spec, seq_spec, tok_spec, tok_spec, full_spec, full_spec, full_spec, full_spec, full_spec),
        out_specs=(seq_spec, seq_spec, full_spec, full_spec, full_spec, full_spec, full_spec),
        check_vma=False,
    )
```

```python
import functools
import heapq
import itertools

import jax
import jax.numpy as jnp
from jax import lax
from jax.experimental import pallas as pl
from jax.experimental.pallas import tpu as pltpu
from jax.sharding import PartitionSpec as P

HEAD_DIM = 128
NORM_EPS = 1e-5
ROPE_BASE = 500000.0
NEG_BIG = -1e30
LOG2E = 1.4426950408889634
ATTN_SCALE = HEAD_DIM**-0.5
EXP2_SCALE = ATTN_SCALE * LOG2E
CHUNK = 64
TWO = 2
FOUR = 4
NEW = jnp.newaxis
BLK = 4 * CHUNK
N_HEADS = 8
N_PAIRS = 8
N_SUPER = 2 * N_PAIRS
MESH = pl.DeviceIdType.MESH
ONE = pl.Squeezed()
GROUP = 4
MADE_AT = 5
PRODUCTS_AT = 7, 9
F32 = jnp.float32
BF16 = jnp.bfloat16

T_SQ, T_LO, T_MX = 0, 2, 6


def rope_tables(positions):
    inv_freq = ROPE_BASE ** (-jnp.arange(0, HEAD_DIM, TWO).astype(F32) / HEAD_DIM)
    angles = positions.astype(F32)[..., None] * inv_freq
    return jnp.cos(angles), jnp.sin(angles)


def dot(a, b, ca, cb):
    return lax.dot_general(a, b, ((ca, cb), ((), ())), preferred_element_type=F32)


def cost(gflop, mib):
    return pl.CostEstimate(flops=gflop * 10**9, bytes_accessed=mib << 20, transcendentals=0)


def params(mib, **more):
    return pltpu.CompilerParams(vmem_limit_bytes=mib << 20, **more)


def row_mean(x):
    return jnp.mean(x, axis=-1, keepdims=True)


def head(h):
    return pl.ds(h * HEAD_DIM, HEAD_DIM)


def head_slice(h):
    return slice(h * HEAD_DIM, (h + 1) * HEAD_DIM)


def dot_t(a, b):
    return dot(a, b, (1,), (1,))


def steps(tab, body):
    b, hf = pl.program_id(0), pl.program_id(1)
    own, first, last_start = tab[T_SQ + hf], tab[T_LO + TWO * b + hf], tab[T_MX + TWO * b + hf]

    def step(s, carry):
        late = s >= N_PAIRS
        at = jnp.where(late, N_SUPER - 1 - s, s), late.astype(jnp.int32)
        full = jnp.logical_and(s < own, s * BLK >= last_start)
        pl.when(full)(lambda: body(s, at, False))
        pl.when(jnp.logical_not(full))(lambda: body(s, at, True))
        return carry

    lax.fori_loop(first, own + 1, step, 0)


def down(row, n):
    return jnp.broadcast_to(row, (n, row.shape[-1])).T


def may_use(s, off, st_ref, qi_ref):
    return jnp.logical_and(off >= st_ref[...] - s * BLK, off <= qi_ref[...] - s * BLK)


def fwd_kernel(tab, q_ref, kv_ref, st_ref, qi_ref, ko_ref, o_ref, lse_ref, q_s, acc, m_s, l_s, k_t, bounds):
    m_s[...] = jnp.full_like(m_s, NEG_BIG)
    l_s[...] = jnp.zeros_like(l_s)
    acc[...] = jnp.zeros_like(acc)
    for i, ref in enumerate((st_ref, qi_ref)):
        bounds[i] = down(ref[...], HEAD_DIM)
    for h in range(N_HEADS):
        q_s[pl.ds(h * BLK, BLK)] = q_ref[:, head(h)]

    @pl.when(pl.program_id(1) == 0)
    def _():
        @pl.loop(0, N_PAIRS)
        def _(pair):
            for hk in range(TWO):
                k_t[pair, hk] = kv_ref[pair, 0, hk].T

    def body(s, at, masked):
        pair, hk = at
        v = kv_ref[pair, 1, hk]
        if masked:
            off = ko_ref[hk] + s * BLK
            mask = [
                jnp.logical_and(off[:, lanes] >= bounds[0], off[:, lanes] <= bounds[1])
                for lanes in (slice(HEAD_DIM), slice(HEAD_DIM, BLK))
            ]
            mask = [jnp.concatenate([m, m], axis=0) for m in mask]
        for g in range(N_HEADS // TWO):
            rows = pl.ds(g * TWO * BLK, TWO * BLK)
            sc = jnp.dot(q_s[rows], k_t[pair, hk], preferred_element_type=F32)
            sc = [sc[:, :HEAD_DIM], sc[:, HEAD_DIM:]]
            if masked:
                sc = [jnp.where(m, x, NEG_BIG) for m, x in zip(mask, sc)]
            m_old = m_s[rows]
            m_new = jnp.maximum(m_old, jnp.max(jnp.maximum(*sc), axis=1, keepdims=True))
            alpha = jnp.exp2((m_old - m_new) * EXP2_SCALE)
            p = [jnp.exp2((x - m_new) * EXP2_SCALE) for x in sc]
            m_s[rows] = m_new
            l_s[rows] = l_s[rows] * alpha + (p[0] + p[1])
            p = jnp.hstack([x.astype(BF16) for x in p])
            acc[rows] = acc[rows] * alpha + jnp.dot(p, v, preferred_element_type=F32)

    steps(tab, body)
    for h in range(N_HEADS):
        rows = pl.ds(h * BLK, BLK)
        total = jnp.sum(l_s[rows], axis=1, keepdims=True)
        o_ref[:, head(h)] = (acc[rows] / total).astype(BF16)
        lse_ref[h] = (m_s[rows] * EXP2_SCALE + jnp.log2(total)).T[:1]


def bwd_kernel(tab, q_ref, do_ref, o_ref, kv_ref, lse_ref, st_ref, qi_ref, ko_ref, cos_ref, sin_ref, dq_ref, dkv_ref, *scratch):
    dq_acc, delta, off_s, q_s, do_s, q_t, do_t, p_s, ds_s = scratch
    dq_acc[...] = jnp.zeros_like(dq_acc)
    for h in range(N_HEADS):
        q, do = q_ref[:, head(h)], do_ref[:, head(h)]
        delta[h] = jnp.sum((do.astype(F32) * o_ref[:, head(h)].astype(F32)).T, axis=0, keepdims=True)
        q_s[pl.ds(h * BLK, BLK)], do_s[pl.ds(h * BLK, BLK)] = q, do
        q_t[h], do_t[h] = q.T, do.T

    @pl.when(pl.program_id(1) == 0)
    def _():
        dkv_ref[...] = jnp.zeros_like(dkv_ref)
        for hk in range(TWO):
            off_s[hk] = down(ko_ref[hk], BLK)

    def body(s, at, masked):
        pair, hk = at
        k = kv_ref[pair, 0, hk]
        v = kv_ref[pair, 1, hk]
        k_t = k.T
        mask = may_use(s, off_s[hk], st_ref, qi_ref) if masked else None
        for first in range(0, N_HEADS, GROUP):
            rows = pl.ds(first * BLK, GROUP * BLK)
            for h in range(first, first + GROUP):
                cols = pl.ds(h * BLK, BLK)
                p = jnp.exp2(jnp.dot(k, q_t[h], preferred_element_type=F32) * EXP2_SCALE - lse_ref[h])
                if masked:
                    p = jnp.where(mask, p, 0.0)
                ds = p * (jnp.dot(v, do_t[h], preferred_element_type=F32) - delta[h])
                p_s[:, cols] = p.astype(BF16)
                ds_s[:, cols] = ds.astype(BF16)
            dkv_ref[pair, 0, hk] += jnp.dot(ds_s[:, rows], q_s[rows], preferred_element_type=F32)
            dkv_ref[pair, 1, hk] += jnp.dot(p_s[:, rows], do_s[rows], preferred_element_type=F32)
            dq_acc[:, rows] += jnp.dot(k_t, ds_s[:, rows], preferred_element_type=F32)

    steps(tab, body)
    cos_t, sin_t = cos_ref[...], sin_ref[...]
    half = HEAD_DIM // TWO
    for h in range(N_HEADS):
        cols = pl.ds(h * BLK, BLK)
        a, c = dq_acc[:half, cols] * ATTN_SCALE, dq_acc[half:, cols] * ATTN_SCALE
        lin = jnp.concatenate([a * cos_t + c * sin_t, c * cos_t - a * sin_t], axis=0)
        dq_ref[:, head(h)] = lin.T.astype(BF16)


def attn_specs():
    def at_tile(b, h, t):
        return (b, h) + (0,) * TWO

    def at_row(b, h, t):
        return (0, 0, b) + (0,) * 3

    tile = pl.BlockSpec((ONE, ONE, BLK, N_HEADS * HEAD_DIM), at_tile)
    row = pl.BlockSpec((ONE, ONE, 1, BLK), at_tile)
    stat = pl.BlockSpec((ONE, ONE, N_HEADS, 1, BLK), lambda b, h, t: (b, h) + (0,) * 3)
    rope = pl.BlockSpec((ONE, ONE, HEAD_DIM // TWO, BLK), at_tile)
    kv = pl.BlockSpec((N_PAIRS, TWO, ONE, TWO, BLK, HEAD_DIM), at_row)
    ko = pl.BlockSpec((TWO, 1, BLK), lambda b, h, t: (0,) * 3)
    return tile, row, stat, kv, ko, rope


def flash_fwd(tab, q, kv, start, qidx, koff):
    tile, row, stat, kvs, ko, _ = attn_specs()
    return pl.pallas_call(
        fwd_kernel,
        name="attn_fwd",
        out_shape=(jax.ShapeDtypeStruct(q.shape, BF16), jax.ShapeDtypeStruct((TWO, TWO, N_HEADS, 1, BLK), F32)),
        grid_spec=pltpu.PrefetchScalarGridSpec(
            num_scalar_prefetch=1,
            grid=(TWO, TWO),
            in_specs=[tile, kvs, row, row, ko],
            out_specs=[tile, stat],
            scratch_shapes=[pltpu.VMEM((N_HEADS * BLK, HEAD_DIM), t) for t in (BF16, F32, F32, F32)]
            + [pltpu.VMEM((N_PAIRS, TWO, HEAD_DIM, BLK), BF16), pltpu.VMEM((TWO, BLK, HEAD_DIM), jnp.int32)],
        ),
        compiler_params=params(63),
        cost_estimate=cost(20, 16),
    )(tab, q, kv, start, qidx, koff)


def flash_bwd(tab, q, do, o, kv, lse, start, qidx, koff, cos_t, sin_t):
    tile, row, stat, kvs, ko, rope = attn_specs()
    return pl.pallas_call(
        bwd_kernel,
        name="attn_bwd",
        out_shape=(
            jax.ShapeDtypeStruct(q.shape, BF16),
            jax.ShapeDtypeStruct(kv.shape, F32),
        ),
        grid_spec=pltpu.PrefetchScalarGridSpec(
            num_scalar_prefetch=1,
            grid=(TWO, TWO),
            in_specs=[tile, tile, tile, kvs, stat, row, row, ko, rope, rope],
            out_specs=[tile, kvs],
            scratch_shapes=[pltpu.VMEM((HEAD_DIM, N_HEADS * BLK), F32), pltpu.VMEM((N_HEADS, 1, BLK), F32)]
            + [pltpu.VMEM((TWO, BLK, BLK), jnp.int32)]
            + [pltpu.VMEM((N_HEADS * BLK, HEAD_DIM), BF16)] * TWO
            + [pltpu.VMEM((N_HEADS, HEAD_DIM, BLK), BF16)] * TWO
            + [pltpu.VMEM((BLK, N_HEADS * BLK), BF16)] * TWO,
        ),
        compiler_params=params(63),
        cost_estimate=cost(50, 32),
    )(tab, q, do, o, kv, lse, start, qidx, koff, cos_t, sin_t)


def turn(x, cos_ref, sin_ref):
    return x * cos_ref[...] + pltpu.roll(x, HEAD_DIM // TWO, 1) * sin_ref[...]


def first_kernel(x_ref, g_ref, wk_ref, wv_ref, cos_ref, sin_ref, h_ref, kv_ref):
    x = x_ref[...].astype(F32)
    h = (x * lax.rsqrt(row_mean(x * x) + NORM_EPS) * g_ref[...]).astype(BF16)
    h_ref[...] = h
    k = jnp.dot(h, wk_ref[...], preferred_element_type=F32)
    v = jnp.dot(h, wv_ref[...], preferred_element_type=F32)
    n = kv_ref.shape[3]
    for i in range(TWO):
        for j, val in enumerate((turn(k[:, head_slice(i)], cos_ref, sin_ref), v[:, head_slice(i)])):
            for c in range(TWO):
                kv_ref[i, c, j] = val[c * n : (c + 1) * n].astype(BF16)


def project(x, gain, w_k, w_v, cos_f, sin_f):
    n = x.shape[0] // TWO
    return pl.pallas_call(
        first_kernel,
        name="norm_kv",
        out_shape=(jax.ShapeDtypeStruct(x.shape, BF16), jax.ShapeDtypeStruct((TWO,) * 3 + (n, HEAD_DIM), BF16)),
        compiler_params=params(63),
        cost_estimate=cost(TWO, 7),
    )(x, gain, w_k, w_v, cos_f, sin_f)


def place(me):
    return me // 8, lax.rem(me // FOUR, TWO), lax.rem(me // TWO, TWO), lax.rem(me, TWO)


def dev(z, y, x, core):
    return ((z * TWO + y) * TWO + x) * TWO + core


def z_peers(z):
    return [(k, lax.rem(z + k, FOUR)) for k in (1, TWO, 3)]


def meet(peers):
    barrier = pltpu.get_barrier_semaphore()
    for d in peers:
        pl.semaphore_signal(barrier, device_id=(d,), device_id_type=MESH)
    pl.semaphore_wait(barrier, len(peers))


def remote(src, dst, send, arrive, to):
    return pltpu.make_async_remote_copy(
        src_ref=src, dst_ref=dst, send_sem=send, recv_sem=arrive, device_id=(to,), device_id_type=MESH
    )


class Line:
    order = (0, 1, -1, TWO, -TWO, 3, -3)

    def __init__(self, me):
        self.z, y, x, core = place(me)
        self.next = {1: dev(self.z + 1, y, x, core), -1: dev(self.z - 1, y, x, core)}
        self.inside = {1: self.z < 3, -1: self.z > 0}

    def held(self, dz):
        return jnp.logical_and(self.z + dz >= 0, self.z + dz <= 3)

    def ways(self, dz):
        for d in self.next:
            if d * dz <= 0:
                yield d, self.inside[d] if dz == 0 else jnp.logical_and(self.inside[d], self.held(dz))


def tiled(n, fetch, use, first=0):
    fetch(first, 0).start()

    @pl.loop(0, n)
    def _(t):
        slot = lax.rem(t, TWO)
        fetch(first + t, slot).wait()

        @pl.when(t + 1 < n)
        def _():
            fetch(first + t + 1, 1 - slot).start()

        use(first + t, slot)


def aligned(t, size=BLK):
    return pl.ds(pl.multiple_of(t * size, size), size)


def exchange_kernel(*refs):
    take = taker(refs)
    kv_ref, h_ref, dy_ref, pos_ref, cos_ref, sin_ref, wq_ref, wo_ref, kv_all, q_u, do_u, pos_u, *dy_rows = take(14)
    own_sem, quad_s, quad_r, z_s, z_r, y_s, y_r, q_home, do_home, wq_buf, wo_buf, w_sem, dy_sem = take(len(refs))
    me = lax.axis_index("cp")
    z, y, x, core = place(me)
    quad, line = quad_of(me), Line(me)
    across = dev(z, 1 - y, x, core)
    meet(quad[1:] + [across] + [dev(zz, y, x, core) for _, zz in z_peers(z)])

    def source(a, d):
        xx, cc = 1 - x if d // TWO else x, 1 - core if d % TWO else core
        return pos_ref.at[cc] if a == 3 else (kv_ref, q_home, do_home)[a].at[xx, cc]

    def target(a, d):
        if a == 3:
            return pos_u.at[d]
        tok = pl.ds(d * CHUNK, CHUNK)
        return kv_all.at[me // FOUR, :, :, :, tok] if a == 0 else (q_u, do_u)[a - 1].at[:, :, tok]

    def quad_copy(a, d):
        return remote(source(a, d), target(a, d), quad_s.at[a, d], quad_r.at[a, d], quad[d])

    def own_copy(a):
        return pltpu.make_async_copy(source(a, 0), target(a, 0), own_sem.at[a])

    def z_copy(part, dz, d):
        block = kv_all.at[TWO * (z + dz) + y, part]
        return remote(block, block, z_s.at[part, (d + 1) // TWO, dz + 3], z_r.at[part, dz - d + 3], line.next[d])

    def y_copy(part, dz, yy=y):
        block = kv_all.at[TWO * (z + dz) + yy, part]
        return remote(block, block, y_s.at[part, dz + 3], y_r.at[part, dz + 3], across)

    parts = range(TWO)
    moves = [(part, dz) for dz in line.order for part in parts]

    def pass_on(count):
        for part, dz in [moves.pop(0) for _ in range(count)]:
            if dz:
                block = kv_all.at[TWO * (z + dz) + y, part]
                arrival = remote(block, block, own_sem.at[0], z_r.at[part, dz + 3], me)
                pl.when(line.held(dz))(arrival.wait_recv)
            for d, on in line.ways(dz):
                pl.when(on)(z_copy(part, dz, d).start)
            pl.when(line.held(dz))(y_copy(part, dz).start)

    n = h_ref.shape[1] // BLK // TWO

    def fetch_q(t, slot):
        return pltpu.make_async_copy(wq_ref.at[:, aligned(t)], wq_buf.at[slot], w_sem.at[0, slot])

    def fetch_o(t, slot):
        return pltpu.make_async_copy(wo_ref.at[aligned(t)], wo_buf.at[slot], w_sem.at[1, slot])

    def put(home, t, val):
        home[t // n, :, :, :, :, aligned(lax.rem(t, n))] = val.astype(BF16).reshape(home.shape[1:-1] + (BLK,))

    def query(t, slot):
        q = jnp.dot(h_ref[...], wq_buf[slot], preferred_element_type=F32)
        put(q_home, t, jnp.hstack([turn(q[:, head_slice(j)], cos_ref, sin_ref) for j in range(BLK // HEAD_DIM)]))

    def pull(t, slot):
        put(do_home, t, dot_t(dy_ref[...], wo_buf[slot]))

    all_moves = list(moves)
    half = dy_ref.shape[0] // TWO
    for i, out in enumerate(dy_rows):
        pltpu.make_async_copy(dy_ref.at[aligned(core if i == 0 else 1 - core, half)], out, dy_sem.at[i]).start()
    for a in (0, 3):
        for d in (1, TWO, 3):
            quad_copy(a, d).start()
        own_copy(a).start()
    for a, (fetch, use) in enumerate(((fetch_q, query), (fetch_o, pull)), 1):
        for near in range(TWO):
            tiled(n, fetch, use, n * (x if near else 1 - x))
            for d in range(TWO):
                if d or not near:
                    quad_copy(a, d if near else d + TWO).start()
            if near:
                own_copy(a).start()
            if len(moves) == len(all_moves):
                own_copy(0).wait()
                for d in (1, TWO, 3):
                    quad_copy(0, d).wait_recv()
            pass_on(TWO)
    pass_on(len(moves))
    for part, dz in all_moves:
        for d, on in line.ways(dz):
            pl.when(on)(z_copy(part, dz, d).wait_send)
        pl.when(line.held(dz))(y_copy(part, dz, 1 - y).wait_recv)
        pl.when(line.held(dz))(y_copy(part, dz).wait_send)
    for a in range(FOUR):
        for d in (1, TWO, 3):
            quad_copy(a, d).wait_send()
            if a > 0:
                quad_copy(a, d).wait_recv()
    for a in (1, TWO, 3):
        own_copy(a).wait()
    for i, out in enumerate(dy_rows):
        pltpu.make_async_copy(dy_ref.at[aligned(core if i == 0 else 1 - core, half)], out, dy_sem.at[i]).wait()


def exchange(kv, h, dy, pos, cos_f, sin_f, w_q, w_o):
    dma = pltpu.SemaphoreType.DMA
    vmem, hbm = pl.BlockSpec(memory_space=pltpu.VMEM), pl.BlockSpec(memory_space=pl.ANY)
    wide = w_q.shape[1] // TWO
    unit = jax.ShapeDtypeStruct((TWO, TWO, BLK, wide), BF16)
    pos_quad = jax.ShapeDtypeStruct((FOUR,) + pos.shape[1:], pos.dtype)
    dy_half = jax.ShapeDtypeStruct((dy.shape[0] // TWO, dy.shape[1]), BF16)
    home = pltpu.VMEM((TWO,) * FOUR + (CHUNK, wide), BF16)
    sems = [dma((FOUR,))] + [dma((FOUR, FOUR))] * TWO + [dma((TWO, TWO, 7))] + [dma((TWO, 7))] * 3
    bufs = [pltpu.VMEM((TWO,) + b, BF16) for b in ((w_q.shape[0], BLK), (BLK, w_o.shape[1]))]
    return pl.pallas_call(
        exchange_kernel,
        name="exchange",
        out_shape=(jax.ShapeDtypeStruct((N_PAIRS,) + (TWO,) * 3 + (BLK, HEAD_DIM), BF16), unit, unit, pos_quad, dy_half, dy_half),
        in_specs=[vmem] * 6 + [hbm] * TWO,
        out_specs=[hbm] * 6,
        scratch_shapes=sems + [home, home] + bufs + [dma((TWO, TWO)), dma((TWO,))],
        compiler_params=params(63, collective_id=1),
        cost_estimate=cost(1, 20),
    )(kv, h, dy, pos, cos_f, sin_f, w_q, w_o)


def taker(refs):
    rest = iter(refs)
    return lambda count: list(itertools.islice(rest, count))


def wo_kernel(*refs):
    take = taker(refs)
    o_ref, *pieces = take(5)
    keep, away, dy_u, o_t, terms, came, load_sem, core_s, core_r = take(len(refs))
    me = lax.axis_index("cp")
    _, y, _, core = place(me)
    meet(quad_of(me)[1:TWO])
    loads = [
        pltpu.make_async_copy(src, dy_u.at[:, :, pl.ds(d * CHUNK, CHUNK)], load_sem.at[d])
        for d, src in enumerate(pieces)
    ]
    for c in loads:
        c.start()
    for h in range(N_HEADS):
        o_t[head(h)] = o_ref[:, :, :, head(h)].reshape(-1, HEAD_DIM).T
    for c in loads:
        c.wait()
    half, tiles = terms.shape[1], terms.shape[TWO] // BLK

    def swap(t):
        return remote(terms.at[0, :, aligned(t)], came.at[:, aligned(t)], core_s.at[t], core_r.at[t], quad_of(me)[1])

    def half_terms(i, to, then):
        @pl.loop(0, tiles)
        def _(t):
            dy = dy_u[:, :, :, aligned(t)].reshape(-1, BLK)
            terms[to, :, aligned(t)] = jnp.dot(o_t[aligned(i, half)], dy, preferred_element_type=F32)
            then(t)

    half_terms(1 - core, 0, lambda t: swap(t).start())
    half_terms(core, 1, lambda t: swap(t).wait_recv())
    rows = keep.shape[1]
    for zz in range(FOUR):
        for out, yy in ((keep, y), (away, 1 - y)):
            at = aligned(TWO * zz + yy, rows)
            out[zz] = terms[1, at] + came[at]
    for t in range(tiles):
        swap(t).wait_send()


def wo_terms(o, pieces):
    dma = pltpu.SemaphoreType.DMA
    vmem, hbm = pl.BlockSpec(memory_space=pltpu.VMEM), pl.BlockSpec(memory_space=pl.ANY)
    n, d, wide = o.shape[0] * o.shape[1] * o.shape[TWO], pieces[0].shape[-1], o.shape[-1]
    half = wide // TWO
    return pl.pallas_call(
        wo_kernel,
        name="wo_terms",
        out_shape=[jax.ShapeDtypeStruct((FOUR, half // N_PAIRS, d), F32)] * TWO,
        in_specs=[vmem] + [hbm] * FOUR,
        out_specs=[vmem] * TWO,
        scratch_shapes=[pltpu.VMEM((TWO, TWO, BLK, d), BF16), pltpu.VMEM((wide, n), BF16)]
        + [pltpu.VMEM((TWO, half, d), F32), pltpu.VMEM((half, d), F32), dma((FOUR,)), dma((d // BLK,)), dma((d // BLK,))],
        compiler_params=params(63, collective_id=3),
        cost_estimate=cost(FOUR, 20),
    )(o, *pieces)


class PairSum:
    def __init__(self, me, kind, cut, src, out, buffers, sems):
        self.me, self.kind, self.src, self.out = me, kind, src, out
        self.size = out.shape[0] // cut
        self.own, self.from_core, self.from_y, self.from_z = buffers
        self.load_sem, self.core_s, self.core_r, self.y_s, self.y_r, self.z_s, self.z_r = sems
        self.z, self.y, x, core = place(me)
        self.partner = dev(self.z, self.y, x, 1 - core)
        self.across = dev(self.z, 1 - self.y, x, core)
        self.next_z = dev(self.z + 1, self.y, x, core), dev(self.z - 1, self.y, x, core)

    def rows(self, j):
        return pl.ds(j * self.size, self.size)

    def mine(self, j, zz):
        at = self.rows(j)
        return self.own.at[zz, self.y, at] if self.kind == "core" else self.own.at[zz, at]

    def load(self, j):
        at = self.rows(j)
        src = self.src.at[:, at] if self.kind else self.src.at[:, self.y, at]
        return pltpu.make_async_copy(src, self.own.at[:, at], self.load_sem.at[j])

    def core_copy(self, j):
        src, dst = (r.at[:, :, self.rows(j)] for r in (self.src, self.from_core))
        return remote(src, dst, self.core_s.at[j], self.core_r.at[j], self.partner)

    def y_copy(self, j):
        src = self.own if self.kind == "core" else self.src
        at = self.rows(j)
        return remote(src.at[:, 1 - self.y, at], self.from_y.at[:, at], self.y_s.at[j], self.y_r.at[j], self.across)

    def z_copy(self, j, way, zz, to):
        at = way, zz + way - 1
        return remote(self.mine(j, zz), self.from_z.at[*at, self.rows(j)], self.z_s.at[j, *at], self.z_r.at[j, *at], to)

    def begin(self, j):
        if self.kind == "core":
            self.core_copy(j).start()
            return
        self.load(j).start()
        if not self.kind:
            self.y_copy(j).start()

    def loaded(self, j):
        if self.kind != "core":
            self.load(j).wait()
        else:
            self.core_copy(j).wait_recv()
            at = self.rows(j)
            for zz in range(FOUR):
                self.own[zz, :, at] += self.from_core[zz, :, at]
            self.y_copy(j).start()
        if self.kind == "z":
            self.hop(j, 0)

    def relay(self, j, way, zz, add):
        if add:
            self.z_copy(j, way, zz, self.me).wait_recv()
            self.mine(j, zz)[...] += self.from_z[way, zz + way - 1, self.rows(j)]
        self.z_copy(j, way, zz, self.next_z[way]).start()

    def hop(self, j, h):
        @pl.when(self.z == h)
        def _():
            for zz in range(3, h, -1):
                self.relay(j, 0, zz, h > 0)

        @pl.when(self.z == 3 - h)
        def _():
            for zz in range(3 - h):
                self.relay(j, 1, zz, h > 0)

    def step(self, j, h):
        if h == 0 and self.kind != "z":
            self.y_copy(j).wait_recv()
            for zz in range(FOUR):
                self.mine(j, zz)[...] += self.from_y[zz, self.rows(j)]
            self.hop(j, 0)
        elif 0 < h < 3:
            self.hop(j, h)
        elif h == 3:
            at = self.rows(j)
            self.out[at] = self.mine(j, self.z)[...]
            for way, on in enumerate((self.z > 0, self.z < 3)):

                @pl.when(on)
                def _(way=way):
                    self.z_copy(j, way, self.z, self.me).wait_recv()
                    self.out[at] += self.from_z[way, self.z + way - 1, at]

    def wait_send(self, j):
        if self.kind == "core":
            self.core_copy(j).wait_send()
        if self.kind != "z":
            self.y_copy(j).wait_send()
        for zz in range(FOUR):
            if zz > 0:
                pl.when(self.z < zz)(self.z_copy(j, 0, zz, self.next_z[0]).wait_send)
            if zz < 3:
                pl.when(self.z > zz)(self.z_copy(j, 1, zz, self.next_z[1]).wait_send)

    @staticmethod
    def scratch(kind, block):
        unused = pltpu.VMEM((8, HEAD_DIM), F32)
        own = pltpu.VMEM(((FOUR, TWO) if kind == "core" else (FOUR,)) + block, F32)
        from_y = unused if kind == "z" else pltpu.VMEM((FOUR,) + block, F32)
        return [own, own if kind == "core" else unused, from_y, pltpu.VMEM((TWO, 3) + block, F32)]

    @staticmethod
    def sems(*dims):
        dma = pltpu.SemaphoreType.DMA
        return [dma(dims)] * 5 + [dma(dims + (TWO, 3))] * TWO


def reduce_kernel(cuts, kinds, work, *refs):
    n = len(cuts)

    take = taker(refs)
    ins, more_in, outs, more_out, made = take(n - 1), take(work.ins), take(n), take(work.outs), take(1)
    buffers, sems = [take(FOUR) for _ in kinds], take(7)
    me = lax.axis_index("cp")
    z, y, x, core = place(me)
    meet(quad_of(me)[1:] + [dev(z, 1 - y, x, core)] + [dev(zz, y, x, core) for _, zz in z_peers(z)])
    job = work(me, more_in, more_out, take(len(refs)))
    sums = [PairSum(me, *a, [r.at[i] for r in sems]) for i, a in enumerate(zip(kinds, cuts, ins + made, outs, buffers))]
    pieces = [(s, j) for s, cut in zip(sums, cuts) for j in range(cut)]
    early, late = pieces[: -cuts[-1]], pieces[-cuts[-1] :]
    for s, j in early:
        s.begin(j)
    for s, j in early:
        s.loaded(j)
    for t in range(len(pieces) + 3):
        if t == MADE_AT:
            job.wq_terms(sums[-1].own, made[0])
            for s, j in late:
                s.begin(j)
        if t == MADE_AT + 1:
            for s, j in late:
                s.loaded(j)
        for h in range(FOUR):
            if 0 <= t - h < len(pieces):
                s, j = pieces[t - h]
                s.step(j, h)
        job.step(t)
    for s, j in pieces:
        s.wait_send(j)
    job.finish()


def quad_of(me):
    z, y, x, core = place(me)
    return [dev(z, y, 1 - x if d // TWO else x, 1 - core if d % TWO else core) for d in range(FOUR)]


class Home:
    def __init__(self, me, src, out, own_sem, send, arrive):
        _, _, x, core = place(me)
        w = src.shape[-1]
        to = out.at[core, :, :, :, pl.ds(x * w, w)]

        def piece(d):
            return src.at[:, :, pl.ds(d * CHUNK, CHUNK)]

        self.own = pltpu.make_async_copy(piece(0), to, own_sem)
        self.copies = [remote(piece(d), to, send.at[d], arrive.at[d], quad_of(me)[d]) for d in (1, TWO, 3)]

    def start(self):
        self.own.start()
        for c in self.copies:
            c.start()

    def wait_recv(self):
        self.own.wait()
        for c in self.copies:
            c.wait_recv()

    def wait_send(self):
        for c in self.copies:
            c.wait_send()


class Products:
    ins, outs = 6, 3

    def __init__(self, me, ins, outs, scratch):
        attn, self.dq, hidden, normed, self.w_o, self.w_q = ins
        self.block_out, self.d_part, self.h_u = outs
        self.attn_home, self.dq_home, self.buf_o, self.buf_q, self.h_own, *sems = scratch
        self.w_sem, self.load_sem, own_sem, quad_s, quad_r = sems
        _, _, _, core = place(me)

        def piece(d):
            return normed.at[1 - core if d % TWO else core]

        def tokens(d):
            return self.h_u.at[:, :, pl.ds(d * CHUNK, CHUNK)]

        self.h_copies = [remote(piece(d), tokens(d), quad_s.at[TWO, d], quad_r.at[TWO, d], quad_of(me)[d]) for d in (1, TWO, 3)]
        self.h_mine = pltpu.make_async_copy(piece(0), self.h_own.at[:, :, pl.ds(0, CHUNK)], own_sem.at[TWO])
        self.h_rest = pltpu.make_async_copy(
            self.h_u.at[:, :, pl.ds(CHUNK, BLK - CHUNK)], self.h_own.at[:, :, pl.ds(CHUNK, BLK - CHUNK)], self.load_sem
        )
        self.h_back = pltpu.make_async_copy(self.h_own.at[:, :, pl.ds(0, CHUNK)], tokens(0), self.load_sem)
        self.residual = pltpu.make_async_copy(hidden, self.block_out, own_sem.at[3])
        self.residual.start()
        for c in self.h_copies:
            c.start()
        self.h_mine.start()
        self.homes = [
            Home(me, src, out, own_sem.at[i], quad_s.at[i], quad_r.at[i])
            for i, (src, out) in enumerate([(attn, self.attn_home), (self.dq, self.dq_home)])
        ]
        for h in self.homes:
            h.start()

    @staticmethod
    def scratch(arrays):
        dma, d = pltpu.SemaphoreType.DMA, arrays[-1].shape[0]
        home = pltpu.VMEM((TWO,) * 3 + (CHUNK, d), BF16)
        buf = [pltpu.VMEM((TWO,) + b, BF16) for b in ((d, BLK), (BLK, d))]
        unit = pltpu.VMEM((TWO, TWO, BLK, d), BF16)
        return [home] * TWO + buf + [unit, dma((TWO, TWO)), dma(()), dma((FOUR,)), dma((3, FOUR)), dma((3, FOUR))]

    @staticmethod
    def results(arrays):
        unit = TWO, TWO, BLK, arrays[-1].shape[0]
        return [jax.ShapeDtypeStruct(arrays[TWO].shape, t) for t in (BF16, F32)] + [jax.ShapeDtypeStruct(unit, BF16)]

    spaces, out_spaces = [pl.ANY, pltpu.VMEM] + [pl.ANY] * FOUR, [pltpu.VMEM] * TWO + [pl.ANY]

    def step(self, t):
        def fetch_o(t, slot):
            return pltpu.make_async_copy(self.w_o.at[:, aligned(t)], self.buf_o.at[slot], self.w_sem.at[0, slot])

        def fetch_q(t, slot):
            return pltpu.make_async_copy(self.w_q.at[aligned(t)], self.buf_q.at[slot], self.w_sem.at[1, slot])

        def project(t, slot):
            at = aligned(t)
            attn = self.attn_home[...].reshape(-1, self.w_o.shape[0])
            out = jnp.dot(attn, self.buf_o[slot], preferred_element_type=F32)
            self.block_out[:, at] = (self.block_out[:, at].astype(F32) + out).astype(BF16)

        def pull(t, slot):
            dq = self.dq_home[...].reshape(-1, self.w_o.shape[0])
            self.d_part[:, aligned(t)] = dot_t(dq, self.buf_q[slot])

        if t in PRODUCTS_AT:
            i = PRODUCTS_AT.index(t)
            self.homes[i].wait_recv()
            if i == 0:
                self.residual.wait()
            tiled(self.w_o.shape[0] // BLK, *((fetch_o, project), (fetch_q, pull))[i])

    def wq_terms(self, own, other):
        self.h_mine.wait()
        self.h_back.start()
        for c in self.h_copies:
            c.wait_recv()
        self.h_back.wait()
        self.h_rest.start()
        self.h_rest.wait()
        core = lax.rem(lax.axis_index("cp"), TWO)
        d_out = self.dq[...].reshape(-1, self.dq.shape[-1])
        for out, half in ((other, 1 - core), (own, core)):

            @pl.loop(0, FOUR)
            def _(zz, out=out, half=half):
                h = self.h_own[:, :, :, aligned(half * FOUR + zz)].reshape(-1, BLK)
                out[zz] = dot(h, d_out, (0,), (0,)).reshape(out.shape[1:])

    def finish(self):
        for c in self.h_copies + self.homes:
            c.wait_send()


class HiddenGradient:
    tiles = FOUR

    def __init__(self, me, dk, dv, ins, outs, scratch):
        self.part, self.w_k, self.w_v, self.x, self.dy, self.gain = ins
        self.dx, self.terms = outs
        self.dk_home, self.dv_home, self.rows, *sems = scratch
        pairs = (dk, self.dk_home), (dv, self.dv_home)
        self.homes = [Home(me, src, out, *[r.at[i] for r in sems]) for i, (src, out) in enumerate(pairs)]
        for h in self.homes:
            h.start()

    @staticmethod
    def scratch(x):
        dma = pltpu.SemaphoreType.DMA
        home = pltpu.VMEM((TWO,) * 3 + (CHUNK, TWO * HEAD_DIM), BF16)
        return [home, home, pltpu.VMEM((8, x.shape[1]), F32), dma((TWO,)), dma((TWO, FOUR)), dma((TWO, FOUR))]

    def tile(self, t):
        if t == 0:
            for h in self.homes:
                h.wait_recv()
            self.rows[...] = jnp.zeros_like(self.rows)
        size = TWO * CHUNK
        at = pl.ds(t * size, size)
        d = self.part[at]
        for home, w in ((self.dk_home, self.w_k), (self.dv_home, self.w_v)):
            d += dot_t(home[t // TWO, t % TWO].reshape(size, -1), w[...])
        d = d.astype(BF16).astype(F32)
        x = self.x[at].astype(F32)
        inv_rms = lax.rsqrt(row_mean(x * x) + NORM_EPS)
        unit, scaled = x * inv_rms, d * self.gain[...]
        dx = inv_rms * (scaled - unit * row_mean(scaled * unit))
        self.dx[at] = (self.dy[at].astype(F32) + dx).astype(BF16)
        self.rows[...] += jnp.sum((d * unit).reshape((-1,) + self.rows.shape), axis=0)
        if t == self.tiles - 1:
            self.terms[...] = jnp.sum(self.rows[...], axis=0, keepdims=True)

    def finish(self):
        for h in self.homes:
            h.wait_send()


def reduce_pairs(arrays, blocks, cuts, kinds, collective_id, work, more):
    vmem, hbm = pl.BlockSpec(memory_space=pltpu.VMEM), pl.BlockSpec(memory_space=pl.ANY)
    n = len(blocks)
    scratch = [pltpu.VMEM((FOUR, TWO) + blocks[-1], F32)]
    scratch += sum((PairSum.scratch(k, b) for k, b in zip(kinds, blocks)), []) + PairSum.sems(n, max(cuts))
    outs = [jax.ShapeDtypeStruct(b, F32) for b in blocks] + work.results(more)
    return pl.pallas_call(
        functools.partial(reduce_kernel, cuts, kinds, work),
        name="reduce_pairs",
        out_shape=outs,
        in_specs=[hbm] * len(arrays) + [pl.BlockSpec(memory_space=m) for m in work.spaces],
        out_specs=[vmem] * n + [pl.BlockSpec(memory_space=m) for m in work.out_spaces],
        scratch_shapes=scratch + work.scratch(more),
        compiler_params=params(63, collective_id=collective_id),
        cost_estimate=cost(1, 20),
    )(*arrays, *more)


HERE = 0, 0, 0
LINKS = "xyud"
ORDERS = "zxy", "zyx", "yxz", "zyx"
WO_CUTS, WQ_CUTS = (0, 2, 6, 8), (0, 3, 6, 8)
SIZES = 7.0, 9.8, 5.6, 2.8
LATENCY, TILES_FROM, TILE_EVERY = 3.0, 14.0, 8.0
SUM_AT = 25.0, 31.0, 37.0, 43.0


def onward(order, key):
    dz, ry, rx = key
    stage = max((order.index(a) for a, r in zip("zyx", key) if r), default=-1)
    for axis in order[stage + 1 :]:
        if axis == "x":
            yield "x", (dz, ry, 1)
        elif axis == "y":
            yield "y", (dz, 1, rx)
        else:
            yield "u", (-1, ry, rx)
            yield "d", (1, ry, rx)
    if stage >= 0 and order[stage] == "z" and abs(dz) < 3:
        yield ("u", (dz - 1, ry, rx)) if dz < 0 else ("d", (dz + 1, ry, rx))


def arrivals():
    busy, times = {}, {}
    starts = [0.0] * 3 + [SUM_AT[-1] + LATENCY]
    here = [(t, z, part, HERE) for part, t in enumerate(starts) for z in range(FOUR)]
    while here:
        now, z, part, key = heapq.heappop(here)
        times.setdefault((part, key), []).append(now)
        for link, there in onward(ORDERS[part], key):
            to = z + {"u": 1, "d": -1}.get(link, 0)
            if 0 <= to <= 3:
                busy[z, link] = max(busy.get((z, link), 0), now) + SIZES[part]
                heapq.heappush(here, (busy[z, link] + LATENCY, to, part, there))
    return sorted((sum(t) / len(t), *at) for at, t in times.items())


def turn_back(dkv_ref, cos_ref, sin_ref, dk_u, dv_u):
    n = TWO * TWO * BLK
    for i in range(TWO):
        for j in range(TWO):
            cos_t, sin_t = (jnp.hstack([t, t * sign]) for t, sign in ((cos_ref[i, j].T, 1), (sin_ref[i, j].T, -1)))
            dk = dkv_ref[pl.ds((i * TWO + j) * BLK, BLK)] * ATTN_SCALE
            dk_u[i, j] = (dk * cos_t + pltpu.roll(dk, HEAD_DIM // TWO, 1) * sin_t).astype(BF16)
    dv_u[...] = dkv_ref[pl.ds(n, n)].astype(BF16).reshape(dv_u.shape)


def wkv_terms(h_own, dk_u, dv_u, outs):
    d_out = jnp.hstack([r[...].reshape(-1, HEAD_DIM) for r in (dk_u, dv_u)])
    for out, half in outs:

        @pl.loop(0, FOUR)
        def _(zz, out=out, half=half):
            h = h_own[:, :, :, aligned(half * FOUR + zz)].reshape(-1, BLK)
            out[zz] = dot(h, d_out, (0,), (0,)).reshape(out.shape[1:])


def gather_kernel(*refs):
    take = taker(refs)
    wo_ref, wq_ref, dkv_ref, cos_ref, sin_ref, h_ref = take(6)
    grad_ins, outs, (dx_ref, dgain_ref) = take(6), take(FOUR), take(TWO)
    own_sem, send_sem, come_sem, core_sem, put_sem, all_terms, g_s, g_r = take(8)
    terms, wkv_own, wkv_ref, h_own, dk_u, dv_u, *stores = take(10)
    buffers, sems, refs = take(FOUR), take(7), take(len(refs))
    me = lax.axis_index("cp")
    z, y, x, core = place(me)
    line = Line(me)
    to = {"x": dev(z, y, 1 - x, core), "y": dev(z, 1 - y, x, core), "u": line.next[1], "d": line.next[-1]}
    partner = dev(z, y, x, 1 - core)
    others = [(i, me ^ i) for i in range(1, all_terms.shape[0])]
    meet([d for _, d in others])
    load_h = pltpu.make_async_copy(h_ref, h_own, own_sem.at[0])
    load_h.start()
    wkv = PairSum(me, "core", 1, wkv_ref, wkv_own, buffers, [r.at[0] for r in sems])

    def windows(part, zz, yy, xx, cc):
        chip = (TWO * zz + yy) * TWO + xx
        wide, narrow = wq_ref.shape[1], wkv_own.shape[1] // TWO
        wo_at = ((xx * TWO + cc) * N_PAIRS + chip // TWO) * wo_ref.shape[0]
        wq_at = (cc * N_PAIRS + chip // TWO) * wq_ref.shape[0]
        if part == 3:
            for i, (store, out) in enumerate(zip(stores[TWO:], outs[TWO:])):
                window = out.at[pl.ds(wq_at, wkv_own.shape[0]), pl.ds(xx * narrow, narrow)]
                yield wkv_own.at[:, head_slice(i)], store.at[chip], window
            return

        def cut(ref, cuts):
            first, last = (c * ref.shape[0] // 8 for c in cuts[part : part + TWO])
            return first, last - first

        at, rows = cut(wo_ref, WO_CUTS)
        here = pl.ds(at, rows)
        yield wo_ref.at[here], stores[0].at[chip, here], outs[0].at[pl.ds(wo_at + at, rows)]
        at, rows = cut(wq_ref, WQ_CUTS)
        here = pl.ds(at, rows)
        yield wq_ref.at[here], stores[1].at[chip, here], outs[1].at[pl.ds(wq_at + at, rows), pl.ds(xx * wide, wide)]

    def block(part, key):
        dz, ry, rx = key
        return windows(part, z + dz, 1 - y if ry else y, 1 - x if rx else x, core)

    def index(part, key):
        return (part, key[0] + 3) + key[1:]

    def send(part, key, link, there):
        sent = send_sem.at[index(part, key) + (LINKS.find(link or "-") + 1,)]
        for shard, store, window in block(part, key):
            src = store if any(key) else shard
            if link:
                remote(src, store, sent, come_sem.at[index(part, there)], to[link]).start()
            else:
                remote(src, window, sent, core_sem.at[index(part, key)], partner).start()
                pltpu.make_async_copy(src, window, put_sem.at[index(part, key)]).start()

    def whole(part, send, arrive):
        size = sum(shard.size for shard, _, _ in block(part, HERE)) // outs[0].shape[1]
        dst = outs[0].at[pl.ds(0, size)]
        return remote(dst, dst, send, arrive, me)

    def when(on, do):
        pl.when(on)(do)

    def each_way(part, key):
        held = line.held(key[0])
        yield None, key, held
        for link, there in onward(ORDERS[part], key):
            inside = {"u": line.inside[1], "d": line.inside[-1]}.get(link)
            yield link, there, held if inside is None else jnp.logical_and(held, inside)

    def pass_on(part, key):
        for link, there, on in each_way(part, key):
            when(on, functools.partial(send, part, key, link, there))

    def term_copy(i, d):
        return remote(terms, all_terms.at[i], g_s.at[i], g_r.at[i], d)

    def tile(t):
        job.tile(t)
        if t == job.tiles - 1:
            for i, d in others:
                term_copy(i, d).start()

    def sum_step(h):
        wkv.step(0, h)

    steps = [(TILES_FROM + t * TILE_EVERY, functools.partial(tile, t)) for t in range(HiddenGradient.tiles)]
    steps += [(at, functools.partial(sum_step, h)) for h, at in enumerate(SUM_AT)]
    steps.sort(key=lambda s: s[0])
    events = arrivals()
    for part in range(3):
        pass_on(part, HERE)
    turn_back(dkv_ref, cos_ref, sin_ref, dk_u, dv_u)
    job = HiddenGradient(me, dk_u, dv_u, grad_ins, (dx_ref, terms), refs)
    load_h.wait()
    wkv_terms(h_own, dk_u, dv_u, ((wkv_ref, 1 - core), (buffers[0], core)))
    wkv.begin(0)
    wkv.loaded(0)
    for now, part, key in events:
        while steps and steps[0][0] <= now:
            steps.pop(0)[1]()
        if any(key):
            arrive = come_sem.at[index(part, key)]
            when(line.held(key[0]), whole(part, own_sem.at[0], arrive).wait_recv)
            pass_on(part, key)
        elif part == 3:
            pass_on(part, key)
    total_gain = terms[...]
    for i, d in others:
        term_copy(i, d).wait_recv()
        total_gain += all_terms[i]
    dgain_ref[...] = total_gain
    for i, d in others:
        term_copy(i, d).wait_send()
    for _, part, key in events:
        for sem in (core_sem, put_sem):
            when(line.held(key[0]), whole(part, own_sem.at[0], sem.at[index(part, key)]).wait_recv)
        for link, there, on in each_way(part, key):
            sent = send_sem.at[index(part, key) + (LINKS.find(link or "-") + 1,)]
            when(on, whole(part, sent, own_sem.at[0]).wait_send)
    wkv.wait_send(0)
    job.finish()


def gather_all(wo, wq, dkv, cos_f, sin_f, h_u, part, w_k, w_v, x, dy, gain, shapes):
    dma = pltpu.SemaphoreType.DMA
    vmem, hbm = pl.BlockSpec(memory_space=pltpu.VMEM), pl.BlockSpec(memory_space=pl.ANY)
    block = w_k.shape[0] // TWO // N_PAIRS, w_k.shape[1]
    parts = len(ORDERS)
    keys = (parts, 7, TWO, TWO)
    terms = 1, x.shape[1]
    scratch = [dma((1,)), dma(keys + (len(LINKS) + 1,)), dma(keys), dma(keys), dma(keys)]
    scratch += [pltpu.VMEM((32,) + terms, F32), dma((32,)), dma((32,)), pltpu.VMEM(terms, F32), pltpu.VMEM(block, F32)]
    scratch += [pltpu.VMEM((FOUR, TWO) + block, F32), pltpu.VMEM(h_u.shape, BF16)]
    scratch += [pltpu.VMEM((TWO, TWO, BLK, HEAD_DIM), BF16)] * TWO
    chips = (TWO * N_PAIRS,)
    scratch += [pltpu.VMEM(chips + b, F32) for b in (wo.shape, wq.shape) + ((block[0], HEAD_DIM),) * TWO]
    return pl.pallas_call(
        gather_kernel,
        name="gather_all",
        out_shape=[jax.ShapeDtypeStruct(s, F32) for s in shapes]
        + [jax.ShapeDtypeStruct(x.shape, BF16), jax.ShapeDtypeStruct(terms, F32)],
        in_specs=[vmem] * 5 + [hbm] + [vmem] * 6,
        out_specs=[hbm] * len(shapes) + [vmem] * TWO,
        scratch_shapes=scratch + PairSum.scratch("core", block) + PairSum.sems(1, 1) + HiddenGradient.scratch(x),
        compiler_params=params(63, collective_id=0),
        cost_estimate=cost(1, 76),
    )(wo, wq, dkv, cos_f, sin_f, h_u, part, w_k, w_v, x, dy, gain)


def perm(x, pairs):
    return lax.ppermute(x, "cp", pairs)


def flip_pairs(d):
    return [(r, r ^ d) for r in range(32)]


def solution(mesh):
    def local_step(hidden, grad_out, positions, seg_ids, w_q, w_k, w_v, w_o, norm_gain):
        n_batch, n_tok, d_model = hidden.shape
        n_rows = n_batch * n_tok
        wide = N_HEADS * HEAD_DIM
        me = lax.axis_index("cp")
        z, y, x, core = place(me)
        quad, pair = me % FOUR, me // FOUR
        relations = range(FOUR)

        def swap(pieces):
            return [perm(p, flip_pairs(d)) if d else p for d, p in enumerate(pieces)]

        gain = norm_gain.astype(F32)
        cos_t, sin_t = rope_tables(positions.reshape(n_rows))
        cos_f, sin_f = jnp.hstack([cos_t, cos_t]), jnp.hstack([-sin_t, sin_t])
        dy_flat = grad_out.reshape(n_rows, d_model)
        normed, kv_home = project(hidden.reshape(n_rows, d_model), gain[NEW], w_k, w_v, cos_f, sin_f)
        pos = jnp.pad(positions.reshape(TWO, TWO, n_tok), ((0, 0), (0, 6), (0, 0)))
        kv_home = kv_home.reshape((TWO,) * 5 + (CHUNK, HEAD_DIM))
        kv_all, q_u, do_u, pos_u, *dy_rows = exchange(kv_home, normed, dy_flat, pos, cos_f, sin_f, w_q, w_o)
        pos_u = pos_u[:, :TWO].reshape((FOUR, TWO, TWO, CHUNK)).transpose(1, TWO, 0, 3).reshape(TWO, TWO, BLK)
        dy_rows = [a.reshape(TWO, TWO, CHUNK, d_model) for a in dy_rows]
        dy_pieces = swap([dy_rows[d % TWO] for d in relations])

        member = quad ^ jnp.arange(FOUR)
        front, back = ((m[:, NEW] * CHUNK + jnp.arange(CHUNK)[NEW]).reshape(BLK) for m in (member, 3 - member))
        offsets = jnp.stack([front, back]).astype(jnp.int32)
        own_super = jnp.stack([pair, N_SUPER - 1 - pair]).astype(jnp.int32)
        q_index = own_super[:, NEW] * BLK + offsets
        start = q_index[NEW] - pos_u
        tab = jnp.concatenate(
            [own_super, (jnp.min(start, axis=-1) // BLK).reshape(-1), jnp.max(start, axis=-1).reshape(-1)]
        )
        start_r = start[:, :, NEW, :]
        q_index_r = jnp.broadcast_to(q_index[NEW, :, NEW, :], start_r.shape)
        cos_u, sin_u = rope_tables(pos_u)
        cos_ut, sin_ut = jnp.swapaxes(cos_u, TWO, 3), jnp.swapaxes(sin_u, TWO, 3)

        koff = offsets[:, NEW]
        attn_u, lse = flash_fwd(tab, q_u, kv_all, start_r, q_index_r, koff)

        wo_keep, wo_away = wo_terms(attn_u, dy_pieces)
        wo_come = perm(wo_away, flip_pairs(FOUR))
        do_u, wo_keep = lax.optimization_barrier((do_u, wo_keep))
        dq_u, dkv = flash_bwd(tab, q_u, do_u, attn_u, kv_all, lse, start_r, q_index_r, koff, cos_ut, sin_ut)
        wo_sum = wo_keep + wo_come

        x_flat = hidden.reshape(n_rows, d_model)
        wo_own, dkv_own, wq_own, block_out, d_part, h_u = reduce_pairs(
            [wo_sum, dkv.reshape(FOUR, TWO, -1, HEAD_DIM)],
            [wo_sum.shape[1:], (dkv.size // N_PAIRS // HEAD_DIM, HEAD_DIM), (d_model // TWO // N_PAIRS, wide)],
            (TWO, 8, 8),
            ("z", "", "core"),
            TWO,
            Products,
            (attn_u, dq_u, x_flat, normed.reshape((TWO,) * 3 + (CHUNK, d_model)), w_o, w_q),
        )
        grad_wo, grad_wq, grad_wk, grad_wv, grad_x, d_gain = gather_all(
            wo_own,
            wq_own,
            dkv_own,
            cos_ut,
            sin_ut,
            h_u,
            d_part,
            w_k,
            w_v,
            x_flat,
            dy_flat,
            gain[NEW],
            [w_o.shape, w_q.shape, w_k.shape, w_v.shape],
        )
        block_out, grad_x = (a.reshape(hidden.shape) for a in (block_out, grad_x))
        return block_out, grad_x, grad_wq, grad_wk, grad_wv, grad_wo, d_gain.reshape(d_model)

    seq_spec = P(None, "cp", None)
    tok_spec = P(None, "cp")
    full_spec = P()
    return jax.shard_map(
        local_step,
        mesh=mesh,
        in_specs=(seq_spec, seq_spec, tok_spec, tok_spec, full_spec, full_spec, full_spec, full_spec, full_spec),
        out_specs=(seq_spec, seq_spec, full_spec, full_spec, full_spec, full_spec, full_spec),
        check_vma=False,
    )
```

```python
import functools
import heapq
import itertools

import jax
import jax.numpy as jnp
from jax import lax
from jax.experimental import pallas as pl
from jax.experimental.pallas import tpu as pltpu
from jax.sharding import PartitionSpec as P

HEAD_DIM = 128
NORM_EPS = 1e-5
ROPE_BASE = 500000.0
NEG_BIG = -1e30
LOG2E = 1.4426950408889634
ATTN_SCALE = HEAD_DIM**-0.5
EXP2_SCALE = ATTN_SCALE * LOG2E
CHUNK = 64
TWO = 2
FOUR = 4
NEW = jnp.newaxis
BLK = 4 * CHUNK
N_HEADS = 8
N_PAIRS = 8
N_SUPER = 2 * N_PAIRS
MESH = pl.DeviceIdType.MESH
ONE = pl.Squeezed()
GROUP = 4
MADE_AT = 5
PRODUCTS_AT = 7, 9
F32 = jnp.float32
BF16 = jnp.bfloat16

T_SQ, T_LO, T_MX = 0, 2, 6


def rope_tables(positions):
    inv_freq = ROPE_BASE ** (-jnp.arange(0, HEAD_DIM, TWO).astype(F32) / HEAD_DIM)
    angles = positions.astype(F32)[..., None] * inv_freq
    return jnp.cos(angles), jnp.sin(angles)


def dot(a, b, ca, cb):
    return lax.dot_general(a, b, ((ca, cb), ((), ())), preferred_element_type=F32)


def cost(gflop, mib):
    return pl.CostEstimate(flops=gflop * 10**9, bytes_accessed=mib << 20, transcendentals=0)


def params(mib, **more):
    return pltpu.CompilerParams(vmem_limit_bytes=mib << 20, **more)


def row_mean(x):
    return jnp.mean(x, axis=-1, keepdims=True)


def head(h):
    return pl.ds(h * HEAD_DIM, HEAD_DIM)


def head_slice(h):
    return slice(h * HEAD_DIM, (h + 1) * HEAD_DIM)


def dot_t(a, b):
    return dot(a, b, (1,), (1,))


def steps(tab, body):
    b, hf = pl.program_id(0), pl.program_id(1)
    own, first, last_start = tab[T_SQ + hf], tab[T_LO + TWO * b + hf], tab[T_MX + TWO * b + hf]

    def step(s, carry):
        late = s >= N_PAIRS
        at = jnp.where(late, N_SUPER - 1 - s, s), late.astype(jnp.int32)
        full = jnp.logical_and(s < own, s * BLK >= last_start)
        pl.when(full)(lambda: body(s, at, False))
        pl.when(jnp.logical_not(full))(lambda: body(s, at, True))
        return carry

    lax.fori_loop(first, own + 1, step, 0)


def down(row, n):
    return jnp.broadcast_to(row, (n, row.shape[-1])).T


def may_use(s, off, st_ref, qi_ref):
    return jnp.logical_and(off >= st_ref[...] - s * BLK, off <= qi_ref[...] - s * BLK)


def fwd_kernel(tab, q_ref, kv_ref, st_ref, qi_ref, ko_ref, o_ref, lse_ref, q_s, acc, m_s, l_s, k_t, bounds):
    m_s[...] = jnp.full_like(m_s, NEG_BIG)
    l_s[...] = jnp.zeros_like(l_s)
    acc[...] = jnp.zeros_like(acc)
    for i, ref in enumerate((st_ref, qi_ref)):
        bounds[i] = down(ref[...], HEAD_DIM)
    for h in range(N_HEADS):
        q_s[pl.ds(h * BLK, BLK)] = q_ref[:, head(h)]

    @pl.when(pl.program_id(1) == 0)
    def _():
        @pl.loop(0, N_PAIRS)
        def _(pair):
            for hk in range(TWO):
                k_t[pair, hk] = kv_ref[pair, 0, hk].T

    def body(s, at, masked):
        pair, hk = at
        v = kv_ref[pair, 1, hk]
        if masked:
            off = ko_ref[hk] + s * BLK
            mask = [
                jnp.logical_and(off[:, lanes] >= bounds[0], off[:, lanes] <= bounds[1])
                for lanes in (slice(HEAD_DIM), slice(HEAD_DIM, BLK))
            ]
            mask = [jnp.concatenate([m, m], axis=0) for m in mask]
        for g in range(N_HEADS // TWO):
            rows = pl.ds(g * TWO * BLK, TWO * BLK)
            sc = jnp.dot(q_s[rows], k_t[pair, hk], preferred_element_type=F32)
            sc = [sc[:, :HEAD_DIM], sc[:, HEAD_DIM:]]
            if masked:
                sc = [jnp.where(m, x, NEG_BIG) for m, x in zip(mask, sc)]
            m_old = m_s[rows]
            m_new = jnp.maximum(m_old, jnp.max(jnp.maximum(*sc), axis=1, keepdims=True))
            alpha = jnp.exp2((m_old - m_new) * EXP2_SCALE)
            p = [jnp.exp2((x - m_new) * EXP2_SCALE) for x in sc]
            m_s[rows] = m_new
            l_s[rows] = l_s[rows] * alpha + (p[0] + p[1])
            p = jnp.hstack([x.astype(BF16) for x in p])
            acc[rows] = acc[rows] * alpha + jnp.dot(p, v, preferred_element_type=F32)

    steps(tab, body)
    for h in range(N_HEADS):
        rows = pl.ds(h * BLK, BLK)
        total = jnp.sum(l_s[rows], axis=1, keepdims=True)
        o_ref[:, head(h)] = (acc[rows] / total).astype(BF16)
        lse_ref[h] = (m_s[rows] * EXP2_SCALE + jnp.log2(total)).T[:1]


def bwd_kernel(tab, q_ref, do_ref, o_ref, kv_ref, lse_ref, st_ref, qi_ref, ko_ref, cos_ref, sin_ref, dq_ref, dkv_ref, *scratch):
    dq_acc, delta, off_s, q_s, do_s, q_t, do_t, p_s, ds_s = scratch
    dq_acc[...] = jnp.zeros_like(dq_acc)
    for h in range(N_HEADS):
        q, do = q_ref[:, head(h)], do_ref[:, head(h)]
        delta[h] = jnp.sum((do.astype(F32) * o_ref[:, head(h)].astype(F32)).T, axis=0, keepdims=True)
        q_s[pl.ds(h * BLK, BLK)], do_s[pl.ds(h * BLK, BLK)] = q, do
        q_t[h], do_t[h] = q.T, do.T

    @pl.when(pl.program_id(1) == 0)
    def _():
        dkv_ref[...] = jnp.zeros_like(dkv_ref)
        for hk in range(TWO):
            off_s[hk] = down(ko_ref[hk], BLK)

    def body(s, at, masked):
        pair, hk = at
        k = kv_ref[pair, 0, hk]
        v = kv_ref[pair, 1, hk]
        k_t = k.T
        mask = may_use(s, off_s[hk], st_ref, qi_ref) if masked else None
        for first in range(0, N_HEADS, GROUP):
            rows = pl.ds(first * BLK, GROUP * BLK)
            for h in range(first, first + GROUP):
                cols = pl.ds(h * BLK, BLK)
                p = jnp.exp2(jnp.dot(k, q_t[h], preferred_element_type=F32) * EXP2_SCALE - lse_ref[h])
                if masked:
                    p = jnp.where(mask, p, 0.0)
                ds = p * (jnp.dot(v, do_t[h], preferred_element_type=F32) - delta[h])
                p_s[:, cols] = p.astype(BF16)
                ds_s[:, cols] = ds.astype(BF16)
            dkv_ref[pair, 0, hk] += jnp.dot(ds_s[:, rows], q_s[rows], preferred_element_type=F32)
            dkv_ref[pair, 1, hk] += jnp.dot(p_s[:, rows], do_s[rows], preferred_element_type=F32)
            dq_acc[:, rows] += jnp.dot(k_t, ds_s[:, rows], preferred_element_type=F32)

    steps(tab, body)
    cos_t, sin_t = cos_ref[...], sin_ref[...]
    half = HEAD_DIM // TWO
    for h in range(N_HEADS):
        cols = pl.ds(h * BLK, BLK)
        a, c = dq_acc[:half, cols] * ATTN_SCALE, dq_acc[half:, cols] * ATTN_SCALE
        lin = jnp.concatenate([a * cos_t + c * sin_t, c * cos_t - a * sin_t], axis=0)
        dq_ref[:, head(h)] = lin.T.astype(BF16)


def attn_specs():
    def at_tile(b, h, t):
        return (b, h) + (0,) * TWO

    def at_row(b, h, t):
        return (0, 0, b) + (0,) * 3

    tile = pl.BlockSpec((ONE, ONE, BLK, N_HEADS * HEAD_DIM), at_tile)
    row = pl.BlockSpec((ONE, ONE, 1, BLK), at_tile)
    stat = pl.BlockSpec((ONE, ONE, N_HEADS, 1, BLK), lambda b, h, t: (b, h) + (0,) * 3)
    rope = pl.BlockSpec((ONE, ONE, HEAD_DIM // TWO, BLK), at_tile)
    kv = pl.BlockSpec((N_PAIRS, TWO, ONE, TWO, BLK, HEAD_DIM), at_row)
    ko = pl.BlockSpec((TWO, 1, BLK), lambda b, h, t: (0,) * 3)
    return tile, row, stat, kv, ko, rope


def flash_fwd(tab, q, kv, start, qidx, koff):
    tile, row, stat, kvs, ko, _ = attn_specs()
    return pl.pallas_call(
        fwd_kernel,
        name="attn_fwd",
        out_shape=(jax.ShapeDtypeStruct(q.shape, BF16), jax.ShapeDtypeStruct((TWO, TWO, N_HEADS, 1, BLK), F32)),
        grid_spec=pltpu.PrefetchScalarGridSpec(
            num_scalar_prefetch=1,
            grid=(TWO, TWO),
            in_specs=[tile, kvs, row, row, ko],
            out_specs=[tile, stat],
            scratch_shapes=[pltpu.VMEM((N_HEADS * BLK, HEAD_DIM), t) for t in (BF16, F32, F32, F32)]
            + [pltpu.VMEM((N_PAIRS, TWO, HEAD_DIM, BLK), BF16), pltpu.VMEM((TWO, BLK, HEAD_DIM), jnp.int32)],
        ),
        compiler_params=params(63),
        cost_estimate=cost(20, 16),
    )(tab, q, kv, start, qidx, koff)


def flash_bwd(tab, q, do, o, kv, lse, start, qidx, koff, cos_t, sin_t):
    tile, row, stat, kvs, ko, rope = attn_specs()
    return pl.pallas_call(
        bwd_kernel,
        name="attn_bwd",
        out_shape=(
            jax.ShapeDtypeStruct(q.shape, BF16),
            jax.ShapeDtypeStruct(kv.shape, F32),
        ),
        grid_spec=pltpu.PrefetchScalarGridSpec(
            num_scalar_prefetch=1,
            grid=(TWO, TWO),
            in_specs=[tile, tile, tile, kvs, stat, row, row, ko, rope, rope],
            out_specs=[tile, kvs],
            scratch_shapes=[pltpu.VMEM((HEAD_DIM, N_HEADS * BLK), F32), pltpu.VMEM((N_HEADS, 1, BLK), F32)]
            + [pltpu.VMEM((TWO, BLK, BLK), jnp.int32)]
            + [pltpu.VMEM((N_HEADS * BLK, HEAD_DIM), BF16)] * TWO
            + [pltpu.VMEM((N_HEADS, HEAD_DIM, BLK), BF16)] * TWO
            + [pltpu.VMEM((BLK, N_HEADS * BLK), BF16)] * TWO,
        ),
        compiler_params=params(63),
        cost_estimate=cost(50, 32),
    )(tab, q, do, o, kv, lse, start, qidx, koff, cos_t, sin_t)


def turn(x, cos_ref, sin_ref):
    return x * cos_ref[...] + pltpu.roll(x, HEAD_DIM // TWO, 1) * sin_ref[...]


def first_kernel(x_ref, g_ref, wk_ref, wv_ref, cos_ref, sin_ref, h_ref, kv_ref):
    x = x_ref[...].astype(F32)
    h = (x * lax.rsqrt(row_mean(x * x) + NORM_EPS) * g_ref[...]).astype(BF16)
    h_ref[...] = h
    k = jnp.dot(h, wk_ref[...], preferred_element_type=F32)
    v = jnp.dot(h, wv_ref[...], preferred_element_type=F32)
    n = kv_ref.shape[3]
    for i in range(TWO):
        for j, val in enumerate((turn(k[:, head_slice(i)], cos_ref, sin_ref), v[:, head_slice(i)])):
            for c in range(TWO):
                kv_ref[i, c, j] = val[c * n : (c + 1) * n].astype(BF16)


def project(x, gain, w_k, w_v, cos_f, sin_f):
    n = x.shape[0] // TWO
    return pl.pallas_call(
        first_kernel,
        name="norm_kv",
        out_shape=(jax.ShapeDtypeStruct(x.shape, BF16), jax.ShapeDtypeStruct((TWO,) * 3 + (n, HEAD_DIM), BF16)),
        compiler_params=params(20),
        cost_estimate=cost(TWO, 7),
    )(x, gain, w_k, w_v, cos_f, sin_f)


def place(me):
    return me // 8, lax.rem(me // FOUR, TWO), lax.rem(me // TWO, TWO), lax.rem(me, TWO)


def dev(z, y, x, core):
    return ((z * TWO + y) * TWO + x) * TWO + core


def z_peers(z):
    return [(k, lax.rem(z + k, FOUR)) for k in (1, TWO, 3)]


def meet(peers):
    barrier = pltpu.get_barrier_semaphore()
    for d in peers:
        pl.semaphore_signal(barrier, device_id=(d,), device_id_type=MESH)
    pl.semaphore_wait(barrier, len(peers))


def remote(src, dst, send, arrive, to):
    return pltpu.make_async_remote_copy(
        src_ref=src, dst_ref=dst, send_sem=send, recv_sem=arrive, device_id=(to,), device_id_type=MESH
    )


class Line:
    order = (0, 1, -1, TWO, -TWO, 3, -3)

    def __init__(self, me):
        self.z, y, x, core = place(me)
        self.next = {1: dev(self.z + 1, y, x, core), -1: dev(self.z - 1, y, x, core)}
        self.inside = {1: self.z < 3, -1: self.z > 0}

    def held(self, dz):
        return jnp.logical_and(self.z + dz >= 0, self.z + dz <= 3)

    def ways(self, dz):
        for d in self.next:
            if d * dz <= 0:
                yield d, self.inside[d] if dz == 0 else jnp.logical_and(self.inside[d], self.held(dz))


def tiled(n, fetch, use, first=0):
    fetch(first, 0).start()

    @pl.loop(0, n)
    def _(t):
        slot = lax.rem(t, TWO)
        fetch(first + t, slot).wait()

        @pl.when(t + 1 < n)
        def _():
            fetch(first + t + 1, 1 - slot).start()

        use(first + t, slot)


def aligned(t, size=BLK):
    return pl.ds(pl.multiple_of(t * size, size), size)


def exchange_kernel(*refs):
    take = taker(refs)
    kv_ref, h_ref, dy_ref, pos_ref, cos_ref, sin_ref, wq_ref, wo_ref, kv_all, q_u, do_u, pos_u, *dy_rows = take(14)
    own_sem, quad_s, quad_r, z_s, z_r, y_s, y_r, q_home, do_home, wq_buf, wo_buf, w_sem, dy_sem = take(len(refs))
    me = lax.axis_index("cp")
    z, y, x, core = place(me)
    quad, line = quad_of(me), Line(me)
    across = dev(z, 1 - y, x, core)
    meet(quad[1:] + [across] + [dev(zz, y, x, core) for _, zz in z_peers(z)])

    def source(a, d):
        xx, cc = 1 - x if d // TWO else x, 1 - core if d % TWO else core
        return pos_ref.at[cc] if a == 3 else (kv_ref, q_home, do_home)[a].at[xx, cc]

    def target(a, d):
        if a == 3:
            return pos_u.at[d]
        tok = pl.ds(d * CHUNK, CHUNK)
        return kv_all.at[me // FOUR, :, :, :, tok] if a == 0 else (q_u, do_u)[a - 1].at[:, :, tok]

    def quad_copy(a, d):
        return remote(source(a, d), target(a, d), quad_s.at[a, d], quad_r.at[a, d], quad[d])

    def own_copy(a):
        return pltpu.make_async_copy(source(a, 0), target(a, 0), own_sem.at[a])

    def z_copy(part, dz, d):
        block = kv_all.at[TWO * (z + dz) + y, part]
        return remote(block, block, z_s.at[part, (d + 1) // TWO, dz + 3], z_r.at[part, dz - d + 3], line.next[d])

    def y_copy(part, dz, yy=y):
        block = kv_all.at[TWO * (z + dz) + yy, part]
        return remote(block, block, y_s.at[part, dz + 3], y_r.at[part, dz + 3], across)

    parts = range(TWO)
    moves = [(part, dz) for dz in line.order for part in parts]

    def pass_on(count):
        for part, dz in [moves.pop(0) for _ in range(count)]:
            if dz:
                block = kv_all.at[TWO * (z + dz) + y, part]
                arrival = remote(block, block, own_sem.at[0], z_r.at[part, dz + 3], me)
                pl.when(line.held(dz))(arrival.wait_recv)
            for d, on in line.ways(dz):
                pl.when(on)(z_copy(part, dz, d).start)
            pl.when(line.held(dz))(y_copy(part, dz).start)

    n = h_ref.shape[1] // BLK // TWO

    def fetch_q(t, slot):
        return pltpu.make_async_copy(wq_ref.at[:, aligned(t)], wq_buf.at[slot], w_sem.at[0, slot])

    def fetch_o(t, slot):
        return pltpu.make_async_copy(wo_ref.at[aligned(t)], wo_buf.at[slot], w_sem.at[1, slot])

    def put(home, t, val):
        home[t // n, :, :, :, :, aligned(lax.rem(t, n))] = val.astype(BF16).reshape(home.shape[1:-1] + (BLK,))

    def query(t, slot):
        q = jnp.dot(h_ref[...], wq_buf[slot], preferred_element_type=F32)
        put(q_home, t, jnp.hstack([turn(q[:, head_slice(j)], cos_ref, sin_ref) for j in range(BLK // HEAD_DIM)]))

    def pull(t, slot):
        put(do_home, t, dot_t(dy_ref[...], wo_buf[slot]))

    all_moves = list(moves)
    half = dy_ref.shape[0] // TWO
    for i, out in enumerate(dy_rows):
        pltpu.make_async_copy(dy_ref.at[aligned(core if i == 0 else 1 - core, half)], out, dy_sem.at[i]).start()
    for a in (0, 3):
        for d in (1, TWO, 3):
            quad_copy(a, d).start()
        own_copy(a).start()
    for a, (fetch, use) in enumerate(((fetch_q, query), (fetch_o, pull)), 1):
        for near in range(TWO):
            tiled(n, fetch, use, n * (x if near else 1 - x))
            for d in range(TWO):
                if d or not near:
                    quad_copy(a, d if near else d + TWO).start()
            if near:
                own_copy(a).start()
            if len(moves) == len(all_moves):
                own_copy(0).wait()
                for d in (1, TWO, 3):
                    quad_copy(0, d).wait_recv()
            pass_on(TWO)
    pass_on(len(moves))
    for part, dz in all_moves:
        for d, on in line.ways(dz):
            pl.when(on)(z_copy(part, dz, d).wait_send)
        pl.when(line.held(dz))(y_copy(part, dz, 1 - y).wait_recv)
        pl.when(line.held(dz))(y_copy(part, dz).wait_send)
    for a in range(FOUR):
        for d in (1, TWO, 3):
            quad_copy(a, d).wait_send()
            if a > 0:
                quad_copy(a, d).wait_recv()
    for a in (1, TWO, 3):
        own_copy(a).wait()
    for i, out in enumerate(dy_rows):
        pltpu.make_async_copy(dy_ref.at[aligned(core if i == 0 else 1 - core, half)], out, dy_sem.at[i]).wait()


def exchange(kv, h, dy, pos, cos_f, sin_f, w_q, w_o):
    dma = pltpu.SemaphoreType.DMA
    vmem, hbm = pl.BlockSpec(memory_space=pltpu.VMEM), pl.BlockSpec(memory_space=pl.ANY)
    wide = w_q.shape[1] // TWO
    unit = jax.ShapeDtypeStruct((TWO, TWO, BLK, wide), BF16)
    pos_quad = jax.ShapeDtypeStruct((FOUR,) + pos.shape[1:], pos.dtype)
    dy_half = jax.ShapeDtypeStruct((dy.shape[0] // TWO, dy.shape[1]), BF16)
    home = pltpu.VMEM((TWO,) * FOUR + (CHUNK, wide), BF16)
    sems = [dma((FOUR,))] + [dma((FOUR, FOUR))] * TWO + [dma((TWO, TWO, 7))] + [dma((TWO, 7))] * 3
    bufs = [pltpu.VMEM((TWO,) + b, BF16) for b in ((w_q.shape[0], BLK), (BLK, w_o.shape[1]))]
    return pl.pallas_call(
        exchange_kernel,
        name="exchange",
        out_shape=(jax.ShapeDtypeStruct((N_PAIRS,) + (TWO,) * 3 + (BLK, HEAD_DIM), BF16), unit, unit, pos_quad, dy_half, dy_half),
        in_specs=[vmem] * 6 + [hbm] * TWO,
        out_specs=[hbm] * 6,
        scratch_shapes=sems + [home, home] + bufs + [dma((TWO, TWO)), dma((TWO,))],
        compiler_params=params(63, collective_id=1),
        cost_estimate=cost(1, 20),
    )(kv, h, dy, pos, cos_f, sin_f, w_q, w_o)


def taker(refs):
    rest = iter(refs)
    return lambda count: list(itertools.islice(rest, count))


def wo_kernel(*refs):
    take = taker(refs)
    o_ref, *pieces = take(5)
    keep, away, dy_u, o_t, terms, came, load_sem, core_s, core_r = take(len(refs))
    me = lax.axis_index("cp")
    _, y, _, core = place(me)
    meet(quad_of(me)[1:TWO])
    loads = [
        pltpu.make_async_copy(src, dy_u.at[:, :, pl.ds(d * CHUNK, CHUNK)], load_sem.at[d])
        for d, src in enumerate(pieces)
    ]
    for c in loads:
        c.start()
    for h in range(N_HEADS):
        o_t[head(h)] = o_ref[:, :, :, head(h)].reshape(-1, HEAD_DIM).T
    for c in loads:
        c.wait()
    half, tiles = terms.shape[1], terms.shape[TWO] // BLK

    def swap(t):
        return remote(terms.at[0, :, aligned(t)], came.at[:, aligned(t)], core_s.at[t], core_r.at[t], quad_of(me)[1])

    def half_terms(i, to, then):
        @pl.loop(0, tiles)
        def _(t):
            dy = dy_u[:, :, :, aligned(t)].reshape(-1, BLK)
            terms[to, :, aligned(t)] = jnp.dot(o_t[aligned(i, half)], dy, preferred_element_type=F32)
            then(t)

    half_terms(1 - core, 0, lambda t: swap(t).start())
    half_terms(core, 1, lambda t: swap(t).wait_recv())
    rows = keep.shape[1]
    for zz in range(FOUR):
        for out, yy in ((keep, y), (away, 1 - y)):
            at = aligned(TWO * zz + yy, rows)
            out[zz] = terms[1, at] + came[at]
    for t in range(tiles):
        swap(t).wait_send()


def wo_terms(o, pieces):
    dma = pltpu.SemaphoreType.DMA
    vmem, hbm = pl.BlockSpec(memory_space=pltpu.VMEM), pl.BlockSpec(memory_space=pl.ANY)
    n, d, wide = o.shape[0] * o.shape[1] * o.shape[TWO], pieces[0].shape[-1], o.shape[-1]
    half = wide // TWO
    return pl.pallas_call(
        wo_kernel,
        name="wo_terms",
        out_shape=[jax.ShapeDtypeStruct((FOUR, half // N_PAIRS, d), F32)] * TWO,
        in_specs=[vmem] + [hbm] * FOUR,
        out_specs=[vmem] * TWO,
        scratch_shapes=[pltpu.VMEM((TWO, TWO, BLK, d), BF16), pltpu.VMEM((wide, n), BF16)]
        + [pltpu.VMEM((TWO, half, d), F32), pltpu.VMEM((half, d), F32), dma((FOUR,)), dma((d // BLK,)), dma((d // BLK,))],
        compiler_params=params(63, collective_id=3),
        cost_estimate=cost(FOUR, 20),
    )(o, *pieces)


class PairSum:
    def __init__(self, me, kind, cut, src, out, buffers, sems):
        self.me, self.kind, self.src, self.out = me, kind, src, out
        self.size = out.shape[0] // cut
        self.own, self.from_core, self.from_y, self.from_z = buffers
        self.load_sem, self.core_s, self.core_r, self.y_s, self.y_r, self.z_s, self.z_r = sems
        self.z, self.y, x, core = place(me)
        self.partner = dev(self.z, self.y, x, 1 - core)
        self.across = dev(self.z, 1 - self.y, x, core)
        self.next_z = dev(self.z + 1, self.y, x, core), dev(self.z - 1, self.y, x, core)

    def rows(self, j):
        return pl.ds(j * self.size, self.size)

    def mine(self, j, zz):
        at = self.rows(j)
        return self.own.at[zz, self.y, at] if self.kind == "core" else self.own.at[zz, at]

    def loads(self, j):
        at = self.rows(j)
        if self.kind == "z":
            pairs = zip(self.src, (self.own, self.from_y))
            return [pltpu.make_async_copy(a.at[:, at], b.at[:, at], s.at[j]) for (a, b), s in zip(pairs, (self.load_sem, self.y_r))]
        return [pltpu.make_async_copy(self.src.at[:, self.y, at], self.own.at[:, at], self.load_sem.at[j])]

    def core_copy(self, j):
        src, dst = (r.at[:, :, self.rows(j)] for r in (self.src, self.from_core))
        return remote(src, dst, self.core_s.at[j], self.core_r.at[j], self.partner)

    def y_copy(self, j):
        src = self.own if self.kind == "core" else self.src
        at = self.rows(j)
        return remote(src.at[:, 1 - self.y, at], self.from_y.at[:, at], self.y_s.at[j], self.y_r.at[j], self.across)

    def z_copy(self, j, way, zz, to):
        at = way, zz + way - 1
        return remote(self.mine(j, zz), self.from_z.at[*at, self.rows(j)], self.z_s.at[j, *at], self.z_r.at[j, *at], to)

    def begin(self, j):
        if self.kind == "core":
            self.core_copy(j).start()
            return
        for c in self.loads(j):
            c.start()
        if not self.kind:
            self.y_copy(j).start()

    def loaded(self, j):
        if self.kind != "core":
            for c in self.loads(j):
                c.wait()
        else:
            self.core_copy(j).wait_recv()
            at = self.rows(j)
            for zz in range(FOUR):
                self.own[zz, :, at] += self.from_core[zz, :, at]
            self.y_copy(j).start()
        if self.kind == "z":
            self.add_y(j)
            self.hop(j, 0)

    def add_y(self, j):
        for zz in range(FOUR):
            self.mine(j, zz)[...] += self.from_y[zz, self.rows(j)]

    def relay(self, j, way, zz, add):
        if add:
            self.z_copy(j, way, zz, self.me).wait_recv()
            self.mine(j, zz)[...] += self.from_z[way, zz + way - 1, self.rows(j)]
        self.z_copy(j, way, zz, self.next_z[way]).start()

    def hop(self, j, h):
        @pl.when(self.z == h)
        def _():
            for zz in range(3, h, -1):
                self.relay(j, 0, zz, h > 0)

        @pl.when(self.z == 3 - h)
        def _():
            for zz in range(3 - h):
                self.relay(j, 1, zz, h > 0)

    def step(self, j, h):
        if h == 0 and self.kind != "z":
            self.y_copy(j).wait_recv()
            self.add_y(j)
            self.hop(j, 0)
        elif 0 < h < 3:
            self.hop(j, h)
        elif h == 3:
            at = self.rows(j)
            self.out[at] = self.mine(j, self.z)[...]
            for way, on in enumerate((self.z > 0, self.z < 3)):

                @pl.when(on)
                def _(way=way):
                    self.z_copy(j, way, self.z, self.me).wait_recv()
                    self.out[at] += self.from_z[way, self.z + way - 1, at]

    def wait_send(self, j):
        if self.kind == "core":
            self.core_copy(j).wait_send()
        if self.kind != "z":
            self.y_copy(j).wait_send()
        for zz in range(FOUR):
            if zz > 0:
                pl.when(self.z < zz)(self.z_copy(j, 0, zz, self.next_z[0]).wait_send)
            if zz < 3:
                pl.when(self.z > zz)(self.z_copy(j, 1, zz, self.next_z[1]).wait_send)

    @staticmethod
    def scratch(kind, block):
        unused = pltpu.VMEM((8, HEAD_DIM), F32)
        own = pltpu.VMEM(((FOUR, TWO) if kind == "core" else (FOUR,)) + block, F32)
        from_y = pltpu.VMEM((FOUR,) + block, F32)
        return [own, own if kind == "core" else unused, from_y, pltpu.VMEM((TWO, 3) + block, F32)]

    @staticmethod
    def sems(*dims):
        dma = pltpu.SemaphoreType.DMA
        return [dma(dims)] * 5 + [dma(dims + (TWO, 3))] * TWO


def reduce_kernel(cuts, kinds, work, *refs):
    n = len(cuts)

    take = taker(refs)
    ins = [take(TWO) if k == "z" else take(1)[0] for k in kinds[:-1]]
    more_in, outs, more_out, made = take(work.ins), take(n), take(work.outs), take(1)
    buffers, sems = [take(FOUR) for _ in kinds], take(7)
    me = lax.axis_index("cp")
    z, y, x, core = place(me)
    meet(quad_of(me)[1:] + [dev(z, 1 - y, x, core)] + [dev(zz, y, x, core) for _, zz in z_peers(z)])
    job = work(me, more_in, more_out, take(len(refs)))
    sums = [PairSum(me, *a, [r.at[i] for r in sems]) for i, a in enumerate(zip(kinds, cuts, ins + made, outs, buffers))]
    pieces = [(s, j) for s, cut in zip(sums, cuts) for j in range(cut)]
    early, late = pieces[: -cuts[-1]], pieces[-cuts[-1] :]
    for s, j in early:
        s.begin(j)
    for s, j in early:
        s.loaded(j)
    for t in range(len(pieces) + 3):
        if t == MADE_AT:
            job.wq_terms(sums[-1].own, made[0])
            for s, j in late:
                s.begin(j)
        if t == MADE_AT + 1:
            for s, j in late:
                s.loaded(j)
        for h in range(FOUR):
            if 0 <= t - h < len(pieces):
                s, j = pieces[t - h]
                s.step(j, h)
        job.step(t)
    for s, j in pieces:
        s.wait_send(j)
    job.finish()


def quad_of(me):
    z, y, x, core = place(me)
    return [dev(z, y, 1 - x if d // TWO else x, 1 - core if d % TWO else core) for d in range(FOUR)]


class Home:
    def __init__(self, me, src, out, own_sem, send, arrive):
        _, _, x, core = place(me)
        w = src.shape[-1]
        to = out.at[core, :, :, :, pl.ds(x * w, w)]

        def piece(d):
            return src.at[:, :, pl.ds(d * CHUNK, CHUNK)]

        self.own = pltpu.make_async_copy(piece(0), to, own_sem)
        self.copies = [remote(piece(d), to, send.at[d], arrive.at[d], quad_of(me)[d]) for d in (1, TWO, 3)]

    def start(self):
        self.own.start()
        for c in self.copies:
            c.start()

    def wait_recv(self):
        self.own.wait()
        for c in self.copies:
            c.wait_recv()

    def wait_send(self):
        for c in self.copies:
            c.wait_send()


class Products:
    ins, outs = 6, 3

    def __init__(self, me, ins, outs, scratch):
        attn, self.dq, hidden, normed, self.w_o, self.w_q = ins
        self.block_out, self.d_part, self.h_u = outs
        self.attn_home, self.dq_home, self.buf_o, self.buf_q, stage, self.h_buf, *sems = scratch
        self.w_sem, self.load_sem, own_sem, quad_s, quad_r = sems
        _, _, _, core = place(me)

        def piece(d):
            return normed.at[1 - core if d % TWO else core]

        def tokens(d):
            return self.h_u.at[:, :, pl.ds(d * CHUNK, CHUNK)]

        self.h_copies = [remote(piece(d), tokens(d), quad_s.at[TWO, d], quad_r.at[TWO, d], quad_of(me)[d]) for d in (1, TWO, 3)]
        self.h_mine = pltpu.make_async_copy(piece(0), stage, own_sem.at[TWO])
        self.h_back = pltpu.make_async_copy(stage, tokens(0), self.load_sem.at[0])
        self.residual = pltpu.make_async_copy(hidden, self.block_out, own_sem.at[3])
        self.residual.start()
        for c in self.h_copies:
            c.start()
        self.h_mine.start()
        self.homes = [
            Home(me, src, out, own_sem.at[i], quad_s.at[i], quad_r.at[i])
            for i, (src, out) in enumerate([(attn, self.attn_home), (self.dq, self.dq_home)])
        ]
        for h in self.homes:
            h.start()

    @staticmethod
    def scratch(arrays):
        dma, d = pltpu.SemaphoreType.DMA, arrays[-1].shape[0]
        home = pltpu.VMEM((TWO,) * 3 + (CHUNK, d), BF16)
        buf = [pltpu.VMEM((TWO,) + b, BF16) for b in ((d, BLK), (BLK, d))]
        tiles = [pltpu.VMEM((TWO, TWO) + b, BF16) for b in ((CHUNK, d), (TWO, BLK, BLK))]
        sems = [dma((TWO, TWO)), dma((TWO,)), dma((FOUR,)), dma((3, FOUR)), dma((3, FOUR))]
        return [home] * TWO + buf + tiles + sems

    @staticmethod
    def results(arrays):
        unit = TWO, TWO, BLK, arrays[-1].shape[0]
        return [jax.ShapeDtypeStruct(arrays[TWO].shape, t) for t in (BF16, F32)] + [jax.ShapeDtypeStruct(unit, BF16)]

    spaces, out_spaces = [pl.ANY, pltpu.VMEM] + [pl.ANY] * FOUR, [pltpu.VMEM] * TWO + [pl.ANY]

    def step(self, t):
        def fetch_o(t, slot):
            return pltpu.make_async_copy(self.w_o.at[:, aligned(t)], self.buf_o.at[slot], self.w_sem.at[0, slot])

        def fetch_q(t, slot):
            return pltpu.make_async_copy(self.w_q.at[aligned(t)], self.buf_q.at[slot], self.w_sem.at[1, slot])

        def project(t, slot):
            at = aligned(t)
            attn = self.attn_home[...].reshape(-1, self.w_o.shape[0])
            out = jnp.dot(attn, self.buf_o[slot], preferred_element_type=F32)
            self.block_out[:, at] = (self.block_out[:, at].astype(F32) + out).astype(BF16)

        def pull(t, slot):
            dq = self.dq_home[...].reshape(-1, self.w_o.shape[0])
            self.d_part[:, aligned(t)] = dot_t(dq, self.buf_q[slot])

        if t in PRODUCTS_AT:
            i = PRODUCTS_AT.index(t)
            self.homes[i].wait_recv()
            if i == 0:
                self.residual.wait()
            tiled(self.w_o.shape[0] // BLK, *((fetch_o, project), (fetch_q, pull))[i])

    def wq_terms(self, own, other):
        self.h_mine.wait()
        self.h_back.start()
        for c in self.h_copies:
            c.wait_recv()
        self.h_back.wait()
        core = lax.rem(lax.axis_index("cp"), TWO)
        d_out = self.dq[...].reshape(-1, self.dq.shape[-1])

        def fetch(t, slot):
            return pltpu.make_async_copy(self.h_u.at[:, :, :, aligned(t)], self.h_buf.at[slot], self.load_sem.at[slot])

        for out, half in ((other, 1 - core), (own, core)):

            def use(t, slot, out=out, half=half):
                h = self.h_buf[slot].reshape(-1, BLK)
                out[t - half * FOUR] = dot(h, d_out, (0,), (0,)).reshape(out.shape[1:])

            tiled(FOUR, fetch, use, half * FOUR)

    def finish(self):
        for c in self.h_copies + self.homes:
            c.wait_send()


class HiddenGradient:
    tiles = FOUR

    def __init__(self, me, dk, dv, ins, outs, scratch):
        self.part, self.w_k, self.w_v, self.x, self.dy, self.gain = ins
        self.dx, self.terms = outs
        self.dk_home, self.dv_home, self.rows, *sems = scratch
        pairs = (dk, self.dk_home), (dv, self.dv_home)
        self.homes = [Home(me, src, out, *[r.at[i] for r in sems]) for i, (src, out) in enumerate(pairs)]
        for h in self.homes:
            h.start()

    @staticmethod
    def scratch(x):
        dma = pltpu.SemaphoreType.DMA
        home = pltpu.VMEM((TWO,) * 3 + (CHUNK, TWO * HEAD_DIM), BF16)
        return [home, home, pltpu.VMEM((8, x.shape[1]), F32), dma((TWO,)), dma((TWO, FOUR)), dma((TWO, FOUR))]

    def tile(self, t):
        if t == 0:
            for h in self.homes:
                h.wait_recv()
            self.rows[...] = jnp.zeros_like(self.rows)
        size = TWO * CHUNK
        at = pl.ds(t * size, size)
        d = self.part[at]
        for home, w in ((self.dk_home, self.w_k), (self.dv_home, self.w_v)):
            d += dot_t(home[t // TWO, t % TWO].reshape(size, -1), w[...])
        d = d.astype(BF16).astype(F32)
        x = self.x[at].astype(F32)
        inv_rms = lax.rsqrt(row_mean(x * x) + NORM_EPS)
        unit, scaled = x * inv_rms, d * self.gain[...]
        dx = inv_rms * (scaled - unit * row_mean(scaled * unit))
        self.dx[at] = (self.dy[at].astype(F32) + dx).astype(BF16)
        self.rows[...] += jnp.sum((d * unit).reshape((-1,) + self.rows.shape), axis=0)
        if t == self.tiles - 1:
            self.terms[...] = jnp.sum(self.rows[...], axis=0, keepdims=True)

    def finish(self):
        for h in self.homes:
            h.wait_send()


def reduce_pairs(arrays, blocks, cuts, kinds, collective_id, work, more):
    vmem, hbm = pl.BlockSpec(memory_space=pltpu.VMEM), pl.BlockSpec(memory_space=pl.ANY)
    n = len(blocks)
    scratch = [pltpu.VMEM((FOUR, TWO) + blocks[-1], F32)]
    scratch += sum((PairSum.scratch(k, b) for k, b in zip(kinds, blocks)), []) + PairSum.sems(n, max(cuts))
    outs = [jax.ShapeDtypeStruct(b, F32) for b in blocks] + work.results(more)
    return pl.pallas_call(
        functools.partial(reduce_kernel, cuts, kinds, work),
        name="reduce_pairs",
        out_shape=outs,
        in_specs=[hbm] * len(arrays) + [pl.BlockSpec(memory_space=m) for m in work.spaces],
        out_specs=[vmem] * n + [pl.BlockSpec(memory_space=m) for m in work.out_spaces],
        scratch_shapes=scratch + work.scratch(more),
        compiler_params=params(63, collective_id=collective_id),
        cost_estimate=cost(1, 20),
    )(*arrays, *more)


HERE = 0, 0, 0
LINKS = "xyud"
ORDERS = "zxy", "zyx", "yxz", "zyx"
WO_CUTS, WQ_CUTS = (0, 2, 6, 8), (0, 3, 6, 8)
SIZES = 7.0, 9.8, 5.6, 2.8
GAIN_AT = 60.0, 72.0, 84.0, 96.0, 108.0
LATENCY, TILES_FROM, TILE_EVERY = 3.0, 14.0, 8.0
SUM_AT = 25.0, 31.0, 37.0, 43.0


def onward(order, key):
    dz, ry, rx = key
    stage = max((order.index(a) for a, r in zip("zyx", key) if r), default=-1)
    for axis in order[stage + 1 :]:
        if axis == "x":
            yield "x", (dz, ry, 1)
        elif axis == "y":
            yield "y", (dz, 1, rx)
        else:
            yield "u", (-1, ry, rx)
            yield "d", (1, ry, rx)
    if stage >= 0 and order[stage] == "z" and abs(dz) < 3:
        yield ("u", (dz - 1, ry, rx)) if dz < 0 else ("d", (dz + 1, ry, rx))


def arrivals():
    busy, times = {}, {}
    starts = [0.0] * 3 + [SUM_AT[-1] + LATENCY]
    here = [(t, z, part, HERE) for part, t in enumerate(starts) for z in range(FOUR)]
    while here:
        now, z, part, key = heapq.heappop(here)
        times.setdefault((part, key), []).append(now)
        for link, there in onward(ORDERS[part], key):
            to = z + {"u": 1, "d": -1}.get(link, 0)
            if 0 <= to <= 3:
                busy[z, link] = max(busy.get((z, link), 0), now) + SIZES[part]
                heapq.heappush(here, (busy[z, link] + LATENCY, to, part, there))
    return sorted((sum(t) / len(t), *at) for at, t in times.items())


def turn_back(dkv_ref, cos_ref, sin_ref, dk_u, dv_u):
    n = TWO * TWO * BLK
    for i in range(TWO):
        for j in range(TWO):
            cos_t, sin_t = (jnp.hstack([t, t * sign]) for t, sign in ((cos_ref[i, j].T, 1), (sin_ref[i, j].T, -1)))
            dk = dkv_ref[pl.ds((i * TWO + j) * BLK, BLK)] * ATTN_SCALE
            dk_u[i, j] = (dk * cos_t + pltpu.roll(dk, HEAD_DIM // TWO, 1) * sin_t).astype(BF16)
    dv_u[...] = dkv_ref[pl.ds(n, n)].astype(BF16).reshape(dv_u.shape)


def wkv_terms(h_own, dk_u, dv_u, outs):
    d_out = jnp.hstack([r[...].reshape(-1, HEAD_DIM) for r in (dk_u, dv_u)])
    for out, half in outs:

        @pl.loop(0, FOUR)
        def _(zz, out=out, half=half):
            h = h_own[:, :, :, aligned(half * FOUR + zz)].reshape(-1, BLK)
            out[zz] = dot(h, d_out, (0,), (0,)).reshape(out.shape[1:])


def gather_kernel(*refs):
    take = taker(refs)
    wo_ref, wq_ref, dkv_ref, cos_ref, sin_ref, h_ref = take(6)
    grad_ins, outs, (dx_ref, dgain_ref) = take(6), take(FOUR), take(TWO)
    own_sem, send_sem, come_sem, core_sem, put_sem, all_terms, totals, g_s, g_r = take(9)
    terms, wkv_own, wkv_ref, h_own, dk_u, dv_u, *stores = take(10)
    buffers, sems, refs = take(FOUR), take(7), take(len(refs))
    me = lax.axis_index("cp")
    z, y, x, core = place(me)
    line = Line(me)
    to = {"x": dev(z, y, 1 - x, core), "y": dev(z, 1 - y, x, core), "u": line.next[1], "d": line.next[-1]}
    partner = dev(z, y, x, 1 - core)
    meet(quad_of(me)[1:] + [to["y"]] + [dev(zz, y, x, core) for _, zz in z_peers(z)])
    load_h = pltpu.make_async_copy(h_ref, h_own, own_sem.at[0])
    load_h.start()
    wkv = PairSum(me, "core", 1, wkv_ref, wkv_own, buffers, [r.at[0] for r in sems])

    def windows(part, zz, yy, xx, cc):
        chip = (TWO * zz + yy) * TWO + xx
        wide, narrow = wq_ref.shape[1], wkv_own.shape[1] // TWO
        wo_at = ((xx * TWO + cc) * N_PAIRS + chip // TWO) * wo_ref.shape[0]
        wq_at = (cc * N_PAIRS + chip // TWO) * wq_ref.shape[0]
        if part == 3:
            for i, (store, out) in enumerate(zip(stores[TWO:], outs[TWO:])):
                window = out.at[pl.ds(wq_at, wkv_own.shape[0]), pl.ds(xx * narrow, narrow)]
                yield wkv_own.at[:, head_slice(i)], store.at[chip], window
            return

        def cut(ref, cuts):
            first, last = (c * ref.shape[0] // 8 for c in cuts[part : part + TWO])
            return first, last - first

        at, rows = cut(wo_ref, WO_CUTS)
        here = pl.ds(at, rows)
        yield wo_ref.at[here], stores[0].at[chip, here], outs[0].at[pl.ds(wo_at + at, rows)]
        at, rows = cut(wq_ref, WQ_CUTS)
        here = pl.ds(at, rows)
        yield wq_ref.at[here], stores[1].at[chip, here], outs[1].at[pl.ds(wq_at + at, rows), pl.ds(xx * wide, wide)]

    def block(part, key):
        dz, ry, rx = key
        return windows(part, z + dz, 1 - y if ry else y, 1 - x if rx else x, core)

    def index(part, key):
        return (part, key[0] + 3) + key[1:]

    def send(part, key, link, there):
        sent = send_sem.at[index(part, key) + (LINKS.find(link or "-") + 1,)]
        for shard, store, window in block(part, key):
            src = store if any(key) else shard
            if link:
                remote(src, store, sent, come_sem.at[index(part, there)], to[link]).start()
            else:
                remote(src, window, sent, core_sem.at[index(part, key)], partner).start()
                pltpu.make_async_copy(src, window, put_sem.at[index(part, key)]).start()

    def whole(part, send, arrive):
        size = sum(shard.size for shard, _, _ in block(part, HERE)) // outs[0].shape[1]
        dst = outs[0].at[pl.ds(0, size)]
        return remote(dst, dst, send, arrive, me)

    def when(on, do):
        pl.when(on)(do)

    def each_way(part, key):
        held = line.held(key[0])
        yield None, key, held
        for link, there in onward(ORDERS[part], key):
            inside = {"u": line.inside[1], "d": line.inside[-1]}.get(link)
            yield link, there, held if inside is None else jnp.logical_and(held, inside)

    def pass_on(part, key):
        for link, there, on in each_way(part, key):
            when(on, functools.partial(send, part, key, link, there))

    def term_copy(i):
        src = terms if i == 0 else totals.at[i - 1]
        return remote(src, all_terms.at[i], g_s.at[i], g_r.at[i], me ^ (1 << i))

    def add_terms(i):
        term_copy(i).wait_recv()
        totals[i] = (terms[...] if i == 0 else totals[i - 1]) + all_terms[i]
        if i + 1 < len(GAIN_AT):
            term_copy(i + 1).start()

    def tile(t):
        job.tile(t)
        if t == job.tiles - 1:
            term_copy(0).start()

    def sum_step(h):
        wkv.step(0, h)

    steps = [(TILES_FROM + t * TILE_EVERY, functools.partial(tile, t)) for t in range(HiddenGradient.tiles)]
    steps += [(at, functools.partial(sum_step, h)) for h, at in enumerate(SUM_AT)]
    steps += [(at, functools.partial(add_terms, i)) for i, at in enumerate(GAIN_AT)]
    steps.sort(key=lambda s: s[0])
    events = arrivals()
    for part in range(3):
        pass_on(part, HERE)
    turn_back(dkv_ref, cos_ref, sin_ref, dk_u, dv_u)
    job = HiddenGradient(me, dk_u, dv_u, grad_ins, (dx_ref, terms), refs)
    load_h.wait()
    wkv_terms(h_own, dk_u, dv_u, ((wkv_ref, 1 - core), (buffers[0], core)))
    wkv.begin(0)
    wkv.loaded(0)
    for now, part, key in events:
        while steps and steps[0][0] <= now:
            steps.pop(0)[1]()
        if any(key):
            arrive = come_sem.at[index(part, key)]
            when(line.held(key[0]), whole(part, own_sem.at[0], arrive).wait_recv)
            pass_on(part, key)
        elif part == 3:
            pass_on(part, key)
    dgain_ref[...] = totals[len(GAIN_AT) - 1]
    for i in range(len(GAIN_AT)):
        term_copy(i).wait_send()
    for _, part, key in events:
        for sem in (core_sem, put_sem):
            when(line.held(key[0]), whole(part, own_sem.at[0], sem.at[index(part, key)]).wait_recv)
        for link, there, on in each_way(part, key):
            sent = send_sem.at[index(part, key) + (LINKS.find(link or "-") + 1,)]
            when(on, whole(part, sent, own_sem.at[0]).wait_send)
    wkv.wait_send(0)
    job.finish()


def gather_all(wo, wq, dkv, cos_f, sin_f, h_u, part, w_k, w_v, x, dy, gain, shapes):
    dma = pltpu.SemaphoreType.DMA
    vmem, hbm = pl.BlockSpec(memory_space=pltpu.VMEM), pl.BlockSpec(memory_space=pl.ANY)
    block = w_k.shape[0] // TWO // N_PAIRS, w_k.shape[1]
    parts = len(ORDERS)
    keys = (parts, 7, TWO, TWO)
    terms = 1, x.shape[1]
    scratch = [dma((1,)), dma(keys + (len(LINKS) + 1,)), dma(keys), dma(keys), dma(keys)]
    n = len(GAIN_AT)
    scratch += [pltpu.VMEM((n,) + terms, F32)] * TWO + [dma((n,)), dma((n,)), pltpu.VMEM(terms, F32), pltpu.VMEM(block, F32)]
    scratch += [pltpu.VMEM((FOUR, TWO) + block, F32), pltpu.VMEM(h_u.shape, BF16)]
    scratch += [pltpu.VMEM((TWO, TWO, BLK, HEAD_DIM), BF16)] * TWO
    chips = (TWO * N_PAIRS,)
    scratch += [pltpu.VMEM(chips + b, F32) for b in (wo.shape, wq.shape) + ((block[0], HEAD_DIM),) * TWO]
    return pl.pallas_call(
        gather_kernel,
        name="gather_all",
        out_shape=[jax.ShapeDtypeStruct(s, F32) for s in shapes]
        + [jax.ShapeDtypeStruct(x.shape, BF16), jax.ShapeDtypeStruct(terms, F32)],
        in_specs=[vmem] * 5 + [hbm] + [vmem] * 6,
        out_specs=[hbm] * len(shapes) + [vmem] * TWO,
        scratch_shapes=scratch + PairSum.scratch("core", block) + PairSum.sems(1, 1) + HiddenGradient.scratch(x),
        compiler_params=params(63, collective_id=0),
        cost_estimate=cost(1, 76),
    )(wo, wq, dkv, cos_f, sin_f, h_u, part, w_k, w_v, x, dy, gain)


def perm(x, pairs):
    return lax.ppermute(x, "cp", pairs)


def flip_pairs(d):
    return [(r, r ^ d) for r in range(32)]


def solution(mesh):
    def local_step(hidden, grad_out, positions, seg_ids, w_q, w_k, w_v, w_o, norm_gain):
        n_batch, n_tok, d_model = hidden.shape
        n_rows = n_batch * n_tok
        wide = N_HEADS * HEAD_DIM
        me = lax.axis_index("cp")
        z, y, x, core = place(me)
        quad, pair = me % FOUR, me // FOUR
        relations = range(FOUR)

        def swap(pieces):
            return [perm(p, flip_pairs(d)) if d else p for d, p in enumerate(pieces)]

        gain = norm_gain.astype(F32)
        cos_t, sin_t = rope_tables(positions.reshape(n_rows))
        cos_f, sin_f = jnp.hstack([cos_t, cos_t]), jnp.hstack([-sin_t, sin_t])
        dy_flat = grad_out.reshape(n_rows, d_model)
        normed, kv_home = project(hidden.reshape(n_rows, d_model), gain[NEW], w_k, w_v, cos_f, sin_f)
        pos = jnp.pad(positions.reshape(TWO, TWO, n_tok), ((0, 0), (0, 6), (0, 0)))
        kv_home = kv_home.reshape((TWO,) * 5 + (CHUNK, HEAD_DIM))
        kv_all, q_u, do_u, pos_u, *dy_rows = exchange(kv_home, normed, dy_flat, pos, cos_f, sin_f, w_q, w_o)
        pos_u = pos_u[:, :TWO].reshape((FOUR, TWO, TWO, CHUNK)).transpose(1, TWO, 0, 3).reshape(TWO, TWO, BLK)
        dy_rows = [a.reshape(TWO, TWO, CHUNK, d_model) for a in dy_rows]
        dy_pieces = swap([dy_rows[d % TWO] for d in relations])

        member = quad ^ jnp.arange(FOUR)
        front, back = ((m[:, NEW] * CHUNK + jnp.arange(CHUNK)[NEW]).reshape(BLK) for m in (member, 3 - member))
        offsets = jnp.stack([front, back]).astype(jnp.int32)
        own_super = jnp.stack([pair, N_SUPER - 1 - pair]).astype(jnp.int32)
        q_index = own_super[:, NEW] * BLK + offsets
        start = q_index[NEW] - pos_u
        tab = jnp.concatenate(
            [own_super, (jnp.min(start, axis=-1) // BLK).reshape(-1), jnp.max(start, axis=-1).reshape(-1)]
        )
        start_r = start[:, :, NEW, :]
        q_index_r = jnp.broadcast_to(q_index[NEW, :, NEW, :], start_r.shape)
        cos_u, sin_u = rope_tables(pos_u)
        cos_ut, sin_ut = jnp.swapaxes(cos_u, TWO, 3), jnp.swapaxes(sin_u, TWO, 3)

        koff = offsets[:, NEW]
        attn_u, lse = flash_fwd(tab, q_u, kv_all, start_r, q_index_r, koff)

        wo_keep, wo_away = wo_terms(attn_u, dy_pieces)
        wo_come = perm(wo_away, flip_pairs(FOUR))
        do_u, wo_keep = lax.optimization_barrier((do_u, wo_keep))
        dq_u, dkv = flash_bwd(tab, q_u, do_u, attn_u, kv_all, lse, start_r, q_index_r, koff, cos_ut, sin_ut)

        x_flat = hidden.reshape(n_rows, d_model)
        wo_own, dkv_own, wq_own, block_out, d_part, h_u = reduce_pairs(
            [wo_keep, wo_come, dkv.reshape(FOUR, TWO, -1, HEAD_DIM)],
            [wo_keep.shape[1:], (dkv.size // N_PAIRS // HEAD_DIM, HEAD_DIM), (d_model // TWO // N_PAIRS, wide)],
            (TWO, 8, 8),
            ("z", "", "core"),
            TWO,
            Products,
            (attn_u, dq_u, x_flat, normed.reshape((TWO,) * 3 + (CHUNK, d_model)), w_o, w_q),
        )
        grad_wo, grad_wq, grad_wk, grad_wv, grad_x, d_gain = gather_all(
            wo_own,
            wq_own,
            dkv_own,
            cos_ut,
            sin_ut,
            h_u,
            d_part,
            w_k,
            w_v,
            x_flat,
            dy_flat,
            gain[NEW],
            [w_o.shape, w_q.shape, w_k.shape, w_v.shape],
        )
        block_out, grad_x = (a.reshape(hidden.shape) for a in (block_out, grad_x))
        return block_out, grad_x, grad_wq, grad_wk, grad_wv, grad_wo, d_gain.reshape(d_model)

    seq_spec = P(None, "cp", None)
    tok_spec = P(None, "cp")
    full_spec = P()
    return jax.shard_map(
        local_step,
        mesh=mesh,
        in_specs=(seq_spec, seq_spec, tok_spec, tok_spec, full_spec, full_spec, full_spec, full_spec, full_spec),
        out_specs=(seq_spec, seq_spec, full_spec, full_spec, full_spec, full_spec, full_spec),
        check_vma=False,
    )
```

```python
import functools
import heapq
import itertools

import jax
import jax.numpy as jnp
from jax import lax
from jax.experimental import pallas as pl
from jax.experimental.pallas import tpu as pltpu
from jax.sharding import PartitionSpec as P

HEAD_DIM = 128
NORM_EPS = 1e-5
ROPE_BASE = 500000.0
NEG_BIG = -1e30
LOG2E = 1.4426950408889634
ATTN_SCALE = HEAD_DIM**-0.5
EXP2_SCALE = ATTN_SCALE * LOG2E
CHUNK = 64
TWO = 2
FOUR = 4
NEW = jnp.newaxis
BLK = 4 * CHUNK
N_HEADS = 8
N_PAIRS = 8
N_SUPER = 2 * N_PAIRS
MESH = pl.DeviceIdType.MESH
ONE = pl.Squeezed()
GROUP = 4
MADE_AT = 5
PRODUCTS_AT = 7, 9
F32 = jnp.float32
BF16 = jnp.bfloat16

T_SQ, T_LO, T_MX = 0, 2, 6


def rope_tables(positions):
    inv_freq = ROPE_BASE ** (-jnp.arange(0, HEAD_DIM, TWO).astype(F32) / HEAD_DIM)
    angles = positions.astype(F32)[..., None] * inv_freq
    return jnp.cos(angles), jnp.sin(angles)


def dot(a, b, ca, cb):
    return lax.dot_general(a, b, ((ca, cb), ((), ())), preferred_element_type=F32)


def cost(gflop, mib):
    return pl.CostEstimate(flops=gflop * 10**9, bytes_accessed=mib << 20, transcendentals=0)


def params(mib, **more):
    return pltpu.CompilerParams(vmem_limit_bytes=mib << 20, **more)


def row_mean(x):
    return jnp.mean(x, axis=-1, keepdims=True)


def head(h):
    return pl.ds(h * HEAD_DIM, HEAD_DIM)


def head_slice(h):
    return slice(h * HEAD_DIM, (h + 1) * HEAD_DIM)


def dot_t(a, b):
    return dot(a, b, (1,), (1,))


def steps(tab, body):
    b, hf = pl.program_id(0), pl.program_id(1)
    own, first, last_start = tab[T_SQ + hf], tab[T_LO + TWO * b + hf], tab[T_MX + TWO * b + hf]

    def step(s, carry):
        late = s >= N_PAIRS
        at = jnp.where(late, N_SUPER - 1 - s, s), late.astype(jnp.int32)
        full = jnp.logical_and(s < own, s * BLK >= last_start)
        pl.when(full)(lambda: body(s, at, False))
        pl.when(jnp.logical_not(full))(lambda: body(s, at, True))
        return carry

    lax.fori_loop(first, own + 1, step, 0)


def down(row, n):
    return jnp.broadcast_to(row, (n, row.shape[-1])).T


def may_use(s, off, st_ref, qi_ref):
    return jnp.logical_and(off >= st_ref[...] - s * BLK, off <= qi_ref[...] - s * BLK)


def fwd_kernel(tab, q_ref, kv_ref, st_ref, qi_ref, ko_ref, o_ref, lse_ref, q_s, acc, m_s, l_s, k_t, bounds):
    m_s[...] = jnp.full_like(m_s, NEG_BIG)
    l_s[...] = jnp.zeros_like(l_s)
    acc[...] = jnp.zeros_like(acc)
    for i, ref in enumerate((st_ref, qi_ref)):
        bounds[i] = down(ref[...], HEAD_DIM)
    for h in range(N_HEADS):
        q_s[pl.ds(h * BLK, BLK)] = q_ref[:, head(h)]

    @pl.when(pl.program_id(1) == 0)
    def _():
        @pl.loop(0, N_PAIRS)
        def _(pair):
            for hk in range(TWO):
                k_t[pair, hk] = kv_ref[pair, 0, hk].T

    def body(s, at, masked):
        pair, hk = at
        v = kv_ref[pair, 1, hk]
        if masked:
            off = ko_ref[hk] + s * BLK
            mask = [
                jnp.logical_and(off[:, lanes] >= bounds[0], off[:, lanes] <= bounds[1])
                for lanes in (slice(HEAD_DIM), slice(HEAD_DIM, BLK))
            ]
            mask = [jnp.concatenate([m, m], axis=0) for m in mask]
        for g in range(N_HEADS // TWO):
            rows = pl.ds(g * TWO * BLK, TWO * BLK)
            sc = jnp.dot(q_s[rows], k_t[pair, hk], preferred_element_type=F32)
            sc = [sc[:, :HEAD_DIM], sc[:, HEAD_DIM:]]
            if masked:
                sc = [jnp.where(m, x, NEG_BIG) for m, x in zip(mask, sc)]
            m_old = m_s[rows]
            m_new = jnp.maximum(m_old, jnp.max(jnp.maximum(*sc), axis=1, keepdims=True))
            alpha = jnp.exp2((m_old - m_new) * EXP2_SCALE)
            p = [jnp.exp2((x - m_new) * EXP2_SCALE) for x in sc]
            m_s[rows] = m_new
            l_s[rows] = l_s[rows] * alpha + (p[0] + p[1])
            p = jnp.hstack([x.astype(BF16) for x in p])
            acc[rows] = acc[rows] * alpha + jnp.dot(p, v, preferred_element_type=F32)

    steps(tab, body)
    for h in range(N_HEADS):
        rows = pl.ds(h * BLK, BLK)
        total = jnp.sum(l_s[rows], axis=1, keepdims=True)
        o_ref[:, head(h)] = (acc[rows] / total).astype(BF16)
        lse_ref[h] = (m_s[rows] * EXP2_SCALE + jnp.log2(total)).T[:1]


def bwd_kernel(tab, q_ref, do_ref, o_ref, kv_ref, lse_ref, st_ref, qi_ref, ko_ref, cos_ref, sin_ref, dq_ref, dkv_ref, *scratch):
    dq_acc, delta, off_s, q_s, do_s, q_t, do_t, p_s, ds_s = scratch
    dq_acc[...] = jnp.zeros_like(dq_acc)
    for h in range(N_HEADS):
        q, do = q_ref[:, head(h)], do_ref[:, head(h)]
        delta[h] = jnp.sum((do.astype(F32) * o_ref[:, head(h)].astype(F32)).T, axis=0, keepdims=True)
        q_s[pl.ds(h * BLK, BLK)], do_s[pl.ds(h * BLK, BLK)] = q, do
        q_t[h], do_t[h] = q.T, do.T

    @pl.when(pl.program_id(1) == 0)
    def _():
        dkv_ref[...] = jnp.zeros_like(dkv_ref)
        for hk in range(TWO):
            off_s[hk] = down(ko_ref[hk], BLK)

    def body(s, at, masked):
        pair, hk = at
        k = kv_ref[pair, 0, hk]
        v = kv_ref[pair, 1, hk]
        k_t = k.T
        mask = may_use(s, off_s[hk], st_ref, qi_ref) if masked else None
        for first in range(0, N_HEADS, GROUP):
            rows = pl.ds(first * BLK, GROUP * BLK)
            for h in range(first, first + GROUP):
                cols = pl.ds(h * BLK, BLK)
                p = jnp.exp2(jnp.dot(k, q_t[h], preferred_element_type=F32) * EXP2_SCALE - lse_ref[h])
                if masked:
                    p = jnp.where(mask, p, 0.0)
                ds = p * (jnp.dot(v, do_t[h], preferred_element_type=F32) - delta[h])
                p_s[:, cols] = p.astype(BF16)
                ds_s[:, cols] = ds.astype(BF16)
            dkv_ref[pair, 0, hk] += jnp.dot(ds_s[:, rows], q_s[rows], preferred_element_type=F32)
            dkv_ref[pair, 1, hk] += jnp.dot(p_s[:, rows], do_s[rows], preferred_element_type=F32)
            dq_acc[:, rows] += jnp.dot(k_t, ds_s[:, rows], preferred_element_type=F32)

    steps(tab, body)
    cos_t, sin_t = cos_ref[...], sin_ref[...]
    half = HEAD_DIM // TWO
    for h in range(N_HEADS):
        cols = pl.ds(h * BLK, BLK)
        a, c = dq_acc[:half, cols] * ATTN_SCALE, dq_acc[half:, cols] * ATTN_SCALE
        lin = jnp.concatenate([a * cos_t + c * sin_t, c * cos_t - a * sin_t], axis=0)
        dq_ref[:, head(h)] = lin.T.astype(BF16)


def attn_specs():
    def at_tile(b, h, t):
        return (b, h) + (0,) * TWO

    def at_row(b, h, t):
        return (0, 0, b) + (0,) * 3

    tile = pl.BlockSpec((ONE, ONE, BLK, N_HEADS * HEAD_DIM), at_tile)
    row = pl.BlockSpec((ONE, ONE, 1, BLK), at_tile)
    stat = pl.BlockSpec((ONE, ONE, N_HEADS, 1, BLK), lambda b, h, t: (b, h) + (0,) * 3)
    rope = pl.BlockSpec((ONE, ONE, HEAD_DIM // TWO, BLK), at_tile)
    kv = pl.BlockSpec((N_PAIRS, TWO, ONE, TWO, BLK, HEAD_DIM), at_row)
    ko = pl.BlockSpec((TWO, 1, BLK), lambda b, h, t: (0,) * 3)
    return tile, row, stat, kv, ko, rope


def flash_fwd(tab, q, kv, start, qidx, koff):
    tile, row, stat, kvs, ko, _ = attn_specs()
    return pl.pallas_call(
        fwd_kernel,
        name="attn_fwd",
        out_shape=(jax.ShapeDtypeStruct(q.shape, BF16), jax.ShapeDtypeStruct((TWO, TWO, N_HEADS, 1, BLK), F32)),
        grid_spec=pltpu.PrefetchScalarGridSpec(
            num_scalar_prefetch=1,
            grid=(TWO, TWO),
            in_specs=[tile, kvs, row, row, ko],
            out_specs=[tile, stat],
            scratch_shapes=[pltpu.VMEM((N_HEADS * BLK, HEAD_DIM), t) for t in (BF16, F32, F32, F32)]
            + [pltpu.VMEM((N_PAIRS, TWO, HEAD_DIM, BLK), BF16), pltpu.VMEM((TWO, BLK, HEAD_DIM), jnp.int32)],
        ),
        compiler_params=params(63),
        cost_estimate=cost(20, 16),
    )(tab, q, kv, start, qidx, koff)


def flash_bwd(tab, q, do, o, kv, lse, start, qidx, koff, cos_t, sin_t):
    tile, row, stat, kvs, ko, rope = attn_specs()
    return pl.pallas_call(
        bwd_kernel,
        name="attn_bwd",
        out_shape=(
            jax.ShapeDtypeStruct(q.shape, BF16),
            jax.ShapeDtypeStruct(kv.shape, F32),
        ),
        grid_spec=pltpu.PrefetchScalarGridSpec(
            num_scalar_prefetch=1,
            grid=(TWO, TWO),
            in_specs=[tile, tile, tile, kvs, stat, row, row, ko, rope, rope],
            out_specs=[tile, kvs],
            scratch_shapes=[pltpu.VMEM((HEAD_DIM, N_HEADS * BLK), F32), pltpu.VMEM((N_HEADS, 1, BLK), F32)]
            + [pltpu.VMEM((TWO, BLK, BLK), jnp.int32)]
            + [pltpu.VMEM((N_HEADS * BLK, HEAD_DIM), BF16)] * TWO
            + [pltpu.VMEM((N_HEADS, HEAD_DIM, BLK), BF16)] * TWO
            + [pltpu.VMEM((BLK, N_HEADS * BLK), BF16)] * TWO,
        ),
        compiler_params=params(63),
        cost_estimate=cost(50, 32),
    )(tab, q, do, o, kv, lse, start, qidx, koff, cos_t, sin_t)


def turn(x, cos_ref, sin_ref):
    return x * cos_ref[...] + pltpu.roll(x, HEAD_DIM // TWO, 1) * sin_ref[...]


def first_kernel(x_ref, g_ref, wk_ref, wv_ref, cos_ref, sin_ref, h_ref, kv_ref):
    x = x_ref[...].astype(F32)
    h = (x * lax.rsqrt(row_mean(x * x) + NORM_EPS) * g_ref[...]).astype(BF16)
    h_ref[...] = h
    k = jnp.dot(h, wk_ref[...], preferred_element_type=F32)
    v = jnp.dot(h, wv_ref[...], preferred_element_type=F32)
    n = kv_ref.shape[3]
    for i in range(TWO):
        for j, val in enumerate((turn(k[:, head_slice(i)], cos_ref, sin_ref), v[:, head_slice(i)])):
            for c in range(TWO):
                kv_ref[i, c, j] = val[c * n : (c + 1) * n].astype(BF16)


def project(x, gain, w_k, w_v, cos_f, sin_f):
    n = x.shape[0] // TWO
    return pl.pallas_call(
        first_kernel,
        name="norm_kv",
        out_shape=(jax.ShapeDtypeStruct(x.shape, BF16), jax.ShapeDtypeStruct((TWO,) * 3 + (n, HEAD_DIM), BF16)),
        compiler_params=params(20),
        cost_estimate=cost(TWO, 7),
    )(x, gain, w_k, w_v, cos_f, sin_f)


def place(me):
    return me // 8, lax.rem(me // FOUR, TWO), lax.rem(me // TWO, TWO), lax.rem(me, TWO)


def dev(z, y, x, core):
    return ((z * TWO + y) * TWO + x) * TWO + core


def z_peers(z):
    return [(k, lax.rem(z + k, FOUR)) for k in (1, TWO, 3)]


def meet(peers):
    barrier = pltpu.get_barrier_semaphore()
    for d in peers:
        pl.semaphore_signal(barrier, device_id=(d,), device_id_type=MESH)
    pl.semaphore_wait(barrier, len(peers))


def remote(src, dst, send, arrive, to):
    return pltpu.make_async_remote_copy(
        src_ref=src, dst_ref=dst, send_sem=send, recv_sem=arrive, device_id=(to,), device_id_type=MESH
    )


class Line:
    order = (0, 1, -1, TWO, -TWO, 3, -3)

    def __init__(self, me):
        self.z, y, x, core = place(me)
        self.next = {1: dev(self.z + 1, y, x, core), -1: dev(self.z - 1, y, x, core)}
        self.inside = {1: self.z < 3, -1: self.z > 0}

    def held(self, dz):
        return jnp.logical_and(self.z + dz >= 0, self.z + dz <= 3)

    def ways(self, dz):
        for d in self.next:
            if d * dz <= 0:
                yield d, self.inside[d] if dz == 0 else jnp.logical_and(self.inside[d], self.held(dz))


def tiled(n, fetch, use, first=0):
    fetch(first, 0).start()

    @pl.loop(0, n)
    def _(t):
        slot = lax.rem(t, TWO)
        fetch(first + t, slot).wait()

        @pl.when(t + 1 < n)
        def _():
            fetch(first + t + 1, 1 - slot).start()

        use(first + t, slot)


def aligned(t, size=BLK):
    return pl.ds(pl.multiple_of(t * size, size), size)


def exchange_kernel(*refs):
    take = taker(refs)
    kv_ref, h_ref, dy_ref, pos_ref, cos_ref, sin_ref, wq_ref, wo_ref, kv_all, q_u, do_u, pos_u, *dy_rows = take(14)
    own_sem, quad_s, quad_r, z_s, z_r, y_s, y_r, q_home, do_home, wq_buf, wo_buf, w_sem, dy_sem = take(len(refs))
    me = lax.axis_index("cp")
    z, y, x, core = place(me)
    quad, line = quad_of(me), Line(me)
    across = dev(z, 1 - y, x, core)
    meet(quad[1:] + [across] + [dev(zz, y, x, core) for _, zz in z_peers(z)])

    def source(a, d):
        xx, cc = 1 - x if d // TWO else x, 1 - core if d % TWO else core
        return pos_ref.at[cc] if a == 3 else (kv_ref, q_home, do_home)[a].at[xx, cc]

    def target(a, d):
        if a == 3:
            return pos_u.at[d]
        tok = pl.ds(d * CHUNK, CHUNK)
        return kv_all.at[me // FOUR, :, :, :, tok] if a == 0 else (q_u, do_u)[a - 1].at[:, :, tok]

    def quad_copy(a, d):
        return remote(source(a, d), target(a, d), quad_s.at[a, d], quad_r.at[a, d], quad[d])

    def own_copy(a):
        return pltpu.make_async_copy(source(a, 0), target(a, 0), own_sem.at[a])

    def z_copy(part, dz, d):
        block = kv_all.at[TWO * (z + dz) + y, part]
        return remote(block, block, z_s.at[part, (d + 1) // TWO, dz + 3], z_r.at[part, dz - d + 3], line.next[d])

    def y_copy(part, dz, yy=y):
        block = kv_all.at[TWO * (z + dz) + yy, part]
        return remote(block, block, y_s.at[part, dz + 3], y_r.at[part, dz + 3], across)

    parts = range(TWO)
    moves = [(part, dz) for dz in line.order for part in parts]

    def pass_on(count):
        for part, dz in [moves.pop(0) for _ in range(count)]:
            if dz:
                block = kv_all.at[TWO * (z + dz) + y, part]
                arrival = remote(block, block, own_sem.at[0], z_r.at[part, dz + 3], me)
                pl.when(line.held(dz))(arrival.wait_recv)
            for d, on in line.ways(dz):
                pl.when(on)(z_copy(part, dz, d).start)
            pl.when(line.held(dz))(y_copy(part, dz).start)

    n = h_ref.shape[1] // BLK // TWO

    def fetch_q(t, slot):
        return pltpu.make_async_copy(wq_ref.at[:, aligned(t)], wq_buf.at[slot], w_sem.at[0, slot])

    def fetch_o(t, slot):
        return pltpu.make_async_copy(wo_ref.at[aligned(t)], wo_buf.at[slot], w_sem.at[1, slot])

    def put(home, t, val):
        home[t // n, :, :, :, :, aligned(lax.rem(t, n))] = val.astype(BF16).reshape(home.shape[1:-1] + (BLK,))

    def query(t, slot):
        q = jnp.dot(h_ref[...], wq_buf[slot], preferred_element_type=F32)
        put(q_home, t, jnp.hstack([turn(q[:, head_slice(j)], cos_ref, sin_ref) for j in range(BLK // HEAD_DIM)]))

    def pull(t, slot):
        put(do_home, t, dot_t(dy_ref[...], wo_buf[slot]))

    all_moves = list(moves)
    half = dy_ref.shape[0] // TWO
    for i, out in enumerate(dy_rows):
        pltpu.make_async_copy(dy_ref.at[aligned(core if i == 0 else 1 - core, half)], out, dy_sem.at[i]).start()
    for a in (0, 3):
        for d in (1, TWO, 3):
            quad_copy(a, d).start()
        own_copy(a).start()
    for a, (fetch, use) in enumerate(((fetch_q, query), (fetch_o, pull)), 1):
        for near in range(TWO):
            tiled(n, fetch, use, n * (x if near else 1 - x))
            for d in range(TWO):
                if d or not near:
                    quad_copy(a, d if near else d + TWO).start()
            if near:
                own_copy(a).start()
            if len(moves) == len(all_moves):
                own_copy(0).wait()
                for d in (1, TWO, 3):
                    quad_copy(0, d).wait_recv()
            pass_on(TWO)
    pass_on(len(moves))
    for part, dz in all_moves:
        for d, on in line.ways(dz):
            pl.when(on)(z_copy(part, dz, d).wait_send)
        pl.when(line.held(dz))(y_copy(part, dz, 1 - y).wait_recv)
        pl.when(line.held(dz))(y_copy(part, dz).wait_send)
    for a in range(FOUR):
        for d in (1, TWO, 3):
            quad_copy(a, d).wait_send()
            if a > 0:
                quad_copy(a, d).wait_recv()
    for a in (1, TWO, 3):
        own_copy(a).wait()
    for i, out in enumerate(dy_rows):
        pltpu.make_async_copy(dy_ref.at[aligned(core if i == 0 else 1 - core, half)], out, dy_sem.at[i]).wait()


def exchange(kv, h, dy, pos, cos_f, sin_f, w_q, w_o):
    dma = pltpu.SemaphoreType.DMA
    vmem, hbm = pl.BlockSpec(memory_space=pltpu.VMEM), pl.BlockSpec(memory_space=pl.ANY)
    wide = w_q.shape[1] // TWO
    unit = jax.ShapeDtypeStruct((TWO, TWO, BLK, wide), BF16)
    pos_quad = jax.ShapeDtypeStruct((FOUR,) + pos.shape[1:], pos.dtype)
    dy_half = jax.ShapeDtypeStruct((dy.shape[0] // TWO, dy.shape[1]), BF16)
    home = pltpu.VMEM((TWO,) * FOUR + (CHUNK, wide), BF16)
    sems = [dma((FOUR,))] + [dma((FOUR, FOUR))] * TWO + [dma((TWO, TWO, 7))] + [dma((TWO, 7))] * 3
    bufs = [pltpu.VMEM((TWO,) + b, BF16) for b in ((w_q.shape[0], BLK), (BLK, w_o.shape[1]))]
    return pl.pallas_call(
        exchange_kernel,
        name="exchange",
        out_shape=(jax.ShapeDtypeStruct((N_PAIRS,) + (TWO,) * 3 + (BLK, HEAD_DIM), BF16), unit, unit, pos_quad, dy_half, dy_half),
        in_specs=[vmem] * 6 + [hbm] * TWO,
        out_specs=[hbm] * 6,
        scratch_shapes=sems + [home, home] + bufs + [dma((TWO, TWO)), dma((TWO,))],
        compiler_params=params(63, collective_id=1),
        cost_estimate=cost(1, 20),
    )(kv, h, dy, pos, cos_f, sin_f, w_q, w_o)


def taker(refs):
    rest = iter(refs)
    return lambda count: list(itertools.islice(rest, count))


def wo_kernel(*refs):
    take = taker(refs)
    o_ref, *pieces = take(5)
    keep, away, dy_u, o_t, terms, came, load_sem, core_s, core_r = take(len(refs))
    me = lax.axis_index("cp")
    _, y, _, core = place(me)
    meet(quad_of(me)[1:TWO])
    loads = [
        pltpu.make_async_copy(src, dy_u.at[:, :, pl.ds(d * CHUNK, CHUNK)], load_sem.at[d])
        for d, src in enumerate(pieces)
    ]
    for c in loads:
        c.start()
    for h in range(N_HEADS):
        o_t[head(h)] = o_ref[:, :, :, head(h)].reshape(-1, HEAD_DIM).T
    for c in loads:
        c.wait()
    half, tiles = terms.shape[1], terms.shape[TWO] // BLK

    def swap(t):
        return remote(terms.at[0, :, aligned(t)], came.at[:, aligned(t)], core_s.at[t], core_r.at[t], quad_of(me)[1])

    def half_terms(i, to, then):
        @pl.loop(0, tiles)
        def _(t):
            dy = dy_u[:, :, :, aligned(t)].reshape(-1, BLK)
            terms[to, :, aligned(t)] = jnp.dot(o_t[aligned(i, half)], dy, preferred_element_type=F32)
            then(t)

    half_terms(1 - core, 0, lambda t: swap(t).start())
    half_terms(core, 1, lambda t: swap(t).wait_recv())
    rows = keep.shape[1]
    for zz in range(FOUR):
        for out, yy in ((keep, y), (away, 1 - y)):
            at = aligned(TWO * zz + yy, rows)
            out[zz] = terms[1, at] + came[at]
    for t in range(tiles):
        swap(t).wait_send()


def wo_terms(o, pieces):
    dma = pltpu.SemaphoreType.DMA
    vmem, hbm = pl.BlockSpec(memory_space=pltpu.VMEM), pl.BlockSpec(memory_space=pl.ANY)
    n, d, wide = o.shape[0] * o.shape[1] * o.shape[TWO], pieces[0].shape[-1], o.shape[-1]
    half = wide // TWO
    return pl.pallas_call(
        wo_kernel,
        name="wo_terms",
        out_shape=[jax.ShapeDtypeStruct((FOUR, half // N_PAIRS, d), F32)] * TWO,
        in_specs=[vmem] + [hbm] * FOUR,
        out_specs=[vmem] * TWO,
        scratch_shapes=[pltpu.VMEM((TWO, TWO, BLK, d), BF16), pltpu.VMEM((wide, n), BF16)]
        + [pltpu.VMEM((TWO, half, d), F32), pltpu.VMEM((half, d), F32), dma((FOUR,)), dma((d // BLK,)), dma((d // BLK,))],
        compiler_params=params(63, collective_id=3),
        cost_estimate=cost(FOUR, 20),
    )(o, *pieces)


class PairSum:
    def __init__(self, me, kind, cut, src, out, buffers, sems):
        self.me, self.kind, self.src, self.out = me, kind, src, out
        self.size = out.shape[0] // cut
        self.own, self.from_core, self.from_y, self.from_z = buffers
        self.load_sem, self.core_s, self.core_r, self.y_s, self.y_r, self.z_s, self.z_r = sems
        self.z, self.y, x, core = place(me)
        self.partner = dev(self.z, self.y, x, 1 - core)
        self.across = dev(self.z, 1 - self.y, x, core)
        self.next_z = dev(self.z + 1, self.y, x, core), dev(self.z - 1, self.y, x, core)

    def rows(self, j):
        return pl.ds(j * self.size, self.size)

    def mine(self, j, zz):
        at = self.rows(j)
        return self.own.at[zz, self.y, at] if self.kind == "core" else self.own.at[zz, at]

    def loads(self, j):
        at = self.rows(j)
        if self.kind == "z":
            pairs = zip(self.src, (self.own, self.from_y))
            return [pltpu.make_async_copy(a.at[:, at], b.at[:, at], s.at[j]) for (a, b), s in zip(pairs, (self.load_sem, self.y_r))]
        return [pltpu.make_async_copy(self.src.at[:, self.y, at], self.own.at[:, at], self.load_sem.at[j])]

    def core_copy(self, j):
        src, dst = (r.at[:, :, self.rows(j)] for r in (self.src, self.from_core))
        return remote(src, dst, self.core_s.at[j], self.core_r.at[j], self.partner)

    def y_copy(self, j):
        src = self.own if self.kind == "core" else self.src
        at = self.rows(j)
        return remote(src.at[:, 1 - self.y, at], self.from_y.at[:, at], self.y_s.at[j], self.y_r.at[j], self.across)

    def z_copy(self, j, way, zz, to):
        at = way, zz + way - 1
        return remote(self.mine(j, zz), self.from_z.at[*at, self.rows(j)], self.z_s.at[j, *at], self.z_r.at[j, *at], to)

    def begin(self, j):
        if self.kind == "core":
            self.core_copy(j).start()
            return
        for c in self.loads(j):
            c.start()
        if not self.kind:
            self.y_copy(j).start()

    def loaded(self, j):
        if self.kind != "core":
            for c in self.loads(j):
                c.wait()
        else:
            self.core_copy(j).wait_recv()
            at = self.rows(j)
            for zz in range(FOUR):
                self.own[zz, :, at] += self.from_core[zz, :, at]
            self.y_copy(j).start()
        if self.kind == "z":
            self.add_y(j)
            self.hop(j, 0)

    def add_y(self, j):
        for zz in range(FOUR):
            self.mine(j, zz)[...] += self.from_y[zz, self.rows(j)]

    def relay(self, j, way, zz, add):
        if add:
            self.z_copy(j, way, zz, self.me).wait_recv()
            self.mine(j, zz)[...] += self.from_z[way, zz + way - 1, self.rows(j)]
        self.z_copy(j, way, zz, self.next_z[way]).start()

    def hop(self, j, h):
        @pl.when(self.z == h)
        def _():
            for zz in range(3, h, -1):
                self.relay(j, 0, zz, h > 0)

        @pl.when(self.z == 3 - h)
        def _():
            for zz in range(3 - h):
                self.relay(j, 1, zz, h > 0)

    def step(self, j, h):
        if h == 0 and self.kind != "z":
            self.y_copy(j).wait_recv()
            self.add_y(j)
            self.hop(j, 0)
        elif 0 < h < 3:
            self.hop(j, h)
        elif h == 3:
            at = self.rows(j)
            self.out[at] = self.mine(j, self.z)[...]
            for way, on in enumerate((self.z > 0, self.z < 3)):

                @pl.when(on)
                def _(way=way):
                    self.z_copy(j, way, self.z, self.me).wait_recv()
                    self.out[at] += self.from_z[way, self.z + way - 1, at]

    def wait_send(self, j):
        if self.kind == "core":
            self.core_copy(j).wait_send()
        if self.kind != "z":
            self.y_copy(j).wait_send()
        for zz in range(FOUR):
            if zz > 0:
                pl.when(self.z < zz)(self.z_copy(j, 0, zz, self.next_z[0]).wait_send)
            if zz < 3:
                pl.when(self.z > zz)(self.z_copy(j, 1, zz, self.next_z[1]).wait_send)

    @staticmethod
    def scratch(kind, block):
        unused = pltpu.VMEM((8, HEAD_DIM), F32)
        own = pltpu.VMEM(((FOUR, TWO) if kind == "core" else (FOUR,)) + block, F32)
        from_y = pltpu.VMEM((FOUR,) + block, F32)
        return [own, own if kind == "core" else unused, from_y, pltpu.VMEM((TWO, 3) + block, F32)]

    @staticmethod
    def sems(*dims):
        dma = pltpu.SemaphoreType.DMA
        return [dma(dims)] * 5 + [dma(dims + (TWO, 3))] * TWO


def reduce_kernel(cuts, kinds, work, *refs):
    n = len(cuts)

    take = taker(refs)
    ins = [take(TWO) if k == "z" else take(1)[0] for k in kinds[:-1]]
    more_in, outs, more_out, made = take(work.ins), take(n), take(work.outs), take(1)
    buffers, sems = [take(FOUR) for _ in kinds], take(7)
    me = lax.axis_index("cp")
    z, y, x, core = place(me)
    meet(quad_of(me)[1:] + [dev(z, 1 - y, x, core)] + [dev(zz, y, x, core) for _, zz in z_peers(z)])
    job = work(me, more_in, more_out, take(len(refs)))
    sums = [PairSum(me, *a, [r.at[i] for r in sems]) for i, a in enumerate(zip(kinds, cuts, ins + made, outs, buffers))]
    pieces = [(s, j) for s, cut in zip(sums, cuts) for j in range(cut)]
    early, late = pieces[: -cuts[-1]], pieces[-cuts[-1] :]
    for s, j in early:
        s.begin(j)
    for s, j in early:
        s.loaded(j)
    for t in range(len(pieces) + 3):
        if t == MADE_AT:
            job.wq_terms(sums[-1].own, made[0])
            for s, j in late:
                s.begin(j)
        if t == MADE_AT + 1:
            for s, j in late:
                s.loaded(j)
        for h in range(FOUR):
            if 0 <= t - h < len(pieces):
                s, j = pieces[t - h]
                s.step(j, h)
        job.step(t)
    for s, j in pieces:
        s.wait_send(j)
    job.finish()


def quad_of(me):
    z, y, x, core = place(me)
    return [dev(z, y, 1 - x if d // TWO else x, 1 - core if d % TWO else core) for d in range(FOUR)]


class Home:
    def __init__(self, me, src, out, own_sem, send, arrive):
        _, _, x, core = place(me)
        w = src.shape[-1]
        to = out.at[core, :, :, :, pl.ds(x * w, w)]

        def piece(d):
            return src.at[:, :, pl.ds(d * CHUNK, CHUNK)]

        self.own = pltpu.make_async_copy(piece(0), to, own_sem)
        self.copies = [remote(piece(d), to, send.at[d], arrive.at[d], quad_of(me)[d]) for d in (1, TWO, 3)]

    def start(self):
        self.own.start()
        for c in self.copies:
            c.start()

    def wait_recv(self):
        self.own.wait()
        for c in self.copies:
            c.wait_recv()

    def wait_send(self):
        for c in self.copies:
            c.wait_send()


class Products:
    ins, outs = 6, 3

    def __init__(self, me, ins, outs, scratch):
        attn, self.dq, hidden, normed, self.w_o, self.w_q = ins
        self.block_out, self.d_part, self.h_u = outs
        self.attn_home, self.dq_home, self.buf_o, self.buf_q, stage, self.h_buf, *sems = scratch
        self.w_sem, self.load_sem, own_sem, quad_s, quad_r = sems
        _, _, _, core = place(me)

        def piece(d):
            return normed.at[1 - core if d % TWO else core]

        def tokens(d):
            return self.h_u.at[:, :, pl.ds(d * CHUNK, CHUNK)]

        self.h_copies = [remote(piece(d), tokens(d), quad_s.at[TWO, d], quad_r.at[TWO, d], quad_of(me)[d]) for d in (1, TWO, 3)]
        self.h_mine = pltpu.make_async_copy(piece(0), stage, own_sem.at[TWO])
        self.h_back = pltpu.make_async_copy(stage, tokens(0), self.load_sem.at[0])
        self.residual = pltpu.make_async_copy(hidden, self.block_out, own_sem.at[3])
        self.residual.start()
        for c in self.h_copies:
            c.start()
        self.h_mine.start()
        self.homes = [
            Home(me, src, out, own_sem.at[i], quad_s.at[i], quad_r.at[i])
            for i, (src, out) in enumerate([(attn, self.attn_home), (self.dq, self.dq_home)])
        ]
        for h in self.homes:
            h.start()

    @staticmethod
    def scratch(arrays):
        dma, d = pltpu.SemaphoreType.DMA, arrays[-1].shape[0]
        home = pltpu.VMEM((TWO,) * 3 + (CHUNK, d), BF16)
        buf = [pltpu.VMEM((TWO,) + b, BF16) for b in ((d, BLK), (BLK, d))]
        tiles = [pltpu.VMEM((TWO, TWO) + b, BF16) for b in ((CHUNK, d), (TWO, BLK, BLK))]
        sems = [dma((TWO, TWO)), dma((TWO,)), dma((FOUR,)), dma((3, FOUR)), dma((3, FOUR))]
        return [home] * TWO + buf + tiles + sems

    @staticmethod
    def results(arrays):
        unit = TWO, TWO, BLK, arrays[-1].shape[0]
        return [jax.ShapeDtypeStruct(arrays[TWO].shape, t) for t in (BF16, F32)] + [jax.ShapeDtypeStruct(unit, BF16)]

    spaces, out_spaces = [pl.ANY, pltpu.VMEM] + [pl.ANY] * FOUR, [pltpu.VMEM] * TWO + [pl.ANY]

    def step(self, t):
        def fetch_o(t, slot):
            return pltpu.make_async_copy(self.w_o.at[:, aligned(t)], self.buf_o.at[slot], self.w_sem.at[0, slot])

        def fetch_q(t, slot):
            return pltpu.make_async_copy(self.w_q.at[aligned(t)], self.buf_q.at[slot], self.w_sem.at[1, slot])

        def project(t, slot):
            at = aligned(t)
            attn = self.attn_home[...].reshape(-1, self.w_o.shape[0])
            out = jnp.dot(attn, self.buf_o[slot], preferred_element_type=F32)
            self.block_out[:, at] = (self.block_out[:, at].astype(F32) + out).astype(BF16)

        def pull(t, slot):
            dq = self.dq_home[...].reshape(-1, self.w_o.shape[0])
            self.d_part[:, aligned(t)] = dot_t(dq, self.buf_q[slot])

        if t in PRODUCTS_AT:
            i = PRODUCTS_AT.index(t)
            self.homes[i].wait_recv()
            if i == 0:
                self.residual.wait()
            tiled(self.w_o.shape[0] // BLK, *((fetch_o, project), (fetch_q, pull))[i])

    def wq_terms(self, own, other):
        self.h_mine.wait()
        self.h_back.start()
        for c in self.h_copies:
            c.wait_recv()
        self.h_back.wait()
        core = lax.rem(lax.axis_index("cp"), TWO)
        d_out = self.dq[...].reshape(-1, self.dq.shape[-1])

        def fetch(t, slot):
            return pltpu.make_async_copy(self.h_u.at[:, :, :, aligned(t)], self.h_buf.at[slot], self.load_sem.at[slot])

        for out, half in ((other, 1 - core), (own, core)):

            def use(t, slot, out=out, half=half):
                h = self.h_buf[slot].reshape(-1, BLK)
                out[t - half * FOUR] = dot(h, d_out, (0,), (0,)).reshape(out.shape[1:])

            tiled(FOUR, fetch, use, half * FOUR)

    def finish(self):
        for c in self.h_copies + self.homes:
            c.wait_send()


class HiddenGradient:
    tiles = FOUR

    def __init__(self, me, dk, dv, ins, outs, scratch):
        self.part, self.w_k, self.w_v, self.x, self.dy, self.gain = ins
        self.dx, self.terms = outs
        self.dk_home, self.dv_home, self.rows, *sems = scratch
        pairs = (dk, self.dk_home), (dv, self.dv_home)
        self.homes = [Home(me, src, out, *[r.at[i] for r in sems]) for i, (src, out) in enumerate(pairs)]
        for h in self.homes:
            h.start()

    @staticmethod
    def scratch(x):
        dma = pltpu.SemaphoreType.DMA
        home = pltpu.VMEM((TWO,) * 3 + (CHUNK, TWO * HEAD_DIM), BF16)
        return [home, home, pltpu.VMEM((8, x.shape[1]), F32), dma((TWO,)), dma((TWO, FOUR)), dma((TWO, FOUR))]

    def tile(self, t):
        if t == 0:
            for h in self.homes:
                h.wait_recv()
            self.rows[...] = jnp.zeros_like(self.rows)
        size = TWO * CHUNK
        at = pl.ds(t * size, size)
        d = self.part[at]
        for home, w in ((self.dk_home, self.w_k), (self.dv_home, self.w_v)):
            d += dot_t(home[t // TWO, t % TWO].reshape(size, -1), w[...])
        d = d.astype(BF16).astype(F32)
        x = self.x[at].astype(F32)
        inv_rms = lax.rsqrt(row_mean(x * x) + NORM_EPS)
        unit, scaled = x * inv_rms, d * self.gain[...]
        dx = inv_rms * (scaled - unit * row_mean(scaled * unit))
        self.dx[at] = (self.dy[at].astype(F32) + dx).astype(BF16)
        self.rows[...] += jnp.sum((d * unit).reshape((-1,) + self.rows.shape), axis=0)
        if t == self.tiles - 1:
            self.terms[...] = jnp.sum(self.rows[...], axis=0, keepdims=True)

    def finish(self):
        for h in self.homes:
            h.wait_send()


def reduce_pairs(arrays, blocks, cuts, kinds, collective_id, work, more):
    vmem, hbm = pl.BlockSpec(memory_space=pltpu.VMEM), pl.BlockSpec(memory_space=pl.ANY)
    n = len(blocks)
    scratch = [pltpu.VMEM((FOUR, TWO) + blocks[-1], F32)]
    scratch += sum((PairSum.scratch(k, b) for k, b in zip(kinds, blocks)), []) + PairSum.sems(n, max(cuts))
    outs = [jax.ShapeDtypeStruct(b, F32) for b in blocks] + work.results(more)
    return pl.pallas_call(
        functools.partial(reduce_kernel, cuts, kinds, work),
        name="reduce_pairs",
        out_shape=outs,
        in_specs=[hbm] * len(arrays) + [pl.BlockSpec(memory_space=m) for m in work.spaces],
        out_specs=[vmem] * n + [pl.BlockSpec(memory_space=m) for m in work.out_spaces],
        scratch_shapes=scratch + work.scratch(more),
        compiler_params=params(63, collective_id=collective_id),
        cost_estimate=cost(1, 20),
    )(*arrays, *more)


HERE = 0, 0, 0
LINKS = "xyud"
ORDERS = "zxy", "zyx", "yxz", "zyx"
CUTS = 0, 40, 96, 128
SIZES = 7.0, 9.8, 5.6, 2.8
GAIN_AT = [60.0 + 12.0 * i for i in range(5)]
LATENCY, TILES_FROM, TILE_EVERY = 3.0, 14.0, 8.0
SUM_AT = [25.0 + 6.0 * i for i in range(4)]


def onward(order, key):
    dz, ry, rx = key
    stage = max((order.index(a) for a, r in zip("zyx", key) if r), default=-1)
    for axis in order[stage + 1 :]:
        if axis == "x":
            yield "x", (dz, ry, 1)
        elif axis == "y":
            yield "y", (dz, 1, rx)
        else:
            yield "u", (-1, ry, rx)
            yield "d", (1, ry, rx)
    if stage >= 0 and order[stage] == "z" and abs(dz) < 3:
        yield ("u", (dz - 1, ry, rx)) if dz < 0 else ("d", (dz + 1, ry, rx))


def arrivals():
    busy, times = {}, {}
    starts = [0.0] * 3 + [SUM_AT[-1] + LATENCY]
    here = [(t, z, part, HERE) for part, t in enumerate(starts) for z in range(FOUR)]
    while here:
        now, z, part, key = heapq.heappop(here)
        times.setdefault((part, key), []).append(now)
        for link, there in onward(ORDERS[part], key):
            to = z + {"u": 1, "d": -1}.get(link, 0)
            if 0 <= to <= 3:
                busy[z, link] = max(busy.get((z, link), 0), now) + SIZES[part]
                heapq.heappush(here, (busy[z, link] + LATENCY, to, part, there))
    return sorted((sum(t) / len(t), *at) for at, t in times.items())


def turn_back(dkv_ref, cos_ref, sin_ref, dk_u, dv_u):
    n = TWO * TWO * BLK
    for i in range(TWO):
        for j in range(TWO):
            cos_t, sin_t = (jnp.hstack([t, t * sign]) for t, sign in ((cos_ref[i, j].T, 1), (sin_ref[i, j].T, -1)))
            dk = dkv_ref[pl.ds((i * TWO + j) * BLK, BLK)] * ATTN_SCALE
            dk_u[i, j] = (dk * cos_t + pltpu.roll(dk, HEAD_DIM // TWO, 1) * sin_t).astype(BF16)
    dv_u[...] = dkv_ref[pl.ds(n, n)].astype(BF16).reshape(dv_u.shape)


def wkv_terms(h_own, dk_u, dv_u, outs):
    d_out = jnp.hstack([r[...].reshape(-1, HEAD_DIM) for r in (dk_u, dv_u)])
    for out, half in outs:

        @pl.loop(0, FOUR)
        def _(zz, out=out, half=half):
            h = h_own[:, :, :, aligned(half * FOUR + zz)].reshape(-1, BLK)
            out[zz] = dot(h, d_out, (0,), (0,)).reshape(out.shape[1:])


def gather_kernel(*refs):
    take = taker(refs)
    wo_ref, wq_ref, dkv_ref, cos_ref, sin_ref, h_ref = take(6)
    grad_ins, outs, (dx_ref, dgain_ref) = take(6), take(FOUR), take(TWO)
    own_sem, send_sem, come_sem, core_sem, put_sem, all_terms, totals, g_s, g_r = take(9)
    terms, wkv_ref, h_own, dk_u, dv_u, store, wkv_store = take(7)
    buffers, sems, refs = take(FOUR), take(7), take(len(refs))
    me = lax.axis_index("cp")
    z, y, x, core = place(me)
    line = Line(me)
    to = {"x": dev(z, y, 1 - x, core), "y": dev(z, 1 - y, x, core), "u": line.next[1], "d": line.next[-1]}
    partner = dev(z, y, x, 1 - core)
    chip_here = me // TWO
    n_wo, wide = wo_ref.shape[0], wq_ref.shape[1]
    store[chip_here, pl.ds(0, n_wo)] = wo_ref[...]
    for i in range(TWO):
        store[chip_here, pl.ds(n_wo, n_wo), pl.ds(i * wide, wide)] = wq_ref[pl.ds(i * n_wo, n_wo)]
    meet(quad_of(me)[1:] + [to["y"]] + [dev(zz, y, x, core) for _, zz in z_peers(z)])
    load_h = pltpu.make_async_copy(h_ref, h_own, own_sem.at[0])
    load_h.start()
    wkv = PairSum(me, "core", 1, wkv_ref, wkv_store.at[chip_here], buffers, [r.at[0] for r in sems])

    def place_of(key):
        dz, ry, rx = key
        return z + dz, 1 - y if ry else y, 1 - x if rx else x

    def block(part, key):
        zz, yy, xx = place_of(key)
        chip = (TWO * zz + yy) * TWO + xx
        return wkv_store.at[chip] if part == 3 else store.at[chip, pl.ds(CUTS[part], CUTS[part + 1] - CUTS[part])]

    def windows(part, key):
        zz, yy, xx = place_of(key)
        pair, src = TWO * zz + yy, block(part, key)
        wo_at, wq_at = ((xx * TWO + core) * N_PAIRS + pair) * n_wo, (core * N_PAIRS + pair) * wq_ref.shape[0]
        if part == 3:
            for i, out in enumerate(outs[TWO:]):
                yield src.at[:, head(i)], out.at[pl.ds(wq_at, wq_ref.shape[0]), pl.ds(xx * HEAD_DIM, HEAD_DIM)]
            return
        first, last = CUTS[part : part + TWO]
        if first < n_wo:
            rows = min(last, n_wo) - first
            yield src.at[pl.ds(0, rows)], outs[0].at[pl.ds(wo_at + first, rows)]
        if last > n_wo:
            skip = max(n_wo - first, 0)
            rows, at = last - first - skip, first + skip - n_wo
            for i in range(TWO):
                window = outs[1].at[pl.ds(wq_at + i * n_wo + at, rows), pl.ds(xx * wide, wide)]
                yield src.at[pl.ds(skip, rows), pl.ds(i * wide, wide)], window

    def index(part, key):
        return (part, key[0] + 3) + key[1:]

    def send(part, key, link, there):
        sent = send_sem.at[index(part, key) + (LINKS.find(link or "-") + 1,)]
        if link:
            remote(block(part, key), block(part, key), sent, come_sem.at[index(part, there)], to[link]).start()
            return
        for src, window in windows(part, key):
            remote(src, window, sent, core_sem.at[index(part, key)], partner).start()
            pltpu.make_async_copy(src, window, put_sem.at[index(part, key)]).start()

    def whole(part, send, arrive):
        size = CUTS[part + 1] - CUTS[part] if part < 3 else wkv_store.size // store.shape[0] // outs[0].shape[1]
        dst = outs[0].at[pl.ds(0, size)]
        return remote(dst, dst, send, arrive, me)

    def when(on, do):
        pl.when(on)(do)

    def each_way(part, key):
        held = line.held(key[0])
        yield None, key, held
        for link, there in onward(ORDERS[part], key):
            inside = {"u": line.inside[1], "d": line.inside[-1]}.get(link)
            yield link, there, held if inside is None else jnp.logical_and(held, inside)

    def pass_on(part, key):
        for link, there, on in each_way(part, key):
            when(on, functools.partial(send, part, key, link, there))

    def term_copy(i):
        src = terms if i == 0 else totals.at[i - 1]
        return remote(src, all_terms.at[i], g_s.at[i], g_r.at[i], me ^ (1 << i))

    def add_terms(i):
        term_copy(i).wait_recv()
        totals[i] = (terms[...] if i == 0 else totals[i - 1]) + all_terms[i]
        if i + 1 < len(GAIN_AT):
            term_copy(i + 1).start()

    def tile(t):
        job.tile(t)
        if t == job.tiles - 1:
            term_copy(0).start()

    def sum_step(h):
        wkv.step(0, h)

    steps = [(TILES_FROM + t * TILE_EVERY, functools.partial(tile, t)) for t in range(HiddenGradient.tiles)]
    steps += [(at, functools.partial(sum_step, h)) for h, at in enumerate(SUM_AT)]
    steps += [(at, functools.partial(add_terms, i)) for i, at in enumerate(GAIN_AT)]
    steps.sort(key=lambda s: s[0])
    events = arrivals()
    for part in range(3):
        pass_on(part, HERE)
    turn_back(dkv_ref, cos_ref, sin_ref, dk_u, dv_u)
    job = HiddenGradient(me, dk_u, dv_u, grad_ins, (dx_ref, terms), refs)
    load_h.wait()
    wkv_terms(h_own, dk_u, dv_u, ((wkv_ref, 1 - core), (buffers[0], core)))
    wkv.begin(0)
    wkv.loaded(0)
    for now, part, key in events:
        while steps and steps[0][0] <= now:
            steps.pop(0)[1]()
        if any(key):
            arrive = come_sem.at[index(part, key)]
            when(line.held(key[0]), whole(part, own_sem.at[0], arrive).wait_recv)
            pass_on(part, key)
        elif part == 3:
            pass_on(part, key)
    dgain_ref[...] = totals[len(GAIN_AT) - 1]
    for i in range(len(GAIN_AT)):
        term_copy(i).wait_send()
    for _, part, key in events:
        for sem in (core_sem, put_sem):
            when(line.held(key[0]), whole(part, own_sem.at[0], sem.at[index(part, key)]).wait_recv)
        for link, there, on in each_way(part, key):
            sent = send_sem.at[index(part, key) + (LINKS.find(link or "-") + 1,)]
            when(on, whole(part, sent, own_sem.at[0]).wait_send)
    wkv.wait_send(0)
    job.finish()


def gather_all(wo, wq, dkv, cos_f, sin_f, h_u, part, w_k, w_v, x, dy, gain, shapes):
    dma = pltpu.SemaphoreType.DMA
    vmem, hbm = pl.BlockSpec(memory_space=pltpu.VMEM), pl.BlockSpec(memory_space=pl.ANY)
    block = w_k.shape[0] // TWO // N_PAIRS, w_k.shape[1]
    parts = len(ORDERS)
    keys = (parts, 7, TWO, TWO)
    terms = 1, x.shape[1]
    scratch = [dma((1,)), dma(keys + (len(LINKS) + 1,)), dma(keys), dma(keys), dma(keys)]
    n = len(GAIN_AT)
    scratch += [pltpu.VMEM((n,) + terms, F32)] * TWO + [dma((n,)), dma((n,)), pltpu.VMEM(terms, F32)]
    scratch += [pltpu.VMEM((FOUR, TWO) + block, F32), pltpu.VMEM(h_u.shape, BF16)]
    scratch += [pltpu.VMEM((TWO, TWO, BLK, HEAD_DIM), BF16)] * TWO
    scratch += [pltpu.VMEM((TWO * N_PAIRS,) + b, F32) for b in ((TWO * wo.shape[0], wo.shape[1]), block)]
    return pl.pallas_call(
        gather_kernel,
        name="gather_all",
        out_shape=[jax.ShapeDtypeStruct(s, F32) for s in shapes]
        + [jax.ShapeDtypeStruct(x.shape, BF16), jax.ShapeDtypeStruct(terms, F32)],
        in_specs=[vmem] * 5 + [hbm] + [vmem] * 6,
        out_specs=[hbm] * len(shapes) + [vmem] * TWO,
        scratch_shapes=scratch + PairSum.scratch("core", block) + PairSum.sems(1, 1) + HiddenGradient.scratch(x),
        compiler_params=params(63, collective_id=0),
        cost_estimate=cost(1, 76),
    )(wo, wq, dkv, cos_f, sin_f, h_u, part, w_k, w_v, x, dy, gain)


def perm(x, pairs):
    return lax.ppermute(x, "cp", pairs)


def flip_pairs(d):
    return [(r, r ^ d) for r in range(32)]


def solution(mesh):
    def local_step(hidden, grad_out, positions, seg_ids, w_q, w_k, w_v, w_o, norm_gain):
        n_batch, n_tok, d_model = hidden.shape
        n_rows = n_batch * n_tok
        wide = N_HEADS * HEAD_DIM
        me = lax.axis_index("cp")
        z, y, x, core = place(me)
        quad, pair = me % FOUR, me // FOUR
        relations = range(FOUR)

        def swap(pieces):
            return [perm(p, flip_pairs(d)) if d else p for d, p in enumerate(pieces)]

        gain = norm_gain.astype(F32)
        cos_t, sin_t = rope_tables(positions.reshape(n_rows))
        cos_f, sin_f = jnp.hstack([cos_t, cos_t]), jnp.hstack([-sin_t, sin_t])
        dy_flat = grad_out.reshape(n_rows, d_model)
        normed, kv_home = project(hidden.reshape(n_rows, d_model), gain[NEW], w_k, w_v, cos_f, sin_f)
        pos = jnp.pad(positions.reshape(TWO, TWO, n_tok), ((0, 0), (0, 6), (0, 0)))
        kv_home = kv_home.reshape((TWO,) * 5 + (CHUNK, HEAD_DIM))
        kv_all, q_u, do_u, pos_u, *dy_rows = exchange(kv_home, normed, dy_flat, pos, cos_f, sin_f, w_q, w_o)
        pos_u = pos_u[:, :TWO].reshape((FOUR, TWO, TWO, CHUNK)).transpose(1, TWO, 0, 3).reshape(TWO, TWO, BLK)
        dy_rows = [a.reshape(TWO, TWO, CHUNK, d_model) for a in dy_rows]
        dy_pieces = swap([dy_rows[d % TWO] for d in relations])

        member = quad ^ jnp.arange(FOUR)
        front, back = ((m[:, NEW] * CHUNK + jnp.arange(CHUNK)[NEW]).reshape(BLK) for m in (member, 3 - member))
        offsets = jnp.stack([front, back]).astype(jnp.int32)
        own_super = jnp.stack([pair, N_SUPER - 1 - pair]).astype(jnp.int32)
        q_index = own_super[:, NEW] * BLK + offsets
        start = q_index[NEW] - pos_u
        tab = jnp.concatenate(
            [own_super, (jnp.min(start, axis=-1) // BLK).reshape(-1), jnp.max(start, axis=-1).reshape(-1)]
        )
        start_r = start[:, :, NEW, :]
        q_index_r = jnp.broadcast_to(q_index[NEW, :, NEW, :], start_r.shape)
        cos_u, sin_u = rope_tables(pos_u)
        cos_ut, sin_ut = jnp.swapaxes(cos_u, TWO, 3), jnp.swapaxes(sin_u, TWO, 3)

        koff = offsets[:, NEW]
        attn_u, lse = flash_fwd(tab, q_u, kv_all, start_r, q_index_r, koff)

        wo_keep, wo_away = wo_terms(attn_u, dy_pieces)
        wo_come = perm(wo_away, flip_pairs(FOUR))
        do_u, wo_keep = lax.optimization_barrier((do_u, wo_keep))
        dq_u, dkv = flash_bwd(tab, q_u, do_u, attn_u, kv_all, lse, start_r, q_index_r, koff, cos_ut, sin_ut)

        x_flat = hidden.reshape(n_rows, d_model)
        wo_own, dkv_own, wq_own, block_out, d_part, h_u = reduce_pairs(
            [wo_keep, wo_come, dkv.reshape(FOUR, TWO, -1, HEAD_DIM)],
            [wo_keep.shape[1:], (dkv.size // N_PAIRS // HEAD_DIM, HEAD_DIM), (d_model // TWO // N_PAIRS, wide)],
            (TWO, 8, 8),
            ("z", "", "core"),
            TWO,
            Products,
            (attn_u, dq_u, x_flat, normed.reshape((TWO,) * 3 + (CHUNK, d_model)), w_o, w_q),
        )
        grad_wo, grad_wq, grad_wk, grad_wv, grad_x, d_gain = gather_all(
            wo_own,
            wq_own,
            dkv_own,
            cos_ut,
            sin_ut,
            h_u,
            d_part,
            w_k,
            w_v,
            x_flat,
            dy_flat,
            gain[NEW],
            [w_o.shape, w_q.shape, w_k.shape, w_v.shape],
        )
        block_out, grad_x = (a.reshape(hidden.shape) for a in (block_out, grad_x))
        return block_out, grad_x, grad_wq, grad_wk, grad_wv, grad_wo, d_gain.reshape(d_model)

    seq_spec = P(None, "cp", None)
    tok_spec = P(None, "cp")
    full_spec = P()
    return jax.shard_map(
        local_step,
        mesh=mesh,
        in_specs=(seq_spec, seq_spec, tok_spec, tok_spec, full_spec, full_spec, full_spec, full_spec, full_spec),
        out_specs=(seq_spec, seq_spec, full_spec, full_spec, full_spec, full_spec, full_spec),
        check_vma=False,
    )
```

```python
import functools
import heapq
import itertools

import jax
import jax.numpy as jnp
from jax import lax
from jax.experimental import pallas as pl
from jax.experimental.pallas import tpu as pltpu
from jax.sharding import PartitionSpec as P

HEAD_DIM = 128
NORM_EPS = 1e-5
ROPE_BASE = 500000.0
NEG_BIG = -1e30
LOG2E = 1.4426950408889634
ATTN_SCALE = HEAD_DIM**-0.5
EXP2_SCALE = ATTN_SCALE * LOG2E
CHUNK = 64
TWO = 2
THREE = 3
FOUR = 4
NEW = jnp.newaxis
BLK = 4 * CHUNK
N_HEADS = 8
N_PAIRS = 8
N_SUPER = 2 * N_PAIRS
MESH = pl.DeviceIdType.MESH
ONE = pl.Squeezed()
GROUP = 4
MADE_AT = 5
PRODUCTS_AT = 7, 9
F32 = jnp.float32
BF16 = jnp.bfloat16

T_SQ, T_LO, T_MX = 0, 2, 6


def rope_tables(positions):
    inv_freq = ROPE_BASE ** (-jnp.arange(0, HEAD_DIM, TWO).astype(F32) / HEAD_DIM)
    angles = positions.astype(F32)[..., None] * inv_freq
    return jnp.cos(angles), jnp.sin(angles)


def dot(a, b, ca, cb):
    return lax.dot_general(a, b, ((ca, cb), ((), ())), preferred_element_type=F32)


def cost(gflop, mib):
    return pl.CostEstimate(flops=gflop * 10**9, bytes_accessed=mib << 20, transcendentals=0)


def params(mib, **more):
    return pltpu.CompilerParams(vmem_limit_bytes=mib << 20, **more)


def row_mean(x):
    return jnp.mean(x, axis=-1, keepdims=True)


def head(h):
    return pl.ds(h * HEAD_DIM, HEAD_DIM)


def head_slice(h):
    return slice(h * HEAD_DIM, (h + 1) * HEAD_DIM)


def dot_t(a, b):
    return dot(a, b, (1,), (1,))


def steps(tab, body):
    b, hf = pl.program_id(0), pl.program_id(1)
    own, first, last_start = tab[T_SQ + hf], tab[T_LO + TWO * b + hf], tab[T_MX + TWO * b + hf]

    def step(s, carry):
        late = s >= N_PAIRS
        at = jnp.where(late, N_SUPER - 1 - s, s), late.astype(jnp.int32)
        full = jnp.logical_and(s < own, s * BLK >= last_start)
        pl.when(full)(lambda: body(s, at, False))
        pl.when(jnp.logical_not(full))(lambda: body(s, at, True))
        return carry

    lax.fori_loop(first, own + 1, step, 0)


def down(row, n):
    return jnp.broadcast_to(row, (n, row.shape[-1])).T


def may_use(s, off, st_ref, qi_ref):
    return jnp.logical_and(off >= st_ref[...] - s * BLK, off <= qi_ref[...] - s * BLK)


def fwd_kernel(tab, q_ref, kv_ref, st_ref, qi_ref, ko_ref, o_ref, lse_ref, q_s, acc, m_s, l_s, k_t, bounds):
    m_s[...] = jnp.full_like(m_s, NEG_BIG)
    l_s[...] = jnp.zeros_like(l_s)
    acc[...] = jnp.zeros_like(acc)
    for i, ref in enumerate((st_ref, qi_ref)):
        bounds[i] = down(ref[...], HEAD_DIM)
    for h in range(N_HEADS):
        q_s[pl.ds(h * BLK, BLK)] = q_ref[:, head(h)]

    @pl.when(pl.program_id(1) == 0)
    def _():
        @pl.loop(0, N_PAIRS)
        def _(pair):
            for hk in range(TWO):
                k_t[pair, hk] = kv_ref[pair, 0, hk].T

    def body(s, at, masked):
        pair, hk = at
        v = kv_ref[pair, 1, hk]
        if masked:
            off = ko_ref[hk] + s * BLK
            mask = [
                jnp.logical_and(off[:, lanes] >= bounds[0], off[:, lanes] <= bounds[1])
                for lanes in (slice(HEAD_DIM), slice(HEAD_DIM, BLK))
            ]
            mask = [jnp.concatenate([m, m], axis=0) for m in mask]
        for g in range(N_HEADS // TWO):
            rows = pl.ds(g * TWO * BLK, TWO * BLK)
            sc = jnp.dot(q_s[rows], k_t[pair, hk], preferred_element_type=F32)
            sc = [sc[:, :HEAD_DIM], sc[:, HEAD_DIM:]]
            if masked:
                sc = [jnp.where(m, x, NEG_BIG) for m, x in zip(mask, sc)]
            m_old = m_s[rows]
            m_new = jnp.maximum(m_old, jnp.max(jnp.maximum(*sc), axis=1, keepdims=True))
            alpha = jnp.exp2((m_old - m_new) * EXP2_SCALE)
            p = [jnp.exp2((x - m_new) * EXP2_SCALE) for x in sc]
            m_s[rows] = m_new
            l_s[rows] = l_s[rows] * alpha + (p[0] + p[1])
            p = jnp.hstack([x.astype(BF16) for x in p])
            acc[rows] = acc[rows] * alpha + jnp.dot(p, v, preferred_element_type=F32)

    steps(tab, body)
    for h in range(N_HEADS):
        rows = pl.ds(h * BLK, BLK)
        total = jnp.sum(l_s[rows], axis=1, keepdims=True)
        o_ref[:, head(h)] = (acc[rows] / total).astype(BF16)
        lse_ref[h] = (m_s[rows] * EXP2_SCALE + jnp.log2(total)).T[:1]


def bwd_kernel(tab, q_ref, do_ref, o_ref, kv_ref, lse_ref, st_ref, qi_ref, ko_ref, cos_ref, sin_ref, dq_ref, dkv_ref, *scratch):
    dq_acc, delta, off_s, q_s, do_s, q_t, do_t, p_s, ds_s = scratch
    dq_acc[...] = jnp.zeros_like(dq_acc)
    for h in range(N_HEADS):
        q, do = q_ref[:, head(h)], do_ref[:, head(h)]
        delta[h] = jnp.sum((do.astype(F32) * o_ref[:, head(h)].astype(F32)).T, axis=0, keepdims=True)
        q_s[pl.ds(h * BLK, BLK)], do_s[pl.ds(h * BLK, BLK)] = q, do
        q_t[h], do_t[h] = q.T, do.T

    @pl.when(pl.program_id(1) == 0)
    def _():
        dkv_ref[...] = jnp.zeros_like(dkv_ref)
        for hk in range(TWO):
            off_s[hk] = down(ko_ref[hk], BLK)

    def body(s, at, masked):
        pair, hk = at
        k = kv_ref[pair, 0, hk]
        v = kv_ref[pair, 1, hk]
        k_t = k.T
        mask = may_use(s, off_s[hk], st_ref, qi_ref) if masked else None
        for first in range(0, N_HEADS, GROUP):
            rows = pl.ds(first * BLK, GROUP * BLK)
            for h in range(first, first + GROUP):
                cols = pl.ds(h * BLK, BLK)
                p = jnp.exp2(jnp.dot(k, q_t[h], preferred_element_type=F32) * EXP2_SCALE - lse_ref[h])
                if masked:
                    p = jnp.where(mask, p, 0.0)
                ds = p * (jnp.dot(v, do_t[h], preferred_element_type=F32) - delta[h])
                p_s[:, cols] = p.astype(BF16)
                ds_s[:, cols] = ds.astype(BF16)
            dkv_ref[pair, 0, hk] += jnp.dot(ds_s[:, rows], q_s[rows], preferred_element_type=F32)
            dkv_ref[pair, 1, hk] += jnp.dot(p_s[:, rows], do_s[rows], preferred_element_type=F32)
            dq_acc[:, rows] += jnp.dot(k_t, ds_s[:, rows], preferred_element_type=F32)

    steps(tab, body)
    cos_t, sin_t = cos_ref[...], sin_ref[...]
    half = HEAD_DIM // TWO
    for h in range(N_HEADS):
        cols = pl.ds(h * BLK, BLK)
        a, c = dq_acc[:half, cols] * ATTN_SCALE, dq_acc[half:, cols] * ATTN_SCALE
        lin = jnp.concatenate([a * cos_t + c * sin_t, c * cos_t - a * sin_t], axis=0)
        dq_ref[:, head(h)] = lin.T.astype(BF16)


def attn_specs():
    def at_tile(b, h, t):
        return (b, h) + (0,) * TWO

    def at_row(b, h, t):
        return (0, 0, b) + (0,) * THREE

    tile = pl.BlockSpec((ONE, ONE, BLK, N_HEADS * HEAD_DIM), at_tile)
    row = pl.BlockSpec((ONE, ONE, 1, BLK), at_tile)
    stat = pl.BlockSpec((ONE, ONE, N_HEADS, 1, BLK), lambda b, h, t: (b, h) + (0,) * THREE)
    rope = pl.BlockSpec((ONE, ONE, HEAD_DIM // TWO, BLK), at_tile)
    kv = pl.BlockSpec((N_PAIRS, TWO, ONE, TWO, BLK, HEAD_DIM), at_row)
    ko = pl.BlockSpec((TWO, 1, BLK), lambda b, h, t: (0,) * THREE)
    return tile, row, stat, kv, ko, rope


def flash_fwd(tab, q, kv, start, qidx, koff):
    tile, row, stat, kvs, ko, _ = attn_specs()
    return pl.pallas_call(
        fwd_kernel,
        name="attn_fwd",
        out_shape=(jax.ShapeDtypeStruct(q.shape, BF16), jax.ShapeDtypeStruct((TWO, TWO, N_HEADS, 1, BLK), F32)),
        grid_spec=pltpu.PrefetchScalarGridSpec(
            num_scalar_prefetch=1,
            grid=(TWO, TWO),
            in_specs=[tile, kvs, row, row, ko],
            out_specs=[tile, stat],
            scratch_shapes=[pltpu.VMEM((N_HEADS * BLK, HEAD_DIM), t) for t in (BF16, F32, F32, F32)]
            + [pltpu.VMEM((N_PAIRS, TWO, HEAD_DIM, BLK), BF16), pltpu.VMEM((TWO, BLK, HEAD_DIM), jnp.int32)],
        ),
        compiler_params=params(63),
        cost_estimate=cost(20, 16),
    )(tab, q, kv, start, qidx, koff)


def flash_bwd(tab, q, do, o, kv, lse, start, qidx, koff, cos_t, sin_t):
    tile, row, stat, kvs, ko, rope = attn_specs()
    return pl.pallas_call(
        bwd_kernel,
        name="attn_bwd",
        out_shape=(
            jax.ShapeDtypeStruct(q.shape, BF16),
            jax.ShapeDtypeStruct(kv.shape, F32),
        ),
        grid_spec=pltpu.PrefetchScalarGridSpec(
            num_scalar_prefetch=1,
            grid=(TWO, TWO),
            in_specs=[tile, tile, tile, kvs, stat, row, row, ko, rope, rope],
            out_specs=[tile, kvs],
            scratch_shapes=[pltpu.VMEM((HEAD_DIM, N_HEADS * BLK), F32), pltpu.VMEM((N_HEADS, 1, BLK), F32)]
            + [pltpu.VMEM((TWO, BLK, BLK), jnp.int32)]
            + [pltpu.VMEM((N_HEADS * BLK, HEAD_DIM), BF16)] * TWO
            + [pltpu.VMEM((N_HEADS, HEAD_DIM, BLK), BF16)] * TWO
            + [pltpu.VMEM((BLK, N_HEADS * BLK), BF16)] * TWO,
        ),
        compiler_params=params(63),
        cost_estimate=cost(50, 32),
    )(tab, q, do, o, kv, lse, start, qidx, koff, cos_t, sin_t)


def turn(x, cos_ref, sin_ref):
    return x * cos_ref[...] + pltpu.roll(x, HEAD_DIM // TWO, 1) * sin_ref[...]


def first_kernel(x_ref, g_ref, wk_ref, wv_ref, cos_ref, sin_ref, h_ref, kv_ref):
    x = x_ref[...].astype(F32)
    h = (x * lax.rsqrt(row_mean(x * x) + NORM_EPS) * g_ref[...]).astype(BF16)
    h_ref[...] = h
    k = jnp.dot(h, wk_ref[...], preferred_element_type=F32)
    v = jnp.dot(h, wv_ref[...], preferred_element_type=F32)
    n = kv_ref.shape[THREE]
    for i in range(TWO):
        for j, val in enumerate((turn(k[:, head_slice(i)], cos_ref, sin_ref), v[:, head_slice(i)])):
            for c in range(TWO):
                kv_ref[i, c, j] = val[c * n : (c + 1) * n].astype(BF16)


def project(x, gain, w_k, w_v, cos_f, sin_f):
    n = x.shape[0] // TWO
    return pl.pallas_call(
        first_kernel,
        name="norm_kv",
        out_shape=(jax.ShapeDtypeStruct(x.shape, BF16), jax.ShapeDtypeStruct((TWO,) * THREE + (n, HEAD_DIM), BF16)),
        compiler_params=params(20),
        cost_estimate=cost(TWO, 7),
    )(x, gain, w_k, w_v, cos_f, sin_f)


def place(me):
    return me // 8, lax.rem(me // FOUR, TWO), lax.rem(me // TWO, TWO), lax.rem(me, TWO)


def dev(z, y, x, core):
    return ((z * TWO + y) * TWO + x) * TWO + core


def z_peers(z):
    return [(k, lax.rem(z + k, FOUR)) for k in (1, TWO, THREE)]


def meet(peers):
    barrier = pltpu.get_barrier_semaphore()
    for d in peers:
        pl.semaphore_signal(barrier, device_id=(d,), device_id_type=MESH)
    pl.semaphore_wait(barrier, len(peers))


def remote(src, dst, send, arrive, to):
    return pltpu.make_async_remote_copy(
        src_ref=src, dst_ref=dst, send_sem=send, recv_sem=arrive, device_id=(to,), device_id_type=MESH
    )


class Line:
    order = (0, 1, -1, TWO, -TWO, THREE, -THREE)

    def __init__(self, me):
        self.z, y, x, core = place(me)
        self.next = {1: dev(self.z + 1, y, x, core), -1: dev(self.z - 1, y, x, core)}
        self.inside = {1: self.z < THREE, -1: self.z > 0}

    def held(self, dz):
        return jnp.logical_and(self.z + dz >= 0, self.z + dz <= THREE)

    def ways(self, dz):
        for d in self.next:
            if d * dz <= 0:
                yield d, self.inside[d] if dz == 0 else jnp.logical_and(self.inside[d], self.held(dz))


def tiled(n, fetch, use, first=0):
    fetch(first, 0).start()

    @pl.loop(0, n)
    def _(t):
        slot = lax.rem(t, TWO)
        fetch(first + t, slot).wait()

        @pl.when(t + 1 < n)
        def _():
            fetch(first + t + 1, 1 - slot).start()

        use(first + t, slot)


def aligned(t, size=BLK):
    return pl.ds(pl.multiple_of(t * size, size), size)


def exchange_kernel(*refs):
    take = taker(refs)
    kv_ref, h_ref, dy_ref, pos_ref, cos_ref, sin_ref, wq_ref, wo_ref, kv_all, q_u, do_u, pos_u, *dy_rows = take(14)
    own_sem, quad_s, quad_r, z_s, z_r, y_s, y_r, q_home, do_home, wq_buf, wo_buf, w_sem, dy_sem = take(len(refs))
    me = lax.axis_index("cp")
    z, y, x, core = place(me)
    quad, line = quad_of(me), Line(me)
    across = dev(z, 1 - y, x, core)
    meet(quad[1:] + [across] + [dev(zz, y, x, core) for _, zz in z_peers(z)])

    def source(a, d):
        xx, cc = 1 - x if d // TWO else x, 1 - core if d % TWO else core
        return pos_ref.at[cc] if a == THREE else (kv_ref, q_home, do_home)[a].at[xx, cc]

    def target(a, d):
        if a == THREE:
            return pos_u.at[d]
        tok = pl.ds(d * CHUNK, CHUNK)
        return kv_all.at[me // FOUR, :, :, :, tok] if a == 0 else (q_u, do_u)[a - 1].at[:, :, tok]

    def quad_copy(a, d):
        return remote(source(a, d), target(a, d), quad_s.at[a, d], quad_r.at[a, d], quad[d])

    def own_copy(a):
        return pltpu.make_async_copy(source(a, 0), target(a, 0), own_sem.at[a])

    def z_copy(part, dz, d):
        block = kv_all.at[TWO * (z + dz) + y, part]
        return remote(block, block, z_s.at[part, (d + 1) // TWO, dz + THREE], z_r.at[part, dz - d + THREE], line.next[d])

    def y_copy(part, dz, yy=y):
        block = kv_all.at[TWO * (z + dz) + yy, part]
        return remote(block, block, y_s.at[part, dz + THREE], y_r.at[part, dz + THREE], across)

    parts = range(TWO)
    moves = [(part, dz) for dz in line.order for part in parts]

    def pass_on(count):
        for part, dz in [moves.pop(0) for _ in range(count)]:
            if dz:
                block = kv_all.at[TWO * (z + dz) + y, part]
                arrival = remote(block, block, own_sem.at[0], z_r.at[part, dz + THREE], me)
                pl.when(line.held(dz))(arrival.wait_recv)
            for d, on in line.ways(dz):
                pl.when(on)(z_copy(part, dz, d).start)
            pl.when(line.held(dz))(y_copy(part, dz).start)

    n = h_ref.shape[1] // BLK // TWO

    def fetch_q(t, slot):
        return pltpu.make_async_copy(wq_ref.at[:, aligned(t)], wq_buf.at[slot], w_sem.at[0, slot])

    def fetch_o(t, slot):
        return pltpu.make_async_copy(wo_ref.at[aligned(t)], wo_buf.at[slot], w_sem.at[1, slot])

    def put(home, t, val):
        home[t // n, :, :, :, :, aligned(lax.rem(t, n))] = val.astype(BF16).reshape(home.shape[1:-1] + (BLK,))

    def query(t, slot):
        q = jnp.dot(h_ref[...], wq_buf[slot], preferred_element_type=F32)
        put(q_home, t, jnp.hstack([turn(q[:, head_slice(j)], cos_ref, sin_ref) for j in range(BLK // HEAD_DIM)]))

    def pull(t, slot):
        put(do_home, t, dot_t(dy_ref[...], wo_buf[slot]))

    all_moves = list(moves)
    half = dy_ref.shape[0] // TWO
    for i, out in enumerate(dy_rows):
        pltpu.make_async_copy(dy_ref.at[aligned(core if i == 0 else 1 - core, half)], out, dy_sem.at[i]).start()
    for a in (0, THREE):
        for d in (1, TWO, THREE):
            quad_copy(a, d).start()
        own_copy(a).start()
    for a, (fetch, use) in enumerate(((fetch_q, query), (fetch_o, pull)), 1):
        for near in range(TWO):
            tiled(n, fetch, use, n * (x if near else 1 - x))
            for d in range(TWO):
                if d or not near:
                    quad_copy(a, d if near else d + TWO).start()
            if near:
                own_copy(a).start()
            if len(moves) == len(all_moves):
                own_copy(0).wait()
                for d in (1, TWO, THREE):
                    quad_copy(0, d).wait_recv()
            pass_on(TWO)
    pass_on(len(moves))
    for part, dz in all_moves:
        for d, on in line.ways(dz):
            pl.when(on)(z_copy(part, dz, d).wait_send)
        pl.when(line.held(dz))(y_copy(part, dz, 1 - y).wait_recv)
        pl.when(line.held(dz))(y_copy(part, dz).wait_send)
    for a in range(FOUR):
        for d in (1, TWO, THREE):
            quad_copy(a, d).wait_send()
            if a > 0:
                quad_copy(a, d).wait_recv()
    for a in (1, TWO, THREE):
        own_copy(a).wait()
    for i, out in enumerate(dy_rows):
        pltpu.make_async_copy(dy_ref.at[aligned(core if i == 0 else 1 - core, half)], out, dy_sem.at[i]).wait()


def exchange(kv, h, dy, pos, cos_f, sin_f, w_q, w_o):
    dma = pltpu.SemaphoreType.DMA
    vmem, hbm = pl.BlockSpec(memory_space=pltpu.VMEM), pl.BlockSpec(memory_space=pl.ANY)
    wide = w_q.shape[1] // TWO
    unit = jax.ShapeDtypeStruct((TWO, TWO, BLK, wide), BF16)
    pos_quad = jax.ShapeDtypeStruct((FOUR,) + pos.shape[1:], pos.dtype)
    dy_half = jax.ShapeDtypeStruct((dy.shape[0] // TWO, dy.shape[1]), BF16)
    home = pltpu.VMEM((TWO,) * FOUR + (CHUNK, wide), BF16)
    sems = [dma((FOUR,))] + [dma((FOUR, FOUR))] * TWO + [dma((TWO, TWO, 7))] + [dma((TWO, 7))] * THREE
    bufs = [pltpu.VMEM((TWO,) + b, BF16) for b in ((w_q.shape[0], BLK), (BLK, w_o.shape[1]))]
    return pl.pallas_call(
        exchange_kernel,
        name="exchange",
        out_shape=(jax.ShapeDtypeStruct((N_PAIRS,) + (TWO,) * THREE + (BLK, HEAD_DIM), BF16), unit, unit, pos_quad, dy_half, dy_half),
        in_specs=[vmem] * 6 + [hbm] * TWO,
        out_specs=[hbm] * 6,
        scratch_shapes=sems + [home, home] + bufs + [dma((TWO, TWO)), dma((TWO,))],
        compiler_params=params(63, collective_id=1),
        cost_estimate=cost(1, 20),
    )(kv, h, dy, pos, cos_f, sin_f, w_q, w_o)


def taker(refs):
    rest = iter(refs)
    return lambda count: list(itertools.islice(rest, count))


def wo_kernel(*refs):
    take = taker(refs)
    o_ref, *pieces = take(5)
    keep, away, dy_u, o_t, terms, came, load_sem, core_s, core_r = take(len(refs))
    me = lax.axis_index("cp")
    _, y, _, core = place(me)
    meet(quad_of(me)[1:TWO])
    loads = [
        pltpu.make_async_copy(src, dy_u.at[:, :, pl.ds(d * CHUNK, CHUNK)], load_sem.at[d])
        for d, src in enumerate(pieces)
    ]
    for c in loads:
        c.start()
    for h in range(N_HEADS):
        o_t[head(h)] = o_ref[:, :, :, head(h)].reshape(-1, HEAD_DIM).T
    for c in loads:
        c.wait()
    half, tiles = terms.shape[1], terms.shape[TWO] // BLK

    def swap(t):
        return remote(terms.at[0, :, aligned(t)], came.at[:, aligned(t)], core_s.at[t], core_r.at[t], quad_of(me)[1])

    def half_terms(i, to, then):
        @pl.loop(0, tiles)
        def _(t):
            dy = dy_u[:, :, :, aligned(t)].reshape(-1, BLK)
            terms[to, :, aligned(t)] = jnp.dot(o_t[aligned(i, half)], dy, preferred_element_type=F32)
            then(t)

    half_terms(1 - core, 0, lambda t: swap(t).start())
    half_terms(core, 1, lambda t: swap(t).wait_recv())
    rows = keep.shape[1]
    for zz in range(FOUR):
        for out, yy in ((keep, y), (away, 1 - y)):
            at = aligned(TWO * zz + yy, rows)
            out[zz] = terms[1, at] + came[at]
    for t in range(tiles):
        swap(t).wait_send()


def wo_terms(o, pieces):
    dma = pltpu.SemaphoreType.DMA
    vmem, hbm = pl.BlockSpec(memory_space=pltpu.VMEM), pl.BlockSpec(memory_space=pl.ANY)
    n, d, wide = o.shape[0] * o.shape[1] * o.shape[TWO], pieces[0].shape[-1], o.shape[-1]
    half = wide // TWO
    return pl.pallas_call(
        wo_kernel,
        name="wo_terms",
        out_shape=[jax.ShapeDtypeStruct((FOUR, half // N_PAIRS, d), F32)] * TWO,
        in_specs=[vmem] + [hbm] * FOUR,
        out_specs=[vmem] * TWO,
        scratch_shapes=[pltpu.VMEM((TWO, TWO, BLK, d), BF16), pltpu.VMEM((wide, n), BF16)]
        + [pltpu.VMEM((TWO, half, d), F32), pltpu.VMEM((half, d), F32), dma((FOUR,)), dma((d // BLK,)), dma((d // BLK,))],
        compiler_params=params(63, collective_id=THREE),
        cost_estimate=cost(FOUR, 20),
    )(o, *pieces)


class PairSum:
    def __init__(self, me, kind, cut, src, out, buffers, sems):
        self.me, self.kind, self.src, self.out = me, kind, src, out
        self.size = out.shape[0] // cut
        self.own, self.from_core, self.from_y, self.from_z = buffers
        self.load_sem, self.core_s, self.core_r, self.y_s, self.y_r, self.z_s, self.z_r = sems
        self.z, self.y, x, core = place(me)
        self.partner = dev(self.z, self.y, x, 1 - core)
        self.across = dev(self.z, 1 - self.y, x, core)
        self.next_z = dev(self.z + 1, self.y, x, core), dev(self.z - 1, self.y, x, core)

    def rows(self, j):
        return pl.ds(j * self.size, self.size)

    def mine(self, j, zz):
        at = self.rows(j)
        return self.own.at[zz, self.y, at] if self.kind == "core" else self.own.at[zz, at]

    def loads(self, j):
        at = self.rows(j)
        if self.kind == "z":
            pairs = zip(self.src, (self.own, self.from_y))
            return [pltpu.make_async_copy(a.at[:, at], b.at[:, at], s.at[j]) for (a, b), s in zip(pairs, (self.load_sem, self.y_r))]
        return [pltpu.make_async_copy(self.src.at[:, self.y, at], self.own.at[:, at], self.load_sem.at[j])]

    def core_copy(self, j):
        src, dst = (r.at[:, :, self.rows(j)] for r in (self.src, self.from_core))
        return remote(src, dst, self.core_s.at[j], self.core_r.at[j], self.partner)

    def y_copy(self, j):
        src = self.own if self.kind == "core" else self.src
        at = self.rows(j)
        return remote(src.at[:, 1 - self.y, at], self.from_y.at[:, at], self.y_s.at[j], self.y_r.at[j], self.across)

    def z_copy(self, j, way, zz, to):
        at = way, zz + way - 1
        return remote(self.mine(j, zz), self.from_z.at[*at, self.rows(j)], self.z_s.at[j, *at], self.z_r.at[j, *at], to)

    def begin(self, j):
        if self.kind == "core":
            self.core_copy(j).start()
            return
        for c in self.loads(j):
            c.start()
        if not self.kind:
            self.y_copy(j).start()

    def loaded(self, j):
        if self.kind != "core":
            for c in self.loads(j):
                c.wait()
        else:
            self.core_copy(j).wait_recv()
            at = self.rows(j)
            for zz in range(FOUR):
                self.own[zz, :, at] += self.from_core[zz, :, at]
            self.y_copy(j).start()
        if self.kind == "z":
            self.add_y(j)
            self.hop(j, 0)

    def add_y(self, j):
        for zz in range(FOUR):
            self.mine(j, zz)[...] += self.from_y[zz, self.rows(j)]

    def relay(self, j, way, zz, add):
        if add:
            self.z_copy(j, way, zz, self.me).wait_recv()
            self.mine(j, zz)[...] += self.from_z[way, zz + way - 1, self.rows(j)]
        self.z_copy(j, way, zz, self.next_z[way]).start()

    def hop(self, j, h):
        @pl.when(self.z == h)
        def _():
            for zz in range(THREE, h, -1):
                self.relay(j, 0, zz, h > 0)

        @pl.when(self.z == THREE - h)
        def _():
            for zz in range(THREE - h):
                self.relay(j, 1, zz, h > 0)

    def step(self, j, h):
        if h == 0 and self.kind != "z":
            self.y_copy(j).wait_recv()
            self.add_y(j)
            self.hop(j, 0)
        elif 0 < h < THREE:
            self.hop(j, h)
        elif h == THREE:
            at = self.rows(j)
            self.out[at] = self.mine(j, self.z)[...]
            for way, on in enumerate((self.z > 0, self.z < THREE)):

                @pl.when(on)
                def _(way=way):
                    self.z_copy(j, way, self.z, self.me).wait_recv()
                    self.out[at] += self.from_z[way, self.z + way - 1, at]

    def wait_send(self, j):
        if self.kind == "core":
            self.core_copy(j).wait_send()
        if self.kind != "z":
            self.y_copy(j).wait_send()
        for zz in range(FOUR):
            if zz > 0:
                pl.when(self.z < zz)(self.z_copy(j, 0, zz, self.next_z[0]).wait_send)
            if zz < THREE:
                pl.when(self.z > zz)(self.z_copy(j, 1, zz, self.next_z[1]).wait_send)

    @staticmethod
    def scratch(kind, block):
        unused = pltpu.VMEM((8, HEAD_DIM), F32)
        own = pltpu.VMEM(((FOUR, TWO) if kind == "core" else (FOUR,)) + block, F32)
        from_y = pltpu.VMEM((FOUR,) + block, F32)
        return [own, own if kind == "core" else unused, from_y, pltpu.VMEM((TWO, THREE) + block, F32)]

    @staticmethod
    def sems(*dims):
        dma = pltpu.SemaphoreType.DMA
        return [dma(dims)] * 5 + [dma(dims + (TWO, THREE))] * TWO


def reduce_kernel(cuts, kinds, work, *refs):
    n = len(cuts)

    take = taker(refs)
    ins = [take(TWO) if k == "z" else take(1)[0] for k in kinds[:-1]]
    more_in, outs, more_out, made = take(work.ins), take(n), take(work.outs), take(1)
    buffers, sems = [take(FOUR) for _ in kinds], take(7)
    me = lax.axis_index("cp")
    z, y, x, core = place(me)
    meet(quad_of(me)[1:] + [dev(z, 1 - y, x, core)] + [dev(zz, y, x, core) for _, zz in z_peers(z)])
    job = work(me, more_in, more_out, take(len(refs)))
    sums = [PairSum(me, *a, [r.at[i] for r in sems]) for i, a in enumerate(zip(kinds, cuts, ins + made, outs, buffers))]
    pieces = [(s, j) for s, cut in zip(sums, cuts) for j in range(cut)]
    early, late = pieces[: -cuts[-1]], pieces[-cuts[-1] :]
    for s, j in early:
        s.begin(j)
    for s, j in early:
        s.loaded(j)
    for t in range(len(pieces) + THREE):
        if t == MADE_AT:
            job.wq_terms(sums[-1].own, made[0])
            for s, j in late:
                s.begin(j)
        if t == MADE_AT + 1:
            for s, j in late:
                s.loaded(j)
        for h in range(FOUR):
            if 0 <= t - h < len(pieces):
                s, j = pieces[t - h]
                s.step(j, h)
        job.step(t)
    for s, j in pieces:
        s.wait_send(j)
    job.finish()


def quad_of(me):
    z, y, x, core = place(me)
    return [dev(z, y, 1 - x if d // TWO else x, 1 - core if d % TWO else core) for d in range(FOUR)]


class Home:
    def __init__(self, me, src, out, own_sem, send, arrive):
        _, _, x, core = place(me)
        w = src.shape[-1]
        to = out.at[core, :, :, :, pl.ds(x * w, w)]

        def piece(d):
            return src.at[:, :, pl.ds(d * CHUNK, CHUNK)]

        self.own = pltpu.make_async_copy(piece(0), to, own_sem)
        self.copies = [remote(piece(d), to, send.at[d], arrive.at[d], quad_of(me)[d]) for d in (1, TWO, THREE)]

    def start(self):
        self.own.start()
        for c in self.copies:
            c.start()

    def wait_recv(self):
        self.own.wait()
        for c in self.copies:
            c.wait_recv()

    def wait_send(self):
        for c in self.copies:
            c.wait_send()


class Products:
    ins, outs = 6, THREE

    def __init__(self, me, ins, outs, scratch):
        attn, self.dq, hidden, normed, self.w_o, self.w_q = ins
        self.block_out, self.d_part, self.h_u = outs
        self.attn_home, self.dq_home, self.buf_o, self.buf_q, stage, self.h_buf, *sems = scratch
        self.w_sem, self.load_sem, own_sem, quad_s, quad_r = sems
        _, _, _, core = place(me)

        def piece(d):
            return normed.at[1 - core if d % TWO else core]

        def tokens(d):
            return self.h_u.at[:, :, pl.ds(d * CHUNK, CHUNK)]

        self.h_copies = [remote(piece(d), tokens(d), quad_s.at[TWO, d], quad_r.at[TWO, d], quad_of(me)[d]) for d in (1, TWO, THREE)]
        self.h_mine = pltpu.make_async_copy(piece(0), stage, own_sem.at[TWO])
        self.h_back = pltpu.make_async_copy(stage, tokens(0), self.load_sem.at[0])
        self.residual = pltpu.make_async_copy(hidden, self.block_out, own_sem.at[THREE])
        self.residual.start()
        for c in self.h_copies:
            c.start()
        self.h_mine.start()
        self.homes = [
            Home(me, src, out, own_sem.at[i], quad_s.at[i], quad_r.at[i])
            for i, (src, out) in enumerate([(attn, self.attn_home), (self.dq, self.dq_home)])
        ]
        for h in self.homes:
            h.start()

    @staticmethod
    def scratch(arrays):
        dma, d = pltpu.SemaphoreType.DMA, arrays[-1].shape[0]
        home = pltpu.VMEM((TWO,) * THREE + (CHUNK, d), BF16)
        buf = [pltpu.VMEM((TWO,) + b, BF16) for b in ((d, BLK), (BLK, d))]
        tiles = [pltpu.VMEM((TWO, TWO) + b, BF16) for b in ((CHUNK, d), (TWO, BLK, BLK))]
        sems = [dma((TWO, TWO)), dma((TWO,)), dma((FOUR,)), dma((THREE, FOUR)), dma((THREE, FOUR))]
        return [home] * TWO + buf + tiles + sems

    @staticmethod
    def results(arrays):
        unit = TWO, TWO, BLK, arrays[-1].shape[0]
        return [jax.ShapeDtypeStruct(arrays[TWO].shape, t) for t in (BF16, F32)] + [jax.ShapeDtypeStruct(unit, BF16)]

    spaces, out_spaces = [pl.ANY, pltpu.VMEM] + [pl.ANY] * FOUR, [pltpu.VMEM] * TWO + [pl.ANY]

    def step(self, t):
        def fetch_o(t, slot):
            return pltpu.make_async_copy(self.w_o.at[:, aligned(t)], self.buf_o.at[slot], self.w_sem.at[0, slot])

        def fetch_q(t, slot):
            return pltpu.make_async_copy(self.w_q.at[aligned(t)], self.buf_q.at[slot], self.w_sem.at[1, slot])

        def project(t, slot):
            at = aligned(t)
            attn = self.attn_home[...].reshape(-1, self.w_o.shape[0])
            out = jnp.dot(attn, self.buf_o[slot], preferred_element_type=F32)
            self.block_out[:, at] = (self.block_out[:, at].astype(F32) + out).astype(BF16)

        def pull(t, slot):
            dq = self.dq_home[...].reshape(-1, self.w_o.shape[0])
            self.d_part[:, aligned(t)] = dot_t(dq, self.buf_q[slot])

        if t in PRODUCTS_AT:
            i = PRODUCTS_AT.index(t)
            self.homes[i].wait_recv()
            if i == 0:
                self.residual.wait()
            tiled(self.w_o.shape[0] // BLK, *((fetch_o, project), (fetch_q, pull))[i])

    def wq_terms(self, own, other):
        self.h_mine.wait()
        self.h_back.start()
        for c in self.h_copies:
            c.wait_recv()
        self.h_back.wait()
        core = lax.rem(lax.axis_index("cp"), TWO)
        d_out = self.dq[...].reshape(-1, self.dq.shape[-1])

        def fetch(t, slot):
            return pltpu.make_async_copy(self.h_u.at[:, :, :, aligned(t)], self.h_buf.at[slot], self.load_sem.at[slot])

        for out, half in ((other, 1 - core), (own, core)):

            def use(t, slot, out=out, half=half):
                h = self.h_buf[slot].reshape(-1, BLK)
                out[t - half * FOUR] = dot(h, d_out, (0,), (0,)).reshape(out.shape[1:])

            tiled(FOUR, fetch, use, half * FOUR)

    def finish(self):
        for c in self.h_copies + self.homes:
            c.wait_send()


class HiddenGradient:
    tiles = FOUR

    def __init__(self, me, dk, dv, ins, outs, scratch):
        self.part, self.w_k, self.w_v, self.x, self.dy, self.gain = ins
        self.dx, self.terms = outs
        self.dk_home, self.dv_home, self.rows, self.part_tile, self.part_sem, *sems = scratch
        pairs = (dk, self.dk_home), (dv, self.dv_home)
        self.homes = [Home(me, src, out, *[r.at[i] for r in sems]) for i, (src, out) in enumerate(pairs)]
        for h in self.homes:
            h.start()

    @staticmethod
    def scratch(x):
        dma = pltpu.SemaphoreType.DMA
        home = pltpu.VMEM((TWO,) * THREE + (CHUNK, TWO * HEAD_DIM), BF16)
        return [home, home, pltpu.VMEM((8, x.shape[1]), F32), pltpu.VMEM((TWO * CHUNK, x.shape[1]), F32), dma(()), dma((TWO,)), dma((TWO, FOUR)), dma((TWO, FOUR))]

    def tile(self, t):
        if t == 0:
            for h in self.homes:
                h.wait_recv()
            self.rows[...] = jnp.zeros_like(self.rows)
        size = TWO * CHUNK
        at = pl.ds(t * size, size)
        load = pltpu.make_async_copy(self.part.at[at], self.part_tile, self.part_sem)
        load.start()
        load.wait()
        d = self.part_tile[...]
        for home, w in ((self.dk_home, self.w_k), (self.dv_home, self.w_v)):
            d += dot_t(home[t // TWO, t % TWO].reshape(size, -1), w[...])
        d = d.astype(BF16).astype(F32)
        x = self.x[at].astype(F32)
        inv_rms = lax.rsqrt(row_mean(x * x) + NORM_EPS)
        unit, scaled = x * inv_rms, d * self.gain[...]
        dx = inv_rms * (scaled - unit * row_mean(scaled * unit))
        self.dx[at] = (self.dy[at].astype(F32) + dx).astype(BF16)
        self.rows[...] += jnp.sum((d * unit).reshape((-1,) + self.rows.shape), axis=0)
        if t == self.tiles - 1:
            self.terms[...] = jnp.sum(self.rows[...], axis=0, keepdims=True)

    def finish(self):
        for h in self.homes:
            h.wait_send()


def reduce_pairs(arrays, blocks, cuts, kinds, collective_id, work, more):
    vmem, hbm = pl.BlockSpec(memory_space=pltpu.VMEM), pl.BlockSpec(memory_space=pl.ANY)
    n = len(blocks)
    scratch = [pltpu.VMEM((FOUR, TWO) + blocks[-1], F32)]
    scratch += sum((PairSum.scratch(k, b) for k, b in zip(kinds, blocks)), []) + PairSum.sems(n, max(cuts))
    outs = [jax.ShapeDtypeStruct(b, F32) for b in blocks] + work.results(more)
    return pl.pallas_call(
        functools.partial(reduce_kernel, cuts, kinds, work),
        name="reduce_pairs",
        out_shape=outs,
        in_specs=[hbm] * len(arrays) + [pl.BlockSpec(memory_space=m) for m in work.spaces],
        out_specs=[vmem] * n + [pl.BlockSpec(memory_space=m) for m in work.out_spaces],
        scratch_shapes=scratch + work.scratch(more),
        compiler_params=params(63, collective_id=collective_id),
        cost_estimate=cost(1, 20),
    )(*arrays, *more)


HERE = 0, 0, 0
LINKS = "xyud"
ORDERS = "zxy", "zyx", "yxz", "zyx"
CUTS = 0, 40, 96, 128
SIZES = 7.0, 9.8, 5.6, 2.8
GAIN_AT = [60.0 + 12.0 * i for i in range(5)]
BEHIND = 4
LATENCY, TILES_FROM, TILE_EVERY = 3.0, 14.0, 8.0
SUM_AT = [25.0 + 6.0 * i for i in range(4)]


def onward(order, key):
    dz, ry, rx = key
    stage = max((order.index(a) for a, r in zip("zyx", key) if r), default=-1)
    for axis in order[stage + 1 :]:
        if axis == "x":
            yield "x", (dz, ry, 1)
        elif axis == "y":
            yield "y", (dz, 1, rx)
        else:
            yield "u", (-1, ry, rx)
            yield "d", (1, ry, rx)
    if stage >= 0 and order[stage] == "z" and abs(dz) < THREE:
        yield ("u", (dz - 1, ry, rx)) if dz < 0 else ("d", (dz + 1, ry, rx))


def arrivals():
    busy, times = {}, {}
    starts = [0.0] * THREE + [SUM_AT[-1] + LATENCY]
    here = [(t, z, part, HERE) for part, t in enumerate(starts) for z in range(FOUR)]
    while here:
        now, z, part, key = heapq.heappop(here)
        times.setdefault((part, key), []).append(now)
        for link, there in onward(ORDERS[part], key):
            to = z + {"u": 1, "d": -1}.get(link, 0)
            if 0 <= to <= THREE:
                busy[z, link] = max(busy.get((z, link), 0), now) + SIZES[part]
                heapq.heappush(here, (busy[z, link] + LATENCY, to, part, there))
    return sorted((sum(t) / len(t), *at) for at, t in times.items())


def turn_back(dkv_ref, cos_ref, sin_ref, dk_u, dv_u):
    n = TWO * TWO * BLK
    for i in range(TWO):
        for j in range(TWO):
            cos_t, sin_t = (jnp.hstack([t, t * sign]) for t, sign in ((cos_ref[i, j].T, 1), (sin_ref[i, j].T, -1)))
            dk = dkv_ref[pl.ds((i * TWO + j) * BLK, BLK)] * ATTN_SCALE
            dk_u[i, j] = (dk * cos_t + pltpu.roll(dk, HEAD_DIM // TWO, 1) * sin_t).astype(BF16)
    dv_u[...] = dkv_ref[pl.ds(n, n)].astype(BF16).reshape(dv_u.shape)


def wkv_terms(h_own, dk_u, dv_u, outs):
    d_out = jnp.hstack([r[...].reshape(-1, HEAD_DIM) for r in (dk_u, dv_u)])
    for out, half in outs:

        @pl.loop(0, FOUR)
        def _(zz, out=out, half=half):
            h = h_own[:, :, :, aligned(half * FOUR + zz)].reshape(-1, BLK)
            out[zz] = dot(h, d_out, (0,), (0,)).reshape(out.shape[1:])


def gather_kernel(*refs):
    take = taker(refs)
    wo_ref, wq_ref, dkv_ref, cos_ref, sin_ref, h_ref = take(6)
    grad_ins, outs, (dx_ref, dgain_ref) = take(6), take(FOUR), take(TWO)
    own_sem, send_sem, come_sem, core_sem, put_sem, all_terms, totals, g_s, g_r = take(9)
    terms, wkv_ref, h_own, dk_u, dv_u, store, wkv_store = take(7)
    buffers, sems, refs = take(FOUR), take(7), take(len(refs))
    me = lax.axis_index("cp")
    z, y, x, core = place(me)
    line = Line(me)
    to = {"x": dev(z, y, 1 - x, core), "y": dev(z, 1 - y, x, core), "u": line.next[1], "d": line.next[-1]}
    partner = dev(z, y, x, 1 - core)
    chip_here = me // TWO
    n_wo, wide = wo_ref.shape[0], wq_ref.shape[1]
    store[core, chip_here, pl.ds(0, n_wo)] = wo_ref[...]
    for i in range(TWO):
        store[core, chip_here, pl.ds(n_wo, n_wo), pl.ds(i * wide, wide)] = wq_ref[pl.ds(i * n_wo, n_wo)]
    meet(quad_of(me)[1:] + [to["y"]] + [dev(zz, y, x, core) for _, zz in z_peers(z)])
    load_h = pltpu.make_async_copy(h_ref, h_own, own_sem.at[0])
    load_h.start()
    wkv = PairSum(me, "core", 1, wkv_ref, wkv_store.at[core, chip_here], buffers, [r.at[0] for r in sems])

    def place_of(key):
        dz, ry, rx = key
        return z + dz, 1 - y if ry else y, 1 - x if rx else x

    def block(part, key, cc=core):
        zz, yy, xx = place_of(key)
        chip = (TWO * zz + yy) * TWO + xx
        return wkv_store.at[cc, chip] if part == THREE else store.at[cc, chip, pl.ds(CUTS[part], CUTS[part + 1] - CUTS[part])]

    def windows(part, key, cc):
        zz, yy, xx = place_of(key)
        pair, src = TWO * zz + yy, block(part, key, cc)
        wo_at, wq_at = ((xx * TWO + cc) * N_PAIRS + pair) * n_wo, (cc * N_PAIRS + pair) * wq_ref.shape[0]
        if part == THREE:
            for i, out in enumerate(outs[TWO:]):
                yield src.at[:, head(i)], out.at[pl.ds(wq_at, wq_ref.shape[0]), pl.ds(xx * HEAD_DIM, HEAD_DIM)]
            return
        first, last = CUTS[part : part + TWO]
        if first < n_wo:
            rows = min(last, n_wo) - first
            yield src.at[pl.ds(0, rows)], outs[0].at[pl.ds(wo_at + first, rows)]
        if last > n_wo:
            skip = max(n_wo - first, 0)
            rows, at = last - first - skip, first + skip - n_wo
            for i in range(TWO):
                window = outs[1].at[pl.ds(wq_at + i * n_wo + at, rows), pl.ds(xx * wide, wide)]
                yield src.at[pl.ds(skip, rows), pl.ds(i * wide, wide)], window

    def index(part, key):
        return (part, key[0] + THREE) + key[1:]

    def send(part, key, link, there):
        sent = send_sem.at[index(part, key) + (LINKS.find(link or "-") + 1,)]
        arrive, device = (come_sem.at[index(part, there)], to[link]) if link else (core_sem.at[index(part, key)], partner)
        remote(block(part, key), block(part, key), sent, arrive, device).start()
        if not link:
            put(part, key, core)

    def put(part, key, cc):
        for src, window in windows(part, key, cc):
            pltpu.make_async_copy(src, window, put_sem.at[(cc,) + index(part, key)]).start()

    def put_other(part, key):
        whole(part, own_sem.at[0], core_sem.at[index(part, key)]).wait_recv()
        put(part, key, 1 - core)

    def whole(part, send, arrive):
        size = CUTS[part + 1] - CUTS[part] if part < THREE else wq_ref.shape[0] * TWO * HEAD_DIM // outs[0].shape[1]
        dst = outs[0].at[pl.ds(0, size)]
        return remote(dst, dst, send, arrive, me)

    def when(on, do):
        pl.when(on)(do)

    def each_way(part, key):
        held = line.held(key[0])
        yield None, key, held
        for link, there in onward(ORDERS[part], key):
            inside = {"u": line.inside[1], "d": line.inside[-1]}.get(link)
            yield link, there, held if inside is None else jnp.logical_and(held, inside)

    def pass_on(part, key):
        for link, there, on in each_way(part, key):
            when(on, functools.partial(send, part, key, link, there))

    def term_copy(i):
        src = terms if i == 0 else totals.at[i - 1]
        return remote(src, all_terms.at[i], g_s.at[i], g_r.at[i], me ^ (1 << i))

    def add_terms(i):
        term_copy(i).wait_recv()
        totals[i] = (terms[...] if i == 0 else totals[i - 1]) + all_terms[i]
        if i + 1 < len(GAIN_AT):
            term_copy(i + 1).start()

    def tile(t):
        job.tile(t)
        if t == job.tiles - 1:
            term_copy(0).start()

    def sum_step(h):
        wkv.step(0, h)

    steps = [(TILES_FROM + t * TILE_EVERY, functools.partial(tile, t)) for t in range(HiddenGradient.tiles)]
    steps += [(at, functools.partial(sum_step, h)) for h, at in enumerate(SUM_AT)]
    steps += [(at, functools.partial(add_terms, i)) for i, at in enumerate(GAIN_AT)]
    steps.sort(key=lambda s: s[0])
    events = arrivals()
    for part in range(THREE):
        pass_on(part, HERE)
    turn_back(dkv_ref, cos_ref, sin_ref, dk_u, dv_u)
    job = HiddenGradient(me, dk_u, dv_u, grad_ins, (dx_ref, terms), refs)
    load_h.wait()
    wkv_terms(h_own, dk_u, dv_u, ((wkv_ref, 1 - core), (buffers[0], core)))
    wkv.begin(0)
    wkv.loaded(0)
    waiting = [(part, HERE) for part in range(THREE)]
    for now, part, key in events:
        while steps and steps[0][0] <= now:
            steps.pop(0)[1]()
        if any(key):
            arrive = come_sem.at[index(part, key)]
            when(line.held(key[0]), whole(part, own_sem.at[0], arrive).wait_recv)
        if any(key) or part == THREE:
            pass_on(part, key)
            waiting.append((part, key))
        if len(waiting) > BEHIND:
            at = waiting.pop(0)
            when(line.held(at[1][0]), functools.partial(put_other, *at))
    for at in waiting:
        when(line.held(at[1][0]), functools.partial(put_other, *at))
    dgain_ref[...] = totals[len(GAIN_AT) - 1]
    for i in range(len(GAIN_AT)):
        term_copy(i).wait_send()
    for _, part, key in events:
        for cc in range(TWO):
            when(line.held(key[0]), whole(part, own_sem.at[0], put_sem.at[(cc,) + index(part, key)]).wait_recv)
        for link, there, on in each_way(part, key):
            sent = send_sem.at[index(part, key) + (LINKS.find(link or "-") + 1,)]
            when(on, whole(part, sent, own_sem.at[0]).wait_send)
    wkv.wait_send(0)
    job.finish()


def gather_all(wo, wq, dkv, cos_f, sin_f, h_u, part, w_k, w_v, x, dy, gain, shapes):
    dma = pltpu.SemaphoreType.DMA
    vmem, hbm = pl.BlockSpec(memory_space=pltpu.VMEM), pl.BlockSpec(memory_space=pl.ANY)
    block = w_k.shape[0] // TWO // N_PAIRS, w_k.shape[1]
    parts = len(ORDERS)
    keys = (parts, 7, TWO, TWO)
    terms = 1, x.shape[1]
    scratch = [dma((1,)), dma(keys + (len(LINKS) + 1,)), dma(keys), dma(keys), dma((TWO,) + keys)]
    n = len(GAIN_AT)
    scratch += [pltpu.VMEM((n,) + terms, F32)] * TWO + [dma((n,)), dma((n,)), pltpu.VMEM(terms, F32)]
    scratch += [pltpu.VMEM((FOUR, TWO) + block, F32), pltpu.VMEM(h_u.shape, BF16)]
    scratch += [pltpu.VMEM((TWO, TWO, BLK, HEAD_DIM), BF16)] * TWO
    scratch += [pltpu.VMEM((TWO, TWO * N_PAIRS) + b, F32) for b in ((TWO * wo.shape[0], wo.shape[1]), block)]
    return pl.pallas_call(
        gather_kernel,
        name="gather_all",
        out_shape=[jax.ShapeDtypeStruct(s, F32) for s in shapes]
        + [jax.ShapeDtypeStruct(x.shape, BF16), jax.ShapeDtypeStruct(terms, F32)],
        in_specs=[vmem] * 5 + [hbm] * TWO + [vmem] * 5,
        out_specs=[hbm] * len(shapes) + [vmem] * TWO,
        scratch_shapes=scratch + PairSum.scratch("core", block) + PairSum.sems(1, 1) + HiddenGradient.scratch(x),
        compiler_params=params(63, collective_id=0),
        cost_estimate=cost(1, 76),
    )(wo, wq, dkv, cos_f, sin_f, h_u, part, w_k, w_v, x, dy, gain)


def perm(x, pairs):
    return lax.ppermute(x, "cp", pairs)


def flip_pairs(d):
    return [(r, r ^ d) for r in range(32)]


def solution(mesh):
    def local_step(hidden, grad_out, positions, seg_ids, w_q, w_k, w_v, w_o, norm_gain):
        n_batch, n_tok, d_model = hidden.shape
        n_rows = n_batch * n_tok
        wide = N_HEADS * HEAD_DIM
        me = lax.axis_index("cp")
        z, y, x, core = place(me)
        quad, pair = me % FOUR, me // FOUR
        relations = range(FOUR)

        def swap(pieces):
            return [perm(p, flip_pairs(d)) if d else p for d, p in enumerate(pieces)]

        gain = norm_gain.astype(F32)
        cos_t, sin_t = rope_tables(positions.reshape(n_rows))
        cos_f, sin_f = jnp.hstack([cos_t, cos_t]), jnp.hstack([-sin_t, sin_t])
        dy_flat = grad_out.reshape(n_rows, d_model)
        normed, kv_home = project(hidden.reshape(n_rows, d_model), gain[NEW], w_k, w_v, cos_f, sin_f)
        pos = jnp.pad(positions.reshape(TWO, TWO, n_tok), ((0, 0), (0, 6), (0, 0)))
        kv_home = kv_home.reshape((TWO,) * 5 + (CHUNK, HEAD_DIM))
        kv_all, q_u, do_u, pos_u, *dy_rows = exchange(kv_home, normed, dy_flat, pos, cos_f, sin_f, w_q, w_o)
        pos_u = pos_u[:, :TWO].reshape((FOUR, TWO, TWO, CHUNK)).transpose(1, TWO, 0, THREE).reshape(TWO, TWO, BLK)
        dy_rows = [a.reshape(TWO, TWO, CHUNK, d_model) for a in dy_rows]
        dy_pieces = swap([dy_rows[d % TWO] for d in relations])

        member = quad ^ jnp.arange(FOUR)
        front, back = ((m[:, NEW] * CHUNK + jnp.arange(CHUNK)[NEW]).reshape(BLK) for m in (member, THREE - member))
        offsets = jnp.stack([front, back]).astype(jnp.int32)
        own_super = jnp.stack([pair, N_SUPER - 1 - pair]).astype(jnp.int32)
        q_index = own_super[:, NEW] * BLK + offsets
        start = q_index[NEW] - pos_u
        tab = jnp.concatenate(
            [own_super, (jnp.min(start, axis=-1) // BLK).reshape(-1), jnp.max(start, axis=-1).reshape(-1)]
        )
        start_r = start[:, :, NEW, :]
        q_index_r = jnp.broadcast_to(q_index[NEW, :, NEW, :], start_r.shape)
        cos_u, sin_u = rope_tables(pos_u)
        cos_ut, sin_ut = jnp.swapaxes(cos_u, TWO, THREE), jnp.swapaxes(sin_u, TWO, THREE)

        koff = offsets[:, NEW]
        attn_u, lse = flash_fwd(tab, q_u, kv_all, start_r, q_index_r, koff)

        wo_keep, wo_away = wo_terms(attn_u, dy_pieces)
        wo_come = perm(wo_away, flip_pairs(FOUR))
        do_u, wo_keep = lax.optimization_barrier((do_u, wo_keep))
        dq_u, dkv = flash_bwd(tab, q_u, do_u, attn_u, kv_all, lse, start_r, q_index_r, koff, cos_ut, sin_ut)

        x_flat = hidden.reshape(n_rows, d_model)
        wo_own, dkv_own, wq_own, block_out, d_part, h_u = reduce_pairs(
            [wo_keep, wo_come, dkv.reshape(FOUR, TWO, -1, HEAD_DIM)],
            [wo_keep.shape[1:], (dkv.size // N_PAIRS // HEAD_DIM, HEAD_DIM), (d_model // TWO // N_PAIRS, wide)],
            (TWO, 8, 8),
            ("z", "", "core"),
            TWO,
            Products,
            (attn_u, dq_u, x_flat, normed.reshape((TWO,) * THREE + (CHUNK, d_model)), w_o, w_q),
        )
        grad_wo, grad_wq, grad_wk, grad_wv, grad_x, d_gain = gather_all(
            wo_own,
            wq_own,
            dkv_own,
            cos_ut,
            sin_ut,
            h_u,
            d_part,
            w_k,
            w_v,
            x_flat,
            dy_flat,
            gain[NEW],
            [w_o.shape, w_q.shape, w_k.shape, w_v.shape],
        )
        block_out, grad_x = (a.reshape(hidden.shape) for a in (block_out, grad_x))
        return block_out, grad_x, grad_wq, grad_wk, grad_wv, grad_wo, d_gain.reshape(d_model)

    seq_spec = P(None, "cp", None)
    tok_spec = P(None, "cp")
    full_spec = P()
    return jax.shard_map(
        local_step,
        mesh=mesh,
        in_specs=(seq_spec, seq_spec, tok_spec, tok_spec, full_spec, full_spec, full_spec, full_spec, full_spec),
        out_specs=(seq_spec, seq_spec, full_spec, full_spec, full_spec, full_spec, full_spec),
        check_vma=False,
    )
```

```python
import functools
import heapq
import itertools

import jax
import jax.numpy as jnp
from jax import lax
from jax.experimental import pallas as pl
from jax.experimental.pallas import tpu as pltpu
from jax.sharding import PartitionSpec as P

HEAD_DIM = 128
NORM_EPS = 1e-5
ROPE_BASE = 500000.0
NEG_BIG = -1e30
LOG2E = 1.4426950408889634
ATTN_SCALE = HEAD_DIM**-0.5
EXP2_SCALE = ATTN_SCALE * LOG2E
CHUNK = 64
TWO = 2
THREE = 3
FOUR = 4
NEW = jnp.newaxis
BLK = 4 * CHUNK
N_HEADS = 8
N_PAIRS = 8
N_SUPER = 2 * N_PAIRS
MESH = pl.DeviceIdType.MESH
ONE = pl.Squeezed()
GROUP = 4
DIRECT = 2
MADE_AT = 5
PRODUCTS_AT = 7, 9
F32 = jnp.float32
BF16 = jnp.bfloat16

T_SQ, T_LO, T_MX = 0, 2, 6


def rope_tables(positions):
    inv_freq = ROPE_BASE ** (-jnp.arange(0, HEAD_DIM, TWO).astype(F32) / HEAD_DIM)
    angles = positions.astype(F32)[..., None] * inv_freq
    return jnp.cos(angles), jnp.sin(angles)


def dot(a, b, ca, cb):
    return lax.dot_general(a, b, ((ca, cb), ((), ())), preferred_element_type=F32)


def cost(gflop, mib):
    return pl.CostEstimate(flops=gflop * 10**9, bytes_accessed=mib << 20, transcendentals=0)


def params(mib, **more):
    return pltpu.CompilerParams(vmem_limit_bytes=mib << 20, **more)


def row_mean(x):
    return jnp.mean(x, axis=-1, keepdims=True)


def head(h):
    return pl.ds(h * HEAD_DIM, HEAD_DIM)


def head_slice(h):
    return slice(h * HEAD_DIM, (h + 1) * HEAD_DIM)


def dot_t(a, b):
    return dot(a, b, (1,), (1,))


def steps(tab, body):
    b, hf = pl.program_id(0), pl.program_id(1)
    own, first, last_start = tab[T_SQ + hf], tab[T_LO + TWO * b + hf], tab[T_MX + TWO * b + hf]

    def step(s, carry):
        late = s >= N_PAIRS
        at = jnp.where(late, N_SUPER - 1 - s, s), late.astype(jnp.int32)
        full = jnp.logical_and(s < own, s * BLK >= last_start)
        pl.when(full)(lambda: body(s, at, False))
        pl.when(jnp.logical_not(full))(lambda: body(s, at, True))
        return carry

    lax.fori_loop(first, own + 1, step, 0)


def down(row, n):
    return jnp.broadcast_to(row, (n, row.shape[-1])).T


def may_use(s, off, st_ref, qi_ref):
    return jnp.logical_and(off >= st_ref[...] - s * BLK, off <= qi_ref[...] - s * BLK)


def fwd_kernel(tab, q_ref, kv_ref, st_ref, qi_ref, ko_ref, o_ref, lse_ref, q_s, acc, m_s, l_s, k_t, bounds):
    m_s[...] = jnp.full_like(m_s, NEG_BIG)
    l_s[...] = jnp.zeros_like(l_s)
    acc[...] = jnp.zeros_like(acc)
    for i, ref in enumerate((st_ref, qi_ref)):
        bounds[i] = down(ref[...], HEAD_DIM)
    for h in range(N_HEADS):
        q_s[pl.ds(h * BLK, BLK)] = q_ref[:, head(h)]

    @pl.when(pl.program_id(1) == 0)
    def _():
        @pl.loop(0, N_PAIRS)
        def _(pair):
            for hk in range(TWO):
                k_t[pair, hk] = kv_ref[pair, 0, hk].T

    def body(s, at, masked):
        pair, hk = at
        v = kv_ref[pair, 1, hk]
        if masked:
            off = ko_ref[hk] + s * BLK
            mask = [
                jnp.logical_and(off[:, lanes] >= bounds[0], off[:, lanes] <= bounds[1])
                for lanes in (slice(HEAD_DIM), slice(HEAD_DIM, BLK))
            ]
            mask = [jnp.concatenate([m, m], axis=0) for m in mask]
        for g in range(N_HEADS // TWO):
            rows = pl.ds(g * TWO * BLK, TWO * BLK)
            sc = jnp.dot(q_s[rows], k_t[pair, hk], preferred_element_type=F32)
            sc = [sc[:, :HEAD_DIM], sc[:, HEAD_DIM:]]
            if masked:
                sc = [jnp.where(m, x, NEG_BIG) for m, x in zip(mask, sc)]
            m_old = m_s[rows]
            m_new = jnp.maximum(m_old, jnp.max(jnp.maximum(*sc), axis=1, keepdims=True))
            alpha = jnp.exp2((m_old - m_new) * EXP2_SCALE)
            p = [jnp.exp2((x - m_new) * EXP2_SCALE) for x in sc]
            m_s[rows] = m_new
            l_s[rows] = l_s[rows] * alpha + (p[0] + p[1])
            p = jnp.hstack([x.astype(BF16) for x in p])
            acc[rows] = acc[rows] * alpha + jnp.dot(p, v, preferred_element_type=F32)

    steps(tab, body)
    for h in range(N_HEADS):
        rows = pl.ds(h * BLK, BLK)
        total = jnp.sum(l_s[rows], axis=1, keepdims=True)
        o_ref[:, head(h)] = (acc[rows] / total).astype(BF16)
        lse_ref[h] = (m_s[rows] * EXP2_SCALE + jnp.log2(total)).T[:1]


def bwd_kernel(tab, q_ref, do_ref, o_ref, kv_ref, lse_ref, st_ref, qi_ref, ko_ref, cos_ref, sin_ref, dq_ref, dkv_ref, *scratch):
    dq_acc, delta, off_s, q_s, do_s, q_t, do_t, p_s, ds_s = scratch
    dq_acc[...] = jnp.zeros_like(dq_acc)
    for h in range(N_HEADS):
        q, do = q_ref[:, head(h)], do_ref[:, head(h)]
        delta[h] = jnp.sum((do.astype(F32) * o_ref[:, head(h)].astype(F32)).T, axis=0, keepdims=True)
        q_s[pl.ds(h * BLK, BLK)], do_s[pl.ds(h * BLK, BLK)] = q, do
        q_t[h], do_t[h] = q.T, do.T

    @pl.when(pl.program_id(1) == 0)
    def _():
        dkv_ref[...] = jnp.zeros_like(dkv_ref)
        for hk in range(TWO):
            off_s[hk] = down(ko_ref[hk], BLK)

    def body(s, at, masked):
        pair, hk = at
        k = kv_ref[pair, 0, hk]
        v = kv_ref[pair, 1, hk]
        k_t = k.T
        mask = may_use(s, off_s[hk], st_ref, qi_ref) if masked else None
        for first in range(0, N_HEADS, GROUP):
            rows = pl.ds(first * BLK, GROUP * BLK)
            for h in range(first, first + GROUP):
                cols = pl.ds(h * BLK, BLK)
                p = jnp.exp2(jnp.dot(k, q_t[h], preferred_element_type=F32) * EXP2_SCALE - lse_ref[h])
                if masked:
                    p = jnp.where(mask, p, 0.0)
                ds = p * (jnp.dot(v, do_t[h], preferred_element_type=F32) - delta[h])
                p_s[:, cols] = p.astype(BF16)
                ds_s[:, cols] = ds.astype(BF16)
            dkv_ref[pair, 0, hk] += jnp.dot(ds_s[:, rows], q_s[rows], preferred_element_type=F32)
            dkv_ref[pair, 1, hk] += jnp.dot(p_s[:, rows], do_s[rows], preferred_element_type=F32)
            dq_acc[:, rows] += jnp.dot(k_t, ds_s[:, rows], preferred_element_type=F32)

    steps(tab, body)
    cos_t, sin_t = cos_ref[...], sin_ref[...]
    half = HEAD_DIM // TWO
    for h in range(N_HEADS):
        cols = pl.ds(h * BLK, BLK)
        a, c = dq_acc[:half, cols] * ATTN_SCALE, dq_acc[half:, cols] * ATTN_SCALE
        lin = jnp.concatenate([a * cos_t + c * sin_t, c * cos_t - a * sin_t], axis=0)
        dq_ref[:, head(h)] = lin.T.astype(BF16)


def attn_specs():
    def at_tile(b, h, t):
        return (b, h) + (0,) * TWO

    def at_row(b, h, t):
        return (0, 0, b) + (0,) * THREE

    tile = pl.BlockSpec((ONE, ONE, BLK, N_HEADS * HEAD_DIM), at_tile)
    row = pl.BlockSpec((ONE, ONE, 1, BLK), at_tile)
    stat = pl.BlockSpec((ONE, ONE, N_HEADS, 1, BLK), lambda b, h, t: (b, h) + (0,) * THREE)
    rope = pl.BlockSpec((ONE, ONE, HEAD_DIM // TWO, BLK), at_tile)
    kv = pl.BlockSpec((N_PAIRS, TWO, ONE, TWO, BLK, HEAD_DIM), at_row)
    ko = pl.BlockSpec((TWO, 1, BLK), lambda b, h, t: (0,) * THREE)
    return tile, row, stat, kv, ko, rope


def flash_fwd(tab, q, kv, start, qidx, koff):
    tile, row, stat, kvs, ko, _ = attn_specs()
    return pl.pallas_call(
        fwd_kernel,
        name="attn_fwd",
        out_shape=(jax.ShapeDtypeStruct(q.shape, BF16), jax.ShapeDtypeStruct((TWO, TWO, N_HEADS, 1, BLK), F32)),
        grid_spec=pltpu.PrefetchScalarGridSpec(
            num_scalar_prefetch=1,
            grid=(TWO, TWO),
            in_specs=[tile, kvs, row, row, ko],
            out_specs=[tile, stat],
            scratch_shapes=[pltpu.VMEM((N_HEADS * BLK, HEAD_DIM), t) for t in (BF16, F32, F32, F32)]
            + [pltpu.VMEM((N_PAIRS, TWO, HEAD_DIM, BLK), BF16), pltpu.VMEM((TWO, BLK, HEAD_DIM), jnp.int32)],
        ),
        compiler_params=params(63),
        cost_estimate=cost(20, 16),
    )(tab, q, kv, start, qidx, koff)


def flash_bwd(tab, q, do, o, kv, lse, start, qidx, koff, cos_t, sin_t):
    tile, row, stat, kvs, ko, rope = attn_specs()
    return pl.pallas_call(
        bwd_kernel,
        name="attn_bwd",
        out_shape=(
            jax.ShapeDtypeStruct(q.shape, BF16),
            jax.ShapeDtypeStruct(kv.shape, F32),
        ),
        grid_spec=pltpu.PrefetchScalarGridSpec(
            num_scalar_prefetch=1,
            grid=(TWO, TWO),
            in_specs=[tile, tile, tile, kvs, stat, row, row, ko, rope, rope],
            out_specs=[tile, kvs],
            scratch_shapes=[pltpu.VMEM((HEAD_DIM, N_HEADS * BLK), F32), pltpu.VMEM((N_HEADS, 1, BLK), F32)]
            + [pltpu.VMEM((TWO, BLK, BLK), jnp.int32)]
            + [pltpu.VMEM((N_HEADS * BLK, HEAD_DIM), BF16)] * TWO
            + [pltpu.VMEM((N_HEADS, HEAD_DIM, BLK), BF16)] * TWO
            + [pltpu.VMEM((BLK, N_HEADS * BLK), BF16)] * TWO,
        ),
        compiler_params=params(63),
        cost_estimate=cost(50, 32),
    )(tab, q, do, o, kv, lse, start, qidx, koff, cos_t, sin_t)


def turn(x, cos_ref, sin_ref):
    return x * cos_ref[...] + pltpu.roll(x, HEAD_DIM // TWO, 1) * sin_ref[...]


def first_kernel(x_ref, g_ref, wk_ref, wv_ref, cos_ref, sin_ref, h_ref, kv_ref):
    x = x_ref[...].astype(F32)
    h = (x * lax.rsqrt(row_mean(x * x) + NORM_EPS) * g_ref[...]).astype(BF16)
    h_ref[...] = h
    k = jnp.dot(h, wk_ref[...], preferred_element_type=F32)
    v = jnp.dot(h, wv_ref[...], preferred_element_type=F32)
    n = kv_ref.shape[THREE]
    for i in range(TWO):
        for j, val in enumerate((turn(k[:, head_slice(i)], cos_ref, sin_ref), v[:, head_slice(i)])):
            for c in range(TWO):
                kv_ref[i, c, j] = val[c * n : (c + 1) * n].astype(BF16)


def project(x, gain, w_k, w_v, cos_f, sin_f):
    n = x.shape[0] // TWO
    return pl.pallas_call(
        first_kernel,
        name="norm_kv",
        out_shape=(jax.ShapeDtypeStruct(x.shape, BF16), jax.ShapeDtypeStruct((TWO,) * THREE + (n, HEAD_DIM), BF16)),
        compiler_params=params(20),
        cost_estimate=cost(TWO, 7),
    )(x, gain, w_k, w_v, cos_f, sin_f)


def place(me):
    return me // 8, lax.rem(me // FOUR, TWO), lax.rem(me // TWO, TWO), lax.rem(me, TWO)


def dev(z, y, x, core):
    return ((z * TWO + y) * TWO + x) * TWO + core


def z_peers(z):
    return [(k, lax.rem(z + k, FOUR)) for k in (1, TWO, THREE)]


def meet(peers):
    barrier = pltpu.get_barrier_semaphore()
    for d in peers:
        pl.semaphore_signal(barrier, device_id=(d,), device_id_type=MESH)
    pl.semaphore_wait(barrier, len(peers))


def remote(src, dst, send, arrive, to):
    return pltpu.make_async_remote_copy(
        src_ref=src, dst_ref=dst, send_sem=send, recv_sem=arrive, device_id=(to,), device_id_type=MESH
    )


class Line:
    order = (0, 1, -1, TWO, -TWO, THREE, -THREE)

    def __init__(self, me):
        self.z, y, x, core = place(me)
        self.next = {1: dev(self.z + 1, y, x, core), -1: dev(self.z - 1, y, x, core)}
        self.inside = {1: self.z < THREE, -1: self.z > 0}

    def held(self, dz):
        return jnp.logical_and(self.z + dz >= 0, self.z + dz <= THREE)

    def ways(self, dz):
        for d in self.next:
            if d * dz <= 0:
                yield d, self.inside[d] if dz == 0 else jnp.logical_and(self.inside[d], self.held(dz))


def tiled(n, fetch, use, first=0):
    fetch(first, 0).start()

    @pl.loop(0, n)
    def _(t):
        slot = lax.rem(t, TWO)
        fetch(first + t, slot).wait()

        @pl.when(t + 1 < n)
        def _():
            fetch(first + t + 1, 1 - slot).start()

        use(first + t, slot)


def aligned(t, size=BLK):
    return pl.ds(pl.multiple_of(t * size, size), size)


def exchange_kernel(*refs):
    take = taker(refs)
    kv_ref, h_ref, dy_ref, pos_ref, cos_ref, sin_ref, wq_ref, wo_ref, kv_all, q_u, do_u, pos_u, *dy_rows = take(14)
    own_sem, quad_s, quad_r, z_s, z_r, y_s, y_r, q_home, do_home, wq_buf, wo_buf, w_sem, dy_sem = take(len(refs))
    me = lax.axis_index("cp")
    z, y, x, core = place(me)
    quad, line = quad_of(me), Line(me)
    across = dev(z, 1 - y, x, core)
    meet(quad[1:] + [across] + [dev(zz, y, x, core) for _, zz in z_peers(z)])

    def source(a, d):
        xx, cc = 1 - x if d // TWO else x, 1 - core if d % TWO else core
        return pos_ref.at[cc] if a == THREE else (kv_ref, q_home, do_home)[a].at[xx, cc]

    def target(a, d):
        if a == THREE:
            return pos_u.at[d]
        tok = pl.ds(d * CHUNK, CHUNK)
        return kv_all.at[me // FOUR, :, :, :, tok] if a == 0 else (q_u, do_u)[a - 1].at[:, :, tok]

    def quad_copy(a, d):
        return remote(source(a, d), target(a, d), quad_s.at[a, d], quad_r.at[a, d], quad[d])

    def own_copy(a):
        return pltpu.make_async_copy(source(a, 0), target(a, 0), own_sem.at[a])

    def z_copy(part, dz, d):
        block = kv_all.at[TWO * (z + dz) + y, part]
        return remote(block, block, z_s.at[part, (d + 1) // TWO, dz + THREE], z_r.at[part, dz - d + THREE], line.next[d])

    def y_copy(part, dz, yy=y):
        block = kv_all.at[TWO * (z + dz) + yy, part]
        return remote(block, block, y_s.at[part, dz + THREE], y_r.at[part, dz + THREE], across)

    parts = range(TWO)
    moves = [(part, dz) for dz in line.order for part in parts]

    def pass_on(count):
        for part, dz in [moves.pop(0) for _ in range(count)]:
            if dz:
                block = kv_all.at[TWO * (z + dz) + y, part]
                arrival = remote(block, block, own_sem.at[0], z_r.at[part, dz + THREE], me)
                pl.when(line.held(dz))(arrival.wait_recv)
            for d, on in line.ways(dz):
                pl.when(on)(z_copy(part, dz, d).start)
            pl.when(line.held(dz))(y_copy(part, dz).start)

    n = h_ref.shape[1] // BLK // TWO

    def fetch_q(t, slot):
        return pltpu.make_async_copy(wq_ref.at[:, aligned(t)], wq_buf.at[slot], w_sem.at[0, slot])

    def fetch_o(t, slot):
        return pltpu.make_async_copy(wo_ref.at[aligned(t)], wo_buf.at[slot], w_sem.at[1, slot])

    def put(home, t, val):
        home[t // n, :, :, :, :, aligned(lax.rem(t, n))] = val.astype(BF16).reshape(home.shape[1:-1] + (BLK,))

    def query(t, slot):
        q = jnp.dot(h_ref[...], wq_buf[slot], preferred_element_type=F32)
        put(q_home, t, jnp.hstack([turn(q[:, head_slice(j)], cos_ref, sin_ref) for j in range(BLK // HEAD_DIM)]))

    def pull(t, slot):
        put(do_home, t, dot_t(dy_ref[...], wo_buf[slot]))

    all_moves = list(moves)
    half = dy_ref.shape[0] // TWO
    for i, out in enumerate(dy_rows):
        pltpu.make_async_copy(dy_ref.at[aligned(core if i == 0 else 1 - core, half)], out, dy_sem.at[i]).start()
    for a in (0, THREE):
        for d in (1, TWO, THREE):
            quad_copy(a, d).start()
        own_copy(a).start()
    for a, (fetch, use) in enumerate(((fetch_q, query), (fetch_o, pull)), 1):
        for near in range(TWO):
            tiled(n, fetch, use, n * (x if near else 1 - x))
            for d in range(TWO):
                if d or not near:
                    quad_copy(a, d if near else d + TWO).start()
            if near:
                own_copy(a).start()
            if len(moves) == len(all_moves):
                own_copy(0).wait()
                for d in (1, TWO, THREE):
                    quad_copy(0, d).wait_recv()
            pass_on(TWO)
    pass_on(len(moves))
    for part, dz in all_moves:
        for d, on in line.ways(dz):
            pl.when(on)(z_copy(part, dz, d).wait_send)
        pl.when(line.held(dz))(y_copy(part, dz, 1 - y).wait_recv)
        pl.when(line.held(dz))(y_copy(part, dz).wait_send)
    for a in range(FOUR):
        for d in (1, TWO, THREE):
            quad_copy(a, d).wait_send()
            if a > 0:
                quad_copy(a, d).wait_recv()
    for a in (1, TWO, THREE):
        own_copy(a).wait()
    for i, out in enumerate(dy_rows):
        pltpu.make_async_copy(dy_ref.at[aligned(core if i == 0 else 1 - core, half)], out, dy_sem.at[i]).wait()


def exchange(kv, h, dy, pos, cos_f, sin_f, w_q, w_o):
    dma = pltpu.SemaphoreType.DMA
    vmem, hbm = pl.BlockSpec(memory_space=pltpu.VMEM), pl.BlockSpec(memory_space=pl.ANY)
    wide = w_q.shape[1] // TWO
    unit = jax.ShapeDtypeStruct((TWO, TWO, BLK, wide), BF16)
    pos_quad = jax.ShapeDtypeStruct((FOUR,) + pos.shape[1:], pos.dtype)
    dy_half = jax.ShapeDtypeStruct((dy.shape[0] // TWO, dy.shape[1]), BF16)
    home = pltpu.VMEM((TWO,) * FOUR + (CHUNK, wide), BF16)
    sems = [dma((FOUR,))] + [dma((FOUR, FOUR))] * TWO + [dma((TWO, TWO, 7))] + [dma((TWO, 7))] * THREE
    bufs = [pltpu.VMEM((TWO,) + b, BF16) for b in ((w_q.shape[0], BLK), (BLK, w_o.shape[1]))]
    return pl.pallas_call(
        exchange_kernel,
        name="exchange",
        out_shape=(jax.ShapeDtypeStruct((N_PAIRS,) + (TWO,) * THREE + (BLK, HEAD_DIM), BF16), unit, unit, pos_quad, dy_half, dy_half),
        in_specs=[vmem] * 6 + [hbm] * TWO,
        out_specs=[hbm] * 6,
        scratch_shapes=sems + [home, home] + bufs + [dma((TWO, TWO)), dma((TWO,))],
        compiler_params=params(63, collective_id=1),
        cost_estimate=cost(1, 20),
    )(kv, h, dy, pos, cos_f, sin_f, w_q, w_o)


def taker(refs):
    rest = iter(refs)
    return lambda count: list(itertools.islice(rest, count))


def wo_kernel(*refs):
    take = taker(refs)
    o_ref, *pieces = take(5)
    keep, away, dy_u, o_t, terms, came, load_sem, core_s, core_r = take(len(refs))
    me = lax.axis_index("cp")
    _, y, _, core = place(me)
    meet(quad_of(me)[1:TWO])
    loads = [
        pltpu.make_async_copy(src, dy_u.at[:, :, pl.ds(d * CHUNK, CHUNK)], load_sem.at[d])
        for d, src in enumerate(pieces)
    ]
    for c in loads:
        c.start()
    for h in range(N_HEADS):
        o_t[head(h)] = o_ref[:, :, :, head(h)].reshape(-1, HEAD_DIM).T
    for c in loads:
        c.wait()
    half, tiles = terms.shape[1], terms.shape[TWO] // BLK

    def swap(t):
        return remote(terms.at[0, :, aligned(t)], came.at[:, aligned(t)], core_s.at[t], core_r.at[t], quad_of(me)[1])

    def half_terms(i, to, then):
        @pl.loop(0, tiles)
        def _(t):
            dy = dy_u[:, :, :, aligned(t)].reshape(-1, BLK)
            terms[to, :, aligned(t)] = jnp.dot(o_t[aligned(i, half)], dy, preferred_element_type=F32)
            then(t)

    half_terms(1 - core, 0, lambda t: swap(t).start())
    half_terms(core, 1, lambda t: swap(t).wait_recv())
    rows = keep.shape[1]
    for zz in range(FOUR):
        for out, yy in ((keep, y), (away, 1 - y)):
            at = aligned(TWO * zz + yy, rows)
            out[zz] = terms[1, at] + came[at]
    for t in range(tiles):
        swap(t).wait_send()


def wo_terms(o, pieces):
    dma = pltpu.SemaphoreType.DMA
    vmem, hbm = pl.BlockSpec(memory_space=pltpu.VMEM), pl.BlockSpec(memory_space=pl.ANY)
    n, d, wide = o.shape[0] * o.shape[1] * o.shape[TWO], pieces[0].shape[-1], o.shape[-1]
    half = wide // TWO
    return pl.pallas_call(
        wo_kernel,
        name="wo_terms",
        out_shape=[jax.ShapeDtypeStruct((FOUR, half // N_PAIRS, d), F32)] * TWO,
        in_specs=[vmem] + [hbm] * FOUR,
        out_specs=[vmem] * TWO,
        scratch_shapes=[pltpu.VMEM((TWO, TWO, BLK, d), BF16), pltpu.VMEM((wide, n), BF16)]
        + [pltpu.VMEM((TWO, half, d), F32), pltpu.VMEM((half, d), F32), dma((FOUR,)), dma((d // BLK,)), dma((d // BLK,))],
        compiler_params=params(63, collective_id=THREE),
        cost_estimate=cost(FOUR, 20),
    )(o, *pieces)


class PairSum:
    def __init__(self, me, kind, cut, src, out, buffers, sems, direct=0):
        self.me, self.kind, self.src, self.out = me, kind, src, out
        self.direct_from = cut - direct
        self.size = out.shape[0] // cut
        self.own, self.from_core, self.from_y, self.from_z = buffers
        self.load_sem, self.core_s, self.core_r, self.y_s, self.y_r, self.z_s, self.z_r = sems
        self.z, self.y, x, core = place(me)
        self.partner = dev(self.z, self.y, x, 1 - core)
        self.line = [(k, zz, dev(zz, self.y, x, core)) for k, zz in z_peers(self.z)]
        self.across = dev(self.z, 1 - self.y, x, core)
        self.next_z = dev(self.z + 1, self.y, x, core), dev(self.z - 1, self.y, x, core)

    def rows(self, j):
        return pl.ds(j * self.size, self.size)

    def mine(self, j, zz):
        at = self.rows(j)
        return self.own.at[zz, self.y, at] if self.kind == "core" else self.own.at[zz, at]

    def loads(self, j):
        at = self.rows(j)
        if self.kind == "z":
            pairs = zip(self.src, (self.own, self.from_y))
            return [pltpu.make_async_copy(a.at[:, at], b.at[:, at], s.at[j]) for (a, b), s in zip(pairs, (self.load_sem, self.y_r))]
        return [pltpu.make_async_copy(self.src.at[:, self.y, at], self.own.at[:, at], self.load_sem.at[j])]

    def core_copy(self, j):
        src, dst = (r.at[:, :, self.rows(j)] for r in (self.src, self.from_core))
        return remote(src, dst, self.core_s.at[j], self.core_r.at[j], self.partner)

    def y_copy(self, j):
        src = self.own if self.kind == "core" else self.src
        at = self.rows(j)
        return remote(src.at[:, 1 - self.y, at], self.from_y.at[:, at], self.y_s.at[j], self.y_r.at[j], self.across)

    def z_copy(self, j, way, zz, to):
        at = way, zz + way - 1
        return remote(self.mine(j, zz), self.from_z.at[*at, self.rows(j)], self.z_s.at[j, *at], self.z_r.at[j, *at], to)

    def begin(self, j):
        if self.kind == "core":
            self.core_copy(j).start()
            return
        for c in self.loads(j):
            c.start()
        if not self.kind:
            self.y_copy(j).start()

    def loaded(self, j):
        if self.kind != "core":
            for c in self.loads(j):
                c.wait()
        else:
            self.core_copy(j).wait_recv()
            at = self.rows(j)
            for zz in range(FOUR):
                self.own[zz, :, at] += self.from_core[zz, :, at]
            self.y_copy(j).start()
        if self.kind == "z":
            self.add_y(j)
            self.hop(j, 0)

    def add_y(self, j):
        for zz in range(FOUR):
            self.mine(j, zz)[...] += self.from_y[zz, self.rows(j)]

    def relay(self, j, way, zz, add):
        if add:
            self.z_copy(j, way, zz, self.me).wait_recv()
            self.mine(j, zz)[...] += self.from_z[way, zz + way - 1, self.rows(j)]
        self.z_copy(j, way, zz, self.next_z[way]).start()

    def hop(self, j, h):
        @pl.when(self.z == h)
        def _():
            for zz in range(THREE, h, -1):
                self.relay(j, 0, zz, h > 0)

        @pl.when(self.z == THREE - h)
        def _():
            for zz in range(THREE - h):
                self.relay(j, 1, zz, h > 0)

    def z_direct(self, j):
        for k, zz, to in self.line:
            at, there = (j, 0, k - 1), self.from_z.at[0, k - 1, self.rows(j)]
            yield remote(self.mine(j, zz), there, self.z_s.at[at], self.z_r.at[at], to), there

    def step(self, j, h):
        if j >= self.direct_from and h > 0:
            if h == 1:
                at = self.rows(j)
                self.out[at] = self.mine(j, self.z)[...]
                for c, arrived in self.z_direct(j):
                    c.wait_recv()
                    self.out[at] += arrived[...]
            return
        if h == 0 and self.kind != "z":
            self.y_copy(j).wait_recv()
            self.add_y(j)
            if j < self.direct_from:
                self.hop(j, 0)
            else:
                for c, _ in self.z_direct(j):
                    c.start()
        elif 0 < h < THREE:
            self.hop(j, h)
        elif h == THREE:
            at = self.rows(j)
            self.out[at] = self.mine(j, self.z)[...]
            for way, on in enumerate((self.z > 0, self.z < THREE)):

                @pl.when(on)
                def _(way=way):
                    self.z_copy(j, way, self.z, self.me).wait_recv()
                    self.out[at] += self.from_z[way, self.z + way - 1, at]

    def wait_send(self, j):
        if self.kind == "core":
            self.core_copy(j).wait_send()
        if self.kind != "z":
            self.y_copy(j).wait_send()
        if j >= self.direct_from:
            for c, _ in self.z_direct(j):
                c.wait_send()
            return
        for zz in range(FOUR):
            if zz > 0:
                pl.when(self.z < zz)(self.z_copy(j, 0, zz, self.next_z[0]).wait_send)
            if zz < THREE:
                pl.when(self.z > zz)(self.z_copy(j, 1, zz, self.next_z[1]).wait_send)

    @staticmethod
    def scratch(kind, block):
        unused = pltpu.VMEM((8, HEAD_DIM), F32)
        own = pltpu.VMEM(((FOUR, TWO) if kind == "core" else (FOUR,)) + block, F32)
        from_y = pltpu.VMEM((FOUR,) + block, F32)
        return [own, own if kind == "core" else unused, from_y, pltpu.VMEM((TWO, THREE) + block, F32)]

    @staticmethod
    def sems(*dims):
        dma = pltpu.SemaphoreType.DMA
        return [dma(dims)] * 5 + [dma(dims + (TWO, THREE))] * TWO


def reduce_kernel(cuts, kinds, work, *refs):
    n = len(cuts)

    take = taker(refs)
    ins = [take(TWO) if k == "z" else take(1)[0] for k in kinds[:-1]]
    more_in, outs, more_out, made = take(work.ins), take(n), take(work.outs), take(1)
    buffers, sems = [take(FOUR) for _ in kinds], take(7)
    me = lax.axis_index("cp")
    z, y, x, core = place(me)
    meet(quad_of(me)[1:] + [dev(z, 1 - y, x, core)] + [dev(zz, y, x, core) for _, zz in z_peers(z)])
    job = work(me, more_in, more_out, take(len(refs)))
    inputs = enumerate(zip(kinds, cuts, ins + made, outs, buffers))
    sums = [PairSum(me, *a, [r.at[i] for r in sems], DIRECT if i == n - 1 else 0) for i, a in inputs]
    pieces = [(s, j) for s, cut in zip(sums, cuts) for j in range(cut)]
    early, late = pieces[: -cuts[-1]], pieces[-cuts[-1] :]
    for s, j in early:
        s.begin(j)
    for s, j in early:
        s.loaded(j)
    for t in range(len(pieces) + THREE):
        if t == MADE_AT:
            job.wq_terms(sums[-1].own, made[0])
            for s, j in late:
                s.begin(j)
        if t == MADE_AT + 1:
            for s, j in late:
                s.loaded(j)
        for h in range(FOUR):
            if 0 <= t - h < len(pieces):
                s, j = pieces[t - h]
                s.step(j, h)
        job.step(t)
    for s, j in pieces:
        s.wait_send(j)
    job.finish()


def quad_of(me):
    z, y, x, core = place(me)
    return [dev(z, y, 1 - x if d // TWO else x, 1 - core if d % TWO else core) for d in range(FOUR)]


class Home:
    def __init__(self, me, src, out, own_sem, send, arrive):
        _, _, x, core = place(me)
        w = src.shape[-1]
        to = out.at[core, :, :, :, pl.ds(x * w, w)]

        def piece(d):
            return src.at[:, :, pl.ds(d * CHUNK, CHUNK)]

        self.own = pltpu.make_async_copy(piece(0), to, own_sem)
        self.copies = [remote(piece(d), to, send.at[d], arrive.at[d], quad_of(me)[d]) for d in (1, TWO, THREE)]

    def start(self):
        self.own.start()
        for c in self.copies:
            c.start()

    def wait_recv(self):
        self.own.wait()
        for c in self.copies:
            c.wait_recv()

    def wait_send(self):
        for c in self.copies:
            c.wait_send()


class Products:
    ins, outs = 6, THREE

    def __init__(self, me, ins, outs, scratch):
        attn, self.dq, hidden, normed, self.w_o, self.w_q = ins
        self.block_out, self.d_part, self.h_u = outs
        self.attn_home, self.dq_home, self.buf_o, self.buf_q, stage, self.h_buf, *sems = scratch
        self.w_sem, self.load_sem, own_sem, quad_s, quad_r = sems
        _, _, _, core = place(me)

        def piece(d):
            return normed.at[1 - core if d % TWO else core]

        def tokens(d):
            return self.h_u.at[:, :, pl.ds(d * CHUNK, CHUNK)]

        self.h_copies = [remote(piece(d), tokens(d), quad_s.at[TWO, d], quad_r.at[TWO, d], quad_of(me)[d]) for d in (1, TWO, THREE)]
        self.h_mine = pltpu.make_async_copy(piece(0), stage, own_sem.at[TWO])
        self.h_back = pltpu.make_async_copy(stage, tokens(0), self.load_sem.at[0])
        self.residual = pltpu.make_async_copy(hidden, self.block_out, own_sem.at[THREE])
        self.residual.start()
        for c in self.h_copies:
            c.start()
        self.h_mine.start()
        self.homes = [
            Home(me, src, out, own_sem.at[i], quad_s.at[i], quad_r.at[i])
            for i, (src, out) in enumerate([(attn, self.attn_home), (self.dq, self.dq_home)])
        ]
        for h in self.homes:
            h.start()

    @staticmethod
    def scratch(arrays):
        dma, d = pltpu.SemaphoreType.DMA, arrays[-1].shape[0]
        home = pltpu.VMEM((TWO,) * THREE + (CHUNK, d), BF16)
        buf = [pltpu.VMEM((TWO,) + b, BF16) for b in ((d, BLK), (BLK, d))]
        tiles = [pltpu.VMEM((TWO, TWO) + b, BF16) for b in ((CHUNK, d), (TWO, BLK, BLK))]
        sems = [dma((TWO, TWO)), dma((TWO,)), dma((FOUR,)), dma((THREE, FOUR)), dma((THREE, FOUR))]
        return [home] * TWO + buf + tiles + sems

    @staticmethod
    def results(arrays):
        unit = TWO, TWO, BLK, arrays[-1].shape[0]
        return [jax.ShapeDtypeStruct(arrays[TWO].shape, t) for t in (BF16, F32)] + [jax.ShapeDtypeStruct(unit, BF16)]

    spaces, out_spaces = [pl.ANY, pltpu.VMEM] + [pl.ANY] * FOUR, [pltpu.VMEM] * TWO + [pl.ANY]

    def step(self, t):
        def fetch_o(t, slot):
            return pltpu.make_async_copy(self.w_o.at[:, aligned(t)], self.buf_o.at[slot], self.w_sem.at[0, slot])

        def fetch_q(t, slot):
            return pltpu.make_async_copy(self.w_q.at[aligned(t)], self.buf_q.at[slot], self.w_sem.at[1, slot])

        def project(t, slot):
            at = aligned(t)
            attn = self.attn_home[...].reshape(-1, self.w_o.shape[0])
            out = jnp.dot(attn, self.buf_o[slot], preferred_element_type=F32)
            self.block_out[:, at] = (self.block_out[:, at].astype(F32) + out).astype(BF16)

        def pull(t, slot):
            dq = self.dq_home[...].reshape(-1, self.w_o.shape[0])
            self.d_part[:, aligned(t)] = dot_t(dq, self.buf_q[slot])

        if t in PRODUCTS_AT:
            i = PRODUCTS_AT.index(t)
            self.homes[i].wait_recv()
            if i == 0:
                self.residual.wait()
            tiled(self.w_o.shape[0] // BLK, *((fetch_o, project), (fetch_q, pull))[i])

    def wq_terms(self, own, other):
        self.h_mine.wait()
        self.h_back.start()
        for c in self.h_copies:
            c.wait_recv()
        self.h_back.wait()
        core = lax.rem(lax.axis_index("cp"), TWO)
        d_out = self.dq[...].reshape(-1, self.dq.shape[-1])

        def fetch(t, slot):
            return pltpu.make_async_copy(self.h_u.at[:, :, :, aligned(t)], self.h_buf.at[slot], self.load_sem.at[slot])

        for out, half in ((other, 1 - core), (own, core)):

            def use(t, slot, out=out, half=half):
                h = self.h_buf[slot].reshape(-1, BLK)
                out[t - half * FOUR] = dot(h, d_out, (0,), (0,)).reshape(out.shape[1:])

            tiled(FOUR, fetch, use, half * FOUR)

    def finish(self):
        for c in self.h_copies + self.homes:
            c.wait_send()


class HiddenGradient:
    tiles = FOUR

    def __init__(self, me, dk, dv, ins, outs, scratch):
        self.part, self.w_k, self.w_v, self.x, self.dy, self.gain = ins
        self.dx, self.terms = outs
        self.dk_home, self.dv_home, self.rows, *sems = scratch
        pairs = (dk, self.dk_home), (dv, self.dv_home)
        self.homes = [Home(me, src, out, *[r.at[i] for r in sems]) for i, (src, out) in enumerate(pairs)]
        for h in self.homes:
            h.start()

    @staticmethod
    def scratch(x):
        dma = pltpu.SemaphoreType.DMA
        home = pltpu.VMEM((TWO,) * THREE + (CHUNK, TWO * HEAD_DIM), BF16)
        return [home, home, pltpu.VMEM((8, x.shape[1]), F32), dma((TWO,)), dma((TWO, FOUR)), dma((TWO, FOUR))]

    def tile(self, t):
        if t == 0:
            for h in self.homes:
                h.wait_recv()
            self.rows[...] = jnp.zeros_like(self.rows)
        size = TWO * CHUNK
        at = pl.ds(t * size, size)
        d = self.part[at]
        for home, w in ((self.dk_home, self.w_k), (self.dv_home, self.w_v)):
            d += dot_t(home[t // TWO, t % TWO].reshape(size, -1), w[...])
        d = d.astype(BF16).astype(F32)
        x = self.x[at].astype(F32)
        inv_rms = lax.rsqrt(row_mean(x * x) + NORM_EPS)
        unit, scaled = x * inv_rms, d * self.gain[...]
        dx = inv_rms * (scaled - unit * row_mean(scaled * unit))
        self.dx[at] = (self.dy[at].astype(F32) + dx).astype(BF16)
        self.rows[...] += jnp.sum((d * unit).reshape((-1,) + self.rows.shape), axis=0)
        if t == self.tiles - 1:
            self.terms[...] = jnp.sum(self.rows[...], axis=0, keepdims=True)

    def finish(self):
        for h in self.homes:
            h.wait_send()


def reduce_pairs(arrays, blocks, cuts, kinds, collective_id, work, more):
    vmem, hbm = pl.BlockSpec(memory_space=pltpu.VMEM), pl.BlockSpec(memory_space=pl.ANY)
    n = len(blocks)
    scratch = [pltpu.VMEM((FOUR, TWO) + blocks[-1], F32)]
    scratch += sum((PairSum.scratch(k, b) for k, b in zip(kinds, blocks)), []) + PairSum.sems(n, max(cuts))
    outs = [jax.ShapeDtypeStruct(b, F32) for b in blocks] + work.results(more)
    return pl.pallas_call(
        functools.partial(reduce_kernel, cuts, kinds, work),
        name="reduce_pairs",
        out_shape=outs,
        in_specs=[hbm] * len(arrays) + [pl.BlockSpec(memory_space=m) for m in work.spaces],
        out_specs=[vmem] * n + [pl.BlockSpec(memory_space=m) for m in work.out_spaces],
        scratch_shapes=scratch + work.scratch(more),
        compiler_params=params(63, collective_id=collective_id),
        cost_estimate=cost(1, 20),
    )(*arrays, *more)


HERE = 0, 0, 0
LINKS = "xyud"
ORDERS = "zxy", "zyx", "yxz", "zyx"
CUTS = 0, 48, 96, 128
SIZES = 8.4, 8.4, 5.6, 2.8
GAIN_AT = [60.0 + 12.0 * i for i in range(5)]
LATENCY, TILES_FROM, TILE_EVERY = 3.0, 14.0, 8.0
SUM_AT = [25.0 + 6.0 * i for i in range(4)]


def onward(order, key):
    dz, ry, rx = key
    stage = max((order.index(a) for a, r in zip("zyx", key) if r), default=-1)
    for axis in order[stage + 1 :]:
        if axis == "x":
            yield "x", (dz, ry, 1)
        elif axis == "y":
            yield "y", (dz, 1, rx)
        else:
            yield "u", (-1, ry, rx)
            yield "d", (1, ry, rx)
    if stage >= 0 and order[stage] == "z" and abs(dz) < THREE:
        yield ("u", (dz - 1, ry, rx)) if dz < 0 else ("d", (dz + 1, ry, rx))


def arrivals():
    busy, times = {}, {}
    starts = [0.0] * THREE + [SUM_AT[-1] + LATENCY]
    here = [(t, z, part, HERE) for part, t in enumerate(starts) for z in range(FOUR)]
    while here:
        now, z, part, key = heapq.heappop(here)
        times.setdefault((part, key), []).append(now)
        for link, there in onward(ORDERS[part], key):
            to = z + {"u": 1, "d": -1}.get(link, 0)
            if 0 <= to <= THREE:
                busy[z, link] = max(busy.get((z, link), 0), now) + SIZES[part]
                heapq.heappush(here, (busy[z, link] + LATENCY, to, part, there))
    return sorted((sum(t) / len(t), *at) for at, t in times.items())


def turn_back(dkv_ref, cos_ref, sin_ref, dk_u, dv_u):
    n = TWO * TWO * BLK
    for i in range(TWO):
        for j in range(TWO):
            cos_t, sin_t = (jnp.hstack([t, t * sign]) for t, sign in ((cos_ref[i, j].T, 1), (sin_ref[i, j].T, -1)))
            dk = dkv_ref[pl.ds((i * TWO + j) * BLK, BLK)] * ATTN_SCALE
            dk_u[i, j] = (dk * cos_t + pltpu.roll(dk, HEAD_DIM // TWO, 1) * sin_t).astype(BF16)
    dv_u[...] = dkv_ref[pl.ds(n, n)].astype(BF16).reshape(dv_u.shape)


def wkv_terms(h_own, dk_u, dv_u, outs):
    d_out = jnp.hstack([r[...].reshape(-1, HEAD_DIM) for r in (dk_u, dv_u)])
    for out, half in outs:

        @pl.loop(0, FOUR)
        def _(zz, out=out, half=half):
            h = h_own[:, :, :, aligned(half * FOUR + zz)].reshape(-1, BLK)
            out[zz] = dot(h, d_out, (0,), (0,)).reshape(out.shape[1:])


def gather_kernel(*refs):
    take = taker(refs)
    wo_ref, wq_ref, dkv_ref, cos_ref, sin_ref, h_ref = take(6)
    grad_ins, outs, (dx_ref, dgain_ref) = take(6), take(FOUR), take(TWO)
    own_sem, send_sem, come_sem, core_sem, put_sem, all_terms, totals, g_s, g_r = take(9)
    terms, wkv_ref, h_own, dk_u, dv_u, store, wkv_store = take(7)
    buffers, sems, refs = take(FOUR), take(7), take(len(refs))
    me = lax.axis_index("cp")
    z, y, x, core = place(me)
    line = Line(me)
    to = {"x": dev(z, y, 1 - x, core), "y": dev(z, 1 - y, x, core), "u": line.next[1], "d": line.next[-1]}
    partner = dev(z, y, x, 1 - core)
    chip_here = me // TWO
    n_wo, wide = wo_ref.shape[0], wq_ref.shape[1]
    store[chip_here, pl.ds(0, n_wo)] = wo_ref[...]
    for i in range(TWO):
        store[chip_here, pl.ds(n_wo, n_wo), pl.ds(i * wide, wide)] = wq_ref[pl.ds(i * n_wo, n_wo)]
    meet(quad_of(me)[1:] + [to["y"]] + [dev(zz, y, x, core) for _, zz in z_peers(z)])
    load_h = pltpu.make_async_copy(h_ref, h_own, own_sem.at[0])
    load_h.start()
    wkv = PairSum(me, "core", 1, wkv_ref, wkv_store.at[chip_here], buffers, [r.at[0] for r in sems])

    def place_of(key):
        dz, ry, rx = key
        return z + dz, 1 - y if ry else y, 1 - x if rx else x

    def block(part, key):
        zz, yy, xx = place_of(key)
        chip = (TWO * zz + yy) * TWO + xx
        return wkv_store.at[chip] if part == THREE else store.at[chip, pl.ds(CUTS[part], CUTS[part + 1] - CUTS[part])]

    def windows(part, key):
        zz, yy, xx = place_of(key)
        pair, src = TWO * zz + yy, block(part, key)
        wo_at, wq_at = ((xx * TWO + core) * N_PAIRS + pair) * n_wo, (core * N_PAIRS + pair) * wq_ref.shape[0]
        if part == THREE:
            for i, out in enumerate(outs[TWO:]):
                yield src.at[:, head(i)], out.at[pl.ds(wq_at, wq_ref.shape[0]), pl.ds(xx * HEAD_DIM, HEAD_DIM)]
            return
        first, last = CUTS[part : part + TWO]
        if first < n_wo:
            rows = min(last, n_wo) - first
            yield src.at[pl.ds(0, rows)], outs[0].at[pl.ds(wo_at + first, rows)]
        if last > n_wo:
            skip = max(n_wo - first, 0)
            rows, at = last - first - skip, first + skip - n_wo
            for i in range(TWO):
                window = outs[1].at[pl.ds(wq_at + i * n_wo + at, rows), pl.ds(xx * wide, wide)]
                yield src.at[pl.ds(skip, rows), pl.ds(i * wide, wide)], window

    def index(part, key):
        return (part, key[0] + THREE) + key[1:]

    def send(part, key, link, there):
        sent = send_sem.at[index(part, key) + (LINKS.find(link or "-") + 1,)]
        if link:
            remote(block(part, key), block(part, key), sent, come_sem.at[index(part, there)], to[link]).start()
            return
        for src, window in windows(part, key):
            remote(src, window, sent, core_sem.at[index(part, key)], partner).start()
            pltpu.make_async_copy(src, window, put_sem.at[index(part, key)]).start()

    def whole(part, send, arrive):
        size = CUTS[part + 1] - CUTS[part] if part < THREE else wkv_store.size // store.shape[0] // outs[0].shape[1]
        dst = outs[0].at[pl.ds(0, size)]
        return remote(dst, dst, send, arrive, me)

    def when(on, do):
        pl.when(on)(do)

    def each_way(part, key):
        held = line.held(key[0])
        yield None, key, held
        for link, there in onward(ORDERS[part], key):
            inside = {"u": line.inside[1], "d": line.inside[-1]}.get(link)
            yield link, there, held if inside is None else jnp.logical_and(held, inside)

    def pass_on(part, key):
        for link, there, on in each_way(part, key):
            when(on, functools.partial(send, part, key, link, there))

    def term_copy(i):
        src = terms if i == 0 else totals.at[i - 1]
        return remote(src, all_terms.at[i], g_s.at[i], g_r.at[i], me ^ (1 << i))

    def add_terms(i):
        term_copy(i).wait_recv()
        totals[i] = (terms[...] if i == 0 else totals[i - 1]) + all_terms[i]
        if i + 1 < len(GAIN_AT):
            term_copy(i + 1).start()

    def tile(t):
        job.tile(t)
        if t == job.tiles - 1:
            term_copy(0).start()

    def sum_step(h):
        wkv.step(0, h)

    steps = [(TILES_FROM + t * TILE_EVERY, functools.partial(tile, t)) for t in range(HiddenGradient.tiles)]
    steps += [(at, functools.partial(sum_step, h)) for h, at in enumerate(SUM_AT)]
    steps += [(at, functools.partial(add_terms, i)) for i, at in enumerate(GAIN_AT)]
    steps.sort(key=lambda s: s[0])
    events = arrivals()
    for part in range(THREE):
        pass_on(part, HERE)
    turn_back(dkv_ref, cos_ref, sin_ref, dk_u, dv_u)
    job = HiddenGradient(me, dk_u, dv_u, grad_ins, (dx_ref, terms), refs)
    load_h.wait()
    wkv_terms(h_own, dk_u, dv_u, ((wkv_ref, 1 - core), (buffers[0], core)))
    wkv.begin(0)
    wkv.loaded(0)
    for now, part, key in events:
        while steps and steps[0][0] <= now:
            steps.pop(0)[1]()
        if any(key):
            arrive = come_sem.at[index(part, key)]
            when(line.held(key[0]), whole(part, own_sem.at[0], arrive).wait_recv)
            pass_on(part, key)
        elif part == THREE:
            pass_on(part, key)
    dgain_ref[...] = totals[len(GAIN_AT) - 1]
    for i in range(len(GAIN_AT)):
        term_copy(i).wait_send()
    for _, part, key in events:
        for sem in (core_sem, put_sem):
            when(line.held(key[0]), whole(part, own_sem.at[0], sem.at[index(part, key)]).wait_recv)
        for link, there, on in each_way(part, key):
            sent = send_sem.at[index(part, key) + (LINKS.find(link or "-") + 1,)]
            when(on, whole(part, sent, own_sem.at[0]).wait_send)
    wkv.wait_send(0)
    job.finish()


def gather_all(wo, wq, dkv, cos_f, sin_f, h_u, part, w_k, w_v, x, dy, gain, shapes):
    dma = pltpu.SemaphoreType.DMA
    vmem, hbm = pl.BlockSpec(memory_space=pltpu.VMEM), pl.BlockSpec(memory_space=pl.ANY)
    block = w_k.shape[0] // TWO // N_PAIRS, w_k.shape[1]
    parts = len(ORDERS)
    keys = (parts, 7, TWO, TWO)
    terms = 1, x.shape[1]
    scratch = [dma((1,)), dma(keys + (len(LINKS) + 1,)), dma(keys), dma(keys), dma(keys)]
    n = len(GAIN_AT)
    scratch += [pltpu.VMEM((n,) + terms, F32)] * TWO + [dma((n,)), dma((n,)), pltpu.VMEM(terms, F32)]
    scratch += [pltpu.VMEM((FOUR, TWO) + block, F32), pltpu.VMEM(h_u.shape, BF16)]
    scratch += [pltpu.VMEM((TWO, TWO, BLK, HEAD_DIM), BF16)] * TWO
    scratch += [pltpu.VMEM((TWO * N_PAIRS,) + b, F32) for b in ((TWO * wo.shape[0], wo.shape[1]), block)]
    return pl.pallas_call(
        gather_kernel,
        name="gather_all",
        out_shape=[jax.ShapeDtypeStruct(s, F32) for s in shapes]
        + [jax.ShapeDtypeStruct(x.shape, BF16), jax.ShapeDtypeStruct(terms, F32)],
        in_specs=[vmem] * 5 + [hbm] + [vmem] * 6,
        out_specs=[hbm] * len(shapes) + [vmem] * TWO,
        scratch_shapes=scratch + PairSum.scratch("core", block) + PairSum.sems(1, 1) + HiddenGradient.scratch(x),
        compiler_params=params(63, collective_id=0),
        cost_estimate=cost(1, 76),
    )(wo, wq, dkv, cos_f, sin_f, h_u, part, w_k, w_v, x, dy, gain)


def perm(x, pairs):
    return lax.ppermute(x, "cp", pairs)


def flip_pairs(d):
    return [(r, r ^ d) for r in range(32)]


def solution(mesh):
    def local_step(hidden, grad_out, positions, seg_ids, w_q, w_k, w_v, w_o, norm_gain):
        n_batch, n_tok, d_model = hidden.shape
        n_rows = n_batch * n_tok
        wide = N_HEADS * HEAD_DIM
        me = lax.axis_index("cp")
        z, y, x, core = place(me)
        quad, pair = me % FOUR, me // FOUR
        relations = range(FOUR)

        def swap(pieces):
            return [perm(p, flip_pairs(d)) if d else p for d, p in enumerate(pieces)]

        gain = norm_gain.astype(F32)
        cos_t, sin_t = rope_tables(positions.reshape(n_rows))
        cos_f, sin_f = jnp.hstack([cos_t, cos_t]), jnp.hstack([-sin_t, sin_t])
        dy_flat = grad_out.reshape(n_rows, d_model)
        normed, kv_home = project(hidden.reshape(n_rows, d_model), gain[NEW], w_k, w_v, cos_f, sin_f)
        pos = jnp.pad(positions.reshape(TWO, TWO, n_tok), ((0, 0), (0, 6), (0, 0)))
        kv_home = kv_home.reshape((TWO,) * 5 + (CHUNK, HEAD_DIM))
        kv_all, q_u, do_u, pos_u, *dy_rows = exchange(kv_home, normed, dy_flat, pos, cos_f, sin_f, w_q, w_o)
        pos_u = pos_u[:, :TWO].reshape((FOUR, TWO, TWO, CHUNK)).transpose(1, TWO, 0, THREE).reshape(TWO, TWO, BLK)
        dy_rows = [a.reshape(TWO, TWO, CHUNK, d_model) for a in dy_rows]
        dy_pieces = swap([dy_rows[d % TWO] for d in relations])

        member = quad ^ jnp.arange(FOUR)
        front, back = ((m[:, NEW] * CHUNK + jnp.arange(CHUNK)[NEW]).reshape(BLK) for m in (member, THREE - member))
        offsets = jnp.stack([front, back]).astype(jnp.int32)
        own_super = jnp.stack([pair, N_SUPER - 1 - pair]).astype(jnp.int32)
        q_index = own_super[:, NEW] * BLK + offsets
        start = q_index[NEW] - pos_u
        tab = jnp.concatenate(
            [own_super, (jnp.min(start, axis=-1) // BLK).reshape(-1), jnp.max(start, axis=-1).reshape(-1)]
        )
        start_r = start[:, :, NEW, :]
        q_index_r = jnp.broadcast_to(q_index[NEW, :, NEW, :], start_r.shape)
        cos_u, sin_u = rope_tables(pos_u)
        cos_ut, sin_ut = jnp.swapaxes(cos_u, TWO, THREE), jnp.swapaxes(sin_u, TWO, THREE)

        koff = offsets[:, NEW]
        attn_u, lse = flash_fwd(tab, q_u, kv_all, start_r, q_index_r, koff)

        wo_keep, wo_away = wo_terms(attn_u, dy_pieces)
        wo_come = perm(wo_away, flip_pairs(FOUR))
        do_u, wo_keep = lax.optimization_barrier((do_u, wo_keep))
        dq_u, dkv = flash_bwd(tab, q_u, do_u, attn_u, kv_all, lse, start_r, q_index_r, koff, cos_ut, sin_ut)

        x_flat = hidden.reshape(n_rows, d_model)
        wo_own, dkv_own, wq_own, block_out, d_part, h_u = reduce_pairs(
            [wo_keep, wo_come, dkv.reshape(FOUR, TWO, -1, HEAD_DIM)],
            [wo_keep.shape[1:], (dkv.size // N_PAIRS // HEAD_DIM, HEAD_DIM), (d_model // TWO // N_PAIRS, wide)],
            (TWO, 8, 8),
            ("z", "", "core"),
            TWO,
            Products,
            (attn_u, dq_u, x_flat, normed.reshape((TWO,) * THREE + (CHUNK, d_model)), w_o, w_q),
        )
        grad_wo, grad_wq, grad_wk, grad_wv, grad_x, d_gain = gather_all(
            wo_own,
            wq_own,
            dkv_own,
            cos_ut,
            sin_ut,
            h_u,
            d_part,
            w_k,
            w_v,
            x_flat,
            dy_flat,
            gain[NEW],
            [w_o.shape, w_q.shape, w_k.shape, w_v.shape],
        )
        block_out, grad_x = (a.reshape(hidden.shape) for a in (block_out, grad_x))
        return block_out, grad_x, grad_wq, grad_wk, grad_wv, grad_wo, d_gain.reshape(d_model)

    seq_spec = P(None, "cp", None)
    tok_spec = P(None, "cp")
    full_spec = P()
    return jax.shard_map(
        local_step,
        mesh=mesh,
        in_specs=(seq_spec, seq_spec, tok_spec, tok_spec, full_spec, full_spec, full_spec, full_spec, full_spec),
        out_specs=(seq_spec, seq_spec, full_spec, full_spec, full_spec, full_spec, full_spec),
        check_vma=False,
    )
```

```python
import functools
import heapq
import itertools

import jax
import jax.numpy as jnp
from jax import lax
from jax.experimental import pallas as pl
from jax.experimental.pallas import tpu as pltpu
from jax.sharding import PartitionSpec as P

HEAD_DIM = 128
NORM_EPS = 1e-5
ROPE_BASE = 500000.0
NEG_BIG = -1e30
LOG2E = 1.4426950408889634
ATTN_SCALE = HEAD_DIM**-0.5
EXP2_SCALE = ATTN_SCALE * LOG2E
CHUNK = 64
TWO = 2
THREE = 3
FOUR = 4
NEW = jnp.newaxis
BLK = 4 * CHUNK
N_HEADS = 8
N_PAIRS = 8
N_SUPER = 2 * N_PAIRS
MESH = pl.DeviceIdType.MESH
ONE = pl.Squeezed()
GROUP = 4
DIRECT = 2
MADE_AT = 5
PRODUCTS_AT = 7, 9
F32 = jnp.float32
BF16 = jnp.bfloat16

T_SQ, T_LO, T_MX = 0, 2, 6


def rope_tables(positions):
    inv_freq = ROPE_BASE ** (-jnp.arange(0, HEAD_DIM, TWO).astype(F32) / HEAD_DIM)
    angles = positions.astype(F32)[..., None] * inv_freq
    return jnp.cos(angles), jnp.sin(angles)


def dot(a, b, ca, cb):
    return lax.dot_general(a, b, ((ca, cb), ((), ())), preferred_element_type=F32)


def cost(gflop, mib):
    return pl.CostEstimate(flops=gflop * 10**9, bytes_accessed=mib << 20, transcendentals=0)


def params(mib, **more):
    return pltpu.CompilerParams(vmem_limit_bytes=mib << 20, **more)


def row_mean(x):
    return jnp.mean(x, axis=-1, keepdims=True)


def head(h):
    return pl.ds(h * HEAD_DIM, HEAD_DIM)


def head_slice(h):
    return slice(h * HEAD_DIM, (h + 1) * HEAD_DIM)


def dot_t(a, b):
    return dot(a, b, (1,), (1,))


def steps(tab, body):
    b, hf = pl.program_id(0), pl.program_id(1)
    own, first, last_start = tab[T_SQ + hf], tab[T_LO + TWO * b + hf], tab[T_MX + TWO * b + hf]

    def place_of(s):
        late = s >= N_PAIRS
        return jnp.where(late, N_SUPER - 1 - s, s), late.astype(jnp.int32)

    full_from = jnp.minimum((last_start + BLK - 1) // BLK, own)
    full_from += lax.rem(own - full_from, TWO)
    count = full_from - first

    @pl.loop(0, count + 1)
    def _(t):
        s = jnp.where(t < count, first + t, own)
        body(s, place_of(s), True)

    @pl.loop(0, (own - full_from) // TWO)
    def _(t):
        for i in range(TWO):
            s = full_from + TWO * t + i
            body(s, place_of(s), False)


def down(row, n):
    return jnp.broadcast_to(row, (n, row.shape[-1])).T


def may_use(s, off, st_ref, qi_ref):
    return jnp.logical_and(off >= st_ref[...] - s * BLK, off <= qi_ref[...] - s * BLK)


def fwd_kernel(tab, q_ref, kv_ref, st_ref, qi_ref, ko_ref, o_ref, lse_ref, q_s, acc, m_s, l_s, k_t, bounds):
    m_s[...] = jnp.full_like(m_s, NEG_BIG)
    l_s[...] = jnp.zeros_like(l_s)
    acc[...] = jnp.zeros_like(acc)
    for i, ref in enumerate((st_ref, qi_ref)):
        bounds[i] = down(ref[...], HEAD_DIM)
    for h in range(N_HEADS):
        q_s[pl.ds(h * BLK, BLK)] = q_ref[:, head(h)]

    @pl.when(pl.program_id(1) == 0)
    def _():
        @pl.loop(0, N_PAIRS)
        def _(pair):
            for hk in range(TWO):
                k_t[pair, hk] = kv_ref[pair, 0, hk].T

    def body(s, at, masked):
        pair, hk = at
        v = kv_ref[pair, 1, hk]
        if masked:
            off = ko_ref[hk] + s * BLK
            mask = [
                jnp.logical_and(off[:, lanes] >= bounds[0], off[:, lanes] <= bounds[1])
                for lanes in (slice(HEAD_DIM), slice(HEAD_DIM, BLK))
            ]
            mask = [jnp.concatenate([m, m], axis=0) for m in mask]
        for g in range(N_HEADS // TWO):
            rows = pl.ds(g * TWO * BLK, TWO * BLK)
            sc = jnp.dot(q_s[rows], k_t[pair, hk], preferred_element_type=F32)
            sc = [sc[:, :HEAD_DIM], sc[:, HEAD_DIM:]]
            if masked:
                sc = [jnp.where(m, x, NEG_BIG) for m, x in zip(mask, sc)]
            m_old = m_s[rows]
            m_new = jnp.maximum(m_old, jnp.max(jnp.maximum(*sc), axis=1, keepdims=True))
            alpha = jnp.exp2((m_old - m_new) * EXP2_SCALE)
            p = [jnp.exp2((x - m_new) * EXP2_SCALE) for x in sc]
            m_s[rows] = m_new
            l_s[rows] = l_s[rows] * alpha + (p[0] + p[1])
            p = jnp.hstack([x.astype(BF16) for x in p])
            acc[rows] = acc[rows] * alpha + jnp.dot(p, v, preferred_element_type=F32)

    steps(tab, body)
    for h in range(N_HEADS):
        rows = pl.ds(h * BLK, BLK)
        total = jnp.sum(l_s[rows], axis=1, keepdims=True)
        o_ref[:, head(h)] = (acc[rows] / total).astype(BF16)
        lse_ref[h] = (m_s[rows] * EXP2_SCALE + jnp.log2(total)).T[:1]


def bwd_kernel(tab, q_ref, do_ref, o_ref, kv_ref, lse_ref, st_ref, qi_ref, ko_ref, cos_ref, sin_ref, dq_ref, dkv_ref, *scratch):
    dq_acc, delta, off_s, q_s, do_s, q_t, do_t, p_s, ds_s = scratch
    dq_acc[...] = jnp.zeros_like(dq_acc)
    for h in range(N_HEADS):
        q, do = q_ref[:, head(h)], do_ref[:, head(h)]
        delta[h] = jnp.sum((do.astype(F32) * o_ref[:, head(h)].astype(F32)).T, axis=0, keepdims=True)
        q_s[pl.ds(h * BLK, BLK)], do_s[pl.ds(h * BLK, BLK)] = q, do
        q_t[h], do_t[h] = q.T, do.T

    @pl.when(pl.program_id(1) == 0)
    def _():
        dkv_ref[...] = jnp.zeros_like(dkv_ref)
        for hk in range(TWO):
            off_s[hk] = down(ko_ref[hk], BLK)

    def body(s, at, masked):
        pair, hk = at
        k = kv_ref[pair, 0, hk]
        v = kv_ref[pair, 1, hk]
        k_t = k.T
        mask = may_use(s, off_s[hk], st_ref, qi_ref) if masked else None
        for first in range(0, N_HEADS, GROUP):
            rows = pl.ds(first * BLK, GROUP * BLK)
            for h in range(first, first + GROUP):
                cols = pl.ds(h * BLK, BLK)
                p = jnp.exp2(jnp.dot(k, q_t[h], preferred_element_type=F32) * EXP2_SCALE - lse_ref[h])
                if masked:
                    p = jnp.where(mask, p, 0.0)
                ds = p * (jnp.dot(v, do_t[h], preferred_element_type=F32) - delta[h])
                p_s[:, cols] = p.astype(BF16)
                ds_s[:, cols] = ds.astype(BF16)
            dkv_ref[pair, 0, hk] += jnp.dot(ds_s[:, rows], q_s[rows], preferred_element_type=F32)
            dkv_ref[pair, 1, hk] += jnp.dot(p_s[:, rows], do_s[rows], preferred_element_type=F32)
            dq_acc[:, rows] += jnp.dot(k_t, ds_s[:, rows], preferred_element_type=F32)

    steps(tab, body)
    cos_t, sin_t = cos_ref[...], sin_ref[...]
    half = HEAD_DIM // TWO
    for h in range(N_HEADS):
        cols = pl.ds(h * BLK, BLK)
        a, c = dq_acc[:half, cols] * ATTN_SCALE, dq_acc[half:, cols] * ATTN_SCALE
        lin = jnp.concatenate([a * cos_t + c * sin_t, c * cos_t - a * sin_t], axis=0)
        dq_ref[:, head(h)] = lin.T.astype(BF16)


def attn_specs():
    def at_tile(b, h, t):
        return (b, h) + (0,) * TWO

    def at_row(b, h, t):
        return (0, 0, b) + (0,) * THREE

    tile = pl.BlockSpec((ONE, ONE, BLK, N_HEADS * HEAD_DIM), at_tile)
    row = pl.BlockSpec((ONE, ONE, 1, BLK), at_tile)
    stat = pl.BlockSpec((ONE, ONE, N_HEADS, 1, BLK), lambda b, h, t: (b, h) + (0,) * THREE)
    rope = pl.BlockSpec((ONE, ONE, HEAD_DIM // TWO, BLK), at_tile)
    kv = pl.BlockSpec((N_PAIRS, TWO, ONE, TWO, BLK, HEAD_DIM), at_row)
    ko = pl.BlockSpec((TWO, 1, BLK), lambda b, h, t: (0,) * THREE)
    return tile, row, stat, kv, ko, rope


def flash_fwd(tab, q, kv, start, qidx, koff):
    tile, row, stat, kvs, ko, _ = attn_specs()
    return pl.pallas_call(
        fwd_kernel,
        name="attn_fwd",
        out_shape=(jax.ShapeDtypeStruct(q.shape, BF16), jax.ShapeDtypeStruct((TWO, TWO, N_HEADS, 1, BLK), F32)),
        grid_spec=pltpu.PrefetchScalarGridSpec(
            num_scalar_prefetch=1,
            grid=(TWO, TWO),
            in_specs=[tile, kvs, row, row, ko],
            out_specs=[tile, stat],
            scratch_shapes=[pltpu.VMEM((N_HEADS * BLK, HEAD_DIM), t) for t in (BF16, F32, F32, F32)]
            + [pltpu.VMEM((N_PAIRS, TWO, HEAD_DIM, BLK), BF16), pltpu.VMEM((TWO, BLK, HEAD_DIM), jnp.int32)],
        ),
        compiler_params=params(63),
        cost_estimate=cost(20, 16),
    )(tab, q, kv, start, qidx, koff)


def flash_bwd(tab, q, do, o, kv, lse, start, qidx, koff, cos_t, sin_t):
    tile, row, stat, kvs, ko, rope = attn_specs()
    return pl.pallas_call(
        bwd_kernel,
        name="attn_bwd",
        out_shape=(
            jax.ShapeDtypeStruct(q.shape, BF16),
            jax.ShapeDtypeStruct(kv.shape, F32),
        ),
        grid_spec=pltpu.PrefetchScalarGridSpec(
            num_scalar_prefetch=1,
            grid=(TWO, TWO),
            in_specs=[tile, tile, tile, kvs, stat, row, row, ko, rope, rope],
            out_specs=[tile, kvs],
            scratch_shapes=[pltpu.VMEM((HEAD_DIM, N_HEADS * BLK), F32), pltpu.VMEM((N_HEADS, 1, BLK), F32)]
            + [pltpu.VMEM((TWO, BLK, BLK), jnp.int32)]
            + [pltpu.VMEM((N_HEADS * BLK, HEAD_DIM), BF16)] * TWO
            + [pltpu.VMEM((N_HEADS, HEAD_DIM, BLK), BF16)] * TWO
            + [pltpu.VMEM((BLK, N_HEADS * BLK), BF16)] * TWO,
        ),
        compiler_params=params(63),
        cost_estimate=cost(50, 32),
    )(tab, q, do, o, kv, lse, start, qidx, koff, cos_t, sin_t)


def turn(x, cos_ref, sin_ref):
    return x * cos_ref[...] + pltpu.roll(x, HEAD_DIM // TWO, 1) * sin_ref[...]


def first_kernel(x_ref, g_ref, wk_ref, wv_ref, cos_ref, sin_ref, h_ref, kv_ref):
    x = x_ref[...].astype(F32)
    h = (x * lax.rsqrt(row_mean(x * x) + NORM_EPS) * g_ref[...]).astype(BF16)
    h_ref[...] = h
    k = jnp.dot(h, wk_ref[...], preferred_element_type=F32)
    v = jnp.dot(h, wv_ref[...], preferred_element_type=F32)
    n = kv_ref.shape[THREE]
    for i in range(TWO):
        for j, val in enumerate((turn(k[:, head_slice(i)], cos_ref, sin_ref), v[:, head_slice(i)])):
            for c in range(TWO):
                kv_ref[i, c, j] = val[c * n : (c + 1) * n].astype(BF16)


def project(x, gain, w_k, w_v, cos_f, sin_f):
    n = x.shape[0] // TWO
    return pl.pallas_call(
        first_kernel,
        name="norm_kv",
        out_shape=(jax.ShapeDtypeStruct(x.shape, BF16), jax.ShapeDtypeStruct((TWO,) * THREE + (n, HEAD_DIM), BF16)),
        compiler_params=params(20),
        cost_estimate=cost(TWO, 7),
    )(x, gain, w_k, w_v, cos_f, sin_f)


def place(me):
    return me // 8, lax.rem(me // FOUR, TWO), lax.rem(me // TWO, TWO), lax.rem(me, TWO)


def dev(z, y, x, core):
    return ((z * TWO + y) * TWO + x) * TWO + core


def z_peers(z):
    return [(k, lax.rem(z + k, FOUR)) for k in (1, TWO, THREE)]


def meet(peers):
    barrier = pltpu.get_barrier_semaphore()
    for d in peers:
        pl.semaphore_signal(barrier, device_id=(d,), device_id_type=MESH)
    pl.semaphore_wait(barrier, len(peers))


def remote(src, dst, send, arrive, to):
    return pltpu.make_async_remote_copy(
        src_ref=src, dst_ref=dst, send_sem=send, recv_sem=arrive, device_id=(to,), device_id_type=MESH
    )


class Line:
    order = (0, 1, -1, TWO, -TWO, THREE, -THREE)

    def __init__(self, me):
        self.z, y, x, core = place(me)
        self.next = {1: dev(self.z + 1, y, x, core), -1: dev(self.z - 1, y, x, core)}
        self.inside = {1: self.z < THREE, -1: self.z > 0}

    def held(self, dz):
        return jnp.logical_and(self.z + dz >= 0, self.z + dz <= THREE)

    def ways(self, dz):
        for d in self.next:
            if d * dz <= 0:
                yield d, self.inside[d] if dz == 0 else jnp.logical_and(self.inside[d], self.held(dz))


def tiled(n, fetch, use, first=0):
    fetch(first, 0).start()

    @pl.loop(0, n)
    def _(t):
        slot = lax.rem(t, TWO)
        fetch(first + t, slot).wait()

        @pl.when(t + 1 < n)
        def _():
            fetch(first + t + 1, 1 - slot).start()

        use(first + t, slot)


def aligned(t, size=BLK):
    return pl.ds(pl.multiple_of(t * size, size), size)


def exchange_kernel(*refs):
    take = taker(refs)
    kv_ref, h_ref, dy_ref, pos_ref, cos_ref, sin_ref, wq_ref, wo_ref, kv_all, q_u, do_u, pos_u, *dy_rows = take(14)
    own_sem, quad_s, quad_r, z_s, z_r, y_s, y_r, q_home, do_home, wq_buf, wo_buf, w_sem, dy_sem = take(len(refs))
    me = lax.axis_index("cp")
    z, y, x, core = place(me)
    quad, line = quad_of(me), Line(me)
    across = dev(z, 1 - y, x, core)
    meet(quad[1:] + [across] + [dev(zz, y, x, core) for _, zz in z_peers(z)])

    def source(a, d):
        xx, cc = 1 - x if d // TWO else x, 1 - core if d % TWO else core
        return pos_ref.at[cc] if a == THREE else (kv_ref, q_home, do_home)[a].at[xx, cc]

    def target(a, d):
        if a == THREE:
            return pos_u.at[d]
        tok = pl.ds(d * CHUNK, CHUNK)
        return kv_all.at[me // FOUR, :, :, :, tok] if a == 0 else (q_u, do_u)[a - 1].at[:, :, tok]

    def quad_copy(a, d):
        return remote(source(a, d), target(a, d), quad_s.at[a, d], quad_r.at[a, d], quad[d])

    def own_copy(a):
        return pltpu.make_async_copy(source(a, 0), target(a, 0), own_sem.at[a])

    def z_copy(part, dz, d):
        block = kv_all.at[TWO * (z + dz) + y, part]
        return remote(block, block, z_s.at[part, (d + 1) // TWO, dz + THREE], z_r.at[part, dz - d + THREE], line.next[d])

    def y_copy(part, dz, yy=y):
        block = kv_all.at[TWO * (z + dz) + yy, part]
        return remote(block, block, y_s.at[part, dz + THREE], y_r.at[part, dz + THREE], across)

    parts = range(TWO)
    moves = [(part, dz) for dz in line.order for part in parts]

    def pass_on(count):
        for part, dz in [moves.pop(0) for _ in range(count)]:
            if dz:
                block = kv_all.at[TWO * (z + dz) + y, part]
                arrival = remote(block, block, own_sem.at[0], z_r.at[part, dz + THREE], me)
                pl.when(line.held(dz))(arrival.wait_recv)
            for d, on in line.ways(dz):
                pl.when(on)(z_copy(part, dz, d).start)
            pl.when(line.held(dz))(y_copy(part, dz).start)

    n = h_ref.shape[1] // BLK // TWO

    def fetch_q(t, slot):
        return pltpu.make_async_copy(wq_ref.at[:, aligned(t)], wq_buf.at[slot], w_sem.at[0, slot])

    def fetch_o(t, slot):
        return pltpu.make_async_copy(wo_ref.at[aligned(t)], wo_buf.at[slot], w_sem.at[1, slot])

    def put(home, t, val):
        home[t // n, :, :, :, :, aligned(lax.rem(t, n))] = val.astype(BF16).reshape(home.shape[1:-1] + (BLK,))

    def query(t, slot):
        q = jnp.dot(h_ref[...], wq_buf[slot], preferred_element_type=F32)
        put(q_home, t, jnp.hstack([turn(q[:, head_slice(j)], cos_ref, sin_ref) for j in range(BLK // HEAD_DIM)]))

    def pull(t, slot):
        put(do_home, t, dot_t(dy_ref[...], wo_buf[slot]))

    all_moves = list(moves)
    half = dy_ref.shape[0] // TWO
    for i, out in enumerate(dy_rows):
        pltpu.make_async_copy(dy_ref.at[aligned(core if i == 0 else 1 - core, half)], out, dy_sem.at[i]).start()
    for a in (0, THREE):
        for d in (1, TWO, THREE):
            quad_copy(a, d).start()
        own_copy(a).start()
    for a, (fetch, use) in enumerate(((fetch_q, query), (fetch_o, pull)), 1):
        for near in range(TWO):
            tiled(n, fetch, use, n * (x if near else 1 - x))
            for d in range(TWO):
                if d or not near:
                    quad_copy(a, d if near else d + TWO).start()
            if near:
                own_copy(a).start()
            if len(moves) == len(all_moves):
                own_copy(0).wait()
                for d in (1, TWO, THREE):
                    quad_copy(0, d).wait_recv()
            pass_on(TWO)
    pass_on(len(moves))
    for part, dz in all_moves:
        for d, on in line.ways(dz):
            pl.when(on)(z_copy(part, dz, d).wait_send)
        pl.when(line.held(dz))(y_copy(part, dz, 1 - y).wait_recv)
        pl.when(line.held(dz))(y_copy(part, dz).wait_send)
    for a in range(FOUR):
        for d in (1, TWO, THREE):
            quad_copy(a, d).wait_send()
            if a > 0:
                quad_copy(a, d).wait_recv()
    for a in (1, TWO, THREE):
        own_copy(a).wait()
    for i, out in enumerate(dy_rows):
        pltpu.make_async_copy(dy_ref.at[aligned(core if i == 0 else 1 - core, half)], out, dy_sem.at[i]).wait()


def exchange(kv, h, dy, pos, cos_f, sin_f, w_q, w_o):
    dma = pltpu.SemaphoreType.DMA
    vmem, hbm = pl.BlockSpec(memory_space=pltpu.VMEM), pl.BlockSpec(memory_space=pl.ANY)
    wide = w_q.shape[1] // TWO
    unit = jax.ShapeDtypeStruct((TWO, TWO, BLK, wide), BF16)
    pos_quad = jax.ShapeDtypeStruct((FOUR,) + pos.shape[1:], pos.dtype)
    dy_half = jax.ShapeDtypeStruct((dy.shape[0] // TWO, dy.shape[1]), BF16)
    home = pltpu.VMEM((TWO,) * FOUR + (CHUNK, wide), BF16)
    sems = [dma((FOUR,))] + [dma((FOUR, FOUR))] * TWO + [dma((TWO, TWO, 7))] + [dma((TWO, 7))] * THREE
    bufs = [pltpu.VMEM((TWO,) + b, BF16) for b in ((w_q.shape[0], BLK), (BLK, w_o.shape[1]))]
    return pl.pallas_call(
        exchange_kernel,
        name="exchange",
        out_shape=(jax.ShapeDtypeStruct((N_PAIRS,) + (TWO,) * THREE + (BLK, HEAD_DIM), BF16), unit, unit, pos_quad, dy_half, dy_half),
        in_specs=[vmem] * 6 + [hbm] * TWO,
        out_specs=[hbm] * 6,
        scratch_shapes=sems + [home, home] + bufs + [dma((TWO, TWO)), dma((TWO,))],
        compiler_params=params(63, collective_id=1),
        cost_estimate=cost(1, 20),
    )(kv, h, dy, pos, cos_f, sin_f, w_q, w_o)


def taker(refs):
    rest = iter(refs)
    return lambda count: list(itertools.islice(rest, count))


def wo_kernel(*refs):
    take = taker(refs)
    o_ref, *pieces = take(5)
    keep, away, dy_u, o_t, terms, came, load_sem, core_s, core_r = take(len(refs))
    me = lax.axis_index("cp")
    _, y, _, core = place(me)
    meet(quad_of(me)[1:TWO])
    loads = [
        pltpu.make_async_copy(src, dy_u.at[:, :, pl.ds(d * CHUNK, CHUNK)], load_sem.at[d])
        for d, src in enumerate(pieces)
    ]
    for c in loads:
        c.start()
    for h in range(N_HEADS):
        o_t[head(h)] = o_ref[:, :, :, head(h)].reshape(-1, HEAD_DIM).T
    for c in loads:
        c.wait()
    half, tiles = terms.shape[1], terms.shape[TWO] // BLK

    def swap(t):
        return remote(terms.at[0, :, aligned(t)], came.at[:, aligned(t)], core_s.at[t], core_r.at[t], quad_of(me)[1])

    def half_terms(i, to, then):
        @pl.loop(0, tiles)
        def _(t):
            dy = dy_u[:, :, :, aligned(t)].reshape(-1, BLK)
            terms[to, :, aligned(t)] = jnp.dot(o_t[aligned(i, half)], dy, preferred_element_type=F32)
            then(t)

    half_terms(1 - core, 0, lambda t: swap(t).start())
    half_terms(core, 1, lambda t: swap(t).wait_recv())
    rows = keep.shape[1]
    for zz in range(FOUR):
        for out, yy in ((keep, y), (away, 1 - y)):
            at = aligned(TWO * zz + yy, rows)
            out[zz] = terms[1, at] + came[at]
    for t in range(tiles):
        swap(t).wait_send()


def wo_terms(o, pieces):
    dma = pltpu.SemaphoreType.DMA
    vmem, hbm = pl.BlockSpec(memory_space=pltpu.VMEM), pl.BlockSpec(memory_space=pl.ANY)
    n, d, wide = o.shape[0] * o.shape[1] * o.shape[TWO], pieces[0].shape[-1], o.shape[-1]
    half = wide // TWO
    return pl.pallas_call(
        wo_kernel,
        name="wo_terms",
        out_shape=[jax.ShapeDtypeStruct((FOUR, half // N_PAIRS, d), F32)] * TWO,
        in_specs=[vmem] + [hbm] * FOUR,
        out_specs=[vmem] * TWO,
        scratch_shapes=[pltpu.VMEM((TWO, TWO, BLK, d), BF16), pltpu.VMEM((wide, n), BF16)]
        + [pltpu.VMEM((TWO, half, d), F32), pltpu.VMEM((half, d), F32), dma((FOUR,)), dma((d // BLK,)), dma((d // BLK,))],
        compiler_params=params(63, collective_id=THREE),
        cost_estimate=cost(FOUR, 20),
    )(o, *pieces)


class PairSum:
    def __init__(self, me, kind, cut, src, out, buffers, sems, direct=0):
        self.me, self.kind, self.src, self.out = me, kind, src, out
        self.direct_from = cut - direct
        self.size = out.shape[0] // cut
        self.own, self.from_core, self.from_y, self.from_z = buffers
        self.load_sem, self.core_s, self.core_r, self.y_s, self.y_r, self.z_s, self.z_r = sems
        self.z, self.y, x, core = place(me)
        self.partner = dev(self.z, self.y, x, 1 - core)
        self.line = [(k, zz, dev(zz, self.y, x, core)) for k, zz in z_peers(self.z)]
        self.across = dev(self.z, 1 - self.y, x, core)
        self.next_z = dev(self.z + 1, self.y, x, core), dev(self.z - 1, self.y, x, core)

    def rows(self, j):
        return pl.ds(j * self.size, self.size)

    def mine(self, j, zz):
        at = self.rows(j)
        return self.own.at[zz, self.y, at] if self.kind == "core" else self.own.at[zz, at]

    def loads(self, j):
        at = self.rows(j)
        if self.kind == "z":
            pairs = zip(self.src, (self.own, self.from_y))
            return [pltpu.make_async_copy(a.at[:, at], b.at[:, at], s.at[j]) for (a, b), s in zip(pairs, (self.load_sem, self.y_r))]
        return [pltpu.make_async_copy(self.src.at[:, self.y, at], self.own.at[:, at], self.load_sem.at[j])]

    def core_copy(self, j):
        src, dst = (r.at[:, :, self.rows(j)] for r in (self.src, self.from_core))
        return remote(src, dst, self.core_s.at[j], self.core_r.at[j], self.partner)

    def y_copy(self, j):
        src = self.own if self.kind == "core" else self.src
        at = self.rows(j)
        return remote(src.at[:, 1 - self.y, at], self.from_y.at[:, at], self.y_s.at[j], self.y_r.at[j], self.across)

    def z_copy(self, j, way, zz, to):
        at = way, zz + way - 1
        return remote(self.mine(j, zz), self.from_z.at[*at, self.rows(j)], self.z_s.at[j, *at], self.z_r.at[j, *at], to)

    def begin(self, j):
        if self.kind == "core":
            self.core_copy(j).start()
            return
        for c in self.loads(j):
            c.start()
        if not self.kind:
            self.y_copy(j).start()

    def loaded(self, j):
        if self.kind != "core":
            for c in self.loads(j):
                c.wait()
        else:
            self.core_copy(j).wait_recv()
            at = self.rows(j)
            for zz in range(FOUR):
                self.own[zz, :, at] += self.from_core[zz, :, at]
            self.y_copy(j).start()
        if self.kind == "z":
            self.add_y(j)
            self.hop(j, 0)

    def add_y(self, j):
        for zz in range(FOUR):
            self.mine(j, zz)[...] += self.from_y[zz, self.rows(j)]

    def relay(self, j, way, zz, add):
        if add:
            self.z_copy(j, way, zz, self.me).wait_recv()
            self.mine(j, zz)[...] += self.from_z[way, zz + way - 1, self.rows(j)]
        self.z_copy(j, way, zz, self.next_z[way]).start()

    def hop(self, j, h):
        @pl.when(self.z == h)
        def _():
            for zz in range(THREE, h, -1):
                self.relay(j, 0, zz, h > 0)

        @pl.when(self.z == THREE - h)
        def _():
            for zz in range(THREE - h):
                self.relay(j, 1, zz, h > 0)

    def z_direct(self, j):
        for k, zz, to in self.line:
            at, there = (j, 0, k - 1), self.from_z.at[0, k - 1, self.rows(j)]
            yield remote(self.mine(j, zz), there, self.z_s.at[at], self.z_r.at[at], to), there

    def step(self, j, h):
        if j >= self.direct_from and h > 0:
            if h == 1:
                at = self.rows(j)
                self.out[at] = self.mine(j, self.z)[...]
                for c, arrived in self.z_direct(j):
                    c.wait_recv()
                    self.out[at] += arrived[...]
            return
        if h == 0 and self.kind != "z":
            self.y_copy(j).wait_recv()
            self.add_y(j)
            if j < self.direct_from:
                self.hop(j, 0)
            else:
                for c, _ in self.z_direct(j):
                    c.start()
        elif 0 < h < THREE:
            self.hop(j, h)
        elif h == THREE:
            at = self.rows(j)
            self.out[at] = self.mine(j, self.z)[...]
            for way, on in enumerate((self.z > 0, self.z < THREE)):

                @pl.when(on)
                def _(way=way):
                    self.z_copy(j, way, self.z, self.me).wait_recv()
                    self.out[at] += self.from_z[way, self.z + way - 1, at]

    def wait_send(self, j):
        if self.kind == "core":
            self.core_copy(j).wait_send()
        if self.kind != "z":
            self.y_copy(j).wait_send()
        if j >= self.direct_from:
            for c, _ in self.z_direct(j):
                c.wait_send()
            return
        for zz in range(FOUR):
            if zz > 0:
                pl.when(self.z < zz)(self.z_copy(j, 0, zz, self.next_z[0]).wait_send)
            if zz < THREE:
                pl.when(self.z > zz)(self.z_copy(j, 1, zz, self.next_z[1]).wait_send)

    @staticmethod
    def scratch(kind, block):
        unused = pltpu.VMEM((8, HEAD_DIM), F32)
        own = pltpu.VMEM(((FOUR, TWO) if kind == "core" else (FOUR,)) + block, F32)
        from_y = pltpu.VMEM((FOUR,) + block, F32)
        return [own, own if kind == "core" else unused, from_y, pltpu.VMEM((TWO, THREE) + block, F32)]

    @staticmethod
    def sems(*dims):
        dma = pltpu.SemaphoreType.DMA
        return [dma(dims)] * 5 + [dma(dims + (TWO, THREE))] * TWO


def reduce_kernel(cuts, kinds, work, *refs):
    n = len(cuts)

    take = taker(refs)
    ins = [take(TWO) if k == "z" else take(1)[0] for k in kinds[:-1]]
    more_in, outs, more_out, made = take(work.ins), take(n), take(work.outs), take(1)
    buffers, sems = [take(FOUR) for _ in kinds], take(7)
    me = lax.axis_index("cp")
    z, y, x, core = place(me)
    meet(quad_of(me)[1:] + [dev(z, 1 - y, x, core)] + [dev(zz, y, x, core) for _, zz in z_peers(z)])
    job = work(me, more_in, more_out, take(len(refs)))
    inputs = enumerate(zip(kinds, cuts, ins + made, outs, buffers))
    sums = [PairSum(me, *a, [r.at[i] for r in sems], DIRECT if i == n - 1 else 0) for i, a in inputs]
    pieces = [(s, j) for s, cut in zip(sums, cuts) for j in range(cut)]
    early, late = pieces[: -cuts[-1]], pieces[-cuts[-1] :]
    for s, j in early:
        s.begin(j)
    for s, j in early:
        s.loaded(j)
    for t in range(len(pieces) + THREE):
        if t == MADE_AT:
            job.wq_terms(sums[-1].own, made[0])
            for s, j in late:
                s.begin(j)
        if t == MADE_AT + 1:
            for s, j in late:
                s.loaded(j)
        for h in range(FOUR):
            if 0 <= t - h < len(pieces):
                s, j = pieces[t - h]
                s.step(j, h)
        job.step(t)
    for s, j in pieces:
        s.wait_send(j)
    job.finish()


def quad_of(me):
    z, y, x, core = place(me)
    return [dev(z, y, 1 - x if d // TWO else x, 1 - core if d % TWO else core) for d in range(FOUR)]


class Home:
    def __init__(self, me, src, out, own_sem, send, arrive):
        _, _, x, core = place(me)
        w = src.shape[-1]
        to = out.at[core, :, :, :, pl.ds(x * w, w)]

        def piece(d):
            return src.at[:, :, pl.ds(d * CHUNK, CHUNK)]

        self.own = pltpu.make_async_copy(piece(0), to, own_sem)
        self.copies = [remote(piece(d), to, send.at[d], arrive.at[d], quad_of(me)[d]) for d in (1, TWO, THREE)]

    def start(self):
        self.own.start()
        for c in self.copies:
            c.start()

    def wait_recv(self):
        self.own.wait()
        for c in self.copies:
            c.wait_recv()

    def wait_send(self):
        for c in self.copies:
            c.wait_send()


class Products:
    ins, outs = 6, THREE

    def __init__(self, me, ins, outs, scratch):
        attn, self.dq, hidden, normed, self.w_o, self.w_q = ins
        self.block_out, self.d_part, self.h_u = outs
        self.attn_home, self.dq_home, self.buf_o, self.buf_q, stage, self.h_buf, *sems = scratch
        self.w_sem, self.load_sem, own_sem, quad_s, quad_r = sems
        _, _, _, core = place(me)

        def piece(d):
            return normed.at[1 - core if d % TWO else core]

        def tokens(d):
            return self.h_u.at[:, :, pl.ds(d * CHUNK, CHUNK)]

        self.h_copies = [remote(piece(d), tokens(d), quad_s.at[TWO, d], quad_r.at[TWO, d], quad_of(me)[d]) for d in (1, TWO, THREE)]
        self.h_mine = pltpu.make_async_copy(piece(0), stage, own_sem.at[TWO])
        self.h_back = pltpu.make_async_copy(stage, tokens(0), self.load_sem.at[0])
        self.residual = pltpu.make_async_copy(hidden, self.block_out, own_sem.at[THREE])
        self.residual.start()
        for c in self.h_copies:
            c.start()
        self.h_mine.start()
        self.homes = [
            Home(me, src, out, own_sem.at[i], quad_s.at[i], quad_r.at[i])
            for i, (src, out) in enumerate([(attn, self.attn_home), (self.dq, self.dq_home)])
        ]
        for h in self.homes:
            h.start()

    @staticmethod
    def scratch(arrays):
        dma, d = pltpu.SemaphoreType.DMA, arrays[-1].shape[0]
        home = pltpu.VMEM((TWO,) * THREE + (CHUNK, d), BF16)
        buf = [pltpu.VMEM((TWO,) + b, BF16) for b in ((d, BLK), (BLK, d))]
        tiles = [pltpu.VMEM((TWO, TWO) + b, BF16) for b in ((CHUNK, d), (TWO, BLK, BLK))]
        sems = [dma((TWO, TWO)), dma((TWO,)), dma((FOUR,)), dma((THREE, FOUR)), dma((THREE, FOUR))]
        return [home] * TWO + buf + tiles + sems

    @staticmethod
    def results(arrays):
        unit = TWO, TWO, BLK, arrays[-1].shape[0]
        return [jax.ShapeDtypeStruct(arrays[TWO].shape, t) for t in (BF16, F32)] + [jax.ShapeDtypeStruct(unit, BF16)]

    spaces, out_spaces = [pl.ANY, pltpu.VMEM] + [pl.ANY] * FOUR, [pltpu.VMEM] * TWO + [pl.ANY]

    def step(self, t):
        def fetch_o(t, slot):
            return pltpu.make_async_copy(self.w_o.at[:, aligned(t)], self.buf_o.at[slot], self.w_sem.at[0, slot])

        def fetch_q(t, slot):
            return pltpu.make_async_copy(self.w_q.at[aligned(t)], self.buf_q.at[slot], self.w_sem.at[1, slot])

        def project(t, slot):
            at = aligned(t)
            attn = self.attn_home[...].reshape(-1, self.w_o.shape[0])
            out = jnp.dot(attn, self.buf_o[slot], preferred_element_type=F32)
            self.block_out[:, at] = (self.block_out[:, at].astype(F32) + out).astype(BF16)

        def pull(t, slot):
            dq = self.dq_home[...].reshape(-1, self.w_o.shape[0])
            self.d_part[:, aligned(t)] = dot_t(dq, self.buf_q[slot])

        if t in PRODUCTS_AT:
            i = PRODUCTS_AT.index(t)
            self.homes[i].wait_recv()
            if i == 0:
                self.residual.wait()
            tiled(self.w_o.shape[0] // BLK, *((fetch_o, project), (fetch_q, pull))[i])

    def wq_terms(self, own, other):
        self.h_mine.wait()
        self.h_back.start()
        for c in self.h_copies:
            c.wait_recv()
        self.h_back.wait()
        core = lax.rem(lax.axis_index("cp"), TWO)
        d_out = self.dq[...].reshape(-1, self.dq.shape[-1])

        def fetch(t, slot):
            return pltpu.make_async_copy(self.h_u.at[:, :, :, aligned(t)], self.h_buf.at[slot], self.load_sem.at[slot])

        for out, half in ((other, 1 - core), (own, core)):

            def use(t, slot, out=out, half=half):
                h = self.h_buf[slot].reshape(-1, BLK)
                out[t - half * FOUR] = dot(h, d_out, (0,), (0,)).reshape(out.shape[1:])

            tiled(FOUR, fetch, use, half * FOUR)

    def finish(self):
        for c in self.h_copies + self.homes:
            c.wait_send()


class HiddenGradient:
    tiles = FOUR

    def __init__(self, me, dk, dv, ins, outs, scratch):
        self.part, self.w_k, self.w_v, self.x, self.dy, self.gain = ins
        self.dx, self.terms = outs
        self.dk_home, self.dv_home, self.rows, *sems = scratch
        pairs = (dk, self.dk_home), (dv, self.dv_home)
        self.homes = [Home(me, src, out, *[r.at[i] for r in sems]) for i, (src, out) in enumerate(pairs)]
        for h in self.homes:
            h.start()

    @staticmethod
    def scratch(x):
        dma = pltpu.SemaphoreType.DMA
        home = pltpu.VMEM((TWO,) * THREE + (CHUNK, TWO * HEAD_DIM), BF16)
        return [home, home, pltpu.VMEM((8, x.shape[1]), F32), dma((TWO,)), dma((TWO, FOUR)), dma((TWO, FOUR))]

    def tile(self, t):
        if t == 0:
            for h in self.homes:
                h.wait_recv()
            self.rows[...] = jnp.zeros_like(self.rows)
        size = TWO * CHUNK
        at = pl.ds(t * size, size)
        d = self.part[at]
        for home, w in ((self.dk_home, self.w_k), (self.dv_home, self.w_v)):
            d += dot_t(home[t // TWO, t % TWO].reshape(size, -1), w[...])
        d = d.astype(BF16).astype(F32)
        x = self.x[at].astype(F32)
        inv_rms = lax.rsqrt(row_mean(x * x) + NORM_EPS)
        unit, scaled = x * inv_rms, d * self.gain[...]
        dx = inv_rms * (scaled - unit * row_mean(scaled * unit))
        self.dx[at] = (self.dy[at].astype(F32) + dx).astype(BF16)
        self.rows[...] += jnp.sum((d * unit).reshape((-1,) + self.rows.shape), axis=0)
        if t == self.tiles - 1:
            self.terms[...] = jnp.sum(self.rows[...], axis=0, keepdims=True)

    def finish(self):
        for h in self.homes:
            h.wait_send()


def reduce_pairs(arrays, blocks, cuts, kinds, collective_id, work, more):
    vmem, hbm = pl.BlockSpec(memory_space=pltpu.VMEM), pl.BlockSpec(memory_space=pl.ANY)
    n = len(blocks)
    scratch = [pltpu.VMEM((FOUR, TWO) + blocks[-1], F32)]
    scratch += sum((PairSum.scratch(k, b) for k, b in zip(kinds, blocks)), []) + PairSum.sems(n, max(cuts))
    outs = [jax.ShapeDtypeStruct(b, F32) for b in blocks] + work.results(more)
    return pl.pallas_call(
        functools.partial(reduce_kernel, cuts, kinds, work),
        name="reduce_pairs",
        out_shape=outs,
        in_specs=[hbm] * len(arrays) + [pl.BlockSpec(memory_space=m) for m in work.spaces],
        out_specs=[vmem] * n + [pl.BlockSpec(memory_space=m) for m in work.out_spaces],
        scratch_shapes=scratch + work.scratch(more),
        compiler_params=params(63, collective_id=collective_id),
        cost_estimate=cost(1, 20),
    )(*arrays, *more)


HERE = 0, 0, 0
LINKS = "xyud"
ORDERS = "zxy", "zyx", "yxz", "zyx"
CUTS = 0, 48, 96, 128
SIZES = 8.4, 8.4, 5.6, 2.8
GAIN_AT = [60.0 + 12.0 * i for i in range(5)]
LATENCY, TILES_FROM, TILE_EVERY = 3.0, 14.0, 8.0
SUM_AT = [25.0 + 6.0 * i for i in range(4)]


def onward(order, key):
    dz, ry, rx = key
    stage = max((order.index(a) for a, r in zip("zyx", key) if r), default=-1)
    for axis in order[stage + 1 :]:
        if axis == "x":
            yield "x", (dz, ry, 1)
        elif axis == "y":
            yield "y", (dz, 1, rx)
        else:
            yield "u", (-1, ry, rx)
            yield "d", (1, ry, rx)
    if stage >= 0 and order[stage] == "z" and abs(dz) < THREE:
        yield ("u", (dz - 1, ry, rx)) if dz < 0 else ("d", (dz + 1, ry, rx))


def arrivals():
    busy, times = {}, {}
    starts = [0.0] * THREE + [SUM_AT[-1] + LATENCY]
    here = [(t, z, part, HERE) for part, t in enumerate(starts) for z in range(FOUR)]
    while here:
        now, z, part, key = heapq.heappop(here)
        times.setdefault((part, key), []).append(now)
        for link, there in onward(ORDERS[part], key):
            to = z + {"u": 1, "d": -1}.get(link, 0)
            if 0 <= to <= THREE:
                busy[z, link] = max(busy.get((z, link), 0), now) + SIZES[part]
                heapq.heappush(here, (busy[z, link] + LATENCY, to, part, there))
    return sorted((sum(t) / len(t), *at) for at, t in times.items())


def turn_back(dkv_ref, cos_ref, sin_ref, dk_u, dv_u):
    n = TWO * TWO * BLK
    for i in range(TWO):
        for j in range(TWO):
            cos_t, sin_t = (jnp.hstack([t, t * sign]) for t, sign in ((cos_ref[i, j].T, 1), (sin_ref[i, j].T, -1)))
            dk = dkv_ref[pl.ds((i * TWO + j) * BLK, BLK)] * ATTN_SCALE
            dk_u[i, j] = (dk * cos_t + pltpu.roll(dk, HEAD_DIM // TWO, 1) * sin_t).astype(BF16)
    dv_u[...] = dkv_ref[pl.ds(n, n)].astype(BF16).reshape(dv_u.shape)


def wkv_terms(h_own, dk_u, dv_u, outs):
    d_out = jnp.hstack([r[...].reshape(-1, HEAD_DIM) for r in (dk_u, dv_u)])
    for out, half in outs:

        @pl.loop(0, FOUR)
        def _(zz, out=out, half=half):
            h = h_own[:, :, :, aligned(half * FOUR + zz)].reshape(-1, BLK)
            out[zz] = dot(h, d_out, (0,), (0,)).reshape(out.shape[1:])


def gather_kernel(*refs):
    take = taker(refs)
    wo_ref, wq_ref, dkv_ref, cos_ref, sin_ref, h_ref = take(6)
    grad_ins, outs, (dx_ref, dgain_ref) = take(6), take(FOUR), take(TWO)
    own_sem, send_sem, come_sem, core_sem, put_sem, all_terms, totals, g_s, g_r = take(9)
    terms, wkv_ref, h_own, dk_u, dv_u, store, wkv_store = take(7)
    buffers, sems, refs = take(FOUR), take(7), take(len(refs))
    me = lax.axis_index("cp")
    z, y, x, core = place(me)
    line = Line(me)
    to = {"x": dev(z, y, 1 - x, core), "y": dev(z, 1 - y, x, core), "u": line.next[1], "d": line.next[-1]}
    partner = dev(z, y, x, 1 - core)
    chip_here = me // TWO
    n_wo, wide = wo_ref.shape[0], wq_ref.shape[1]
    store[chip_here, pl.ds(0, n_wo)] = wo_ref[...]
    for i in range(TWO):
        store[chip_here, pl.ds(n_wo, n_wo), pl.ds(i * wide, wide)] = wq_ref[pl.ds(i * n_wo, n_wo)]
    meet(quad_of(me)[1:] + [to["y"]] + [dev(zz, y, x, core) for _, zz in z_peers(z)])
    load_h = pltpu.make_async_copy(h_ref, h_own, own_sem.at[0])
    load_h.start()
    wkv = PairSum(me, "core", 1, wkv_ref, wkv_store.at[chip_here], buffers, [r.at[0] for r in sems])

    def place_of(key):
        dz, ry, rx = key
        return z + dz, 1 - y if ry else y, 1 - x if rx else x

    def block(part, key):
        zz, yy, xx = place_of(key)
        chip = (TWO * zz + yy) * TWO + xx
        return wkv_store.at[chip] if part == THREE else store.at[chip, pl.ds(CUTS[part], CUTS[part + 1] - CUTS[part])]

    def windows(part, key):
        zz, yy, xx = place_of(key)
        pair, src = TWO * zz + yy, block(part, key)
        wo_at, wq_at = ((xx * TWO + core) * N_PAIRS + pair) * n_wo, (core * N_PAIRS + pair) * wq_ref.shape[0]
        if part == THREE:
            for i, out in enumerate(outs[TWO:]):
                yield src.at[:, head(i)], out.at[pl.ds(wq_at, wq_ref.shape[0]), pl.ds(xx * HEAD_DIM, HEAD_DIM)]
            return
        first, last = CUTS[part : part + TWO]
        if first < n_wo:
            rows = min(last, n_wo) - first
            yield src.at[pl.ds(0, rows)], outs[0].at[pl.ds(wo_at + first, rows)]
        if last > n_wo:
            skip = max(n_wo - first, 0)
            rows, at = last - first - skip, first + skip - n_wo
            for i in range(TWO):
                window = outs[1].at[pl.ds(wq_at + i * n_wo + at, rows), pl.ds(xx * wide, wide)]
                yield src.at[pl.ds(skip, rows), pl.ds(i * wide, wide)], window

    def index(part, key):
        return (part, key[0] + THREE) + key[1:]

    def send(part, key, link, there):
        sent = send_sem.at[index(part, key) + (LINKS.find(link or "-") + 1,)]
        if link:
            remote(block(part, key), block(part, key), sent, come_sem.at[index(part, there)], to[link]).start()
            return
        for src, window in windows(part, key):
            remote(src, window, sent, core_sem.at[index(part, key)], partner).start()
            pltpu.make_async_copy(src, window, put_sem.at[index(part, key)]).start()

    def whole(part, send, arrive):
        size = CUTS[part + 1] - CUTS[part] if part < THREE else wkv_store.size // store.shape[0] // outs[0].shape[1]
        dst = outs[0].at[pl.ds(0, size)]
        return remote(dst, dst, send, arrive, me)

    def when(on, do):
        pl.when(on)(do)

    def each_way(part, key):
        held = line.held(key[0])
        yield None, key, held
        for link, there in onward(ORDERS[part], key):
            inside = {"u": line.inside[1], "d": line.inside[-1]}.get(link)
            yield link, there, held if inside is None else jnp.logical_and(held, inside)

    def pass_on(part, key):
        for link, there, on in each_way(part, key):
            when(on, functools.partial(send, part, key, link, there))

    def term_copy(i):
        src = terms if i == 0 else totals.at[i - 1]
        return remote(src, all_terms.at[i], g_s.at[i], g_r.at[i], me ^ (1 << i))

    def add_terms(i):
        term_copy(i).wait_recv()
        totals[i] = (terms[...] if i == 0 else totals[i - 1]) + all_terms[i]
        if i + 1 < len(GAIN_AT):
            term_copy(i + 1).start()

    def tile(t):
        job.tile(t)
        if t == job.tiles - 1:
            term_copy(0).start()

    def sum_step(h):
        wkv.step(0, h)

    steps = [(TILES_FROM + t * TILE_EVERY, functools.partial(tile, t)) for t in range(HiddenGradient.tiles)]
    steps += [(at, functools.partial(sum_step, h)) for h, at in enumerate(SUM_AT)]
    steps += [(at, functools.partial(add_terms, i)) for i, at in enumerate(GAIN_AT)]
    steps.sort(key=lambda s: s[0])
    events = arrivals()
    for part in range(THREE):
        pass_on(part, HERE)
    turn_back(dkv_ref, cos_ref, sin_ref, dk_u, dv_u)
    job = HiddenGradient(me, dk_u, dv_u, grad_ins, (dx_ref, terms), refs)
    load_h.wait()
    wkv_terms(h_own, dk_u, dv_u, ((wkv_ref, 1 - core), (buffers[0], core)))
    wkv.begin(0)
    wkv.loaded(0)
    for now, part, key in events:
        while steps and steps[0][0] <= now:
            steps.pop(0)[1]()
        if any(key):
            arrive = come_sem.at[index(part, key)]
            when(line.held(key[0]), whole(part, own_sem.at[0], arrive).wait_recv)
            pass_on(part, key)
        elif part == THREE:
            pass_on(part, key)
    dgain_ref[...] = totals[len(GAIN_AT) - 1]
    for i in range(len(GAIN_AT)):
        term_copy(i).wait_send()
    for _, part, key in events:
        for sem in (core_sem, put_sem):
            when(line.held(key[0]), whole(part, own_sem.at[0], sem.at[index(part, key)]).wait_recv)
        for link, there, on in each_way(part, key):
            sent = send_sem.at[index(part, key) + (LINKS.find(link or "-") + 1,)]
            when(on, whole(part, sent, own_sem.at[0]).wait_send)
    wkv.wait_send(0)
    job.finish()


def gather_all(wo, wq, dkv, cos_f, sin_f, h_u, part, w_k, w_v, x, dy, gain, shapes):
    dma = pltpu.SemaphoreType.DMA
    vmem, hbm = pl.BlockSpec(memory_space=pltpu.VMEM), pl.BlockSpec(memory_space=pl.ANY)
    block = w_k.shape[0] // TWO // N_PAIRS, w_k.shape[1]
    parts = len(ORDERS)
    keys = (parts, 7, TWO, TWO)
    terms = 1, x.shape[1]
    scratch = [dma((1,)), dma(keys + (len(LINKS) + 1,)), dma(keys), dma(keys), dma(keys)]
    n = len(GAIN_AT)
    scratch += [pltpu.VMEM((n,) + terms, F32)] * TWO + [dma((n,)), dma((n,)), pltpu.VMEM(terms, F32)]
    scratch += [pltpu.VMEM((FOUR, TWO) + block, F32), pltpu.VMEM(h_u.shape, BF16)]
    scratch += [pltpu.VMEM((TWO, TWO, BLK, HEAD_DIM), BF16)] * TWO
    scratch += [pltpu.VMEM((TWO * N_PAIRS,) + b, F32) for b in ((TWO * wo.shape[0], wo.shape[1]), block)]
    return pl.pallas_call(
        gather_kernel,
        name="gather_all",
        out_shape=[jax.ShapeDtypeStruct(s, F32) for s in shapes]
        + [jax.ShapeDtypeStruct(x.shape, BF16), jax.ShapeDtypeStruct(terms, F32)],
        in_specs=[vmem] * 5 + [hbm] + [vmem] * 6,
        out_specs=[hbm] * len(shapes) + [vmem] * TWO,
        scratch_shapes=scratch + PairSum.scratch("core", block) + PairSum.sems(1, 1) + HiddenGradient.scratch(x),
        compiler_params=params(63, collective_id=0),
        cost_estimate=cost(1, 76),
    )(wo, wq, dkv, cos_f, sin_f, h_u, part, w_k, w_v, x, dy, gain)


def perm(x, pairs):
    return lax.ppermute(x, "cp", pairs)


def flip_pairs(d):
    return [(r, r ^ d) for r in range(32)]


def solution(mesh):
    def local_step(hidden, grad_out, positions, seg_ids, w_q, w_k, w_v, w_o, norm_gain):
        n_batch, n_tok, d_model = hidden.shape
        n_rows = n_batch * n_tok
        wide = N_HEADS * HEAD_DIM
        me = lax.axis_index("cp")
        z, y, x, core = place(me)
        quad, pair = me % FOUR, me // FOUR
        relations = range(FOUR)

        def swap(pieces):
            return [perm(p, flip_pairs(d)) if d else p for d, p in enumerate(pieces)]

        gain = norm_gain.astype(F32)
        cos_t, sin_t = rope_tables(positions.reshape(n_rows))
        cos_f, sin_f = jnp.hstack([cos_t, cos_t]), jnp.hstack([-sin_t, sin_t])
        dy_flat = grad_out.reshape(n_rows, d_model)
        normed, kv_home = project(hidden.reshape(n_rows, d_model), gain[NEW], w_k, w_v, cos_f, sin_f)
        pos = jnp.pad(positions.reshape(TWO, TWO, n_tok), ((0, 0), (0, 6), (0, 0)))
        kv_home = kv_home.reshape((TWO,) * 5 + (CHUNK, HEAD_DIM))
        kv_all, q_u, do_u, pos_u, *dy_rows = exchange(kv_home, normed, dy_flat, pos, cos_f, sin_f, w_q, w_o)
        pos_u = pos_u[:, :TWO].reshape((FOUR, TWO, TWO, CHUNK)).transpose(1, TWO, 0, THREE).reshape(TWO, TWO, BLK)
        dy_rows = [a.reshape(TWO, TWO, CHUNK, d_model) for a in dy_rows]
        dy_pieces = swap([dy_rows[d % TWO] for d in relations])

        member = quad ^ jnp.arange(FOUR)
        front, back = ((m[:, NEW] * CHUNK + jnp.arange(CHUNK)[NEW]).reshape(BLK) for m in (member, THREE - member))
        offsets = jnp.stack([front, back]).astype(jnp.int32)
        own_super = jnp.stack([pair, N_SUPER - 1 - pair]).astype(jnp.int32)
        q_index = own_super[:, NEW] * BLK + offsets
        start = q_index[NEW] - pos_u
        tab = jnp.concatenate(
            [own_super, (jnp.min(start, axis=-1) // BLK).reshape(-1), jnp.max(start, axis=-1).reshape(-1)]
        )
        start_r = start[:, :, NEW, :]
        q_index_r = jnp.broadcast_to(q_index[NEW, :, NEW, :], start_r.shape)
        cos_u, sin_u = rope_tables(pos_u)
        cos_ut, sin_ut = jnp.swapaxes(cos_u, TWO, THREE), jnp.swapaxes(sin_u, TWO, THREE)

        koff = offsets[:, NEW]
        attn_u, lse = flash_fwd(tab, q_u, kv_all, start_r, q_index_r, koff)

        wo_keep, wo_away = wo_terms(attn_u, dy_pieces)
        wo_come = perm(wo_away, flip_pairs(FOUR))
        do_u, wo_keep = lax.optimization_barrier((do_u, wo_keep))
        dq_u, dkv = flash_bwd(tab, q_u, do_u, attn_u, kv_all, lse, start_r, q_index_r, koff, cos_ut, sin_ut)

        x_flat = hidden.reshape(n_rows, d_model)
        wo_own, dkv_own, wq_own, block_out, d_part, h_u = reduce_pairs(
            [wo_keep, wo_come, dkv.reshape(FOUR, TWO, -1, HEAD_DIM)],
            [wo_keep.shape[1:], (dkv.size // N_PAIRS // HEAD_DIM, HEAD_DIM), (d_model // TWO // N_PAIRS, wide)],
            (TWO, 8, 8),
            ("z", "", "core"),
            TWO,
            Products,
            (attn_u, dq_u, x_flat, normed.reshape((TWO,) * THREE + (CHUNK, d_model)), w_o, w_q),
        )
        grad_wo, grad_wq, grad_wk, grad_wv, grad_x, d_gain = gather_all(
            wo_own,
            wq_own,
            dkv_own,
            cos_ut,
            sin_ut,
            h_u,
            d_part,
            w_k,
            w_v,
            x_flat,
            dy_flat,
            gain[NEW],
            [w_o.shape, w_q.shape, w_k.shape, w_v.shape],
        )
        block_out, grad_x = (a.reshape(hidden.shape) for a in (block_out, grad_x))
        return block_out, grad_x, grad_wq, grad_wk, grad_wv, grad_wo, d_gain.reshape(d_model)

    seq_spec = P(None, "cp", None)
    tok_spec = P(None, "cp")
    full_spec = P()
    return jax.shard_map(
        local_step,
        mesh=mesh,
        in_specs=(seq_spec, seq_spec, tok_spec, tok_spec, full_spec, full_spec, full_spec, full_spec, full_spec),
        out_specs=(seq_spec, seq_spec, full_spec, full_spec, full_spec, full_spec, full_spec),
        check_vma=False,
    )
```

```python
import functools
import heapq
import itertools

import jax
import jax.numpy as jnp
from jax import lax
from jax.experimental import pallas as pl
from jax.experimental.pallas import tpu as pltpu
from jax.sharding import PartitionSpec as P

HEAD_DIM = 128
NORM_EPS = 1e-5
ROPE_BASE = 500000.0
NEG_BIG = -1e30
LOG2E = 1.4426950408889634
ATTN_SCALE = HEAD_DIM**-0.5
EXP2_SCALE = ATTN_SCALE * LOG2E
CHUNK = 64
TWO = 2
THREE = 3
FOUR = 4
NEW = jnp.newaxis
BLK = 4 * CHUNK
N_HEADS = 8
N_PAIRS = 8
N_SUPER = 2 * N_PAIRS
MESH = pl.DeviceIdType.MESH
ONE = pl.Squeezed()
GROUP = 4
DIRECT = 2
MADE_AT = 5
PRODUCTS_AT = 7, 9
F32 = jnp.float32
BF16 = jnp.bfloat16

T_SQ, T_LO, T_MX = 0, 2, 6


def rope_tables(positions):
    inv_freq = ROPE_BASE ** (-jnp.arange(0, HEAD_DIM, TWO).astype(F32) / HEAD_DIM)
    angles = positions.astype(F32)[..., None] * inv_freq
    return jnp.cos(angles), jnp.sin(angles)


def dot(a, b, ca, cb):
    return lax.dot_general(a, b, ((ca, cb), ((), ())), preferred_element_type=F32)


def cost(gflop, mib):
    return pl.CostEstimate(flops=gflop * 10**9, bytes_accessed=mib << 20, transcendentals=0)


def params(mib, **more):
    return pltpu.CompilerParams(vmem_limit_bytes=mib << 20, **more)


def row_mean(x):
    return jnp.mean(x, axis=-1, keepdims=True)


def head(h):
    return pl.ds(h * HEAD_DIM, HEAD_DIM)


def head_slice(h):
    return slice(h * HEAD_DIM, (h + 1) * HEAD_DIM)


def dot_t(a, b):
    return dot(a, b, (1,), (1,))


def steps(tab, body):
    b, hf = pl.program_id(0), pl.program_id(1)
    own, first, last_start = tab[T_SQ + hf], tab[T_LO + TWO * b + hf], tab[T_MX + TWO * b + hf]

    def place_of(s):
        late = s >= N_PAIRS
        return jnp.where(late, N_SUPER - 1 - s, s), late.astype(jnp.int32)

    full_from = jnp.minimum((last_start + BLK - 1) // BLK, own)
    full_from += lax.rem(own - full_from, TWO)
    count = full_from - first

    @pl.loop(0, count + 1)
    def _(t):
        s = jnp.where(t < count, first + t, own)
        body(s, place_of(s), True)

    @pl.loop(0, (own - full_from) // TWO)
    def _(t):
        for i in range(TWO):
            s = full_from + TWO * t + i
            body(s, place_of(s), False)


def down(row, n):
    return jnp.broadcast_to(row, (n, row.shape[-1])).T


def may_use(s, off, st_ref, qi_ref):
    return jnp.logical_and(off >= st_ref[...] - s * BLK, off <= qi_ref[...] - s * BLK)


def fwd_kernel(tab, q_ref, kv_ref, st_ref, qi_ref, ko_ref, o_ref, lse_ref, q_s, acc, m_s, l_s, k_t, bounds):
    m_s[...] = jnp.full_like(m_s, NEG_BIG)
    l_s[...] = jnp.zeros_like(l_s)
    acc[...] = jnp.zeros_like(acc)
    for i, ref in enumerate((st_ref, qi_ref)):
        bounds[i] = down(ref[...], HEAD_DIM)
    for h in range(N_HEADS):
        q_s[pl.ds(h * BLK, BLK)] = q_ref[:, head(h)]

    @pl.when(pl.program_id(1) == 0)
    def _():
        @pl.loop(0, N_PAIRS)
        def _(pair):
            for hk in range(TWO):
                k_t[pair, hk] = kv_ref[pair, 0, hk].T

    def body(s, at, masked):
        pair, hk = at
        v = kv_ref[pair, 1, hk]
        if masked:
            off = ko_ref[hk] + s * BLK
            mask = [
                jnp.logical_and(off[:, lanes] >= bounds[0], off[:, lanes] <= bounds[1])
                for lanes in (slice(HEAD_DIM), slice(HEAD_DIM, BLK))
            ]
            mask = [jnp.concatenate([m, m], axis=0) for m in mask]
        for g in range(N_HEADS // TWO):
            rows = pl.ds(g * TWO * BLK, TWO * BLK)
            sc = jnp.dot(q_s[rows], k_t[pair, hk], preferred_element_type=F32)
            sc = [sc[:, :HEAD_DIM], sc[:, HEAD_DIM:]]
            if masked:
                sc = [jnp.where(m, x, NEG_BIG) for m, x in zip(mask, sc)]
            m_old = m_s[rows]
            m_new = jnp.maximum(m_old, jnp.max(jnp.maximum(*sc), axis=1, keepdims=True))
            alpha = jnp.exp2((m_old - m_new) * EXP2_SCALE)
            p = [jnp.exp2((x - m_new) * EXP2_SCALE) for x in sc]
            m_s[rows] = m_new
            l_s[rows] = l_s[rows] * alpha + (p[0] + p[1])
            p = jnp.hstack([x.astype(BF16) for x in p])
            acc[rows] = acc[rows] * alpha + jnp.dot(p, v, preferred_element_type=F32)

    steps(tab, body)
    for h in range(N_HEADS):
        rows = pl.ds(h * BLK, BLK)
        total = jnp.sum(l_s[rows], axis=1, keepdims=True)
        o_ref[:, head(h)] = (acc[rows] / total).astype(BF16)
        lse_ref[h] = (m_s[rows] * EXP2_SCALE + jnp.log2(total)).T[:1]


def bwd_kernel(tab, q_ref, do_ref, o_ref, kv_ref, lse_ref, st_ref, qi_ref, ko_ref, cos_ref, sin_ref, dq_ref, dkv_ref, *scratch):
    dq_acc, delta, off_s, q_s, do_s, q_t, do_t, p_s, ds_s = scratch
    dq_acc[...] = jnp.zeros_like(dq_acc)
    for h in range(N_HEADS):
        q, do = q_ref[:, head(h)], do_ref[:, head(h)]
        delta[h] = jnp.sum((do.astype(F32) * o_ref[:, head(h)].astype(F32)).T, axis=0, keepdims=True)
        q_s[pl.ds(h * BLK, BLK)], do_s[pl.ds(h * BLK, BLK)] = q, do
        q_t[h], do_t[h] = q.T, do.T

    @pl.when(pl.program_id(1) == 0)
    def _():
        dkv_ref[...] = jnp.zeros_like(dkv_ref)
        for hk in range(TWO):
            off_s[hk] = down(ko_ref[hk], BLK)

    def body(s, at, masked):
        pair, hk = at
        k = kv_ref[pair, 0, hk]
        v = kv_ref[pair, 1, hk]
        k_t = k.T
        mask = may_use(s, off_s[hk], st_ref, qi_ref) if masked else None
        for first in range(0, N_HEADS, GROUP):
            rows = pl.ds(first * BLK, GROUP * BLK)
            for h in range(first, first + GROUP):
                cols = pl.ds(h * BLK, BLK)
                p = jnp.exp2(jnp.dot(k, q_t[h], preferred_element_type=F32) * EXP2_SCALE - lse_ref[h])
                if masked:
                    p = jnp.where(mask, p, 0.0)
                ds = p * (jnp.dot(v, do_t[h], preferred_element_type=F32) - delta[h])
                p_s[:, cols] = p.astype(BF16)
                ds_s[:, cols] = ds.astype(BF16)
            dkv_ref[pair, 0, hk] += jnp.dot(ds_s[:, rows], q_s[rows], preferred_element_type=F32)
            dkv_ref[pair, 1, hk] += jnp.dot(p_s[:, rows], do_s[rows], preferred_element_type=F32)
            dq_acc[:, rows] += jnp.dot(k_t, ds_s[:, rows], preferred_element_type=F32)

    steps(tab, body)
    cos_t, sin_t = cos_ref[...], sin_ref[...]
    half = HEAD_DIM // TWO
    for h in range(N_HEADS):
        cols = pl.ds(h * BLK, BLK)
        a, c = dq_acc[:half, cols] * ATTN_SCALE, dq_acc[half:, cols] * ATTN_SCALE
        lin = jnp.concatenate([a * cos_t + c * sin_t, c * cos_t - a * sin_t], axis=0)
        dq_ref[:, head(h)] = lin.T.astype(BF16)


def attn_specs():
    def at_tile(b, h, t):
        return (b, h) + (0,) * TWO

    def at_row(b, h, t):
        return (0, 0, b) + (0,) * THREE

    tile = pl.BlockSpec((ONE, ONE, BLK, N_HEADS * HEAD_DIM), at_tile)
    row = pl.BlockSpec((ONE, ONE, 1, BLK), at_tile)
    stat = pl.BlockSpec((ONE, ONE, N_HEADS, 1, BLK), lambda b, h, t: (b, h) + (0,) * THREE)
    rope = pl.BlockSpec((ONE, ONE, HEAD_DIM // TWO, BLK), at_tile)
    kv = pl.BlockSpec((N_PAIRS, TWO, ONE, TWO, BLK, HEAD_DIM), at_row)
    ko = pl.BlockSpec((TWO, 1, BLK), lambda b, h, t: (0,) * THREE)
    return tile, row, stat, kv, ko, rope


def flash_fwd(tab, q, kv, start, qidx, koff):
    tile, row, stat, kvs, ko, _ = attn_specs()
    return pl.pallas_call(
        fwd_kernel,
        name="attn_fwd",
        out_shape=(jax.ShapeDtypeStruct(q.shape, BF16), jax.ShapeDtypeStruct((TWO, TWO, N_HEADS, 1, BLK), F32)),
        grid_spec=pltpu.PrefetchScalarGridSpec(
            num_scalar_prefetch=1,
            grid=(TWO, TWO),
            in_specs=[tile, kvs, row, row, ko],
            out_specs=[tile, stat],
            scratch_shapes=[pltpu.VMEM((N_HEADS * BLK, HEAD_DIM), t) for t in (BF16, F32, F32, F32)]
            + [pltpu.VMEM((N_PAIRS, TWO, HEAD_DIM, BLK), BF16), pltpu.VMEM((TWO, BLK, HEAD_DIM), jnp.int32)],
        ),
        compiler_params=params(63),
        cost_estimate=cost(20, 16),
    )(tab, q, kv, start, qidx, koff)


def flash_bwd(tab, q, do, o, kv, lse, start, qidx, koff, cos_t, sin_t):
    tile, row, stat, kvs, ko, rope = attn_specs()
    return pl.pallas_call(
        bwd_kernel,
        name="attn_bwd",
        out_shape=(
            jax.ShapeDtypeStruct(q.shape, BF16),
            jax.ShapeDtypeStruct(kv.shape, F32),
        ),
        grid_spec=pltpu.PrefetchScalarGridSpec(
            num_scalar_prefetch=1,
            grid=(TWO, TWO),
            in_specs=[tile, tile, tile, kvs, stat, row, row, ko, rope, rope],
            out_specs=[tile, kvs],
            scratch_shapes=[pltpu.VMEM((HEAD_DIM, N_HEADS * BLK), F32), pltpu.VMEM((N_HEADS, 1, BLK), F32)]
            + [pltpu.VMEM((TWO, BLK, BLK), jnp.int32)]
            + [pltpu.VMEM((N_HEADS * BLK, HEAD_DIM), BF16)] * TWO
            + [pltpu.VMEM((N_HEADS, HEAD_DIM, BLK), BF16)] * TWO
            + [pltpu.VMEM((BLK, N_HEADS * BLK), BF16)] * TWO,
        ),
        compiler_params=params(63),
        cost_estimate=cost(50, 32),
    )(tab, q, do, o, kv, lse, start, qidx, koff, cos_t, sin_t)


def turn(x, cos_ref, sin_ref):
    return x * cos_ref[...] + pltpu.roll(x, HEAD_DIM // TWO, 1) * sin_ref[...]


def first_kernel(x_ref, g_ref, wk_ref, wv_ref, cos_ref, sin_ref, h_ref, kv_ref):
    x = x_ref[...].astype(F32)
    h = (x * lax.rsqrt(row_mean(x * x) + NORM_EPS) * g_ref[...]).astype(BF16)
    h_ref[...] = h
    k = jnp.dot(h, wk_ref[...], preferred_element_type=F32)
    v = jnp.dot(h, wv_ref[...], preferred_element_type=F32)
    n = kv_ref.shape[THREE]
    for i in range(TWO):
        for j, val in enumerate((turn(k[:, head_slice(i)], cos_ref, sin_ref), v[:, head_slice(i)])):
            for c in range(TWO):
                kv_ref[i, c, j] = val[c * n : (c + 1) * n].astype(BF16)


def project(x, gain, w_k, w_v, cos_f, sin_f):
    n = x.shape[0] // TWO
    return pl.pallas_call(
        first_kernel,
        name="norm_kv",
        out_shape=(jax.ShapeDtypeStruct(x.shape, BF16), jax.ShapeDtypeStruct((TWO,) * THREE + (n, HEAD_DIM), BF16)),
        compiler_params=params(20),
        cost_estimate=cost(TWO, 7),
    )(x, gain, w_k, w_v, cos_f, sin_f)


def place(me):
    return me // 8, lax.rem(me // FOUR, TWO), lax.rem(me // TWO, TWO), lax.rem(me, TWO)


def dev(z, y, x, core):
    return ((z * TWO + y) * TWO + x) * TWO + core


def z_peers(z):
    return [(k, lax.rem(z + k, FOUR)) for k in (1, TWO, THREE)]


def announce(peers):
    barrier = pltpu.get_barrier_semaphore()
    for d in peers:
        pl.semaphore_signal(barrier, device_id=(d,), device_id_type=MESH)
    return lambda: pl.semaphore_wait(barrier, len(peers))


def meet(peers):
    announce(peers)()


def remote(src, dst, send, arrive, to):
    return pltpu.make_async_remote_copy(
        src_ref=src, dst_ref=dst, send_sem=send, recv_sem=arrive, device_id=(to,), device_id_type=MESH
    )


class Line:
    order = (0, 1, -1, TWO, -TWO, THREE, -THREE)

    def __init__(self, me):
        self.z, y, x, core = place(me)
        self.next = {1: dev(self.z + 1, y, x, core), -1: dev(self.z - 1, y, x, core)}
        self.inside = {1: self.z < THREE, -1: self.z > 0}

    def held(self, dz):
        return jnp.logical_and(self.z + dz >= 0, self.z + dz <= THREE)

    def ways(self, dz):
        for d in self.next:
            if d * dz <= 0:
                yield d, self.inside[d] if dz == 0 else jnp.logical_and(self.inside[d], self.held(dz))


def tiled(n, fetch, use, first=0):
    fetch(first, 0).start()

    @pl.loop(0, n)
    def _(t):
        slot = lax.rem(t, TWO)
        fetch(first + t, slot).wait()

        @pl.when(t + 1 < n)
        def _():
            fetch(first + t + 1, 1 - slot).start()

        use(first + t, slot)


def aligned(t, size=BLK):
    return pl.ds(pl.multiple_of(t * size, size), size)


def exchange_kernel(*refs):
    take = taker(refs)
    kv_ref, h_ref, dy_ref, pos_ref, cos_ref, sin_ref, wq_ref, wo_ref, kv_all, q_u, do_u, pos_u, *dy_rows = take(14)
    own_sem, quad_s, quad_r, z_s, z_r, y_s, y_r, q_home, do_home, wq_buf, wo_buf, w_sem, dy_sem = take(len(refs))
    me = lax.axis_index("cp")
    z, y, x, core = place(me)
    quad, line = quad_of(me), Line(me)
    across = dev(z, 1 - y, x, core)
    meet(quad[1:] + [across] + [dev(zz, y, x, core) for _, zz in z_peers(z)])

    def source(a, d):
        xx, cc = 1 - x if d // TWO else x, 1 - core if d % TWO else core
        return pos_ref.at[cc] if a == THREE else (kv_ref, q_home, do_home)[a].at[xx, cc]

    def target(a, d):
        if a == THREE:
            return pos_u.at[d]
        tok = pl.ds(d * CHUNK, CHUNK)
        return kv_all.at[me // FOUR, :, :, :, tok] if a == 0 else (q_u, do_u)[a - 1].at[:, :, tok]

    def quad_copy(a, d):
        return remote(source(a, d), target(a, d), quad_s.at[a, d], quad_r.at[a, d], quad[d])

    def own_copy(a):
        return pltpu.make_async_copy(source(a, 0), target(a, 0), own_sem.at[a])

    def z_copy(part, dz, d):
        block = kv_all.at[TWO * (z + dz) + y, part]
        return remote(block, block, z_s.at[part, (d + 1) // TWO, dz + THREE], z_r.at[part, dz - d + THREE], line.next[d])

    def y_copy(part, dz, yy=y):
        block = kv_all.at[TWO * (z + dz) + yy, part]
        return remote(block, block, y_s.at[part, dz + THREE], y_r.at[part, dz + THREE], across)

    parts = range(TWO)
    moves = [(part, dz) for dz in line.order for part in parts]

    def pass_on(count):
        for part, dz in [moves.pop(0) for _ in range(count)]:
            if dz:
                block = kv_all.at[TWO * (z + dz) + y, part]
                arrival = remote(block, block, own_sem.at[0], z_r.at[part, dz + THREE], me)
                pl.when(line.held(dz))(arrival.wait_recv)
            for d, on in line.ways(dz):
                pl.when(on)(z_copy(part, dz, d).start)
            pl.when(line.held(dz))(y_copy(part, dz).start)

    n = h_ref.shape[1] // BLK // TWO

    def fetch_q(t, slot):
        return pltpu.make_async_copy(wq_ref.at[:, aligned(t)], wq_buf.at[slot], w_sem.at[0, slot])

    def fetch_o(t, slot):
        return pltpu.make_async_copy(wo_ref.at[aligned(t)], wo_buf.at[slot], w_sem.at[1, slot])

    def put(home, t, val):
        home[t // n, :, :, :, :, aligned(lax.rem(t, n))] = val.astype(BF16).reshape(home.shape[1:-1] + (BLK,))

    def query(t, slot):
        q = jnp.dot(h_ref[...], wq_buf[slot], preferred_element_type=F32)
        put(q_home, t, jnp.hstack([turn(q[:, head_slice(j)], cos_ref, sin_ref) for j in range(BLK // HEAD_DIM)]))

    def pull(t, slot):
        put(do_home, t, dot_t(dy_ref[...], wo_buf[slot]))

    all_moves = list(moves)
    half = dy_ref.shape[0] // TWO
    for i, out in enumerate(dy_rows):
        pltpu.make_async_copy(dy_ref.at[aligned(core if i == 0 else 1 - core, half)], out, dy_sem.at[i]).start()
    for a in (0, THREE):
        for d in (1, TWO, THREE):
            quad_copy(a, d).start()
        own_copy(a).start()
    for a, (fetch, use) in enumerate(((fetch_q, query), (fetch_o, pull)), 1):
        for near in range(TWO):
            tiled(n, fetch, use, n * (x if near else 1 - x))
            for d in range(TWO):
                if d or not near:
                    quad_copy(a, d if near else d + TWO).start()
            if near:
                own_copy(a).start()
            if len(moves) == len(all_moves):
                own_copy(0).wait()
                for d in (1, TWO, THREE):
                    quad_copy(0, d).wait_recv()
            pass_on(TWO)
    pass_on(len(moves))
    for part, dz in all_moves:
        for d, on in line.ways(dz):
            pl.when(on)(z_copy(part, dz, d).wait_send)
        pl.when(line.held(dz))(y_copy(part, dz, 1 - y).wait_recv)
        pl.when(line.held(dz))(y_copy(part, dz).wait_send)
    for a in range(FOUR):
        for d in (1, TWO, THREE):
            quad_copy(a, d).wait_send()
            if a > 0:
                quad_copy(a, d).wait_recv()
    for a in (1, TWO, THREE):
        own_copy(a).wait()
    for i, out in enumerate(dy_rows):
        pltpu.make_async_copy(dy_ref.at[aligned(core if i == 0 else 1 - core, half)], out, dy_sem.at[i]).wait()


def exchange(kv, h, dy, pos, cos_f, sin_f, w_q, w_o):
    dma = pltpu.SemaphoreType.DMA
    vmem, hbm = pl.BlockSpec(memory_space=pltpu.VMEM), pl.BlockSpec(memory_space=pl.ANY)
    wide = w_q.shape[1] // TWO
    unit = jax.ShapeDtypeStruct((TWO, TWO, BLK, wide), BF16)
    pos_quad = jax.ShapeDtypeStruct((FOUR,) + pos.shape[1:], pos.dtype)
    dy_half = jax.ShapeDtypeStruct((dy.shape[0] // TWO, dy.shape[1]), BF16)
    home = pltpu.VMEM((TWO,) * FOUR + (CHUNK, wide), BF16)
    sems = [dma((FOUR,))] + [dma((FOUR, FOUR))] * TWO + [dma((TWO, TWO, 7))] + [dma((TWO, 7))] * THREE
    bufs = [pltpu.VMEM((TWO,) + b, BF16) for b in ((w_q.shape[0], BLK), (BLK, w_o.shape[1]))]
    return pl.pallas_call(
        exchange_kernel,
        name="exchange",
        out_shape=(jax.ShapeDtypeStruct((N_PAIRS,) + (TWO,) * THREE + (BLK, HEAD_DIM), BF16), unit, unit, pos_quad, dy_half, dy_half),
        in_specs=[vmem] * 6 + [hbm] * TWO,
        out_specs=[hbm] * 6,
        scratch_shapes=sems + [home, home] + bufs + [dma((TWO, TWO)), dma((TWO,))],
        compiler_params=params(63, collective_id=1),
        cost_estimate=cost(1, 20),
    )(kv, h, dy, pos, cos_f, sin_f, w_q, w_o)


def taker(refs):
    rest = iter(refs)
    return lambda count: list(itertools.islice(rest, count))


def wo_kernel(*refs):
    take = taker(refs)
    o_ref, *pieces = take(5)
    keep, away, dy_u, o_t, terms, came, load_sem, core_s, core_r = take(len(refs))
    me = lax.axis_index("cp")
    _, y, _, core = place(me)
    all_here = announce(quad_of(me)[1:TWO])
    loads = [
        pltpu.make_async_copy(src, dy_u.at[:, :, pl.ds(d * CHUNK, CHUNK)], load_sem.at[d])
        for d, src in enumerate(pieces)
    ]
    for c in loads:
        c.start()
    for h in range(N_HEADS):
        o_t[head(h)] = o_ref[:, :, :, head(h)].reshape(-1, HEAD_DIM).T
    for c in loads:
        c.wait()
    all_here()
    half, tiles = terms.shape[1], terms.shape[TWO] // BLK

    def swap(t):
        return remote(terms.at[0, :, aligned(t)], came.at[:, aligned(t)], core_s.at[t], core_r.at[t], quad_of(me)[1])

    def half_terms(i, to, then):
        @pl.loop(0, tiles)
        def _(t):
            dy = dy_u[:, :, :, aligned(t)].reshape(-1, BLK)
            terms[to, :, aligned(t)] = jnp.dot(o_t[aligned(i, half)], dy, preferred_element_type=F32)
            then(t)

    half_terms(1 - core, 0, lambda t: swap(t).start())
    half_terms(core, 1, lambda t: swap(t).wait_recv())
    rows = keep.shape[1]
    for zz in range(FOUR):
        for out, yy in ((keep, y), (away, 1 - y)):
            at = aligned(TWO * zz + yy, rows)
            out[zz] = terms[1, at] + came[at]
    for t in range(tiles):
        swap(t).wait_send()


def wo_terms(o, pieces):
    dma = pltpu.SemaphoreType.DMA
    vmem, hbm = pl.BlockSpec(memory_space=pltpu.VMEM), pl.BlockSpec(memory_space=pl.ANY)
    n, d, wide = o.shape[0] * o.shape[1] * o.shape[TWO], pieces[0].shape[-1], o.shape[-1]
    half = wide // TWO
    return pl.pallas_call(
        wo_kernel,
        name="wo_terms",
        out_shape=[jax.ShapeDtypeStruct((FOUR, half // N_PAIRS, d), F32)] * TWO,
        in_specs=[vmem] + [hbm] * FOUR,
        out_specs=[vmem] * TWO,
        scratch_shapes=[pltpu.VMEM((TWO, TWO, BLK, d), BF16), pltpu.VMEM((wide, n), BF16)]
        + [pltpu.VMEM((TWO, half, d), F32), pltpu.VMEM((half, d), F32), dma((FOUR,)), dma((d // BLK,)), dma((d // BLK,))],
        compiler_params=params(63, collective_id=THREE),
        cost_estimate=cost(FOUR, 20),
    )(o, *pieces)


class PairSum:
    def __init__(self, me, kind, cut, src, out, buffers, sems, direct=0):
        self.me, self.kind, self.src, self.out = me, kind, src, out
        self.direct_from = cut - direct
        self.size = out.shape[0] // cut
        self.own, self.from_core, self.from_y, self.from_z = buffers
        self.load_sem, self.core_s, self.core_r, self.y_s, self.y_r, self.z_s, self.z_r = sems
        self.z, self.y, x, core = place(me)
        self.partner = dev(self.z, self.y, x, 1 - core)
        self.line = [(k, zz, dev(zz, self.y, x, core)) for k, zz in z_peers(self.z)]
        self.across = dev(self.z, 1 - self.y, x, core)
        self.next_z = dev(self.z + 1, self.y, x, core), dev(self.z - 1, self.y, x, core)

    def rows(self, j):
        return pl.ds(j * self.size, self.size)

    def mine(self, j, zz):
        at = self.rows(j)
        return self.own.at[zz, self.y, at] if self.kind == "core" else self.own.at[zz, at]

    def loads(self, j):
        at = self.rows(j)
        if self.kind == "z":
            pairs = zip(self.src, (self.own, self.from_y))
            return [pltpu.make_async_copy(a.at[:, at], b.at[:, at], s.at[j]) for (a, b), s in zip(pairs, (self.load_sem, self.y_r))]
        return [pltpu.make_async_copy(self.src.at[:, self.y, at], self.own.at[:, at], self.load_sem.at[j])]

    def core_copy(self, j):
        src, dst = (r.at[:, :, self.rows(j)] for r in (self.src, self.from_core))
        return remote(src, dst, self.core_s.at[j], self.core_r.at[j], self.partner)

    def y_copy(self, j):
        src = self.own if self.kind == "core" else self.src
        at = self.rows(j)
        return remote(src.at[:, 1 - self.y, at], self.from_y.at[:, at], self.y_s.at[j], self.y_r.at[j], self.across)

    def z_copy(self, j, way, zz, to):
        at = way, zz + way - 1
        return remote(self.mine(j, zz), self.from_z.at[*at, self.rows(j)], self.z_s.at[j, *at], self.z_r.at[j, *at], to)

    def begin(self, j):
        if self.kind == "core":
            self.core_copy(j).start()
            return
        for c in self.loads(j):
            c.start()
        if not self.kind:
            self.y_copy(j).start()

    def loaded(self, j):
        if self.kind != "core":
            for c in self.loads(j):
                c.wait()
        else:
            self.core_copy(j).wait_recv()
            at = self.rows(j)
            for zz in range(FOUR):
                self.own[zz, :, at] += self.from_core[zz, :, at]
            self.y_copy(j).start()
        if self.kind == "z":
            self.add_y(j)
            self.hop(j, 0)

    def add_y(self, j):
        for zz in range(FOUR):
            self.mine(j, zz)[...] += self.from_y[zz, self.rows(j)]

    def relay(self, j, way, zz, add):
        if add:
            self.z_copy(j, way, zz, self.me).wait_recv()
            self.mine(j, zz)[...] += self.from_z[way, zz + way - 1, self.rows(j)]
        self.z_copy(j, way, zz, self.next_z[way]).start()

    def hop(self, j, h):
        @pl.when(self.z == h)
        def _():
            for zz in range(THREE, h, -1):
                self.relay(j, 0, zz, h > 0)

        @pl.when(self.z == THREE - h)
        def _():
            for zz in range(THREE - h):
                self.relay(j, 1, zz, h > 0)

    def z_direct(self, j):
        for k, zz, to in self.line:
            at, there = (j, 0, k - 1), self.from_z.at[0, k - 1, self.rows(j)]
            yield remote(self.mine(j, zz), there, self.z_s.at[at], self.z_r.at[at], to), there

    def step(self, j, h):
        if j >= self.direct_from and h > 0:
            if h == 1:
                at = self.rows(j)
                self.out[at] = self.mine(j, self.z)[...]
                for c, arrived in self.z_direct(j):
                    c.wait_recv()
                    self.out[at] += arrived[...]
            return
        if h == 0 and self.kind != "z":
            self.y_copy(j).wait_recv()
            self.add_y(j)
            if j < self.direct_from:
                self.hop(j, 0)
            else:
                for c, _ in self.z_direct(j):
                    c.start()
        elif 0 < h < THREE:
            self.hop(j, h)
        elif h == THREE:
            at = self.rows(j)
            self.out[at] = self.mine(j, self.z)[...]
            for way, on in enumerate((self.z > 0, self.z < THREE)):

                @pl.when(on)
                def _(way=way):
                    self.z_copy(j, way, self.z, self.me).wait_recv()
                    self.out[at] += self.from_z[way, self.z + way - 1, at]

    def wait_send(self, j):
        if self.kind == "core":
            self.core_copy(j).wait_send()
        if self.kind != "z":
            self.y_copy(j).wait_send()
        if j >= self.direct_from:
            for c, _ in self.z_direct(j):
                c.wait_send()
            return
        for zz in range(FOUR):
            if zz > 0:
                pl.when(self.z < zz)(self.z_copy(j, 0, zz, self.next_z[0]).wait_send)
            if zz < THREE:
                pl.when(self.z > zz)(self.z_copy(j, 1, zz, self.next_z[1]).wait_send)

    @staticmethod
    def scratch(kind, block):
        unused = pltpu.VMEM((8, HEAD_DIM), F32)
        own = pltpu.VMEM(((FOUR, TWO) if kind == "core" else (FOUR,)) + block, F32)
        from_y = pltpu.VMEM((FOUR,) + block, F32)
        return [own, own if kind == "core" else unused, from_y, pltpu.VMEM((TWO, THREE) + block, F32)]

    @staticmethod
    def sems(*dims):
        dma = pltpu.SemaphoreType.DMA
        return [dma(dims)] * 5 + [dma(dims + (TWO, THREE))] * TWO


def reduce_kernel(cuts, kinds, work, *refs):
    n = len(cuts)

    take = taker(refs)
    ins = [take(TWO) if k == "z" else take(1)[0] for k in kinds[:-1]]
    more_in, outs, more_out, made = take(work.ins), take(n), take(work.outs), take(1)
    buffers, sems = [take(FOUR) for _ in kinds], take(7)
    me = lax.axis_index("cp")
    z, y, x, core = place(me)
    meet(quad_of(me)[1:] + [dev(z, 1 - y, x, core)] + [dev(zz, y, x, core) for _, zz in z_peers(z)])
    job = work(me, more_in, more_out, take(len(refs)))
    inputs = enumerate(zip(kinds, cuts, ins + made, outs, buffers))
    sums = [PairSum(me, *a, [r.at[i] for r in sems], DIRECT if i == n - 1 else 0) for i, a in inputs]
    pieces = [(s, j) for s, cut in zip(sums, cuts) for j in range(cut)]
    early, late = pieces[: -cuts[-1]], pieces[-cuts[-1] :]
    for s, j in early:
        s.begin(j)
    for s, j in early:
        s.loaded(j)
    for t in range(len(pieces) + THREE):
        if t == MADE_AT:
            job.wq_terms(sums[-1].own, made[0])
            for s, j in late:
                s.begin(j)
        if t == MADE_AT + 1:
            for s, j in late:
                s.loaded(j)
        for h in range(FOUR):
            if 0 <= t - h < len(pieces):
                s, j = pieces[t - h]
                s.step(j, h)
        job.step(t)
    for s, j in pieces:
        s.wait_send(j)
    job.finish()


def quad_of(me):
    z, y, x, core = place(me)
    return [dev(z, y, 1 - x if d // TWO else x, 1 - core if d % TWO else core) for d in range(FOUR)]


class Home:
    def __init__(self, me, src, out, own_sem, send, arrive):
        _, _, x, core = place(me)
        w = src.shape[-1]
        to = out.at[core, :, :, :, pl.ds(x * w, w)]

        def piece(d):
            return src.at[:, :, pl.ds(d * CHUNK, CHUNK)]

        self.own = pltpu.make_async_copy(piece(0), to, own_sem)
        self.copies = [remote(piece(d), to, send.at[d], arrive.at[d], quad_of(me)[d]) for d in (1, TWO, THREE)]

    def start(self):
        self.own.start()
        for c in self.copies:
            c.start()

    def wait_recv(self):
        self.own.wait()
        for c in self.copies:
            c.wait_recv()

    def wait_send(self):
        for c in self.copies:
            c.wait_send()


class Products:
    ins, outs = 6, THREE

    def __init__(self, me, ins, outs, scratch):
        attn, self.dq, hidden, normed, self.w_o, self.w_q = ins
        self.block_out, self.d_part, self.h_u = outs
        self.attn_home, self.dq_home, self.buf_o, self.buf_q, stage, self.h_buf, *sems = scratch
        self.w_sem, self.load_sem, own_sem, quad_s, quad_r = sems
        _, _, _, core = place(me)

        def piece(d):
            return normed.at[1 - core if d % TWO else core]

        def tokens(d):
            return self.h_u.at[:, :, pl.ds(d * CHUNK, CHUNK)]

        self.h_copies = [remote(piece(d), tokens(d), quad_s.at[TWO, d], quad_r.at[TWO, d], quad_of(me)[d]) for d in (1, TWO, THREE)]
        self.h_mine = pltpu.make_async_copy(piece(0), stage, own_sem.at[TWO])
        self.h_back = pltpu.make_async_copy(stage, tokens(0), self.load_sem.at[0])
        self.residual = pltpu.make_async_copy(hidden, self.block_out, own_sem.at[THREE])
        self.residual.start()
        for c in self.h_copies:
            c.start()
        self.h_mine.start()
        self.homes = [
            Home(me, src, out, own_sem.at[i], quad_s.at[i], quad_r.at[i])
            for i, (src, out) in enumerate([(attn, self.attn_home), (self.dq, self.dq_home)])
        ]
        for h in self.homes:
            h.start()

    @staticmethod
    def scratch(arrays):
        dma, d = pltpu.SemaphoreType.DMA, arrays[-1].shape[0]
        home = pltpu.VMEM((TWO,) * THREE + (CHUNK, d), BF16)
        buf = [pltpu.VMEM((TWO,) + b, BF16) for b in ((d, BLK), (BLK, d))]
        tiles = [pltpu.VMEM((TWO, TWO) + b, BF16) for b in ((CHUNK, d), (TWO, BLK, BLK))]
        sems = [dma((TWO, TWO)), dma((TWO,)), dma((FOUR,)), dma((THREE, FOUR)), dma((THREE, FOUR))]
        return [home] * TWO + buf + tiles + sems

    @staticmethod
    def results(arrays):
        unit = TWO, TWO, BLK, arrays[-1].shape[0]
        return [jax.ShapeDtypeStruct(arrays[TWO].shape, t) for t in (BF16, F32)] + [jax.ShapeDtypeStruct(unit, BF16)]

    spaces, out_spaces = [pl.ANY, pltpu.VMEM] + [pl.ANY] * FOUR, [pltpu.VMEM] * TWO + [pl.ANY]

    def step(self, t):
        def fetch_o(t, slot):
            return pltpu.make_async_copy(self.w_o.at[:, aligned(t)], self.buf_o.at[slot], self.w_sem.at[0, slot])

        def fetch_q(t, slot):
            return pltpu.make_async_copy(self.w_q.at[aligned(t)], self.buf_q.at[slot], self.w_sem.at[1, slot])

        def project(t, slot):
            at = aligned(t)
            attn = self.attn_home[...].reshape(-1, self.w_o.shape[0])
            out = jnp.dot(attn, self.buf_o[slot], preferred_element_type=F32)
            self.block_out[:, at] = (self.block_out[:, at].astype(F32) + out).astype(BF16)

        def pull(t, slot):
            dq = self.dq_home[...].reshape(-1, self.w_o.shape[0])
            self.d_part[:, aligned(t)] = dot_t(dq, self.buf_q[slot])

        if t in PRODUCTS_AT:
            i = PRODUCTS_AT.index(t)
            self.homes[i].wait_recv()
            if i == 0:
                self.residual.wait()
            tiled(self.w_o.shape[0] // BLK, *((fetch_o, project), (fetch_q, pull))[i])

    def wq_terms(self, own, other):
        self.h_mine.wait()
        self.h_back.start()
        for c in self.h_copies:
            c.wait_recv()
        self.h_back.wait()
        core = lax.rem(lax.axis_index("cp"), TWO)
        d_out = self.dq[...].reshape(-1, self.dq.shape[-1])

        def fetch(t, slot):
            return pltpu.make_async_copy(self.h_u.at[:, :, :, aligned(t)], self.h_buf.at[slot], self.load_sem.at[slot])

        for out, half in ((other, 1 - core), (own, core)):

            def use(t, slot, out=out, half=half):
                h = self.h_buf[slot].reshape(-1, BLK)
                out[t - half * FOUR] = dot(h, d_out, (0,), (0,)).reshape(out.shape[1:])

            tiled(FOUR, fetch, use, half * FOUR)

    def finish(self):
        for c in self.h_copies + self.homes:
            c.wait_send()


class HiddenGradient:
    tiles = FOUR

    def __init__(self, me, dk, dv, ins, outs, scratch):
        self.part, self.w_k, self.w_v, self.x, self.dy, self.gain = ins
        self.dx, self.terms = outs
        self.dk_home, self.dv_home, self.rows, *sems = scratch
        pairs = (dk, self.dk_home), (dv, self.dv_home)
        self.homes = [Home(me, src, out, *[r.at[i] for r in sems]) for i, (src, out) in enumerate(pairs)]
        for h in self.homes:
            h.start()

    @staticmethod
    def scratch(x):
        dma = pltpu.SemaphoreType.DMA
        home = pltpu.VMEM((TWO,) * THREE + (CHUNK, TWO * HEAD_DIM), BF16)
        return [home, home, pltpu.VMEM((8, x.shape[1]), F32), dma((TWO,)), dma((TWO, FOUR)), dma((TWO, FOUR))]

    def tile(self, t):
        if t == 0:
            for h in self.homes:
                h.wait_recv()
            self.rows[...] = jnp.zeros_like(self.rows)
        size = TWO * CHUNK
        at = pl.ds(t * size, size)
        d = self.part[at]
        for home, w in ((self.dk_home, self.w_k), (self.dv_home, self.w_v)):
            d += dot_t(home[t // TWO, t % TWO].reshape(size, -1), w[...])
        d = d.astype(BF16).astype(F32)
        x = self.x[at].astype(F32)
        inv_rms = lax.rsqrt(row_mean(x * x) + NORM_EPS)
        unit, scaled = x * inv_rms, d * self.gain[...]
        dx = inv_rms * (scaled - unit * row_mean(scaled * unit))
        self.dx[at] = (self.dy[at].astype(F32) + dx).astype(BF16)
        self.rows[...] += jnp.sum((d * unit).reshape((-1,) + self.rows.shape), axis=0)
        if t == self.tiles - 1:
            self.terms[...] = jnp.sum(self.rows[...], axis=0, keepdims=True)

    def finish(self):
        for h in self.homes:
            h.wait_send()


def reduce_pairs(arrays, blocks, cuts, kinds, collective_id, work, more):
    vmem, hbm = pl.BlockSpec(memory_space=pltpu.VMEM), pl.BlockSpec(memory_space=pl.ANY)
    n = len(blocks)
    scratch = [pltpu.VMEM((FOUR, TWO) + blocks[-1], F32)]
    scratch += sum((PairSum.scratch(k, b) for k, b in zip(kinds, blocks)), []) + PairSum.sems(n, max(cuts))
    outs = [jax.ShapeDtypeStruct(b, F32) for b in blocks] + work.results(more)
    return pl.pallas_call(
        functools.partial(reduce_kernel, cuts, kinds, work),
        name="reduce_pairs",
        out_shape=outs,
        in_specs=[hbm] * len(arrays) + [pl.BlockSpec(memory_space=m) for m in work.spaces],
        out_specs=[vmem] * n + [pl.BlockSpec(memory_space=m) for m in work.out_spaces],
        scratch_shapes=scratch + work.scratch(more),
        compiler_params=params(63, collective_id=collective_id),
        cost_estimate=cost(1, 20),
    )(*arrays, *more)


HERE = 0, 0, 0
LINKS = "xyud"
ORDERS = "zxy", "zyx", "yxz", "zyx"
CUTS = 0, 48, 96, 128
SIZES = 8.4, 8.4, 5.6, 2.8
GAIN_AT = [60.0 + 12.0 * i for i in range(5)]
LATENCY, TILES_FROM, TILE_EVERY = 3.0, 14.0, 8.0
SUM_AT = [25.0 + 6.0 * i for i in range(4)]


def onward(order, key):
    dz, ry, rx = key
    stage = max((order.index(a) for a, r in zip("zyx", key) if r), default=-1)
    for axis in order[stage + 1 :]:
        if axis == "x":
            yield "x", (dz, ry, 1)
        elif axis == "y":
            yield "y", (dz, 1, rx)
        else:
            yield "u", (-1, ry, rx)
            yield "d", (1, ry, rx)
    if stage >= 0 and order[stage] == "z" and abs(dz) < THREE:
        yield ("u", (dz - 1, ry, rx)) if dz < 0 else ("d", (dz + 1, ry, rx))


def arrivals():
    busy, times = {}, {}
    starts = [0.0] * THREE + [SUM_AT[-1] + LATENCY]
    here = [(t, z, part, HERE) for part, t in enumerate(starts) for z in range(FOUR)]
    while here:
        now, z, part, key = heapq.heappop(here)
        times.setdefault((part, key), []).append(now)
        for link, there in onward(ORDERS[part], key):
            to = z + {"u": 1, "d": -1}.get(link, 0)
            if 0 <= to <= THREE:
                busy[z, link] = max(busy.get((z, link), 0), now) + SIZES[part]
                heapq.heappush(here, (busy[z, link] + LATENCY, to, part, there))
    return sorted((sum(t) / len(t), *at) for at, t in times.items())


def turn_back(dkv_ref, cos_ref, sin_ref, dk_u, dv_u):
    n = TWO * TWO * BLK
    for i in range(TWO):
        for j in range(TWO):
            cos_t, sin_t = (jnp.hstack([t, t * sign]) for t, sign in ((cos_ref[i, j].T, 1), (sin_ref[i, j].T, -1)))
            dk = dkv_ref[pl.ds((i * TWO + j) * BLK, BLK)] * ATTN_SCALE
            dk_u[i, j] = (dk * cos_t + pltpu.roll(dk, HEAD_DIM // TWO, 1) * sin_t).astype(BF16)
    dv_u[...] = dkv_ref[pl.ds(n, n)].astype(BF16).reshape(dv_u.shape)


def wkv_terms(h_own, dk_u, dv_u, outs):
    d_out = jnp.hstack([r[...].reshape(-1, HEAD_DIM) for r in (dk_u, dv_u)])
    for out, half in outs:

        @pl.loop(0, FOUR)
        def _(zz, out=out, half=half):
            h = h_own[:, :, :, aligned(half * FOUR + zz)].reshape(-1, BLK)
            out[zz] = dot(h, d_out, (0,), (0,)).reshape(out.shape[1:])


def gather_kernel(*refs):
    take = taker(refs)
    wo_ref, wq_ref, dkv_ref, cos_ref, sin_ref, h_ref = take(6)
    grad_ins, outs, (dx_ref, dgain_ref) = take(6), take(FOUR), take(TWO)
    own_sem, send_sem, come_sem, core_sem, put_sem, all_terms, totals, g_s, g_r = take(9)
    terms, wkv_ref, h_own, dk_u, dv_u, store, wkv_store = take(7)
    buffers, sems, refs = take(FOUR), take(7), take(len(refs))
    me = lax.axis_index("cp")
    z, y, x, core = place(me)
    line = Line(me)
    to = {"x": dev(z, y, 1 - x, core), "y": dev(z, 1 - y, x, core), "u": line.next[1], "d": line.next[-1]}
    partner = dev(z, y, x, 1 - core)
    all_here = announce(quad_of(me)[1:] + [to["y"]] + [dev(zz, y, x, core) for _, zz in z_peers(z)])
    chip_here = me // TWO
    n_wo, wide = wo_ref.shape[0], wq_ref.shape[1]
    store[chip_here, pl.ds(0, n_wo)] = wo_ref[...]
    for i in range(TWO):
        store[chip_here, pl.ds(n_wo, n_wo), pl.ds(i * wide, wide)] = wq_ref[pl.ds(i * n_wo, n_wo)]
    turn_back(dkv_ref, cos_ref, sin_ref, dk_u, dv_u)
    all_here()
    load_h = pltpu.make_async_copy(h_ref, h_own, own_sem.at[0])
    load_h.start()
    wkv = PairSum(me, "core", 1, wkv_ref, wkv_store.at[chip_here], buffers, [r.at[0] for r in sems])

    def place_of(key):
        dz, ry, rx = key
        return z + dz, 1 - y if ry else y, 1 - x if rx else x

    def block(part, key):
        zz, yy, xx = place_of(key)
        chip = (TWO * zz + yy) * TWO + xx
        return wkv_store.at[chip] if part == THREE else store.at[chip, pl.ds(CUTS[part], CUTS[part + 1] - CUTS[part])]

    def windows(part, key):
        zz, yy, xx = place_of(key)
        pair, src = TWO * zz + yy, block(part, key)
        wo_at, wq_at = ((xx * TWO + core) * N_PAIRS + pair) * n_wo, (core * N_PAIRS + pair) * wq_ref.shape[0]
        if part == THREE:
            for i, out in enumerate(outs[TWO:]):
                yield src.at[:, head(i)], out.at[pl.ds(wq_at, wq_ref.shape[0]), pl.ds(xx * HEAD_DIM, HEAD_DIM)]
            return
        first, last = CUTS[part : part + TWO]
        if first < n_wo:
            rows = min(last, n_wo) - first
            yield src.at[pl.ds(0, rows)], outs[0].at[pl.ds(wo_at + first, rows)]
        if last > n_wo:
            skip = max(n_wo - first, 0)
            rows, at = last - first - skip, first + skip - n_wo
            for i in range(TWO):
                window = outs[1].at[pl.ds(wq_at + i * n_wo + at, rows), pl.ds(xx * wide, wide)]
                yield src.at[pl.ds(skip, rows), pl.ds(i * wide, wide)], window

    def index(part, key):
        return (part, key[0] + THREE) + key[1:]

    def send(part, key, link, there):
        sent = send_sem.at[index(part, key) + (LINKS.find(link or "-") + 1,)]
        if link:
            remote(block(part, key), block(part, key), sent, come_sem.at[index(part, there)], to[link]).start()
            return
        for src, window in windows(part, key):
            remote(src, window, sent, core_sem.at[index(part, key)], partner).start()
            pltpu.make_async_copy(src, window, put_sem.at[index(part, key)]).start()

    def whole(part, send, arrive):
        size = CUTS[part + 1] - CUTS[part] if part < THREE else wkv_store.size // store.shape[0] // outs[0].shape[1]
        dst = outs[0].at[pl.ds(0, size)]
        return remote(dst, dst, send, arrive, me)

    def when(on, do):
        pl.when(on)(do)

    def each_way(part, key):
        held = line.held(key[0])
        yield None, key, held
        for link, there in onward(ORDERS[part], key):
            inside = {"u": line.inside[1], "d": line.inside[-1]}.get(link)
            yield link, there, held if inside is None else jnp.logical_and(held, inside)

    def pass_on(part, key):
        for link, there, on in each_way(part, key):
            when(on, functools.partial(send, part, key, link, there))

    def term_copy(i):
        src = terms if i == 0 else totals.at[i - 1]
        return remote(src, all_terms.at[i], g_s.at[i], g_r.at[i], me ^ (1 << i))

    def add_terms(i):
        term_copy(i).wait_recv()
        totals[i] = (terms[...] if i == 0 else totals[i - 1]) + all_terms[i]
        if i + 1 < len(GAIN_AT):
            term_copy(i + 1).start()

    def tile(t):
        job.tile(t)
        if t == job.tiles - 1:
            term_copy(0).start()

    def sum_step(h):
        wkv.step(0, h)

    steps = [(TILES_FROM + t * TILE_EVERY, functools.partial(tile, t)) for t in range(HiddenGradient.tiles)]
    steps += [(at, functools.partial(sum_step, h)) for h, at in enumerate(SUM_AT)]
    steps += [(at, functools.partial(add_terms, i)) for i, at in enumerate(GAIN_AT)]
    steps.sort(key=lambda s: s[0])
    events = arrivals()
    for part in range(THREE):
        pass_on(part, HERE)
    job = HiddenGradient(me, dk_u, dv_u, grad_ins, (dx_ref, terms), refs)
    load_h.wait()
    wkv_terms(h_own, dk_u, dv_u, ((wkv_ref, 1 - core), (buffers[0], core)))
    wkv.begin(0)
    wkv.loaded(0)
    for now, part, key in events:
        while steps and steps[0][0] <= now:
            steps.pop(0)[1]()
        if any(key):
            arrive = come_sem.at[index(part, key)]
            when(line.held(key[0]), whole(part, own_sem.at[0], arrive).wait_recv)
            pass_on(part, key)
        elif part == THREE:
            pass_on(part, key)
    dgain_ref[...] = totals[len(GAIN_AT) - 1]
    for i in range(len(GAIN_AT)):
        term_copy(i).wait_send()
    for _, part, key in events:
        for sem in (core_sem, put_sem):
            when(line.held(key[0]), whole(part, own_sem.at[0], sem.at[index(part, key)]).wait_recv)
        for link, there, on in each_way(part, key):
            sent = send_sem.at[index(part, key) + (LINKS.find(link or "-") + 1,)]
            when(on, whole(part, sent, own_sem.at[0]).wait_send)
    wkv.wait_send(0)
    job.finish()


def gather_all(wo, wq, dkv, cos_f, sin_f, h_u, part, w_k, w_v, x, dy, gain, shapes):
    dma = pltpu.SemaphoreType.DMA
    vmem, hbm = pl.BlockSpec(memory_space=pltpu.VMEM), pl.BlockSpec(memory_space=pl.ANY)
    block = w_k.shape[0] // TWO // N_PAIRS, w_k.shape[1]
    parts = len(ORDERS)
    keys = (parts, 7, TWO, TWO)
    terms = 1, x.shape[1]
    scratch = [dma((1,)), dma(keys + (len(LINKS) + 1,)), dma(keys), dma(keys), dma(keys)]
    n = len(GAIN_AT)
    scratch += [pltpu.VMEM((n,) + terms, F32)] * TWO + [dma((n,)), dma((n,)), pltpu.VMEM(terms, F32)]
    scratch += [pltpu.VMEM((FOUR, TWO) + block, F32), pltpu.VMEM(h_u.shape, BF16)]
    scratch += [pltpu.VMEM((TWO, TWO, BLK, HEAD_DIM), BF16)] * TWO
    scratch += [pltpu.VMEM((TWO * N_PAIRS,) + b, F32) for b in ((TWO * wo.shape[0], wo.shape[1]), block)]
    return pl.pallas_call(
        gather_kernel,
        name="gather_all",
        out_shape=[jax.ShapeDtypeStruct(s, F32) for s in shapes]
        + [jax.ShapeDtypeStruct(x.shape, BF16), jax.ShapeDtypeStruct(terms, F32)],
        in_specs=[vmem] * 5 + [hbm] + [vmem] * 6,
        out_specs=[hbm] * len(shapes) + [vmem] * TWO,
        scratch_shapes=scratch + PairSum.scratch("core", block) + PairSum.sems(1, 1) + HiddenGradient.scratch(x),
        compiler_params=params(63, collective_id=0),
        cost_estimate=cost(1, 76),
    )(wo, wq, dkv, cos_f, sin_f, h_u, part, w_k, w_v, x, dy, gain)


def perm(x, pairs):
    return lax.ppermute(x, "cp", pairs)


def flip_pairs(d):
    return [(r, r ^ d) for r in range(32)]


def solution(mesh):
    def local_step(hidden, grad_out, positions, seg_ids, w_q, w_k, w_v, w_o, norm_gain):
        n_batch, n_tok, d_model = hidden.shape
        n_rows = n_batch * n_tok
        wide = N_HEADS * HEAD_DIM
        me = lax.axis_index("cp")
        z, y, x, core = place(me)
        quad, pair = me % FOUR, me // FOUR
        relations = range(FOUR)

        def swap(pieces):
            return [perm(p, flip_pairs(d)) if d else p for d, p in enumerate(pieces)]

        gain = norm_gain.astype(F32)
        cos_t, sin_t = rope_tables(positions.reshape(n_rows))
        cos_f, sin_f = jnp.hstack([cos_t, cos_t]), jnp.hstack([-sin_t, sin_t])
        dy_flat = grad_out.reshape(n_rows, d_model)
        normed, kv_home = project(hidden.reshape(n_rows, d_model), gain[NEW], w_k, w_v, cos_f, sin_f)
        pos = jnp.pad(positions.reshape(TWO, TWO, n_tok), ((0, 0), (0, 6), (0, 0)))
        kv_home = kv_home.reshape((TWO,) * 5 + (CHUNK, HEAD_DIM))
        kv_all, q_u, do_u, pos_u, *dy_rows = exchange(kv_home, normed, dy_flat, pos, cos_f, sin_f, w_q, w_o)
        pos_u = pos_u[:, :TWO].reshape((FOUR, TWO, TWO, CHUNK)).transpose(1, TWO, 0, THREE).reshape(TWO, TWO, BLK)
        dy_rows = [a.reshape(TWO, TWO, CHUNK, d_model) for a in dy_rows]
        dy_pieces = swap([dy_rows[d % TWO] for d in relations])

        member = quad ^ jnp.arange(FOUR)
        front, back = ((m[:, NEW] * CHUNK + jnp.arange(CHUNK)[NEW]).reshape(BLK) for m in (member, THREE - member))
        offsets = jnp.stack([front, back]).astype(jnp.int32)
        own_super = jnp.stack([pair, N_SUPER - 1 - pair]).astype(jnp.int32)
        q_index = own_super[:, NEW] * BLK + offsets
        start = q_index[NEW] - pos_u
        tab = jnp.concatenate(
            [own_super, (jnp.min(start, axis=-1) // BLK).reshape(-1), jnp.max(start, axis=-1).reshape(-1)]
        )
        start_r = start[:, :, NEW, :]
        q_index_r = jnp.broadcast_to(q_index[NEW, :, NEW, :], start_r.shape)
        cos_u, sin_u = rope_tables(pos_u)
        cos_ut, sin_ut = jnp.swapaxes(cos_u, TWO, THREE), jnp.swapaxes(sin_u, TWO, THREE)

        koff = offsets[:, NEW]
        attn_u, lse = flash_fwd(tab, q_u, kv_all, start_r, q_index_r, koff)

        wo_keep, wo_away = wo_terms(attn_u, dy_pieces)
        wo_come = perm(wo_away, flip_pairs(FOUR))
        do_u, wo_keep = lax.optimization_barrier((do_u, wo_keep))
        dq_u, dkv = flash_bwd(tab, q_u, do_u, attn_u, kv_all, lse, start_r, q_index_r, koff, cos_ut, sin_ut)

        x_flat = hidden.reshape(n_rows, d_model)
        wo_own, dkv_own, wq_own, block_out, d_part, h_u = reduce_pairs(
            [wo_keep, wo_come, dkv.reshape(FOUR, TWO, -1, HEAD_DIM)],
            [wo_keep.shape[1:], (dkv.size // N_PAIRS // HEAD_DIM, HEAD_DIM), (d_model // TWO // N_PAIRS, wide)],
            (TWO, 8, 8),
            ("z", "", "core"),
            TWO,
            Products,
            (attn_u, dq_u, x_flat, normed.reshape((TWO,) * THREE + (CHUNK, d_model)), w_o, w_q),
        )
        grad_wo, grad_wq, grad_wk, grad_wv, grad_x, d_gain = gather_all(
            wo_own,
            wq_own,
            dkv_own,
            cos_ut,
            sin_ut,
            h_u,
            d_part,
            w_k,
            w_v,
            x_flat,
            dy_flat,
            gain[NEW],
            [w_o.shape, w_q.shape, w_k.shape, w_v.shape],
        )
        block_out, grad_x = (a.reshape(hidden.shape) for a in (block_out, grad_x))
        return block_out, grad_x, grad_wq, grad_wk, grad_wv, grad_wo, d_gain.reshape(d_model)

    seq_spec = P(None, "cp", None)
    tok_spec = P(None, "cp")
    full_spec = P()
    return jax.shard_map(
        local_step,
        mesh=mesh,
        in_specs=(seq_spec, seq_spec, tok_spec, tok_spec, full_spec, full_spec, full_spec, full_spec, full_spec),
        out_specs=(seq_spec, seq_spec, full_spec, full_spec, full_spec, full_spec, full_spec),
        check_vma=False,
    )
```

```python
import functools
import heapq
import itertools

import jax
import jax.numpy as jnp
from jax import lax
from jax.experimental import pallas as pl
from jax.experimental.pallas import tpu as pltpu
from jax.sharding import PartitionSpec as P

HEAD_DIM = 128
NORM_EPS = 1e-5
ROPE_BASE = 500000.0
NEG_BIG = -1e30
LOG2E = 1.4426950408889634
ATTN_SCALE = HEAD_DIM**-0.5
EXP2_SCALE = ATTN_SCALE * LOG2E
CHUNK = 64
TWO = 2
THREE = 3
FOUR = 4
NEW = jnp.newaxis
BLK = 4 * CHUNK
N_HEADS = 8
N_PAIRS = 8
N_SUPER = 2 * N_PAIRS
MESH = pl.DeviceIdType.MESH
ONE = pl.Squeezed()
GROUP = 4
DIRECT = 2
MADE_AT = 5
PRODUCTS_AT = 7, 9
F32 = jnp.float32
BF16 = jnp.bfloat16

T_SQ, T_LO, T_MX = 0, 2, 6


def rope_tables(positions):
    inv_freq = ROPE_BASE ** (-jnp.arange(0, HEAD_DIM, TWO).astype(F32) / HEAD_DIM)
    angles = positions.astype(F32)[..., None] * inv_freq
    return jnp.cos(angles), jnp.sin(angles)


def dot(a, b, ca, cb):
    return lax.dot_general(a, b, ((ca, cb), ((), ())), preferred_element_type=F32)


def cost(gflop, mib):
    return pl.CostEstimate(flops=gflop * 10**9, bytes_accessed=mib << 20, transcendentals=0)


def params(mib, **more):
    return pltpu.CompilerParams(vmem_limit_bytes=mib << 20, **more)


def row_mean(x):
    return jnp.mean(x, axis=-1, keepdims=True)


def head(h):
    return pl.ds(h * HEAD_DIM, HEAD_DIM)


def head_slice(h):
    return slice(h * HEAD_DIM, (h + 1) * HEAD_DIM)


def dot_t(a, b):
    return dot(a, b, (1,), (1,))


def steps(tab, body):
    b, hf = pl.program_id(0), pl.program_id(1)
    own, first, last_start = tab[T_SQ + hf], tab[T_LO + TWO * b + hf], tab[T_MX + TWO * b + hf]

    def place_of(s):
        late = s >= N_PAIRS
        return jnp.where(late, N_SUPER - 1 - s, s), late.astype(jnp.int32)

    full_from = jnp.minimum((last_start + BLK - 1) // BLK, own)
    full_from += lax.rem(own - full_from, TWO)
    count = full_from - first

    @pl.loop(0, count + 1)
    def _(t):
        s = jnp.where(t < count, first + t, own)
        body(s, place_of(s), True)

    @pl.loop(0, (own - full_from) // TWO)
    def _(t):
        for i in range(TWO):
            s = full_from + TWO * t + i
            body(s, place_of(s), False)


def down(row, n):
    return jnp.broadcast_to(row, (n, row.shape[-1])).T


def may_use(s, off, st_ref, qi_ref):
    return jnp.logical_and(off >= st_ref[...] - s * BLK, off <= qi_ref[...] - s * BLK)


def fwd_kernel(tab, q_ref, kv_ref, st_ref, qi_ref, ko_ref, o_ref, lse_ref, q_s, acc, m_s, l_s, k_t, bounds):
    m_s[...] = jnp.full_like(m_s, NEG_BIG)
    l_s[...] = jnp.zeros_like(l_s)
    acc[...] = jnp.zeros_like(acc)
    for i, ref in enumerate((st_ref, qi_ref)):
        bounds[i] = down(ref[...], HEAD_DIM)
    for h in range(N_HEADS):
        q_s[pl.ds(h * BLK, BLK)] = q_ref[:, head(h)]

    @pl.when(pl.program_id(1) == 0)
    def _():
        @pl.loop(0, N_PAIRS)
        def _(pair):
            for hk in range(TWO):
                k_t[pair, hk] = kv_ref[pair, 0, hk].T

    def body(s, at, masked):
        pair, hk = at
        v = kv_ref[pair, 1, hk]
        if masked:
            off = ko_ref[hk] + s * BLK
            mask = [
                jnp.logical_and(off[:, lanes] >= bounds[0], off[:, lanes] <= bounds[1])
                for lanes in (slice(HEAD_DIM), slice(HEAD_DIM, BLK))
            ]
            mask = [jnp.concatenate([m, m], axis=0) for m in mask]
        for g in range(N_HEADS // TWO):
            rows = pl.ds(g * TWO * BLK, TWO * BLK)
            sc = jnp.dot(q_s[rows], k_t[pair, hk], preferred_element_type=F32)
            sc = [sc[:, :HEAD_DIM], sc[:, HEAD_DIM:]]
            if masked:
                sc = [jnp.where(m, x, NEG_BIG) for m, x in zip(mask, sc)]
            m_old = m_s[rows]
            m_new = jnp.maximum(m_old, jnp.max(jnp.maximum(*sc), axis=1, keepdims=True))
            alpha = jnp.exp2((m_old - m_new) * EXP2_SCALE)
            p = [jnp.exp2((x - m_new) * EXP2_SCALE) for x in sc]
            m_s[rows] = m_new
            l_s[rows] = l_s[rows] * alpha + (p[0] + p[1])
            p = jnp.hstack([x.astype(BF16) for x in p])
            acc[rows] = acc[rows] * alpha + jnp.dot(p, v, preferred_element_type=F32)

    steps(tab, body)
    for h in range(N_HEADS):
        rows = pl.ds(h * BLK, BLK)
        total = jnp.sum(l_s[rows], axis=1, keepdims=True)
        o_ref[:, head(h)] = (acc[rows] / total).astype(BF16)
        lse_ref[h] = (m_s[rows] * EXP2_SCALE + jnp.log2(total)).T[:1]


def bwd_kernel(tab, q_ref, do_ref, o_ref, kv_ref, lse_ref, st_ref, qi_ref, ko_ref, cos_ref, sin_ref, dq_ref, dkv_ref, *scratch):
    dq_acc, delta, off_s, q_s, do_s, q_t, do_t, p_s, ds_s = scratch
    dq_acc[...] = jnp.zeros_like(dq_acc)
    for h in range(N_HEADS):
        q, do = q_ref[:, head(h)], do_ref[:, head(h)]
        delta[h] = jnp.sum((do.astype(F32) * o_ref[:, head(h)].astype(F32)).T, axis=0, keepdims=True)
        q_s[pl.ds(h * BLK, BLK)], do_s[pl.ds(h * BLK, BLK)] = q, do
        q_t[h], do_t[h] = q.T, do.T

    @pl.when(pl.program_id(1) == 0)
    def _():
        dkv_ref[...] = jnp.zeros_like(dkv_ref)
        for hk in range(TWO):
            off_s[hk] = down(ko_ref[hk], BLK)

    def body(s, at, masked):
        pair, hk = at
        k = kv_ref[pair, 0, hk]
        v = kv_ref[pair, 1, hk]
        k_t = k.T
        mask = may_use(s, off_s[hk], st_ref, qi_ref) if masked else None
        for first in range(0, N_HEADS, GROUP):
            rows = pl.ds(first * BLK, GROUP * BLK)
            for h in range(first, first + GROUP):
                cols = pl.ds(h * BLK, BLK)
                p = jnp.exp2(jnp.dot(k, q_t[h], preferred_element_type=F32) * EXP2_SCALE - lse_ref[h])
                if masked:
                    p = jnp.where(mask, p, 0.0)
                ds = p * (jnp.dot(v, do_t[h], preferred_element_type=F32) - delta[h])
                p_s[:, cols] = p.astype(BF16)
                ds_s[:, cols] = ds.astype(BF16)
            dkv_ref[pair, 0, hk] += jnp.dot(ds_s[:, rows], q_s[rows], preferred_element_type=F32)
            dkv_ref[pair, 1, hk] += jnp.dot(p_s[:, rows], do_s[rows], preferred_element_type=F32)
            dq_acc[:, rows] += jnp.dot(k_t, ds_s[:, rows], preferred_element_type=F32)

    steps(tab, body)
    cos_t, sin_t = cos_ref[...], sin_ref[...]
    half = HEAD_DIM // TWO
    for h in range(N_HEADS):
        cols = pl.ds(h * BLK, BLK)
        a, c = dq_acc[:half, cols] * ATTN_SCALE, dq_acc[half:, cols] * ATTN_SCALE
        lin = jnp.concatenate([a * cos_t + c * sin_t, c * cos_t - a * sin_t], axis=0)
        dq_ref[:, head(h)] = lin.T.astype(BF16)


def attn_specs():
    def at_tile(b, h, t):
        return (b, h) + (0,) * TWO

    def at_row(b, h, t):
        return (0, 0, b) + (0,) * THREE

    tile = pl.BlockSpec((ONE, ONE, BLK, N_HEADS * HEAD_DIM), at_tile)
    row = pl.BlockSpec((ONE, ONE, 1, BLK), at_tile)
    stat = pl.BlockSpec((ONE, ONE, N_HEADS, 1, BLK), lambda b, h, t: (b, h) + (0,) * THREE)
    rope = pl.BlockSpec((ONE, ONE, HEAD_DIM // TWO, BLK), at_tile)
    kv = pl.BlockSpec((N_PAIRS, TWO, ONE, TWO, BLK, HEAD_DIM), at_row)
    ko = pl.BlockSpec((TWO, 1, BLK), lambda b, h, t: (0,) * THREE)
    return tile, row, stat, kv, ko, rope


def flash_fwd(tab, q, kv, start, qidx, koff):
    tile, row, stat, kvs, ko, _ = attn_specs()
    return pl.pallas_call(
        fwd_kernel,
        name="attn_fwd",
        out_shape=(jax.ShapeDtypeStruct(q.shape, BF16), jax.ShapeDtypeStruct((TWO, TWO, N_HEADS, 1, BLK), F32)),
        grid_spec=pltpu.PrefetchScalarGridSpec(
            num_scalar_prefetch=1,
            grid=(TWO, TWO),
            in_specs=[tile, kvs, row, row, ko],
            out_specs=[tile, stat],
            scratch_shapes=[pltpu.VMEM((N_HEADS * BLK, HEAD_DIM), t) for t in (BF16, F32, F32, F32)]
            + [pltpu.VMEM((N_PAIRS, TWO, HEAD_DIM, BLK), BF16), pltpu.VMEM((TWO, BLK, HEAD_DIM), jnp.int32)],
        ),
        compiler_params=params(63),
        cost_estimate=cost(20, 16),
    )(tab, q, kv, start, qidx, koff)


def flash_bwd(tab, q, do, o, kv, lse, start, qidx, koff, cos_t, sin_t):
    tile, row, stat, kvs, ko, rope = attn_specs()
    return pl.pallas_call(
        bwd_kernel,
        name="attn_bwd",
        out_shape=(
            jax.ShapeDtypeStruct(q.shape, BF16),
            jax.ShapeDtypeStruct(kv.shape, F32),
        ),
        grid_spec=pltpu.PrefetchScalarGridSpec(
            num_scalar_prefetch=1,
            grid=(TWO, TWO),
            in_specs=[tile, tile, tile, kvs, stat, row, row, ko, rope, rope],
            out_specs=[tile, kvs],
            scratch_shapes=[pltpu.VMEM((HEAD_DIM, N_HEADS * BLK), F32), pltpu.VMEM((N_HEADS, 1, BLK), F32)]
            + [pltpu.VMEM((TWO, BLK, BLK), jnp.int32)]
            + [pltpu.VMEM((N_HEADS * BLK, HEAD_DIM), BF16)] * TWO
            + [pltpu.VMEM((N_HEADS, HEAD_DIM, BLK), BF16)] * TWO
            + [pltpu.VMEM((BLK, N_HEADS * BLK), BF16)] * TWO,
        ),
        compiler_params=params(63),
        cost_estimate=cost(50, 32),
    )(tab, q, do, o, kv, lse, start, qidx, koff, cos_t, sin_t)


def turn(x, cos_ref, sin_ref):
    return x * cos_ref[...] + pltpu.roll(x, HEAD_DIM // TWO, 1) * sin_ref[...]


def first_kernel(x_ref, g_ref, wk_ref, wv_ref, cos_ref, sin_ref, h_ref, kv_ref):
    x = x_ref[...].astype(F32)
    h = (x * lax.rsqrt(row_mean(x * x) + NORM_EPS) * g_ref[...]).astype(BF16)
    h_ref[...] = h
    k = jnp.dot(h, wk_ref[...], preferred_element_type=F32)
    v = jnp.dot(h, wv_ref[...], preferred_element_type=F32)
    for i in range(TWO):
        kv_ref[i, 0] = turn(k[:, head_slice(i)], cos_ref, sin_ref).astype(BF16)
        kv_ref[i, 1] = v[:, head_slice(i)].astype(BF16)


def project(x, gain, w_k, w_v, cos_f, sin_f):
    n = TWO * CHUNK
    tile = pl.BlockSpec((n, x.shape[1]), lambda i: (i, 0))
    rope = pl.BlockSpec((n, HEAD_DIM), lambda i: (i, 0))
    whole = [pl.BlockSpec(a.shape, lambda i: (0, 0)) for a in (gain, w_k, w_v)]
    return pl.pallas_call(
        first_kernel,
        name="norm_kv",
        grid=(x.shape[0] // n,),
        out_shape=(jax.ShapeDtypeStruct(x.shape, BF16), jax.ShapeDtypeStruct((TWO,) * THREE + (TWO * n, HEAD_DIM), BF16)),
        in_specs=[tile] + whole + [rope, rope],
        out_specs=[tile, pl.BlockSpec((TWO, ONE, TWO, n, HEAD_DIM), lambda i: (0, i // TWO, 0, i % TWO, 0))],
        compiler_params=params(63),
        cost_estimate=cost(TWO, 7),
    )(x, gain, w_k, w_v, cos_f, sin_f)


def place(me):
    return me // 8, lax.rem(me // FOUR, TWO), lax.rem(me // TWO, TWO), lax.rem(me, TWO)


def dev(z, y, x, core):
    return ((z * TWO + y) * TWO + x) * TWO + core


def z_peers(z):
    return [(k, lax.rem(z + k, FOUR)) for k in (1, TWO, THREE)]


def announce(peers):
    barrier = pltpu.get_barrier_semaphore()
    for d in peers:
        pl.semaphore_signal(barrier, device_id=(d,), device_id_type=MESH)
    return lambda: pl.semaphore_wait(barrier, len(peers))


def meet(peers):
    announce(peers)()


def remote(src, dst, send, arrive, to):
    return pltpu.make_async_remote_copy(
        src_ref=src, dst_ref=dst, send_sem=send, recv_sem=arrive, device_id=(to,), device_id_type=MESH
    )


class Line:
    order = (0, 1, -1, TWO, -TWO, THREE, -THREE)

    def __init__(self, me):
        self.z, y, x, core = place(me)
        self.next = {1: dev(self.z + 1, y, x, core), -1: dev(self.z - 1, y, x, core)}
        self.inside = {1: self.z < THREE, -1: self.z > 0}

    def held(self, dz):
        return jnp.logical_and(self.z + dz >= 0, self.z + dz <= THREE)

    def ways(self, dz):
        for d in self.next:
            if d * dz <= 0:
                yield d, self.inside[d] if dz == 0 else jnp.logical_and(self.inside[d], self.held(dz))


def tiled(n, fetch, use, first=0):
    fetch(first, 0).start()

    @pl.loop(0, n)
    def _(t):
        slot = lax.rem(t, TWO)
        fetch(first + t, slot).wait()

        @pl.when(t + 1 < n)
        def _():
            fetch(first + t + 1, 1 - slot).start()

        use(first + t, slot)


def aligned(t, size=BLK):
    return pl.ds(pl.multiple_of(t * size, size), size)


def exchange_kernel(*refs):
    take = taker(refs)
    kv_ref, h_ref, dy_ref, pos_ref, cos_ref, sin_ref, wq_ref, wo_ref, kv_all, q_u, do_u, pos_u, *dy_rows = take(14)
    own_sem, quad_s, quad_r, z_s, z_r, y_s, y_r, q_home, do_home, wq_buf, wo_buf, w_sem, dy_sem, h_own, dy_own = take(len(refs))
    me = lax.axis_index("cp")
    z, y, x, core = place(me)
    quad, line = quad_of(me), Line(me)
    across = dev(z, 1 - y, x, core)
    meet(quad[1:] + [across] + [dev(zz, y, x, core) for _, zz in z_peers(z)])

    def source(a, d):
        xx, cc = 1 - x if d // TWO else x, 1 - core if d % TWO else core
        return pos_ref.at[cc] if a == THREE else (kv_ref, q_home, do_home)[a].at[xx, cc]

    def target(a, d):
        if a == THREE:
            return pos_u.at[d]
        tok = pl.ds(d * CHUNK, CHUNK)
        return kv_all.at[me // FOUR, :, :, :, tok] if a == 0 else (q_u, do_u)[a - 1].at[:, :, tok]

    def quad_copy(a, d):
        return remote(source(a, d), target(a, d), quad_s.at[a, d], quad_r.at[a, d], quad[d])

    def own_copy(a):
        return pltpu.make_async_copy(source(a, 0), target(a, 0), own_sem.at[a])

    def z_copy(part, dz, d):
        block = kv_all.at[TWO * (z + dz) + y, part]
        return remote(block, block, z_s.at[part, (d + 1) // TWO, dz + THREE], z_r.at[part, dz - d + THREE], line.next[d])

    def y_copy(part, dz, yy=y):
        block = kv_all.at[TWO * (z + dz) + yy, part]
        return remote(block, block, y_s.at[part, dz + THREE], y_r.at[part, dz + THREE], across)

    parts = range(TWO)
    moves = [(part, dz) for dz in line.order for part in parts]

    def pass_on(count):
        for part, dz in [moves.pop(0) for _ in range(count)]:
            if dz:
                block = kv_all.at[TWO * (z + dz) + y, part]
                arrival = remote(block, block, own_sem.at[0], z_r.at[part, dz + THREE], me)
                pl.when(line.held(dz))(arrival.wait_recv)
            for d, on in line.ways(dz):
                pl.when(on)(z_copy(part, dz, d).start)
            pl.when(line.held(dz))(y_copy(part, dz).start)

    n = h_ref.shape[1] // BLK // TWO

    def fetch_q(t, slot):
        return pltpu.make_async_copy(wq_ref.at[:, aligned(t)], wq_buf.at[slot], w_sem.at[0, slot])

    def fetch_o(t, slot):
        return pltpu.make_async_copy(wo_ref.at[aligned(t)], wo_buf.at[slot], w_sem.at[1, slot])

    def put(home, t, val):
        home[t // n, :, :, :, :, aligned(lax.rem(t, n))] = val.astype(BF16).reshape(home.shape[1:-1] + (BLK,))

    def query(t, slot):
        q = jnp.dot(h_own[...], wq_buf[slot], preferred_element_type=F32)
        put(q_home, t, jnp.hstack([turn(q[:, head_slice(j)], cos_ref, sin_ref) for j in range(BLK // HEAD_DIM)]))

    def pull(t, slot):
        put(do_home, t, dot_t(dy_own[...], wo_buf[slot]))

    all_moves = list(moves)
    loads = [pltpu.make_async_copy(a, b, dy_sem.at[i]) for i, (a, b) in enumerate(((h_ref, h_own), (dy_ref, dy_own)))]
    half = dy_own.shape[0] // TWO

    def dy_copy(i):
        return pltpu.make_async_copy(dy_own.at[aligned(1 - core if i else core, half)], dy_rows[i], dy_sem.at[i])

    for a in (0, THREE):
        for d in (1, TWO, THREE):
            quad_copy(a, d).start()
        own_copy(a).start()
    for c in loads:
        c.start()
    for c in loads:
        c.wait()
    for i in range(TWO):
        dy_copy(i).start()
    for a, (fetch, use) in enumerate(((fetch_q, query), (fetch_o, pull)), 1):
        for near in range(TWO):
            tiled(n, fetch, use, n * (x if near else 1 - x))
            for d in range(TWO):
                if d or not near:
                    quad_copy(a, d if near else d + TWO).start()
            if near:
                own_copy(a).start()
            if len(moves) == len(all_moves):
                own_copy(0).wait()
                for d in (1, TWO, THREE):
                    quad_copy(0, d).wait_recv()
            pass_on(TWO)
    pass_on(len(moves))
    for part, dz in all_moves:
        for d, on in line.ways(dz):
            pl.when(on)(z_copy(part, dz, d).wait_send)
        pl.when(line.held(dz))(y_copy(part, dz, 1 - y).wait_recv)
        pl.when(line.held(dz))(y_copy(part, dz).wait_send)
    for a in range(FOUR):
        for d in (1, TWO, THREE):
            quad_copy(a, d).wait_send()
            if a > 0:
                quad_copy(a, d).wait_recv()
    for a in (1, TWO, THREE):
        own_copy(a).wait()
    for i in range(TWO):
        dy_copy(i).wait()


def exchange(kv, h, dy, pos, cos_f, sin_f, w_q, w_o):
    dma = pltpu.SemaphoreType.DMA
    vmem, hbm = pl.BlockSpec(memory_space=pltpu.VMEM), pl.BlockSpec(memory_space=pl.ANY)
    wide = w_q.shape[1] // TWO
    unit = jax.ShapeDtypeStruct((TWO, TWO, BLK, wide), BF16)
    pos_quad = jax.ShapeDtypeStruct((FOUR,) + pos.shape[1:], pos.dtype)
    dy_half = jax.ShapeDtypeStruct((dy.shape[0] // TWO, dy.shape[1]), BF16)
    home = pltpu.VMEM((TWO,) * FOUR + (CHUNK, wide), BF16)
    sems = [dma((FOUR,))] + [dma((FOUR, FOUR))] * TWO + [dma((TWO, TWO, 7))] + [dma((TWO, 7))] * THREE
    bufs = [pltpu.VMEM((TWO,) + b, BF16) for b in ((w_q.shape[0], BLK), (BLK, w_o.shape[1]))]
    return pl.pallas_call(
        exchange_kernel,
        name="exchange",
        out_shape=(jax.ShapeDtypeStruct((N_PAIRS,) + (TWO,) * THREE + (BLK, HEAD_DIM), BF16), unit, unit, pos_quad, dy_half, dy_half),
        in_specs=[vmem] + [hbm] * TWO + [vmem] * THREE + [hbm] * TWO,
        out_specs=[hbm] * 6,
        scratch_shapes=sems + [home, home] + bufs + [dma((TWO, TWO)), dma((TWO,))] + [pltpu.VMEM(h.shape, BF16)] * TWO,
        compiler_params=params(63, collective_id=1),
        cost_estimate=cost(1, 20),
    )(kv, h, dy, pos, cos_f, sin_f, w_q, w_o)


def taker(refs):
    rest = iter(refs)
    return lambda count: list(itertools.islice(rest, count))


def wo_kernel(*refs):
    take = taker(refs)
    o_ref, *pieces = take(5)
    keep_ref, away_ref, dy_u, o_t, terms, came, load_sem, core_s, core_r, keep, away, out_sem = take(len(refs))
    me = lax.axis_index("cp")
    _, y, _, core = place(me)
    all_here = announce(quad_of(me)[1:TWO])
    loads = [
        pltpu.make_async_copy(src, dy_u.at[:, :, pl.ds(d * CHUNK, CHUNK)], load_sem.at[d])
        for d, src in enumerate(pieces)
    ]
    for c in loads:
        c.start()
    for h in range(N_HEADS):
        o_t[head(h)] = o_ref[:, :, :, head(h)].reshape(-1, HEAD_DIM).T
    for c in loads:
        c.wait()
    all_here()
    half, tiles = terms.shape[1], terms.shape[TWO] // BLK

    def swap(t):
        return remote(terms.at[0, :, aligned(t)], came.at[:, aligned(t)], core_s.at[t], core_r.at[t], quad_of(me)[1])

    def half_terms(i, to, then):
        @pl.loop(0, tiles)
        def _(t):
            dy = dy_u[:, :, :, aligned(t)].reshape(-1, BLK)
            terms[to, :, aligned(t)] = jnp.dot(o_t[aligned(i, half)], dy, preferred_element_type=F32)
            then(t)

    half_terms(1 - core, 0, lambda t: swap(t).start())
    half_terms(core, 1, lambda t: swap(t).wait_recv())
    rows = keep.shape[1]

    def results(zz):
        pairs = (keep, keep_ref), (away, away_ref)
        return [pltpu.make_async_copy(a.at[zz], b.at[zz], out_sem.at[i, zz]) for i, (a, b) in enumerate(pairs)]

    for zz in range(FOUR):
        for out, yy in ((keep, y), (away, 1 - y)):
            at = aligned(TWO * zz + yy, rows)
            out[zz] = terms[1, at] + came[at]
        for c in results(zz):
            c.start()
    for zz in range(FOUR):
        for c in results(zz):
            c.wait()
    for t in range(tiles):
        swap(t).wait_send()


def wo_terms(o, pieces):
    dma = pltpu.SemaphoreType.DMA
    vmem, hbm = pl.BlockSpec(memory_space=pltpu.VMEM), pl.BlockSpec(memory_space=pl.ANY)
    n, d, wide = o.shape[0] * o.shape[1] * o.shape[TWO], pieces[0].shape[-1], o.shape[-1]
    half = wide // TWO
    return pl.pallas_call(
        wo_kernel,
        name="wo_terms",
        out_shape=[jax.ShapeDtypeStruct((FOUR, half // N_PAIRS, d), F32)] * TWO,
        in_specs=[vmem] + [hbm] * FOUR,
        out_specs=[hbm] * TWO,
        scratch_shapes=[pltpu.VMEM((TWO, TWO, BLK, d), BF16), pltpu.VMEM((wide, n), BF16)]
        + [pltpu.VMEM((TWO, half, d), F32), pltpu.VMEM((half, d), F32), dma((FOUR,)), dma((d // BLK,)), dma((d // BLK,))]
        + [pltpu.VMEM((FOUR, half // N_PAIRS, d), F32)] * TWO
        + [dma((TWO, FOUR))],
        compiler_params=params(63, collective_id=THREE),
        cost_estimate=cost(FOUR, 20),
    )(o, *pieces)


class PairSum:
    def __init__(self, me, kind, cut, src, out, buffers, sems, direct=0):
        self.me, self.kind, self.src, self.out = me, kind, src, out
        self.direct_from = cut - direct
        self.size = out.shape[0] // cut
        self.own, self.from_core, self.from_y, self.from_z = buffers
        self.load_sem, self.core_s, self.core_r, self.y_s, self.y_r, self.z_s, self.z_r = sems
        self.z, self.y, x, core = place(me)
        self.partner = dev(self.z, self.y, x, 1 - core)
        self.line = [(k, zz, dev(zz, self.y, x, core)) for k, zz in z_peers(self.z)]
        self.across = dev(self.z, 1 - self.y, x, core)
        self.next_z = dev(self.z + 1, self.y, x, core), dev(self.z - 1, self.y, x, core)

    def rows(self, j):
        return pl.ds(j * self.size, self.size)

    def mine(self, j, zz):
        at = self.rows(j)
        return self.own.at[zz, self.y, at] if self.kind == "core" else self.own.at[zz, at]

    def loads(self, j):
        at = self.rows(j)
        if self.kind == "z":
            pairs = zip(self.src, (self.own, self.from_y))
            return [pltpu.make_async_copy(a.at[:, at], b.at[:, at], s.at[j]) for (a, b), s in zip(pairs, (self.load_sem, self.y_r))]
        return [pltpu.make_async_copy(self.src.at[:, self.y, at], self.own.at[:, at], self.load_sem.at[j])]

    def core_copy(self, j):
        src, dst = (r.at[:, :, self.rows(j)] for r in (self.src, self.from_core))
        return remote(src, dst, self.core_s.at[j], self.core_r.at[j], self.partner)

    def y_copy(self, j):
        src = self.own if self.kind == "core" else self.src
        at = self.rows(j)
        return remote(src.at[:, 1 - self.y, at], self.from_y.at[:, at], self.y_s.at[j], self.y_r.at[j], self.across)

    def z_copy(self, j, way, zz, to):
        at = way, zz + way - 1
        return remote(self.mine(j, zz), self.from_z.at[*at, self.rows(j)], self.z_s.at[j, *at], self.z_r.at[j, *at], to)

    def begin(self, j):
        if self.kind == "core":
            self.core_copy(j).start()
            return
        for c in self.loads(j):
            c.start()
        if not self.kind:
            self.y_copy(j).start()

    def loaded(self, j):
        if self.kind != "core":
            for c in self.loads(j):
                c.wait()
        else:
            self.core_copy(j).wait_recv()
            at = self.rows(j)
            for zz in range(FOUR):
                self.own[zz, :, at] += self.from_core[zz, :, at]
            self.y_copy(j).start()
        if self.kind == "z":
            self.add_y(j)
            self.hop(j, 0)

    def add_y(self, j):
        for zz in range(FOUR):
            self.mine(j, zz)[...] += self.from_y[zz, self.rows(j)]

    def relay(self, j, way, zz, add):
        if add:
            self.z_copy(j, way, zz, self.me).wait_recv()
            self.mine(j, zz)[...] += self.from_z[way, zz + way - 1, self.rows(j)]
        self.z_copy(j, way, zz, self.next_z[way]).start()

    def hop(self, j, h):
        @pl.when(self.z == h)
        def _():
            for zz in range(THREE, h, -1):
                self.relay(j, 0, zz, h > 0)

        @pl.when(self.z == THREE - h)
        def _():
            for zz in range(THREE - h):
                self.relay(j, 1, zz, h > 0)

    def z_direct(self, j):
        for k, zz, to in self.line:
            at, there = (j, 0, k - 1), self.from_z.at[0, k - 1, self.rows(j)]
            yield remote(self.mine(j, zz), there, self.z_s.at[at], self.z_r.at[at], to), there

    def step(self, j, h):
        if j >= self.direct_from and h > 0:
            if h == 1:
                at = self.rows(j)
                self.out[at] = self.mine(j, self.z)[...]
                for c, arrived in self.z_direct(j):
                    c.wait_recv()
                    self.out[at] += arrived[...]
            return
        if h == 0 and self.kind != "z":
            self.y_copy(j).wait_recv()
            self.add_y(j)
            if j < self.direct_from:
                self.hop(j, 0)
            else:
                for c, _ in self.z_direct(j):
                    c.start()
        elif 0 < h < THREE:
            self.hop(j, h)
        elif h == THREE:
            at = self.rows(j)
            self.out[at] = self.mine(j, self.z)[...]
            for way, on in enumerate((self.z > 0, self.z < THREE)):

                @pl.when(on)
                def _(way=way):
                    self.z_copy(j, way, self.z, self.me).wait_recv()
                    self.out[at] += self.from_z[way, self.z + way - 1, at]

    def wait_send(self, j):
        if self.kind == "core":
            self.core_copy(j).wait_send()
        if self.kind != "z":
            self.y_copy(j).wait_send()
        if j >= self.direct_from:
            for c, _ in self.z_direct(j):
                c.wait_send()
            return
        for zz in range(FOUR):
            if zz > 0:
                pl.when(self.z < zz)(self.z_copy(j, 0, zz, self.next_z[0]).wait_send)
            if zz < THREE:
                pl.when(self.z > zz)(self.z_copy(j, 1, zz, self.next_z[1]).wait_send)

    @staticmethod
    def scratch(kind, block):
        unused = pltpu.VMEM((8, HEAD_DIM), F32)
        own = pltpu.VMEM(((FOUR, TWO) if kind == "core" else (FOUR,)) + block, F32)
        from_y = pltpu.VMEM((FOUR,) + block, F32)
        return [own, own if kind == "core" else unused, from_y, pltpu.VMEM((TWO, THREE) + block, F32)]

    @staticmethod
    def sems(*dims):
        dma = pltpu.SemaphoreType.DMA
        return [dma(dims)] * 5 + [dma(dims + (TWO, THREE))] * TWO


def reduce_kernel(cuts, kinds, work, *refs):
    n = len(cuts)

    take = taker(refs)
    ins = [take(TWO) if k == "z" else take(1)[0] for k in kinds[:-1]]
    more_in, outs, more_out, made = take(work.ins), take(n), take(work.outs), take(1)
    buffers, sems = [take(FOUR) for _ in kinds], take(7)
    me = lax.axis_index("cp")
    z, y, x, core = place(me)
    meet(quad_of(me)[1:] + [dev(z, 1 - y, x, core)] + [dev(zz, y, x, core) for _, zz in z_peers(z)])
    job = work(me, more_in, more_out, take(len(refs)))
    inputs = enumerate(zip(kinds, cuts, ins + made, outs, buffers))
    sums = [PairSum(me, *a, [r.at[i] for r in sems], DIRECT if i == n - 1 else 0) for i, a in inputs]
    pieces = [(s, j) for s, cut in zip(sums, cuts) for j in range(cut)]
    early, late = pieces[: -cuts[-1]], pieces[-cuts[-1] :]
    for s, j in early:
        s.begin(j)
    for s, j in early:
        s.loaded(j)
    for t in range(len(pieces) + THREE):
        if t == MADE_AT:
            job.wq_terms(sums[-1].own, made[0])
            for s, j in late:
                s.begin(j)
        if t == MADE_AT + 1:
            for s, j in late:
                s.loaded(j)
        for h in range(FOUR):
            if 0 <= t - h < len(pieces):
                s, j = pieces[t - h]
                s.step(j, h)
        job.step(t)
    for s, j in pieces:
        s.wait_send(j)
    job.finish()


def quad_of(me):
    z, y, x, core = place(me)
    return [dev(z, y, 1 - x if d // TWO else x, 1 - core if d % TWO else core) for d in range(FOUR)]


class Home:
    def __init__(self, me, src, out, own_sem, send, arrive):
        _, _, x, core = place(me)
        w = src.shape[-1]
        to = out.at[core, :, :, :, pl.ds(x * w, w)]

        def piece(d):
            return src.at[:, :, pl.ds(d * CHUNK, CHUNK)]

        self.own = pltpu.make_async_copy(piece(0), to, own_sem)
        self.copies = [remote(piece(d), to, send.at[d], arrive.at[d], quad_of(me)[d]) for d in (1, TWO, THREE)]

    def start(self):
        self.own.start()
        for c in self.copies:
            c.start()

    def wait_recv(self):
        self.own.wait()
        for c in self.copies:
            c.wait_recv()

    def wait_send(self):
        for c in self.copies:
            c.wait_send()


class Products:
    ins, outs = 6, THREE

    def __init__(self, me, ins, outs, scratch):
        attn, self.dq, hidden, normed, self.w_o, self.w_q = ins
        self.out_refs, self.h_u = outs[:TWO], outs[TWO]
        self.block_out, self.d_part, self.attn_home, self.dq_home, self.buf_o, self.buf_q, stage, self.h_buf, *sems = scratch
        self.w_sem, self.load_sem, own_sem, quad_s, quad_r = sems
        _, _, _, core = place(me)

        def piece(d):
            return normed.at[1 - core if d % TWO else core]

        def tokens(d):
            return self.h_u.at[:, :, pl.ds(d * CHUNK, CHUNK)]

        self.h_copies = [remote(piece(d), tokens(d), quad_s.at[TWO, d], quad_r.at[TWO, d], quad_of(me)[d]) for d in (1, TWO, THREE)]
        self.h_mine = pltpu.make_async_copy(piece(0), stage, own_sem.at[TWO])
        self.h_back = pltpu.make_async_copy(stage, tokens(0), self.load_sem.at[0])
        self.residual = pltpu.make_async_copy(hidden, self.block_out, own_sem.at[THREE])
        self.residual.start()
        for c in self.h_copies:
            c.start()
        self.h_mine.start()
        self.homes = [
            Home(me, src, out, own_sem.at[i], quad_s.at[i], quad_r.at[i])
            for i, (src, out) in enumerate([(attn, self.attn_home), (self.dq, self.dq_home)])
        ]
        for h in self.homes:
            h.start()

    @staticmethod
    def scratch(arrays):
        dma, d = pltpu.SemaphoreType.DMA, arrays[-1].shape[0]
        home = pltpu.VMEM((TWO,) * THREE + (CHUNK, d), BF16)
        buf = [pltpu.VMEM((TWO,) + b, BF16) for b in ((d, BLK), (BLK, d))]
        tiles = [pltpu.VMEM((TWO, TWO) + b, BF16) for b in ((CHUNK, d), (TWO, BLK, BLK))]
        sems = [dma((TWO, TWO)), dma((TWO,)), dma((FOUR,)), dma((THREE, FOUR)), dma((THREE, FOUR))]
        products = [pltpu.VMEM(arrays[TWO].shape, t) for t in (BF16, F32)]
        return products + [home] * TWO + buf + tiles + sems

    @staticmethod
    def results(arrays):
        unit = TWO, TWO, BLK, arrays[-1].shape[0]
        return [jax.ShapeDtypeStruct(arrays[TWO].shape, t) for t in (BF16, F32)] + [jax.ShapeDtypeStruct(unit, BF16)]

    spaces, out_spaces = [pl.ANY, pltpu.VMEM] + [pl.ANY] * FOUR, [pl.ANY] * THREE

    def step(self, t):
        def fetch_o(t, slot):
            return pltpu.make_async_copy(self.w_o.at[:, aligned(t)], self.buf_o.at[slot], self.w_sem.at[0, slot])

        def fetch_q(t, slot):
            return pltpu.make_async_copy(self.w_q.at[aligned(t)], self.buf_q.at[slot], self.w_sem.at[1, slot])

        def project(t, slot):
            at = aligned(t)
            attn = self.attn_home[...].reshape(-1, self.w_o.shape[0])
            out = jnp.dot(attn, self.buf_o[slot], preferred_element_type=F32)
            self.block_out[:, at] = (self.block_out[:, at].astype(F32) + out).astype(BF16)

        def pull(t, slot):
            dq = self.dq_home[...].reshape(-1, self.w_o.shape[0])
            self.d_part[:, aligned(t)] = dot_t(dq, self.buf_q[slot])

        if t in PRODUCTS_AT:
            i = PRODUCTS_AT.index(t)
            self.homes[i].wait_recv()
            if i == 0:
                self.residual.wait()
            tiled(self.w_o.shape[0] // BLK, *((fetch_o, project), (fetch_q, pull))[i])
            self.write(i).start()

    def write(self, i):
        src = (self.block_out, self.d_part)[i]
        return pltpu.make_async_copy(src, self.out_refs[i], self.w_sem.at[i, 0])

    def wq_terms(self, own, other):
        self.h_mine.wait()
        self.h_back.start()
        for c in self.h_copies:
            c.wait_recv()
        self.h_back.wait()
        core = lax.rem(lax.axis_index("cp"), TWO)
        d_out = self.dq[...].reshape(-1, self.dq.shape[-1])

        def fetch(t, slot):
            return pltpu.make_async_copy(self.h_u.at[:, :, :, aligned(t)], self.h_buf.at[slot], self.load_sem.at[slot])

        for out, half in ((other, 1 - core), (own, core)):

            def use(t, slot, out=out, half=half):
                h = self.h_buf[slot].reshape(-1, BLK)
                out[t - half * FOUR] = dot(h, d_out, (0,), (0,)).reshape(out.shape[1:])

            tiled(FOUR, fetch, use, half * FOUR)

    def finish(self):
        for c in self.h_copies + self.homes:
            c.wait_send()
        for i in range(TWO):
            self.write(i).wait()


class HiddenGradient:
    tiles = FOUR

    def __init__(self, me, dk, dv, ins, outs, scratch):
        self.part, w_k, w_v, self.x, self.dy, self.gain = ins
        self.dx, self.terms = outs
        self.dk_home, self.dv_home, self.rows, self.w_k, self.w_v, *rest = scratch
        self.part_tile, self.x_tile, self.dy_tile, self.dx_tile, self.tile_sem, *sems = rest
        pairs = (w_k, self.w_k), (w_v, self.w_v)
        self.weights = [pltpu.make_async_copy(src, dst, self.tile_sem.at[i]) for i, (src, dst) in enumerate(pairs)]
        for c in self.weights:
            c.start()
        pairs = (dk, self.dk_home), (dv, self.dv_home)
        self.homes = [Home(me, src, out, *[r.at[i] for r in sems]) for i, (src, out) in enumerate(pairs)]
        for h in self.homes:
            h.start()

    @staticmethod
    def scratch(x):
        dma = pltpu.SemaphoreType.DMA
        home = pltpu.VMEM((TWO,) * THREE + (CHUNK, TWO * HEAD_DIM), BF16)
        tile = TWO * CHUNK, x.shape[1]
        weight = pltpu.VMEM((x.shape[1], TWO * HEAD_DIM), BF16)
        tiles = [pltpu.VMEM(tile, F32)] + [pltpu.VMEM(tile, BF16)] * THREE
        sems = [dma((FOUR,)), dma((TWO,)), dma((TWO, FOUR)), dma((TWO, FOUR))]
        return [home, home, pltpu.VMEM((8, x.shape[1]), F32), weight, weight] + tiles + sems

    def tile(self, t):
        if t == 0:
            for c in self.weights:
                c.wait()
            for h in self.homes:
                h.wait_recv()
            self.rows[...] = jnp.zeros_like(self.rows)
        size = TWO * CHUNK
        at = pl.ds(t * size, size)
        pairs = (self.part, self.part_tile), (self.x, self.x_tile), (self.dy, self.dy_tile)
        loads = [pltpu.make_async_copy(src.at[at], dst, self.tile_sem.at[i]) for i, (src, dst) in enumerate(pairs)]
        for c in loads:
            c.start()
        for c in loads:
            c.wait()
        d = self.part_tile[...]
        for home, w in ((self.dk_home, self.w_k), (self.dv_home, self.w_v)):
            d += dot_t(home[t // TWO, t % TWO].reshape(size, -1), w[...])
        d = d.astype(BF16).astype(F32)
        x = self.x_tile[...].astype(F32)
        inv_rms = lax.rsqrt(row_mean(x * x) + NORM_EPS)
        unit, scaled = x * inv_rms, d * self.gain[...]
        dx = inv_rms * (scaled - unit * row_mean(scaled * unit))
        self.dx_tile[...] = (self.dy_tile[...].astype(F32) + dx).astype(BF16)
        store = pltpu.make_async_copy(self.dx_tile, self.dx.at[at], self.tile_sem.at[THREE])
        store.start()
        self.rows[...] += jnp.sum((d * unit).reshape((-1,) + self.rows.shape), axis=0)
        store.wait()
        if t == self.tiles - 1:
            self.terms[...] = jnp.sum(self.rows[...], axis=0, keepdims=True)

    def finish(self):
        for h in self.homes:
            h.wait_send()


def reduce_pairs(arrays, blocks, cuts, kinds, collective_id, work, more):
    vmem, hbm = pl.BlockSpec(memory_space=pltpu.VMEM), pl.BlockSpec(memory_space=pl.ANY)
    n = len(blocks)
    scratch = [pltpu.VMEM((FOUR, TWO) + blocks[-1], F32)]
    scratch += sum((PairSum.scratch(k, b) for k, b in zip(kinds, blocks)), []) + PairSum.sems(n, max(cuts))
    outs = [jax.ShapeDtypeStruct(b, F32) for b in blocks] + work.results(more)
    return pl.pallas_call(
        functools.partial(reduce_kernel, cuts, kinds, work),
        name="reduce_pairs",
        out_shape=outs,
        in_specs=[hbm] * len(arrays) + [pl.BlockSpec(memory_space=m) for m in work.spaces],
        out_specs=[vmem] * n + [pl.BlockSpec(memory_space=m) for m in work.out_spaces],
        scratch_shapes=scratch + work.scratch(more),
        compiler_params=params(63, collective_id=collective_id),
        cost_estimate=cost(1, 20),
    )(*arrays, *more)


HERE = 0, 0, 0
LINKS = "xyud"
ORDERS = "zxy", "zyx", "yxz", "zyx"
CUTS = 0, 48, 96, 128
SIZES = 8.4, 8.4, 5.6, 2.8
GAIN_AT = [60.0 + 12.0 * i for i in range(5)]
LATENCY, TILES_FROM, TILE_EVERY = 3.0, 14.0, 8.0
SUM_AT = [25.0 + 6.0 * i for i in range(4)]


def onward(order, key):
    dz, ry, rx = key
    stage = max((order.index(a) for a, r in zip("zyx", key) if r), default=-1)
    for axis in order[stage + 1 :]:
        if axis == "x":
            yield "x", (dz, ry, 1)
        elif axis == "y":
            yield "y", (dz, 1, rx)
        else:
            yield "u", (-1, ry, rx)
            yield "d", (1, ry, rx)
    if stage >= 0 and order[stage] == "z" and abs(dz) < THREE:
        yield ("u", (dz - 1, ry, rx)) if dz < 0 else ("d", (dz + 1, ry, rx))


def arrivals():
    busy, times = {}, {}
    starts = [0.0] * THREE + [SUM_AT[-1] + LATENCY]
    here = [(t, z, part, HERE) for part, t in enumerate(starts) for z in range(FOUR)]
    while here:
        now, z, part, key = heapq.heappop(here)
        times.setdefault((part, key), []).append(now)
        for link, there in onward(ORDERS[part], key):
            to = z + {"u": 1, "d": -1}.get(link, 0)
            if 0 <= to <= THREE:
                busy[z, link] = max(busy.get((z, link), 0), now) + SIZES[part]
                heapq.heappush(here, (busy[z, link] + LATENCY, to, part, there))
    return sorted((sum(t) / len(t), *at) for at, t in times.items())


def turn_back(dkv_ref, cos_ref, sin_ref, dk_u, dv_u):
    n = TWO * TWO * BLK
    for i in range(TWO):
        for j in range(TWO):
            cos_t, sin_t = (jnp.hstack([t, t * sign]) for t, sign in ((cos_ref[i, j].T, 1), (sin_ref[i, j].T, -1)))
            dk = dkv_ref[pl.ds((i * TWO + j) * BLK, BLK)] * ATTN_SCALE
            dk_u[i, j] = (dk * cos_t + pltpu.roll(dk, HEAD_DIM // TWO, 1) * sin_t).astype(BF16)
    dv_u[...] = dkv_ref[pl.ds(n, n)].astype(BF16).reshape(dv_u.shape)


def wkv_terms(h_ref, h_buf, sem, dk_u, dv_u, outs):
    d_out = jnp.hstack([r[...].reshape(-1, HEAD_DIM) for r in (dk_u, dv_u)])

    def fetch(t, slot):
        return pltpu.make_async_copy(h_ref.at[:, :, :, aligned(t)], h_buf.at[slot], sem.at[slot])

    for out, half in outs:

        def use(t, slot, out=out, half=half):
            h = h_buf[slot].reshape(-1, BLK)
            out[t - half * FOUR] = dot(h, d_out, (0,), (0,)).reshape(out.shape[1:])

        tiled(FOUR, fetch, use, half * FOUR)


def gather_kernel(*refs):
    take = taker(refs)
    wo_ref, wq_ref, dkv_ref, cos_ref, sin_ref, h_ref = take(6)
    grad_ins, outs, (dx_ref, dgain_ref) = take(6), take(FOUR), take(TWO)
    own_sem, send_sem, come_sem, core_sem, put_sem, all_terms, totals, g_s, g_r = take(9)
    terms, wkv_ref, h_buf, h_sem, dk_u, dv_u, store, wkv_store = take(8)
    buffers, sems, refs = take(FOUR), take(7), take(len(refs))
    me = lax.axis_index("cp")
    z, y, x, core = place(me)
    line = Line(me)
    to = {"x": dev(z, y, 1 - x, core), "y": dev(z, 1 - y, x, core), "u": line.next[1], "d": line.next[-1]}
    partner = dev(z, y, x, 1 - core)
    all_here = announce(quad_of(me)[1:] + [to["y"]] + [dev(zz, y, x, core) for _, zz in z_peers(z)])
    chip_here = me // TWO
    n_wo, wide = wo_ref.shape[0], wq_ref.shape[1]
    store[chip_here, pl.ds(0, n_wo)] = wo_ref[...]
    for i in range(TWO):
        store[chip_here, pl.ds(n_wo, n_wo), pl.ds(i * wide, wide)] = wq_ref[pl.ds(i * n_wo, n_wo)]
    turn_back(dkv_ref, cos_ref, sin_ref, dk_u, dv_u)
    all_here()
    wkv = PairSum(me, "core", 1, wkv_ref, wkv_store.at[chip_here], buffers, [r.at[0] for r in sems])

    def place_of(key):
        dz, ry, rx = key
        return z + dz, 1 - y if ry else y, 1 - x if rx else x

    def block(part, key):
        zz, yy, xx = place_of(key)
        chip = (TWO * zz + yy) * TWO + xx
        return wkv_store.at[chip] if part == THREE else store.at[chip, pl.ds(CUTS[part], CUTS[part + 1] - CUTS[part])]

    def windows(part, key):
        zz, yy, xx = place_of(key)
        pair, src = TWO * zz + yy, block(part, key)
        wo_at, wq_at = ((xx * TWO + core) * N_PAIRS + pair) * n_wo, (core * N_PAIRS + pair) * wq_ref.shape[0]
        if part == THREE:
            for i, out in enumerate(outs[TWO:]):
                yield src.at[:, head(i)], out.at[pl.ds(wq_at, wq_ref.shape[0]), pl.ds(xx * HEAD_DIM, HEAD_DIM)]
            return
        first, last = CUTS[part : part + TWO]
        if first < n_wo:
            rows = min(last, n_wo) - first
            yield src.at[pl.ds(0, rows)], outs[0].at[pl.ds(wo_at + first, rows)]
        if last > n_wo:
            skip = max(n_wo - first, 0)
            rows, at = last - first - skip, first + skip - n_wo
            for i in range(TWO):
                window = outs[1].at[pl.ds(wq_at + i * n_wo + at, rows), pl.ds(xx * wide, wide)]
                yield src.at[pl.ds(skip, rows), pl.ds(i * wide, wide)], window

    def index(part, key):
        return (part, key[0] + THREE) + key[1:]

    def send(part, key, link, there):
        sent = send_sem.at[index(part, key) + (LINKS.find(link or "-") + 1,)]
        if link:
            remote(block(part, key), block(part, key), sent, come_sem.at[index(part, there)], to[link]).start()
            return
        for src, window in windows(part, key):
            remote(src, window, sent, core_sem.at[index(part, key)], partner).start()
            pltpu.make_async_copy(src, window, put_sem.at[index(part, key)]).start()

    def whole(part, send, arrive):
        size = CUTS[part + 1] - CUTS[part] if part < THREE else wkv_store.size // store.shape[0] // outs[0].shape[1]
        dst = outs[0].at[pl.ds(0, size)]
        return remote(dst, dst, send, arrive, me)

    def when(on, do):
        pl.when(on)(do)

    def each_way(part, key):
        held = line.held(key[0])
        yield None, key, held
        for link, there in onward(ORDERS[part], key):
            inside = {"u": line.inside[1], "d": line.inside[-1]}.get(link)
            yield link, there, held if inside is None else jnp.logical_and(held, inside)

    def pass_on(part, key):
        for link, there, on in each_way(part, key):
            when(on, functools.partial(send, part, key, link, there))

    def term_copy(i):
        src = terms if i == 0 else totals.at[i - 1]
        return remote(src, all_terms.at[i], g_s.at[i], g_r.at[i], me ^ (1 << i))

    def add_terms(i):
        term_copy(i).wait_recv()
        totals[i] = (terms[...] if i == 0 else totals[i - 1]) + all_terms[i]
        if i + 1 < len(GAIN_AT):
            term_copy(i + 1).start()

    def tile(t):
        job.tile(t)
        if t == job.tiles - 1:
            term_copy(0).start()

    def sum_step(h):
        wkv.step(0, h)

    steps = [(TILES_FROM + t * TILE_EVERY, functools.partial(tile, t)) for t in range(HiddenGradient.tiles)]
    steps += [(at, functools.partial(sum_step, h)) for h, at in enumerate(SUM_AT)]
    steps += [(at, functools.partial(add_terms, i)) for i, at in enumerate(GAIN_AT)]
    steps.sort(key=lambda s: s[0])
    events = arrivals()
    for part in range(THREE):
        pass_on(part, HERE)
    job = HiddenGradient(me, dk_u, dv_u, grad_ins, (dx_ref, terms), refs)
    wkv_terms(h_ref, h_buf, h_sem, dk_u, dv_u, ((wkv_ref, 1 - core), (buffers[0], core)))
    wkv.begin(0)
    wkv.loaded(0)
    for now, part, key in events:
        while steps and steps[0][0] <= now:
            steps.pop(0)[1]()
        if any(key):
            arrive = come_sem.at[index(part, key)]
            when(line.held(key[0]), whole(part, own_sem.at[0], arrive).wait_recv)
            pass_on(part, key)
        elif part == THREE:
            pass_on(part, key)
    dgain_ref[...] = totals[len(GAIN_AT) - 1]
    for i in range(len(GAIN_AT)):
        term_copy(i).wait_send()
    for _, part, key in events:
        for sem in (core_sem, put_sem):
            when(line.held(key[0]), whole(part, own_sem.at[0], sem.at[index(part, key)]).wait_recv)
        for link, there, on in each_way(part, key):
            sent = send_sem.at[index(part, key) + (LINKS.find(link or "-") + 1,)]
            when(on, whole(part, sent, own_sem.at[0]).wait_send)
    wkv.wait_send(0)
    job.finish()


def gather_all(wo, wq, dkv, cos_f, sin_f, h_u, part, w_k, w_v, x, dy, gain, shapes):
    dma = pltpu.SemaphoreType.DMA
    vmem, hbm = pl.BlockSpec(memory_space=pltpu.VMEM), pl.BlockSpec(memory_space=pl.ANY)
    block = w_k.shape[0] // TWO // N_PAIRS, w_k.shape[1]
    parts = len(ORDERS)
    keys = (parts, 7, TWO, TWO)
    terms = 1, x.shape[1]
    scratch = [dma((1,)), dma(keys + (len(LINKS) + 1,)), dma(keys), dma(keys), dma(keys)]
    n = len(GAIN_AT)
    scratch += [pltpu.VMEM((n,) + terms, F32)] * TWO + [dma((n,)), dma((n,)), pltpu.VMEM(terms, F32)]
    scratch += [pltpu.VMEM((FOUR, TWO) + block, F32), pltpu.VMEM((TWO, TWO, TWO, BLK, BLK), BF16), dma((TWO,))]
    scratch += [pltpu.VMEM((TWO, TWO, BLK, HEAD_DIM), BF16)] * TWO
    scratch += [pltpu.VMEM((TWO * N_PAIRS,) + b, F32) for b in ((TWO * wo.shape[0], wo.shape[1]), block)]
    return pl.pallas_call(
        gather_kernel,
        name="gather_all",
        out_shape=[jax.ShapeDtypeStruct(s, F32) for s in shapes]
        + [jax.ShapeDtypeStruct(x.shape, BF16), jax.ShapeDtypeStruct(terms, F32)],
        in_specs=[vmem] * 5 + [hbm] * 6 + [vmem],
        out_specs=[hbm] * (len(shapes) + 1) + [vmem],
        scratch_shapes=scratch + PairSum.scratch("core", block) + PairSum.sems(1, 1) + HiddenGradient.scratch(x),
        compiler_params=params(63, collective_id=0),
        cost_estimate=cost(1, 76),
    )(wo, wq, dkv, cos_f, sin_f, h_u, part, w_k, w_v, x, dy, gain)


def perm(x, pairs):
    return lax.ppermute(x, "cp", pairs)


def flip_pairs(d):
    return [(r, r ^ d) for r in range(32)]


def solution(mesh):
    def local_step(hidden, grad_out, positions, seg_ids, w_q, w_k, w_v, w_o, norm_gain):
        n_batch, n_tok, d_model = hidden.shape
        n_rows = n_batch * n_tok
        wide = N_HEADS * HEAD_DIM
        me = lax.axis_index("cp")
        z, y, x, core = place(me)
        quad, pair = me % FOUR, me // FOUR
        relations = range(FOUR)

        def swap(pieces):
            return [perm(p, flip_pairs(d)) if d else p for d, p in enumerate(pieces)]

        gain = norm_gain.astype(F32)
        cos_t, sin_t = rope_tables(positions.reshape(n_rows))
        cos_f, sin_f = jnp.hstack([cos_t, cos_t]), jnp.hstack([-sin_t, sin_t])
        dy_flat = grad_out.reshape(n_rows, d_model)
        normed, kv_home = project(hidden.reshape(n_rows, d_model), gain[NEW], w_k, w_v, cos_f, sin_f)
        pos = jnp.pad(positions.reshape(TWO, TWO, n_tok), ((0, 0), (0, 6), (0, 0)))
        kv_home = kv_home.reshape((TWO,) * 5 + (CHUNK, HEAD_DIM))
        kv_all, q_u, do_u, pos_u, *dy_rows = exchange(kv_home, normed, dy_flat, pos, cos_f, sin_f, w_q, w_o)
        pos_u = pos_u[:, :TWO].reshape((FOUR, TWO, TWO, CHUNK)).transpose(1, TWO, 0, THREE).reshape(TWO, TWO, BLK)
        dy_rows = [a.reshape(TWO, TWO, CHUNK, d_model) for a in dy_rows]
        dy_pieces = swap([dy_rows[d % TWO] for d in relations])

        member = quad ^ jnp.arange(FOUR)
        front, back = ((m[:, NEW] * CHUNK + jnp.arange(CHUNK)[NEW]).reshape(BLK) for m in (member, THREE - member))
        offsets = jnp.stack([front, back]).astype(jnp.int32)
        own_super = jnp.stack([pair, N_SUPER - 1 - pair]).astype(jnp.int32)
        q_index = own_super[:, NEW] * BLK + offsets
        start = q_index[NEW] - pos_u
        tab = jnp.concatenate(
            [own_super, (jnp.min(start, axis=-1) // BLK).reshape(-1), jnp.max(start, axis=-1).reshape(-1)]
        )
        start_r = start[:, :, NEW, :]
        q_index_r = jnp.broadcast_to(q_index[NEW, :, NEW, :], start_r.shape)
        cos_u, sin_u = rope_tables(pos_u)
        cos_ut, sin_ut = jnp.swapaxes(cos_u, TWO, THREE), jnp.swapaxes(sin_u, TWO, THREE)

        koff = offsets[:, NEW]
        attn_u, lse = flash_fwd(tab, q_u, kv_all, start_r, q_index_r, koff)

        wo_keep, wo_away = wo_terms(attn_u, dy_pieces)
        wo_come = perm(wo_away, flip_pairs(FOUR))
        do_u, wo_keep = lax.optimization_barrier((do_u, wo_keep))
        dq_u, dkv = flash_bwd(tab, q_u, do_u, attn_u, kv_all, lse, start_r, q_index_r, koff, cos_ut, sin_ut)

        x_flat = hidden.reshape(n_rows, d_model)
        wo_own, dkv_own, wq_own, block_out, d_part, h_u = reduce_pairs(
            [wo_keep, wo_come, dkv.reshape(FOUR, TWO, -1, HEAD_DIM)],
            [wo_keep.shape[1:], (dkv.size // N_PAIRS // HEAD_DIM, HEAD_DIM), (d_model // TWO // N_PAIRS, wide)],
            (TWO, 8, 8),
            ("z", "", "core"),
            TWO,
            Products,
            (attn_u, dq_u, x_flat, normed.reshape((TWO,) * THREE + (CHUNK, d_model)), w_o, w_q),
        )
        grad_wo, grad_wq, grad_wk, grad_wv, grad_x, d_gain = gather_all(
            wo_own,
            wq_own,
            dkv_own,
            cos_ut,
            sin_ut,
            h_u,
            d_part,
            w_k,
            w_v,
            x_flat,
            dy_flat,
            gain[NEW],
            [w_o.shape, w_q.shape, w_k.shape, w_v.shape],
        )
        block_out, grad_x = (a.reshape(hidden.shape) for a in (block_out, grad_x))
        return block_out, grad_x, grad_wq, grad_wk, grad_wv, grad_wo, d_gain.reshape(d_model)

    seq_spec = P(None, "cp", None)
    tok_spec = P(None, "cp")
    full_spec = P()
    return jax.shard_map(
        local_step,
        mesh=mesh,
        in_specs=(seq_spec, seq_spec, tok_spec, tok_spec, full_spec, full_spec, full_spec, full_spec, full_spec),
        out_specs=(seq_spec, seq_spec, full_spec, full_spec, full_spec, full_spec, full_spec),
        check_vma=False,
    )
```

```python
import functools
import heapq
import itertools

import jax
import jax.numpy as jnp
from jax import lax
from jax.experimental import pallas as pl
from jax.experimental.pallas import tpu as pltpu
from jax.sharding import PartitionSpec as P

HEAD_DIM = 128
NORM_EPS = 1e-5
ROPE_BASE = 500000.0
NEG_BIG = -1e30
LOG2E = 1.4426950408889634
ATTN_SCALE = HEAD_DIM**-0.5
EXP2_SCALE = ATTN_SCALE * LOG2E
CHUNK = 64
TWO = 2
THREE = 3
FOUR = 4
NEW = jnp.newaxis
BLK = 4 * CHUNK
N_HEADS = 8
N_PAIRS = 8
N_SUPER = 2 * N_PAIRS
MESH = pl.DeviceIdType.MESH
ONE = pl.Squeezed()
GROUP = 4
DIRECT = 2
MADE_AT = 5
PRODUCTS_AT = 7, 9
F32 = jnp.float32
BF16 = jnp.bfloat16

T_SQ, T_LO, T_MX = 0, 2, 6


def rope_tables(positions):
    inv_freq = ROPE_BASE ** (-jnp.arange(0, HEAD_DIM, TWO).astype(F32) / HEAD_DIM)
    angles = positions.astype(F32)[..., None] * inv_freq
    return jnp.cos(angles), jnp.sin(angles)


def dot(a, b, ca, cb):
    return lax.dot_general(a, b, ((ca, cb), ((), ())), preferred_element_type=F32)


def cost(gflop, mib):
    return pl.CostEstimate(flops=gflop * 10**9, bytes_accessed=mib << 20, transcendentals=0)


def params(mib, **more):
    return pltpu.CompilerParams(vmem_limit_bytes=mib << 20, **more)


def row_mean(x):
    return jnp.mean(x, axis=-1, keepdims=True)


def head(h):
    return pl.ds(h * HEAD_DIM, HEAD_DIM)


def head_slice(h):
    return slice(h * HEAD_DIM, (h + 1) * HEAD_DIM)


def dot_t(a, b):
    return dot(a, b, (1,), (1,))


def steps(tab, body):
    b, hf = pl.program_id(0), pl.program_id(1)
    own, first, last_start = tab[T_SQ + hf], tab[T_LO + TWO * b + hf], tab[T_MX + TWO * b + hf]

    def place_of(s):
        late = s >= N_PAIRS
        return jnp.where(late, N_SUPER - 1 - s, s), late.astype(jnp.int32)

    full_from = jnp.minimum((last_start + BLK - 1) // BLK, own)
    full_from += lax.rem(own - full_from, TWO)
    count = full_from - first

    @pl.loop(0, count + 1)
    def _(t):
        s = jnp.where(t < count, first + t, own)
        body(s, place_of(s), True)

    @pl.loop(0, (own - full_from) // TWO)
    def _(t):
        for i in range(TWO):
            s = full_from + TWO * t + i
            body(s, place_of(s), False)


def down(row, n):
    return jnp.broadcast_to(row, (n, row.shape[-1])).T


def offsets_of(tab, qi_ref, hk):
    return qi_ref[hk] - tab[T_SQ + hk] * BLK


def may_use(s, off, start, index):
    return jnp.logical_and(off >= start - s * BLK, off <= index - s * BLK)


def fwd_kernel(tab, q_ref, kv_ref, st_ref, qi_ref, o_ref, lse_ref, q_s, acc, m_s, l_s, k_t, bounds):
    m_s[...] = jnp.full_like(m_s, NEG_BIG)
    l_s[...] = jnp.zeros_like(l_s)
    acc[...] = jnp.zeros_like(acc)
    for i, row in enumerate((st_ref[...], qi_ref[pl.program_id(1)])):
        bounds[i] = down(row, HEAD_DIM)
    for h in range(N_HEADS):
        q_s[pl.ds(h * BLK, BLK)] = q_ref[:, head(h)]

    @pl.when(pl.program_id(1) == 0)
    def _():
        @pl.loop(0, N_PAIRS)
        def _(pair):
            for hk in range(TWO):
                k_t[pair, hk] = kv_ref[pair, 0, hk].T

    def body(s, at, masked):
        pair, hk = at
        v = kv_ref[pair, 1, hk]
        if masked:
            off = offsets_of(tab, qi_ref, hk) + s * BLK
            mask = [
                jnp.logical_and(off[:, lanes] >= bounds[0], off[:, lanes] <= bounds[1])
                for lanes in (slice(HEAD_DIM), slice(HEAD_DIM, BLK))
            ]
            mask = [jnp.concatenate([m, m], axis=0) for m in mask]
        for g in range(N_HEADS // TWO):
            rows = pl.ds(g * TWO * BLK, TWO * BLK)
            sc = jnp.dot(q_s[rows], k_t[pair, hk], preferred_element_type=F32)
            sc = [sc[:, :HEAD_DIM], sc[:, HEAD_DIM:]]
            if masked:
                sc = [jnp.where(m, x, NEG_BIG) for m, x in zip(mask, sc)]
            m_old = m_s[rows]
            m_new = jnp.maximum(m_old, jnp.max(jnp.maximum(*sc), axis=1, keepdims=True))
            alpha = jnp.exp2((m_old - m_new) * EXP2_SCALE)
            p = [jnp.exp2((x - m_new) * EXP2_SCALE) for x in sc]
            m_s[rows] = m_new
            l_s[rows] = l_s[rows] * alpha + (p[0] + p[1])
            p = jnp.hstack([x.astype(BF16) for x in p])
            acc[rows] = acc[rows] * alpha + jnp.dot(p, v, preferred_element_type=F32)

    steps(tab, body)
    for h in range(N_HEADS):
        rows = pl.ds(h * BLK, BLK)
        total = jnp.sum(l_s[rows], axis=1, keepdims=True)
        o_ref[:, head(h)] = (acc[rows] / total).astype(BF16)
        lse_ref[h] = (m_s[rows] * EXP2_SCALE + jnp.log2(total)).T[:1]


def bwd_kernel(tab, q_ref, do_ref, o_ref, kv_ref, lse_ref, st_ref, qi_ref, cos_ref, sin_ref, dq_ref, dkv_ref, *scratch):
    dq_acc, delta, off_s, q_s, do_s, q_t, do_t, p_s, ds_s = scratch
    dq_acc[...] = jnp.zeros_like(dq_acc)
    for h in range(N_HEADS):
        q, do = q_ref[:, head(h)], do_ref[:, head(h)]
        delta[h] = jnp.sum((do.astype(F32) * o_ref[:, head(h)].astype(F32)).T, axis=0, keepdims=True)
        q_s[pl.ds(h * BLK, BLK)], do_s[pl.ds(h * BLK, BLK)] = q, do
        q_t[h], do_t[h] = q.T, do.T

    @pl.when(pl.program_id(1) == 0)
    def _():
        dkv_ref[...] = jnp.zeros_like(dkv_ref)
        for hk in range(TWO):
            off_s[hk] = down(offsets_of(tab, qi_ref, hk), BLK)

    def body(s, at, masked):
        pair, hk = at
        k = kv_ref[pair, 0, hk]
        v = kv_ref[pair, 1, hk]
        k_t = k.T
        mask = may_use(s, off_s[hk], st_ref[...], qi_ref[pl.program_id(1)]) if masked else None
        for first in range(0, N_HEADS, GROUP):
            rows = pl.ds(first * BLK, GROUP * BLK)
            for h in range(first, first + GROUP):
                cols = pl.ds(h * BLK, BLK)
                p = jnp.exp2(jnp.dot(k, q_t[h], preferred_element_type=F32) * EXP2_SCALE - lse_ref[h])
                if masked:
                    p = jnp.where(mask, p, 0.0)
                ds = p * (jnp.dot(v, do_t[h], preferred_element_type=F32) - delta[h])
                p_s[:, cols] = p.astype(BF16)
                ds_s[:, cols] = ds.astype(BF16)
            dkv_ref[pair, 0, hk] += jnp.dot(ds_s[:, rows], q_s[rows], preferred_element_type=F32)
            dkv_ref[pair, 1, hk] += jnp.dot(p_s[:, rows], do_s[rows], preferred_element_type=F32)
            dq_acc[:, rows] += jnp.dot(k_t, ds_s[:, rows], preferred_element_type=F32)

    steps(tab, body)
    cos_t, sin_t = cos_ref[...], sin_ref[...]
    half = HEAD_DIM // TWO
    for h in range(N_HEADS):
        cols = pl.ds(h * BLK, BLK)
        a, c = dq_acc[:half, cols] * ATTN_SCALE, dq_acc[half:, cols] * ATTN_SCALE
        lin = jnp.concatenate([a * cos_t + c * sin_t, c * cos_t - a * sin_t], axis=0)
        dq_ref[:, head(h)] = lin.T.astype(BF16)


def attn_specs():
    def at_tile(b, h, t):
        return (b, h) + (0,) * TWO

    def at_row(b, h, t):
        return (0, 0, b) + (0,) * THREE

    tile = pl.BlockSpec((ONE, ONE, BLK, N_HEADS * HEAD_DIM), at_tile)
    row = pl.BlockSpec((ONE, ONE, 1, BLK), at_tile)
    stat = pl.BlockSpec((ONE, ONE, N_HEADS, 1, BLK), lambda b, h, t: (b, h) + (0,) * THREE)
    rope = pl.BlockSpec((ONE, ONE, HEAD_DIM // TWO, BLK), at_tile)
    kv = pl.BlockSpec((N_PAIRS, TWO, ONE, TWO, BLK, HEAD_DIM), at_row)
    ko = pl.BlockSpec((TWO, 1, BLK), lambda b, h, t: (0,) * THREE)
    return tile, row, stat, kv, ko, rope


def flash_fwd(tab, q, kv, start, index):
    tile, row, stat, kvs, ko, _ = attn_specs()
    return pl.pallas_call(
        fwd_kernel,
        name="attn_fwd",
        out_shape=(jax.ShapeDtypeStruct(q.shape, BF16), jax.ShapeDtypeStruct((TWO, TWO, N_HEADS, 1, BLK), F32)),
        grid_spec=pltpu.PrefetchScalarGridSpec(
            num_scalar_prefetch=1,
            grid=(TWO, TWO),
            in_specs=[tile, kvs, row, ko],
            out_specs=[tile, stat],
            scratch_shapes=[pltpu.VMEM((N_HEADS * BLK, HEAD_DIM), t) for t in (BF16, F32, F32, F32)]
            + [pltpu.VMEM((N_PAIRS, TWO, HEAD_DIM, BLK), BF16), pltpu.VMEM((TWO, BLK, HEAD_DIM), jnp.int32)],
        ),
        compiler_params=params(63),
        cost_estimate=cost(20, 16),
    )(tab, q, kv, start, index)


def flash_bwd(tab, q, do, o, kv, lse, start, index, cos_t, sin_t):
    tile, row, stat, kvs, ko, rope = attn_specs()
    return pl.pallas_call(
        bwd_kernel,
        name="attn_bwd",
        out_shape=(
            jax.ShapeDtypeStruct(q.shape, BF16),
            jax.ShapeDtypeStruct(kv.shape, F32),
        ),
        grid_spec=pltpu.PrefetchScalarGridSpec(
            num_scalar_prefetch=1,
            grid=(TWO, TWO),
            in_specs=[tile, tile, tile, kvs, stat, row, ko, rope, rope],
            out_specs=[tile, kvs],
            scratch_shapes=[pltpu.VMEM((HEAD_DIM, N_HEADS * BLK), F32), pltpu.VMEM((N_HEADS, 1, BLK), F32)]
            + [pltpu.VMEM((TWO, BLK, BLK), jnp.int32)]
            + [pltpu.VMEM((N_HEADS * BLK, HEAD_DIM), BF16)] * TWO
            + [pltpu.VMEM((N_HEADS, HEAD_DIM, BLK), BF16)] * TWO
            + [pltpu.VMEM((BLK, N_HEADS * BLK), BF16)] * TWO,
        ),
        compiler_params=params(63),
        cost_estimate=cost(50, 32),
    )(tab, q, do, o, kv, lse, start, index, cos_t, sin_t)


def turn(x, cos_ref, sin_ref):
    return x * cos_ref[...] + pltpu.roll(x, HEAD_DIM // TWO, 1) * sin_ref[...]


def first_kernel(x_ref, g_ref, wk_ref, wv_ref, cos_ref, sin_ref, h_ref, kv_ref):
    x = x_ref[...].astype(F32)
    h = (x * lax.rsqrt(row_mean(x * x) + NORM_EPS) * g_ref[...]).astype(BF16)
    h_ref[...] = h
    k = jnp.dot(h, wk_ref[...], preferred_element_type=F32)
    v = jnp.dot(h, wv_ref[...], preferred_element_type=F32)
    n = kv_ref.shape[THREE]
    for i in range(TWO):
        for j, val in enumerate((turn(k[:, head_slice(i)], cos_ref, sin_ref), v[:, head_slice(i)])):
            for c in range(TWO):
                kv_ref[i, c, j] = val[c * n : (c + 1) * n].astype(BF16)


def project(x, gain, w_k, w_v, cos_f, sin_f):
    n = x.shape[0] // TWO
    return pl.pallas_call(
        first_kernel,
        name="norm_kv",
        out_shape=(jax.ShapeDtypeStruct(x.shape, BF16), jax.ShapeDtypeStruct((TWO,) * THREE + (n, HEAD_DIM), BF16)),
        compiler_params=params(63),
        cost_estimate=cost(TWO, 7),
    )(x, gain, w_k, w_v, cos_f, sin_f)


def place(me):
    return me // 8, lax.rem(me // FOUR, TWO), lax.rem(me // TWO, TWO), lax.rem(me, TWO)


def dev(z, y, x, core):
    return ((z * TWO + y) * TWO + x) * TWO + core


def z_peers(z):
    return [(k, lax.rem(z + k, FOUR)) for k in (1, TWO, THREE)]


def announce(peers):
    barrier = pltpu.get_barrier_semaphore()
    for d in peers:
        pl.semaphore_signal(barrier, device_id=(d,), device_id_type=MESH)
    return lambda: pl.semaphore_wait(barrier, len(peers))


def meet(peers):
    announce(peers)()


def remote(src, dst, send, arrive, to):
    return pltpu.make_async_remote_copy(
        src_ref=src, dst_ref=dst, send_sem=send, recv_sem=arrive, device_id=(to,), device_id_type=MESH
    )


class Line:
    order = (0, 1, -1, TWO, -TWO, THREE, -THREE)

    def __init__(self, me):
        self.z, y, x, core = place(me)
        self.next = {1: dev(self.z + 1, y, x, core), -1: dev(self.z - 1, y, x, core)}
        self.inside = {1: self.z < THREE, -1: self.z > 0}

    def held(self, dz):
        return jnp.logical_and(self.z + dz >= 0, self.z + dz <= THREE)

    def ways(self, dz):
        for d in self.next:
            if d * dz <= 0:
                yield d, self.inside[d] if dz == 0 else jnp.logical_and(self.inside[d], self.held(dz))


def tiled(n, fetch, use, first=0):
    fetch(first, 0).start()

    @pl.loop(0, n)
    def _(t):
        slot = lax.rem(t, TWO)
        fetch(first + t, slot).wait()

        @pl.when(t + 1 < n)
        def _():
            fetch(first + t + 1, 1 - slot).start()

        use(first + t, slot)


def aligned(t, size=BLK):
    return pl.ds(pl.multiple_of(t * size, size), size)


def exchange_kernel(*refs):
    take = taker(refs)
    kv_ref, h_ref, dy_ref, pos_ref, cos_ref, sin_ref, wq_ref, wo_ref, kv_all, q_u, do_u, pos_u, *dy_rows, dy_first = take(16)
    own_sem, quad_s, quad_r, z_s, z_r, y_s, y_r, q_home, do_home, wq_buf, wo_buf, w_sem, dy_sem, first_sem, h_own, dy_own, *rope = take(len(refs))
    me = lax.axis_index("cp")
    z, y, x, core = place(me)
    quad, line = quad_of(me), Line(me)
    across = dev(z, 1 - y, x, core)
    meet(quad[1:] + [across] + [dev(zz, y, x, core) for _, zz in z_peers(z)])

    def source(a, d):
        xx, cc = 1 - x if d // TWO else x, 1 - core if d % TWO else core
        return pos_ref.at[cc] if a == THREE else (kv_ref, q_home, do_home)[a].at[xx, cc]

    def target(a, d):
        if a == THREE:
            return pos_u.at[d]
        tok = pl.ds(d * CHUNK, CHUNK)
        return kv_all.at[me // FOUR, :, :, :, tok] if a == 0 else (q_u, do_u)[a - 1].at[:, :, tok]

    def quad_copy(a, d):
        return remote(source(a, d), target(a, d), quad_s.at[a, d], quad_r.at[a, d], quad[d])

    def own_copy(a):
        return pltpu.make_async_copy(source(a, 0), target(a, 0), own_sem.at[a])

    def z_copy(part, dz, d):
        block = kv_all.at[TWO * (z + dz) + y, part]
        return remote(block, block, z_s.at[part, (d + 1) // TWO, dz + THREE], z_r.at[part, dz - d + THREE], line.next[d])

    def y_copy(part, dz, yy=y):
        block = kv_all.at[TWO * (z + dz) + yy, part]
        return remote(block, block, y_s.at[part, dz + THREE], y_r.at[part, dz + THREE], across)

    parts = range(TWO)
    moves = [(part, dz) for dz in line.order for part in parts]

    def pass_on(count):
        for part, dz in [moves.pop(0) for _ in range(count)]:
            if dz:
                block = kv_all.at[TWO * (z + dz) + y, part]
                arrival = remote(block, block, own_sem.at[0], z_r.at[part, dz + THREE], me)
                pl.when(line.held(dz))(arrival.wait_recv)
            for d, on in line.ways(dz):
                pl.when(on)(z_copy(part, dz, d).start)
            pl.when(line.held(dz))(y_copy(part, dz).start)

    n = h_ref.shape[1] // BLK // TWO

    def fetch_q(t, slot):
        return pltpu.make_async_copy(wq_ref.at[:, aligned(t)], wq_buf.at[slot], w_sem.at[0, slot])

    def fetch_o(t, slot):
        return pltpu.make_async_copy(wo_ref.at[aligned(t)], wo_buf.at[slot], w_sem.at[1, slot])

    def put(home, t, val):
        home[t // n, :, :, :, :, aligned(lax.rem(t, n))] = val.astype(BF16).reshape(home.shape[1:-1] + (BLK,))

    def query(t, slot):
        q = jnp.dot(h_own[...], wq_buf[slot], preferred_element_type=F32)
        put(q_home, t, jnp.hstack([turn(q[:, head_slice(j)], *rope) for j in range(BLK // HEAD_DIM)]))

    def pull(t, slot):
        put(do_home, t, dot_t(dy_own[...], wo_buf[slot]))

    all_moves = list(moves)
    pairs = (h_ref, h_own), (dy_ref, dy_own), (cos_ref, rope[0]), (sin_ref, rope[1])
    loads = [pltpu.make_async_copy(a, b, dy_sem.at[i]) for i, (a, b) in enumerate(pairs)]
    half = dy_own.shape[0] // TWO

    def dy_copy(i):
        at, n = (1 - core if i else core) * half, half - CHUNK if i == TWO else half
        return pltpu.make_async_copy(dy_own.at[pl.ds(at + half - n, n)], dy_rows[i], dy_sem.at[i])

    def first_copy():
        return remote(dy_own.at[pl.ds((1 - core) * half, CHUNK)], dy_first, first_sem.at[0], first_sem.at[1], quad[THREE])

    for a in (0, THREE):
        for d in (1, TWO, THREE):
            quad_copy(a, d).start()
        own_copy(a).start()
    for c in loads:
        c.start()
    for c in loads:
        c.wait()
    for i in range(THREE):
        dy_copy(i).start()
    for a, (fetch, use) in enumerate(((fetch_q, query), (fetch_o, pull)), 1):
        for near in range(TWO):
            tiled(n, fetch, use, n * (x if near else 1 - x))
            for d in range(TWO):
                if d or not near:
                    quad_copy(a, d if near else d + TWO).start()
            if near:
                own_copy(a).start()
            if len(moves) == len(all_moves):
                own_copy(0).wait()
                for d in (1, TWO, THREE):
                    quad_copy(0, d).wait_recv()
            pass_on(TWO)
    first_copy().start()
    pass_on(len(moves))
    for part, dz in all_moves:
        for d, on in line.ways(dz):
            pl.when(on)(z_copy(part, dz, d).wait_send)
        pl.when(line.held(dz))(y_copy(part, dz, 1 - y).wait_recv)
        pl.when(line.held(dz))(y_copy(part, dz).wait_send)
    for a in range(FOUR):
        for d in (1, TWO, THREE):
            quad_copy(a, d).wait_send()
            if a > 0:
                quad_copy(a, d).wait_recv()
    for a in (1, TWO, THREE):
        own_copy(a).wait()
    for i in range(THREE):
        dy_copy(i).wait()
    first_copy().wait()


def exchange(kv, h, dy, pos, cos_f, sin_f, w_q, w_o):
    dma = pltpu.SemaphoreType.DMA
    vmem, hbm = pl.BlockSpec(memory_space=pltpu.VMEM), pl.BlockSpec(memory_space=pl.ANY)
    wide = w_q.shape[1] // TWO
    unit = jax.ShapeDtypeStruct((TWO, TWO, BLK, wide), BF16)
    pos_quad = jax.ShapeDtypeStruct((FOUR,) + pos.shape[1:], pos.dtype)
    half = dy.shape[0] // TWO
    dy_parts = [jax.ShapeDtypeStruct((n, dy.shape[1]), BF16) for n in (half, half, half - CHUNK, CHUNK)]
    home = pltpu.VMEM((TWO,) * FOUR + (CHUNK, wide), BF16)
    sems = [dma((FOUR,))] + [dma((FOUR, FOUR))] * TWO + [dma((TWO, TWO, 7))] + [dma((TWO, 7))] * THREE
    bufs = [pltpu.VMEM((TWO,) + b, BF16) for b in ((w_q.shape[0], BLK), (BLK, w_o.shape[1]))]
    return pl.pallas_call(
        exchange_kernel,
        name="exchange",
        out_shape=(jax.ShapeDtypeStruct((N_PAIRS,) + (TWO,) * THREE + (BLK, HEAD_DIM), BF16), unit, unit, pos_quad, *dy_parts),
        in_specs=[vmem] + [hbm] * 7,
        out_specs=[hbm] * 8,
        scratch_shapes=sems + [home, home] + bufs
        + [dma((TWO, TWO)), dma((FOUR,)), dma((TWO,))]
        + [pltpu.VMEM(h.shape, BF16)] * TWO
        + [pltpu.VMEM(cos_f.shape, F32)] * TWO,
        compiler_params=params(63, collective_id=1),
        cost_estimate=cost(1, 20),
    )(kv, h, dy, pos, cos_f, sin_f, w_q, w_o)


def taker(refs):
    rest = iter(refs)
    return lambda count: list(itertools.islice(rest, count))


def wo_kernel(*refs):
    take = taker(refs)
    o_ref, *pieces = take(6)
    keep_ref, away_ref, dy_u, o_t, terms, came, load_sem, core_s, core_r, keep, away, out_sem = take(len(refs))
    me = lax.axis_index("cp")
    _, y, _, core = place(me)
    all_here = announce(quad_of(me)[1:TWO])
    loads = []
    for d, src in enumerate(pieces):
        for i in range(src.shape[0]):
            row = i + (d == THREE)
            to = dy_u.at[row // TWO, row % TWO, pl.ds(min(d, THREE) * CHUNK, CHUNK)]
            loads.append(pltpu.make_async_copy(src.at[i], to, load_sem.at[len(loads)]))
    for c in loads:
        c.start()
    for h in range(N_HEADS):
        o_t[head(h)] = o_ref[:, :, :, head(h)].reshape(-1, HEAD_DIM).T
    for c in loads:
        c.wait()
    all_here()
    half, tiles = terms.shape[1], terms.shape[TWO] // BLK

    def swap(t):
        return remote(terms.at[0, :, aligned(t)], came.at[:, aligned(t)], core_s.at[t], core_r.at[t], quad_of(me)[1])

    def half_terms(i, to, then):
        @pl.loop(0, tiles)
        def _(t):
            dy = dy_u[:, :, :, aligned(t)].reshape(-1, BLK)
            terms[to, :, aligned(t)] = jnp.dot(o_t[aligned(i, half)], dy, preferred_element_type=F32)
            then(t)

    half_terms(1 - core, 0, lambda t: swap(t).start())
    half_terms(core, 1, lambda t: swap(t).wait_recv())
    rows = keep.shape[1]

    def results(zz):
        pairs = (keep, keep_ref), (away, away_ref)
        return [pltpu.make_async_copy(a.at[zz], b.at[zz], out_sem.at[i, zz]) for i, (a, b) in enumerate(pairs)]

    for zz in range(FOUR):
        for out, yy in ((keep, y), (away, 1 - y)):
            at = aligned(TWO * zz + yy, rows)
            out[zz] = terms[1, at] + came[at]
        for c in results(zz):
            c.start()
    for zz in range(FOUR):
        for c in results(zz):
            c.wait()
    for t in range(tiles):
        swap(t).wait_send()


def wo_terms(o, pieces):
    dma = pltpu.SemaphoreType.DMA
    vmem, hbm = pl.BlockSpec(memory_space=pltpu.VMEM), pl.BlockSpec(memory_space=pl.ANY)
    n, d, wide = o.shape[0] * o.shape[1] * o.shape[TWO], pieces[0].shape[-1], o.shape[-1]
    half = wide // TWO
    return pl.pallas_call(
        wo_kernel,
        name="wo_terms",
        out_shape=[jax.ShapeDtypeStruct((FOUR, half // N_PAIRS, d), F32)] * TWO,
        in_specs=[vmem] + [hbm] * len(pieces),
        out_specs=[hbm] * TWO,
        scratch_shapes=[pltpu.VMEM((TWO, TWO, BLK, d), BF16), pltpu.VMEM((wide, n), BF16)]
        + [pltpu.VMEM((TWO, half, d), F32), pltpu.VMEM((half, d), F32), dma((FOUR * FOUR,)), dma((d // BLK,)), dma((d // BLK,))]
        + [pltpu.VMEM((FOUR, half // N_PAIRS, d), F32)] * TWO
        + [dma((TWO, FOUR))],
        compiler_params=params(63, collective_id=THREE),
        cost_estimate=cost(FOUR, 20),
    )(o, *pieces)


class PairSum:
    def __init__(self, me, kind, cut, src, out, buffers, sems, direct=0):
        self.me, self.kind, self.src, self.out = me, kind, src, out
        self.direct_from = cut - direct
        self.size = out.shape[0] // cut
        self.own, self.from_core, self.from_y, self.from_z = buffers
        self.load_sem, self.core_s, self.core_r, self.y_s, self.y_r, self.z_s, self.z_r = sems
        self.z, self.y, x, core = place(me)
        self.partner = dev(self.z, self.y, x, 1 - core)
        self.line = [(k, zz, dev(zz, self.y, x, core)) for k, zz in z_peers(self.z)]
        self.across = dev(self.z, 1 - self.y, x, core)
        self.next_z = dev(self.z + 1, self.y, x, core), dev(self.z - 1, self.y, x, core)

    def rows(self, j):
        return pl.ds(j * self.size, self.size)

    def mine(self, j, zz):
        at = self.rows(j)
        return self.own.at[zz, self.y, at] if self.kind == "core" else self.own.at[zz, at]

    def loads(self, j):
        at = self.rows(j)
        if self.kind == "z":
            pairs = zip(self.src, (self.own, self.from_y))
            return [pltpu.make_async_copy(a.at[:, at], b.at[:, at], s.at[j]) for (a, b), s in zip(pairs, (self.load_sem, self.y_r))]
        return [pltpu.make_async_copy(self.src.at[:, self.y, at], self.own.at[:, at], self.load_sem.at[j])]

    def core_copy(self, j):
        src, dst = (r.at[:, :, self.rows(j)] for r in (self.src, self.from_core))
        return remote(src, dst, self.core_s.at[j], self.core_r.at[j], self.partner)

    def y_copy(self, j):
        src = self.own if self.kind == "core" else self.src
        at = self.rows(j)
        return remote(src.at[:, 1 - self.y, at], self.from_y.at[:, at], self.y_s.at[j], self.y_r.at[j], self.across)

    def z_copy(self, j, way, zz, to):
        at = way, zz + way - 1
        return remote(self.mine(j, zz), self.from_z.at[*at, self.rows(j)], self.z_s.at[j, *at], self.z_r.at[j, *at], to)

    def begin(self, j):
        if self.kind == "core":
            self.core_copy(j).start()
            return
        for c in self.loads(j):
            c.start()
        if not self.kind:
            self.y_copy(j).start()

    def loaded(self, j):
        if self.kind != "core":
            for c in self.loads(j):
                c.wait()
        else:
            self.core_copy(j).wait_recv()
            at = self.rows(j)
            for zz in range(FOUR):
                self.own[zz, :, at] += self.from_core[zz, :, at]
            self.y_copy(j).start()
        if self.kind == "z":
            self.add_y(j)
            self.hop(j, 0)

    def add_y(self, j):
        for zz in range(FOUR):
            self.mine(j, zz)[...] += self.from_y[zz, self.rows(j)]

    def relay(self, j, way, zz, add):
        if add:
            self.z_copy(j, way, zz, self.me).wait_recv()
            self.mine(j, zz)[...] += self.from_z[way, zz + way - 1, self.rows(j)]
        self.z_copy(j, way, zz, self.next_z[way]).start()

    def hop(self, j, h):
        @pl.when(self.z == h)
        def _():
            for zz in range(THREE, h, -1):
                self.relay(j, 0, zz, h > 0)

        @pl.when(self.z == THREE - h)
        def _():
            for zz in range(THREE - h):
                self.relay(j, 1, zz, h > 0)

    def z_direct(self, j):
        for k, zz, to in self.line:
            at, there = (j, 0, k - 1), self.from_z.at[0, k - 1, self.rows(j)]
            yield remote(self.mine(j, zz), there, self.z_s.at[at], self.z_r.at[at], to), there

    def step(self, j, h):
        if j >= self.direct_from and h > 0:
            if h == 1:
                at = self.rows(j)
                self.out[at] = self.mine(j, self.z)[...]
                for c, arrived in self.z_direct(j):
                    c.wait_recv()
                    self.out[at] += arrived[...]
            return
        if h == 0 and self.kind != "z":
            self.y_copy(j).wait_recv()
            self.add_y(j)
            if j < self.direct_from:
                self.hop(j, 0)
            else:
                for c, _ in self.z_direct(j):
                    c.start()
        elif 0 < h < THREE:
            self.hop(j, h)
        elif h == THREE:
            at = self.rows(j)
            self.out[at] = self.mine(j, self.z)[...]
            for way, on in enumerate((self.z > 0, self.z < THREE)):

                @pl.when(on)
                def _(way=way):
                    self.z_copy(j, way, self.z, self.me).wait_recv()
                    self.out[at] += self.from_z[way, self.z + way - 1, at]

    def wait_send(self, j):
        if self.kind == "core":
            self.core_copy(j).wait_send()
        if self.kind != "z":
            self.y_copy(j).wait_send()
        if j >= self.direct_from:
            for c, _ in self.z_direct(j):
                c.wait_send()
            return
        for zz in range(FOUR):
            if zz > 0:
                pl.when(self.z < zz)(self.z_copy(j, 0, zz, self.next_z[0]).wait_send)
            if zz < THREE:
                pl.when(self.z > zz)(self.z_copy(j, 1, zz, self.next_z[1]).wait_send)

    @staticmethod
    def scratch(kind, block):
        unused = pltpu.VMEM((8, HEAD_DIM), F32)
        own = pltpu.VMEM(((FOUR, TWO) if kind == "core" else (FOUR,)) + block, F32)
        from_y = pltpu.VMEM((FOUR,) + block, F32)
        return [own, own if kind == "core" else unused, from_y, pltpu.VMEM((TWO, THREE) + block, F32)]

    @staticmethod
    def sems(*dims):
        dma = pltpu.SemaphoreType.DMA
        return [dma(dims)] * 5 + [dma(dims + (TWO, THREE))] * TWO


def reduce_kernel(cuts, kinds, work, *refs):
    n = len(cuts)

    take = taker(refs)
    ins = [take(TWO) if k == "z" else take(1)[0] for k in kinds[:-1]]
    more_in, outs, more_out, made = take(work.ins), take(n), take(work.outs), take(1)
    buffers, sems = [take(FOUR) for _ in kinds], take(7)
    me = lax.axis_index("cp")
    z, y, x, core = place(me)
    meet(quad_of(me)[1:] + [dev(z, 1 - y, x, core)] + [dev(zz, y, x, core) for _, zz in z_peers(z)])
    job = work(me, more_in, more_out, take(len(refs)))
    inputs = enumerate(zip(kinds, cuts, ins + made, outs, buffers))
    sums = [PairSum(me, *a, [r.at[i] for r in sems], DIRECT if i == n - 1 else 0) for i, a in inputs]
    pieces = [(s, j) for s, cut in zip(sums, cuts) for j in range(cut)]
    early, late = pieces[: -cuts[-1]], pieces[-cuts[-1] :]
    for s, j in early:
        s.begin(j)
    for s, j in early:
        s.loaded(j)
    for t in range(len(pieces) + THREE):
        if t == MADE_AT:
            job.wq_terms(sums[-1].own, made[0])
            for s, j in late:
                s.begin(j)
        if t == MADE_AT + 1:
            for s, j in late:
                s.loaded(j)
        for h in range(FOUR):
            if 0 <= t - h < len(pieces):
                s, j = pieces[t - h]
                s.step(j, h)
        job.step(t)
    for s, j in pieces:
        s.wait_send(j)
    job.finish()


def quad_of(me):
    z, y, x, core = place(me)
    return [dev(z, y, 1 - x if d // TWO else x, 1 - core if d % TWO else core) for d in range(FOUR)]


class Home:
    def __init__(self, me, src, out, own_sem, send, arrive):
        _, _, x, core = place(me)
        w = src.shape[-1]
        to = out.at[core, :, :, :, pl.ds(x * w, w)]

        def piece(d):
            return src.at[:, :, pl.ds(d * CHUNK, CHUNK)]

        self.own = pltpu.make_async_copy(piece(0), to, own_sem)
        self.copies = [remote(piece(d), to, send.at[d], arrive.at[d], quad_of(me)[d]) for d in (1, TWO, THREE)]

    def start(self):
        self.own.start()
        for c in self.copies:
            c.start()

    def wait_recv(self):
        self.own.wait()
        for c in self.copies:
            c.wait_recv()

    def wait_send(self):
        for c in self.copies:
            c.wait_send()


class Products:
    ins, outs = 6, THREE

    def __init__(self, me, ins, outs, scratch):
        attn, self.dq, hidden, normed, self.w_o, self.w_q = ins
        self.out_refs, self.h_u = outs[:TWO], outs[TWO]
        self.block_out, self.d_part, self.attn_home, self.dq_home, self.buf_o, self.buf_q, stage, self.h_buf, *sems = scratch
        self.w_sem, self.load_sem, own_sem, quad_s, quad_r = sems
        _, _, _, core = place(me)

        def piece(d):
            return normed.at[1 - core if d % TWO else core]

        def tokens(d):
            return self.h_u.at[:, :, pl.ds(d * CHUNK, CHUNK)]

        self.h_copies = [remote(piece(d), tokens(d), quad_s.at[TWO, d], quad_r.at[TWO, d], quad_of(me)[d]) for d in (1, TWO, THREE)]
        self.h_mine = pltpu.make_async_copy(piece(0), stage, own_sem.at[TWO])
        self.h_back = pltpu.make_async_copy(stage, tokens(0), self.load_sem.at[0])
        self.residual = pltpu.make_async_copy(hidden, self.block_out, own_sem.at[THREE])
        self.residual.start()
        for c in self.h_copies:
            c.start()
        self.h_mine.start()
        self.homes = [
            Home(me, src, out, own_sem.at[i], quad_s.at[i], quad_r.at[i])
            for i, (src, out) in enumerate([(attn, self.attn_home), (self.dq, self.dq_home)])
        ]
        for h in self.homes:
            h.start()

    @staticmethod
    def scratch(arrays):
        dma, d = pltpu.SemaphoreType.DMA, arrays[-1].shape[0]
        home = pltpu.VMEM((TWO,) * THREE + (CHUNK, d), BF16)
        buf = [pltpu.VMEM((TWO,) + b, BF16) for b in ((d, BLK), (BLK, d))]
        tiles = [pltpu.VMEM((TWO, TWO) + b, BF16) for b in ((CHUNK, d), (TWO, BLK, BLK))]
        sems = [dma((TWO, TWO)), dma((TWO,)), dma((FOUR,)), dma((THREE, FOUR)), dma((THREE, FOUR))]
        products = [pltpu.VMEM(arrays[TWO].shape, t) for t in (BF16, F32)]
        return products + [home] * TWO + buf + tiles + sems

    @staticmethod
    def results(arrays):
        unit = TWO, TWO, BLK, arrays[-1].shape[0]
        return [jax.ShapeDtypeStruct(arrays[TWO].shape, t) for t in (BF16, F32)] + [jax.ShapeDtypeStruct(unit, BF16)]

    spaces, out_spaces = [pl.ANY, pltpu.VMEM] + [pl.ANY] * FOUR, [pl.ANY] * THREE

    def step(self, t):
        def fetch_o(t, slot):
            return pltpu.make_async_copy(self.w_o.at[:, aligned(t)], self.buf_o.at[slot], self.w_sem.at[0, slot])

        def fetch_q(t, slot):
            return pltpu.make_async_copy(self.w_q.at[aligned(t)], self.buf_q.at[slot], self.w_sem.at[1, slot])

        def project(t, slot):
            at = aligned(t)
            attn = self.attn_home[...].reshape(-1, self.w_o.shape[0])
            out = jnp.dot(attn, self.buf_o[slot], preferred_element_type=F32)
            self.block_out[:, at] = (self.block_out[:, at].astype(F32) + out).astype(BF16)

        def pull(t, slot):
            dq = self.dq_home[...].reshape(-1, self.w_o.shape[0])
            self.d_part[:, aligned(t)] = dot_t(dq, self.buf_q[slot])

        if t in PRODUCTS_AT:
            i = PRODUCTS_AT.index(t)
            self.homes[i].wait_recv()
            if i == 0:
                self.residual.wait()
            tiled(self.w_o.shape[0] // BLK, *((fetch_o, project), (fetch_q, pull))[i])
            self.write(i).start()

    def write(self, i):
        src = (self.block_out, self.d_part)[i]
        return pltpu.make_async_copy(src, self.out_refs[i], self.w_sem.at[i, 0])

    def wq_terms(self, own, other):
        self.h_mine.wait()
        self.h_back.start()
        for c in self.h_copies:
            c.wait_recv()
        self.h_back.wait()
        core = lax.rem(lax.axis_index("cp"), TWO)
        d_out = self.dq[...].reshape(-1, self.dq.shape[-1])

        def fetch(t, slot):
            return pltpu.make_async_copy(self.h_u.at[:, :, :, aligned(t)], self.h_buf.at[slot], self.load_sem.at[slot])

        for out, half in ((other, 1 - core), (own, core)):

            def use(t, slot, out=out, half=half):
                h = self.h_buf[slot].reshape(-1, BLK)
                out[t - half * FOUR] = dot(h, d_out, (0,), (0,)).reshape(out.shape[1:])

            tiled(FOUR, fetch, use, half * FOUR)

    def finish(self):
        for c in self.h_copies + self.homes:
            c.wait_send()
        for i in range(TWO):
            self.write(i).wait()


class HiddenGradient:
    tiles = FOUR

    def __init__(self, me, dk, dv, ins, outs, scratch):
        self.part, w_k, w_v, self.x, self.dy, self.gain = ins
        self.dx, self.terms = outs
        self.dk_home, self.dv_home, self.rows, self.w_k, self.w_v, *rest = scratch
        self.part_tile, self.x_tile, self.dy_tile, self.dx_tile, self.tile_sem, *sems = rest
        pairs = (w_k, self.w_k), (w_v, self.w_v)
        self.weights = [pltpu.make_async_copy(src, dst, self.tile_sem.at[i]) for i, (src, dst) in enumerate(pairs)]
        for c in self.weights:
            c.start()
        pairs = (dk, self.dk_home), (dv, self.dv_home)
        self.homes = [Home(me, src, out, *[r.at[i] for r in sems]) for i, (src, out) in enumerate(pairs)]
        for h in self.homes:
            h.start()

    @staticmethod
    def scratch(x):
        dma = pltpu.SemaphoreType.DMA
        home = pltpu.VMEM((TWO,) * THREE + (CHUNK, TWO * HEAD_DIM), BF16)
        tile = TWO * CHUNK, x.shape[1]
        weight = pltpu.VMEM((x.shape[1], TWO * HEAD_DIM), BF16)
        tiles = [pltpu.VMEM(tile, F32)] + [pltpu.VMEM(tile, BF16)] * THREE
        sems = [dma((FOUR,)), dma((TWO,)), dma((TWO, FOUR)), dma((TWO, FOUR))]
        return [home, home, pltpu.VMEM((8, x.shape[1]), F32), weight, weight] + tiles + sems

    def tile(self, t):
        if t == 0:
            for c in self.weights:
                c.wait()
            for h in self.homes:
                h.wait_recv()
            self.rows[...] = jnp.zeros_like(self.rows)
        size = TWO * CHUNK
        at = pl.ds(t * size, size)
        pairs = (self.part, self.part_tile), (self.x, self.x_tile), (self.dy, self.dy_tile)
        loads = [pltpu.make_async_copy(src.at[at], dst, self.tile_sem.at[i]) for i, (src, dst) in enumerate(pairs)]
        for c in loads:
            c.start()
        for c in loads:
            c.wait()
        d = self.part_tile[...]
        for home, w in ((self.dk_home, self.w_k), (self.dv_home, self.w_v)):
            d += dot_t(home[t // TWO, t % TWO].reshape(size, -1), w[...])
        d = d.astype(BF16).astype(F32)
        x = self.x_tile[...].astype(F32)
        inv_rms = lax.rsqrt(row_mean(x * x) + NORM_EPS)
        unit, scaled = x * inv_rms, d * self.gain[...]
        dx = inv_rms * (scaled - unit * row_mean(scaled * unit))
        self.dx_tile[...] = (self.dy_tile[...].astype(F32) + dx).astype(BF16)
        store = pltpu.make_async_copy(self.dx_tile, self.dx.at[at], self.tile_sem.at[THREE])
        store.start()
        self.rows[...] += jnp.sum((d * unit).reshape((-1,) + self.rows.shape), axis=0)
        store.wait()
        if t == self.tiles - 1:
            self.terms[...] = jnp.sum(self.rows[...], axis=0, keepdims=True)

    def finish(self):
        for h in self.homes:
            h.wait_send()


def reduce_pairs(arrays, blocks, cuts, kinds, collective_id, work, more):
    vmem, hbm = pl.BlockSpec(memory_space=pltpu.VMEM), pl.BlockSpec(memory_space=pl.ANY)
    n = len(blocks)
    scratch = [pltpu.VMEM((FOUR, TWO) + blocks[-1], F32)]
    scratch += sum((PairSum.scratch(k, b) for k, b in zip(kinds, blocks)), []) + PairSum.sems(n, max(cuts))
    outs = [jax.ShapeDtypeStruct(b, F32) for b in blocks] + work.results(more)
    return pl.pallas_call(
        functools.partial(reduce_kernel, cuts, kinds, work),
        name="reduce_pairs",
        out_shape=outs,
        in_specs=[hbm] * len(arrays) + [pl.BlockSpec(memory_space=m) for m in work.spaces],
        out_specs=[vmem] * n + [pl.BlockSpec(memory_space=m) for m in work.out_spaces],
        scratch_shapes=scratch + work.scratch(more),
        compiler_params=params(63, collective_id=collective_id),
        cost_estimate=cost(1, 20),
    )(*arrays, *more)


HERE = 0, 0, 0
LINKS = "xyud"
ORDERS = "zxy", "zyx", "yxz", "zyx"
CUTS = 0, 48, 96, 128
SIZES = 8.4, 8.4, 5.6, 2.8
GAIN_AT = [60.0 + 12.0 * i for i in range(5)]
LATENCY, TILES_FROM, TILE_EVERY = 3.0, 14.0, 8.0
SUM_AT = [25.0 + 6.0 * i for i in range(4)]


def onward(order, key):
    dz, ry, rx = key
    stage = max((order.index(a) for a, r in zip("zyx", key) if r), default=-1)
    for axis in order[stage + 1 :]:
        if axis == "x":
            yield "x", (dz, ry, 1)
        elif axis == "y":
            yield "y", (dz, 1, rx)
        else:
            yield "u", (-1, ry, rx)
            yield "d", (1, ry, rx)
    if stage >= 0 and order[stage] == "z" and abs(dz) < THREE:
        yield ("u", (dz - 1, ry, rx)) if dz < 0 else ("d", (dz + 1, ry, rx))


def arrivals():
    busy, times = {}, {}
    starts = [0.0] * THREE + [SUM_AT[-1] + LATENCY]
    here = [(t, z, part, HERE) for part, t in enumerate(starts) for z in range(FOUR)]
    while here:
        now, z, part, key = heapq.heappop(here)
        times.setdefault((part, key), []).append(now)
        for link, there in onward(ORDERS[part], key):
            to = z + {"u": 1, "d": -1}.get(link, 0)
            if 0 <= to <= THREE:
                busy[z, link] = max(busy.get((z, link), 0), now) + SIZES[part]
                heapq.heappush(here, (busy[z, link] + LATENCY, to, part, there))
    return sorted((sum(t) / len(t), *at) for at, t in times.items())


def turn_back(dkv_ref, cos_ref, sin_ref, dk_u, dv_u):
    n = TWO * TWO * BLK
    for i in range(TWO):
        for j in range(TWO):
            cos_t, sin_t = (jnp.hstack([t, t * sign]) for t, sign in ((cos_ref[i, j].T, 1), (sin_ref[i, j].T, -1)))
            dk = dkv_ref[pl.ds((i * TWO + j) * BLK, BLK)] * ATTN_SCALE
            dk_u[i, j] = (dk * cos_t + pltpu.roll(dk, HEAD_DIM // TWO, 1) * sin_t).astype(BF16)
    dv_u[...] = dkv_ref[pl.ds(n, n)].astype(BF16).reshape(dv_u.shape)


def wkv_terms(h_ref, h_buf, sem, dk_u, dv_u, outs):
    d_out = jnp.hstack([r[...].reshape(-1, HEAD_DIM) for r in (dk_u, dv_u)])

    def fetch(t, slot):
        return pltpu.make_async_copy(h_ref.at[:, :, :, aligned(t)], h_buf.at[slot], sem.at[slot])

    for out, half in outs:

        def use(t, slot, out=out, half=half):
            h = h_buf[slot].reshape(-1, BLK)
            out[t - half * FOUR] = dot(h, d_out, (0,), (0,)).reshape(out.shape[1:])

        tiled(FOUR, fetch, use, half * FOUR)


def gather_kernel(*refs):
    take = taker(refs)
    wo_ref, wq_ref, dkv_ref, cos_ref, sin_ref, h_ref = take(6)
    grad_ins, outs, (dx_ref, dgain_ref) = take(6), take(FOUR), take(TWO)
    own_sem, send_sem, come_sem, core_sem, put_sem, all_terms, totals, g_s, g_r = take(9)
    terms, wkv_ref, h_buf, h_sem, dk_u, dv_u, store, wkv_store = take(8)
    buffers, sems, refs = take(FOUR), take(7), take(len(refs))
    me = lax.axis_index("cp")
    z, y, x, core = place(me)
    line = Line(me)
    to = {"x": dev(z, y, 1 - x, core), "y": dev(z, 1 - y, x, core), "u": line.next[1], "d": line.next[-1]}
    partner = dev(z, y, x, 1 - core)
    all_here = announce(quad_of(me)[1:] + [to["y"]] + [dev(zz, y, x, core) for _, zz in z_peers(z)])
    chip_here = me // TWO
    n_wo, wide = wo_ref.shape[0], wq_ref.shape[1]
    store[chip_here, pl.ds(0, n_wo)] = wo_ref[...]
    for i in range(TWO):
        store[chip_here, pl.ds(n_wo, n_wo), pl.ds(i * wide, wide)] = wq_ref[pl.ds(i * n_wo, n_wo)]
    turn_back(dkv_ref, cos_ref, sin_ref, dk_u, dv_u)
    all_here()
    wkv = PairSum(me, "core", 1, wkv_ref, wkv_store.at[chip_here], buffers, [r.at[0] for r in sems])

    def place_of(key):
        dz, ry, rx = key
        return z + dz, 1 - y if ry else y, 1 - x if rx else x

    def block(part, key):
        zz, yy, xx = place_of(key)
        chip = (TWO * zz + yy) * TWO + xx
        return wkv_store.at[chip] if part == THREE else store.at[chip, pl.ds(CUTS[part], CUTS[part + 1] - CUTS[part])]

    def windows(part, key):
        zz, yy, xx = place_of(key)
        pair, src = TWO * zz + yy, block(part, key)
        wo_at, wq_at = ((xx * TWO + core) * N_PAIRS + pair) * n_wo, (core * N_PAIRS + pair) * wq_ref.shape[0]
        if part == THREE:
            for i, out in enumerate(outs[TWO:]):
                yield src.at[:, head(i)], out.at[pl.ds(wq_at, wq_ref.shape[0]), pl.ds(xx * HEAD_DIM, HEAD_DIM)]
            return
        first, last = CUTS[part : part + TWO]
        if first < n_wo:
            rows = min(last, n_wo) - first
            yield src.at[pl.ds(0, rows)], outs[0].at[pl.ds(wo_at + first, rows)]
        if last > n_wo:
            skip = max(n_wo - first, 0)
            rows, at = last - first - skip, first + skip - n_wo
            for i in range(TWO):
                window = outs[1].at[pl.ds(wq_at + i * n_wo + at, rows), pl.ds(xx * wide, wide)]
                yield src.at[pl.ds(skip, rows), pl.ds(i * wide, wide)], window

    def index(part, key):
        return (part, key[0] + THREE) + key[1:]

    def send(part, key, link, there):
        sent = send_sem.at[index(part, key) + (LINKS.find(link or "-") + 1,)]
        if link:
            remote(block(part, key), block(part, key), sent, come_sem.at[index(part, there)], to[link]).start()
            return
        for src, window in windows(part, key):
            remote(src, window, sent, core_sem.at[index(part, key)], partner).start()
            pltpu.make_async_copy(src, window, put_sem.at[index(part, key)]).start()

    def whole(part, send, arrive):
        size = CUTS[part + 1] - CUTS[part] if part < THREE else wkv_store.size // store.shape[0] // outs[0].shape[1]
        dst = outs[0].at[pl.ds(0, size)]
        return remote(dst, dst, send, arrive, me)

    def when(on, do):
        pl.when(on)(do)

    def each_way(part, key):
        held = line.held(key[0])
        yield None, key, held
        for link, there in onward(ORDERS[part], key):
            inside = {"u": line.inside[1], "d": line.inside[-1]}.get(link)
            yield link, there, held if inside is None else jnp.logical_and(held, inside)

    def pass_on(part, key):
        for link, there, on in each_way(part, key):
            when(on, functools.partial(send, part, key, link, there))

    def term_copy(i):
        src = terms if i == 0 else totals.at[i - 1]
        return remote(src, all_terms.at[i], g_s.at[i], g_r.at[i], me ^ (1 << i))

    def add_terms(i):
        term_copy(i).wait_recv()
        totals[i] = (terms[...] if i == 0 else totals[i - 1]) + all_terms[i]
        if i + 1 < len(GAIN_AT):
            term_copy(i + 1).start()

    def tile(t):
        job.tile(t)
        if t == job.tiles - 1:
            term_copy(0).start()

    def sum_step(h):
        wkv.step(0, h)

    steps = [(TILES_FROM + t * TILE_EVERY, functools.partial(tile, t)) for t in range(HiddenGradient.tiles)]
    steps += [(at, functools.partial(sum_step, h)) for h, at in enumerate(SUM_AT)]
    steps += [(at, functools.partial(add_terms, i)) for i, at in enumerate(GAIN_AT)]
    steps.sort(key=lambda s: s[0])
    events = arrivals()
    for part in range(THREE):
        pass_on(part, HERE)
    job = HiddenGradient(me, dk_u, dv_u, grad_ins, (dx_ref, terms), refs)
    wkv_terms(h_ref, h_buf, h_sem, dk_u, dv_u, ((wkv_ref, 1 - core), (buffers[0], core)))
    wkv.begin(0)
    wkv.loaded(0)
    for now, part, key in events:
        while steps and steps[0][0] <= now:
            steps.pop(0)[1]()
        if any(key):
            arrive = come_sem.at[index(part, key)]
            when(line.held(key[0]), whole(part, own_sem.at[0], arrive).wait_recv)
            pass_on(part, key)
        elif part == THREE:
            pass_on(part, key)
    dgain_ref[...] = totals[len(GAIN_AT) - 1]
    for i in range(len(GAIN_AT)):
        term_copy(i).wait_send()
    for _, part, key in events:
        for sem in (core_sem, put_sem):
            when(line.held(key[0]), whole(part, own_sem.at[0], sem.at[index(part, key)]).wait_recv)
        for link, there, on in each_way(part, key):
            sent = send_sem.at[index(part, key) + (LINKS.find(link or "-") + 1,)]
            when(on, whole(part, sent, own_sem.at[0]).wait_send)
    wkv.wait_send(0)
    job.finish()


def gather_all(wo, wq, dkv, cos_f, sin_f, h_u, part, w_k, w_v, x, dy, gain, shapes):
    dma = pltpu.SemaphoreType.DMA
    vmem, hbm = pl.BlockSpec(memory_space=pltpu.VMEM), pl.BlockSpec(memory_space=pl.ANY)
    block = w_k.shape[0] // TWO // N_PAIRS, w_k.shape[1]
    parts = len(ORDERS)
    keys = (parts, 7, TWO, TWO)
    terms = 1, x.shape[1]
    scratch = [dma((1,)), dma(keys + (len(LINKS) + 1,)), dma(keys), dma(keys), dma(keys)]
    n = len(GAIN_AT)
    scratch += [pltpu.VMEM((n,) + terms, F32)] * TWO + [dma((n,)), dma((n,)), pltpu.VMEM(terms, F32)]
    scratch += [pltpu.VMEM((FOUR, TWO) + block, F32), pltpu.VMEM((TWO, TWO, TWO, BLK, BLK), BF16), dma((TWO,))]
    scratch += [pltpu.VMEM((TWO, TWO, BLK, HEAD_DIM), BF16)] * TWO
    scratch += [pltpu.VMEM((TWO * N_PAIRS,) + b, F32) for b in ((TWO * wo.shape[0], wo.shape[1]), block)]
    return pl.pallas_call(
        gather_kernel,
        name="gather_all",
        out_shape=[jax.ShapeDtypeStruct(s, F32) for s in shapes]
        + [jax.ShapeDtypeStruct(x.shape, BF16), jax.ShapeDtypeStruct(terms, F32)],
        in_specs=[vmem] * 5 + [hbm] * 6 + [vmem],
        out_specs=[hbm] * (len(shapes) + 1) + [vmem],
        scratch_shapes=scratch + PairSum.scratch("core", block) + PairSum.sems(1, 1) + HiddenGradient.scratch(x),
        compiler_params=params(63, collective_id=0),
        cost_estimate=cost(1, 76),
    )(wo, wq, dkv, cos_f, sin_f, h_u, part, w_k, w_v, x, dy, gain)


def perm(x, pairs):
    return lax.ppermute(x, "cp", pairs)


def flip_pairs(d):
    return [(r, r ^ d) for r in range(32)]


def solution(mesh):
    def local_step(hidden, grad_out, positions, seg_ids, w_q, w_k, w_v, w_o, norm_gain):
        n_batch, n_tok, d_model = hidden.shape
        n_rows = n_batch * n_tok
        wide = N_HEADS * HEAD_DIM
        me = lax.axis_index("cp")
        z, y, x, core = place(me)
        quad, pair = me % FOUR, me // FOUR

        def swap(pieces):
            return [perm(p, flip_pairs(d)) if d else p for d, p in enumerate(pieces)]

        gain = norm_gain.astype(F32)
        cos_t, sin_t = rope_tables(positions.reshape(n_rows))
        cos_f, sin_f = jnp.hstack([cos_t, cos_t]), jnp.hstack([-sin_t, sin_t])
        dy_flat = grad_out.reshape(n_rows, d_model)
        normed, kv_home = project(hidden.reshape(n_rows, d_model), gain[NEW], w_k, w_v, cos_f, sin_f)
        pos = positions.reshape(TWO, TWO, n_tok)
        kv_home = kv_home.reshape((TWO,) * 5 + (CHUNK, HEAD_DIM))
        kv_all, q_u, do_u, pos_u, *dy_rows, dy_first = exchange(kv_home, normed, dy_flat, pos, cos_f, sin_f, w_q, w_o)
        pos_u = pos_u.reshape((FOUR, TWO, TWO, CHUNK)).transpose(1, TWO, 0, THREE).reshape(TWO, TWO, BLK)
        dy_rows = [a.reshape(-1, CHUNK, d_model) for a in dy_rows]
        dy_pieces = [*swap([dy_rows[0], dy_rows[1], dy_rows[0], dy_rows[TWO]]), dy_first[NEW]]

        member = quad ^ jnp.arange(FOUR)
        front, back = ((m[:, NEW] * CHUNK + jnp.arange(CHUNK)[NEW]).reshape(BLK) for m in (member, THREE - member))
        offsets = jnp.stack([front, back]).astype(jnp.int32)
        own_super = jnp.stack([pair, N_SUPER - 1 - pair]).astype(jnp.int32)
        q_index = own_super[:, NEW] * BLK + offsets
        start = q_index[NEW] - pos_u
        tab = jnp.concatenate(
            [own_super, (jnp.min(start, axis=-1) // BLK).reshape(-1), jnp.max(start, axis=-1).reshape(-1)]
        )
        start_r = start[:, :, NEW, :]
        index_r = q_index[:, NEW]
        cos_u, sin_u = rope_tables(pos_u)
        cos_ut, sin_ut = jnp.swapaxes(cos_u, TWO, THREE), jnp.swapaxes(sin_u, TWO, THREE)

        attn_u, lse = flash_fwd(tab, q_u, kv_all, start_r, index_r)

        wo_keep, wo_away = wo_terms(attn_u, dy_pieces)
        wo_come = perm(wo_away, flip_pairs(FOUR))
        do_u, wo_keep = lax.optimization_barrier((do_u, wo_keep))
        dq_u, dkv = flash_bwd(tab, q_u, do_u, attn_u, kv_all, lse, start_r, index_r, cos_ut, sin_ut)

        x_flat = hidden.reshape(n_rows, d_model)
        wo_own, dkv_own, wq_own, block_out, d_part, h_u = reduce_pairs(
            [wo_keep, wo_come, dkv.reshape(FOUR, TWO, -1, HEAD_DIM)],
            [wo_keep.shape[1:], (dkv.size // N_PAIRS // HEAD_DIM, HEAD_DIM), (d_model // TWO // N_PAIRS, wide)],
            (TWO, 8, 8),
            ("z", "", "core"),
            TWO,
            Products,
            (attn_u, dq_u, x_flat, normed.reshape((TWO,) * THREE + (CHUNK, d_model)), w_o, w_q),
        )
        grad_wo, grad_wq, grad_wk, grad_wv, grad_x, d_gain = gather_all(
            wo_own,
            wq_own,
            dkv_own,
            cos_ut,
            sin_ut,
            h_u,
            d_part,
            w_k,
            w_v,
            x_flat,
            dy_flat,
            gain[NEW],
            [w_o.shape, w_q.shape, w_k.shape, w_v.shape],
        )
        block_out, grad_x = (a.reshape(hidden.shape) for a in (block_out, grad_x))
        return block_out, grad_x, grad_wq, grad_wk, grad_wv, grad_wo, d_gain.reshape(d_model)

    seq_spec = P(None, "cp", None)
    tok_spec = P(None, "cp")
    full_spec = P()
    return jax.shard_map(
        local_step,
        mesh=mesh,
        in_specs=(seq_spec, seq_spec, tok_spec, tok_spec, full_spec, full_spec, full_spec, full_spec, full_spec),
        out_specs=(seq_spec, seq_spec, full_spec, full_spec, full_spec, full_spec, full_spec),
        check_vma=False,
    )
```

```python
import functools
import heapq
import itertools

import jax
import jax.numpy as jnp
from jax import lax
from jax.experimental import pallas as pl
from jax.experimental.pallas import tpu as pltpu
from jax.sharding import PartitionSpec as P

HEAD_DIM = 128
NORM_EPS = 1e-5
ROPE_BASE = 500000.0
NEG_BIG = -1e30
LOG2E = 1.4426950408889634
ATTN_SCALE = HEAD_DIM**-0.5
EXP2_SCALE = ATTN_SCALE * LOG2E
CHUNK = 64
TWO = 2
THREE = 3
FOUR = 4
NEW = jnp.newaxis
BLK = 4 * CHUNK
N_HEADS = 8
N_PAIRS = 8
N_SUPER = 2 * N_PAIRS
MESH = pl.DeviceIdType.MESH
ONE = pl.Squeezed()
GROUP = 8
DIRECT = 2
MADE_AT = 5
PRODUCTS_AT = 7, 9
F32 = jnp.float32
BF16 = jnp.bfloat16

T_SQ, T_LO, T_MX = 0, 2, 6


def rope_tables(positions):
    inv_freq = ROPE_BASE ** (-jnp.arange(0, HEAD_DIM, TWO).astype(F32) / HEAD_DIM)
    angles = positions.astype(F32)[..., None] * inv_freq
    return jnp.cos(angles), jnp.sin(angles)


def dot(a, b, ca, cb):
    return lax.dot_general(a, b, ((ca, cb), ((), ())), preferred_element_type=F32)


def cost(gflop, mib):
    return pl.CostEstimate(flops=gflop * 10**9, bytes_accessed=mib << 20, transcendentals=0)


def params(mib, **more):
    return pltpu.CompilerParams(vmem_limit_bytes=mib << 20, **more)


def row_mean(x):
    return jnp.mean(x, axis=-1, keepdims=True)


def head(h):
    return pl.ds(h * HEAD_DIM, HEAD_DIM)


def head_slice(h):
    return slice(h * HEAD_DIM, (h + 1) * HEAD_DIM)


def dot_t(a, b):
    return dot(a, b, (1,), (1,))


def steps(tab, body):
    b, hf = pl.program_id(0), pl.program_id(1)
    own, first, last_start = tab[T_SQ + hf], tab[T_LO + TWO * b + hf], tab[T_MX + TWO * b + hf]

    def place_of(s):
        late = s >= N_PAIRS
        return jnp.where(late, N_SUPER - 1 - s, s), late.astype(jnp.int32)

    full_from = jnp.minimum((last_start + BLK - 1) // BLK, own)
    full_from += lax.rem(own - full_from, TWO)
    count = full_from - first

    @pl.loop(0, count + 1)
    def _(t):
        s = jnp.where(t < count, first + t, own)
        body(s, place_of(s), True)

    @pl.loop(0, (own - full_from) // TWO)
    def _(t):
        for i in range(TWO):
            s = full_from + TWO * t + i
            body(s, place_of(s), False)


def down(row, n):
    return jnp.broadcast_to(row, (n, row.shape[-1])).T


def offsets_of(tab, qi_ref, hk):
    return qi_ref[hk] - tab[T_SQ + hk] * BLK


def may_use(s, off, start, index):
    return jnp.logical_and(off >= start - s * BLK, off <= index - s * BLK)


def fwd_kernel(tab, q_ref, kv_ref, st_ref, qi_ref, o_ref, lse_ref, q_s, acc, m_s, l_s, k_t, bounds):
    m_s[...] = jnp.full_like(m_s, NEG_BIG)
    l_s[...] = jnp.zeros_like(l_s)
    acc[...] = jnp.zeros_like(acc)
    for i, row in enumerate((st_ref[...], qi_ref[pl.program_id(1)])):
        bounds[i] = down(row, HEAD_DIM)
    for h in range(N_HEADS):
        q_s[pl.ds(h * BLK, BLK)] = q_ref[:, head(h)]

    @pl.when(pl.program_id(1) == 0)
    def _():
        @pl.loop(0, N_PAIRS)
        def _(pair):
            for hk in range(TWO):
                k_t[pair, hk] = kv_ref[pair, 0, hk].T

    def body(s, at, masked):
        pair, hk = at
        v = kv_ref[pair, 1, hk]
        if masked:
            off = offsets_of(tab, qi_ref, hk) + s * BLK
            mask = [
                jnp.logical_and(off[:, lanes] >= bounds[0], off[:, lanes] <= bounds[1])
                for lanes in (slice(HEAD_DIM), slice(HEAD_DIM, BLK))
            ]
            mask = [jnp.concatenate([m, m], axis=0) for m in mask]
        for g in range(N_HEADS // TWO):
            rows = pl.ds(g * TWO * BLK, TWO * BLK)
            sc = jnp.dot(q_s[rows], k_t[pair, hk], preferred_element_type=F32)
            sc = [sc[:, :HEAD_DIM], sc[:, HEAD_DIM:]]
            if masked:
                sc = [jnp.where(m, x, NEG_BIG) for m, x in zip(mask, sc)]
            m_old = m_s[rows]
            m_new = jnp.maximum(m_old, jnp.max(jnp.maximum(*sc), axis=1, keepdims=True))
            alpha = jnp.exp2((m_old - m_new) * EXP2_SCALE)
            p = [jnp.exp2((x - m_new) * EXP2_SCALE) for x in sc]
            m_s[rows] = m_new
            l_s[rows] = l_s[rows] * alpha + (p[0] + p[1])
            p = jnp.hstack([x.astype(BF16) for x in p])
            acc[rows] = acc[rows] * alpha + jnp.dot(p, v, preferred_element_type=F32)

    steps(tab, body)
    for h in range(N_HEADS):
        rows = pl.ds(h * BLK, BLK)
        total = jnp.sum(l_s[rows], axis=1, keepdims=True)
        o_ref[:, head(h)] = (acc[rows] / total).astype(BF16)
        lse_ref[h] = (m_s[rows] * EXP2_SCALE + jnp.log2(total)).T[:1]


def bwd_kernel(tab, q_ref, do_ref, o_ref, kv_ref, lse_ref, st_ref, qi_ref, cos_ref, sin_ref, dq_ref, dkv_ref, *scratch):
    dq_acc, delta, off_s, q_s, do_s, q_t, do_t, p_s, ds_s = scratch
    dq_acc[...] = jnp.zeros_like(dq_acc)
    for h in range(N_HEADS):
        q, do = q_ref[:, head(h)], do_ref[:, head(h)]
        delta[h] = jnp.sum((do.astype(F32) * o_ref[:, head(h)].astype(F32)).T, axis=0, keepdims=True)
        q_s[pl.ds(h * BLK, BLK)], do_s[pl.ds(h * BLK, BLK)] = q, do
        q_t[h], do_t[h] = q.T, do.T

    @pl.when(pl.program_id(1) == 0)
    def _():
        dkv_ref[...] = jnp.zeros_like(dkv_ref)
        for hk in range(TWO):
            off_s[hk] = down(offsets_of(tab, qi_ref, hk), BLK)

    def body(s, at, masked):
        pair, hk = at
        k = kv_ref[pair, 0, hk]
        v = kv_ref[pair, 1, hk]
        k_t = k.T
        mask = may_use(s, off_s[hk], st_ref[...], qi_ref[pl.program_id(1)]) if masked else None
        for first in range(0, N_HEADS, GROUP):
            rows = pl.ds(first * BLK, GROUP * BLK)
            for h in range(first, first + GROUP):
                cols = pl.ds(h * BLK, BLK)
                p = jnp.exp2(jnp.dot(k, q_t[h], preferred_element_type=F32) * EXP2_SCALE - lse_ref[h])
                if masked:
                    p = jnp.where(mask, p, 0.0)
                ds = p * (jnp.dot(v, do_t[h], preferred_element_type=F32) - delta[h])
                p_s[:, cols] = p.astype(BF16)
                ds_s[:, cols] = ds.astype(BF16)
            dkv_ref[pair, 0, hk] += jnp.dot(ds_s[:, rows], q_s[rows], preferred_element_type=F32)
            dkv_ref[pair, 1, hk] += jnp.dot(p_s[:, rows], do_s[rows], preferred_element_type=F32)
            dq_acc[:, rows] += jnp.dot(k_t, ds_s[:, rows], preferred_element_type=F32)

    steps(tab, body)
    cos_t, sin_t = cos_ref[...], sin_ref[...]
    half = HEAD_DIM // TWO
    for h in range(N_HEADS):
        cols = pl.ds(h * BLK, BLK)
        a, c = dq_acc[:half, cols] * ATTN_SCALE, dq_acc[half:, cols] * ATTN_SCALE
        lin = jnp.concatenate([a * cos_t + c * sin_t, c * cos_t - a * sin_t], axis=0)
        dq_ref[:, head(h)] = lin.T.astype(BF16)


def attn_specs():
    def at_tile(b, h, t):
        return (b, h) + (0,) * TWO

    def at_row(b, h, t):
        return (0, 0, b) + (0,) * THREE

    tile = pl.BlockSpec((ONE, ONE, BLK, N_HEADS * HEAD_DIM), at_tile)
    row = pl.BlockSpec((ONE, ONE, 1, BLK), at_tile)
    stat = pl.BlockSpec((ONE, ONE, N_HEADS, 1, BLK), lambda b, h, t: (b, h) + (0,) * THREE)
    rope = pl.BlockSpec((ONE, ONE, HEAD_DIM // TWO, BLK), at_tile)
    kv = pl.BlockSpec((N_PAIRS, TWO, ONE, TWO, BLK, HEAD_DIM), at_row)
    ko = pl.BlockSpec((TWO, 1, BLK), lambda b, h, t: (0,) * THREE)
    return tile, row, stat, kv, ko, rope


def flash_fwd(tab, q, kv, start, index):
    tile, row, stat, kvs, ko, _ = attn_specs()
    return pl.pallas_call(
        fwd_kernel,
        name="attn_fwd",
        out_shape=(jax.ShapeDtypeStruct(q.shape, BF16), jax.ShapeDtypeStruct((TWO, TWO, N_HEADS, 1, BLK), F32)),
        grid_spec=pltpu.PrefetchScalarGridSpec(
            num_scalar_prefetch=1,
            grid=(TWO, TWO),
            in_specs=[tile, kvs, row, ko],
            out_specs=[tile, stat],
            scratch_shapes=[pltpu.VMEM((N_HEADS * BLK, HEAD_DIM), t) for t in (BF16, F32, F32, F32)]
            + [pltpu.VMEM((N_PAIRS, TWO, HEAD_DIM, BLK), BF16), pltpu.VMEM((TWO, BLK, HEAD_DIM), jnp.int32)],
        ),
        compiler_params=params(63),
        cost_estimate=cost(20, 16),
    )(tab, q, kv, start, index)


def flash_bwd(tab, q, do, o, kv, lse, start, index, cos_t, sin_t):
    tile, row, stat, kvs, ko, rope = attn_specs()
    return pl.pallas_call(
        bwd_kernel,
        name="attn_bwd",
        out_shape=(
            jax.ShapeDtypeStruct(q.shape, BF16),
            jax.ShapeDtypeStruct(kv.shape, F32),
        ),
        grid_spec=pltpu.PrefetchScalarGridSpec(
            num_scalar_prefetch=1,
            grid=(TWO, TWO),
            in_specs=[tile, tile, tile, kvs, stat, row, ko, rope, rope],
            out_specs=[tile, kvs],
            scratch_shapes=[pltpu.VMEM((HEAD_DIM, N_HEADS * BLK), F32), pltpu.VMEM((N_HEADS, 1, BLK), F32)]
            + [pltpu.VMEM((TWO, BLK, BLK), jnp.int32)]
            + [pltpu.VMEM((N_HEADS * BLK, HEAD_DIM), BF16)] * TWO
            + [pltpu.VMEM((N_HEADS, HEAD_DIM, BLK), BF16)] * TWO
            + [pltpu.VMEM((BLK, N_HEADS * BLK), BF16)] * TWO,
        ),
        compiler_params=params(63),
        cost_estimate=cost(50, 32),
    )(tab, q, do, o, kv, lse, start, index, cos_t, sin_t)


def turn(x, cos_ref, sin_ref):
    return x * cos_ref[...] + pltpu.roll(x, HEAD_DIM // TWO, 1) * sin_ref[...]


def first_kernel(x_ref, g_ref, wk_ref, wv_ref, cos_ref, sin_ref, h_ref, kv_ref):
    x = x_ref[...].astype(F32)
    h = (x * lax.rsqrt(row_mean(x * x) + NORM_EPS) * g_ref[...]).astype(BF16)
    h_ref[...] = h
    k = jnp.dot(h, wk_ref[...], preferred_element_type=F32)
    v = jnp.dot(h, wv_ref[...], preferred_element_type=F32)
    n = kv_ref.shape[THREE]
    for i in range(TWO):
        for j, val in enumerate((turn(k[:, head_slice(i)], cos_ref, sin_ref), v[:, head_slice(i)])):
            for c in range(TWO):
                kv_ref[i, c, j] = val[c * n : (c + 1) * n].astype(BF16)


def project(x, gain, w_k, w_v, cos_f, sin_f):
    n = x.shape[0] // TWO
    return pl.pallas_call(
        first_kernel,
        name="norm_kv",
        out_shape=(jax.ShapeDtypeStruct(x.shape, BF16), jax.ShapeDtypeStruct((TWO,) * THREE + (n, HEAD_DIM), BF16)),
        compiler_params=params(63),
        cost_estimate=cost(TWO, 7),
    )(x, gain, w_k, w_v, cos_f, sin_f)


def place(me):
    return me // 8, lax.rem(me // FOUR, TWO), lax.rem(me // TWO, TWO), lax.rem(me, TWO)


def dev(z, y, x, core):
    return ((z * TWO + y) * TWO + x) * TWO + core


def z_peers(z):
    return [(k, lax.rem(z + k, FOUR)) for k in (1, TWO, THREE)]


def announce(peers):
    barrier = pltpu.get_barrier_semaphore()
    for d in peers:
        pl.semaphore_signal(barrier, device_id=(d,), device_id_type=MESH)
    return lambda: pl.semaphore_wait(barrier, len(peers))


def meet(peers):
    announce(peers)()


def remote(src, dst, send, arrive, to):
    return pltpu.make_async_remote_copy(
        src_ref=src, dst_ref=dst, send_sem=send, recv_sem=arrive, device_id=(to,), device_id_type=MESH
    )


class Line:
    order = (0, 1, -1, TWO, -TWO, THREE, -THREE)

    def __init__(self, me):
        self.z, y, x, core = place(me)
        self.next = {1: dev(self.z + 1, y, x, core), -1: dev(self.z - 1, y, x, core)}
        self.inside = {1: self.z < THREE, -1: self.z > 0}

    def held(self, dz):
        return jnp.logical_and(self.z + dz >= 0, self.z + dz <= THREE)

    def ways(self, dz):
        for d in self.next:
            if d * dz <= 0:
                yield d, self.inside[d] if dz == 0 else jnp.logical_and(self.inside[d], self.held(dz))


def tiled(n, fetch, use, first=0):
    fetch(first, 0).start()

    @pl.loop(0, n)
    def _(t):
        slot = lax.rem(t, TWO)
        fetch(first + t, slot).wait()

        @pl.when(t + 1 < n)
        def _():
            fetch(first + t + 1, 1 - slot).start()

        use(first + t, slot)


def aligned(t, size=BLK):
    return pl.ds(pl.multiple_of(t * size, size), size)


def exchange_kernel(*refs):
    take = taker(refs)
    kv_ref, h_ref, dy_ref, pos_ref, cos_ref, sin_ref, wq_ref, wo_ref, kv_all, q_u, do_u, pos_u, *dy_rows = take(14)
    own_sem, quad_s, quad_r, z_s, z_r, y_s, y_r, q_home, do_home, wq_buf, wo_buf, w_sem, dy_sem, h_own, dy_own = take(len(refs))
    me = lax.axis_index("cp")
    z, y, x, core = place(me)
    quad, line = quad_of(me), Line(me)
    across = dev(z, 1 - y, x, core)
    meet(quad[1:] + [across] + [dev(zz, y, x, core) for _, zz in z_peers(z)])

    def source(a, d):
        xx, cc = 1 - x if d // TWO else x, 1 - core if d % TWO else core
        return pos_ref.at[cc] if a == THREE else (kv_ref, q_home, do_home)[a].at[xx, cc]

    def target(a, d):
        if a == THREE:
            return pos_u.at[d]
        tok = pl.ds(d * CHUNK, CHUNK)
        return kv_all.at[me // FOUR, :, :, :, tok] if a == 0 else (q_u, do_u)[a - 1].at[:, :, tok]

    def quad_copy(a, d):
        return remote(source(a, d), target(a, d), quad_s.at[a, d], quad_r.at[a, d], quad[d])

    def own_copy(a):
        return pltpu.make_async_copy(source(a, 0), target(a, 0), own_sem.at[a])

    def z_copy(part, dz, d):
        block = kv_all.at[TWO * (z + dz) + y, part]
        return remote(block, block, z_s.at[part, (d + 1) // TWO, dz + THREE], z_r.at[part, dz - d + THREE], line.next[d])

    def y_copy(part, dz, yy=y):
        block = kv_all.at[TWO * (z + dz) + yy, part]
        return remote(block, block, y_s.at[part, dz + THREE], y_r.at[part, dz + THREE], across)

    parts = range(TWO)
    moves = [(part, dz) for dz in line.order for part in parts]

    def pass_on(count):
        for part, dz in [moves.pop(0) for _ in range(count)]:
            if dz:
                block = kv_all.at[TWO * (z + dz) + y, part]
                arrival = remote(block, block, own_sem.at[0], z_r.at[part, dz + THREE], me)
                pl.when(line.held(dz))(arrival.wait_recv)
            for d, on in line.ways(dz):
                pl.when(on)(z_copy(part, dz, d).start)
            pl.when(line.held(dz))(y_copy(part, dz).start)

    n = h_ref.shape[1] // BLK // TWO

    def fetch_q(t, slot):
        return pltpu.make_async_copy(wq_ref.at[:, aligned(t)], wq_buf.at[slot], w_sem.at[0, slot])

    def fetch_o(t, slot):
        return pltpu.make_async_copy(wo_ref.at[aligned(t)], wo_buf.at[slot], w_sem.at[1, slot])

    def put(home, t, val):
        home[t // n, :, :, :, :, aligned(lax.rem(t, n))] = val.astype(BF16).reshape(home.shape[1:-1] + (BLK,))

    def query(t, slot):
        q = jnp.dot(h_own[...], wq_buf[slot], preferred_element_type=F32)
        put(q_home, t, jnp.hstack([turn(q[:, head_slice(j)], cos_ref, sin_ref) for j in range(BLK // HEAD_DIM)]))

    def pull(t, slot):
        put(do_home, t, dot_t(dy_own[...], wo_buf[slot]))

    all_moves = list(moves)
    loads = [pltpu.make_async_copy(a, b, dy_sem.at[i]) for i, (a, b) in enumerate(((h_ref, h_own), (dy_ref, dy_own)))]
    half = dy_own.shape[0] // TWO

    def dy_copy(i):
        return pltpu.make_async_copy(dy_own.at[aligned(1 - core if i else core, half)], dy_rows[i], dy_sem.at[i])

    for a in (0, THREE):
        for d in (1, TWO, THREE):
            quad_copy(a, d).start()
        own_copy(a).start()
    for c in loads:
        c.start()
    for c in loads:
        c.wait()
    for i in range(TWO):
        dy_copy(i).start()
    for a, (fetch, use) in enumerate(((fetch_q, query), (fetch_o, pull)), 1):
        for near in range(TWO):
            tiled(n, fetch, use, n * (x if near else 1 - x))
            for d in range(TWO):
                if d or not near:
                    quad_copy(a, d if near else d + TWO).start()
            if near:
                own_copy(a).start()
            if len(moves) == len(all_moves):
                own_copy(0).wait()
                for d in (1, TWO, THREE):
                    quad_copy(0, d).wait_recv()
            pass_on(TWO)
    pass_on(len(moves))
    for part, dz in all_moves:
        for d, on in line.ways(dz):
            pl.when(on)(z_copy(part, dz, d).wait_send)
        pl.when(line.held(dz))(y_copy(part, dz, 1 - y).wait_recv)
        pl.when(line.held(dz))(y_copy(part, dz).wait_send)
    for a in range(FOUR):
        for d in (1, TWO, THREE):
            quad_copy(a, d).wait_send()
            if a > 0:
                quad_copy(a, d).wait_recv()
    for a in (1, TWO, THREE):
        own_copy(a).wait()
    for i in range(TWO):
        dy_copy(i).wait()


def exchange(kv, h, dy, pos, cos_f, sin_f, w_q, w_o):
    dma = pltpu.SemaphoreType.DMA
    vmem, hbm = pl.BlockSpec(memory_space=pltpu.VMEM), pl.BlockSpec(memory_space=pl.ANY)
    wide = w_q.shape[1] // TWO
    unit = jax.ShapeDtypeStruct((TWO, TWO, BLK, wide), BF16)
    pos_quad = jax.ShapeDtypeStruct((FOUR,) + pos.shape[1:], pos.dtype)
    dy_half = jax.ShapeDtypeStruct((dy.shape[0] // TWO, dy.shape[1]), BF16)
    home = pltpu.VMEM((TWO,) * FOUR + (CHUNK, wide), BF16)
    sems = [dma((FOUR,))] + [dma((FOUR, FOUR))] * TWO + [dma((TWO, TWO, 7))] + [dma((TWO, 7))] * THREE
    bufs = [pltpu.VMEM((TWO,) + b, BF16) for b in ((w_q.shape[0], BLK), (BLK, w_o.shape[1]))]
    return pl.pallas_call(
        exchange_kernel,
        name="exchange",
        out_shape=(jax.ShapeDtypeStruct((N_PAIRS,) + (TWO,) * THREE + (BLK, HEAD_DIM), BF16), unit, unit, pos_quad, dy_half, dy_half),
        in_specs=[vmem] + [hbm] * THREE + [vmem] * TWO + [hbm] * TWO,
        out_specs=[hbm] * 6,
        scratch_shapes=sems + [home, home] + bufs + [dma((TWO, TWO)), dma((TWO,))] + [pltpu.VMEM(h.shape, BF16)] * TWO,
        compiler_params=params(63, collective_id=1),
        cost_estimate=cost(1, 20),
    )(kv, h, dy, pos, cos_f, sin_f, w_q, w_o)


def taker(refs):
    rest = iter(refs)
    return lambda count: list(itertools.islice(rest, count))


def wo_kernel(*refs):
    take = taker(refs)
    o_ref, *pieces = take(5)
    keep_ref, away_ref, dy_u, o_t, terms, came, load_sem, core_s, core_r, keep, away, out_sem = take(len(refs))
    me = lax.axis_index("cp")
    _, y, _, core = place(me)
    all_here = announce(quad_of(me)[1:TWO])
    loads = [
        pltpu.make_async_copy(src, dy_u.at[:, :, pl.ds(d * CHUNK, CHUNK)], load_sem.at[d])
        for d, src in enumerate(pieces)
    ]
    for c in loads:
        c.start()
    for h in range(N_HEADS):
        o_t[head(h)] = o_ref[:, :, :, head(h)].reshape(-1, HEAD_DIM).T
    for c in loads:
        c.wait()
    all_here()
    half, tiles = terms.shape[1], terms.shape[TWO] // BLK

    def swap(t):
        return remote(terms.at[0, :, aligned(t)], came.at[:, aligned(t)], core_s.at[t], core_r.at[t], quad_of(me)[1])

    def half_terms(i, to, then):
        @pl.loop(0, tiles)
        def _(t):
            dy = dy_u[:, :, :, aligned(t)].reshape(-1, BLK)
            terms[to, :, aligned(t)] = jnp.dot(o_t[aligned(i, half)], dy, preferred_element_type=F32)
            then(t)

    half_terms(1 - core, 0, lambda t: swap(t).start())
    half_terms(core, 1, lambda t: swap(t).wait_recv())
    rows = keep.shape[1]

    def results(zz):
        pairs = (keep, keep_ref), (away, away_ref)
        return [pltpu.make_async_copy(a.at[zz], b.at[zz], out_sem.at[i, zz]) for i, (a, b) in enumerate(pairs)]

    for zz in range(FOUR):
        for out, yy in ((keep, y), (away, 1 - y)):
            at = aligned(TWO * zz + yy, rows)
            out[zz] = terms[1, at] + came[at]
        for c in results(zz):
            c.start()
    for zz in range(FOUR):
        for c in results(zz):
            c.wait()
    for t in range(tiles):
        swap(t).wait_send()


def wo_terms(o, pieces):
    dma = pltpu.SemaphoreType.DMA
    vmem, hbm = pl.BlockSpec(memory_space=pltpu.VMEM), pl.BlockSpec(memory_space=pl.ANY)
    n, d, wide = o.shape[0] * o.shape[1] * o.shape[TWO], pieces[0].shape[-1], o.shape[-1]
    half = wide // TWO
    return pl.pallas_call(
        wo_kernel,
        name="wo_terms",
        out_shape=[jax.ShapeDtypeStruct((FOUR, half // N_PAIRS, d), F32)] * TWO,
        in_specs=[vmem] + [hbm] * FOUR,
        out_specs=[hbm] * TWO,
        scratch_shapes=[pltpu.VMEM((TWO, TWO, BLK, d), BF16), pltpu.VMEM((wide, n), BF16)]
        + [pltpu.VMEM((TWO, half, d), F32), pltpu.VMEM((half, d), F32), dma((FOUR,)), dma((d // BLK,)), dma((d // BLK,))]
        + [pltpu.VMEM((FOUR, half // N_PAIRS, d), F32)] * TWO
        + [dma((TWO, FOUR))],
        compiler_params=params(63, collective_id=THREE),
        cost_estimate=cost(FOUR, 20),
    )(o, *pieces)


class PairSum:
    def __init__(self, me, kind, cut, src, out, buffers, sems, direct=0):
        self.me, self.kind, self.src, self.out = me, kind, src, out
        self.direct_from = cut - direct
        self.size = out.shape[0] // cut
        self.own, self.from_core, self.from_y, self.from_z = buffers
        self.load_sem, self.core_s, self.core_r, self.y_s, self.y_r, self.z_s, self.z_r = sems
        self.z, self.y, x, core = place(me)
        self.partner = dev(self.z, self.y, x, 1 - core)
        self.line = [(k, zz, dev(zz, self.y, x, core)) for k, zz in z_peers(self.z)]
        self.across = dev(self.z, 1 - self.y, x, core)
        self.next_z = dev(self.z + 1, self.y, x, core), dev(self.z - 1, self.y, x, core)

    def rows(self, j):
        return pl.ds(j * self.size, self.size)

    def mine(self, j, zz):
        at = self.rows(j)
        return self.own.at[zz, self.y, at] if self.kind == "core" else self.own.at[zz, at]

    def loads(self, j):
        at = self.rows(j)
        if self.kind == "z":
            pairs = zip(self.src, (self.own, self.from_y))
            return [pltpu.make_async_copy(a.at[:, at], b.at[:, at], s.at[j]) for (a, b), s in zip(pairs, (self.load_sem, self.y_r))]
        return [pltpu.make_async_copy(self.src.at[:, self.y, at], self.own.at[:, at], self.load_sem.at[j])]

    def core_copy(self, j):
        src, dst = (r.at[:, :, self.rows(j)] for r in (self.src, self.from_core))
        return remote(src, dst, self.core_s.at[j], self.core_r.at[j], self.partner)

    def y_copy(self, j):
        src = self.own if self.kind == "core" else self.src
        at = self.rows(j)
        return remote(src.at[:, 1 - self.y, at], self.from_y.at[:, at], self.y_s.at[j], self.y_r.at[j], self.across)

    def z_copy(self, j, way, zz, to):
        at = way, zz + way - 1
        return remote(self.mine(j, zz), self.from_z.at[*at, self.rows(j)], self.z_s.at[j, *at], self.z_r.at[j, *at], to)

    def begin(self, j):
        if self.kind == "core":
            self.core_copy(j).start()
            return
        for c in self.loads(j):
            c.start()
        if not self.kind:
            self.y_copy(j).start()

    def loaded(self, j):
        if self.kind != "core":
            for c in self.loads(j):
                c.wait()
        else:
            self.core_copy(j).wait_recv()
            at = self.rows(j)
            for zz in range(FOUR):
                self.own[zz, :, at] += self.from_core[zz, :, at]
            self.y_copy(j).start()
        if self.kind == "z":
            self.add_y(j)
            self.hop(j, 0)

    def add_y(self, j):
        for zz in range(FOUR):
            self.mine(j, zz)[...] += self.from_y[zz, self.rows(j)]

    def relay(self, j, way, zz, add):
        if add:
            self.z_copy(j, way, zz, self.me).wait_recv()
            self.mine(j, zz)[...] += self.from_z[way, zz + way - 1, self.rows(j)]
        self.z_copy(j, way, zz, self.next_z[way]).start()

    def hop(self, j, h):
        @pl.when(self.z == h)
        def _():
            for zz in range(THREE, h, -1):
                self.relay(j, 0, zz, h > 0)

        @pl.when(self.z == THREE - h)
        def _():
            for zz in range(THREE - h):
                self.relay(j, 1, zz, h > 0)

    def z_direct(self, j):
        for k, zz, to in self.line:
            at, there = (j, 0, k - 1), self.from_z.at[0, k - 1, self.rows(j)]
            yield remote(self.mine(j, zz), there, self.z_s.at[at], self.z_r.at[at], to), there

    def step(self, j, h):
        if j >= self.direct_from and h > 0:
            if h == 1:
                at = self.rows(j)
                self.out[at] = self.mine(j, self.z)[...]
                for c, arrived in self.z_direct(j):
                    c.wait_recv()
                    self.out[at] += arrived[...]
            return
        if h == 0 and self.kind != "z":
            self.y_copy(j).wait_recv()
            self.add_y(j)
            if j < self.direct_from:
                self.hop(j, 0)
            else:
                for c, _ in self.z_direct(j):
                    c.start()
        elif 0 < h < THREE:
            self.hop(j, h)
        elif h == THREE:
            at = self.rows(j)
            self.out[at] = self.mine(j, self.z)[...]
            for way, on in enumerate((self.z > 0, self.z < THREE)):

                @pl.when(on)
                def _(way=way):
                    self.z_copy(j, way, self.z, self.me).wait_recv()
                    self.out[at] += self.from_z[way, self.z + way - 1, at]

    def wait_send(self, j):
        if self.kind == "core":
            self.core_copy(j).wait_send()
        if self.kind != "z":
            self.y_copy(j).wait_send()
        if j >= self.direct_from:
            for c, _ in self.z_direct(j):
                c.wait_send()
            return
        for zz in range(FOUR):
            if zz > 0:
                pl.when(self.z < zz)(self.z_copy(j, 0, zz, self.next_z[0]).wait_send)
            if zz < THREE:
                pl.when(self.z > zz)(self.z_copy(j, 1, zz, self.next_z[1]).wait_send)

    @staticmethod
    def scratch(kind, block):
        unused = pltpu.VMEM((8, HEAD_DIM), F32)
        own = pltpu.VMEM(((FOUR, TWO) if kind == "core" else (FOUR,)) + block, F32)
        from_y = pltpu.VMEM((FOUR,) + block, F32)
        return [own, own if kind == "core" else unused, from_y, pltpu.VMEM((TWO, THREE) + block, F32)]

    @staticmethod
    def sems(*dims):
        dma = pltpu.SemaphoreType.DMA
        return [dma(dims)] * 5 + [dma(dims + (TWO, THREE))] * TWO


def reduce_kernel(cuts, kinds, work, *refs):
    n = len(cuts)

    take = taker(refs)
    ins = [take(TWO) if k == "z" else take(1)[0] for k in kinds[:-1]]
    more_in, outs, more_out, made = take(work.ins), take(n), take(work.outs), take(1)
    buffers, sems = [take(FOUR) for _ in kinds], take(7)
    me = lax.axis_index("cp")
    z, y, x, core = place(me)
    meet(quad_of(me)[1:] + [dev(z, 1 - y, x, core)] + [dev(zz, y, x, core) for _, zz in z_peers(z)])
    job = work(me, more_in, more_out, take(len(refs)))
    inputs = enumerate(zip(kinds, cuts, ins + made, outs, buffers))
    sums = [PairSum(me, *a, [r.at[i] for r in sems], DIRECT if i == n - 1 else 0) for i, a in inputs]
    pieces = [(s, j) for s, cut in zip(sums, cuts) for j in range(cut)]
    early, late = pieces[: -cuts[-1]], pieces[-cuts[-1] :]
    for s, j in early:
        s.begin(j)
    for s, j in early:
        s.loaded(j)
    for t in range(len(pieces) + THREE):
        if t == MADE_AT:
            job.wq_terms(sums[-1].own, made[0])
            for s, j in late:
                s.begin(j)
        if t == MADE_AT + 1:
            for s, j in late:
                s.loaded(j)
        for h in range(FOUR):
            if 0 <= t - h < len(pieces):
                s, j = pieces[t - h]
                s.step(j, h)
        job.step(t)
    for s, j in pieces:
        s.wait_send(j)
    job.finish()


def quad_of(me):
    z, y, x, core = place(me)
    return [dev(z, y, 1 - x if d // TWO else x, 1 - core if d % TWO else core) for d in range(FOUR)]


class Home:
    def __init__(self, me, src, out, own_sem, send, arrive):
        _, _, x, core = place(me)
        w = src.shape[-1]
        to = out.at[core, :, :, :, pl.ds(x * w, w)]

        def piece(d):
            return src.at[:, :, pl.ds(d * CHUNK, CHUNK)]

        self.own = pltpu.make_async_copy(piece(0), to, own_sem)
        self.copies = [remote(piece(d), to, send.at[d], arrive.at[d], quad_of(me)[d]) for d in (1, TWO, THREE)]

    def start(self):
        self.own.start()
        for c in self.copies:
            c.start()

    def wait_recv(self):
        self.own.wait()
        for c in self.copies:
            c.wait_recv()

    def wait_send(self):
        for c in self.copies:
            c.wait_send()


class Products:
    ins, outs = 6, THREE

    def __init__(self, me, ins, outs, scratch):
        attn, self.dq, hidden, normed, self.w_o, self.w_q = ins
        self.out_refs, self.h_u = outs[:TWO], outs[TWO]
        self.block_out, self.d_part, self.attn_home, self.dq_home, self.buf_o, self.buf_q, stage, self.h_buf, *sems = scratch
        self.w_sem, self.load_sem, own_sem, quad_s, quad_r = sems
        _, _, _, core = place(me)

        def piece(d):
            return normed.at[1 - core if d % TWO else core]

        def tokens(d):
            return self.h_u.at[:, :, pl.ds(d * CHUNK, CHUNK)]

        self.h_copies = [remote(piece(d), tokens(d), quad_s.at[TWO, d], quad_r.at[TWO, d], quad_of(me)[d]) for d in (1, TWO, THREE)]
        self.h_mine = pltpu.make_async_copy(piece(0), stage, own_sem.at[TWO])
        self.h_back = pltpu.make_async_copy(stage, tokens(0), self.load_sem.at[0])
        self.residual = pltpu.make_async_copy(hidden, self.block_out, own_sem.at[THREE])
        self.residual.start()
        for c in self.h_copies:
            c.start()
        self.h_mine.start()
        self.homes = [
            Home(me, src, out, own_sem.at[i], quad_s.at[i], quad_r.at[i])
            for i, (src, out) in enumerate([(attn, self.attn_home), (self.dq, self.dq_home)])
        ]
        for h in self.homes:
            h.start()

    @staticmethod
    def scratch(arrays):
        dma, d = pltpu.SemaphoreType.DMA, arrays[-1].shape[0]
        home = pltpu.VMEM((TWO,) * THREE + (CHUNK, d), BF16)
        buf = [pltpu.VMEM((TWO,) + b, BF16) for b in ((d, BLK), (BLK, d))]
        tiles = [pltpu.VMEM((TWO, TWO) + b, BF16) for b in ((CHUNK, d), (TWO, BLK, BLK))]
        sems = [dma((TWO, TWO)), dma((TWO,)), dma((FOUR,)), dma((THREE, FOUR)), dma((THREE, FOUR))]
        products = [pltpu.VMEM(arrays[TWO].shape, t) for t in (BF16, F32)]
        return products + [home] * TWO + buf + tiles + sems

    @staticmethod
    def results(arrays):
        unit = TWO, TWO, BLK, arrays[-1].shape[0]
        return [jax.ShapeDtypeStruct(arrays[TWO].shape, t) for t in (BF16, F32)] + [jax.ShapeDtypeStruct(unit, BF16)]

    spaces, out_spaces = [pl.ANY, pltpu.VMEM] + [pl.ANY] * FOUR, [pl.ANY] * THREE

    def step(self, t):
        def fetch_o(t, slot):
            return pltpu.make_async_copy(self.w_o.at[:, aligned(t)], self.buf_o.at[slot], self.w_sem.at[0, slot])

        def fetch_q(t, slot):
            return pltpu.make_async_copy(self.w_q.at[aligned(t)], self.buf_q.at[slot], self.w_sem.at[1, slot])

        def project(t, slot):
            at = aligned(t)
            attn = self.attn_home[...].reshape(-1, self.w_o.shape[0])
            out = jnp.dot(attn, self.buf_o[slot], preferred_element_type=F32)
            self.block_out[:, at] = (self.block_out[:, at].astype(F32) + out).astype(BF16)

        def pull(t, slot):
            dq = self.dq_home[...].reshape(-1, self.w_o.shape[0])
            self.d_part[:, aligned(t)] = dot_t(dq, self.buf_q[slot])

        if t in PRODUCTS_AT:
            i = PRODUCTS_AT.index(t)
            self.homes[i].wait_recv()
            if i == 0:
                self.residual.wait()
            tiled(self.w_o.shape[0] // BLK, *((fetch_o, project), (fetch_q, pull))[i])
            self.write(i).start()

    def write(self, i):
        src = (self.block_out, self.d_part)[i]
        return pltpu.make_async_copy(src, self.out_refs[i], self.w_sem.at[i, 0])

    def wq_terms(self, own, other):
        self.h_mine.wait()
        self.h_back.start()
        for c in self.h_copies:
            c.wait_recv()
        self.h_back.wait()
        core = lax.rem(lax.axis_index("cp"), TWO)
        d_out = self.dq[...].reshape(-1, self.dq.shape[-1])

        def fetch(t, slot):
            return pltpu.make_async_copy(self.h_u.at[:, :, :, aligned(t)], self.h_buf.at[slot], self.load_sem.at[slot])

        for out, half in ((other, 1 - core), (own, core)):

            def use(t, slot, out=out, half=half):
                h = self.h_buf[slot].reshape(-1, BLK)
                out[t - half * FOUR] = dot(h, d_out, (0,), (0,)).reshape(out.shape[1:])

            tiled(FOUR, fetch, use, half * FOUR)

    def finish(self):
        for c in self.h_copies + self.homes:
            c.wait_send()
        for i in range(TWO):
            self.write(i).wait()


class HiddenGradient:
    tiles = FOUR

    def __init__(self, me, dk, dv, ins, outs, scratch):
        self.part, w_k, w_v, self.x, self.dy, self.gain = ins
        self.dx, self.terms = outs
        self.dk_home, self.dv_home, self.rows, self.w_k, self.w_v, *rest = scratch
        self.part_tile, self.x_tile, self.dy_tile, self.dx_tile, self.tile_sem, *sems = rest
        pairs = (w_k, self.w_k), (w_v, self.w_v)
        self.weights = [pltpu.make_async_copy(src, dst, self.tile_sem.at[i]) for i, (src, dst) in enumerate(pairs)]
        for c in self.weights:
            c.start()
        pairs = (dk, self.dk_home), (dv, self.dv_home)
        self.homes = [Home(me, src, out, *[r.at[i] for r in sems]) for i, (src, out) in enumerate(pairs)]
        for h in self.homes:
            h.start()

    @staticmethod
    def scratch(x):
        dma = pltpu.SemaphoreType.DMA
        home = pltpu.VMEM((TWO,) * THREE + (CHUNK, TWO * HEAD_DIM), BF16)
        tile = TWO * CHUNK, x.shape[1]
        weight = pltpu.VMEM((x.shape[1], TWO * HEAD_DIM), BF16)
        tiles = [pltpu.VMEM(tile, F32)] + [pltpu.VMEM(tile, BF16)] * THREE
        sems = [dma((FOUR,)), dma((TWO,)), dma((TWO, FOUR)), dma((TWO, FOUR))]
        return [home, home, pltpu.VMEM((8, x.shape[1]), F32), weight, weight] + tiles + sems

    def tile(self, t):
        if t == 0:
            for c in self.weights:
                c.wait()
            for h in self.homes:
                h.wait_recv()
            self.rows[...] = jnp.zeros_like(self.rows)
        size = TWO * CHUNK
        at = pl.ds(t * size, size)
        pairs = (self.part, self.part_tile), (self.x, self.x_tile), (self.dy, self.dy_tile)
        loads = [pltpu.make_async_copy(src.at[at], dst, self.tile_sem.at[i]) for i, (src, dst) in enumerate(pairs)]
        for c in loads:
            c.start()
        for c in loads:
            c.wait()
        d = self.part_tile[...]
        for home, w in ((self.dk_home, self.w_k), (self.dv_home, self.w_v)):
            d += dot_t(home[t // TWO, t % TWO].reshape(size, -1), w[...])
        d = d.astype(BF16).astype(F32)
        x = self.x_tile[...].astype(F32)
        inv_rms = lax.rsqrt(row_mean(x * x) + NORM_EPS)
        unit, scaled = x * inv_rms, d * self.gain[...]
        dx = inv_rms * (scaled - unit * row_mean(scaled * unit))
        self.dx_tile[...] = (self.dy_tile[...].astype(F32) + dx).astype(BF16)
        store = pltpu.make_async_copy(self.dx_tile, self.dx.at[at], self.tile_sem.at[THREE])
        store.start()
        self.rows[...] += jnp.sum((d * unit).reshape((-1,) + self.rows.shape), axis=0)
        store.wait()
        if t == self.tiles - 1:
            self.terms[...] = jnp.sum(self.rows[...], axis=0, keepdims=True)

    def finish(self):
        for h in self.homes:
            h.wait_send()


def reduce_pairs(arrays, blocks, cuts, kinds, collective_id, work, more):
    vmem, hbm = pl.BlockSpec(memory_space=pltpu.VMEM), pl.BlockSpec(memory_space=pl.ANY)
    n = len(blocks)
    scratch = [pltpu.VMEM((FOUR, TWO) + blocks[-1], F32)]
    scratch += sum((PairSum.scratch(k, b) for k, b in zip(kinds, blocks)), []) + PairSum.sems(n, max(cuts))
    outs = [jax.ShapeDtypeStruct(b, F32) for b in blocks] + work.results(more)
    return pl.pallas_call(
        functools.partial(reduce_kernel, cuts, kinds, work),
        name="reduce_pairs",
        out_shape=outs,
        in_specs=[hbm] * len(arrays) + [pl.BlockSpec(memory_space=m) for m in work.spaces],
        out_specs=[vmem] * n + [pl.BlockSpec(memory_space=m) for m in work.out_spaces],
        scratch_shapes=scratch + work.scratch(more),
        compiler_params=params(63, collective_id=collective_id),
        cost_estimate=cost(1, 20),
    )(*arrays, *more)


HERE = 0, 0, 0
LINKS = "xyud"
ORDERS = "zxy", "zyx", "yxz", "zyx"
CUTS = 0, 48, 96, 128
SIZES = 8.4, 8.4, 5.6, 2.8
GAIN_AT = [60.0 + 12.0 * i for i in range(5)]
LATENCY, TILES_FROM, TILE_EVERY = 3.0, 14.0, 8.0
SUM_AT = [25.0 + 6.0 * i for i in range(4)]


def onward(order, key):
    dz, ry, rx = key
    stage = max((order.index(a) for a, r in zip("zyx", key) if r), default=-1)
    for axis in order[stage + 1 :]:
        if axis == "x":
            yield "x", (dz, ry, 1)
        elif axis == "y":
            yield "y", (dz, 1, rx)
        else:
            yield "u", (-1, ry, rx)
            yield "d", (1, ry, rx)
    if stage >= 0 and order[stage] == "z" and abs(dz) < THREE:
        yield ("u", (dz - 1, ry, rx)) if dz < 0 else ("d", (dz + 1, ry, rx))


def arrivals():
    busy, times = {}, {}
    starts = [0.0] * THREE + [SUM_AT[-1] + LATENCY]
    here = [(t, z, part, HERE) for part, t in enumerate(starts) for z in range(FOUR)]
    while here:
        now, z, part, key = heapq.heappop(here)
        times.setdefault((part, key), []).append(now)
        for link, there in onward(ORDERS[part], key):
            to = z + {"u": 1, "d": -1}.get(link, 0)
            if 0 <= to <= THREE:
                busy[z, link] = max(busy.get((z, link), 0), now) + SIZES[part]
                heapq.heappush(here, (busy[z, link] + LATENCY, to, part, there))
    return sorted((sum(t) / len(t), *at) for at, t in times.items())


def turn_back(dkv_ref, cos_ref, sin_ref, dk_u, dv_u):
    n = TWO * TWO * BLK
    for i in range(TWO):
        for j in range(TWO):
            cos_t, sin_t = (jnp.hstack([t, t * sign]) for t, sign in ((cos_ref[i, j].T, 1), (sin_ref[i, j].T, -1)))
            dk = dkv_ref[pl.ds((i * TWO + j) * BLK, BLK)] * ATTN_SCALE
            dk_u[i, j] = (dk * cos_t + pltpu.roll(dk, HEAD_DIM // TWO, 1) * sin_t).astype(BF16)
    dv_u[...] = dkv_ref[pl.ds(n, n)].astype(BF16).reshape(dv_u.shape)


def wkv_terms(h_ref, h_buf, sem, dk_u, dv_u, outs):
    d_out = jnp.hstack([r[...].reshape(-1, HEAD_DIM) for r in (dk_u, dv_u)])

    def fetch(t, slot):
        return pltpu.make_async_copy(h_ref.at[:, :, :, aligned(t)], h_buf.at[slot], sem.at[slot])

    for out, half in outs:

        def use(t, slot, out=out, half=half):
            h = h_buf[slot].reshape(-1, BLK)
            out[t - half * FOUR] = dot(h, d_out, (0,), (0,)).reshape(out.shape[1:])

        tiled(FOUR, fetch, use, half * FOUR)


def gather_kernel(*refs):
    take = taker(refs)
    wo_ref, wq_ref, dkv_ref, cos_ref, sin_ref, h_ref = take(6)
    grad_ins, outs, (dx_ref, dgain_ref) = take(6), take(FOUR), take(TWO)
    own_sem, send_sem, come_sem, core_sem, put_sem, all_terms, totals, g_s, g_r = take(9)
    terms, wkv_ref, h_buf, h_sem, dk_u, dv_u, store, wkv_store = take(8)
    buffers, sems, refs = take(FOUR), take(7), take(len(refs))
    me = lax.axis_index("cp")
    z, y, x, core = place(me)
    line = Line(me)
    to = {"x": dev(z, y, 1 - x, core), "y": dev(z, 1 - y, x, core), "u": line.next[1], "d": line.next[-1]}
    partner = dev(z, y, x, 1 - core)
    all_here = announce(quad_of(me)[1:] + [to["y"]] + [dev(zz, y, x, core) for _, zz in z_peers(z)])
    chip_here = me // TWO
    n_wo, wide = wo_ref.shape[0], wq_ref.shape[1]
    store[chip_here, pl.ds(0, n_wo)] = wo_ref[...]
    for i in range(TWO):
        store[chip_here, pl.ds(n_wo, n_wo), pl.ds(i * wide, wide)] = wq_ref[pl.ds(i * n_wo, n_wo)]
    turn_back(dkv_ref, cos_ref, sin_ref, dk_u, dv_u)
    all_here()
    wkv = PairSum(me, "core", 1, wkv_ref, wkv_store.at[chip_here], buffers, [r.at[0] for r in sems])

    def place_of(key):
        dz, ry, rx = key
        return z + dz, 1 - y if ry else y, 1 - x if rx else x

    def block(part, key):
        zz, yy, xx = place_of(key)
        chip = (TWO * zz + yy) * TWO + xx
        return wkv_store.at[chip] if part == THREE else store.at[chip, pl.ds(CUTS[part], CUTS[part + 1] - CUTS[part])]

    def windows(part, key):
        zz, yy, xx = place_of(key)
        pair, src = TWO * zz + yy, block(part, key)
        wo_at, wq_at = ((xx * TWO + core) * N_PAIRS + pair) * n_wo, (core * N_PAIRS + pair) * wq_ref.shape[0]
        if part == THREE:
            for i, out in enumerate(outs[TWO:]):
                yield src.at[:, head(i)], out.at[pl.ds(wq_at, wq_ref.shape[0]), pl.ds(xx * HEAD_DIM, HEAD_DIM)]
            return
        first, last = CUTS[part : part + TWO]
        if first < n_wo:
            rows = min(last, n_wo) - first
            yield src.at[pl.ds(0, rows)], outs[0].at[pl.ds(wo_at + first, rows)]
        if last > n_wo:
            skip = max(n_wo - first, 0)
            rows, at = last - first - skip, first + skip - n_wo
            for i in range(TWO):
                window = outs[1].at[pl.ds(wq_at + i * n_wo + at, rows), pl.ds(xx * wide, wide)]
                yield src.at[pl.ds(skip, rows), pl.ds(i * wide, wide)], window

    def index(part, key):
        return (part, key[0] + THREE) + key[1:]

    def send(part, key, link, there):
        sent = send_sem.at[index(part, key) + (LINKS.find(link or "-") + 1,)]
        if link:
            remote(block(part, key), block(part, key), sent, come_sem.at[index(part, there)], to[link]).start()
            return
        for src, window in windows(part, key):
            remote(src, window, sent, core_sem.at[index(part, key)], partner).start()
            pltpu.make_async_copy(src, window, put_sem.at[index(part, key)]).start()

    def whole(part, send, arrive):
        size = CUTS[part + 1] - CUTS[part] if part < THREE else wkv_store.size // store.shape[0] // outs[0].shape[1]
        dst = outs[0].at[pl.ds(0, size)]
        return remote(dst, dst, send, arrive, me)

    def when(on, do):
        pl.when(on)(do)

    def each_way(part, key):
        held = line.held(key[0])
        yield None, key, held
        for link, there in onward(ORDERS[part], key):
            inside = {"u": line.inside[1], "d": line.inside[-1]}.get(link)
            yield link, there, held if inside is None else jnp.logical_and(held, inside)

    def pass_on(part, key):
        for link, there, on in each_way(part, key):
            when(on, functools.partial(send, part, key, link, there))

    def term_copy(i):
        src = terms if i == 0 else totals.at[i - 1]
        return remote(src, all_terms.at[i], g_s.at[i], g_r.at[i], me ^ (1 << i))

    def add_terms(i):
        term_copy(i).wait_recv()
        totals[i] = (terms[...] if i == 0 else totals[i - 1]) + all_terms[i]
        if i + 1 < len(GAIN_AT):
            term_copy(i + 1).start()

    def tile(t):
        job.tile(t)
        if t == job.tiles - 1:
            term_copy(0).start()

    def sum_step(h):
        wkv.step(0, h)

    steps = [(TILES_FROM + t * TILE_EVERY, functools.partial(tile, t)) for t in range(HiddenGradient.tiles)]
    steps += [(at, functools.partial(sum_step, h)) for h, at in enumerate(SUM_AT)]
    steps += [(at, functools.partial(add_terms, i)) for i, at in enumerate(GAIN_AT)]
    steps.sort(key=lambda s: s[0])
    events = arrivals()
    for part in range(THREE):
        pass_on(part, HERE)
    job = HiddenGradient(me, dk_u, dv_u, grad_ins, (dx_ref, terms), refs)
    wkv_terms(h_ref, h_buf, h_sem, dk_u, dv_u, ((wkv_ref, 1 - core), (buffers[0], core)))
    wkv.begin(0)
    wkv.loaded(0)
    for now, part, key in events:
        while steps and steps[0][0] <= now:
            steps.pop(0)[1]()
        if any(key):
            arrive = come_sem.at[index(part, key)]
            when(line.held(key[0]), whole(part, own_sem.at[0], arrive).wait_recv)
            pass_on(part, key)
        elif part == THREE:
            pass_on(part, key)
    dgain_ref[...] = totals[len(GAIN_AT) - 1]
    for i in range(len(GAIN_AT)):
        term_copy(i).wait_send()
    for _, part, key in events:
        for sem in (core_sem, put_sem):
            when(line.held(key[0]), whole(part, own_sem.at[0], sem.at[index(part, key)]).wait_recv)
        for link, there, on in each_way(part, key):
            sent = send_sem.at[index(part, key) + (LINKS.find(link or "-") + 1,)]
            when(on, whole(part, sent, own_sem.at[0]).wait_send)
    wkv.wait_send(0)
    job.finish()


def gather_all(wo, wq, dkv, cos_f, sin_f, h_u, part, w_k, w_v, x, dy, gain, shapes):
    dma = pltpu.SemaphoreType.DMA
    vmem, hbm = pl.BlockSpec(memory_space=pltpu.VMEM), pl.BlockSpec(memory_space=pl.ANY)
    block = w_k.shape[0] // TWO // N_PAIRS, w_k.shape[1]
    parts = len(ORDERS)
    keys = (parts, 7, TWO, TWO)
    terms = 1, x.shape[1]
    scratch = [dma((1,)), dma(keys + (len(LINKS) + 1,)), dma(keys), dma(keys), dma(keys)]
    n = len(GAIN_AT)
    scratch += [pltpu.VMEM((n,) + terms, F32)] * TWO + [dma((n,)), dma((n,)), pltpu.VMEM(terms, F32)]
    scratch += [pltpu.VMEM((FOUR, TWO) + block, F32), pltpu.VMEM((TWO, TWO, TWO, BLK, BLK), BF16), dma((TWO,))]
    scratch += [pltpu.VMEM((TWO, TWO, BLK, HEAD_DIM), BF16)] * TWO
    scratch += [pltpu.VMEM((TWO * N_PAIRS,) + b, F32) for b in ((TWO * wo.shape[0], wo.shape[1]), block)]
    return pl.pallas_call(
        gather_kernel,
        name="gather_all",
        out_shape=[jax.ShapeDtypeStruct(s, F32) for s in shapes]
        + [jax.ShapeDtypeStruct(x.shape, BF16), jax.ShapeDtypeStruct(terms, F32)],
        in_specs=[vmem] * 5 + [hbm] * 6 + [vmem],
        out_specs=[hbm] * (len(shapes) + 1) + [vmem],
        scratch_shapes=scratch + PairSum.scratch("core", block) + PairSum.sems(1, 1) + HiddenGradient.scratch(x),
        compiler_params=params(63, collective_id=0),
        cost_estimate=cost(1, 76),
    )(wo, wq, dkv, cos_f, sin_f, h_u, part, w_k, w_v, x, dy, gain)


def perm(x, pairs):
    return lax.ppermute(x, "cp", pairs)


def flip_pairs(d):
    return [(r, r ^ d) for r in range(32)]


def solution(mesh):
    def local_step(hidden, grad_out, positions, seg_ids, w_q, w_k, w_v, w_o, norm_gain):
        n_batch, n_tok, d_model = hidden.shape
        n_rows = n_batch * n_tok
        wide = N_HEADS * HEAD_DIM
        me = lax.axis_index("cp")
        z, y, x, core = place(me)
        quad, pair = me % FOUR, me // FOUR
        relations = range(FOUR)

        def swap(pieces):
            return [perm(p, flip_pairs(d)) if d else p for d, p in enumerate(pieces)]

        gain = norm_gain.astype(F32)
        cos_t, sin_t = rope_tables(positions.reshape(n_rows))
        cos_f, sin_f = jnp.hstack([cos_t, cos_t]), jnp.hstack([-sin_t, sin_t])
        dy_flat = grad_out.reshape(n_rows, d_model)
        normed, kv_home = project(hidden.reshape(n_rows, d_model), gain[NEW], w_k, w_v, cos_f, sin_f)
        pos = positions.reshape(TWO, TWO, n_tok)
        kv_home = kv_home.reshape((TWO,) * 5 + (CHUNK, HEAD_DIM))
        kv_all, q_u, do_u, pos_u, *dy_rows = exchange(kv_home, normed, dy_flat, pos, cos_f, sin_f, w_q, w_o)
        pos_u = pos_u.reshape((FOUR, TWO, TWO, CHUNK)).transpose(1, TWO, 0, THREE).reshape(TWO, TWO, BLK)
        dy_rows = [a.reshape(TWO, TWO, CHUNK, d_model) for a in dy_rows]
        dy_pieces = swap([dy_rows[d % TWO] for d in relations])

        member = quad ^ jnp.arange(FOUR)
        front, back = ((m[:, NEW] * CHUNK + jnp.arange(CHUNK)[NEW]).reshape(BLK) for m in (member, THREE - member))
        offsets = jnp.stack([front, back]).astype(jnp.int32)
        own_super = jnp.stack([pair, N_SUPER - 1 - pair]).astype(jnp.int32)
        q_index = own_super[:, NEW] * BLK + offsets
        start = q_index[NEW] - pos_u
        tab = jnp.concatenate(
            [own_super, (jnp.min(start, axis=-1) // BLK).reshape(-1), jnp.max(start, axis=-1).reshape(-1)]
        )
        start_r = start[:, :, NEW, :]
        index_r = q_index[:, NEW]
        cos_u, sin_u = rope_tables(pos_u)
        cos_ut, sin_ut = jnp.swapaxes(cos_u, TWO, THREE), jnp.swapaxes(sin_u, TWO, THREE)

        attn_u, lse = flash_fwd(tab, q_u, kv_all, start_r, index_r)

        wo_keep, wo_away = wo_terms(attn_u, dy_pieces)
        wo_come = perm(wo_away, flip_pairs(FOUR))
        do_u, wo_keep = lax.optimization_barrier((do_u, wo_keep))
        dq_u, dkv = flash_bwd(tab, q_u, do_u, attn_u, kv_all, lse, start_r, index_r, cos_ut, sin_ut)

        x_flat = hidden.reshape(n_rows, d_model)
        wo_own, dkv_own, wq_own, block_out, d_part, h_u = reduce_pairs(
            [wo_keep, wo_come, dkv.reshape(FOUR, TWO, -1, HEAD_DIM)],
            [wo_keep.shape[1:], (dkv.size // N_PAIRS // HEAD_DIM, HEAD_DIM), (d_model // TWO // N_PAIRS, wide)],
            (TWO, 8, 8),
            ("z", "", "core"),
            TWO,
            Products,
            (attn_u, dq_u, x_flat, normed.reshape((TWO,) * THREE + (CHUNK, d_model)), w_o, w_q),
        )
        grad_wo, grad_wq, grad_wk, grad_wv, grad_x, d_gain = gather_all(
            wo_own,
            wq_own,
            dkv_own,
            cos_ut,
            sin_ut,
            h_u,
            d_part,
            w_k,
            w_v,
            x_flat,
            dy_flat,
            gain[NEW],
            [w_o.shape, w_q.shape, w_k.shape, w_v.shape],
        )
        block_out, grad_x = (a.reshape(hidden.shape) for a in (block_out, grad_x))
        return block_out, grad_x, grad_wq, grad_wk, grad_wv, grad_wo, d_gain.reshape(d_model)

    seq_spec = P(None, "cp", None)
    tok_spec = P(None, "cp")
    full_spec = P()
    return jax.shard_map(
        local_step,
        mesh=mesh,
        in_specs=(seq_spec, seq_spec, tok_spec, tok_spec, full_spec, full_spec, full_spec, full_spec, full_spec),
        out_specs=(seq_spec, seq_spec, full_spec, full_spec, full_spec, full_spec, full_spec),
        check_vma=False,
    )
```

```python
import functools
import heapq
import itertools

import jax
import jax.numpy as jnp
from jax import lax
from jax.experimental import pallas as pl
from jax.experimental.pallas import tpu as pltpu
from jax.sharding import PartitionSpec as P

HEAD_DIM = 128
NORM_EPS = 1e-5
ROPE_BASE = 500000.0
NEG_BIG = -1e30
LOG2E = 1.4426950408889634
ATTN_SCALE = HEAD_DIM**-0.5
EXP2_SCALE = ATTN_SCALE * LOG2E
CHUNK = 64
TWO = 2
THREE = 3
FOUR = 4
NEW = jnp.newaxis
BLK = 4 * CHUNK
N_HEADS = 8
N_PAIRS = 8
N_SUPER = 2 * N_PAIRS
MESH = pl.DeviceIdType.MESH
ONE = pl.Squeezed()
GROUP = 4
DIRECT = 2
MADE_AT = 5
PRODUCTS_AT = 7, 9
F32 = jnp.float32
BF16 = jnp.bfloat16

T_SQ, T_LO, T_MX = 0, 2, 6


def rope_tables(positions):
    inv_freq = ROPE_BASE ** (-jnp.arange(0, HEAD_DIM, TWO).astype(F32) / HEAD_DIM)
    angles = positions.astype(F32)[..., None] * inv_freq
    return jnp.cos(angles), jnp.sin(angles)


def dot(a, b, ca, cb):
    return lax.dot_general(a, b, ((ca, cb), ((), ())), preferred_element_type=F32)


def cost(gflop, mib):
    return pl.CostEstimate(flops=gflop * 10**9, bytes_accessed=mib << 20, transcendentals=0)


def params(mib, **more):
    return pltpu.CompilerParams(vmem_limit_bytes=mib << 20, **more)


def row_mean(x):
    return jnp.mean(x, axis=-1, keepdims=True)


def head(h):
    return pl.ds(h * HEAD_DIM, HEAD_DIM)


def head_slice(h):
    return slice(h * HEAD_DIM, (h + 1) * HEAD_DIM)


def dot_t(a, b):
    return dot(a, b, (1,), (1,))


def steps(tab, body):
    b, hf = pl.program_id(0), pl.program_id(1)
    own, first, last_start = tab[T_SQ + hf], tab[T_LO + TWO * b + hf], tab[T_MX + TWO * b + hf]

    def place_of(s):
        late = s >= N_PAIRS
        return jnp.where(late, N_SUPER - 1 - s, s), late.astype(jnp.int32)

    full_from = jnp.minimum((last_start + BLK - 1) // BLK, own)
    full_from += lax.rem(own - full_from, TWO)
    count = full_from - first

    @pl.loop(0, count + 1)
    def _(t):
        s = jnp.where(t < count, first + t, own)
        body(s, place_of(s), True)

    @pl.loop(0, (own - full_from) // TWO)
    def _(t):
        for i in range(TWO):
            s = full_from + TWO * t + i
            body(s, place_of(s), False)


def down(row, n):
    return jnp.broadcast_to(row, (n, row.shape[-1])).T


def offsets_of(tab, qi_ref, hk):
    return qi_ref[hk] - tab[T_SQ + hk] * BLK


def may_use(s, off, start, index):
    return jnp.logical_and(off >= start - s * BLK, off <= index - s * BLK)


def fwd_kernel(tab, q_ref, do_ref, kv_ref, st_ref, qi_ref, o_ref, lse_ref, delta_ref, q_s, acc, m_s, l_s, k_t, bounds):
    m_s[...] = jnp.full_like(m_s, NEG_BIG)
    l_s[...] = jnp.zeros_like(l_s)
    acc[...] = jnp.zeros_like(acc)
    for i, row in enumerate((st_ref[...], qi_ref[pl.program_id(1)])):
        bounds[i] = down(row, HEAD_DIM)
    for h in range(N_HEADS):
        q_s[pl.ds(h * BLK, BLK)] = q_ref[:, head(h)]

    @pl.when(pl.program_id(1) == 0)
    def _():
        @pl.loop(0, N_PAIRS)
        def _(pair):
            for hk in range(TWO):
                k_t[pair, hk] = kv_ref[pair, 0, hk].T

    def body(s, at, masked):
        pair, hk = at
        v = kv_ref[pair, 1, hk]
        if masked:
            off = offsets_of(tab, qi_ref, hk) + s * BLK
            mask = [
                jnp.logical_and(off[:, lanes] >= bounds[0], off[:, lanes] <= bounds[1])
                for lanes in (slice(HEAD_DIM), slice(HEAD_DIM, BLK))
            ]
            mask = [jnp.concatenate([m, m], axis=0) for m in mask]
        for g in range(N_HEADS // TWO):
            rows = pl.ds(g * TWO * BLK, TWO * BLK)
            sc = jnp.dot(q_s[rows], k_t[pair, hk], preferred_element_type=F32)
            sc = [sc[:, :HEAD_DIM], sc[:, HEAD_DIM:]]
            if masked:
                sc = [jnp.where(m, x, NEG_BIG) for m, x in zip(mask, sc)]
            m_old = m_s[rows]
            m_new = jnp.maximum(m_old, jnp.max(jnp.maximum(*sc), axis=1, keepdims=True))
            alpha = jnp.exp2((m_old - m_new) * EXP2_SCALE)
            p = [jnp.exp2((x - m_new) * EXP2_SCALE) for x in sc]
            m_s[rows] = m_new
            l_s[rows] = l_s[rows] * alpha + (p[0] + p[1])
            p = jnp.hstack([x.astype(BF16) for x in p])
            acc[rows] = acc[rows] * alpha + jnp.dot(p, v, preferred_element_type=F32)

    steps(tab, body)
    for h in range(N_HEADS):
        rows = pl.ds(h * BLK, BLK)
        total = jnp.sum(l_s[rows], axis=1, keepdims=True)
        o = (acc[rows] / total).astype(BF16)
        o_ref[:, head(h)] = o
        lse = m_s[rows] * EXP2_SCALE + jnp.log2(total)
        delta = jnp.sum(o.astype(F32) * do_ref[:, head(h)].astype(F32), axis=1, keepdims=True)
        both = jnp.where(lax.broadcasted_iota(jnp.int32, lse.shape, 1) == 0, lse, delta).T
        lse_ref[h], delta_ref[h] = both[:1], both[1:TWO]


def bwd_kernel(tab, q_ref, do_ref, kv_ref, lse_ref, delta, st_ref, qi_ref, cos_ref, sin_ref, dq_ref, dkv_ref, *scratch):
    dq_acc, off_s, q_s, do_s, q_t, do_t, p_s, ds_s = scratch
    dq_acc[...] = jnp.zeros_like(dq_acc)
    for h in range(N_HEADS):
        q, do = q_ref[:, head(h)], do_ref[:, head(h)]
        q_s[pl.ds(h * BLK, BLK)], do_s[pl.ds(h * BLK, BLK)] = q, do
        q_t[h], do_t[h] = q.T, do.T

    @pl.when(pl.program_id(1) == 0)
    def _():
        dkv_ref[...] = jnp.zeros_like(dkv_ref)
        for hk in range(TWO):
            off_s[hk] = down(offsets_of(tab, qi_ref, hk), BLK)

    def body(s, at, masked):
        pair, hk = at
        k = kv_ref[pair, 0, hk]
        v = kv_ref[pair, 1, hk]
        k_t = k.T
        mask = may_use(s, off_s[hk], st_ref[...], qi_ref[pl.program_id(1)]) if masked else None
        for first in range(0, N_HEADS, GROUP):
            rows = pl.ds(first * BLK, GROUP * BLK)
            for h in range(first, first + GROUP):
                cols = pl.ds(h * BLK, BLK)
                p = jnp.exp2(jnp.dot(k, q_t[h], preferred_element_type=F32) * EXP2_SCALE - lse_ref[h])
                if masked:
                    p = jnp.where(mask, p, 0.0)
                ds = p * (jnp.dot(v, do_t[h], preferred_element_type=F32) - delta[h])
                p_s[:, cols] = p.astype(BF16)
                ds_s[:, cols] = ds.astype(BF16)
            dkv_ref[pair, 0, hk] += jnp.dot(ds_s[:, rows], q_s[rows], preferred_element_type=F32)
            dkv_ref[pair, 1, hk] += jnp.dot(p_s[:, rows], do_s[rows], preferred_element_type=F32)
            dq_acc[:, rows] += jnp.dot(k_t, ds_s[:, rows], preferred_element_type=F32)

    steps(tab, body)
    cos_t, sin_t = cos_ref[...], sin_ref[...]
    half = HEAD_DIM // TWO
    for h in range(N_HEADS):
        cols = pl.ds(h * BLK, BLK)
        a, c = dq_acc[:half, cols] * ATTN_SCALE, dq_acc[half:, cols] * ATTN_SCALE
        lin = jnp.concatenate([a * cos_t + c * sin_t, c * cos_t - a * sin_t], axis=0)
        dq_ref[:, head(h)] = lin.T.astype(BF16)


def attn_specs():
    def at_tile(b, h, t):
        return (b, h) + (0,) * TWO

    def at_row(b, h, t):
        return (0, 0, b) + (0,) * THREE

    tile = pl.BlockSpec((ONE, ONE, BLK, N_HEADS * HEAD_DIM), at_tile)
    row = pl.BlockSpec((ONE, ONE, 1, BLK), at_tile)
    stat = pl.BlockSpec((ONE, ONE, N_HEADS, 1, BLK), lambda b, h, t: (b, h) + (0,) * THREE)
    rope = pl.BlockSpec((ONE, ONE, HEAD_DIM // TWO, BLK), at_tile)
    kv = pl.BlockSpec((N_PAIRS, TWO, ONE, TWO, BLK, HEAD_DIM), at_row)
    ko = pl.BlockSpec((TWO, 1, BLK), lambda b, h, t: (0,) * THREE)
    return tile, row, stat, kv, ko, rope


def flash_fwd(tab, q, do, kv, start, index):
    tile, row, stat, kvs, ko, _ = attn_specs()
    return pl.pallas_call(
        fwd_kernel,
        name="attn_fwd",
        out_shape=[jax.ShapeDtypeStruct(q.shape, BF16)] + [jax.ShapeDtypeStruct((TWO, TWO, N_HEADS, 1, BLK), F32)] * TWO,
        grid_spec=pltpu.PrefetchScalarGridSpec(
            num_scalar_prefetch=1,
            grid=(TWO, TWO),
            in_specs=[tile, tile, kvs, row, ko],
            out_specs=[tile, stat, stat],
            scratch_shapes=[pltpu.VMEM((N_HEADS * BLK, HEAD_DIM), t) for t in (BF16, F32, F32, F32)]
            + [pltpu.VMEM((N_PAIRS, TWO, HEAD_DIM, BLK), BF16), pltpu.VMEM((TWO, BLK, HEAD_DIM), jnp.int32)],
        ),
        compiler_params=params(63),
        cost_estimate=cost(20, 16),
    )(tab, q, do, kv, start, index)


def flash_bwd(tab, q, do, kv, lse, delta, start, index, cos_t, sin_t):
    tile, row, stat, kvs, ko, rope = attn_specs()
    return pl.pallas_call(
        bwd_kernel,
        name="attn_bwd",
        out_shape=(
            jax.ShapeDtypeStruct(q.shape, BF16),
            jax.ShapeDtypeStruct(kv.shape, F32),
        ),
        grid_spec=pltpu.PrefetchScalarGridSpec(
            num_scalar_prefetch=1,
            grid=(TWO, TWO),
            in_specs=[tile, tile, kvs, stat, stat, row, ko, rope, rope],
            out_specs=[tile, kvs],
            scratch_shapes=[pltpu.VMEM((HEAD_DIM, N_HEADS * BLK), F32)]
            + [pltpu.VMEM((TWO, BLK, BLK), jnp.int32)]
            + [pltpu.VMEM((N_HEADS * BLK, HEAD_DIM), BF16)] * TWO
            + [pltpu.VMEM((N_HEADS, HEAD_DIM, BLK), BF16)] * TWO
            + [pltpu.VMEM((BLK, N_HEADS * BLK), BF16)] * TWO,
        ),
        compiler_params=params(63),
        cost_estimate=cost(50, 32),
    )(tab, q, do, kv, lse, delta, start, index, cos_t, sin_t)


def turn(x, cos_ref, sin_ref):
    return x * cos_ref[...] + pltpu.roll(x, HEAD_DIM // TWO, 1) * sin_ref[...]


def first_kernel(x_ref, g_ref, wk_ref, wv_ref, cos_ref, sin_ref, h_ref, kv_ref):
    x = x_ref[...].astype(F32)
    h = (x * lax.rsqrt(row_mean(x * x) + NORM_EPS) * g_ref[...]).astype(BF16)
    h_ref[...] = h
    k = jnp.dot(h, wk_ref[...], preferred_element_type=F32)
    v = jnp.dot(h, wv_ref[...], preferred_element_type=F32)
    n = kv_ref.shape[THREE]
    for i in range(TWO):
        for j, val in enumerate((turn(k[:, head_slice(i)], cos_ref, sin_ref), v[:, head_slice(i)])):
            for c in range(TWO):
                kv_ref[i, c, j] = val[c * n : (c + 1) * n].astype(BF16)


def project(x, gain, w_k, w_v, cos_f, sin_f):
    n = x.shape[0] // TWO
    return pl.pallas_call(
        first_kernel,
        name="norm_kv",
        out_shape=(jax.ShapeDtypeStruct(x.shape, BF16), jax.ShapeDtypeStruct((TWO,) * THREE + (n, HEAD_DIM), BF16)),
        compiler_params=params(63),
        cost_estimate=cost(TWO, 7),
    )(x, gain, w_k, w_v, cos_f, sin_f)


def place(me):
    return me // 8, lax.rem(me // FOUR, TWO), lax.rem(me // TWO, TWO), lax.rem(me, TWO)


def dev(z, y, x, core):
    return ((z * TWO + y) * TWO + x) * TWO + core


def z_peers(z):
    return [(k, lax.rem(z + k, FOUR)) for k in (1, TWO, THREE)]


def announce(peers):
    barrier = pltpu.get_barrier_semaphore()
    for d in peers:
        pl.semaphore_signal(barrier, device_id=(d,), device_id_type=MESH)
    return lambda: pl.semaphore_wait(barrier, len(peers))


def meet(peers):
    announce(peers)()


def remote(src, dst, send, arrive, to):
    return pltpu.make_async_remote_copy(
        src_ref=src, dst_ref=dst, send_sem=send, recv_sem=arrive, device_id=(to,), device_id_type=MESH
    )


class Line:
    order = (0, 1, -1, TWO, -TWO, THREE, -THREE)

    def __init__(self, me):
        self.z, y, x, core = place(me)
        self.next = {1: dev(self.z + 1, y, x, core), -1: dev(self.z - 1, y, x, core)}
        self.inside = {1: self.z < THREE, -1: self.z > 0}

    def held(self, dz):
        return jnp.logical_and(self.z + dz >= 0, self.z + dz <= THREE)

    def ways(self, dz):
        for d in self.next:
            if d * dz <= 0:
                yield d, self.inside[d] if dz == 0 else jnp.logical_and(self.inside[d], self.held(dz))


def tiled(n, fetch, use, first=0):
    fetch(first, 0).start()

    @pl.loop(0, n)
    def _(t):
        slot = lax.rem(t, TWO)
        fetch(first + t, slot).wait()

        @pl.when(t + 1 < n)
        def _():
            fetch(first + t + 1, 1 - slot).start()

        use(first + t, slot)


def aligned(t, size=BLK):
    return pl.ds(pl.multiple_of(t * size, size), size)


def exchange_kernel(*refs):
    take = taker(refs)
    kv_ref, h_ref, dy_ref, pos_ref, cos_ref, sin_ref, wq_ref, wo_ref, kv_all, q_u, do_u, pos_u, *dy_rows = take(14)
    own_sem, quad_s, quad_r, z_s, z_r, y_s, y_r, q_home, do_home, wq_buf, wo_buf, w_sem, dy_sem, h_own, dy_own = take(len(refs))
    me = lax.axis_index("cp")
    z, y, x, core = place(me)
    quad, line = quad_of(me), Line(me)
    across = dev(z, 1 - y, x, core)
    loads = [pltpu.make_async_copy(a, b, dy_sem.at[i]) for i, (a, b) in enumerate(((h_ref, h_own), (dy_ref, dy_own)))]
    for c in loads:
        c.start()
    meet(quad[1:] + [across] + [dev(zz, y, x, core) for _, zz in z_peers(z)])

    def source(a, d):
        xx, cc = 1 - x if d // TWO else x, 1 - core if d % TWO else core
        return pos_ref.at[cc] if a == THREE else (kv_ref, q_home, do_home)[a].at[xx, cc]

    def target(a, d):
        if a == THREE:
            return pos_u.at[d]
        tok = pl.ds(d * CHUNK, CHUNK)
        return kv_all.at[me // FOUR, :, :, :, tok] if a == 0 else (q_u, do_u)[a - 1].at[:, :, tok]

    def quad_copy(a, d):
        return remote(source(a, d), target(a, d), quad_s.at[a, d], quad_r.at[a, d], quad[d])

    def own_copy(a):
        return pltpu.make_async_copy(source(a, 0), target(a, 0), own_sem.at[a])

    def z_copy(part, dz, d):
        block = kv_all.at[TWO * (z + dz) + y, part]
        return remote(block, block, z_s.at[part, (d + 1) // TWO, dz + THREE], z_r.at[part, dz - d + THREE], line.next[d])

    def y_copy(part, dz, yy=y):
        block = kv_all.at[TWO * (z + dz) + yy, part]
        return remote(block, block, y_s.at[part, dz + THREE], y_r.at[part, dz + THREE], across)

    parts = range(TWO)
    moves = [(part, dz) for dz in line.order for part in parts]

    def pass_on(count):
        for part, dz in [moves.pop(0) for _ in range(count)]:
            if dz:
                block = kv_all.at[TWO * (z + dz) + y, part]
                arrival = remote(block, block, own_sem.at[0], z_r.at[part, dz + THREE], me)
                pl.when(line.held(dz))(arrival.wait_recv)
            for d, on in line.ways(dz):
                pl.when(on)(z_copy(part, dz, d).start)
            pl.when(line.held(dz))(y_copy(part, dz).start)

    n = h_ref.shape[1] // BLK // TWO

    def fetch_q(t, slot):
        return pltpu.make_async_copy(wq_ref.at[:, aligned(t)], wq_buf.at[slot], w_sem.at[0, slot])

    def fetch_o(t, slot):
        return pltpu.make_async_copy(wo_ref.at[aligned(t)], wo_buf.at[slot], w_sem.at[1, slot])

    def put(home, t, val):
        home[t // n, :, :, :, :, aligned(lax.rem(t, n))] = val.astype(BF16).reshape(home.shape[1:-1] + (BLK,))

    def query(t, slot):
        q = jnp.dot(h_own[...], wq_buf[slot], preferred_element_type=F32)
        put(q_home, t, jnp.hstack([turn(q[:, head_slice(j)], cos_ref, sin_ref) for j in range(BLK // HEAD_DIM)]))

    def pull(t, slot):
        put(do_home, t, dot_t(dy_own[...], wo_buf[slot]))

    all_moves = list(moves)
    half = dy_own.shape[0] // TWO

    def dy_copy(i):
        return pltpu.make_async_copy(dy_own.at[aligned(1 - core if i else core, half)], dy_rows[i], dy_sem.at[i])

    for a in (0, THREE):
        for d in (1, TWO, THREE):
            quad_copy(a, d).start()
        own_copy(a).start()
    loads[0].wait()
    for a, (fetch, use) in enumerate(((fetch_q, query), (fetch_o, pull)), 1):
        for near in range(TWO):
            tiled(n, fetch, use, n * (x if near else 1 - x))
            for d in range(TWO):
                if d or not near:
                    quad_copy(a, d if near else d + TWO).start()
            if near:
                own_copy(a).start()
            if len(moves) == len(all_moves):
                loads[1].wait()
                for i in range(TWO):
                    dy_copy(i).start()
                own_copy(0).wait()
                for d in (1, TWO, THREE):
                    quad_copy(0, d).wait_recv()
            pass_on(TWO)
    pass_on(len(moves))
    for part, dz in all_moves:
        for d, on in line.ways(dz):
            pl.when(on)(z_copy(part, dz, d).wait_send)
        pl.when(line.held(dz))(y_copy(part, dz, 1 - y).wait_recv)
        pl.when(line.held(dz))(y_copy(part, dz).wait_send)
    for a in range(FOUR):
        for d in (1, TWO, THREE):
            quad_copy(a, d).wait_send()
            if a > 0:
                quad_copy(a, d).wait_recv()
    for a in (1, TWO, THREE):
        own_copy(a).wait()
    for i in range(TWO):
        dy_copy(i).wait()


def exchange(kv, h, dy, pos, cos_f, sin_f, w_q, w_o):
    dma = pltpu.SemaphoreType.DMA
    vmem, hbm = pl.BlockSpec(memory_space=pltpu.VMEM), pl.BlockSpec(memory_space=pl.ANY)
    wide = w_q.shape[1] // TWO
    unit = jax.ShapeDtypeStruct((TWO, TWO, BLK, wide), BF16)
    pos_quad = jax.ShapeDtypeStruct((FOUR,) + pos.shape[1:], pos.dtype)
    dy_half = jax.ShapeDtypeStruct((dy.shape[0] // TWO, dy.shape[1]), BF16)
    home = pltpu.VMEM((TWO,) * FOUR + (CHUNK, wide), BF16)
    sems = [dma((FOUR,))] + [dma((FOUR, FOUR))] * TWO + [dma((TWO, TWO, 7))] + [dma((TWO, 7))] * THREE
    bufs = [pltpu.VMEM((TWO,) + b, BF16) for b in ((w_q.shape[0], BLK), (BLK, w_o.shape[1]))]
    return pl.pallas_call(
        exchange_kernel,
        name="exchange",
        out_shape=(jax.ShapeDtypeStruct((N_PAIRS,) + (TWO,) * THREE + (BLK, HEAD_DIM), BF16), unit, unit, pos_quad, dy_half, dy_half),
        in_specs=[vmem] + [hbm] * THREE + [vmem] * TWO + [hbm] * TWO,
        out_specs=[hbm] * 6,
        scratch_shapes=sems + [home, home] + bufs + [dma((TWO, TWO)), dma((TWO,))] + [pltpu.VMEM(h.shape, BF16)] * TWO,
        compiler_params=params(63, collective_id=1),
        cost_estimate=cost(1, 20),
    )(kv, h, dy, pos, cos_f, sin_f, w_q, w_o)


def taker(refs):
    rest = iter(refs)
    return lambda count: list(itertools.islice(rest, count))


def wo_kernel(*refs):
    take = taker(refs)
    o_ref, *pieces = take(5)
    keep_ref, away_ref, dy_u, o_t, terms, came, load_sem, core_s, core_r, keep, away, out_sem = take(len(refs))
    me = lax.axis_index("cp")
    _, y, _, core = place(me)
    all_here = announce(quad_of(me)[1:TWO])
    loads = [
        pltpu.make_async_copy(src, dy_u.at[:, :, pl.ds(d * CHUNK, CHUNK)], load_sem.at[d])
        for d, src in enumerate(pieces)
    ]
    for c in loads:
        c.start()
    for h in range(N_HEADS):
        o_t[head(h)] = o_ref[:, :, :, head(h)].reshape(-1, HEAD_DIM).T
    for c in loads:
        c.wait()
    all_here()
    half, tiles = terms.shape[1], terms.shape[TWO] // BLK

    def swap(t):
        return remote(terms.at[0, :, aligned(t)], came.at[:, aligned(t)], core_s.at[t], core_r.at[t], quad_of(me)[1])

    def half_terms(i, to, then):
        @pl.loop(0, tiles)
        def _(t):
            dy = dy_u[:, :, :, aligned(t)].reshape(-1, BLK)
            terms[to, :, aligned(t)] = jnp.dot(o_t[aligned(i, half)], dy, preferred_element_type=F32)
            then(t)

    half_terms(1 - core, 0, lambda t: swap(t).start())
    half_terms(core, 1, lambda t: swap(t).wait_recv())
    rows = keep.shape[1]

    def results(zz):
        pairs = (keep, keep_ref), (away, away_ref)
        return [pltpu.make_async_copy(a.at[zz], b.at[zz], out_sem.at[i, zz]) for i, (a, b) in enumerate(pairs)]

    for zz in range(FOUR):
        for out, yy in ((keep, y), (away, 1 - y)):
            at = aligned(TWO * zz + yy, rows)
            out[zz] = terms[1, at] + came[at]
        for c in results(zz):
            c.start()
    for zz in range(FOUR):
        for c in results(zz):
            c.wait()
    for t in range(tiles):
        swap(t).wait_send()


def wo_terms(o, pieces):
    dma = pltpu.SemaphoreType.DMA
    vmem, hbm = pl.BlockSpec(memory_space=pltpu.VMEM), pl.BlockSpec(memory_space=pl.ANY)
    n, d, wide = o.shape[0] * o.shape[1] * o.shape[TWO], pieces[0].shape[-1], o.shape[-1]
    half = wide // TWO
    return pl.pallas_call(
        wo_kernel,
        name="wo_terms",
        out_shape=[jax.ShapeDtypeStruct((FOUR, half // N_PAIRS, d), F32)] * TWO,
        in_specs=[vmem] + [hbm] * FOUR,
        out_specs=[hbm] * TWO,
        scratch_shapes=[pltpu.VMEM((TWO, TWO, BLK, d), BF16), pltpu.VMEM((wide, n), BF16)]
        + [pltpu.VMEM((TWO, half, d), F32), pltpu.VMEM((half, d), F32), dma((FOUR,)), dma((d // BLK,)), dma((d // BLK,))]
        + [pltpu.VMEM((FOUR, half // N_PAIRS, d), F32)] * TWO
        + [dma((TWO, FOUR))],
        compiler_params=params(63, collective_id=THREE),
        cost_estimate=cost(FOUR, 20),
    )(o, *pieces)


class PairSum:
    def __init__(self, me, kind, cut, src, out, buffers, sems, direct=0):
        self.me, self.kind, self.src, self.out = me, kind, src, out
        self.direct_from = cut - direct
        self.size = out.shape[0] // cut
        self.own, self.from_core, self.from_y, self.from_z = buffers
        self.load_sem, self.core_s, self.core_r, self.y_s, self.y_r, self.z_s, self.z_r = sems
        self.z, self.y, x, core = place(me)
        self.partner = dev(self.z, self.y, x, 1 - core)
        self.line = [(k, zz, dev(zz, self.y, x, core)) for k, zz in z_peers(self.z)]
        self.across = dev(self.z, 1 - self.y, x, core)
        self.next_z = dev(self.z + 1, self.y, x, core), dev(self.z - 1, self.y, x, core)

    def rows(self, j):
        return pl.ds(j * self.size, self.size)

    def mine(self, j, zz):
        at = self.rows(j)
        return self.own.at[zz, self.y, at] if self.kind == "core" else self.own.at[zz, at]

    def loads(self, j):
        at = self.rows(j)
        if self.kind == "z":
            pairs = zip(self.src, (self.own, self.from_y))
            return [pltpu.make_async_copy(a.at[:, at], b.at[:, at], s.at[j]) for (a, b), s in zip(pairs, (self.load_sem, self.y_r))]
        return [pltpu.make_async_copy(self.src.at[:, self.y, at], self.own.at[:, at], self.load_sem.at[j])]

    def core_copy(self, j):
        src, dst = (r.at[:, :, self.rows(j)] for r in (self.src, self.from_core))
        return remote(src, dst, self.core_s.at[j], self.core_r.at[j], self.partner)

    def y_copy(self, j):
        src = self.own if self.kind == "core" else self.src
        at = self.rows(j)
        return remote(src.at[:, 1 - self.y, at], self.from_y.at[:, at], self.y_s.at[j], self.y_r.at[j], self.across)

    def z_copy(self, j, way, zz, to):
        at = way, zz + way - 1
        return remote(self.mine(j, zz), self.from_z.at[*at, self.rows(j)], self.z_s.at[j, *at], self.z_r.at[j, *at], to)

    def begin(self, j):
        if self.kind == "core":
            self.core_copy(j).start()
            return
        for c in self.loads(j):
            c.start()
        if not self.kind:
            self.y_copy(j).start()

    def loaded(self, j):
        if self.kind != "core":
            for c in self.loads(j):
                c.wait()
        else:
            self.core_copy(j).wait_recv()
            at = self.rows(j)
            for zz in range(FOUR):
                self.own[zz, :, at] += self.from_core[zz, :, at]
            self.y_copy(j).start()
        if self.kind == "z":
            self.add_y(j)
            self.hop(j, 0)

    def add_y(self, j):
        for zz in range(FOUR):
            self.mine(j, zz)[...] += self.from_y[zz, self.rows(j)]

    def relay(self, j, way, zz, add):
        if add:
            self.z_copy(j, way, zz, self.me).wait_recv()
            self.mine(j, zz)[...] += self.from_z[way, zz + way - 1, self.rows(j)]
        self.z_copy(j, way, zz, self.next_z[way]).start()

    def hop(self, j, h):
        @pl.when(self.z == h)
        def _():
            for zz in range(THREE, h, -1):
                self.relay(j, 0, zz, h > 0)

        @pl.when(self.z == THREE - h)
        def _():
            for zz in range(THREE - h):
                self.relay(j, 1, zz, h > 0)

    def z_direct(self, j):
        for k, zz, to in self.line:
            at, there = (j, 0, k - 1), self.from_z.at[0, k - 1, self.rows(j)]
            yield remote(self.mine(j, zz), there, self.z_s.at[at], self.z_r.at[at], to), there

    def step(self, j, h):
        if j >= self.direct_from and h > 0:
            if h == 1:
                at = self.rows(j)
                self.out[at] = self.mine(j, self.z)[...]
                for c, arrived in self.z_direct(j):
                    c.wait_recv()
                    self.out[at] += arrived[...]
            return
        if h == 0 and self.kind != "z":
            self.y_copy(j).wait_recv()
            self.add_y(j)
            if j < self.direct_from:
                self.hop(j, 0)
            else:
                for c, _ in self.z_direct(j):
                    c.start()
        elif 0 < h < THREE:
            self.hop(j, h)
        elif h == THREE:
            at = self.rows(j)
            self.out[at] = self.mine(j, self.z)[...]
            for way, on in enumerate((self.z > 0, self.z < THREE)):

                @pl.when(on)
                def _(way=way):
                    self.z_copy(j, way, self.z, self.me).wait_recv()
                    self.out[at] += self.from_z[way, self.z + way - 1, at]

    def wait_send(self, j):
        if self.kind == "core":
            self.core_copy(j).wait_send()
        if self.kind != "z":
            self.y_copy(j).wait_send()
        if j >= self.direct_from:
            for c, _ in self.z_direct(j):
                c.wait_send()
            return
        for zz in range(FOUR):
            if zz > 0:
                pl.when(self.z < zz)(self.z_copy(j, 0, zz, self.next_z[0]).wait_send)
            if zz < THREE:
                pl.when(self.z > zz)(self.z_copy(j, 1, zz, self.next_z[1]).wait_send)

    @staticmethod
    def scratch(kind, block):
        unused = pltpu.VMEM((8, HEAD_DIM), F32)
        own = pltpu.VMEM(((FOUR, TWO) if kind == "core" else (FOUR,)) + block, F32)
        from_y = pltpu.VMEM((FOUR,) + block, F32)
        return [own, own if kind == "core" else unused, from_y, pltpu.VMEM((TWO, THREE) + block, F32)]

    @staticmethod
    def sems(*dims):
        dma = pltpu.SemaphoreType.DMA
        return [dma(dims)] * 5 + [dma(dims + (TWO, THREE))] * TWO


def reduce_kernel(cuts, kinds, work, *refs):
    n = len(cuts)

    take = taker(refs)
    ins = [take(TWO) if k == "z" else take(1)[0] for k in kinds[:-1]]
    more_in, outs, more_out, made = take(work.ins), take(n), take(work.outs), take(1)
    buffers, sems = [take(FOUR) for _ in kinds], take(7)
    me = lax.axis_index("cp")
    z, y, x, core = place(me)
    meet(quad_of(me)[1:] + [dev(z, 1 - y, x, core)] + [dev(zz, y, x, core) for _, zz in z_peers(z)])
    job = work(me, more_in, more_out, take(len(refs)))
    inputs = enumerate(zip(kinds, cuts, ins + made, outs, buffers))
    sums = [PairSum(me, *a, [r.at[i] for r in sems], DIRECT if i == n - 1 else 0) for i, a in inputs]
    pieces = [(s, j) for s, cut in zip(sums, cuts) for j in range(cut)]
    early, late = pieces[: -cuts[-1]], pieces[-cuts[-1] :]
    for s, j in early:
        s.begin(j)
    for s, j in early:
        s.loaded(j)
    for t in range(len(pieces) + THREE):
        if t == MADE_AT:
            job.wq_terms(sums[-1].own, made[0])
            for s, j in late:
                s.begin(j)
        if t == MADE_AT + 1:
            for s, j in late:
                s.loaded(j)
        for h in range(FOUR):
            if 0 <= t - h < len(pieces):
                s, j = pieces[t - h]
                s.step(j, h)
        job.step(t)
    for s, j in pieces:
        s.wait_send(j)
    job.finish()


def quad_of(me):
    z, y, x, core = place(me)
    return [dev(z, y, 1 - x if d // TWO else x, 1 - core if d % TWO else core) for d in range(FOUR)]


class Home:
    def __init__(self, me, src, out, own_sem, send, arrive):
        _, _, x, core = place(me)
        w = src.shape[-1]
        to = out.at[core, :, :, :, pl.ds(x * w, w)]

        def piece(d):
            return src.at[:, :, pl.ds(d * CHUNK, CHUNK)]

        self.own = pltpu.make_async_copy(piece(0), to, own_sem)
        self.copies = [remote(piece(d), to, send.at[d], arrive.at[d], quad_of(me)[d]) for d in (1, TWO, THREE)]

    def start(self):
        self.own.start()
        for c in self.copies:
            c.start()

    def wait_recv(self):
        self.own.wait()
        for c in self.copies:
            c.wait_recv()

    def wait_send(self):
        for c in self.copies:
            c.wait_send()


class Products:
    ins, outs = 6, THREE

    def __init__(self, me, ins, outs, scratch):
        attn, self.dq, hidden, normed, self.w_o, self.w_q = ins
        self.out_refs, self.h_u = outs[:TWO], outs[TWO]
        self.block_out, self.d_part, self.attn_home, self.dq_home, self.buf_o, self.buf_q, stage, self.h_buf, *sems = scratch
        self.w_sem, self.load_sem, own_sem, quad_s, quad_r = sems
        _, _, _, core = place(me)

        def piece(d):
            return normed.at[1 - core if d % TWO else core]

        def tokens(d):
            return self.h_u.at[:, :, pl.ds(d * CHUNK, CHUNK)]

        self.h_copies = [remote(piece(d), tokens(d), quad_s.at[TWO, d], quad_r.at[TWO, d], quad_of(me)[d]) for d in (1, TWO, THREE)]
        self.h_mine = pltpu.make_async_copy(piece(0), stage, own_sem.at[TWO])
        self.h_back = pltpu.make_async_copy(stage, tokens(0), self.load_sem.at[0])
        self.residual = pltpu.make_async_copy(hidden, self.block_out, own_sem.at[THREE])
        self.residual.start()
        for c in self.h_copies:
            c.start()
        self.h_mine.start()
        self.homes = [
            Home(me, src, out, own_sem.at[i], quad_s.at[i], quad_r.at[i])
            for i, (src, out) in enumerate([(attn, self.attn_home), (self.dq, self.dq_home)])
        ]
        for h in self.homes:
            h.start()

    @staticmethod
    def scratch(arrays):
        dma, d = pltpu.SemaphoreType.DMA, arrays[-1].shape[0]
        home = pltpu.VMEM((TWO,) * THREE + (CHUNK, d), BF16)
        buf = [pltpu.VMEM((TWO,) + b, BF16) for b in ((d, BLK), (BLK, d))]
        tiles = [pltpu.VMEM((TWO, TWO) + b, BF16) for b in ((CHUNK, d), (TWO, BLK, BLK))]
        sems = [dma((TWO, TWO)), dma((TWO,)), dma((FOUR,)), dma((THREE, FOUR)), dma((THREE, FOUR))]
        products = [pltpu.VMEM(arrays[TWO].shape, t) for t in (BF16, F32)]
        return products + [home] * TWO + buf + tiles + sems

    @staticmethod
    def results(arrays):
        unit = TWO, TWO, BLK, arrays[-1].shape[0]
        return [jax.ShapeDtypeStruct(arrays[TWO].shape, t) for t in (BF16, F32)] + [jax.ShapeDtypeStruct(unit, BF16)]

    spaces, out_spaces = [pl.ANY, pltpu.VMEM] + [pl.ANY] * FOUR, [pl.ANY] * THREE

    def step(self, t):
        def fetch_o(t, slot):
            return pltpu.make_async_copy(self.w_o.at[:, aligned(t)], self.buf_o.at[slot], self.w_sem.at[0, slot])

        def fetch_q(t, slot):
            return pltpu.make_async_copy(self.w_q.at[aligned(t)], self.buf_q.at[slot], self.w_sem.at[1, slot])

        def project(t, slot):
            at = aligned(t)
            attn = self.attn_home[...].reshape(-1, self.w_o.shape[0])
            out = jnp.dot(attn, self.buf_o[slot], preferred_element_type=F32)
            self.block_out[:, at] = (self.block_out[:, at].astype(F32) + out).astype(BF16)

        def pull(t, slot):
            dq = self.dq_home[...].reshape(-1, self.w_o.shape[0])
            self.d_part[:, aligned(t)] = dot_t(dq, self.buf_q[slot])

        if t in PRODUCTS_AT:
            i = PRODUCTS_AT.index(t)
            self.homes[i].wait_recv()
            if i == 0:
                self.residual.wait()
            tiled(self.w_o.shape[0] // BLK, *((fetch_o, project), (fetch_q, pull))[i])
            self.write(i).start()

    def write(self, i):
        src = (self.block_out, self.d_part)[i]
        return pltpu.make_async_copy(src, self.out_refs[i], self.w_sem.at[i, 0])

    def wq_terms(self, own, other):
        self.h_mine.wait()
        self.h_back.start()
        for c in self.h_copies:
            c.wait_recv()
        self.h_back.wait()
        core = lax.rem(lax.axis_index("cp"), TWO)
        d_out = self.dq[...].reshape(-1, self.dq.shape[-1])

        def fetch(t, slot):
            return pltpu.make_async_copy(self.h_u.at[:, :, :, aligned(t)], self.h_buf.at[slot], self.load_sem.at[slot])

        for out, half in ((other, 1 - core), (own, core)):

            def use(t, slot, out=out, half=half):
                h = self.h_buf[slot].reshape(-1, BLK)
                out[t - half * FOUR] = dot(h, d_out, (0,), (0,)).reshape(out.shape[1:])

            tiled(FOUR, fetch, use, half * FOUR)

    def finish(self):
        for c in self.h_copies + self.homes:
            c.wait_send()
        for i in range(TWO):
            self.write(i).wait()


class HiddenGradient:
    tiles = FOUR

    def __init__(self, me, dk, dv, ins, outs, scratch):
        self.part, w_k, w_v, self.x, self.dy, self.gain = ins
        self.dx, self.terms = outs
        self.dk_home, self.dv_home, self.rows, self.w_k, self.w_v, *rest = scratch
        self.part_tile, self.x_tile, self.dy_tile, self.dx_tile, self.tile_sem, *sems = rest
        pairs = (w_k, self.w_k), (w_v, self.w_v)
        self.weights = [pltpu.make_async_copy(src, dst, self.tile_sem.at[i]) for i, (src, dst) in enumerate(pairs)]
        for c in self.weights:
            c.start()
        pairs = (dk, self.dk_home), (dv, self.dv_home)
        self.homes = [Home(me, src, out, *[r.at[i] for r in sems]) for i, (src, out) in enumerate(pairs)]
        for h in self.homes:
            h.start()

    @staticmethod
    def scratch(x):
        dma = pltpu.SemaphoreType.DMA
        home = pltpu.VMEM((TWO,) * THREE + (CHUNK, TWO * HEAD_DIM), BF16)
        tile = TWO * CHUNK, x.shape[1]
        weight = pltpu.VMEM((x.shape[1], TWO * HEAD_DIM), BF16)
        tiles = [pltpu.VMEM(tile, F32)] + [pltpu.VMEM(tile, BF16)] * THREE
        sems = [dma((FOUR,)), dma((TWO,)), dma((TWO, FOUR)), dma((TWO, FOUR))]
        return [home, home, pltpu.VMEM((8, x.shape[1]), F32), weight, weight] + tiles + sems

    def tile(self, t):
        if t == 0:
            for c in self.weights:
                c.wait()
            for h in self.homes:
                h.wait_recv()
            self.rows[...] = jnp.zeros_like(self.rows)
        size = TWO * CHUNK
        at = pl.ds(t * size, size)
        pairs = (self.part, self.part_tile), (self.x, self.x_tile), (self.dy, self.dy_tile)
        loads = [pltpu.make_async_copy(src.at[at], dst, self.tile_sem.at[i]) for i, (src, dst) in enumerate(pairs)]
        for c in loads:
            c.start()
        for c in loads:
            c.wait()
        d = self.part_tile[...]
        for home, w in ((self.dk_home, self.w_k), (self.dv_home, self.w_v)):
            d += dot_t(home[t // TWO, t % TWO].reshape(size, -1), w[...])
        d = d.astype(BF16).astype(F32)
        x = self.x_tile[...].astype(F32)
        inv_rms = lax.rsqrt(row_mean(x * x) + NORM_EPS)
        unit, scaled = x * inv_rms, d * self.gain[...]
        dx = inv_rms * (scaled - unit * row_mean(scaled * unit))
        self.dx_tile[...] = (self.dy_tile[...].astype(F32) + dx).astype(BF16)
        store = pltpu.make_async_copy(self.dx_tile, self.dx.at[at], self.tile_sem.at[THREE])
        store.start()
        self.rows[...] += jnp.sum((d * unit).reshape((-1,) + self.rows.shape), axis=0)
        store.wait()
        if t == self.tiles - 1:
            self.terms[...] = jnp.sum(self.rows[...], axis=0, keepdims=True)

    def finish(self):
        for h in self.homes:
            h.wait_send()


def reduce_pairs(arrays, blocks, cuts, kinds, collective_id, work, more):
    vmem, hbm = pl.BlockSpec(memory_space=pltpu.VMEM), pl.BlockSpec(memory_space=pl.ANY)
    n = len(blocks)
    scratch = [pltpu.VMEM((FOUR, TWO) + blocks[-1], F32)]
    scratch += sum((PairSum.scratch(k, b) for k, b in zip(kinds, blocks)), []) + PairSum.sems(n, max(cuts))
    outs = [jax.ShapeDtypeStruct(b, F32) for b in blocks] + work.results(more)
    return pl.pallas_call(
        functools.partial(reduce_kernel, cuts, kinds, work),
        name="reduce_pairs",
        out_shape=outs,
        in_specs=[hbm] * len(arrays) + [pl.BlockSpec(memory_space=m) for m in work.spaces],
        out_specs=[vmem] * n + [pl.BlockSpec(memory_space=m) for m in work.out_spaces],
        scratch_shapes=scratch + work.scratch(more),
        compiler_params=params(63, collective_id=collective_id),
        cost_estimate=cost(1, 20),
    )(*arrays, *more)


HERE = 0, 0, 0
LINKS = "xyud"
ORDERS = "zxy", "zyx", "yxz", "zyx"
CUTS = 0, 48, 96, 128
SIZES = 8.4, 8.4, 5.6, 2.8
GAIN_AT = [60.0 + 12.0 * i for i in range(5)]
LATENCY, TILES_FROM, TILE_EVERY = 3.0, 14.0, 8.0
SUM_AT = [25.0 + 6.0 * i for i in range(4)]


def onward(order, key):
    dz, ry, rx = key
    stage = max((order.index(a) for a, r in zip("zyx", key) if r), default=-1)
    for axis in order[stage + 1 :]:
        if axis == "x":
            yield "x", (dz, ry, 1)
        elif axis == "y":
            yield "y", (dz, 1, rx)
        else:
            yield "u", (-1, ry, rx)
            yield "d", (1, ry, rx)
    if stage >= 0 and order[stage] == "z" and abs(dz) < THREE:
        yield ("u", (dz - 1, ry, rx)) if dz < 0 else ("d", (dz + 1, ry, rx))


def arrivals():
    busy, times = {}, {}
    starts = [0.0] * THREE + [SUM_AT[-1] + LATENCY]
    here = [(t, z, part, HERE) for part, t in enumerate(starts) for z in range(FOUR)]
    while here:
        now, z, part, key = heapq.heappop(here)
        times.setdefault((part, key), []).append(now)
        for link, there in onward(ORDERS[part], key):
            to = z + {"u": 1, "d": -1}.get(link, 0)
            if 0 <= to <= THREE:
                busy[z, link] = max(busy.get((z, link), 0), now) + SIZES[part]
                heapq.heappush(here, (busy[z, link] + LATENCY, to, part, there))
    return sorted((sum(t) / len(t), *at) for at, t in times.items())


def turn_back(dkv_ref, cos_ref, sin_ref, dk_u, dv_u):
    n = TWO * TWO * BLK
    for i in range(TWO):
        for j in range(TWO):
            cos_t, sin_t = (jnp.hstack([t, t * sign]) for t, sign in ((cos_ref[i, j].T, 1), (sin_ref[i, j].T, -1)))
            dk = dkv_ref[pl.ds((i * TWO + j) * BLK, BLK)] * ATTN_SCALE
            dk_u[i, j] = (dk * cos_t + pltpu.roll(dk, HEAD_DIM // TWO, 1) * sin_t).astype(BF16)
    dv_u[...] = dkv_ref[pl.ds(n, n)].astype(BF16).reshape(dv_u.shape)


def wkv_terms(h_ref, h_buf, sem, dk_u, dv_u, outs):
    d_out = jnp.hstack([r[...].reshape(-1, HEAD_DIM) for r in (dk_u, dv_u)])

    def fetch(t, slot):
        return pltpu.make_async_copy(h_ref.at[:, :, :, aligned(t)], h_buf.at[slot], sem.at[slot])

    for out, half in outs:

        def use(t, slot, out=out, half=half):
            h = h_buf[slot].reshape(-1, BLK)
            out[t - half * FOUR] = dot(h, d_out, (0,), (0,)).reshape(out.shape[1:])

        tiled(FOUR, fetch, use, half * FOUR)


def gather_kernel(*refs):
    take = taker(refs)
    wo_ref, wq_ref, dkv_ref, cos_ref, sin_ref, h_ref = take(6)
    grad_ins, outs, (dx_ref, dgain_ref) = take(6), take(FOUR), take(TWO)
    own_sem, send_sem, come_sem, core_sem, put_sem, all_terms, totals, g_s, g_r = take(9)
    terms, wkv_ref, h_buf, h_sem, dk_u, dv_u, store, wkv_store = take(8)
    buffers, sems, refs = take(FOUR), take(7), take(len(refs))
    me = lax.axis_index("cp")
    z, y, x, core = place(me)
    line = Line(me)
    to = {"x": dev(z, y, 1 - x, core), "y": dev(z, 1 - y, x, core), "u": line.next[1], "d": line.next[-1]}
    partner = dev(z, y, x, 1 - core)
    all_here = announce(quad_of(me)[1:] + [to["y"]] + [dev(zz, y, x, core) for _, zz in z_peers(z)])
    chip_here = me // TWO
    n_wo, wide = wo_ref.shape[0], wq_ref.shape[1]
    store[chip_here, pl.ds(0, n_wo)] = wo_ref[...]
    for i in range(TWO):
        store[chip_here, pl.ds(n_wo, n_wo), pl.ds(i * wide, wide)] = wq_ref[pl.ds(i * n_wo, n_wo)]
    turn_back(dkv_ref, cos_ref, sin_ref, dk_u, dv_u)
    all_here()
    wkv = PairSum(me, "core", 1, wkv_ref, wkv_store.at[chip_here], buffers, [r.at[0] for r in sems])

    def place_of(key):
        dz, ry, rx = key
        return z + dz, 1 - y if ry else y, 1 - x if rx else x

    def block(part, key):
        zz, yy, xx = place_of(key)
        chip = (TWO * zz + yy) * TWO + xx
        return wkv_store.at[chip] if part == THREE else store.at[chip, pl.ds(CUTS[part], CUTS[part + 1] - CUTS[part])]

    def windows(part, key):
        zz, yy, xx = place_of(key)
        pair, src = TWO * zz + yy, block(part, key)
        wo_at, wq_at = ((xx * TWO + core) * N_PAIRS + pair) * n_wo, (core * N_PAIRS + pair) * wq_ref.shape[0]
        if part == THREE:
            for i, out in enumerate(outs[TWO:]):
                yield src.at[:, head(i)], out.at[pl.ds(wq_at, wq_ref.shape[0]), pl.ds(xx * HEAD_DIM, HEAD_DIM)]
            return
        first, last = CUTS[part : part + TWO]
        if first < n_wo:
            rows = min(last, n_wo) - first
            yield src.at[pl.ds(0, rows)], outs[0].at[pl.ds(wo_at + first, rows)]
        if last > n_wo:
            skip = max(n_wo - first, 0)
            rows, at = last - first - skip, first + skip - n_wo
            for i in range(TWO):
                window = outs[1].at[pl.ds(wq_at + i * n_wo + at, rows), pl.ds(xx * wide, wide)]
                yield src.at[pl.ds(skip, rows), pl.ds(i * wide, wide)], window

    def index(part, key):
        return (part, key[0] + THREE) + key[1:]

    def send(part, key, link, there):
        sent = send_sem.at[index(part, key) + (LINKS.find(link or "-") + 1,)]
        if link:
            remote(block(part, key), block(part, key), sent, come_sem.at[index(part, there)], to[link]).start()
            return
        for src, window in windows(part, key):
            remote(src, window, sent, core_sem.at[index(part, key)], partner).start()
            pltpu.make_async_copy(src, window, put_sem.at[index(part, key)]).start()

    def whole(part, send, arrive):
        size = CUTS[part + 1] - CUTS[part] if part < THREE else wkv_store.size // store.shape[0] // outs[0].shape[1]
        dst = outs[0].at[pl.ds(0, size)]
        return remote(dst, dst, send, arrive, me)

    def when(on, do):
        pl.when(on)(do)

    def each_way(part, key):
        held = line.held(key[0])
        yield None, key, held
        for link, there in onward(ORDERS[part], key):
            inside = {"u": line.inside[1], "d": line.inside[-1]}.get(link)
            yield link, there, held if inside is None else jnp.logical_and(held, inside)

    def pass_on(part, key):
        for link, there, on in each_way(part, key):
            when(on, functools.partial(send, part, key, link, there))

    def term_copy(i):
        src = terms if i == 0 else totals.at[i - 1]
        return remote(src, all_terms.at[i], g_s.at[i], g_r.at[i], me ^ (1 << i))

    def add_terms(i):
        term_copy(i).wait_recv()
        totals[i] = (terms[...] if i == 0 else totals[i - 1]) + all_terms[i]
        if i + 1 < len(GAIN_AT):
            term_copy(i + 1).start()

    def tile(t):
        job.tile(t)
        if t == job.tiles - 1:
            term_copy(0).start()

    def sum_step(h):
        wkv.step(0, h)

    steps = [(TILES_FROM + t * TILE_EVERY, functools.partial(tile, t)) for t in range(HiddenGradient.tiles)]
    steps += [(at, functools.partial(sum_step, h)) for h, at in enumerate(SUM_AT)]
    steps += [(at, functools.partial(add_terms, i)) for i, at in enumerate(GAIN_AT)]
    steps.sort(key=lambda s: s[0])
    events = arrivals()
    for part in range(THREE):
        pass_on(part, HERE)
    job = HiddenGradient(me, dk_u, dv_u, grad_ins, (dx_ref, terms), refs)
    wkv_terms(h_ref, h_buf, h_sem, dk_u, dv_u, ((wkv_ref, 1 - core), (buffers[0], core)))
    wkv.begin(0)
    wkv.loaded(0)
    for now, part, key in events:
        while steps and steps[0][0] <= now:
            steps.pop(0)[1]()
        if any(key):
            arrive = come_sem.at[index(part, key)]
            when(line.held(key[0]), whole(part, own_sem.at[0], arrive).wait_recv)
            pass_on(part, key)
        elif part == THREE:
            pass_on(part, key)
    dgain_ref[...] = totals[len(GAIN_AT) - 1]
    for i in range(len(GAIN_AT)):
        term_copy(i).wait_send()
    for _, part, key in events:
        for sem in (core_sem, put_sem):
            when(line.held(key[0]), whole(part, own_sem.at[0], sem.at[index(part, key)]).wait_recv)
        for link, there, on in each_way(part, key):
            sent = send_sem.at[index(part, key) + (LINKS.find(link or "-") + 1,)]
            when(on, whole(part, sent, own_sem.at[0]).wait_send)
    wkv.wait_send(0)
    job.finish()


def gather_all(wo, wq, dkv, cos_f, sin_f, h_u, part, w_k, w_v, x, dy, gain, shapes):
    dma = pltpu.SemaphoreType.DMA
    vmem, hbm = pl.BlockSpec(memory_space=pltpu.VMEM), pl.BlockSpec(memory_space=pl.ANY)
    block = w_k.shape[0] // TWO // N_PAIRS, w_k.shape[1]
    parts = len(ORDERS)
    keys = (parts, 7, TWO, TWO)
    terms = 1, x.shape[1]
    scratch = [dma((1,)), dma(keys + (len(LINKS) + 1,)), dma(keys), dma(keys), dma(keys)]
    n = len(GAIN_AT)
    scratch += [pltpu.VMEM((n,) + terms, F32)] * TWO + [dma((n,)), dma((n,)), pltpu.VMEM(terms, F32)]
    scratch += [pltpu.VMEM((FOUR, TWO) + block, F32), pltpu.VMEM((TWO, TWO, TWO, BLK, BLK), BF16), dma((TWO,))]
    scratch += [pltpu.VMEM((TWO, TWO, BLK, HEAD_DIM), BF16)] * TWO
    scratch += [pltpu.VMEM((TWO * N_PAIRS,) + b, F32) for b in ((TWO * wo.shape[0], wo.shape[1]), block)]
    return pl.pallas_call(
        gather_kernel,
        name="gather_all",
        out_shape=[jax.ShapeDtypeStruct(s, F32) for s in shapes]
        + [jax.ShapeDtypeStruct(x.shape, BF16), jax.ShapeDtypeStruct(terms, F32)],
        in_specs=[vmem] * 5 + [hbm] * 6 + [vmem],
        out_specs=[hbm] * (len(shapes) + 1) + [vmem],
        scratch_shapes=scratch + PairSum.scratch("core", block) + PairSum.sems(1, 1) + HiddenGradient.scratch(x),
        compiler_params=params(63, collective_id=0),
        cost_estimate=cost(1, 76),
    )(wo, wq, dkv, cos_f, sin_f, h_u, part, w_k, w_v, x, dy, gain)


def perm(x, pairs):
    return lax.ppermute(x, "cp", pairs)


def flip_pairs(d):
    return [(r, r ^ d) for r in range(32)]


def solution(mesh):
    def local_step(hidden, grad_out, positions, seg_ids, w_q, w_k, w_v, w_o, norm_gain):
        n_batch, n_tok, d_model = hidden.shape
        n_rows = n_batch * n_tok
        wide = N_HEADS * HEAD_DIM
        me = lax.axis_index("cp")
        z, y, x, core = place(me)
        quad, pair = me % FOUR, me // FOUR
        relations = range(FOUR)

        def swap(pieces):
            return [perm(p, flip_pairs(d)) if d else p for d, p in enumerate(pieces)]

        gain = norm_gain.astype(F32)
        cos_t, sin_t = rope_tables(positions.reshape(n_rows))
        cos_f, sin_f = jnp.hstack([cos_t, cos_t]), jnp.hstack([-sin_t, sin_t])
        dy_flat = grad_out.reshape(n_rows, d_model)
        normed, kv_home = project(hidden.reshape(n_rows, d_model), gain[NEW], w_k, w_v, cos_f, sin_f)
        pos = positions.reshape(TWO, TWO, n_tok)
        kv_home = kv_home.reshape((TWO,) * 5 + (CHUNK, HEAD_DIM))
        kv_all, q_u, do_u, pos_u, *dy_rows = exchange(kv_home, normed, dy_flat, pos, cos_f, sin_f, w_q, w_o)
        pos_u = pos_u.reshape((FOUR, TWO, TWO, CHUNK)).transpose(1, TWO, 0, THREE).reshape(TWO, TWO, BLK)
        dy_rows = [a.reshape(TWO, TWO, CHUNK, d_model) for a in dy_rows]
        dy_pieces = swap([dy_rows[d % TWO] for d in relations])

        member = quad ^ jnp.arange(FOUR)
        front, back = ((m[:, NEW] * CHUNK + jnp.arange(CHUNK)[NEW]).reshape(BLK) for m in (member, THREE - member))
        offsets = jnp.stack([front, back]).astype(jnp.int32)
        own_super = jnp.stack([pair, N_SUPER - 1 - pair]).astype(jnp.int32)
        q_index = own_super[:, NEW] * BLK + offsets
        start = q_index[NEW] - pos_u
        tab = jnp.concatenate(
            [own_super, (jnp.min(start, axis=-1) // BLK).reshape(-1), jnp.max(start, axis=-1).reshape(-1)]
        )
        start_r = start[:, :, NEW, :]
        index_r = q_index[:, NEW]
        cos_u, sin_u = rope_tables(pos_u)
        cos_ut, sin_ut = jnp.swapaxes(cos_u, TWO, THREE), jnp.swapaxes(sin_u, TWO, THREE)

        attn_u, lse, delta = flash_fwd(tab, q_u, do_u, kv_all, start_r, index_r)

        wo_keep, wo_away = wo_terms(attn_u, dy_pieces)
        wo_come = perm(wo_away, flip_pairs(FOUR))
        do_u, wo_keep = lax.optimization_barrier((do_u, wo_keep))
        dq_u, dkv = flash_bwd(tab, q_u, do_u, kv_all, lse, delta, start_r, index_r, cos_ut, sin_ut)

        x_flat = hidden.reshape(n_rows, d_model)
        wo_own, dkv_own, wq_own, block_out, d_part, h_u = reduce_pairs(
            [wo_keep, wo_come, dkv.reshape(FOUR, TWO, -1, HEAD_DIM)],
            [wo_keep.shape[1:], (dkv.size // N_PAIRS // HEAD_DIM, HEAD_DIM), (d_model // TWO // N_PAIRS, wide)],
            (TWO, 8, 8),
            ("z", "", "core"),
            TWO,
            Products,
            (attn_u, dq_u, x_flat, normed.reshape((TWO,) * THREE + (CHUNK, d_model)), w_o, w_q),
        )
        grad_wo, grad_wq, grad_wk, grad_wv, grad_x, d_gain = gather_all(
            wo_own,
            wq_own,
            dkv_own,
            cos_ut,
            sin_ut,
            h_u,
            d_part,
            w_k,
            w_v,
            x_flat,
            dy_flat,
            gain[NEW],
            [w_o.shape, w_q.shape, w_k.shape, w_v.shape],
        )
        block_out, grad_x = (a.reshape(hidden.shape) for a in (block_out, grad_x))
        return block_out, grad_x, grad_wq, grad_wk, grad_wv, grad_wo, d_gain.reshape(d_model)

    seq_spec = P(None, "cp", None)
    tok_spec = P(None, "cp")
    full_spec = P()
    return jax.shard_map(
        local_step,
        mesh=mesh,
        in_specs=(seq_spec, seq_spec, tok_spec, tok_spec, full_spec, full_spec, full_spec, full_spec, full_spec),
        out_specs=(seq_spec, seq_spec, full_spec, full_spec, full_spec, full_spec, full_spec),
        check_vma=False,
    )
```
